32 devices in a mesh: dp: 2 (over x), ty: 4 (over z), tx: 4 (over y, core).
Axes of the slice: x: 2, y: 2, z: 4, core: 2. Of those that a mesh axis runs over, the one named last changes fastest.
Arguments:
- hidden: bfloat16 [8192, 2048], P(('dp', 'ty'), 'tx'), parts along dimension 0
- positions: int32 [8192], P(('dp', 'tx')), parts along dimension 0
- g_ffn: bfloat16 [2048], P('tx')
- w_gate: bfloat16 [2048, 8192], P('tx', 'ty')
- w_up: bfloat16 [2048, 8192], P('tx', 'ty')
- w_down: bfloat16 [8192, 2048], P('ty', 'tx')
- g_attn: bfloat16 [2048], P('tx')
- w_q: bfloat16 [2048, 32, 64], P('tx', 'ty')
- w_kv: bfloat16 [2048, 16, 64], P('tx', 'ty')
- grad_h2: bfloat16 [8192, 2048], P(('dp', 'ty'), 'tx'), parts along dimension 0
- grad_q: bfloat16 [8192, 32, 64], P(('dp', 'tx'), 'ty'), parts along dimension 0
- grad_kv: bfloat16 [8192, 16, 64], P(('dp', 'tx'), 'ty'), parts along dimension 0
Outputs:
- output 1: bfloat16 [8192, 2048], P(('dp', 'ty'), 'tx'), parts along dimension 0
- output 2: bfloat16 [8192, 32, 64], P(('dp', 'tx'), 'ty'), parts along dimension 0
- output 3: bfloat16 [8192, 16, 64], P(('dp', 'tx'), 'ty'), parts along dimension 0
- output 4: bfloat16 [8192, 2048], P(('dp', 'ty'), 'tx'), parts along dimension 0
- output 5: float32 [4096], P(('dp', 'tx')), parts along dimension 0
- output 6: float32 [4096], P(('dp', 'tx')), parts along dimension 0
- output 7: float32 [4096, 8192], P(('dp', 'tx'), 'ty'), parts along dimension 0
- output 8: float32 [4096, 8192], P(('dp', 'tx'), 'ty'), parts along dimension 0
- output 9: float32 [16384, 2048], P(('dp', 'ty'), 'tx'), parts along dimension 0
- output 10: float32 [4096, 32, 64], P(('dp', 'tx'), 'ty'), parts along dimension 0
- output 11: float32 [4096, 16, 64], P(('dp', 'tx'), 'ty'), parts along dimension 0
There are 2 independent parts. The reference program is written for one: setup_inputs(seed, part) draws one part's arguments, and reference() takes and returns one part's arrays. A program takes and returns all parts, laid end to end along the dimension named above; an argument that names none is the same for every part.
All inputs are finite; a program needn't handle non-finite values.
Results may differ from the reference program's by a relative error of at most 0.02.
Values are sent between devices in bfloat16 or wider.
A program may use at most 1 GiB of HBM per device.

```python
import jax
import jax.numpy as jnp
from jax import lax

TOKENS = 4096
MODEL_DIM = 2048
FFN_DIM = 8192
NUM_HEADS = 32
KV_HEADS = 8
HEAD_DIM = 64
MAX_POS = 4096
KV_SLOTS = 2 * KV_HEADS
NORM_EPS = 1e-5
ROPE_BASE = 10000.0


def setup_inputs(seed: int = 0, part: int = 0) -> dict:
    part_keys = jax.random.split(jax.random.fold_in(jax.random.key(seed), part), 7)
    shared_keys = jax.random.split(jax.random.key(seed + 7919), 7)
    row_tilt = jax.random.uniform(part_keys[0], (TOKENS, 1), minval=-0.8, maxval=0.8)
    row_level = jax.random.uniform(part_keys[1], (TOKENS, 1), minval=-0.5, maxval=0.5)
    col_wave = jnp.cos(jnp.pi * (jnp.arange(MODEL_DIM, dtype=jnp.float32) + 0.5) / MODEL_DIM)
    hidden = jax.random.normal(part_keys[2], (TOKENS, MODEL_DIM)) * jnp.exp(row_tilt * col_wave[None, :] + row_level)
    positions = jax.random.randint(part_keys[3], (TOKENS,), 0, MAX_POS, dtype=jnp.int32)
    grad_h2 = jax.random.normal(part_keys[4], (TOKENS, MODEL_DIM))
    grad_q = jax.random.normal(part_keys[5], (TOKENS, NUM_HEADS, HEAD_DIM))
    grad_kv = jax.random.normal(part_keys[6], (TOKENS, KV_SLOTS, HEAD_DIM))
    g_ffn = 1.0 + 0.3 * jax.random.normal(shared_keys[0], (MODEL_DIM,))
    g_attn = 1.0 + 0.3 * jax.random.normal(shared_keys[1], (MODEL_DIM,))
    w_gate = jax.random.normal(shared_keys[2], (MODEL_DIM, FFN_DIM)) * MODEL_DIM ** -0.5
    w_up = jax.random.normal(shared_keys[3], (MODEL_DIM, FFN_DIM)) * MODEL_DIM ** -0.5
    w_down = jax.random.normal(shared_keys[4], (FFN_DIM, MODEL_DIM)) * FFN_DIM ** -0.5
    w_q = jax.random.normal(shared_keys[5], (MODEL_DIM, NUM_HEADS, HEAD_DIM)) * MODEL_DIM ** -0.5
    w_kv = jax.random.normal(shared_keys[6], (MODEL_DIM, KV_SLOTS, HEAD_DIM)) * MODEL_DIM ** -0.5
    return {
        "hidden": hidden.astype(jnp.bfloat16),
        "positions": positions,
        "g_ffn": g_ffn.astype(jnp.bfloat16),
        "w_gate": w_gate.astype(jnp.bfloat16),
        "w_up": w_up.astype(jnp.bfloat16),
        "w_down": w_down.astype(jnp.bfloat16),
        "g_attn": g_attn.astype(jnp.bfloat16),
        "w_q": w_q.astype(jnp.bfloat16),
        "w_kv": w_kv.astype(jnp.bfloat16),
        "grad_h2": grad_h2.astype(jnp.bfloat16),
        "grad_q": grad_q.astype(jnp.bfloat16),
        "grad_kv": grad_kv.astype(jnp.bfloat16),
    }


def rms_scale(values):
    return lax.rsqrt(jnp.mean(values * values, axis=-1, keepdims=True) + NORM_EPS)


def rms_backward(values, inv_rms, gain, grad_out):
    scaled = grad_out * gain.astype(jnp.float32)
    grad_gain = jnp.sum(grad_out * values * inv_rms, axis=0)
    inner_dot = jnp.mean(scaled * values, axis=-1, keepdims=True)
    grad_in = inv_rms * scaled - values * (inv_rms * inv_rms * inv_rms) * inner_dot
    return grad_gain, grad_in


def rope_tables(positions):
    inv_freq = ROPE_BASE ** (-jnp.arange(0, HEAD_DIM, 2, dtype=jnp.float32) / HEAD_DIM)
    angles = positions.astype(jnp.float32)[:, None] * inv_freq[None, :]
    return jnp.cos(angles)[:, None, :], jnp.sin(angles)[:, None, :]


def rotate(values, cos_h, sin_h):
    pair_view = values.reshape(values.shape[:-1] + (values.shape[-1] // 2, 2))
    even_part = pair_view[..., 0]
    odd_part = pair_view[..., 1]
    turned = jnp.stack([even_part * cos_h - odd_part * sin_h, even_part * sin_h + odd_part * cos_h], axis=-1)
    return turned.reshape(values.shape)


def reference(hidden, positions, g_ffn, w_gate, w_up, w_down, g_attn, w_q, w_kv, grad_h2, grad_q, grad_kv):
    hidden_wide = hidden.astype(jnp.float32)
    inv_ffn = rms_scale(hidden_wide)
    normed = (hidden_wide * inv_ffn * g_ffn.astype(jnp.float32)).astype(jnp.bfloat16)
    gate_pre = jnp.dot(normed, w_gate, preferred_element_type=jnp.float32).astype(jnp.bfloat16).astype(jnp.float32)
    up_pre = jnp.dot(normed, w_up, preferred_element_type=jnp.float32).astype(jnp.bfloat16).astype(jnp.float32)
    gate_sig = jax.nn.sigmoid(gate_pre)
    hidden_act = (gate_pre * gate_sig * up_pre).astype(jnp.bfloat16)
    mlp_out = jnp.dot(hidden_act, w_down, preferred_element_type=jnp.float32)
    resid = (hidden_wide + mlp_out).astype(jnp.bfloat16)
    resid_wide = resid.astype(jnp.float32)
    inv_attn = rms_scale(resid_wide)
    normed2 = (resid_wide * inv_attn * g_attn.astype(jnp.float32)).astype(jnp.bfloat16)
    cos_t, sin_t = rope_tables(positions)
    kv_flag = (jnp.arange(KV_SLOTS) < KV_HEADS).astype(jnp.float32)[None, :, None]
    cos_kv = kv_flag * cos_t + (1.0 - kv_flag)
    sin_kv = kv_flag * sin_t
    normed2_wide = normed2.astype(jnp.float32)
    q_proj = jnp.einsum("td,dhk->thk", normed2_wide, w_q.astype(jnp.float32))
    kv_proj = jnp.einsum("td,dhk->thk", normed2_wide, w_kv.astype(jnp.float32))
    q_out = rotate(q_proj, cos_t, sin_t).astype(jnp.bfloat16)
    kv_out = rotate(kv_proj, cos_kv, sin_kv).astype(jnp.bfloat16)
    back_q = rotate(grad_q.astype(jnp.float32), cos_t, -sin_t).astype(jnp.bfloat16).astype(jnp.float32)
    back_kv = rotate(grad_kv.astype(jnp.float32), cos_kv, -sin_kv).astype(jnp.bfloat16).astype(jnp.float32)
    grad_wq = jnp.einsum("td,thk->dhk", normed2_wide, back_q)
    grad_wkv = jnp.einsum("td,thk->dhk", normed2_wide, back_kv)
    grad_n2 = jnp.einsum("thk,dhk->td", back_q, w_q.astype(jnp.float32)) + jnp.einsum("thk,dhk->td", back_kv, w_kv.astype(jnp.float32))
    grad_gattn, grad_attn_in = rms_backward(resid_wide, inv_attn, g_attn, grad_n2)
    grad_res = grad_h2.astype(jnp.float32) + grad_attn_in
    res_half = grad_res.astype(jnp.bfloat16)
    grad_wdown = jnp.dot(hidden_act.T, res_half, preferred_element_type=jnp.float32)
    grad_act = jnp.dot(res_half, w_down.T, preferred_element_type=jnp.float32)
    grad_gate = (grad_act * up_pre * gate_sig * (1.0 + gate_pre * (1.0 - gate_sig))).astype(jnp.bfloat16)
    grad_up = (grad_act * gate_pre * gate_sig).astype(jnp.bfloat16)
    grad_wgate = jnp.dot(normed.T, grad_gate, preferred_element_type=jnp.float32)
    grad_wup = jnp.dot(normed.T, grad_up, preferred_element_type=jnp.float32)
    grad_n = jnp.dot(grad_gate, w_gate.T, preferred_element_type=jnp.float32) + jnp.dot(grad_up, w_up.T, preferred_element_type=jnp.float32)
    grad_gffn, grad_ffn_in = rms_backward(hidden_wide, inv_ffn, g_ffn, grad_n)
    grad_hidden = (grad_res + grad_ffn_in).astype(jnp.bfloat16)
    return (resid, q_out, kv_out, grad_hidden, grad_gffn, grad_gattn, grad_wgate, grad_wup, grad_wdown, grad_wq, grad_wkv)
```

```python
import jax
import jax.numpy as jnp
from jax import lax
from jax.sharding import PartitionSpec as P

NORM_EPS = 1e-5
ROPE_BASE = 10000.0
ROWS_ROWS = (((0,), (0,)), ((), ()))
COLS_COLS = (((1,), (1,)), ((), ()))
F32 = jnp.float32
BF16 = jnp.bfloat16


def rotate(values, cos_h, sin_h):
    pair_view = values.reshape(values.shape[:-1] + (values.shape[-1] // 2, 2))
    even_part = pair_view[..., 0]
    odd_part = pair_view[..., 1]
    turned = jnp.stack([even_part * cos_h - odd_part * sin_h, even_part * sin_h + odd_part * cos_h], axis=-1)
    return turned.reshape(values.shape)


def rope_tables(positions, head_dim):
    inv_freq = ROPE_BASE ** (-jnp.arange(0, head_dim, 2, dtype=F32) / head_dim)
    angles = positions.astype(F32)[:, None] * inv_freq[None, :]
    return jnp.cos(angles)[:, None, :], jnp.sin(angles)[:, None, :]


def dot(a, b, dims=(((1,), (0,)), ((), ()))):
    return lax.dot_general(a, b, dims, preferred_element_type=F32)


def norm_backward(values, inv_rms, gain, grad_out, model_dim):
    scaled = grad_out * gain
    grad_gain = jnp.sum(grad_out * values * inv_rms, axis=0)
    inner_dot = jnp.sum(scaled * values, axis=1, keepdims=True) / model_dim
    grad_in = inv_rms * scaled - values * (inv_rms * inv_rms * inv_rms) * inner_dot
    return grad_gain, grad_in


def solution(mesh):
    nz = mesh.shape["ty"]
    nt = mesh.shape["tx"]

    def xor_tx(x, k):
        return lax.ppermute(x, "tx", [(i, i ^ k) for i in range(nt)])

    def swap_dp(x):
        return lax.ppermute(x, "dp", [(0, 1), (1, 0)])

    def shift_z(x, pairs):
        return lax.ppermute(x, "ty", pairs)

    def local_step(hidden, positions, g_ffn, w_gate, w_up, w_down, g_attn, w_q, w_kv, grad_h2, grad_q, grad_kv):
        tx = lax.axis_index("tx")
        ty = lax.axis_index("ty")
        dp = lax.axis_index("dp")
        dt = hidden.shape[1]
        model_dim = dt * nt
        sub = hidden.shape[0] // nt
        head_dim = w_q.shape[2]
        kv_local = w_kv.shape[1]
        heads = w_q.shape[1] + kv_local
        width = heads * head_dim

        def to_rows(x):
            parts = x.reshape(nt, sub, dt)
            got = [parts[tx]]
            for k in range(1, nt):
                got.append(xor_tx(parts[tx ^ k], k))
            return jnp.concatenate(got, axis=1)

        def from_rows(x):
            out = jnp.zeros((nt, sub, dt), x.dtype)
            out = lax.dynamic_update_index_in_dim(out, x[:, :dt], tx, 0)
            for k in range(1, nt):
                piece = xor_tx(x[:, k * dt:(k + 1) * dt], k)
                out = lax.dynamic_update_index_in_dim(out, piece, tx ^ k, 0)
            return out.reshape(nt * sub, dt)

        def gather_w(w, axis):
            mate = xor_tx(w, 1)
            half = w.shape[0] // 2
            mine = lax.dynamic_slice_in_dim(w, dp * half, half, 0)
            near = xor_tx(mine, 2)
            far = swap_dp(near)
            other = jnp.where(dp == 0, jnp.concatenate([near, far], 0), jnp.concatenate([far, near], 0))
            diag = xor_tx(other, 1)
            return jnp.concatenate([w, mate, other, diag], axis=axis)

        def reduce_w(blocks):
            sent = xor_tx(jnp.concatenate([blocks[1], blocks[3]], 0).astype(BF16), 1)
            rows = blocks[0].shape[0]
            keep = blocks[0] + sent[:rows].astype(F32)
            cross = blocks[2] + sent[rows:].astype(F32)
            back = xor_tx(cross.astype(BF16), 2)
            return keep + back.astype(F32)

        def gather_z(block):
            right = [(0, 1), (1, 2), (2, 3)]
            left = [(1, 0), (2, 1), (3, 2)]
            r1 = shift_z(block, right)
            l1 = shift_z(block, left)
            r2 = shift_z(r1, right[1:])
            l2 = shift_z(l1, left[:-1])
            r3 = shift_z(r2, right[2:])
            l3 = shift_z(l2, left[:1])
            out = jnp.zeros((nz + 1,) + block.shape, block.dtype)
            out = lax.dynamic_update_index_in_dim(out, block, ty, 0)
            for step, (r, l) in enumerate(((r1, l1), (r2, l2), (r3, l3)), 1):
                out = lax.dynamic_update_index_in_dim(out, r, jnp.where(ty >= step, ty - step, nz), 0)
                out = lax.dynamic_update_index_in_dim(out, l, jnp.where(ty + step < nz, ty + step, nz), 0)
            return out[:nz].reshape((nz * block.shape[0],) + block.shape[1:])

        def scatter_z(part):
            blocks = part.reshape((nz, part.shape[0] // nz) + part.shape[1:])

            def pick(offset):
                return lax.dynamic_index_in_dim(blocks, jnp.clip(ty + offset, 0, nz - 1), 0, keepdims=False)

            r1 = shift_z(pick(3), [(0, 1)])
            l1 = shift_z(pick(-3), [(3, 2)])
            r2 = shift_z((pick(2).astype(F32) + r1.astype(F32)).astype(BF16), [(0, 1), (1, 2)])
            l2 = shift_z((pick(-2).astype(F32) + l1.astype(F32)).astype(BF16), [(3, 2), (2, 1)])
            r3 = shift_z((pick(1).astype(F32) + r2.astype(F32)).astype(BF16), [(0, 1), (1, 2), (2, 3)])
            l3 = shift_z((pick(-1).astype(F32) + l2.astype(F32)).astype(BF16), [(3, 2), (2, 1), (1, 0)])
            return pick(0).astype(F32) + r3.astype(F32) + l3.astype(F32)

        gains = lax.all_gather(jnp.stack([g_ffn, g_attn]).astype(F32), "tx")
        gains_rel = jnp.stack([gains[tx ^ k] for k in range(nt)], axis=1).reshape(2, model_dim)
        gain_ffn, gain_attn = gains_rel[0], gains_rel[1]

        rows = to_rows(hidden).astype(F32)
        inv_ffn = lax.rsqrt(jnp.sum(rows * rows, axis=1, keepdims=True) / model_dim + NORM_EPS)
        normed = (rows * inv_ffn * gain_ffn).astype(BF16)
        normed_all = gather_z(normed)

        cos_t, sin_t = rope_tables(positions, head_dim)
        kv_index = ty * kv_local + jnp.arange(kv_local)
        kv_flag = (kv_index < kv_local * nz // 2).astype(F32)[None, :, None]
        cos_kv = kv_flag * cos_t + (1.0 - kv_flag)
        sin_kv = kv_flag * sin_t
        back_q = rotate(grad_q.astype(F32), cos_t, -sin_t).astype(BF16)
        back_kv = rotate(grad_kv.astype(F32), cos_kv, -sin_kv).astype(BF16)
        back = jnp.concatenate([back_q, back_kv], axis=1).reshape(nt, sub, width)
        back_all = jnp.zeros((nt, sub, width), BF16)
        back_all = lax.dynamic_update_index_in_dim(back_all, back[tx], tx, 0)
        for k in range(1, nt):
            back_all = lax.dynamic_update_index_in_dim(back_all, xor_tx(back[tx ^ k], k), tx ^ k, 0)
        back_all = back_all.reshape(nt * sub, width)

        w_qkv = gather_w(jnp.concatenate([w_q, w_kv], axis=1).reshape(dt, width), 0)
        gate_w = gather_w(w_gate, 0)
        up_w = gather_w(w_up, 0)
        down_w = gather_w(w_down, 1)

        n2_part = dot(back_all, w_qkv, COLS_COLS).astype(BF16)
        grad_n2 = scatter_z(n2_part)

        gate_pre = dot(normed_all, gate_w).astype(BF16).astype(F32)
        up_pre = dot(normed_all, up_w).astype(BF16).astype(F32)
        gate_sig = jax.nn.sigmoid(gate_pre)
        hidden_act = (gate_pre * gate_sig * up_pre).astype(BF16)
        mlp_out = scatter_z(dot(hidden_act, down_w).astype(BF16))
        resid = (rows + mlp_out).astype(BF16)
        resid_out = from_rows(resid)
        resid_wide = resid.astype(F32)
        inv_attn = lax.rsqrt(jnp.sum(resid_wide * resid_wide, axis=1, keepdims=True) / model_dim + NORM_EPS)
        normed2 = (resid_wide * inv_attn * gain_attn).astype(BF16)

        gattn, grad_attn_in = norm_backward(resid_wide, inv_attn, gain_attn, grad_n2, model_dim)
        grad_res = to_rows(grad_h2).astype(F32) + grad_attn_in
        res_all = gather_z(grad_res.astype(BF16))
        grad_act = dot(res_all, down_w, COLS_COLS)
        grad_gate = (grad_act * up_pre * gate_sig * (1.0 + gate_pre * (1.0 - gate_sig))).astype(BF16)
        grad_up = (grad_act * gate_pre * gate_sig).astype(BF16)
        n_part = (dot(grad_gate, gate_w, COLS_COLS) + dot(grad_up, up_w, COLS_COLS)).astype(BF16)
        grad_n = scatter_z(n_part)
        normed2_all = gather_z(normed2)

        wd = dot(hidden_act, res_all, ROWS_ROWS)
        grad_wdown = reduce_w([wd[:, k * dt:(k + 1) * dt] for k in range(nt)])
        wg = dot(normed_all, grad_gate, ROWS_ROWS)
        grad_wgate = reduce_w([wg[k * dt:(k + 1) * dt] for k in range(nt)])
        wu = dot(normed_all, grad_up, ROWS_ROWS)
        grad_wup = reduce_w([wu[k * dt:(k + 1) * dt] for k in range(nt)])

        qkv = dot(normed2_all, w_qkv).astype(BF16).reshape(nz, sub, width)
        qkv_home = jnp.zeros((nt, sub, width), BF16)
        qkv_home = lax.dynamic_update_index_in_dim(qkv_home, qkv[tx], tx, 0)
        for k in range(1, nt):
            qkv_home = lax.dynamic_update_index_in_dim(qkv_home, xor_tx(qkv[tx ^ k], k), tx ^ k, 0)
        qkv_home = qkv_home.reshape(nt * sub, heads, head_dim).astype(F32)
        q_out = rotate(qkv_home[:, :heads - kv_local], cos_t, sin_t).astype(BF16)
        kv_out = rotate(qkv_home[:, heads - kv_local:], cos_kv, sin_kv).astype(BF16)
        wqkv_g = dot(normed2_all, back_all, ROWS_ROWS)
        grad_wqkv = reduce_w([wqkv_g[k * dt:(k + 1) * dt] for k in range(nt)]).reshape(dt, heads, head_dim)
        grad_wq = grad_wqkv[:, :heads - kv_local]
        grad_wkv = grad_wqkv[:, heads - kv_local:]

        gffn, grad_ffn_in = norm_backward(rows, inv_ffn, gain_ffn, grad_n, model_dim)
        grad_hidden = from_rows((grad_res + grad_ffn_in).astype(BF16))

        both = jnp.stack([gffn, gattn]).reshape(2, nt, dt)
        spread = jnp.zeros((2, nt, dt), F32)
        for k in range(nt):
            spread = lax.dynamic_update_index_in_dim(spread, both[:, k], tx ^ k, 1)
        total = lax.psum(spread, ("ty", "tx"))
        grad_gffn, grad_gattn = total[0, tx], total[1, tx]
        return (resid_out, q_out, kv_out, grad_hidden, grad_gffn, grad_gattn, grad_wgate, grad_wup, grad_wdown, grad_wq, grad_wkv)

    row_spec = P(("dp", "ty"), "tx")
    head_spec = P(("dp", "tx"), "ty", None)
    in_specs = (row_spec, P(("dp", "tx")), P("tx"), P("tx", "ty"), P("tx", "ty"), P("ty", "tx"), P("tx"), P("tx", "ty", None), P("tx", "ty", None), row_spec, head_spec, head_spec)
    out_specs = (row_spec, head_spec, head_spec, row_spec, P(("dp", "tx")), P(("dp", "tx")), P(("dp", "tx"), "ty"), P(("dp", "tx"), "ty"), P(("dp", "ty"), "tx"), head_spec, head_spec)
    return jax.shard_map(local_step, mesh=mesh, in_specs=in_specs, out_specs=out_specs, check_vma=False)
```

```python
import jax
import jax.numpy as jnp
from jax import lax
from jax.experimental import pallas as pl
from jax.experimental.pallas import tpu as pltpu
from jax.sharding import PartitionSpec as P

NORM_EPS = 1e-5
ROPE_BASE = 10000.0
ROWS_ROWS = (((0,), (0,)), ((), ()))
COLS_COLS = (((1,), (1,)), ((), ()))
F32 = jnp.float32
BF16 = jnp.bfloat16


def rotate(values, cos_h, sin_h):
    pair_view = values.reshape(values.shape[:-1] + (values.shape[-1] // 2, 2))
    even_part = pair_view[..., 0]
    odd_part = pair_view[..., 1]
    turned = jnp.stack([even_part * cos_h - odd_part * sin_h, even_part * sin_h + odd_part * cos_h], axis=-1)
    return turned.reshape(values.shape)


def rope_tables(positions, head_dim):
    inv_freq = ROPE_BASE ** (-jnp.arange(0, head_dim, 2, dtype=F32) / head_dim)
    angles = positions.astype(F32)[:, None] * inv_freq[None, :]
    return jnp.cos(angles)[:, None, :], jnp.sin(angles)[:, None, :]


def dot(a, b, dims=(((1,), (0,)), ((), ()))):
    return lax.dot_general(a, b, dims, preferred_element_type=F32)


def norm_backward(values, inv_rms, gain, grad_out, model_dim):
    scaled = grad_out * gain
    grad_gain = jnp.sum(grad_out * values * inv_rms, axis=0)
    inner_dot = jnp.sum(scaled * values, axis=1, keepdims=True) / model_dim
    grad_in = inv_rms * scaled - values * (inv_rms * inv_rms * inv_rms) * inner_dot
    return grad_gain, grad_in


MESH = pl.DeviceIdType.MESH
ANY = pl.BlockSpec(memory_space=pl.ANY)
VMEM = pltpu.VMEM
NT_DIMS = (((1,), (1,)), ((), ()))
VMEM_LIMIT = 67000000


def ds(start, size, align=None):
    if isinstance(start, int):
        return pl.ds(start, size)
    return pl.ds(pl.multiple_of(start, align or size), size)


def mid(z):
    return jnp.logical_and(z > 0, z < 3)


def end(z):
    return jnp.logical_or(z == 0, z == 3)


def slots(z):
    return (z + 1 - 2 * (z % 2), 2 - z // 2, 3 - 3 * (z // 2))


class Wires:
    def __init__(self, send, recv, local):
        self.send, self.recv, self.local = send, recv, local
        self.n_remote = 0
        self.n_local = 0

    def take(self, n=1):
        base = self.n_remote
        self.n_remote += n
        return base

    def copy(self, src, dst, si, ri, **dev):
        return pltpu.make_async_remote_copy(
            src_ref=src, dst_ref=dst, send_sem=self.send.at[si], recv_sem=self.recv.at[ri],
            device_id=dev, device_id_type=MESH)

    def here(self, src, dst):
        i = self.n_local
        self.n_local += 1
        c = pltpu.make_async_copy(src, dst, self.local.at[i])
        c.start()
        return c


def entry_barrier(axes, z):
    sem = pltpu.get_barrier_semaphore()
    for dev in axes:
        pl.semaphore_signal(sem, inc=1, device_id=dev, device_id_type=MESH)

    @pl.when(z > 0)
    def _():
        pl.semaphore_signal(sem, inc=1, device_id={"ty": z - 1}, device_id_type=MESH)

    @pl.when(z < 3)
    def _():
        pl.semaphore_signal(sem, inc=1, device_id={"ty": z + 1}, device_id_type=MESH)

    @pl.when(mid(z))
    def _():
        pl.semaphore_wait(sem, len(axes) + 2)

    @pl.when(end(z))
    def _():
        pl.semaphore_wait(sem, len(axes) + 1)


class LineGather:
    def __init__(self, net, buf, rows, z):
        self.net, self.buf, self.rows, self.z = net, buf, rows, z
        self.base = net.take(8)
        self.slots = slots(z)

    def blk(self, b):
        return self.buf.at[ds(b * self.rows, self.rows), :]

    def cp(self, b, side, target):
        return self.net.copy(self.blk(b), self.blk(b), self.base + side * 4 + b, self.base + b, ty=target)

    def start(self):
        z = self.z

        @pl.when(z < 3)
        def _():
            self.cp(z, 0, z + 1).start()

        @pl.when(z > 0)
        def _():
            self.cp(z, 1, z - 1).start()

    def take(self, i):
        b = self.slots[i]
        self.cp(b, 0, self.z).wait_recv()

    def forward(self, i):
        z, b = self.z, self.slots[i]
        target = 3 - z if i == 0 else 3 * (z - 1)
        self.cp(b, 0, target).start()

    def step1(self):
        self.take(0)

        @pl.when(mid(self.z))
        def _():
            self.forward(0)
            self.take(1)
            self.forward(1)

    def step2(self):
        @pl.when(end(self.z))
        def _():
            self.take(1)

    def step3(self):
        self.take(2)

        @pl.when(mid(self.z))
        def _():
            self.forward(2)

    def drain(self):
        z = self.z

        @pl.when(z < 3)
        def _():
            self.cp(z, 0, z + 1).wait_send()

        @pl.when(z > 0)
        def _():
            self.cp(z, 1, z - 1).wait_send()

        @pl.when(mid(z))
        def _():
            for i in range(3):
                self.cp(self.slots[i], 0, 3 - z if i == 0 else 3 * (z - 1)).wait_send()


class LineScatter:
    def __init__(self, net, part, rbuf, rows, z):
        self.net, self.part, self.rbuf, self.rows, self.z = net, part, rbuf, rows, z
        self.base = net.take(5)
        self.slots = slots(z)
        one = (z % 2) * (1 - z // 2)
        self.dst = (self.slots[0] + (1 - z % 2) * (3 - z), self.slots[1] + 2 * one, self.slots[2])
        self.target = (z + 1 - 2 * (z % 2), 1 + z % 2, 1 + z % 2)

    def cp(self, i):
        return self.net.copy(
            self.part.at[ds(self.slots[i] * self.rows, self.rows), :], self.rbuf.at[ds(self.dst[i] * self.rows, self.rows), :],
            self.base + i, self.base + self.dst[i], ty=self.target[i])

    def wait_slot(self, s):
        view = self.rbuf.at[ds(s * self.rows, self.rows), :]
        self.net.copy(view, view, self.base, self.base + s, ty=self.z).wait_recv()

    def send_end(self, i):
        @pl.when(end(self.z))
        def _():
            self.cp(i).start()

    def send_mid(self, i):
        @pl.when(mid(self.z))
        def _():
            b = self.slots[i]
            self.wait_slot(b)
            step = min(32, self.rows)

            @pl.loop(0, self.rows // step)
            def _(r):
                view = ds(b * self.rows + r * step, step, step)
                self.part[view, :] = (self.part[view, :].astype(F32) + self.rbuf[view, :].astype(F32)).astype(BF16)

            self.cp(i).start()

    def finish(self):
        z = self.z

        @pl.when(z < 3)
        def _():
            self.wait_slot(z)

        @pl.when(z > 0)
        def _():
            self.wait_slot(4)

    def drain(self):
        for i in range(3):
            self.cp(i).wait_send()


class WeightGather:
    def __init__(self, net, w, full, pos, by_rows, chunks):
        self.net, self.w, self.full, self.by_rows = net, w, full, by_rows
        self.dp, self.t1, self.t2 = pos
        self.len = w.shape[0]
        self.width = w.shape[0] if by_rows else w.shape[1]
        self.chunks = chunks
        self.piece = self.len // 2 // chunks
        self.base = net.take(1 + 4 * chunks)

    def dst(self, k, off, n):
        if self.by_rows:
            return self.full.at[ds(k * self.width + off, n, min(n, 16)), :]
        return self.full.at[ds(off, n, 16), pl.ds(k * self.width, self.width)]

    def off(self, half, ch):
        return half * (self.len // 2) + ch * self.piece

    def near(self, ch):
        o = self.off(self.dp, ch)
        i = self.base + 1 + ch
        return self.net.copy(self.w.at[ds(o, self.piece, 16), :], self.dst(2, o, self.piece), i, i, tx=self.t2)

    def cross(self, ch, half):
        o = self.off(half, ch)
        i = self.base + 1 + self.chunks + ch
        return self.net.copy(self.dst(2, o, self.piece), self.dst(2, o, self.piece), i, i, dp=1 - self.dp)

    def diag(self, ch, which, half):
        o = self.off(half, ch)
        i = self.base + 1 + (2 + which) * self.chunks + ch
        return self.net.copy(self.dst(2, o, self.piece), self.dst(3, o, self.piece), i, i, tx=self.t1)

    def mate(self):
        return self.net.copy(self.w, self.dst(1, 0, self.len), self.base, self.base, tx=self.t1)

    def start_y(self):
        for ch in range(self.chunks):
            self.near(ch).start()

    def start_local(self):
        self.own = self.net.here(self.w, self.dst(0, 0, self.len))
        self.mate().start()

    def y_event(self, ch):
        self.near(ch).wait_recv()
        self.cross(ch, self.dp).start()
        self.diag(ch, 0, self.dp).start()

    def x_event(self, ch):
        self.cross(ch, 1 - self.dp).wait_recv()
        self.diag(ch, 1, 1 - self.dp).start()

    def finish(self):
        self.own.wait()
        self.mate().wait_recv()
        for ch in range(self.chunks):
            self.diag(ch, 0, self.dp).wait_recv()
            self.diag(ch, 1, 1 - self.dp).wait_recv()

    def drain(self):
        self.mate().wait_send()
        for ch in range(self.chunks):
            self.near(ch).wait_send()
            self.cross(ch, self.dp).wait_send()
            self.diag(ch, 0, self.dp).wait_send()
            self.diag(ch, 1, 1 - self.dp).wait_send()


def places():
    dp, z, tx = lax.axis_index("dp"), lax.axis_index("ty"), lax.axis_index("tx")
    return dp, z, tx, (tx, tx + 1 - 2 * (tx % 2), (tx + 2) % 4, 3 - tx)


def kernel_a(hid, eqh, dh2h, wg, wu, wd, wq, gin,
             n_o, a_o, b_o, u_o, wg_o, wu_o, wd_o, wq_o, eq_o, h_o, dh2_o, dn2_o, g_o,
             rows, n_v, a_v, b_v, u_v, wg_v, wu_v, wq_v, eq_v, p_v, rbuf, gains, dn2_v, send, recv, local):
    dp, z, tx, peer = places()
    sub, dim = rows.shape
    dt = dim // 4
    ff = wg.shape[1]
    tile = min(512, ff)
    dtile = min(512, dim)
    net = Wires(send, recv, local)
    entry_barrier([{"tx": peer[1]}, {"tx": peer[2]}, {"tx": peer[3]}, {"dp": 1 - dp}], z)

    pos = (dp, peer[1], peer[2])
    far_first = (2, 3, 1)
    g_id, h_id, e_id, d_id = net.take(4), net.take(4), net.take(4), net.take(4)

    def g_cp(k):
        return net.copy(gin, gains.at[:, pl.ds(k * dt, dt)], g_id + k, g_id + k, tx=peer[k])

    def h_cp(k):
        return net.copy(hid.at[ds(peer[k] * sub, sub), :], rows.at[:, pl.ds(k * dt, dt)], h_id + k, h_id + k, tx=peer[k])

    def e_cp(k, block):
        return net.copy(eqh.at[ds(peer[k] * sub, sub), :], eq_v.at[ds(block * sub, sub), :], e_id + k, e_id + k, tx=peer[k])

    def d_cp(k):
        return net.copy(dh2h.at[ds(peer[k] * sub, sub), :], dh2_o.at[:, pl.ds(k * dt, dt)], d_id + k, d_id + k, tx=peer[k])

    gate = WeightGather(net, wg, wg_v, pos, True, 2)
    up = WeightGather(net, wu, wu_v, pos, True, 2)
    down = WeightGather(net, wd, wd_o, pos, False, 2)
    qkv = WeightGather(net, wq, wq_v, pos, True, 1)
    ag = LineGather(net, n_v, sub, z)
    rsc = LineScatter(net, p_v, rbuf, sub, z)

    for k in far_first:
        g_cp(k).start()
    for k in far_first:
        h_cp(k).start()
    g_own = net.here(gin, gains.at[:, pl.ds(0, dt)])
    h_own = net.here(hid.at[ds(tx * sub, sub), :], rows.at[:, pl.ds(0, dt)])
    for k in far_first:
        e_cp(k, tx).start()
    e_own = net.here(eqh.at[ds(tx * sub, sub), :], eq_v.at[ds(tx * sub, sub), :])
    for w in (qkv, gate, up, down):
        w.start_y()
    for k in far_first:
        d_cp(k).start()
    for w in (qkv, gate, up, down):
        w.start_local()
    d_own = net.here(dh2h.at[ds(tx * sub, sub), :], dh2_o.at[:, pl.ds(0, dt)])

    for k in far_first:
        g_cp(k).wait_recv()
        h_cp(k).wait_recv()
    g_own.wait()
    h_own.wait()

    @pl.loop(0, sub // 16)
    def _(r):
        x = rows[ds(r * 16, 16), :].astype(F32)
        inv = lax.rsqrt(jnp.sum(x * x, axis=1, keepdims=True) / dim + NORM_EPS)
        n_v[ds(z * sub + r * 16, 16), :] = (x * inv * gains[0:1, :]).astype(BF16)

    outs = [net.here(rows, h_o), net.here(gains, g_o)]
    ag.start()
    for k in far_first:
        e_cp(k, peer[k]).wait_recv()
    e_own.wait()
    ag.step1()
    qkv.y_event(0)
    gate.y_event(0)
    qkv.x_event(0)
    qkv.finish()

    @pl.loop(0, 4)
    def _(b):
        @pl.loop(0, dim // dtile)
        def _(j):
            w = wq_v[ds(j * dtile, dtile), :]
            p_v[ds(b * sub, sub), ds(j * dtile, dtile)] = dot(eq_v[ds(b * sub, sub), :], w, NT_DIMS).astype(BF16)

    for i in (2, 1, 0):
        rsc.send_end(i)
    gate.x_event(0)
    ag.step2()
    ag.step3()
    gate.y_event(1)
    gate.x_event(1)
    up.y_event(0)
    rsc.send_mid(2)
    gate.finish()

    def gate_block(b):
        @pl.loop(0, ff // tile)
        def _(j):
            cols = ds(j * tile, tile)
            a_v[ds(b * sub, sub), cols] = dot(n_v[ds(b * sub, sub), :], wg_v[:, cols]).astype(BF16)

    def up_block(b):
        @pl.loop(0, ff // tile)
        def _(j):
            cols = ds(j * tile, tile)
            bb = dot(n_v[ds(b * sub, sub), :], wu_v[:, cols]).astype(BF16)
            b_v[ds(b * sub, sub), cols] = bb
            aa = a_v[ds(b * sub, sub), cols].astype(F32)
            u_v[ds(b * sub, sub), cols] = (aa * jax.nn.sigmoid(aa) * bb.astype(F32)).astype(BF16)

    gate_block(z)
    gate_block(ag.slots[0])
    gate_block(ag.slots[1])
    up.x_event(0)
    up.y_event(1)
    gate_block(ag.slots[2])
    outs += [net.here(n_v, n_o), net.here(a_v, a_o), net.here(wg_v, wg_o), net.here(wq_v, wq_o), net.here(eq_v, eq_o)]
    up.x_event(1)
    down.y_event(0)
    rsc.send_mid(1)
    rsc.send_mid(0)
    up.finish()
    up_block(z)
    up_block(ag.slots[0])
    down.x_event(0)
    down.y_event(1)
    up_block(ag.slots[1])
    up_block(ag.slots[2])
    outs += [net.here(b_v, b_o), net.here(u_v, u_o), net.here(wu_v, wu_o)]
    down.x_event(1)
    rsc.finish()

    @pl.loop(0, sub // 16)
    def _(r):
        dn2_v[ds(r * 16, 16), :] = p_v[ds(z * sub + r * 16, 16), :].astype(F32)

    @pl.when(z < 3)
    def _():
        @pl.loop(0, sub // 16)
        def _(r):
            dn2_v[ds(r * 16, 16), :] += rbuf[ds(z * sub + r * 16, 16), :].astype(F32)

    @pl.when(z > 0)
    def _():
        @pl.loop(0, sub // 16)
        def _(r):
            dn2_v[ds(r * 16, 16), :] += rbuf[ds(4 * sub + r * 16, 16), :].astype(F32)

    outs.append(net.here(dn2_v, dn2_o))
    down.finish()
    for k in far_first:
        d_cp(k).wait_recv()
    d_own.wait()
    for c in outs:
        c.wait()
    for k in far_first:
        g_cp(k).wait_send()
        h_cp(k).wait_send()
        e_cp(k, tx).wait_send()
        d_cp(k).wait_send()
    for w in (qkv, gate, up, down):
        w.drain()
    ag.drain()
    rsc.drain()


def call_a(hid, eqh, dh2h, wg, wu, wd, wq, gin):
    tokens, dt = hid.shape
    sub, dim, ff, width = tokens // 4, dt * 4, wg.shape[1], wq.shape[1]
    s = jax.ShapeDtypeStruct
    tok_ff = s((tokens, ff), BF16)
    shapes = (s((tokens, dim), BF16), tok_ff, tok_ff, tok_ff, s((dim, ff), BF16), s((dim, ff), BF16), s((ff, dim), BF16),
              s((dim, width), BF16), s((tokens, width), BF16), s((sub, dim), BF16), s((sub, dim), BF16), s((sub, dim), F32), s((8, dim), F32))
    return pl.pallas_call(
        kernel_a, out_shape=shapes, in_specs=[ANY] * 8, out_specs=[ANY] * len(shapes),
        scratch_shapes=[
            VMEM((sub, dim), BF16), VMEM((tokens, dim), BF16), VMEM((tokens, ff), BF16), VMEM((tokens, ff), BF16), VMEM((tokens, ff), BF16),
            VMEM((dim, ff), BF16), VMEM((dim, ff), BF16), VMEM((dim, width), BF16), VMEM((tokens, width), BF16), VMEM((tokens, dim), BF16),
            VMEM((5 * sub, dim), BF16), VMEM((8, dim), F32), VMEM((sub, dim), F32),
            pltpu.SemaphoreType.DMA((64,)), pltpu.SemaphoreType.DMA((64,)), pltpu.SemaphoreType.DMA((20,))],
        compiler_params=pltpu.CompilerParams(collective_id=0, has_side_effects=True, vmem_limit_bytes=VMEM_LIMIT),
        cost_estimate=pl.CostEstimate(flops=20 * tokens * dim * ff, bytes_accessed=100000000, transcendentals=0), name="phase_a",
    )(hid, eqh, dh2h, wg, wu, wd, wq, gin)


def kernel_b(u_h, wd_h, h_h, dh2_h, dn2_h, a_h, b_h, g_h,
             e_o, da_o, db_o, n2_o, dres_o, home_o, dg_o,
             u_v, wd_v, h_v, dh2_v, dn2_v, a_v, b_v, gains, e_v, p_v, rbuf, res_v, n2_v, dres_v, dg_v, send, recv, local):
    dp, z, tx, peer = places()
    tokens, ff = u_v.shape
    sub, dim = h_v.shape
    dt = dim // 4
    tile = min(512, ff)
    dtile = min(512, dim)
    net = Wires(send, recv, local)
    loads = [net.here(u_h, u_v), net.here(wd_h, wd_v)]
    rows_in = [net.here(h_h, h_v), net.here(dn2_h, dn2_v), net.here(dh2_h, dh2_v), net.here(g_h, gains), net.here(a_h, a_v), net.here(b_h, b_v)]
    entry_barrier([{"tx": peer[1]}, {"tx": peer[2]}, {"tx": peer[3]}], z)
    far_first = (2, 3, 1)
    o_id = net.take(4)

    def o_cp(k, block):
        return net.copy(res_v.at[:, pl.ds(k * dt, dt)], home_o.at[ds(block * sub, sub), :], o_id + k, o_id + k, tx=peer[k])

    rsc = LineScatter(net, p_v, rbuf, sub, z)
    ag = LineGather(net, e_v, sub, z)
    for c in loads:
        c.wait()

    def down_block(b):
        @pl.loop(0, dim // dtile)
        def _(j):
            cols = ds(j * dtile, dtile)
            p_v[ds(b * sub, sub), cols] = dot(u_v[ds(b * sub, sub), :], wd_v[:, cols]).astype(BF16)

    for i in (2, 1, 0):
        down_block(ag.slots[i])
        rsc.send_end(i)
    down_block(z)
    for i in (2, 1, 0):
        rsc.send_mid(i)
    for c in rows_in:
        c.wait()
    rsc.finish()
    dg_v[...] = jnp.zeros_like(dg_v)
    step = 16

    def mlp(r):
        return p_v[ds(z * sub + r * step, step), :].astype(F32)

    def from_right(r):
        return rbuf[ds(z * sub + r * step, step), :].astype(F32)

    def from_left(r):
        return rbuf[ds(4 * sub + r * step, step), :].astype(F32)

    def norm_rows(total):
        @pl.loop(0, sub // step)
        def _(r):
            view = ds(r * step, step)
            resid = (h_v[view, :].astype(F32) + total(r)).astype(BF16)
            res_v[view, :] = resid
            x = resid.astype(F32)
            inv = lax.rsqrt(jnp.sum(x * x, axis=1, keepdims=True) / dim + NORM_EPS)
            xhat = x * inv
            gain = gains[1:2, :]
            n2_v[view, :] = (xhat * gain).astype(BF16)
            dy = dn2_v[view, :]
            part = dy * xhat
            dg_v[...] += part[:8] + part[8:]
            inner = jnp.sum(part * gain, axis=1, keepdims=True) / dim
            dres = dh2_v[view, :].astype(F32) + inv * (dy * gain) - xhat * (inv * inner)
            dres_v[view, :] = dres
            e_v[ds(z * sub + r * step, step), :] = dres.astype(BF16)

    @pl.when(z == 0)
    def _():
        norm_rows(lambda r: mlp(r) + from_right(r))

    @pl.when(z == 3)
    def _():
        norm_rows(lambda r: mlp(r) + from_left(r))

    @pl.when(mid(z))
    def _():
        norm_rows(lambda r: mlp(r) + from_right(r) + from_left(r))

    ag.start()
    for k in far_first:
        o_cp(k, tx).start()
    outs = [net.here(res_v.at[:, pl.ds(0, dt)], home_o.at[ds(tx * sub, sub), :]), net.here(n2_v, n2_o), net.here(dres_v, dres_o), net.here(dg_v, dg_o)]

    def back_block(b):
        rows = ds(b * sub, sub)

        @pl.loop(0, ff // tile)
        def _(j):
            cols = ds(j * tile, tile)
            du = dot(e_v[rows, :], wd_v[ds(j * tile, tile), :], NT_DIMS)
            aa = a_v[rows, cols].astype(F32)
            bb = b_v[rows, cols].astype(F32)
            sig = jax.nn.sigmoid(aa)
            a_v[rows, cols] = (du * bb * sig * (1.0 + aa * (1.0 - sig))).astype(BF16)
            b_v[rows, cols] = (du * aa * sig).astype(BF16)

    back_block(z)
    ag.step1()
    back_block(ag.slots[0])
    ag.step2()
    back_block(ag.slots[1])
    ag.step3()
    back_block(ag.slots[2])
    outs += [net.here(e_v, e_o), net.here(a_v, da_o), net.here(b_v, db_o)]
    for k in far_first:
        o_cp(k, peer[k]).wait_recv()
    for c in outs:
        c.wait()
    for k in far_first:
        o_cp(k, tx).wait_send()
    ag.drain()
    rsc.drain()


def call_b(u, wd, h, dh2, dn2, a, b, gains):
    tokens, ff = u.shape
    sub, dim = h.shape
    s = jax.ShapeDtypeStruct
    shapes = (s((tokens, dim), BF16), s((tokens, ff), BF16), s((tokens, ff), BF16), s((sub, dim), BF16), s((sub, dim), F32),
              s((tokens, dim // 4), BF16), s((8, dim), F32))
    return pl.pallas_call(
        kernel_b, out_shape=shapes, in_specs=[ANY] * 8, out_specs=[ANY] * len(shapes),
        scratch_shapes=[
            VMEM((tokens, ff), BF16), VMEM((ff, dim), BF16), VMEM((sub, dim), BF16), VMEM((sub, dim), BF16), VMEM((sub, dim), F32),
            VMEM((tokens, ff), BF16), VMEM((tokens, ff), BF16), VMEM((8, dim), F32), VMEM((tokens, dim), BF16), VMEM((tokens, dim), BF16),
            VMEM((5 * sub, dim), BF16), VMEM((sub, dim), BF16), VMEM((sub, dim), BF16), VMEM((sub, dim), F32), VMEM((8, dim), F32),
            pltpu.SemaphoreType.DMA((24,)), pltpu.SemaphoreType.DMA((24,)), pltpu.SemaphoreType.DMA((20,))],
        compiler_params=pltpu.CompilerParams(collective_id=1, has_side_effects=True, vmem_limit_bytes=VMEM_LIMIT),
        cost_estimate=pl.CostEstimate(flops=20 * tokens * dim * ff, bytes_accessed=60000000, transcendentals=0), name="phase_b",
    )(u, wd, h, dh2, dn2, a, b, gains)


def solution(mesh):
    nz = mesh.shape["ty"]
    nt = mesh.shape["tx"]

    def xor_tx(x, k):
        return lax.ppermute(x, "tx", [(i, i ^ k) for i in range(nt)])

    def swap_dp(x):
        return lax.ppermute(x, "dp", [(0, 1), (1, 0)])

    def shift_z(x, pairs):
        return lax.ppermute(x, "ty", pairs)

    def local_step(hidden, positions, g_ffn, w_gate, w_up, w_down, g_attn, w_q, w_kv, grad_h2, grad_q, grad_kv):
        tx = lax.axis_index("tx")
        ty = lax.axis_index("ty")
        dp = lax.axis_index("dp")
        dt = hidden.shape[1]
        model_dim = dt * nt
        sub = hidden.shape[0] // nt
        head_dim = w_q.shape[2]
        kv_local = w_kv.shape[1]
        heads = w_q.shape[1] + kv_local
        width = heads * head_dim

        def to_rows(x):
            parts = x.reshape(nt, sub, dt)
            got = [parts[tx]]
            for k in range(1, nt):
                got.append(xor_tx(parts[tx ^ k], k))
            return jnp.concatenate(got, axis=1)

        def from_rows(x):
            out = jnp.zeros((nt, sub, dt), x.dtype)
            out = lax.dynamic_update_index_in_dim(out, x[:, :dt], tx, 0)
            for k in range(1, nt):
                piece = xor_tx(x[:, k * dt:(k + 1) * dt], k)
                out = lax.dynamic_update_index_in_dim(out, piece, tx ^ k, 0)
            return out.reshape(nt * sub, dt)

        def gather_w(w, axis):
            mate = xor_tx(w, 1)
            half = w.shape[0] // 2
            mine = lax.dynamic_slice_in_dim(w, dp * half, half, 0)
            near = xor_tx(mine, 2)
            far = swap_dp(near)
            other = jnp.where(dp == 0, jnp.concatenate([near, far], 0), jnp.concatenate([far, near], 0))
            diag = xor_tx(other, 1)
            return jnp.concatenate([w, mate, other, diag], axis=axis)

        def reduce_w(blocks):
            sent = xor_tx(jnp.concatenate([blocks[1], blocks[3]], 0).astype(BF16), 1)
            rows = blocks[0].shape[0]
            keep = blocks[0] + sent[:rows].astype(F32)
            cross = blocks[2] + sent[rows:].astype(F32)
            back = xor_tx(cross.astype(BF16), 2)
            return keep + back.astype(F32)

        def gather_z(block):
            right = [(0, 1), (1, 2), (2, 3)]
            left = [(1, 0), (2, 1), (3, 2)]
            r1 = shift_z(block, right)
            l1 = shift_z(block, left)
            r2 = shift_z(r1, right[1:])
            l2 = shift_z(l1, left[:-1])
            r3 = shift_z(r2, right[2:])
            l3 = shift_z(l2, left[:1])
            out = jnp.zeros((nz + 1,) + block.shape, block.dtype)
            out = lax.dynamic_update_index_in_dim(out, block, ty, 0)
            for step, (r, l) in enumerate(((r1, l1), (r2, l2), (r3, l3)), 1):
                out = lax.dynamic_update_index_in_dim(out, r, jnp.where(ty >= step, ty - step, nz), 0)
                out = lax.dynamic_update_index_in_dim(out, l, jnp.where(ty + step < nz, ty + step, nz), 0)
            return out[:nz].reshape((nz * block.shape[0],) + block.shape[1:])

        def scatter_z(part):
            blocks = part.reshape((nz, part.shape[0] // nz) + part.shape[1:])

            def pick(offset):
                return lax.dynamic_index_in_dim(blocks, jnp.clip(ty + offset, 0, nz - 1), 0, keepdims=False)

            r1 = shift_z(pick(3), [(0, 1)])
            l1 = shift_z(pick(-3), [(3, 2)])
            r2 = shift_z((pick(2).astype(F32) + r1.astype(F32)).astype(BF16), [(0, 1), (1, 2)])
            l2 = shift_z((pick(-2).astype(F32) + l1.astype(F32)).astype(BF16), [(3, 2), (2, 1)])
            r3 = shift_z((pick(1).astype(F32) + r2.astype(F32)).astype(BF16), [(0, 1), (1, 2), (2, 3)])
            l3 = shift_z((pick(-1).astype(F32) + l2.astype(F32)).astype(BF16), [(3, 2), (2, 1), (1, 0)])
            return pick(0).astype(F32) + r3.astype(F32) + l3.astype(F32)

        cos_t, sin_t = rope_tables(positions, head_dim)
        kv_index = ty * kv_local + jnp.arange(kv_local)
        kv_flag = (kv_index < kv_local * nz // 2).astype(F32)[None, :, None]
        cos_kv = kv_flag * cos_t + (1.0 - kv_flag)
        sin_kv = kv_flag * sin_t
        back_q = rotate(grad_q.astype(F32), cos_t, -sin_t).astype(BF16)
        back_kv = rotate(grad_kv.astype(F32), cos_kv, -sin_kv).astype(BF16)
        back = jnp.concatenate([back_q, back_kv], axis=1).reshape(nt * sub, width)
        w_qkv_own = jnp.concatenate([w_q, w_kv], axis=1).reshape(dt, width)
        gin = jnp.concatenate([jnp.stack([g_ffn, g_attn]).astype(F32), jnp.zeros((6, dt), F32)])

        (normed_all, a_all, b_all, u_all, gate_w, up_w, down_w, w_qkv, back_all, h_rows, dh2_rows, dn2_rows, gains) = call_a(
            hidden, back, grad_h2, w_gate, w_up, w_down, w_qkv_own, gin)
        res_all, grad_gate, grad_up, normed2, grad_res, resid_out, gattn8 = call_b(
            u_all, down_w, h_rows, dh2_rows, dn2_rows, a_all, b_all, gains)
        gain_ffn = gains[0]
        rows = h_rows.astype(F32)
        inv_ffn = lax.rsqrt(jnp.sum(rows * rows, axis=1, keepdims=True) / model_dim + NORM_EPS)
        gattn = jnp.sum(gattn8, axis=0)
        hidden_act = u_all

        n_part = (dot(grad_gate, gate_w, COLS_COLS) + dot(grad_up, up_w, COLS_COLS)).astype(BF16)
        grad_n = scatter_z(n_part)
        normed2_all = gather_z(normed2)

        wd = dot(hidden_act, res_all, ROWS_ROWS)
        grad_wdown = reduce_w([wd[:, k * dt:(k + 1) * dt] for k in range(nt)])
        wg = dot(normed_all, grad_gate, ROWS_ROWS)
        grad_wgate = reduce_w([wg[k * dt:(k + 1) * dt] for k in range(nt)])
        wu = dot(normed_all, grad_up, ROWS_ROWS)
        grad_wup = reduce_w([wu[k * dt:(k + 1) * dt] for k in range(nt)])

        qkv = dot(normed2_all, w_qkv).astype(BF16).reshape(nz, sub, width)
        qkv_home = jnp.zeros((nt, sub, width), BF16)
        qkv_home = lax.dynamic_update_index_in_dim(qkv_home, qkv[tx], tx, 0)
        for k in range(1, nt):
            qkv_home = lax.dynamic_update_index_in_dim(qkv_home, xor_tx(qkv[tx ^ k], k), tx ^ k, 0)
        qkv_home = qkv_home.reshape(nt * sub, heads, head_dim).astype(F32)
        q_out = rotate(qkv_home[:, :heads - kv_local], cos_t, sin_t).astype(BF16)
        kv_out = rotate(qkv_home[:, heads - kv_local:], cos_kv, sin_kv).astype(BF16)
        wqkv_g = dot(normed2_all, back_all, ROWS_ROWS)
        grad_wqkv = reduce_w([wqkv_g[k * dt:(k + 1) * dt] for k in range(nt)]).reshape(dt, heads, head_dim)
        grad_wq = grad_wqkv[:, :heads - kv_local]
        grad_wkv = grad_wqkv[:, heads - kv_local:]

        gffn, grad_ffn_in = norm_backward(rows, inv_ffn, gain_ffn, grad_n, model_dim)
        grad_hidden = from_rows((grad_res + grad_ffn_in).astype(BF16))

        both = jnp.stack([gffn, gattn]).reshape(2, nt, dt)
        spread = jnp.zeros((2, nt, dt), F32)
        for k in range(nt):
            spread = lax.dynamic_update_index_in_dim(spread, both[:, k], tx ^ k, 1)
        total = spread
        total = total + xor_tx(total, 1)
        total = total + xor_tx(total, 2)
        total = total + lax.ppermute(total, "ty", [(i, i ^ 1) for i in range(nz)])
        total = total + lax.ppermute(total, "ty", [(i, i ^ 3) for i in range(nz)])
        grad_gffn, grad_gattn = total[0, tx], total[1, tx]
        return (resid_out, q_out, kv_out, grad_hidden, grad_gffn, grad_gattn, grad_wgate, grad_wup, grad_wdown, grad_wq, grad_wkv)

    row_spec = P(("dp", "ty"), "tx")
    head_spec = P(("dp", "tx"), "ty", None)
    in_specs = (row_spec, P(("dp", "tx")), P("tx"), P("tx", "ty"), P("tx", "ty"), P("ty", "tx"), P("tx"), P("tx", "ty", None), P("tx", "ty", None), row_spec, head_spec, head_spec)
    out_specs = (row_spec, head_spec, head_spec, row_spec, P(("dp", "tx")), P(("dp", "tx")), P(("dp", "tx"), "ty"), P(("dp", "tx"), "ty"), P(("dp", "ty"), "tx"), head_spec, head_spec)
    return jax.shard_map(local_step, mesh=mesh, in_specs=in_specs, out_specs=out_specs, check_vma=False)
```

```python
import functools

import jax
import jax.numpy as jnp
from jax import lax
from jax.experimental import pallas as pl
from jax.experimental.pallas import tpu as pltpu
from jax.sharding import PartitionSpec as P

NORM_EPS = 1e-5
ROPE_BASE = 10000.0
F32 = jnp.float32
BF16 = jnp.bfloat16


def dot(a, b, dims=(((1,), (0,)), ((), ()))):
    return lax.dot_general(a, b, dims, preferred_element_type=F32)


MESH = pl.DeviceIdType.MESH
ANY = pl.BlockSpec(memory_space=pl.ANY)
VMEM = pltpu.VMEM
NT_DIMS = (((1,), (1,)), ((), ()))
VMEM_LIMIT = 67000000


def ds(start, size, align=None):
    if isinstance(start, int):
        return pl.ds(start, size)
    return pl.ds(pl.multiple_of(start, align or size), size)


def mid(z):
    return jnp.logical_and(z > 0, z < 3)


def end(z):
    return jnp.logical_or(z == 0, z == 3)


def slots(z):
    return (z + 1 - 2 * (z % 2), 2 - z // 2, 3 - 3 * (z // 2))


def turn(src, dst, rows, width, q_width, cos_ref, sin_ref, swap_ref, back):
    step = min(256, rows)

    @pl.loop(0, rows // step)
    def _(r):
        for c in range(width // 128):
            cols = pl.ds(c * 128, 128)
            table = ds(r * step + (0 if c * 128 < q_width else rows), step, step)
            x = src[ds(r * step, step), cols]
            main = x.astype(F32) * cos_ref[table, :]
            side = dot(x, swap_ref[...]) * sin_ref[table, :]
            dst[ds(r * step, step), cols] = (main - side if back else main + side).astype(BF16)


class Wires:
    def __init__(self, send, recv, local):
        self.send, self.recv, self.local = send, recv, local
        self.n_remote = 0
        self.n_local = 0

    def take(self, n=1):
        base = self.n_remote
        self.n_remote += n
        assert self.n_remote <= self.send.shape[0]
        return base

    def copy(self, src, dst, si, ri, **dev):
        return pltpu.make_async_remote_copy(
            src_ref=src, dst_ref=dst, send_sem=self.send.at[si], recv_sem=self.recv.at[ri],
            device_id=dev, device_id_type=MESH)

    def here(self, src, dst):
        i = self.n_local
        self.n_local += 1
        assert i < self.local.shape[0]
        c = pltpu.make_async_copy(src, dst, self.local.at[i])
        c.start()
        return c


def entry_barrier(axes, z):
    sem = pltpu.get_barrier_semaphore()
    for dev in axes:
        pl.semaphore_signal(sem, inc=1, device_id=dev, device_id_type=MESH)

    @pl.when(z > 0)
    def _():
        pl.semaphore_signal(sem, inc=1, device_id={"ty": z - 1}, device_id_type=MESH)

    @pl.when(z < 3)
    def _():
        pl.semaphore_signal(sem, inc=1, device_id={"ty": z + 1}, device_id_type=MESH)

    @pl.when(mid(z))
    def _():
        pl.semaphore_wait(sem, len(axes) + 2)

    @pl.when(end(z))
    def _():
        pl.semaphore_wait(sem, len(axes) + 1)


class LineGather:
    def __init__(self, net, buf, rows, z):
        self.net, self.buf, self.rows, self.z = net, buf, rows, z
        self.base = net.take(8)
        self.slots = slots(z)

    def blk(self, b):
        return self.buf.at[ds(b * self.rows, self.rows), :]

    def cp(self, b, side, target):
        return self.net.copy(self.blk(b), self.blk(b), self.base + side * 4 + b, self.base + b, ty=target)

    def start(self):
        z = self.z

        @pl.when(z < 3)
        def _():
            self.cp(z, 0, z + 1).start()

        @pl.when(z > 0)
        def _():
            self.cp(z, 1, z - 1).start()

    def take(self, i):
        b = self.slots[i]
        self.cp(b, 0, self.z).wait_recv()

    def forward(self, i):
        z, b = self.z, self.slots[i]
        target = 3 - z if i == 0 else 3 * (z - 1)
        self.cp(b, 0, target).start()

    def step1(self):
        self.take(0)

        @pl.when(mid(self.z))
        def _():
            self.forward(0)
            self.take(1)
            self.forward(1)

    def step2(self):
        @pl.when(end(self.z))
        def _():
            self.take(1)

    def step3(self):
        self.take(2)

        @pl.when(mid(self.z))
        def _():
            self.forward(2)

    def drain(self):
        z = self.z

        @pl.when(z < 3)
        def _():
            self.cp(z, 0, z + 1).wait_send()

        @pl.when(z > 0)
        def _():
            self.cp(z, 1, z - 1).wait_send()

        @pl.when(mid(z))
        def _():
            for i in range(3):
                self.cp(self.slots[i], 0, 3 - z if i == 0 else 3 * (z - 1)).wait_send()


class LineScatter:
    def __init__(self, net, part, rbuf, rows, z):
        self.net, self.part, self.rbuf, self.rows, self.z = net, part, rbuf, rows, z
        self.base = net.take(5)
        self.slots = slots(z)
        one = (z % 2) * (1 - z // 2)
        self.dst = (self.slots[0] + (1 - z % 2) * (3 - z), self.slots[1] + 2 * one, self.slots[2])
        self.target = (z + 1 - 2 * (z % 2), 1 + z % 2, 1 + z % 2)

    def cp(self, i):
        return self.net.copy(
            self.part.at[ds(self.slots[i] * self.rows, self.rows), :], self.rbuf.at[ds(self.dst[i] * self.rows, self.rows), :],
            self.base + i, self.base + self.dst[i], ty=self.target[i])

    def wait_slot(self, s):
        view = self.rbuf.at[ds(s * self.rows, self.rows), :]
        self.net.copy(view, view, self.base, self.base + s, ty=self.z).wait_recv()

    def send_end(self, i):
        @pl.when(end(self.z))
        def _():
            self.cp(i).start()

    def send_mid(self, i):
        @pl.when(mid(self.z))
        def _():
            b = self.slots[i]
            self.wait_slot(b)
            step = min(32, self.rows)

            @pl.loop(0, self.rows // step)
            def _(r):
                view = ds(b * self.rows + r * step, step, step)
                self.part[view, :] = (self.part[view, :].astype(F32) + self.rbuf[view, :].astype(F32)).astype(BF16)

            self.cp(i).start()

    def finish(self):
        z = self.z

        @pl.when(z < 3)
        def _():
            self.wait_slot(z)

        @pl.when(z > 0)
        def _():
            self.wait_slot(4)

    def drain(self):
        for i in range(3):
            self.cp(i).wait_send()


class WeightGather:
    def __init__(self, net, w, full, pos, by_rows, chunks):
        self.net, self.w, self.full, self.by_rows = net, w, full, by_rows
        self.dp, self.t1, self.t2 = pos
        self.len = w.shape[0]
        self.width = w.shape[0] if by_rows else w.shape[1]
        self.chunks = chunks
        self.piece = self.len // 2 // chunks
        self.base = net.take(1 + 4 * chunks)

    def dst(self, k, off, n):
        if self.by_rows:
            return self.full.at[ds(k * self.width + off, n, min(n, 16)), :]
        return self.full.at[ds(off, n, 16), pl.ds(k * self.width, self.width)]

    def off(self, half, ch):
        return half * (self.len // 2) + ch * self.piece

    def near(self, ch):
        o = self.off(self.dp, ch)
        i = self.base + 1 + ch
        return self.net.copy(self.w.at[ds(o, self.piece, 16), :], self.dst(2, o, self.piece), i, i, tx=self.t2)

    def cross(self, ch, half):
        o = self.off(half, ch)
        i = self.base + 1 + self.chunks + ch
        return self.net.copy(self.dst(2, o, self.piece), self.dst(2, o, self.piece), i, i, dp=1 - self.dp)

    def diag(self, ch, which, half):
        o = self.off(half, ch)
        i = self.base + 1 + (2 + which) * self.chunks + ch
        return self.net.copy(self.dst(2, o, self.piece), self.dst(3, o, self.piece), i, i, tx=self.t1)

    def mate(self):
        return self.net.copy(self.w, self.dst(1, 0, self.len), self.base, self.base, tx=self.t1)

    def start_y(self):
        for ch in range(self.chunks):
            self.near(ch).start()

    def start_local(self):
        self.own = self.net.here(self.w, self.dst(0, 0, self.len))
        self.mate().start()

    def y_event(self, ch):
        self.near(ch).wait_recv()
        self.cross(ch, self.dp).start()
        self.diag(ch, 0, self.dp).start()

    def x_event(self, ch):
        self.cross(ch, 1 - self.dp).wait_recv()
        self.diag(ch, 1, 1 - self.dp).start()

    def finish(self):
        self.own.wait()
        self.mate().wait_recv()
        for ch in range(self.chunks):
            self.diag(ch, 0, self.dp).wait_recv()
            self.diag(ch, 1, 1 - self.dp).wait_recv()

    def drain(self):
        self.mate().wait_send()
        for ch in range(self.chunks):
            self.near(ch).wait_send()
            self.cross(ch, self.dp).wait_send()
            self.diag(ch, 0, self.dp).wait_send()
            self.diag(ch, 1, 1 - self.dp).wait_send()


def places():
    dp, z, tx = lax.axis_index("dp"), lax.axis_index("ty"), lax.axis_index("tx")
    return dp, z, tx, (tx, tx + 1 - 2 * (tx % 2), (tx + 2) % 4, 3 - tx)


def kernel_a(q_width, hid, eqh, cosh, sinh, swaph, dh2h, wg, wu, wd, wq, gin,
             n_o, a_o, b_o, u_o, wg_o, wu_o, wd_o, wq_o, eq_o, h_o, dh2_o, dn2_o, g_o,
             rows, n_v, a_v, b_v, u_v, wg_v, wu_v, wq_v, eq_v, p_v, rbuf, gains, dn2_v, cos_v, sin_v, swap_v, send, recv, local):
    dp, z, tx, peer = places()
    sub, dim = rows.shape
    width = eq_v.shape[1]
    dt = dim // 4
    ff = wg.shape[1]
    tile = min(512, ff)
    dtile = min(512, dim)
    net = Wires(send, recv, local)
    eq_raw = p_v.at[:, pl.ds(0, width)]
    turn_in = [net.here(eqh, eq_raw), net.here(cosh, cos_v), net.here(sinh, sin_v), net.here(swaph, swap_v)]
    entry_barrier([{"tx": peer[1]}, {"tx": peer[2]}, {"tx": peer[3]}, {"dp": 1 - dp}], z)

    pos = (dp, peer[1], peer[2])
    far_first = (2, 3, 1)
    g_id, h_id, e_id, d_id = net.take(4), net.take(4), net.take(4), net.take(4)

    def g_cp(k):
        return net.copy(gin, gains.at[:, pl.ds(k * dt, dt)], g_id + k, g_id + k, tx=peer[k])

    def h_cp(k):
        return net.copy(hid.at[ds(peer[k] * sub, sub), :], rows.at[:, pl.ds(k * dt, dt)], h_id + k, h_id + k, tx=peer[k])

    def e_cp(k, block):
        return net.copy(p_v.at[ds(peer[k] * sub, sub), pl.ds(0, width)], eq_v.at[ds(block * sub, sub), :], e_id + k, e_id + k, tx=peer[k])

    def d_cp(k):
        return net.copy(dh2h.at[ds(peer[k] * sub, sub), :], dh2_o.at[:, pl.ds(k * dt, dt)], d_id + k, d_id + k, tx=peer[k])

    gate = WeightGather(net, wg, wg_v, pos, True, 2)
    up = WeightGather(net, wu, wu_v, pos, True, 2)
    down = WeightGather(net, wd, wd_o, pos, False, 2)
    qkv = WeightGather(net, wq, wq_v, pos, True, 1)
    ag = LineGather(net, n_v, sub, z)
    rsc = LineScatter(net, p_v, rbuf, sub, z)

    for k in far_first:
        g_cp(k).start()
    for k in far_first:
        h_cp(k).start()
    g_own = net.here(gin, gains.at[:, pl.ds(0, dt)])
    h_own = net.here(hid.at[ds(tx * sub, sub), :], rows.at[:, pl.ds(0, dt)])
    for c in turn_in:
        c.wait()
    turn(p_v, p_v, 4 * sub, width, q_width, cos_v, sin_v, swap_v, True)
    for k in far_first:
        e_cp(k, tx).start()
    e_own = net.here(p_v.at[ds(tx * sub, sub), pl.ds(0, width)], eq_v.at[ds(tx * sub, sub), :])
    for w in (qkv, gate, up, down):
        w.start_y()
    for k in far_first:
        d_cp(k).start()
    for w in (qkv, gate, up, down):
        w.start_local()
    d_own = net.here(dh2h.at[ds(tx * sub, sub), :], dh2_o.at[:, pl.ds(0, dt)])

    for k in far_first:
        g_cp(k).wait_recv()
        h_cp(k).wait_recv()
    g_own.wait()
    h_own.wait()

    @pl.loop(0, sub // 16)
    def _(r):
        x = rows[ds(r * 16, 16), :].astype(F32)
        inv = lax.rsqrt(jnp.sum(x * x, axis=1, keepdims=True) / dim + NORM_EPS)
        n_v[ds(z * sub + r * 16, 16), :] = (x * inv * gains[0:1, :]).astype(BF16)

    outs = [net.here(rows, h_o), net.here(gains, g_o)]
    ag.start()
    for k in far_first:
        e_cp(k, peer[k]).wait_recv()
    e_own.wait()
    ag.step1()
    qkv.y_event(0)
    gate.y_event(0)
    qkv.x_event(0)
    qkv.finish()
    for k in far_first:
        e_cp(k, tx).wait_send()

    @pl.loop(0, 4)
    def _(b):
        @pl.loop(0, dim // dtile)
        def _(j):
            w = wq_v[ds(j * dtile, dtile), :]
            p_v[ds(b * sub, sub), ds(j * dtile, dtile)] = dot(eq_v[ds(b * sub, sub), :], w, NT_DIMS).astype(BF16)

    for i in (2, 1, 0):
        rsc.send_end(i)
    gate.x_event(0)
    ag.step2()
    ag.step3()
    gate.y_event(1)
    gate.x_event(1)
    up.y_event(0)
    rsc.send_mid(2)
    gate.finish()

    def gate_block(b):
        @pl.loop(0, ff // tile)
        def _(j):
            cols = ds(j * tile, tile)
            a_v[ds(b * sub, sub), cols] = dot(n_v[ds(b * sub, sub), :], wg_v[:, cols]).astype(BF16)

    def up_block(b):
        @pl.loop(0, ff // tile)
        def _(j):
            cols = ds(j * tile, tile)
            bb = dot(n_v[ds(b * sub, sub), :], wu_v[:, cols]).astype(BF16)
            b_v[ds(b * sub, sub), cols] = bb
            aa = a_v[ds(b * sub, sub), cols].astype(F32)
            u_v[ds(b * sub, sub), cols] = (aa * jax.nn.sigmoid(aa) * bb.astype(F32)).astype(BF16)

    gate_block(z)
    gate_block(ag.slots[0])
    gate_block(ag.slots[1])
    up.x_event(0)
    up.y_event(1)
    gate_block(ag.slots[2])
    outs += [net.here(n_v, n_o), net.here(a_v, a_o), net.here(wg_v, wg_o), net.here(wq_v, wq_o), net.here(eq_v, eq_o)]
    up.x_event(1)
    down.y_event(0)
    rsc.send_mid(1)
    rsc.send_mid(0)
    up.finish()
    up_block(z)
    up_block(ag.slots[0])
    down.x_event(0)
    down.y_event(1)
    up_block(ag.slots[1])
    up_block(ag.slots[2])
    outs += [net.here(b_v, b_o), net.here(u_v, u_o), net.here(wu_v, wu_o)]
    down.x_event(1)
    rsc.finish()

    @pl.loop(0, sub // 16)
    def _(r):
        dn2_v[ds(r * 16, 16), :] = p_v[ds(z * sub + r * 16, 16), :].astype(F32)

    @pl.when(z < 3)
    def _():
        @pl.loop(0, sub // 16)
        def _(r):
            dn2_v[ds(r * 16, 16), :] += rbuf[ds(z * sub + r * 16, 16), :].astype(F32)

    @pl.when(z > 0)
    def _():
        @pl.loop(0, sub // 16)
        def _(r):
            dn2_v[ds(r * 16, 16), :] += rbuf[ds(4 * sub + r * 16, 16), :].astype(F32)

    outs.append(net.here(dn2_v, dn2_o))
    down.finish()
    for k in far_first:
        d_cp(k).wait_recv()
    d_own.wait()
    for c in outs:
        c.wait()
    for k in far_first:
        g_cp(k).wait_send()
        h_cp(k).wait_send()
        d_cp(k).wait_send()
    for w in (qkv, gate, up, down):
        w.drain()
    ag.drain()
    rsc.drain()


def call_a(q_width, hid, eqh, cos_t, sin_t, swap, dh2h, wg, wu, wd, wq, gin):
    tokens, dt = hid.shape
    sub, dim, ff, width = tokens // 4, dt * 4, wg.shape[1], wq.shape[1]
    s = jax.ShapeDtypeStruct
    tok_ff = s((tokens, ff), BF16)
    shapes = (s((tokens, dim), BF16), tok_ff, tok_ff, tok_ff, s((dim, ff), BF16), s((dim, ff), BF16), s((ff, dim), BF16),
              s((dim, width), BF16), s((tokens, width), BF16), s((sub, dim), BF16), s((sub, dim), BF16), s((sub, dim), F32), s((8, dim), F32))
    return pl.pallas_call(
        functools.partial(kernel_a, q_width), out_shape=shapes, in_specs=[ANY] * 11, out_specs=[ANY] * len(shapes),
        scratch_shapes=[
            VMEM((sub, dim), BF16), VMEM((tokens, dim), BF16), VMEM((tokens, ff), BF16), VMEM((tokens, ff), BF16), VMEM((tokens, ff), BF16),
            VMEM((dim, ff), BF16), VMEM((dim, ff), BF16), VMEM((dim, width), BF16), VMEM((tokens, width), BF16), VMEM((tokens, dim), BF16),
            VMEM((5 * sub, dim), BF16), VMEM((8, dim), F32), VMEM((sub, dim), F32), VMEM((2 * tokens, 128), F32), VMEM((2 * tokens, 128), F32), VMEM((128, 128), BF16),
            pltpu.SemaphoreType.DMA((64,)), pltpu.SemaphoreType.DMA((64,)), pltpu.SemaphoreType.DMA((32,))],
        compiler_params=pltpu.CompilerParams(collective_id=0, has_side_effects=True, vmem_limit_bytes=VMEM_LIMIT),
        cost_estimate=pl.CostEstimate(flops=20 * tokens * dim * ff, bytes_accessed=100000000, transcendentals=0), name="phase_a",
    )(hid, eqh, cos_t, sin_t, swap, dh2h, wg, wu, wd, wq, gin)


def kernel_b(u_h, wd_h, h_h, dh2_h, dn2_h, a_h, b_h, g_h,
             e_o, da_o, db_o, n2_o, dres_o, home_o, dg_o, ux_o, ex_o,
             u_v, wd_v, h_v, dh2_v, dn2_v, a_v, b_v, gains, e_v, p_v, rbuf, res_v, n2_v, dres_v, dg_v, send, recv, local):
    dp, z, tx, peer = places()
    tokens, ff = u_v.shape
    sub, dim = h_v.shape
    dt = dim // 4
    tile = min(512, ff)
    dtile = min(512, dim)
    net = Wires(send, recv, local)
    loads = [net.here(u_h, u_v), net.here(wd_h, wd_v)]
    rows_in = [net.here(h_h, h_v), net.here(dn2_h, dn2_v), net.here(dh2_h, dh2_v), net.here(g_h, gains), net.here(a_h, a_v), net.here(b_h, b_v)]
    entry_barrier([{"tx": peer[1]}, {"tx": peer[2]}, {"tx": peer[3]}], z)
    far_first = (2, 3, 1)
    o_id = net.take(4)

    def o_cp(k, block):
        return net.copy(res_v.at[:, pl.ds(k * dt, dt)], home_o.at[ds(block * sub, sub), :], o_id + k, o_id + k, tx=peer[k])

    u_id, x_id = net.take(3), net.take(12)

    def ux_cp(k):
        src = ux_o.at[1] if k == 3 else u_h
        return net.copy(src, ux_o.at[k - 1], u_id + k - 1, u_id + k - 1, tx=peer[1] if k == 3 else peer[k])

    def ex_cp(k, b):
        i = x_id + (k - 1) * 4 + b
        rows = ds(b * sub, sub)
        return net.copy(e_v.at[rows, pl.ds(k * dt, dt)], ex_o.at[k - 1, rows, :], i, i, tx=peer[k])

    ux_cp(2).start()
    ux_cp(1).start()
    rsc = LineScatter(net, p_v, rbuf, sub, z)
    ag = LineGather(net, e_v, sub, z)
    for c in loads:
        c.wait()

    def down_block(b):
        @pl.loop(0, dim // dtile)
        def _(j):
            cols = ds(j * dtile, dtile)
            p_v[ds(b * sub, sub), cols] = dot(u_v[ds(b * sub, sub), :], wd_v[:, cols]).astype(BF16)

    for i in (2, 1, 0):
        down_block(ag.slots[i])
        rsc.send_end(i)
    down_block(z)
    for i in (2, 1, 0):
        rsc.send_mid(i)
    for c in rows_in:
        c.wait()
    rsc.finish()
    dg_v[...] = jnp.zeros_like(dg_v)
    step = 16

    def mlp(r):
        return p_v[ds(z * sub + r * step, step), :].astype(F32)

    def from_right(r):
        return rbuf[ds(z * sub + r * step, step), :].astype(F32)

    def from_left(r):
        return rbuf[ds(4 * sub + r * step, step), :].astype(F32)

    def norm_rows(total):
        @pl.loop(0, sub // step)
        def _(r):
            view = ds(r * step, step)
            resid = (h_v[view, :].astype(F32) + total(r)).astype(BF16)
            res_v[view, :] = resid
            x = resid.astype(F32)
            inv = lax.rsqrt(jnp.sum(x * x, axis=1, keepdims=True) / dim + NORM_EPS)
            xhat = x * inv
            gain = gains[1:2, :]
            n2_v[view, :] = (xhat * gain).astype(BF16)
            dy = dn2_v[view, :]
            part = dy * xhat
            dg_v[...] += part[:8] + part[8:]
            inner = jnp.sum(part * gain, axis=1, keepdims=True) / dim
            dres = dh2_v[view, :].astype(F32) + inv * (dy * gain) - xhat * (inv * inner)
            dres_v[view, :] = dres
            e_v[ds(z * sub + r * step, step), :] = dres.astype(BF16)

    @pl.when(z == 0)
    def _():
        norm_rows(lambda r: mlp(r) + from_right(r))

    @pl.when(z == 3)
    def _():
        norm_rows(lambda r: mlp(r) + from_left(r))

    @pl.when(mid(z))
    def _():
        norm_rows(lambda r: mlp(r) + from_right(r) + from_left(r))

    ag.start()
    for k in far_first:
        o_cp(k, tx).start()
    outs = [net.here(res_v.at[:, pl.ds(0, dt)], home_o.at[ds(tx * sub, sub), :]), net.here(n2_v, n2_o), net.here(dres_v, dres_o), net.here(dg_v, dg_o)]

    def back_block(b):
        rows = ds(b * sub, sub)

        @pl.loop(0, ff // tile)
        def _(j):
            cols = ds(j * tile, tile)
            du = dot(e_v[rows, :], wd_v[ds(j * tile, tile), :], NT_DIMS)
            aa = a_v[rows, cols].astype(F32)
            bb = b_v[rows, cols].astype(F32)
            sig = jax.nn.sigmoid(aa)
            a_v[rows, cols] = (du * bb * sig * (1.0 + aa * (1.0 - sig))).astype(BF16)
            b_v[rows, cols] = (du * aa * sig).astype(BF16)

    def spread(b):
        for k in far_first:
            ex_cp(k, b).start()

    spread(z)
    back_block(z)
    ag.step1()
    spread(ag.slots[0])
    back_block(ag.slots[0])
    ag.step2()
    spread(ag.slots[1])
    ux_cp(2).wait_recv()
    ux_cp(3).start()
    back_block(ag.slots[1])
    ag.step3()
    spread(ag.slots[2])
    back_block(ag.slots[2])
    outs += [net.here(e_v, e_o), net.here(a_v, da_o), net.here(b_v, db_o)]
    for k in far_first:
        o_cp(k, peer[k]).wait_recv()
        for b in range(4):
            ex_cp(k, b).wait_recv()
    ux_cp(1).wait_recv()
    ux_cp(3).wait_recv()
    for c in outs:
        c.wait()
    for k in far_first:
        o_cp(k, tx).wait_send()
        ux_cp(k).wait_send()
        for b in range(4):
            ex_cp(k, b).wait_send()
    ag.drain()
    rsc.drain()


def call_b(u, wd, h, dh2, dn2, a, b, gains):
    tokens, ff = u.shape
    sub, dim = h.shape
    s = jax.ShapeDtypeStruct
    shapes = (s((tokens, dim), BF16), s((tokens, ff), BF16), s((tokens, ff), BF16), s((sub, dim), BF16), s((sub, dim), F32),
              s((tokens, dim // 4), BF16), s((8, dim), F32), s((3, tokens, ff), BF16), s((3, tokens, dim // 4), BF16))
    return pl.pallas_call(
        kernel_b, out_shape=shapes, in_specs=[ANY] * 8, out_specs=[ANY] * len(shapes),
        scratch_shapes=[
            VMEM((tokens, ff), BF16), VMEM((ff, dim), BF16), VMEM((sub, dim), BF16), VMEM((sub, dim), BF16), VMEM((sub, dim), F32),
            VMEM((tokens, ff), BF16), VMEM((tokens, ff), BF16), VMEM((8, dim), F32), VMEM((tokens, dim), BF16), VMEM((tokens, dim), BF16),
            VMEM((5 * sub, dim), BF16), VMEM((sub, dim), BF16), VMEM((sub, dim), BF16), VMEM((sub, dim), F32), VMEM((8, dim), F32),
            pltpu.SemaphoreType.DMA((40,)), pltpu.SemaphoreType.DMA((40,)), pltpu.SemaphoreType.DMA((20,))],
        compiler_params=pltpu.CompilerParams(collective_id=1, has_side_effects=True, vmem_limit_bytes=VMEM_LIMIT),
        cost_estimate=pl.CostEstimate(flops=20 * tokens * dim * ff, bytes_accessed=60000000, transcendentals=0), name="phase_b",
    )(u, wd, h, dh2, dn2, a, b, gains)


ROWS_ROWS = (((0,), (0,)), ((), ()))


class GradReduce:
    def __init__(self, net, peer, tile, tiles, st3, st1, cross, stage, got2, got0, got_y, out, out_tiles):
        self.net, self.peer, self.tile, self.tiles = net, peer, tile, tiles
        self.st3, self.st1, self.cross, self.stage = st3, st1, cross, stage
        self.got2, self.got0, self.got_y, self.out, self.out_tiles = got2, got0, got_y, out, out_tiles
        self.base = net.take(3)
        self.w = out.shape[1] // tiles

    def cp(self, i):
        src, dst, to = ((self.st3, self.got2, 1), (self.st1, self.got0, 1), (self.cross, self.got_y, 2))[i]
        return self.net.copy(src, dst, self.base + i, self.base + i, tx=self.peer[to])

    def fill(self, k, ref):
        @pl.loop(0, self.tiles)
        def _(j):
            ref[:, ds(j * self.w, self.w)] = self.tile(k, j).astype(BF16)

    def step3(self):
        self.fill(3, self.st3)
        self.cp(0).start()

    def step1(self):
        self.fill(1, self.st1)
        self.cp(1).start()

    def step2(self):
        self.cp(0).wait_recv()
        self.net.here(self.got2, self.stage).wait()

        @pl.loop(0, self.tiles)
        def _(j):
            cols = ds(j * self.w, self.w)
            self.cross[:, cols] = (self.tile(2, j) + self.stage[:, cols].astype(F32)).astype(BF16)

        self.cp(2).start()

    def step0(self):
        self.cp(1).wait_recv()
        self.net.here(self.got0, self.stage).wait()
        for j in range(self.tiles):
            cols = pl.ds(j * self.w, self.w)
            if j >= 2:
                self.copies[j - 2].wait()
            else:
                if j == 0:
                    self.copies = []
            place = self.out_tiles.at[j % 2, :, pl.ds(0, self.w)]
            self.out_tiles[j % 2, :, pl.ds(0, self.w)] = self.tile(0, j) + self.stage[:, cols].astype(F32)
            self.copies.append(self.net.here(place, self.out.at[:, cols]))
        for c in self.copies[-2:]:
            c.wait()

    def sent_locally(self):
        self.cp(0).wait_send()
        self.cp(1).wait_send()

    def finish(self):
        self.cp(2).wait_send()
        self.cp(2).wait_recv()


def kernel_c(q_width, da_h, db_h, wg_h, wu_h, n_h, u_h, ux_h, e_h, ex_h, n2_h, eq_h, wq_h, h_h, dres_h, g_h, dga_h, cosh, sinh, swaph,
             wgo, wgy, wuo, wuy, wdo, wqo, wqy, q_o, dh_o, dg_o, g2, g0, u2, u0, q2, q0, qx,
             wg_v, wu_v, da_v, db_v, n_v, p_v, rbuf, n2_v, st3, st1, cross_g, cross_u, stage, tiles_v, dres_v, wq_v, eq_v,
             gains, dg_v, dgr, dgz, cos_v, sin_v, swap_v, send, recv, local):
    dp, z, tx, peer = places()
    tokens, ff = da_v.shape
    sub, dim = dres_v.shape
    dt = dim // 4
    width = eq_v.shape[1]
    tile = ff // 4
    dtile = min(512, dim)
    qt = min(256, tile)
    far_first = (2, 3, 1)
    net = Wires(send, recv, local)
    n2_in = net.here(n2_h, n2_v.at[ds(z * sub, sub), :])
    first = [net.here(n_h, n_v), net.here(da_h, da_v)]
    second = [net.here(db_h, db_v), net.here(wg_h, wg_v), net.here(wu_h, wu_v)]
    third = [net.here(wq_h, wq_v), net.here(eq_h, eq_v), net.here(dres_h, dres_v), net.here(g_h, gains),
             net.here(dga_h, dg_v.at[pl.ds(8, 8), :]), net.here(cosh, cos_v), net.here(sinh, sin_v), net.here(swaph, swap_v)]
    sem = pltpu.get_barrier_semaphore()
    zs = tuple((z + i) % 4 for i in range(4))
    for i in (1, 2, 3):
        pl.semaphore_signal(sem, inc=1, device_id={"tx": peer[i]}, device_id_type=MESH)
        pl.semaphore_signal(sem, inc=1, device_id={"ty": zs[i]}, device_id_type=MESH)
    pl.semaphore_wait(sem, 6)
    rsc = LineScatter(net, p_v, rbuf, sub, z)
    ag = LineGather(net, n2_v, sub, z)
    q_id, h_id, t_id, z_id = net.take(4), net.take(4), net.take(4), net.take(4)

    def grad_tile(lhs, rhs, w):
        def go(k, j):
            cols = pl.ds(j * w, w) if isinstance(j, int) else ds(j * w, w)
            return dot(lhs[:, pl.ds(k * dt, dt)], rhs[:, cols], ROWS_ROWS)
        return go

    gate = GradReduce(net, peer, grad_tile(n_v, da_v, tile), ff // tile, st3, st1, cross_g, stage, g2, g0, wgy, wgo, tiles_v)
    up = GradReduce(net, peer, grad_tile(n_v, db_v, tile), ff // tile, st3, st1, cross_u, stage, u2, u0, wuy, wuo, tiles_v)
    half = tokens // 2

    def corner(r, c):
        return da_v.at[pl.ds(r * dt, dt), pl.ds(c * width, width)]

    qkv = GradReduce(net, peer, grad_tile(n2_v, eq_v, qt), width // qt, corner(0, 0), corner(1, 0), corner(0, 1), corner(1, 1),
                     q2, q0, wqy, wqo, tiles_v)

    def dn_block(b):
        rows = ds(b * sub, sub)

        @pl.loop(0, dim // dtile)
        def _(j):
            wr = ds(j * dtile, dtile)
            p_v[rows, wr] = (dot(da_v[rows, :], wg_v[wr, :], NT_DIMS) + dot(db_v[rows, :], wu_v[wr, :], NT_DIMS)).astype(BF16)

    n2_in.wait()
    ag.start()
    for c in first:
        c.wait()
    gate.step3()
    gate.step1()
    gate.step2()
    for c in second:
        c.wait()
    dn_block(ag.slots[2])
    rsc.send_end(2)
    ag.step1()
    dn_block(ag.slots[1])
    rsc.send_end(1)
    dn_block(ag.slots[0])
    rsc.send_end(0)
    rsc.send_mid(2)
    dn_block(z)
    gate.step0()
    gate.sent_locally()
    up.step3()
    up.step1()
    ag.step2()
    up.step2()
    rsc.send_mid(1)
    rsc.send_mid(0)

    e_in = [net.here(e_h.at[:, pl.ds(0, dt)], wu_v.at[pl.ds(0, tokens), pl.ds(0, dt)])]
    for k in (1, 2, 3):
        e_in.append(net.here(ex_h.at[k - 1], wu_v.at[pl.ds(0, tokens), pl.ds(k * dt, dt)]))

    def u_place(j, k):
        return wg_v.at[pl.ds((j % 2) * tokens, tokens), pl.ds(k * tile, tile)]

    def u_load(j):
        cols = pl.ds(j * tile, tile)
        return [net.here(u_h.at[:, cols] if k == 0 else ux_h.at[k - 1, :, cols], u_place(j, k)) for k in range(4)]

    def down_tile(j, slot, loads):
        for c in loads:
            c.wait()
        acc = None
        for k in range(4):
            part = dot(u_place(j, k)[...], wu_v[pl.ds(0, tokens), pl.ds(k * dt, dt)], ROWS_ROWS)
            acc = part if acc is None else acc + part
        tiles_v[slot, pl.ds(0, tile), pl.ds(0, dt)] = acc
        return net.here(tiles_v.at[slot, pl.ds(0, tile), pl.ds(0, dt)], wdo.at[pl.ds(j * tile, tile), :])

    up.step0()
    up.sent_locally()
    h_in = net.here(h_h, st3.at[pl.ds(0, sub), :])
    n_tiles = ff // tile
    loads = {0: u_load(0)}
    if n_tiles > 1:
        loads[1] = u_load(1)
    for c in e_in:
        c.wait()
    done = {0: down_tile(0, 0, loads[0])}
    if n_tiles > 1:
        done[1] = down_tile(1, 1, loads[1])
    for c in third:
        c.wait()
    ag.step3()

    @pl.loop(0, 4)
    def _(b):
        rows = ds(b * sub, sub)

        @pl.loop(0, width // qt)
        def _(j):
            cols = ds(j * qt, qt)
            n_v[rows, cols] = dot(n2_v[rows, :], wq_v[:, cols]).astype(BF16)

    def q_cp(k, block):
        return net.copy(n_v.at[ds(peer[k] * sub, sub), pl.ds(0, width)], qx.at[ds(block * sub, sub), :], q_id + k, q_id + k, tx=peer[k])

    for k in far_first:
        q_cp(k, tx).start()
    q_own = net.here(n_v.at[ds(tx * sub, sub), pl.ds(0, width)], qx.at[ds(tx * sub, sub), :])
    for c in done.values():
        c.wait()
    qkv.step3()
    qkv.step1()
    qkv.step2()
    h_in.wait()
    rsc.finish()
    dg_v[pl.ds(0, 8), :] = jnp.zeros((8, dim), F32)
    step = 16

    def norm_rows(right, left):
        @pl.loop(0, sub // step)
        def _(r):
            view = ds(r * step, step)
            dy = p_v[ds(z * sub + r * step, step), :].astype(F32)
            if right:
                dy += rbuf[ds(z * sub + r * step, step), :].astype(F32)
            if left:
                dy += rbuf[ds(4 * sub + r * step, step), :].astype(F32)
            x = st3[view, :].astype(F32)
            inv = lax.rsqrt(jnp.sum(x * x, axis=1, keepdims=True) / dim + NORM_EPS)
            xhat = x * inv
            gain = gains[0:1, :]
            part = dy * xhat
            dg_v[pl.ds(0, 8), :] += part[:8] + part[8:]
            inner = jnp.sum(part * gain, axis=1, keepdims=True) / dim
            db_v[view, :] = (dres_v[view, :] + inv * (dy * gain) - xhat * (inv * inner)).astype(BF16)

    @pl.when(z == 0)
    def _():
        norm_rows(True, False)

    @pl.when(z == 3)
    def _():
        norm_rows(False, True)

    @pl.when(mid(z))
    def _():
        norm_rows(True, True)

    def h_cp(k, block):
        return net.copy(db_v.at[pl.ds(0, sub), pl.ds(k * dt, dt)], dh_o.at[ds(block * sub, sub), :], h_id + k, h_id + k, tx=peer[k])

    def t_cp(k):
        return net.copy(dg_v.at[:, pl.ds(k * dt, dt)], dgr.at[k], t_id + k, t_id + k, tx=peer[k])

    def z_cp(i):
        return net.copy(dgr.at[0], dgz.at[i], z_id + i, z_id + i, ty=zs[i])

    for k in far_first:
        t_cp(k).start()
    for k in far_first:
        h_cp(k, tx).start()
    h_own = net.here(db_v.at[pl.ds(0, sub), pl.ds(0, dt)], dh_o.at[ds(tx * sub, sub), :])
    qkv.step0()
    for j in range(2, n_tiles):
        loads[j] = u_load(j)
    done = [down_tile(j, j % 2, loads[j]) for j in range(2, n_tiles)]
    for k in far_first:
        q_cp(k, peer[k]).wait_recv()
    q_own.wait()
    net.here(qx, n_v.at[:, pl.ds(width, width)]).wait()
    turned = n_v.at[:, pl.ds(width, width)]
    turn(turned, turned, tokens, width, q_width, cos_v, sin_v, swap_v, False)
    q_out = net.here(turned, q_o)
    for k in far_first:
        t_cp(k).wait_recv()
    dgr[0] = dg_v[:, pl.ds(0, dt)] + dgr[1] + dgr[2] + dgr[3]
    for i in (1, 2, 3):
        z_cp(i).start()
    for i in (1, 2, 3):
        z_cp(i).wait_recv()
    dgz[0] = dgr[0] + dgz[1] + dgz[2] + dgz[3]
    dg_out = net.here(dgz.at[0], dg_o)
    for k in far_first:
        h_cp(k, peer[k]).wait_recv()
    for c in done + [q_out, dg_out, h_own]:
        c.wait()
    gate.finish()
    up.finish()
    qkv.sent_locally()
    qkv.finish()
    for k in far_first:
        q_cp(k, tx).wait_send()
        h_cp(k, tx).wait_send()
        t_cp(k).wait_send()
        z_cp(k).wait_send()
    ag.drain()
    rsc.drain()


def call_c(q_width, *args):
    tokens, ff = args[0].shape
    sub, dim = args[9].shape
    dt, width = dim // 4, args[10].shape[1]
    tile = ff // 4
    s = jax.ShapeDtypeStruct
    wf, wb = s((dt, ff), F32), s((dt, ff), BF16)
    qf, qb = s((dt, width), F32), s((dt, width), BF16)
    shapes = (wf, wb, wf, wb, s((ff, dt), F32), qf, qb, s((tokens, width), BF16), s((tokens, dt), BF16), s((16, dt), F32),
              wb, wb, wb, wb, qb, qb, s((tokens, width), BF16))
    return pl.pallas_call(
        functools.partial(kernel_c, q_width), out_shape=shapes, in_specs=[ANY] * len(args), out_specs=[ANY] * len(shapes),
        scratch_shapes=[
            VMEM((dim, ff), BF16), VMEM((dim, ff), BF16), VMEM((tokens, ff), BF16), VMEM((tokens, ff), BF16), VMEM((tokens, dim), BF16),
            VMEM((tokens, dim), BF16), VMEM((5 * sub, dim), BF16), VMEM((tokens, dim), BF16),
            VMEM((dt, ff), BF16), VMEM((dt, ff), BF16), VMEM((dt, ff), BF16), VMEM((dt, ff), BF16), VMEM((dt, ff), BF16),
            VMEM((2, max(dt, tile), max(dt, tile)), F32), VMEM((sub, dim), F32), VMEM((dim, width), BF16), VMEM((tokens, width), BF16),
            VMEM((8, dim), F32), VMEM((16, dim), F32), VMEM((4, 16, dt), F32), VMEM((4, 16, dt), F32), VMEM((2 * tokens, 128), F32), VMEM((2 * tokens, 128), F32), VMEM((128, 128), BF16),
            pltpu.SemaphoreType.DMA((48,)), pltpu.SemaphoreType.DMA((48,)), pltpu.SemaphoreType.DMA((72,))],
        compiler_params=pltpu.CompilerParams(collective_id=2, has_side_effects=True, vmem_limit_bytes=VMEM_LIMIT),
        cost_estimate=pl.CostEstimate(flops=20 * tokens * dim * ff, bytes_accessed=100000000, transcendentals=0), name="phase_c",
    )(*args)


def solution(mesh):
    def local_step(hidden, positions, g_ffn, w_gate, w_up, w_down, g_attn, w_q, w_kv, grad_h2, grad_q, grad_kv):
        tokens, dt = hidden.shape
        q_heads, head_dim = w_q.shape[1:]
        kv_heads = w_kv.shape[1]
        q_width, kv_width = q_heads * head_dim, kv_heads * head_dim
        width = q_width + kv_width

        lane = jnp.arange(128)
        inv_freq = ROPE_BASE ** (-((lane % head_dim) // 2 * 2).astype(F32) / head_dim)
        angles = positions.astype(F32)[:, None] * inv_freq[None, :]
        turned = jnp.where(lax.axis_index("ty") < mesh.shape["ty"] // 2, angles, 0.0)
        angles = jnp.concatenate([angles, turned])
        cos_t = jnp.cos(angles)
        swap = (lane[:, None] == (lane + 1 - lane % 2 * 2)[None, :]).astype(BF16)
        sin_t = jnp.sin(angles) * jnp.where(lane % 2 == 0, -1.0, 1.0)[None, :]

        back = jnp.concatenate([grad_q.reshape(tokens, q_width), grad_kv.reshape(tokens, kv_width)], axis=1)
        w_qkv_own = jnp.concatenate([w_q.reshape(dt, q_width), w_kv.reshape(dt, kv_width)], axis=1)
        gin = jnp.concatenate([jnp.stack([g_ffn, g_attn]).astype(F32), jnp.zeros((6, dt), F32)])

        (normed_all, a_all, b_all, u_all, gate_w, up_w, down_w, w_qkv, back_all, h_rows, dh2_rows, dn2_rows, gains) = call_a(
            q_width, hidden, back, cos_t, sin_t, swap, grad_h2, w_gate, w_up, w_down, w_qkv_own, gin)
        res_all, grad_gate, grad_up, normed2, grad_res, resid_out, gattn8, u_other, e_other = call_b(
            u_all, down_w, h_rows, dh2_rows, dn2_rows, a_all, b_all, gains)
        (wg_own, wg_far, wu_own, wu_far, grad_wdown, wq_own, wq_far, qkv_out, grad_hidden, gain_grads, *_) = call_c(
            q_width, grad_gate, grad_up, gate_w, up_w, normed_all, u_all, u_other, res_all, e_other, normed2, back_all, w_qkv,
            h_rows, grad_res, gains, gattn8, cos_t, sin_t, swap)
        grad_wgate = wg_own + wg_far.astype(F32)
        grad_wup = wu_own + wu_far.astype(F32)
        grad_wqkv = wq_own + wq_far.astype(F32)
        grad_wq = grad_wqkv[:, :q_width].reshape(dt, q_heads, head_dim)
        grad_wkv = grad_wqkv[:, q_width:].reshape(dt, kv_heads, head_dim)
        q_out = qkv_out[:, :q_width].reshape(tokens, q_heads, head_dim)
        kv_out = qkv_out[:, q_width:].reshape(tokens, kv_heads, head_dim)
        grad_gffn = jnp.sum(gain_grads[:8], axis=0)
        grad_gattn = jnp.sum(gain_grads[8:], axis=0)
        return (resid_out, q_out, kv_out, grad_hidden, grad_gffn, grad_gattn, grad_wgate, grad_wup, grad_wdown, grad_wq, grad_wkv)

    row_spec = P(("dp", "ty"), "tx")
    head_spec = P(("dp", "tx"), "ty", None)
    in_specs = (row_spec, P(("dp", "tx")), P("tx"), P("tx", "ty"), P("tx", "ty"), P("ty", "tx"), P("tx"), P("tx", "ty", None), P("tx", "ty", None), row_spec, head_spec, head_spec)
    out_specs = (row_spec, head_spec, head_spec, row_spec, P(("dp", "tx")), P(("dp", "tx")), P(("dp", "tx"), "ty"), P(("dp", "tx"), "ty"), P(("dp", "ty"), "tx"), head_spec, head_spec)
    return jax.shard_map(local_step, mesh=mesh, in_specs=in_specs, out_specs=out_specs, check_vma=False)
```

```python
import functools

import jax
import jax.numpy as jnp
from jax import lax
from jax.experimental import pallas as pl
from jax.experimental.pallas import tpu as pltpu
from jax.sharding import PartitionSpec as P

NORM_EPS = 1e-5
ROPE_BASE = 10000.0
F32 = jnp.float32
BF16 = jnp.bfloat16


def dot(a, b, dims=(((1,), (0,)), ((), ()))):
    return lax.dot_general(a, b, dims, preferred_element_type=F32)


MESH = pl.DeviceIdType.MESH
ANY = pl.BlockSpec(memory_space=pl.ANY)
VMEM = pltpu.VMEM
NT_DIMS = (((1,), (1,)), ((), ()))
VMEM_LIMIT = 67000000


def ds(start, size, align=None):
    if isinstance(start, int):
        return pl.ds(start, size)
    return pl.ds(pl.multiple_of(start, align or size), size)


def mid(z):
    return jnp.logical_and(z > 0, z < 3)


def end(z):
    return jnp.logical_or(z == 0, z == 3)


def slots(z):
    return (z + 1 - 2 * (z % 2), 2 - z // 2, 3 - 3 * (z // 2))


def turn(src, dst, rows, width, q_width, table_ref, swap_ref, back):
    step = rows // 4

    @pl.loop(0, 4)
    def _(r):
        for c in range(width // 128):
            cols = pl.ds(c * 128, 128)
            table = ds(r * 128 + (0 if c * 128 < q_width else 512), 128)
            x = src[ds(r * step, step), cols]
            main = x.astype(F32) * table_ref[:, table]
            side = dot(x, swap_ref[...]) * table_ref[:, ds(r * 128 + (1024 if c * 128 < q_width else 1536), 128)]
            dst[ds(r * step, step), cols] = (main - side if back else main + side).astype(BF16)


class Wires:
    def __init__(self, send, recv, local):
        self.send, self.recv, self.local = send, recv, local
        self.n_remote = 0
        self.n_local = 0

    def take(self, n=1):
        base = self.n_remote
        self.n_remote += n
        assert self.n_remote <= self.send.shape[0]
        return base

    def copy(self, src, dst, si, ri, **dev):
        return pltpu.make_async_remote_copy(
            src_ref=src, dst_ref=dst, send_sem=self.send.at[si], recv_sem=self.recv.at[ri],
            device_id=dev, device_id_type=MESH)

    def here(self, src, dst):
        i = self.n_local
        self.n_local += 1
        assert i < self.local.shape[0]
        c = pltpu.make_async_copy(src, dst, self.local.at[i])
        c.start()
        return c


def entry_barrier(axes, z):
    sem = pltpu.get_barrier_semaphore()
    for dev in axes:
        pl.semaphore_signal(sem, inc=1, device_id=dev, device_id_type=MESH)

    @pl.when(z > 0)
    def _():
        pl.semaphore_signal(sem, inc=1, device_id={"ty": z - 1}, device_id_type=MESH)

    @pl.when(z < 3)
    def _():
        pl.semaphore_signal(sem, inc=1, device_id={"ty": z + 1}, device_id_type=MESH)

    @pl.when(mid(z))
    def _():
        pl.semaphore_wait(sem, len(axes) + 2)

    @pl.when(end(z))
    def _():
        pl.semaphore_wait(sem, len(axes) + 1)


class LineGather:
    def __init__(self, net, buf, rows, z, off=0, part=None):
        self.net, self.buf, self.rows, self.z, self.off, self.part = net, buf, rows, z, off, part or rows
        self.base = net.take(8)
        self.slots = slots(z)

    def blk(self, b):
        return self.buf.at[ds(b * self.rows + self.off, self.part), :]

    def cp(self, b, side, target):
        return self.net.copy(self.blk(b), self.blk(b), self.base + side * 4 + b, self.base + b, ty=target)

    def start(self):
        z = self.z

        @pl.when(z < 3)
        def _():
            self.cp(z, 0, z + 1).start()

        @pl.when(z > 0)
        def _():
            self.cp(z, 1, z - 1).start()

    def take(self, i):
        b = self.slots[i]
        self.cp(b, 0, self.z).wait_recv()

    def forward(self, i):
        z, b = self.z, self.slots[i]
        target = 3 - z if i == 0 else 3 * (z - 1)
        self.cp(b, 0, target).start()

    def step1(self):
        self.take(0)

        @pl.when(mid(self.z))
        def _():
            self.forward(0)
            self.take(1)
            self.forward(1)

    def step2(self):
        @pl.when(end(self.z))
        def _():
            self.take(1)

    def step3_mid(self):
        @pl.when(mid(self.z))
        def _():
            self.take(2)
            self.forward(2)

    def step3_end(self):
        @pl.when(end(self.z))
        def _():
            self.take(2)

    def drain(self):
        z = self.z

        @pl.when(z < 3)
        def _():
            self.cp(z, 0, z + 1).wait_send()

        @pl.when(z > 0)
        def _():
            self.cp(z, 1, z - 1).wait_send()

        @pl.when(mid(z))
        def _():
            for i in range(3):
                self.cp(self.slots[i], 0, 3 - z if i == 0 else 3 * (z - 1)).wait_send()


class LineScatter:
    def __init__(self, net, part, rbuf, rows, z, off=0, size=None):
        self.net, self.part, self.rbuf, self.rows, self.z, self.off, self.size = net, part, rbuf, rows, z, off, size or rows
        self.base = net.take(5)
        self.slots = slots(z)
        one = (z % 2) * (1 - z // 2)
        self.dst = (self.slots[0] + (1 - z % 2) * (3 - z), self.slots[1] + 2 * one, self.slots[2])
        self.target = (z + 1 - 2 * (z % 2), 1 + z % 2, 1 + z % 2)

    def cp(self, i):
        return self.net.copy(
            self.part.at[self.view(self.slots[i]), :], self.rbuf.at[self.view(self.dst[i]), :],
            self.base + i, self.base + self.dst[i], ty=self.target[i])

    def view(self, b):
        return ds(b * self.rows + self.off, self.size)

    def wait_slot(self, s):
        view = self.rbuf.at[self.view(s), :]
        self.net.copy(view, view, self.base, self.base + s, ty=self.z).wait_recv()

    def send_end(self, i):
        @pl.when(end(self.z))
        def _():
            self.cp(i).start()

    def send_mid(self, i):
        @pl.when(mid(self.z))
        def _():
            b = self.slots[i]
            self.wait_slot(b)
            step = 16

            @pl.loop(0, self.size // step)
            def _(r):
                view = ds(b * self.rows + self.off + r * step, step)
                self.part[view, :] = (self.part[view, :].astype(F32) + self.rbuf[view, :].astype(F32)).astype(BF16)

            self.cp(i).start()

    def finish(self):
        z = self.z

        @pl.when(z < 3)
        def _():
            self.wait_slot(z)

        @pl.when(z > 0)
        def _():
            self.wait_slot(4)

    def drain(self):
        for i in range(3):
            self.cp(i).wait_send()


class WeightGather:
    def __init__(self, net, w, full, pos, by_rows, chunks):
        self.net, self.w, self.full, self.by_rows = net, w, full, by_rows
        self.dp, self.t1, self.t2 = pos
        self.len = w.shape[0]
        self.width = w.shape[0] if by_rows else w.shape[1]
        self.chunks = chunks
        self.piece = self.len // 2 // chunks
        self.base = net.take(1 + 4 * chunks)

    def dst(self, k, off, n):
        if self.by_rows:
            return self.full.at[ds(k * self.width + off, n, min(n, 16)), :]
        return self.full.at[ds(off, n, 16), pl.ds(k * self.width, self.width)]

    def off(self, half, ch):
        return half * (self.len // 2) + ch * self.piece

    def near(self, ch):
        o = self.off(self.dp, ch)
        i = self.base + 1 + ch
        return self.net.copy(self.w.at[ds(o, self.piece, 16), :], self.dst(2, o, self.piece), i, i, tx=self.t2)

    def cross(self, ch, half):
        o = self.off(half, ch)
        i = self.base + 1 + self.chunks + ch
        return self.net.copy(self.dst(2, o, self.piece), self.dst(2, o, self.piece), i, i, dp=1 - self.dp)

    def diag(self, ch, which, half):
        o = self.off(half, ch)
        i = self.base + 1 + (2 + which) * self.chunks + ch
        return self.net.copy(self.dst(2, o, self.piece), self.dst(3, o, self.piece), i, i, tx=self.t1)

    def mate(self):
        return self.net.copy(self.w, self.dst(1, 0, self.len), self.base, self.base, tx=self.t1)

    def start_y(self):
        for ch in range(self.chunks):
            self.near(ch).start()

    def start_local(self):
        self.own = self.net.here(self.w, self.dst(0, 0, self.len))
        self.mate().start()

    def y_event(self, ch):
        self.near(ch).wait_recv()
        self.cross(ch, self.dp).start()
        self.diag(ch, 0, self.dp).start()

    def x_event(self, ch):
        self.cross(ch, 1 - self.dp).wait_recv()
        self.diag(ch, 1, 1 - self.dp).start()

    def finish(self):
        self.own.wait()
        self.mate().wait_recv()
        for ch in range(self.chunks):
            self.diag(ch, 0, self.dp).wait_recv()
            self.diag(ch, 1, 1 - self.dp).wait_recv()

    def drain(self):
        self.mate().wait_send()
        for ch in range(self.chunks):
            self.near(ch).wait_send()
            self.cross(ch, self.dp).wait_send()
            self.diag(ch, 0, self.dp).wait_send()
            self.diag(ch, 1, 1 - self.dp).wait_send()


def places():
    dp, z, tx = lax.axis_index("dp"), lax.axis_index("ty"), lax.axis_index("tx")
    return dp, z, tx, (tx, tx + 1 - 2 * (tx % 2), (tx + 2) % 4, 3 - tx)


def kernel_ab(q_width, hid, eqh, tabh, swaph, dh2h, wg, wu, wd, wq, gin,
              n_o, da_o, db_o, u_o, wg_o, wu_o, wq_o, eq_o, h_o, g_o, e_o, n2_o, dres_o, home_o, dg_o, ux_o, ex_o,
              rows, dh2_v, n2_v, res_v, dres_v, n_v, a_v, b_v, wg_v, wu_v, wd_v, wq_v, eq_v, p_v, rbuf, rbuf2, gains, dg_v, swap_v, send, recv, local):
    dp, z, tx, peer = places()
    sub, dim = rows.shape
    tokens = 4 * sub
    width = eq_v.shape[1]
    dt = dim // 4
    ff = wg.shape[1]
    wide = min(1024, ff)
    tile = min(512, ff)
    dwide = min(1024, dim)
    dtile = min(512, dim)
    hs = sub // 2
    net = Wires(send, recv, local)
    turn_in = [net.here(eqh, p_v.at[:, pl.ds(0, width)]), net.here(tabh, dres_v), net.here(swaph, swap_v)]
    entry_barrier([{"tx": peer[1]}, {"tx": peer[2]}, {"tx": peer[3]}, {"dp": 1 - dp}], z)

    pos = (dp, peer[1], peer[2])
    far_first = (2, 3, 1)
    g_id, h_id, e_id, d_id, o_id, u_id, x_id = (net.take(4), net.take(4), net.take(4), net.take(4), net.take(4), net.take(3), net.take(24))
    u_v = wg_v.at[pl.ds(0, tokens), :]
    e_v = wg_v.at[pl.ds(tokens, tokens), :]

    def g_cp(k):
        return net.copy(gin, gains.at[:, pl.ds(k * dt, dt)], g_id + k, g_id + k, tx=peer[k])

    def h_cp(k):
        return net.copy(hid.at[ds(peer[k] * sub, sub), :], rows.at[:, pl.ds(k * dt, dt)], h_id + k, h_id + k, tx=peer[k])

    def e_cp(k, block):
        return net.copy(p_v.at[ds(peer[k] * sub, sub), pl.ds(0, width)], eq_v.at[ds(block * sub, sub), :], e_id + k, e_id + k, tx=peer[k])

    def d_cp(k):
        return net.copy(dh2h.at[ds(peer[k] * sub, sub), :], dh2_v.at[:, pl.ds(k * dt, dt)], d_id + k, d_id + k, tx=peer[k])

    def o_cp(k, block):
        return net.copy(res_v.at[:, pl.ds(k * dt, dt)], home_o.at[ds(block * sub, sub), :], o_id + k, o_id + k, tx=peer[k])

    def ux_cp(k):
        src = ux_o.at[1] if k == 3 else u_v
        return net.copy(src, ux_o.at[k - 1], u_id + k - 1, u_id + k - 1, tx=peer[1] if k == 3 else peer[k])

    def ex_cp(k, b, half):
        i = x_id + half * 12 + (k - 1) * 4 + b
        view = ds(b * sub + half * hs, hs)
        return net.copy(wg_v.at[ds(tokens + b * sub + half * hs, hs), pl.ds(k * dt, dt)], ex_o.at[k - 1, view, :], i, i, tx=peer[k])

    gate = WeightGather(net, wg, wg_v, pos, True, 2)
    up = WeightGather(net, wu, wu_v, pos, True, 2)
    down = WeightGather(net, wd, wd_v, pos, False, 2)
    qkv = WeightGather(net, wq, wq_v, pos, True, 1)
    ag = LineGather(net, n_v, sub, z)
    rsc = LineScatter(net, p_v, rbuf, sub, z)
    rs2 = [LineScatter(net, n_v, rbuf2, sub, z, h * hs, hs) for h in range(2)]
    ag2 = [LineGather(net, e_v, sub, z, h * hs, hs) for h in range(2)]

    for k in far_first:
        g_cp(k).start()
    for k in far_first:
        h_cp(k).start()
    g_own = net.here(gin, gains.at[:, pl.ds(0, dt)])
    h_own = net.here(hid.at[ds(tx * sub, sub), :], rows.at[:, pl.ds(0, dt)])
    for w in (qkv, gate, up, down):
        w.start_local()
    for c in turn_in:
        c.wait()
    turn(p_v, p_v, tokens, width, q_width, dres_v, swap_v, True)
    for k in far_first:
        e_cp(k, tx).start()
    e_own = net.here(p_v.at[ds(tx * sub, sub), pl.ds(0, width)], eq_v.at[ds(tx * sub, sub), :])
    for w in (qkv, gate, up, down):
        w.start_y()
    for k in far_first:
        d_cp(k).start()
    d_own = net.here(dh2h.at[ds(tx * sub, sub), :], dh2_v.at[:, pl.ds(0, dt)])

    for k in far_first:
        g_cp(k).wait_recv()
        h_cp(k).wait_recv()
    g_own.wait()
    h_own.wait()

    @pl.loop(0, sub // 16)
    def _(r):
        x = rows[ds(r * 16, 16), :].astype(F32)
        inv = lax.rsqrt(jnp.sum(x * x, axis=1, keepdims=True) / dim + NORM_EPS)
        n_v[ds(z * sub + r * 16, 16), :] = (x * inv * gains[0:1, :]).astype(BF16)

    ag.start()
    outs = [net.here(rows, h_o), net.here(gains, g_o)]
    for k in far_first:
        e_cp(k, peer[k]).wait_recv()
    e_own.wait()
    ag.step1()
    qkv.y_event(0)
    qkv.x_event(0)
    qkv.finish()
    for k in far_first:
        e_cp(k, tx).wait_send()

    def n2_block(b):
        @pl.loop(0, dim // dtile)
        def _(j):
            w = wq_v[ds(j * dtile, dtile), :]
            p_v[ds(b * sub, sub), ds(j * dtile, dtile)] = dot(eq_v[ds(b * sub, sub), :], w, NT_DIMS).astype(BF16)

    for i in (2, 1, 0):
        n2_block(ag.slots[i])
        rsc.send_end(i)
    n2_block(z)
    gate.y_event(0)
    gate.y_event(1)
    gate.x_event(0)
    ag.step2()
    ag.step3_mid()
    up.y_event(0)
    gate.x_event(1)
    gate.finish()

    def gate_block(b):
        @pl.loop(0, ff // wide)
        def _(j):
            cols = ds(j * wide, wide)
            a_v[ds(b * sub, sub), cols] = dot(n_v[ds(b * sub, sub), :], wg_v[:, cols]).astype(BF16)

    def up_block(b):
        @pl.loop(0, ff // wide)
        def _(j):
            cols = ds(j * wide, wide)
            bb = dot(n_v[ds(b * sub, sub), :], wu_v[:, cols]).astype(BF16)
            b_v[ds(b * sub, sub), cols] = bb
            aa = a_v[ds(b * sub, sub), cols].astype(F32)
            wg_v[ds(b * sub, sub), cols] = (aa * jax.nn.sigmoid(aa) * bb.astype(F32)).astype(BF16)

    wg_out = net.here(wg_v, wg_o)
    outs += [net.here(wq_v, wq_o), net.here(eq_v, eq_o)]
    gate_block(z)
    gate_block(ag.slots[0])
    rsc.send_mid(2)
    gate_block(ag.slots[1])
    up.y_event(1)
    up.x_event(0)
    ag.step3_end()
    gate_block(ag.slots[2])
    n_out = net.here(n_v, n_o)
    wg_out.wait()
    down.y_event(0)
    up.x_event(1)
    up.finish()
    outs.append(net.here(wu_v, wu_o))
    up_block(z)
    rsc.send_mid(1)
    rsc.send_mid(0)
    up_block(ag.slots[0])
    down.y_event(1)
    down.x_event(0)
    up_block(ag.slots[1])
    up_block(ag.slots[2])
    outs.append(net.here(u_v, u_o))
    ag.drain()
    gate.drain()
    n_out.wait()
    for k in far_first:
        d_cp(k).wait_recv()
    d_own.wait()
    down.x_event(1)
    down.finish()
    ux_cp(2).start()
    ux_cp(1).start()

    def down_block(b):
        @pl.loop(0, dim // dwide)
        def _(j):
            cols = ds(j * dwide, dwide)
            n_v[ds(b * sub, sub), cols] = dot(wg_v[ds(b * sub, sub), :], wd_v[:, cols]).astype(BF16)

    for i in (2, 1, 0):
        down_block(ag.slots[i])
        rs2[0].send_end(i)
    down_block(z)
    dg_v[...] = jnp.zeros_like(dg_v)
    for i in (2, 1, 0):
        rs2[0].send_mid(i)
    rsc.finish()
    step = 16

    def norm_rows(first, right, left):
        @pl.loop(0, hs // step)
        def _(r):
            at = first + r * step
            view, mine = ds(at, step), ds(z * sub + at, step)
            total = rows[view, :].astype(F32) + n_v[mine, :].astype(F32)
            dy = p_v[mine, :].astype(F32)
            if right:
                total += rbuf2[mine, :].astype(F32)
                dy += rbuf[mine, :].astype(F32)
            if left:
                total += rbuf2[ds(4 * sub + at, step), :].astype(F32)
                dy += rbuf[ds(4 * sub + at, step), :].astype(F32)
            resid = total.astype(BF16)
            res_v[view, :] = resid
            x = resid.astype(F32)
            inv = lax.rsqrt(jnp.sum(x * x, axis=1, keepdims=True) / dim + NORM_EPS)
            xhat = x * inv
            gain = gains[1:2, :]
            n2_v[view, :] = (xhat * gain).astype(BF16)
            part = dy * xhat
            dg_v[...] += part[:8] + part[8:]
            inner = jnp.sum(part * gain, axis=1, keepdims=True) / dim
            dres = dh2_v[view, :].astype(F32) + inv * (dy * gain) - xhat * (inv * inner)
            dres_v[view, pl.ds(0, dim)] = dres
            wg_v[ds(tokens + z * sub + at, step), :] = dres.astype(BF16)

    def norm_half(half):
        @pl.when(z == 0)
        def _():
            norm_rows(half * hs, True, False)

        @pl.when(z == 3)
        def _():
            norm_rows(half * hs, False, True)

        @pl.when(mid(z))
        def _():
            norm_rows(half * hs, True, True)

    def spread(b, half):
        for k in far_first:
            ex_cp(k, b, half).start()

    def back_block(b):
        view = ds(b * sub, sub)

        @pl.loop(0, ff // tile)
        def _(j):
            cols = ds(j * tile, tile)
            du = dot(wg_v[ds(tokens + b * sub, sub), :], wd_v[ds(j * tile, tile), :], NT_DIMS)
            aa = a_v[view, cols].astype(F32)
            bb = b_v[view, cols].astype(F32)
            sig = jax.nn.sigmoid(aa)
            a_v[view, cols] = (du * bb * sig * (1.0 + aa * (1.0 - sig))).astype(BF16)
            b_v[view, cols] = (du * aa * sig).astype(BF16)

    s1, s2, s3 = ag.slots
    rs2[0].finish()
    norm_half(0)
    ag2[0].start()
    for i in (2, 1, 0):
        rs2[1].send_end(i)
    spread(z, 0)
    ag2[0].step1()
    rs2[1].send_mid(2)
    ag2[0].step2()
    ag2[0].step3_mid()
    rs2[1].send_mid(1)
    rs2[1].send_mid(0)
    spread(s1, 0)
    spread(s2, 0)
    rs2[1].finish()
    norm_half(1)
    ag2[1].start()
    for k in far_first:
        o_cp(k, tx).start()
    outs += [net.here(res_v.at[:, pl.ds(0, dt)], home_o.at[ds(tx * sub, sub), :]), net.here(n2_v, n2_o), net.here(dres_v.at[:, pl.ds(0, dim)], dres_o), net.here(dg_v, dg_o)]
    spread(z, 1)
    ag2[0].step3_end()
    spread(s3, 0)
    back_block(z)
    ag2[1].step1()
    spread(s1, 1)
    back_block(s1)
    ag2[1].step2()
    ag2[1].step3_mid()
    spread(s2, 1)
    ux_cp(2).wait_recv()
    ux_cp(3).start()
    back_block(s2)
    ag2[1].step3_end()
    spread(s3, 1)
    outs.append(net.here(e_v, e_o))
    back_block(s3)
    outs += [net.here(a_v, da_o), net.here(b_v, db_o)]
    for k in far_first:
        o_cp(k, peer[k]).wait_recv()
        for b in range(4):
            ex_cp(k, b, 0).wait_recv()
            ex_cp(k, b, 1).wait_recv()
    ux_cp(1).wait_recv()
    ux_cp(3).wait_recv()
    for c in outs:
        c.wait()
    for k in far_first:
        g_cp(k).wait_send()
        h_cp(k).wait_send()
        d_cp(k).wait_send()
        o_cp(k, tx).wait_send()
        ux_cp(k).wait_send()
        for b in range(4):
            ex_cp(k, b, 0).wait_send()
            ex_cp(k, b, 1).wait_send()
    for w in (qkv, up, down):
        w.drain()
    rsc.drain()
    for h in range(2):
        rs2[h].drain()
        ag2[h].drain()


def call_ab(q_width, hid, eqh, tab, swap, dh2h, wg, wu, wd, wq, gin):
    tokens, dt = hid.shape
    sub, dim, ff, width = tokens // 4, dt * 4, wg.shape[1], wq.shape[1]
    s = jax.ShapeDtypeStruct
    tok_ff, tok_d, row = s((tokens, ff), BF16), s((tokens, dim), BF16), s((sub, dim), BF16)
    shapes = (tok_d, tok_ff, tok_ff, tok_ff, s((dim, ff), BF16), s((dim, ff), BF16), s((dim, width), BF16), s((tokens, width), BF16),
              row, s((8, dim), F32), tok_d, row, s((sub, dim), F32), s((tokens, dt), BF16), s((8, dim), F32),
              s((3, tokens, ff), BF16), s((3, tokens, dt), BF16))
    vrow, vtok, vff = VMEM((sub, dim), BF16), VMEM((tokens, dim), BF16), VMEM((tokens, ff), BF16)
    return pl.pallas_call(
        functools.partial(kernel_ab, q_width), out_shape=shapes, in_specs=[ANY] * 10, out_specs=[ANY] * len(shapes),
        scratch_shapes=[
            vrow, vrow, vrow, vrow, VMEM((sub, max(dim, 2048)), F32), vtok, vff, vff, VMEM((dim, ff), BF16), VMEM((dim, ff), BF16), VMEM((ff, dim), BF16),
            VMEM((dim, width), BF16), VMEM((tokens, width), BF16), vtok, VMEM((5 * sub, dim), BF16), VMEM((5 * sub, dim), BF16),
            VMEM((8, dim), F32), VMEM((8, dim), F32), VMEM((128, 128), BF16),
            pltpu.SemaphoreType.DMA((136,)), pltpu.SemaphoreType.DMA((136,)), pltpu.SemaphoreType.DMA((40,))],
        compiler_params=pltpu.CompilerParams(collective_id=0, has_side_effects=True, vmem_limit_bytes=VMEM_LIMIT),
        cost_estimate=pl.CostEstimate(flops=20 * tokens * dim * ff, bytes_accessed=100000000, transcendentals=0), name="phase_ab",
    )(hid, eqh, tab, swap, dh2h, wg, wu, wd, wq, gin)


ROWS_ROWS = (((0,), (0,)), ((), ()))


class GradReduce:
    def __init__(self, net, peer, tile, tiles, st3, st1, cross, stage, got2, got0, got_y, out, out_tiles):
        self.net, self.peer, self.tile, self.tiles = net, peer, tile, tiles
        self.st3, self.st1, self.cross, self.stage = st3, st1, cross, stage
        self.got2, self.got0, self.got_y, self.out, self.out_tiles = got2, got0, got_y, out, out_tiles
        self.base = net.take(3)
        self.w = out.shape[1] // tiles

    def cp(self, i):
        src, dst, to = ((self.st3, self.got2, 1), (self.st1, self.got0, 1), (self.cross, self.got_y, 2))[i]
        return self.net.copy(src, dst, self.base + i, self.base + i, tx=self.peer[to])

    def fill(self, k, ref):
        @pl.loop(0, self.tiles)
        def _(j):
            ref[:, ds(j * self.w, self.w)] = self.tile(k, j).astype(BF16)

    def step3(self):
        self.fill(3, self.st3)
        self.cp(0).start()

    def step1(self):
        self.fill(1, self.st1)
        self.cp(1).start()

    def step2(self):
        self.cp(0).wait_recv()
        self.net.here(self.got2, self.stage).wait()

        @pl.loop(0, self.tiles)
        def _(j):
            cols = ds(j * self.w, self.w)
            self.cross[:, cols] = (self.tile(2, j) + self.stage[:, cols].astype(F32)).astype(BF16)

        self.cp(2).start()

    def step0(self):
        self.cp(1).wait_recv()
        self.net.here(self.got0, self.stage).wait()
        for j in range(self.tiles):
            cols = pl.ds(j * self.w, self.w)
            if j >= 2:
                self.copies[j - 2].wait()
            else:
                if j == 0:
                    self.copies = []
            place = self.out_tiles.at[j % 2, :, pl.ds(0, self.w)]
            self.out_tiles[j % 2, :, pl.ds(0, self.w)] = self.tile(0, j) + self.stage[:, cols].astype(F32)
            self.copies.append(self.net.here(place, self.out.at[:, cols]))
        for c in self.copies[-2:]:
            c.wait()

    def sent_locally(self):
        self.cp(0).wait_send()
        self.cp(1).wait_send()

    def finish(self):
        self.cp(2).wait_send()
        self.cp(2).wait_recv()


def kernel_c(q_width, da_h, db_h, wg_h, wu_h, n_h, u_h, ux_h, e_h, ex_h, n2_h, eq_h, wq_h, h_h, dres_h, g_h, dga_h, tabh, swaph,
             wgo, wgy, wuo, wuy, wdo, wqo, wqy, q_o, dh_o, dg_o, g2, g0, u2, u0, q2, q0, qx,
             wg_v, wu_v, da_v, db_v, n_v, p_v, rbuf, n2_v, st3, st1, cross_g, cross_u, stage, tiles_v, dres_v, wq_v, eq_v,
             gains, dg_v, dgr, dgz, tab_v, swap_v, send, recv, local):
    dp, z, tx, peer = places()
    tokens, ff = da_v.shape
    sub, dim = dres_v.shape
    dt = dim // 4
    width = eq_v.shape[1]
    tile = ff // 4
    dtile = min(512, dim)
    qt = min(256, tile)
    far_first = (2, 3, 1)
    net = Wires(send, recv, local)
    n2_in = net.here(n2_h, n2_v.at[ds(z * sub, sub), :])
    first = [net.here(n_h, n_v), net.here(da_h, da_v)]
    second = [net.here(db_h, db_v), net.here(wg_h, wg_v), net.here(wu_h, wu_v)]
    third = [net.here(wq_h, wq_v), net.here(eq_h, eq_v), net.here(dres_h, dres_v), net.here(g_h, gains),
             net.here(dga_h, dg_v.at[pl.ds(8, 8), :]), net.here(tabh, tab_v), net.here(swaph, swap_v)]
    sem = pltpu.get_barrier_semaphore()
    zs = tuple((z + i) % 4 for i in range(4))
    for i in (1, 2, 3):
        pl.semaphore_signal(sem, inc=1, device_id={"tx": peer[i]}, device_id_type=MESH)
        pl.semaphore_signal(sem, inc=1, device_id={"ty": zs[i]}, device_id_type=MESH)
    pl.semaphore_wait(sem, 6)
    rsc = LineScatter(net, p_v, rbuf, sub, z)
    ag = LineGather(net, n2_v, sub, z)
    q_id, h_id, t_id, z_id = net.take(4), net.take(4), net.take(4), net.take(4)

    def grad_tile(lhs, rhs, w):
        def go(k, j):
            cols = pl.ds(j * w, w) if isinstance(j, int) else ds(j * w, w)
            return dot(lhs[:, pl.ds(k * dt, dt)], rhs[:, cols], ROWS_ROWS)
        return go

    gate = GradReduce(net, peer, grad_tile(n_v, da_v, tile), ff // tile, st3, st1, cross_g, stage, g2, g0, wgy, wgo, tiles_v)
    up = GradReduce(net, peer, grad_tile(n_v, db_v, tile), ff // tile, st3, st1, cross_u, stage, u2, u0, wuy, wuo, tiles_v)
    half = tokens // 2

    def corner(r, c):
        return da_v.at[pl.ds(r * dt, dt), pl.ds(c * width, width)]

    qkv = GradReduce(net, peer, grad_tile(n2_v, eq_v, qt), width // qt, corner(0, 0), corner(1, 0), corner(0, 1), corner(1, 1),
                     q2, q0, wqy, wqo, tiles_v)

    def dn_block(b):
        rows = ds(b * sub, sub)

        @pl.loop(0, dim // dtile)
        def _(j):
            wr = ds(j * dtile, dtile)
            p_v[rows, wr] = (dot(da_v[rows, :], wg_v[wr, :], NT_DIMS) + dot(db_v[rows, :], wu_v[wr, :], NT_DIMS)).astype(BF16)

    n2_in.wait()
    ag.start()
    for c in first:
        c.wait()
    gate.step3()
    gate.step1()
    gate.step2()
    for c in second:
        c.wait()
    dn_block(ag.slots[2])
    rsc.send_end(2)
    ag.step1()
    dn_block(ag.slots[1])
    rsc.send_end(1)
    dn_block(ag.slots[0])
    rsc.send_end(0)
    rsc.send_mid(2)
    dn_block(z)
    gate.step0()
    gate.sent_locally()
    up.step3()
    up.step1()
    ag.step2()
    ag.step3_mid()
    up.step2()
    rsc.send_mid(1)
    rsc.send_mid(0)

    e_in = [net.here(e_h.at[:, pl.ds(0, dt)], wu_v.at[pl.ds(0, tokens), pl.ds(0, dt)])]
    for k in (1, 2, 3):
        e_in.append(net.here(ex_h.at[k - 1], wu_v.at[pl.ds(0, tokens), pl.ds(k * dt, dt)]))

    def u_place(j, k):
        return wg_v.at[pl.ds((j % 2) * tokens, tokens), pl.ds(k * tile, tile)]

    def u_load(j):
        cols = pl.ds(j * tile, tile)
        return [net.here(u_h.at[:, cols] if k == 0 else ux_h.at[k - 1, :, cols], u_place(j, k)) for k in range(4)]

    def down_tile(j, slot, loads):
        for c in loads:
            c.wait()
        acc = None
        for k in range(4):
            part = dot(u_place(j, k)[...], wu_v[pl.ds(0, tokens), pl.ds(k * dt, dt)], ROWS_ROWS)
            acc = part if acc is None else acc + part
        tiles_v[slot, pl.ds(0, tile), pl.ds(0, dt)] = acc
        return net.here(tiles_v.at[slot, pl.ds(0, tile), pl.ds(0, dt)], wdo.at[pl.ds(j * tile, tile), :])

    up.step0()
    up.sent_locally()
    h_in = net.here(h_h, st3.at[pl.ds(0, sub), :])
    n_tiles = ff // tile
    loads = {0: u_load(0)}
    if n_tiles > 1:
        loads[1] = u_load(1)
    for c in e_in:
        c.wait()
    done = {0: down_tile(0, 0, loads[0])}
    if n_tiles > 1:
        done[1] = down_tile(1, 1, loads[1])
    for c in third:
        c.wait()
    ag.step3_end()

    @pl.loop(0, 4)
    def _(b):
        rows = ds(b * sub, sub)

        @pl.loop(0, width // qt)
        def _(j):
            cols = ds(j * qt, qt)
            n_v[rows, cols] = dot(n2_v[rows, :], wq_v[:, cols]).astype(BF16)

    def q_cp(k, block):
        return net.copy(n_v.at[ds(peer[k] * sub, sub), pl.ds(0, width)], qx.at[ds(block * sub, sub), :], q_id + k, q_id + k, tx=peer[k])

    for k in far_first:
        q_cp(k, tx).start()
    q_own = net.here(n_v.at[ds(tx * sub, sub), pl.ds(0, width)], qx.at[ds(tx * sub, sub), :])
    for c in done.values():
        c.wait()
    qkv.step3()
    qkv.step1()
    qkv.step2()
    h_in.wait()
    rsc.finish()
    dg_v[pl.ds(0, 8), :] = jnp.zeros((8, dim), F32)
    step = 16

    def norm_rows(right, left):
        @pl.loop(0, sub // step)
        def _(r):
            view = ds(r * step, step)
            dy = p_v[ds(z * sub + r * step, step), :].astype(F32)
            if right:
                dy += rbuf[ds(z * sub + r * step, step), :].astype(F32)
            if left:
                dy += rbuf[ds(4 * sub + r * step, step), :].astype(F32)
            x = st3[view, :].astype(F32)
            inv = lax.rsqrt(jnp.sum(x * x, axis=1, keepdims=True) / dim + NORM_EPS)
            xhat = x * inv
            gain = gains[0:1, :]
            part = dy * xhat
            dg_v[pl.ds(0, 8), :] += part[:8] + part[8:]
            inner = jnp.sum(part * gain, axis=1, keepdims=True) / dim
            db_v[view, :] = (dres_v[view, :] + inv * (dy * gain) - xhat * (inv * inner)).astype(BF16)

    @pl.when(z == 0)
    def _():
        norm_rows(True, False)

    @pl.when(z == 3)
    def _():
        norm_rows(False, True)

    @pl.when(mid(z))
    def _():
        norm_rows(True, True)

    def h_cp(k, block):
        return net.copy(db_v.at[pl.ds(0, sub), pl.ds(k * dt, dt)], dh_o.at[ds(block * sub, sub), :], h_id + k, h_id + k, tx=peer[k])

    def t_cp(k):
        return net.copy(dg_v.at[:, pl.ds(k * dt, dt)], dgr.at[k], t_id + k, t_id + k, tx=peer[k])

    def z_cp(i):
        return net.copy(dgr.at[0], dgz.at[i], z_id + i, z_id + i, ty=zs[i])

    for k in far_first:
        t_cp(k).start()
    for k in far_first:
        h_cp(k, tx).start()
    h_own = net.here(db_v.at[pl.ds(0, sub), pl.ds(0, dt)], dh_o.at[ds(tx * sub, sub), :])
    qkv.step0()
    for j in range(2, n_tiles):
        loads[j] = u_load(j)
    done = [down_tile(j, j % 2, loads[j]) for j in range(2, n_tiles)]
    for k in far_first:
        q_cp(k, peer[k]).wait_recv()
    q_own.wait()
    net.here(qx, n_v.at[:, pl.ds(width, width)]).wait()
    turned = n_v.at[:, pl.ds(width, width)]
    turn(turned, turned, tokens, width, q_width, tab_v, swap_v, False)
    q_out = net.here(turned, q_o)
    for k in far_first:
        t_cp(k).wait_recv()
    dgr[0] = dg_v[:, pl.ds(0, dt)] + dgr[1] + dgr[2] + dgr[3]
    for i in (1, 2, 3):
        z_cp(i).start()
    for i in (1, 2, 3):
        z_cp(i).wait_recv()
    dgz[0] = dgr[0] + dgz[1] + dgz[2] + dgz[3]
    dg_out = net.here(dgz.at[0], dg_o)
    for k in far_first:
        h_cp(k, peer[k]).wait_recv()
    for c in done + [q_out, dg_out, h_own]:
        c.wait()
    gate.finish()
    up.finish()
    qkv.sent_locally()
    qkv.finish()
    for k in far_first:
        q_cp(k, tx).wait_send()
        h_cp(k, tx).wait_send()
        t_cp(k).wait_send()
        z_cp(k).wait_send()
    ag.drain()
    rsc.drain()


def call_c(q_width, *args):
    tokens, ff = args[0].shape
    sub, dim = args[9].shape
    dt, width = dim // 4, args[10].shape[1]
    tile = ff // 4
    s = jax.ShapeDtypeStruct
    wf, wb = s((dt, ff), F32), s((dt, ff), BF16)
    qf, qb = s((dt, width), F32), s((dt, width), BF16)
    shapes = (wf, wb, wf, wb, s((ff, dt), F32), qf, qb, s((tokens, width), BF16), s((tokens, dt), BF16), s((16, dt), F32),
              wb, wb, wb, wb, qb, qb, s((tokens, width), BF16))
    return pl.pallas_call(
        functools.partial(kernel_c, q_width), out_shape=shapes, in_specs=[ANY] * len(args), out_specs=[ANY] * len(shapes),
        scratch_shapes=[
            VMEM((dim, ff), BF16), VMEM((dim, ff), BF16), VMEM((tokens, ff), BF16), VMEM((tokens, ff), BF16), VMEM((tokens, dim), BF16),
            VMEM((tokens, dim), BF16), VMEM((5 * sub, dim), BF16), VMEM((tokens, dim), BF16),
            VMEM((dt, ff), BF16), VMEM((dt, ff), BF16), VMEM((dt, ff), BF16), VMEM((dt, ff), BF16), VMEM((dt, ff), BF16),
            VMEM((2, max(dt, tile), max(dt, tile)), F32), VMEM((sub, dim), F32), VMEM((dim, width), BF16), VMEM((tokens, width), BF16),
            VMEM((8, dim), F32), VMEM((16, dim), F32), VMEM((4, 16, dt), F32), VMEM((4, 16, dt), F32), VMEM((sub, 2048), F32), VMEM((128, 128), BF16),
            pltpu.SemaphoreType.DMA((48,)), pltpu.SemaphoreType.DMA((48,)), pltpu.SemaphoreType.DMA((72,))],
        compiler_params=pltpu.CompilerParams(collective_id=2, has_side_effects=True, vmem_limit_bytes=VMEM_LIMIT),
        cost_estimate=pl.CostEstimate(flops=20 * tokens * dim * ff, bytes_accessed=100000000, transcendentals=0), name="phase_c",
    )(*args)


def solution(mesh):
    def local_step(hidden, positions, g_ffn, w_gate, w_up, w_down, g_attn, w_q, w_kv, grad_h2, grad_q, grad_kv):
        tokens, dt = hidden.shape
        q_heads, head_dim = w_q.shape[1:]
        kv_heads = w_kv.shape[1]
        q_width, kv_width = q_heads * head_dim, kv_heads * head_dim
        width = q_width + kv_width

        lane = jnp.arange(128)
        inv_freq = ROPE_BASE ** (-((lane % head_dim) // 2 * 2).astype(F32) / head_dim)
        angles = positions.astype(F32)[:, None] * inv_freq[None, :]
        cos_t = jnp.cos(angles)
        swap = (lane[:, None] == (lane + 1 - lane % 2 * 2)[None, :]).astype(BF16)
        sin_t = jnp.sin(angles) * jnp.where(lane % 2 == 0, -1.0, 1.0)[None, :]

        turns = lax.axis_index("ty") < mesh.shape["ty"] // 2
        table = jnp.stack([cos_t, jnp.where(turns, cos_t, 1.0), sin_t, jnp.where(turns, sin_t, 0.0)])
        table = table.reshape(4, 4, tokens // 4, 128).transpose(2, 0, 1, 3).reshape(tokens // 4, 2048)
        back = jnp.concatenate([grad_q.reshape(tokens, q_width), grad_kv.reshape(tokens, kv_width)], axis=1)
        w_qkv_own = jnp.concatenate([w_q.reshape(dt, q_width), w_kv.reshape(dt, kv_width)], axis=1)
        gin = jnp.concatenate([jnp.stack([g_ffn, g_attn]).astype(F32), jnp.zeros((6, dt), F32)])

        (normed_all, grad_gate, grad_up, u_all, gate_w, up_w, w_qkv, back_all, h_rows, gains, res_all, normed2, grad_res, resid_out, gattn8,
         u_other, e_other) = call_ab(q_width, hidden, back, table, swap, grad_h2, w_gate, w_up, w_down, w_qkv_own, gin)
        (wg_own, wg_far, wu_own, wu_far, grad_wdown, wq_own, wq_far, qkv_out, grad_hidden, gain_grads, *_) = call_c(
            q_width, grad_gate, grad_up, gate_w, up_w, normed_all, u_all, u_other, res_all, e_other, normed2, back_all, w_qkv,
            h_rows, grad_res, gains, gattn8, table, swap)
        grad_wgate = wg_own + wg_far.astype(F32)
        grad_wup = wu_own + wu_far.astype(F32)
        grad_wqkv = wq_own + wq_far.astype(F32)
        grad_wq = grad_wqkv[:, :q_width].reshape(dt, q_heads, head_dim)
        grad_wkv = grad_wqkv[:, q_width:].reshape(dt, kv_heads, head_dim)
        q_out = qkv_out[:, :q_width].reshape(tokens, q_heads, head_dim)
        kv_out = qkv_out[:, q_width:].reshape(tokens, kv_heads, head_dim)
        grad_gffn = jnp.sum(gain_grads[:8], axis=0)
        grad_gattn = jnp.sum(gain_grads[8:], axis=0)
        return (resid_out, q_out, kv_out, grad_hidden, grad_gffn, grad_gattn, grad_wgate, grad_wup, grad_wdown, grad_wq, grad_wkv)

    row_spec = P(("dp", "ty"), "tx")
    head_spec = P(("dp", "tx"), "ty", None)
    in_specs = (row_spec, P(("dp", "tx")), P("tx"), P("tx", "ty"), P("tx", "ty"), P("ty", "tx"), P("tx"), P("tx", "ty", None), P("tx", "ty", None), row_spec, head_spec, head_spec)
    out_specs = (row_spec, head_spec, head_spec, row_spec, P(("dp", "tx")), P(("dp", "tx")), P(("dp", "tx"), "ty"), P(("dp", "tx"), "ty"), P(("dp", "ty"), "tx"), head_spec, head_spec)
    return jax.shard_map(local_step, mesh=mesh, in_specs=in_specs, out_specs=out_specs, check_vma=False)
```

```python
import functools

import jax
import jax.numpy as jnp
from jax import lax
from jax.experimental import pallas as pl
from jax.experimental.pallas import tpu as pltpu
from jax.sharding import PartitionSpec as P

NORM_EPS = 1e-5
ROPE_BASE = 10000.0
F32 = jnp.float32
BF16 = jnp.bfloat16


def dot(a, b, dims=(((1,), (0,)), ((), ()))):
    return lax.dot_general(a, b, dims, preferred_element_type=F32)


MESH = pl.DeviceIdType.MESH
ANY = pl.BlockSpec(memory_space=pl.ANY)
VMEM = pltpu.VMEM
NT_DIMS = (((1,), (1,)), ((), ()))
VMEM_LIMIT = 67000000


def ds(start, size, align=None):
    if isinstance(start, int):
        return pl.ds(start, size)
    return pl.ds(pl.multiple_of(start, align or size), size)


def mid(z):
    return jnp.logical_and(z > 0, z < 3)


def end(z):
    return jnp.logical_or(z == 0, z == 3)


def slots(z):
    return (z + 1 - 2 * (z % 2), 2 - z // 2, 3 - 3 * (z // 2))


def turn(src, dst, rows, width, q_width, table_ref, swap_ref, back):
    step = rows // 4

    @pl.loop(0, 4)
    def _(r):
        for c in range(width // 128):
            cols = pl.ds(c * 128, 128)
            table = ds(r * 128 + (0 if c * 128 < q_width else 512), 128)
            x = src[ds(r * step, step), cols]
            main = x.astype(F32) * table_ref[:, table]
            side = dot(x, swap_ref[...]) * table_ref[:, ds(r * 128 + (1024 if c * 128 < q_width else 1536), 128)]
            dst[ds(r * step, step), cols] = (main - side if back else main + side).astype(BF16)


def pick(i, z):
    s1, s2, s3 = slots(z)
    first, last = (3 - i) // 3, (i // 2) * (i % 2)
    return z * first + s1 * ((i % 2) * (1 - i // 2)) + s2 * ((i // 2) * (1 - i % 2)) + s3 * last


class Wires:
    def __init__(self, send, recv, local):
        self.send, self.recv, self.local = send, recv, local
        self.n_remote = 0
        self.n_local = 0

    def take(self, n=1):
        base = self.n_remote
        self.n_remote += n
        assert self.n_remote <= self.send.shape[0]
        return base

    def copy(self, src, dst, si, ri, **dev):
        return pltpu.make_async_remote_copy(
            src_ref=src, dst_ref=dst, send_sem=self.send.at[si], recv_sem=self.recv.at[ri],
            device_id=dev, device_id_type=MESH)

    def here(self, src, dst):
        i = self.n_local
        self.n_local += 1
        assert i < self.local.shape[0]
        c = pltpu.make_async_copy(src, dst, self.local.at[i])
        c.start()
        return c


def entry_barrier(axes, z):
    sem = pltpu.get_barrier_semaphore()
    for dev in axes:
        pl.semaphore_signal(sem, inc=1, device_id=dev, device_id_type=MESH)

    @pl.when(z > 0)
    def _():
        pl.semaphore_signal(sem, inc=1, device_id={"ty": z - 1}, device_id_type=MESH)

    @pl.when(z < 3)
    def _():
        pl.semaphore_signal(sem, inc=1, device_id={"ty": z + 1}, device_id_type=MESH)

    @pl.when(mid(z))
    def _():
        pl.semaphore_wait(sem, len(axes) + 2)

    @pl.when(end(z))
    def _():
        pl.semaphore_wait(sem, len(axes) + 1)


class LineGather:
    def __init__(self, net, buf, rows, z, off=0, part=None):
        self.net, self.buf, self.rows, self.z, self.off, self.part = net, buf, rows, z, off, part or rows
        self.base = net.take(8)
        self.slots = slots(z)

    def blk(self, b):
        return self.buf.at[ds(b * self.rows + self.off, self.part), :]

    def cp(self, b, side, target):
        return self.net.copy(self.blk(b), self.blk(b), self.base + side * 4 + b, self.base + b, ty=target)

    def start(self):
        z = self.z

        @pl.when(z < 3)
        def _():
            self.cp(z, 0, z + 1).start()

        @pl.when(z > 0)
        def _():
            self.cp(z, 1, z - 1).start()

    def take(self, i):
        b = self.slots[i]
        self.cp(b, 0, self.z).wait_recv()

    def forward(self, i):
        z, b = self.z, self.slots[i]
        target = 3 - z if i == 0 else 3 * (z - 1)
        self.cp(b, 0, target).start()

    def step1(self):
        self.take(0)

        @pl.when(mid(self.z))
        def _():
            self.forward(0)
            self.take(1)
            self.forward(1)

    def near_end(self):
        @pl.when(end(self.z))
        def _():
            self.take(0)

    def near_mid(self):
        @pl.when(mid(self.z))
        def _():
            self.take(1)
            self.forward(1)

    def far_mid(self):
        @pl.when(mid(self.z))
        def _():
            self.take(0)
            self.forward(0)

    def step2(self):
        @pl.when(end(self.z))
        def _():
            self.take(1)

    def step3_mid(self):
        @pl.when(mid(self.z))
        def _():
            self.take(2)
            self.forward(2)

    def step3_end(self):
        @pl.when(end(self.z))
        def _():
            self.take(2)

    def drain(self):
        z = self.z

        @pl.when(z < 3)
        def _():
            self.cp(z, 0, z + 1).wait_send()

        @pl.when(z > 0)
        def _():
            self.cp(z, 1, z - 1).wait_send()

        @pl.when(mid(z))
        def _():
            for i in range(3):
                self.cp(self.slots[i], 0, 3 - z if i == 0 else 3 * (z - 1)).wait_send()


class LineScatter:
    def __init__(self, net, part, rbuf, rows, z, off=0, size=None):
        self.net, self.part, self.rbuf, self.rows, self.z, self.off, self.size = net, part, rbuf, rows, z, off, size or rows
        self.base = net.take(5)
        self.slots = slots(z)
        one = (z % 2) * (1 - z // 2)
        self.dst = (self.slots[0] + (1 - z % 2) * (3 - z), self.slots[1] + 2 * one, self.slots[2])
        self.target = (z + 1 - 2 * (z % 2), 1 + z % 2, 1 + z % 2)

    def cp(self, i):
        return self.net.copy(
            self.part.at[self.view(self.slots[i]), :], self.rbuf.at[self.view(self.dst[i]), :],
            self.base + i, self.base + self.dst[i], ty=self.target[i])

    def view(self, b):
        return ds(b * self.rows + self.off, self.size)

    def wait_slot(self, s):
        view = self.rbuf.at[self.view(s), :]
        self.net.copy(view, view, self.base, self.base + s, ty=self.z).wait_recv()

    def send_end(self, i):
        @pl.when(end(self.z))
        def _():
            self.cp(i).start()

    def send_mid(self, i):
        @pl.when(mid(self.z))
        def _():
            b = self.slots[i]
            self.wait_slot(b)
            step = 16

            @pl.loop(0, self.size // step)
            def _(r):
                view = ds(b * self.rows + self.off + r * step, step)
                self.part[view, :] = (self.part[view, :].astype(F32) + self.rbuf[view, :].astype(F32)).astype(BF16)

            self.cp(i).start()

    def finish(self):
        z = self.z

        @pl.when(z < 3)
        def _():
            self.wait_slot(z)

        @pl.when(z > 0)
        def _():
            self.wait_slot(4)

    def drain(self):
        for i in range(3):
            self.cp(i).wait_send()


class WeightGather:
    def __init__(self, net, w, full, pos, by_rows, chunks, direct=0):
        self.net, self.w, self.full, self.by_rows = net, w, full, by_rows
        self.dp, self.t1, self.t2 = pos
        self.len = w.shape[0]
        self.width = w.shape[0] if by_rows else w.shape[1]
        self.chunks = chunks
        self.piece = self.len // 2 // chunks
        self.direct = direct
        self.base = net.take(1 + 4 * chunks + direct)

    def dst(self, k, off, n):
        if self.by_rows:
            return self.full.at[ds(k * self.width + off, n, min(n, 16)), :]
        return self.full.at[ds(off, n, 16), pl.ds(k * self.width, self.width)]

    def off(self, half, ch):
        return half * (self.len // 2) + ch * self.piece

    def near(self, ch):
        o = self.off(self.dp, ch)
        i = self.base + 1 + ch
        return self.net.copy(self.w.at[ds(o, self.piece, 16), :], self.dst(2, o, self.piece), i, i, tx=self.t2)

    def cross(self, ch, half):
        o = self.off(half, ch)
        i = self.base + 1 + self.chunks + ch
        return self.net.copy(self.dst(2, o, self.piece), self.dst(2, o, self.piece), i, i, dp=1 - self.dp)

    def diag(self, ch, which, half):
        o = self.off(half, ch)
        i = self.base + 1 + (2 + which) * self.chunks + ch
        return self.net.copy(self.dst(2, o, self.piece), self.dst(3, o, self.piece), i, i, tx=self.t1)

    def mate(self):
        return self.net.copy(self.w, self.dst(1, 0, self.len), self.base, self.base, tx=self.t1)

    def straight(self, n, half):
        o = self.off(half, self.chunks - 1 - n)
        i = self.base + 1 + 4 * self.chunks + n
        return self.net.copy(self.w.at[ds(o, self.piece, 16), :], self.dst(2, o, self.piece), i, i, tx=self.t2)

    def start_y(self):
        for ch in range(self.chunks):
            self.near(ch).start()
        for n in range(self.direct):
            self.straight(n, 1 - self.dp).start()

    def start_local(self):
        self.own = self.net.here(self.w, self.dst(0, 0, self.len))
        self.mate().start()

    def y_event(self, ch):
        self.near(ch).wait_recv()
        if ch < self.chunks - self.direct:
            self.cross(ch, self.dp).start()
        self.diag(ch, 0, self.dp).start()

    def x_event(self, ch):
        if ch < self.chunks - self.direct:
            self.cross(ch, 1 - self.dp).wait_recv()
        else:
            self.straight(self.chunks - 1 - ch, 1 - self.dp).wait_recv()
        self.diag(ch, 1, 1 - self.dp).start()

    def finish(self):
        self.own.wait()
        self.mate().wait_recv()
        for ch in range(self.chunks):
            self.diag(ch, 0, self.dp).wait_recv()
            self.diag(ch, 1, 1 - self.dp).wait_recv()

    def drain(self):
        self.mate().wait_send()
        for ch in range(self.chunks):
            self.near(ch).wait_send()
            if ch < self.chunks - self.direct:
                self.cross(ch, self.dp).wait_send()
            else:
                self.straight(self.chunks - 1 - ch, 1 - self.dp).wait_send()
            self.diag(ch, 0, self.dp).wait_send()
            self.diag(ch, 1, 1 - self.dp).wait_send()


def places():
    dp, z, tx = lax.axis_index("dp"), lax.axis_index("ty"), lax.axis_index("tx")
    return dp, z, tx, (tx, tx + 1 - 2 * (tx % 2), (tx + 2) % 4, 3 - tx)


def kernel_ab(q_width, hid, eqh, tabh, swaph, dh2h, wg, wu, wd, wq, gin,
              n_o, da_o, db_o, u_o, wg_o, wu_o, wq_o, eq_o, h_o, g_o, e_o, n2_o, dres_o, home_o, dg_o, ux_o, ex_o,
              rows, dh2_v, n2_v, res_v, dres_v, n_v, a_v, b_v, wg_v, wu_v, wd_v, wq_v, eq_v, p_v, rbuf, rbuf2, gains, dg_v, swap_v, send, recv, local):
    dp, z, tx, peer = places()
    sub, dim = rows.shape
    tokens = 4 * sub
    width = eq_v.shape[1]
    dt = dim // 4
    ff = wg.shape[1]
    wide = min(1024, ff)
    tile = min(512, ff)
    dwide = min(1024, dim)
    dtile = min(512, dim)
    hs = sub // 2
    net = Wires(send, recv, local)
    turn_in = [net.here(eqh, p_v.at[:, pl.ds(0, width)]), net.here(tabh, dres_v), net.here(swaph, swap_v)]
    entry_barrier([{"tx": peer[1]}, {"tx": peer[2]}, {"tx": peer[3]}, {"dp": 1 - dp}], z)

    pos = (dp, peer[1], peer[2])
    far_first = (2, 3, 1)
    g_id, h_id, e_id, d_id, o_id, u_id, x_id = (net.take(4), net.take(4), net.take(4), net.take(4), net.take(4), net.take(12), net.take(24))
    u_v = wg_v.at[pl.ds(0, tokens), :]
    e_v = wg_v.at[pl.ds(tokens, tokens), :]

    def g_cp(k):
        return net.copy(gin, gains.at[:, pl.ds(k * dt, dt)], g_id + k, g_id + k, tx=peer[k])

    def h_cp(k):
        return net.copy(hid.at[ds(peer[k] * sub, sub), :], rows.at[:, pl.ds(k * dt, dt)], h_id + k, h_id + k, tx=peer[k])

    def e_cp(k, block):
        return net.copy(p_v.at[ds(peer[k] * sub, sub), pl.ds(0, width)], eq_v.at[ds(block * sub, sub), :], e_id + k, e_id + k, tx=peer[k])

    def d_cp(k):
        return net.copy(dh2h.at[ds(peer[k] * sub, sub), :], dh2_v.at[:, pl.ds(k * dt, dt)], d_id + k, d_id + k, tx=peer[k])

    def o_cp(k, block):
        return net.copy(res_v.at[:, pl.ds(k * dt, dt)], home_o.at[ds(block * sub, sub), :], o_id + k, o_id + k, tx=peer[k])

    def ux_cp(k, b):
        view = ds(b * sub, sub)
        src = ux_o.at[1, view, :] if k == 3 else wg_v.at[view, :]
        i = u_id + (k - 1) * 4 + b
        return net.copy(src, ux_o.at[k - 1, view, :], i, i, tx=peer[1] if k == 3 else peer[k])

    def ex_cp(k, b, half):
        i = x_id + half * 12 + (k - 1) * 4 + b
        view = ds(b * sub + half * hs, hs)
        return net.copy(wg_v.at[ds(tokens + b * sub + half * hs, hs), pl.ds(k * dt, dt)], ex_o.at[k - 1, view, :], i, i, tx=peer[k])

    gate = WeightGather(net, wg, wg_v, pos, True, 2)
    up = WeightGather(net, wu, wu_v, pos, True, 2)
    down = WeightGather(net, wd, wd_v, pos, False, 4, 1)
    qkv = WeightGather(net, wq, wq_v, pos, True, 1)
    ag = LineGather(net, n_v, sub, z)
    rsc = LineScatter(net, p_v, rbuf, sub, z)
    rs2 = [LineScatter(net, n_v, rbuf2, sub, z, h * hs, hs) for h in range(2)]
    ag2 = [LineGather(net, e_v, sub, z, h * hs, hs) for h in range(2)]

    for k in far_first:
        g_cp(k).start()
    for k in far_first:
        h_cp(k).start()
    g_own = net.here(gin, gains.at[:, pl.ds(0, dt)])
    h_own = net.here(hid.at[ds(tx * sub, sub), :], rows.at[:, pl.ds(0, dt)])
    for w in (qkv, gate, up, down):
        w.start_local()
    for c in turn_in:
        c.wait()
    turn(p_v, p_v, tokens, width, q_width, dres_v, swap_v, True)
    for k in far_first:
        e_cp(k, tx).start()
    e_own = net.here(p_v.at[ds(tx * sub, sub), pl.ds(0, width)], eq_v.at[ds(tx * sub, sub), :])
    for w in (qkv, gate, up, down):
        w.start_y()
    for k in far_first:
        d_cp(k).start()
    d_own = net.here(dh2h.at[ds(tx * sub, sub), :], dh2_v.at[:, pl.ds(0, dt)])

    for k in far_first:
        g_cp(k).wait_recv()
        h_cp(k).wait_recv()
    g_own.wait()
    h_own.wait()

    @pl.loop(0, sub // 16)
    def _(r):
        x = rows[ds(r * 16, 16), :].astype(F32)
        inv = lax.rsqrt(jnp.sum(x * x, axis=1, keepdims=True) / dim + NORM_EPS)
        n_v[ds(z * sub + r * 16, 16), :] = (x * inv * gains[0:1, :]).astype(BF16)

    ag.start()
    outs = [net.here(rows, h_o), net.here(gains, g_o)]
    for k in far_first:
        e_cp(k, peer[k]).wait_recv()
    e_own.wait()
    ag.step1()
    qkv.y_event(0)
    qkv.x_event(0)
    qkv.finish()
    for k in far_first:
        e_cp(k, tx).wait_send()

    def n2_block(b):
        @pl.loop(0, dim // dtile)
        def _(j):
            w = wq_v[ds(j * dtile, dtile), :]
            p_v[ds(b * sub, sub), ds(j * dtile, dtile)] = dot(eq_v[ds(b * sub, sub), :], w, NT_DIMS).astype(BF16)

    @pl.loop(0, 4)
    def _(i):
        n2_block(pick(3 - i, z))
        for step in range(3):
            pl.when(i == step)(lambda step=step: rsc.send_end(2 - step))

    gate.y_event(0)
    gate.y_event(1)
    gate.x_event(0)
    ag.step2()
    ag.step3_mid()
    up.y_event(0)
    gate.x_event(1)
    gate.finish()

    def gate_block(b):
        @pl.loop(0, ff // wide)
        def _(j):
            cols = ds(j * wide, wide)
            a_v[ds(b * sub, sub), cols] = dot(n_v[ds(b * sub, sub), :], wg_v[:, cols]).astype(BF16)

    def up_block(b):
        @pl.loop(0, ff // wide)
        def _(j):
            cols = ds(j * wide, wide)
            bb = dot(n_v[ds(b * sub, sub), :], wu_v[:, cols]).astype(BF16)
            b_v[ds(b * sub, sub), cols] = bb
            aa = a_v[ds(b * sub, sub), cols].astype(F32)
            wg_v[ds(b * sub, sub), cols] = (aa * jax.nn.sigmoid(aa) * bb.astype(F32)).astype(BF16)

    wg_out = net.here(wg_v, wg_o)
    outs += [net.here(wq_v, wq_o), net.here(eq_v, eq_o)]
    def gate_events_2():
        rsc.send_mid(2)

    def gate_events_3():
        up.y_event(1)
        up.x_event(0)
        ag.step3_end()

    @pl.loop(0, 4)
    def _(i):
        pl.when(i == 2)(gate_events_2)
        pl.when(i == 3)(gate_events_3)
        gate_block(pick(i, z))

    n_out = net.here(n_v, n_o)
    wg_out.wait()
    down.y_event(0)
    up.x_event(1)
    up.finish()
    outs.append(net.here(wu_v, wu_o))

    def up_events_1():
        rsc.send_mid(1)
        rsc.send_mid(0)

    def up_events_2():
        down.y_event(1)
        down.x_event(0)

    def up_events_3():
        down.y_event(2)
        down.x_event(1)

    @pl.loop(0, 4)
    def _(i):
        pl.when(i == 1)(up_events_1)
        pl.when(i == 2)(up_events_2)
        pl.when(i == 3)(up_events_3)
        b = pick(i, z)
        up_block(b)
        ux_cp(2, b).start()
        ux_cp(1, b).start()

    outs.append(net.here(u_v, u_o))
    ag.drain()
    gate.drain()
    n_out.wait()
    down.y_event(3)
    down.x_event(2)
    down.x_event(3)
    down.finish()

    def down_block(b):
        @pl.loop(0, dim // dwide)
        def _(j):
            cols = ds(j * dwide, dwide)
            n_v[ds(b * sub, sub), cols] = dot(wg_v[ds(b * sub, sub), :], wd_v[:, cols]).astype(BF16)

    @pl.loop(0, 4)
    def _(i):
        down_block(pick(3 - i, z))
        for step in range(3):
            pl.when(i == step)(lambda step=step: rs2[0].send_end(2 - step))

    rs2[1].send_end(2)
    dg_v[...] = jnp.zeros_like(dg_v)
    for k in far_first:
        d_cp(k).wait_recv()
    d_own.wait()
    for i in (2, 1, 0):
        rs2[0].send_mid(i)
    rsc.finish()
    step = 16

    def norm_half(half):
        @pl.loop(0, hs // step)
        def _(r):
            at = half * hs + r * step
            view, mine, far = ds(at, step), ds(z * sub + at, step), ds(4 * sub + at, step)

            def whole(part, got):
                right = jnp.where(z < 3, got[mine, :].astype(F32), 0.0)
                left = jnp.where(z > 0, got[far, :].astype(F32), 0.0)
                return part[mine, :].astype(F32) + right + left

            resid = (rows[view, :].astype(F32) + whole(n_v, rbuf2)).astype(BF16)
            dy = whole(p_v, rbuf)
            res_v[view, :] = resid
            x = resid.astype(F32)
            inv = lax.rsqrt(jnp.sum(x * x, axis=1, keepdims=True) / dim + NORM_EPS)
            xhat = x * inv
            gain = gains[1:2, :]
            n2_v[view, :] = (xhat * gain).astype(BF16)
            part = dy * xhat
            dg_v[...] += part[:8] + part[8:]
            inner = jnp.sum(part * gain, axis=1, keepdims=True) / dim
            dres = dh2_v[view, :].astype(F32) + inv * (dy * gain) - xhat * (inv * inner)
            dres_v[view, pl.ds(0, dim)] = dres
            wg_v[ds(tokens + z * sub + at, step), :] = dres.astype(BF16)

    def spread(b, half):
        for k in far_first:
            ex_cp(k, b, half).start()

    def back_block(b):
        view = ds(b * sub, sub)

        @pl.loop(0, ff // tile)
        def _(j):
            cols = ds(j * tile, tile)
            du = dot(wg_v[ds(tokens + b * sub, sub), :], wd_v[ds(j * tile, tile), :], NT_DIMS)
            aa = a_v[view, cols].astype(F32)
            bb = b_v[view, cols].astype(F32)
            sig = jax.nn.sigmoid(aa)
            a_v[view, cols] = (du * bb * sig * (1.0 + aa * (1.0 - sig))).astype(BF16)
            b_v[view, cols] = (du * aa * sig).astype(BF16)

    s1, s2, s3 = ag.slots
    rs2[0].finish()
    norm_half(0)
    ag2[0].start()
    rs2[1].send_end(1)
    rs2[1].send_end(0)
    rs2[1].send_mid(2)
    ag2[0].near_mid()
    ag2[0].far_mid()
    rs2[1].send_mid(1)
    rs2[1].send_mid(0)
    ag2[0].step3_mid()
    spread(z, 0)
    rs2[1].finish()
    norm_half(1)
    ag2[1].start()
    ag2[0].near_end()
    spread(z, 1)
    for k in far_first:
        o_cp(k, tx).start()
    outs += [net.here(res_v.at[:, pl.ds(0, dt)], home_o.at[ds(tx * sub, sub), :]), net.here(n2_v, n2_o), net.here(dres_v.at[:, pl.ds(0, dim)], dres_o), net.here(dg_v, dg_o)]

    def back_events_1():
        ag2[1].near_mid()
        ag2[1].far_mid()
        spread(s1, 0)
        ag2[0].step2()
        spread(s2, 0)
        ag2[1].near_end()
        spread(s1, 1)

    def back_events_2():
        ag2[1].step2()
        spread(s2, 1)
        ag2[0].step3_end()
        spread(s3, 0)
        ag2[1].step3_mid()
        for j in range(4):
            ux_cp(2, ag_order[j]).wait_recv()
            ux_cp(3, ag_order[j]).start()

    def back_events_3():
        ag2[1].step3_end()
        spread(s3, 1)

    ag_order = (z, s1, s2, s3)

    @pl.loop(0, 4)
    def _(i):
        pl.when(i == 1)(back_events_1)
        pl.when(i == 2)(back_events_2)
        pl.when(i == 3)(back_events_3)
        back_block(pick(i, z))

    outs.append(net.here(e_v, e_o))
    outs += [net.here(a_v, da_o), net.here(b_v, db_o)]
    for k in far_first:
        o_cp(k, peer[k]).wait_recv()
        for b in range(4):
            ex_cp(k, b, 0).wait_recv()
            ex_cp(k, b, 1).wait_recv()
    for b in range(4):
        ux_cp(1, b).wait_recv()
        ux_cp(3, b).wait_recv()
    for c in outs:
        c.wait()
    for k in far_first:
        g_cp(k).wait_send()
        h_cp(k).wait_send()
        d_cp(k).wait_send()
        o_cp(k, tx).wait_send()
        for b in range(4):
            ux_cp(k, b).wait_send()
            ex_cp(k, b, 0).wait_send()
            ex_cp(k, b, 1).wait_send()
    for w in (qkv, up, down):
        w.drain()
    rsc.drain()
    for h in range(2):
        rs2[h].drain()
        ag2[h].drain()


def call_ab(q_width, hid, eqh, tab, swap, dh2h, wg, wu, wd, wq, gin):
    tokens, dt = hid.shape
    sub, dim, ff, width = tokens // 4, dt * 4, wg.shape[1], wq.shape[1]
    s = jax.ShapeDtypeStruct
    tok_ff, tok_d, row = s((tokens, ff), BF16), s((tokens, dim), BF16), s((sub, dim), BF16)
    shapes = (tok_d, tok_ff, tok_ff, tok_ff, s((dim, ff), BF16), s((dim, ff), BF16), s((dim, width), BF16), s((tokens, width), BF16),
              row, s((8, dim), F32), tok_d, row, s((sub, dim), F32), s((tokens, dt), BF16), s((8, dim), F32),
              s((3, tokens, ff), BF16), s((3, tokens, dt), BF16))
    vrow, vtok, vff = VMEM((sub, dim), BF16), VMEM((tokens, dim), BF16), VMEM((tokens, ff), BF16)
    return pl.pallas_call(
        functools.partial(kernel_ab, q_width), out_shape=shapes, in_specs=[ANY] * 10, out_specs=[ANY] * len(shapes),
        scratch_shapes=[
            vrow, vrow, vrow, vrow, VMEM((sub, max(dim, 2048)), F32), vtok, vff, vff, VMEM((dim, ff), BF16), VMEM((dim, ff), BF16), VMEM((ff, dim), BF16),
            VMEM((dim, width), BF16), VMEM((tokens, width), BF16), vtok, VMEM((5 * sub, dim), BF16), VMEM((5 * sub, dim), BF16),
            VMEM((8, dim), F32), VMEM((8, dim), F32), VMEM((128, 128), BF16),
            pltpu.SemaphoreType.DMA((160,)), pltpu.SemaphoreType.DMA((160,)), pltpu.SemaphoreType.DMA((40,))],
        compiler_params=pltpu.CompilerParams(collective_id=0, has_side_effects=True, vmem_limit_bytes=VMEM_LIMIT),
        cost_estimate=pl.CostEstimate(flops=20 * tokens * dim * ff, bytes_accessed=100000000, transcendentals=0), name="phase_ab",
    )(hid, eqh, tab, swap, dh2h, wg, wu, wd, wq, gin)


ROWS_ROWS = (((0,), (0,)), ((), ()))


class GradReduce:
    def __init__(self, net, peer, tile, tiles, st3, st1, cross, stage, got2, got0, got_y, out, out_tiles):
        self.net, self.peer, self.tile, self.tiles = net, peer, tile, tiles
        self.st3, self.st1, self.cross, self.stage = st3, st1, cross, stage
        self.got2, self.got0, self.got_y, self.out, self.out_tiles = got2, got0, got_y, out, out_tiles
        self.base = net.take(3)
        self.w = out.shape[1] // tiles

    def cp(self, i):
        src, dst, to = ((self.st3, self.got2, 1), (self.st1, self.got0, 1), (self.cross, self.got_y, 2))[i]
        return self.net.copy(src, dst, self.base + i, self.base + i, tx=self.peer[to])

    def fill(self, k, ref):
        @pl.loop(0, self.tiles)
        def _(j):
            ref[:, ds(j * self.w, self.w)] = self.tile(k, j).astype(BF16)

    def step3(self):
        self.fill(3, self.st3)
        self.cp(0).start()

    def step1(self):
        self.fill(1, self.st1)
        self.cp(1).start()

    def step2(self):
        self.cp(0).wait_recv()
        self.net.here(self.got2, self.stage).wait()

        @pl.loop(0, self.tiles)
        def _(j):
            cols = ds(j * self.w, self.w)
            self.cross[:, cols] = (self.tile(2, j) + self.stage[:, cols].astype(F32)).astype(BF16)

        self.cp(2).start()

    def step0(self, far):
        self.cp(1).wait_recv()
        self.cp(2).wait_recv()
        loads = [self.net.here(self.got0, self.stage), self.net.here(self.got_y, far)]
        for c in loads:
            c.wait()
        base = self.net.n_local
        self.net.n_local += 2

        def put(j, slot):
            src = self.out_tiles.at[slot, :, pl.ds(0, self.w)]
            return pltpu.make_async_copy(src, self.out.at[:, ds(j * self.w, self.w)], self.net.local.at[base + slot])

        @pl.loop(0, self.tiles)
        def _(j):
            cols = ds(j * self.w, self.w)
            slot = j % 2

            @pl.when(j >= 2)
            def _():
                put(j, slot).wait()

            self.out_tiles[slot, :, pl.ds(0, self.w)] = self.tile(0, j) + (self.stage[:, cols].astype(F32) + far[:, cols].astype(F32))
            put(j, slot).start()

        for slot in range(min(2, self.tiles)):
            put(slot, slot).wait()

    def sent_locally(self):
        self.cp(0).wait_send()
        self.cp(1).wait_send()

    def sent(self):
        self.cp(2).wait_send()


def kernel_c(q_width, da_h, db_h, wg_h, wu_h, n_h, u_h, ux_h, e_h, ex_h, n2_h, eq_h, wq_h, h_h, dres_h, g_h, dga_h, tabh, swaph,
             wgo, wgy, wuo, wuy, wdo, wqo, wqy, q_o, dh_o, dg_o, g2, g0, u2, u0, q2, q0, qx,
             wg_v, wu_v, da_v, db_v, n_v, p_v, rbuf, n2_v, st3, st1, cross_g, cross_u, stage, tiles_v, dres_v, wq_v, eq_v,
             gains, dg_v, dgr, dgz, tab_v, swap_v, send, recv, local):
    dp, z, tx, peer = places()
    tokens, ff = da_v.shape
    sub, dim = dres_v.shape
    dt = dim // 4
    width = eq_v.shape[1]
    tile = ff // 4
    dtile = min(512, dim)
    qt = min(256, tile)
    far_first = (2, 3, 1)
    net = Wires(send, recv, local)
    n2_in = net.here(n2_h, n2_v.at[ds(z * sub, sub), :])
    first = [net.here(n_h, n_v), net.here(da_h, da_v)]
    second = [net.here(db_h, db_v), net.here(wg_h, wg_v), net.here(wu_h, wu_v)]
    third = [net.here(wq_h, wq_v), net.here(eq_h, eq_v), net.here(dres_h, dres_v), net.here(g_h, gains),
             net.here(dga_h, dg_v.at[pl.ds(8, 8), :]), net.here(tabh, tab_v), net.here(swaph, swap_v)]
    sem = pltpu.get_barrier_semaphore()
    zs = tuple((z + i) % 4 for i in range(4))
    for i in (1, 2, 3):
        pl.semaphore_signal(sem, inc=1, device_id={"tx": peer[i]}, device_id_type=MESH)
        pl.semaphore_signal(sem, inc=1, device_id={"ty": zs[i]}, device_id_type=MESH)
    pl.semaphore_wait(sem, 6)
    rsc = LineScatter(net, p_v, rbuf, sub, z)
    ag = LineGather(net, n2_v, sub, z)
    q_id, h_id, t_id, z_id = net.take(4), net.take(4), net.take(4), net.take(4)

    def grad_tile(lhs, rhs, w):
        def go(k, j):
            cols = pl.ds(j * w, w) if isinstance(j, int) else ds(j * w, w)
            return dot(lhs[:, pl.ds(k * dt, dt)], rhs[:, cols], ROWS_ROWS)
        return go

    gate = GradReduce(net, peer, grad_tile(n_v, da_v, tile), ff // tile, st3, st1, cross_g, stage, g2, g0, wgy, wgo, tiles_v)
    up = GradReduce(net, peer, grad_tile(n_v, db_v, tile), ff // tile, st3, st1, cross_u, stage, u2, u0, wuy, wuo, tiles_v)
    half = tokens // 2

    def corner(r, c):
        return da_v.at[pl.ds(r * dt, dt), pl.ds(c * width, width)]

    qkv = GradReduce(net, peer, grad_tile(n2_v, eq_v, qt), width // qt, corner(0, 0), corner(1, 0), corner(0, 1), corner(1, 1),
                     q2, q0, wqy, wqo, tiles_v)

    def dn_block(b):
        rows = ds(b * sub, sub)

        @pl.loop(0, dim // dtile)
        def _(j):
            wr = ds(j * dtile, dtile)
            p_v[rows, wr] = (dot(da_v[rows, :], wg_v[wr, :], NT_DIMS) + dot(db_v[rows, :], wu_v[wr, :], NT_DIMS)).astype(BF16)

    n2_in.wait()
    ag.start()
    for c in first:
        c.wait()
    gate.step3()
    gate.step1()
    gate.step2()
    for c in second:
        c.wait()

    @pl.loop(0, 4)
    def _(i):
        pl.when(i == 1)(ag.step1)
        dn_block(pick(3 - i, z))
        for step in range(3):
            pl.when(i == step)(lambda step=step: rsc.send_end(2 - step))

    gate.sent_locally()
    up.step3()
    up.step1()
    up.step2()
    rsc.send_mid(2)
    ag.step2()
    ag.step3_mid()
    up.sent_locally()
    h_in = net.here(h_h, st3.at[pl.ds(0, sub), :])
    gate.step0(st1)
    gate.sent()

    e_in = [net.here(e_h.at[:, pl.ds(0, dt)], wu_v.at[pl.ds(0, tokens), pl.ds(0, dt)])]
    for k in (1, 2, 3):
        e_in.append(net.here(ex_h.at[k - 1], wu_v.at[pl.ds(0, tokens), pl.ds(k * dt, dt)]))

    def u_place(j, k):
        return wg_v.at[pl.ds((j % 2) * tokens, tokens), pl.ds(k * tile, tile)]

    def u_load(j):
        cols = pl.ds(j * tile, tile)
        return [net.here(u_h.at[:, cols] if k == 0 else ux_h.at[k - 1, :, cols], u_place(j, k)) for k in range(4)]

    def down_tile(j, slot, loads):
        for c in loads:
            c.wait()
        acc = None
        for k in range(4):
            part = dot(u_place(j, k)[...], wu_v[pl.ds(0, tokens), pl.ds(k * dt, dt)], ROWS_ROWS)
            acc = part if acc is None else acc + part
        tiles_v[slot, pl.ds(0, tile), pl.ds(0, dt)] = acc
        return net.here(tiles_v.at[slot, pl.ds(0, tile), pl.ds(0, dt)], wdo.at[pl.ds(j * tile, tile), :])

    n_tiles = ff // tile
    loads = {0: u_load(0), 1: u_load(1)}
    rsc.send_mid(1)
    rsc.send_mid(0)
    for c in e_in:
        c.wait()
    done = [down_tile(0, 0, loads[0]), down_tile(1, 1, loads[1])]
    loads = {2: u_load(2), 3: u_load(3)}
    for c in third:
        c.wait()
    ag.step3_end()

    @pl.loop(0, 4)
    def _(b):
        rows = ds(b * sub, sub)

        @pl.loop(0, width // qt)
        def _(j):
            cols = ds(j * qt, qt)
            wu_v[ds(tokens + b * sub, sub), cols] = dot(n2_v[rows, :], wq_v[:, cols]).astype(BF16)

    def q_cp(k, block):
        return net.copy(wu_v.at[ds(tokens + peer[k] * sub, sub), pl.ds(0, width)], qx.at[ds(block * sub, sub), :], q_id + k, q_id + k, tx=peer[k])

    for k in far_first:
        q_cp(k, tx).start()
    q_own = net.here(wu_v.at[ds(tokens + tx * sub, sub), pl.ds(0, width)], qx.at[ds(tx * sub, sub), :])
    for c in done:
        c.wait()
    qkv.step3()
    qkv.step1()
    done = [down_tile(2, 0, loads[2]), down_tile(3, 1, loads[3])]
    h_in.wait()
    rsc.finish()
    dg_v[pl.ds(0, 8), :] = jnp.zeros((8, dim), F32)
    step = 16

    @pl.loop(0, sub // step)
    def _(r):
        view, mine, far = ds(r * step, step), ds(z * sub + r * step, step), ds(4 * sub + r * step, step)
        right = jnp.where(z < 3, rbuf[mine, :].astype(F32), 0.0)
        left = jnp.where(z > 0, rbuf[far, :].astype(F32), 0.0)
        dy = p_v[mine, :].astype(F32) + right + left
        x = st3[view, :].astype(F32)
        inv = lax.rsqrt(jnp.sum(x * x, axis=1, keepdims=True) / dim + NORM_EPS)
        xhat = x * inv
        gain = gains[0:1, :]
        part = dy * xhat
        dg_v[pl.ds(0, 8), :] += part[:8] + part[8:]
        inner = jnp.sum(part * gain, axis=1, keepdims=True) / dim
        st1[view, :] = (dres_v[view, :] + inv * (dy * gain) - xhat * (inv * inner)).astype(BF16)

    def h_cp(k, block):
        return net.copy(st1.at[pl.ds(0, sub), pl.ds(k * dt, dt)], dh_o.at[ds(block * sub, sub), :], h_id + k, h_id + k, tx=peer[k])

    def t_cp(k):
        return net.copy(dg_v.at[:, pl.ds(k * dt, dt)], dgr.at[k], t_id + k, t_id + k, tx=peer[k])

    def z_cp(i):
        return net.copy(dgr.at[0], dgz.at[i], z_id + i, z_id + i, ty=zs[i])

    for k in far_first:
        t_cp(k).start()
    for k in far_first:
        h_cp(k, tx).start()
    h_own = net.here(st1.at[pl.ds(0, sub), pl.ds(0, dt)], dh_o.at[ds(tx * sub, sub), :])
    qkv.step2()
    up.sent()
    for c in done:
        c.wait()
    up.step0(cross_g)
    for k in far_first:
        q_cp(k, peer[k]).wait_recv()
    q_own.wait()
    turned = wu_v.at[pl.ds(tokens, tokens), pl.ds(width, width)]
    net.here(qx, turned).wait()
    turn(turned, turned, tokens, width, q_width, tab_v, swap_v, False)
    q_out = net.here(turned, q_o)
    for k in far_first:
        t_cp(k).wait_recv()
    dgr[0] = dg_v[:, pl.ds(0, dt)] + dgr[1] + dgr[2] + dgr[3]
    for i in (1, 2, 3):
        z_cp(i).start()
    for i in (1, 2, 3):
        z_cp(i).wait_recv()
    dgz[0] = dgr[0] + dgz[1] + dgz[2] + dgz[3]
    dg_out = net.here(dgz.at[0], dg_o)
    for k in far_first:
        h_cp(k, peer[k]).wait_recv()
    qkv.step0(cross_g.at[:, pl.ds(0, width)])
    for c in (q_out, dg_out, h_own):
        c.wait()
    qkv.sent_locally()
    qkv.sent()
    for k in far_first:
        q_cp(k, tx).wait_send()
        h_cp(k, tx).wait_send()
        t_cp(k).wait_send()
        z_cp(k).wait_send()
    ag.drain()
    rsc.drain()


def call_c(q_width, *args):
    tokens, ff = args[0].shape
    sub, dim = args[9].shape
    dt, width = dim // 4, args[10].shape[1]
    tile = ff // 4
    s = jax.ShapeDtypeStruct
    wf, wb = s((dt, ff), F32), s((dt, ff), BF16)
    qf, qb = s((dt, width), F32), s((dt, width), BF16)
    shapes = (wf, wb, wf, wb, s((ff, dt), F32), qf, qb, s((tokens, width), BF16), s((tokens, dt), BF16), s((16, dt), F32),
              wb, wb, wb, wb, qb, qb, s((tokens, width), BF16))
    return pl.pallas_call(
        functools.partial(kernel_c, q_width), out_shape=shapes, in_specs=[ANY] * len(args), out_specs=[ANY] * len(shapes),
        scratch_shapes=[
            VMEM((dim, ff), BF16), VMEM((dim, ff), BF16), VMEM((tokens, ff), BF16), VMEM((tokens, ff), BF16), VMEM((tokens, dim), BF16),
            VMEM((tokens, dim), BF16), VMEM((5 * sub, dim), BF16), VMEM((tokens, dim), BF16),
            VMEM((dt, ff), BF16), VMEM((dt, ff), BF16), VMEM((dt, ff), BF16), VMEM((dt, ff), BF16), VMEM((dt, ff), BF16),
            VMEM((2, max(dt, tile), max(dt, tile)), F32), VMEM((sub, dim), F32), VMEM((dim, width), BF16), VMEM((tokens, width), BF16),
            VMEM((8, dim), F32), VMEM((16, dim), F32), VMEM((4, 16, dt), F32), VMEM((4, 16, dt), F32), VMEM((sub, 2048), F32), VMEM((128, 128), BF16),
            pltpu.SemaphoreType.DMA((48,)), pltpu.SemaphoreType.DMA((48,)), pltpu.SemaphoreType.DMA((72,))],
        compiler_params=pltpu.CompilerParams(collective_id=2, has_side_effects=True, vmem_limit_bytes=VMEM_LIMIT),
        cost_estimate=pl.CostEstimate(flops=20 * tokens * dim * ff, bytes_accessed=100000000, transcendentals=0), name="phase_c",
    )(*args)


def solution(mesh):
    def local_step(hidden, positions, g_ffn, w_gate, w_up, w_down, g_attn, w_q, w_kv, grad_h2, grad_q, grad_kv):
        tokens, dt = hidden.shape
        q_heads, head_dim = w_q.shape[1:]
        kv_heads = w_kv.shape[1]
        q_width, kv_width = q_heads * head_dim, kv_heads * head_dim
        width = q_width + kv_width

        lane = jnp.arange(128)
        inv_freq = ROPE_BASE ** (-((lane % head_dim) // 2 * 2).astype(F32) / head_dim)
        angles = positions.astype(F32)[:, None] * inv_freq[None, :]
        cos_t = jnp.cos(angles)
        swap = (lane[:, None] == (lane + 1 - lane % 2 * 2)[None, :]).astype(BF16)
        sin_t = jnp.sin(angles) * jnp.where(lane % 2 == 0, -1.0, 1.0)[None, :]

        turns = lax.axis_index("ty") < mesh.shape["ty"] // 2
        table = jnp.stack([cos_t, jnp.where(turns, cos_t, 1.0), sin_t, jnp.where(turns, sin_t, 0.0)])
        table = table.reshape(4, 4, tokens // 4, 128).transpose(2, 0, 1, 3).reshape(tokens // 4, 2048)
        back = jnp.concatenate([grad_q.reshape(tokens, q_width), grad_kv.reshape(tokens, kv_width)], axis=1)
        w_qkv_own = jnp.concatenate([w_q.reshape(dt, q_width), w_kv.reshape(dt, kv_width)], axis=1)
        gin = jnp.concatenate([jnp.stack([g_ffn, g_attn]).astype(F32), jnp.zeros((6, dt), F32)])

        (normed_all, grad_gate, grad_up, u_all, gate_w, up_w, w_qkv, back_all, h_rows, gains, res_all, normed2, grad_res, resid_out, gattn8,
         u_other, e_other) = call_ab(q_width, hidden, back, table, swap, grad_h2, w_gate, w_up, w_down, w_qkv_own, gin)
        (grad_wgate, _, grad_wup, _, grad_wdown, grad_wqkv, _, qkv_out, grad_hidden, gain_grads, *_) = call_c(
            q_width, grad_gate, grad_up, gate_w, up_w, normed_all, u_all, u_other, res_all, e_other, normed2, back_all, w_qkv,
            h_rows, grad_res, gains, gattn8, table, swap)
        grad_wq = grad_wqkv[:, :q_width].reshape(dt, q_heads, head_dim)
        grad_wkv = grad_wqkv[:, q_width:].reshape(dt, kv_heads, head_dim)
        q_out = qkv_out[:, :q_width].reshape(tokens, q_heads, head_dim)
        kv_out = qkv_out[:, q_width:].reshape(tokens, kv_heads, head_dim)
        grad_gffn = jnp.sum(gain_grads[:8], axis=0)
        grad_gattn = jnp.sum(gain_grads[8:], axis=0)
        return (resid_out, q_out, kv_out, grad_hidden, grad_gffn, grad_gattn, grad_wgate, grad_wup, grad_wdown, grad_wq, grad_wkv)

    row_spec = P(("dp", "ty"), "tx")
    head_spec = P(("dp", "tx"), "ty", None)
    in_specs = (row_spec, P(("dp", "tx")), P("tx"), P("tx", "ty"), P("tx", "ty"), P("ty", "tx"), P("tx"), P("tx", "ty", None), P("tx", "ty", None), row_spec, head_spec, head_spec)
    out_specs = (row_spec, head_spec, head_spec, row_spec, P(("dp", "tx")), P(("dp", "tx")), P(("dp", "tx"), "ty"), P(("dp", "tx"), "ty"), P(("dp", "ty"), "tx"), head_spec, head_spec)
    return jax.shard_map(local_step, mesh=mesh, in_specs=in_specs, out_specs=out_specs, check_vma=False)
```

```python
import functools

import jax
import jax.numpy as jnp
import numpy as np
from jax import lax
from jax.experimental import pallas as pl
from jax.experimental.pallas import tpu as pltpu
from jax.sharding import PartitionSpec as P

NORM_EPS = 1e-5
ROPE_BASE = 10000.0
F32 = jnp.float32
BF16 = jnp.bfloat16


def dot(a, b, dims=(((1,), (0,)), ((), ()))):
    return lax.dot_general(a, b, dims, preferred_element_type=F32)


MESH = pl.DeviceIdType.MESH
ANY = pl.BlockSpec(memory_space=pl.ANY)
VMEM = pltpu.VMEM
NT_DIMS = (((1,), (1,)), ((), ()))
VMEM_LIMIT = 67000000


def ds(start, size, align=None):
    if isinstance(start, int):
        return pl.ds(start, size)
    return pl.ds(pl.multiple_of(start, align or size), size)


def mid(z):
    return jnp.logical_and(z > 0, z < 3)


def end(z):
    return jnp.logical_or(z == 0, z == 3)


def slots(z):
    return (z + 1 - 2 * (z % 2), 2 - z // 2, 3 - 3 * (z // 2))


def turn(src, dst, rows, width, q_width, table_ref, swap_ref, back):
    step = rows // 4

    @pl.loop(0, 4)
    def _(r):
        for c in range(width // 128):
            cols = pl.ds(c * 128, 128)
            table = ds(r * 128 + (0 if c * 128 < q_width else 512), 128)
            x = src[ds(r * step, step), cols]
            main = x.astype(F32) * table_ref[:, table]
            side = dot(x, swap_ref[...]) * table_ref[:, ds(r * 128 + (1024 if c * 128 < q_width else 1536), 128)]
            dst[ds(r * step, step), cols] = (main - side if back else main + side).astype(BF16)


def pick(i, z):
    s1, s2, s3 = slots(z)
    first, last = (3 - i) // 3, (i // 2) * (i % 2)
    return z * first + s1 * ((i % 2) * (1 - i // 2)) + s2 * ((i // 2) * (1 - i % 2)) + s3 * last


class Wires:
    def __init__(self, send, recv, local):
        self.send, self.recv, self.local = send, recv, local
        self.n_remote = 0
        self.n_local = 0

    def take(self, n=1):
        base = self.n_remote
        self.n_remote += n
        assert self.n_remote <= self.send.shape[0]
        return base

    def copy(self, src, dst, si, ri, **dev):
        return pltpu.make_async_remote_copy(
            src_ref=src, dst_ref=dst, send_sem=self.send.at[si], recv_sem=self.recv.at[ri],
            device_id=dev, device_id_type=MESH)

    def here(self, src, dst):
        i = self.n_local
        self.n_local += 1
        assert i < self.local.shape[0]
        c = pltpu.make_async_copy(src, dst, self.local.at[i])
        c.start()
        return c


def entry_barrier(axes, z):
    sem = pltpu.get_barrier_semaphore()
    for dev in axes:
        pl.semaphore_signal(sem, inc=1, device_id=dev, device_id_type=MESH)

    @pl.when(z > 0)
    def _():
        pl.semaphore_signal(sem, inc=1, device_id={"ty": z - 1}, device_id_type=MESH)

    @pl.when(z < 3)
    def _():
        pl.semaphore_signal(sem, inc=1, device_id={"ty": z + 1}, device_id_type=MESH)

    @pl.when(mid(z))
    def _():
        pl.semaphore_wait(sem, len(axes) + 2)

    @pl.when(end(z))
    def _():
        pl.semaphore_wait(sem, len(axes) + 1)


class LineGather:
    def __init__(self, net, buf, rows, z, off=0, part=None):
        self.net, self.buf, self.rows, self.z, self.off, self.part = net, buf, rows, z, off, part or rows
        self.base = net.take(8)
        self.slots = slots(z)

    def blk(self, b):
        return self.buf.at[ds(b * self.rows + self.off, self.part), :]

    def cp(self, b, side, target):
        return self.net.copy(self.blk(b), self.blk(b), self.base + side * 4 + b, self.base + b, ty=target)

    def start(self):
        z = self.z

        @pl.when(z < 3)
        def _():
            self.cp(z, 0, z + 1).start()

        @pl.when(z > 0)
        def _():
            self.cp(z, 1, z - 1).start()

    def take(self, i):
        b = self.slots[i]
        self.cp(b, 0, self.z).wait_recv()

    def forward(self, i):
        z, b = self.z, self.slots[i]
        target = 3 - z if i == 0 else 3 * (z - 1)
        self.cp(b, 0, target).start()

    def step1(self):
        self.take(0)

        @pl.when(mid(self.z))
        def _():
            self.forward(0)
            self.take(1)
            self.forward(1)

    def near_end(self):
        @pl.when(end(self.z))
        def _():
            self.take(0)

    def near_mid(self):
        @pl.when(mid(self.z))
        def _():
            self.take(1)
            self.forward(1)

    def far_mid(self):
        @pl.when(mid(self.z))
        def _():
            self.take(0)
            self.forward(0)

    def step2(self):
        @pl.when(end(self.z))
        def _():
            self.take(1)

    def step3_mid(self):
        @pl.when(mid(self.z))
        def _():
            self.take(2)
            self.forward(2)

    def step3_end(self):
        @pl.when(end(self.z))
        def _():
            self.take(2)

    def drain(self):
        z = self.z

        @pl.when(z < 3)
        def _():
            self.cp(z, 0, z + 1).wait_send()

        @pl.when(z > 0)
        def _():
            self.cp(z, 1, z - 1).wait_send()

        @pl.when(mid(z))
        def _():
            for i in range(3):
                self.cp(self.slots[i], 0, 3 - z if i == 0 else 3 * (z - 1)).wait_send()


class LineScatter:
    def __init__(self, net, part, rbuf, rows, z, off=0, size=None):
        self.net, self.part, self.rbuf, self.rows, self.z, self.off, self.size = net, part, rbuf, rows, z, off, size or rows
        self.base = net.take(5)
        self.slots = slots(z)
        one = (z % 2) * (1 - z // 2)
        self.dst = (self.slots[0] + (1 - z % 2) * (3 - z), self.slots[1] + 2 * one, self.slots[2])
        self.target = (z + 1 - 2 * (z % 2), 1 + z % 2, 1 + z % 2)

    def cp(self, i):
        return self.net.copy(
            self.part.at[self.view(self.slots[i]), :], self.rbuf.at[self.view(self.dst[i]), :],
            self.base + i, self.base + self.dst[i], ty=self.target[i])

    def view(self, b):
        return ds(b * self.rows + self.off, self.size)

    def wait_slot(self, s):
        view = self.rbuf.at[self.view(s), :]
        self.net.copy(view, view, self.base, self.base + s, ty=self.z).wait_recv()

    def send_end(self, i):
        @pl.when(end(self.z))
        def _():
            self.cp(i).start()

    def send_mid(self, i):
        @pl.when(mid(self.z))
        def _():
            b = self.slots[i]
            self.wait_slot(b)
            step = 16

            @pl.loop(0, self.size // step)
            def _(r):
                view = ds(b * self.rows + self.off + r * step, step)
                self.part[view, :] = (self.part[view, :].astype(F32) + self.rbuf[view, :].astype(F32)).astype(BF16)

            self.cp(i).start()

    def finish(self):
        z = self.z

        @pl.when(z < 3)
        def _():
            self.wait_slot(z)

        @pl.when(z > 0)
        def _():
            self.wait_slot(4)

    def drain(self):
        for i in range(3):
            self.cp(i).wait_send()


class WeightGather:
    def __init__(self, net, w, full, pos, by_rows, chunks, direct=0):
        self.net, self.w, self.full, self.by_rows = net, w, full, by_rows
        self.dp, self.t1, self.t2 = pos
        self.len = w.shape[0]
        self.width = w.shape[0] if by_rows else w.shape[1]
        self.chunks = chunks
        self.piece = self.len // 2 // chunks
        self.direct = direct
        self.base = net.take(1 + 4 * chunks + direct)

    def dst(self, k, off, n):
        if self.by_rows:
            return self.full.at[ds(k * self.width + off, n, min(n, 16)), :]
        return self.full.at[ds(off, n, 16), pl.ds(k * self.width, self.width)]

    def off(self, half, ch):
        return half * (self.len // 2) + ch * self.piece

    def near(self, ch):
        o = self.off(self.dp, ch)
        i = self.base + 1 + ch
        return self.net.copy(self.w.at[ds(o, self.piece, 16), :], self.dst(2, o, self.piece), i, i, tx=self.t2)

    def cross(self, ch, half):
        o = self.off(half, ch)
        i = self.base + 1 + self.chunks + ch
        return self.net.copy(self.dst(2, o, self.piece), self.dst(2, o, self.piece), i, i, dp=1 - self.dp)

    def diag(self, ch, which, half):
        o = self.off(half, ch)
        i = self.base + 1 + (2 + which) * self.chunks + ch
        return self.net.copy(self.dst(2, o, self.piece), self.dst(3, o, self.piece), i, i, tx=self.t1)

    def mate(self):
        return self.net.copy(self.w, self.dst(1, 0, self.len), self.base, self.base, tx=self.t1)

    def straight(self, n, half):
        o = self.off(half, self.chunks - 1 - n)
        i = self.base + 1 + 4 * self.chunks + n
        return self.net.copy(self.w.at[ds(o, self.piece, 16), :], self.dst(2, o, self.piece), i, i, tx=self.t2)

    def start_y(self):
        for ch in range(self.chunks):
            self.near(ch).start()
        for n in range(self.direct):
            self.straight(n, 1 - self.dp).start()

    def start_local(self):
        self.own = self.net.here(self.w, self.dst(0, 0, self.len))
        self.mate().start()

    def y_event(self, ch):
        self.near(ch).wait_recv()
        if ch < self.chunks - self.direct:
            self.cross(ch, self.dp).start()
        self.diag(ch, 0, self.dp).start()

    def x_event(self, ch):
        if ch < self.chunks - self.direct:
            self.cross(ch, 1 - self.dp).wait_recv()
        else:
            self.straight(self.chunks - 1 - ch, 1 - self.dp).wait_recv()
        self.diag(ch, 1, 1 - self.dp).start()

    def finish(self):
        self.own.wait()
        self.mate().wait_recv()
        for ch in range(self.chunks):
            self.diag(ch, 0, self.dp).wait_recv()
            self.diag(ch, 1, 1 - self.dp).wait_recv()

    def drain(self):
        self.mate().wait_send()
        for ch in range(self.chunks):
            self.near(ch).wait_send()
            if ch < self.chunks - self.direct:
                self.cross(ch, self.dp).wait_send()
            else:
                self.straight(self.chunks - 1 - ch, 1 - self.dp).wait_send()
            self.diag(ch, 0, self.dp).wait_send()
            self.diag(ch, 1, 1 - self.dp).wait_send()


def places():
    dp, z, tx = lax.axis_index("dp"), lax.axis_index("ty"), lax.axis_index("tx")
    return dp, z, tx, (tx, tx + 1 - 2 * (tx % 2), (tx + 2) % 4, 3 - tx)


ROWS_ROWS = (((0,), (0,)), ((), ()))


class GradReduce:
    def __init__(self, net, peer, tile, tiles, st3, st1, cross, stage, got2, got0, got_y, out, out_tiles):
        self.net, self.peer, self.tile, self.tiles = net, peer, tile, tiles
        self.st3, self.st1, self.cross, self.stage = st3, st1, cross, stage
        self.got2, self.got0, self.got_y, self.out, self.out_tiles = got2, got0, got_y, out, out_tiles
        self.src = None
        self.base = net.take(3)
        self.w = out.shape[1] // tiles

    def cp(self, i):
        src, dst, to = ((self.st3, self.got2, 1), (self.st1, self.got0, 1), (self.src or self.cross, self.got_y, 2))[i]
        return self.net.copy(src, dst, self.base + i, self.base + i, tx=self.peer[to])

    def fill(self, k, ref):
        @pl.loop(0, self.tiles)
        def _(j):
            ref[:, ds(j * self.w, self.w)] = self.tile(k, j).astype(BF16)

    def step3(self):
        self.fill(3, self.st3)
        self.cp(0).start()

    def step1(self):
        self.fill(1, self.st1)
        self.cp(1).start()

    def step2(self, received=False):
        if not received:
            self.cp(0).wait_recv()
        self.net.here(self.got2, self.stage).wait()

        @pl.loop(0, self.tiles)
        def _(j):
            cols = ds(j * self.w, self.w)
            self.cross[:, cols] = (self.tile(2, j) + self.stage[:, cols].astype(F32)).astype(BF16)

    def send(self, src=None):
        self.src = src
        self.cp(2).start()

    def step0(self, far):
        self.cp(1).wait_recv()
        self.cp(2).wait_recv()
        loads = [self.net.here(self.got0, self.stage), self.net.here(self.got_y, far)]
        for c in loads:
            c.wait()
        base = self.net.n_local
        self.net.n_local += 2

        def put(j, slot):
            src = self.out_tiles.at[slot, :, pl.ds(0, self.w)]
            return pltpu.make_async_copy(src, self.out.at[:, ds(j * self.w, self.w)], self.net.local.at[base + slot])

        @pl.loop(0, self.tiles)
        def _(j):
            cols = ds(j * self.w, self.w)
            slot = j % 2

            @pl.when(j >= 2)
            def _():
                put(j, slot).wait()

            self.out_tiles[slot, :, pl.ds(0, self.w)] = self.tile(0, j) + (self.stage[:, cols].astype(F32) + far[:, cols].astype(F32))
            put(j, slot).start()

        for slot in range(min(2, self.tiles)):
            put(slot, slot).wait()

    def sent_locally(self):
        self.cp(0).wait_send()
        self.cp(1).wait_send()

    def sent(self):
        self.cp(2).wait_send()


def kernel_ab(q_width, hid, eqh, ekvh, angh, swaph, dh2h, wg, wu, wd, wq, gin,
              n_o, da_o, db_o, u_o, wg_o, wu_o, wq_o, eq_o, h_o, g_o, e_o, n2_o, dres_o, home_o, dg_o, ux_o, ex_o, tab_o, g2_o, d2_o, d0_o, dc_o,
              rows, dh2_v, n2_v, res_v, dres_v, n_v, a_v, b_v, wg_v, wu_v, wd_v, wq_v, eq_v, p_v, rbuf, rbuf2, gains, dg_v, swap_v, send, recv, local):
    dp, z, tx, peer = places()
    sub, dim = rows.shape
    tokens = 4 * sub
    width = eq_v.shape[1]
    dt = dim // 4
    ff = wg.shape[1]
    wide = min(1024, ff)
    tile = min(512, ff)
    dwide = min(1024, dim)
    dtile = min(512, dim)
    hs = sub // 2
    net = Wires(send, recv, local)
    turn_in = [net.here(eqh, p_v.at[:, pl.ds(0, q_width)]), net.here(ekvh, p_v.at[:, pl.ds(q_width, width - q_width)]), net.here(swaph, swap_v)]
    turn_in += [net.here(angh.at[pl.ds(i * sub, sub), :], dres_v.at[:, pl.ds(i * 128, 128)]) for i in range(4)]
    entry_barrier([{"tx": peer[1]}, {"tx": peer[2]}, {"tx": peer[3]}, {"dp": 1 - dp}], z)

    pos = (dp, peer[1], peer[2])
    far_first = (2, 3, 1)
    g_id, h_id, e_id, d_id, o_id, u_id, x_id = (net.take(4), net.take(4), net.take(4), net.take(4), net.take(4), net.take(12), net.take(24))
    u_v = wg_v.at[pl.ds(0, tokens), :]
    e_v = wg_v.at[pl.ds(tokens, tokens), :]

    def g_cp(k):
        return net.copy(gin, gains.at[:, pl.ds(k * dt, dt)], g_id + k, g_id + k, tx=peer[k])

    def h_cp(k):
        return net.copy(hid.at[ds(peer[k] * sub, sub), :], rows.at[:, pl.ds(k * dt, dt)], h_id + k, h_id + k, tx=peer[k])

    def e_cp(k, block):
        return net.copy(p_v.at[ds(peer[k] * sub, sub), pl.ds(0, width)], eq_v.at[ds(block * sub, sub), :], e_id + k, e_id + k, tx=peer[k])

    def d_cp(k):
        return net.copy(dh2h.at[ds(peer[k] * sub, sub), :], dh2_v.at[:, pl.ds(k * dt, dt)], d_id + k, d_id + k, tx=peer[k])

    def o_cp(k, block):
        return net.copy(res_v.at[:, pl.ds(k * dt, dt)], home_o.at[ds(block * sub, sub), :], o_id + k, o_id + k, tx=peer[k])

    def ux_cp(k, b):
        view = ds(b * sub, sub)
        cols = pl.ds(0, ff - ff // 4)
        src = ux_o.at[1, view, :] if k == 3 else wg_v.at[view, cols]
        i = u_id + (k - 1) * 4 + b
        return net.copy(src, ux_o.at[k - 1, view, :], i, i, tx=peer[1] if k == 3 else peer[k])

    def ex_cp(k, b, half):
        i = x_id + half * 12 + (k - 1) * 4 + b
        view = ds(b * sub + half * hs, hs)
        return net.copy(wg_v.at[ds(tokens + b * sub + half * hs, hs), pl.ds(k * dt, dt)], ex_o.at[k - 1, view, :], i, i, tx=peer[k])

    gate = WeightGather(net, wg, wg_v, pos, True, 2)
    up = WeightGather(net, wu, wu_v, pos, True, 2)
    down = WeightGather(net, wd, wd_v, pos, False, 4, 1)
    qkv = WeightGather(net, wq, wq_v, pos, True, 1)
    ag = LineGather(net, n_v, sub, z)
    rsc = LineScatter(net, p_v, rbuf, sub, z)
    rs2 = [LineScatter(net, n_v, rbuf2, sub, z, h * hs, hs) for h in range(2)]
    ag2 = [LineGather(net, e_v, sub, z, h * hs, hs) for h in range(2)]

    for k in far_first:
        g_cp(k).start()
    for k in far_first:
        h_cp(k).start()
    g_own = net.here(gin, gains.at[:, pl.ds(0, dt)])
    h_own = net.here(hid.at[ds(tx * sub, sub), :], rows.at[:, pl.ds(0, dt)])
    for w in (qkv, gate, up, down):
        w.start_local()
    for c in turn_in:
        c.wait()

    @pl.loop(0, 4)
    def _(i):
        cos_q, cos_kv, sin_q, sin_kv = (ds(i * 128 + n * 512, 128) for n in range(4))
        angles = dres_v[:, cos_q]
        dres_v[:, sin_q] = jnp.sin(angles)
        dres_v[:, cos_q] = jnp.cos(angles)

        @pl.when(z < 2)
        def _():
            dres_v[:, cos_kv] = dres_v[:, cos_q]
            dres_v[:, sin_kv] = dres_v[:, sin_q]

        @pl.when(z >= 2)
        def _():
            dres_v[:, cos_kv] = jnp.ones((sub, 128), F32)
            dres_v[:, sin_kv] = jnp.zeros((sub, 128), F32)

    tab_out = net.here(dres_v.at[:, pl.ds(0, 2048)], tab_o)
    turn(p_v, p_v, tokens, width, q_width, dres_v, swap_v, True)
    for k in far_first:
        e_cp(k, tx).start()
    e_own = net.here(p_v.at[ds(tx * sub, sub), pl.ds(0, width)], eq_v.at[ds(tx * sub, sub), :])
    for w in (qkv, gate, up, down):
        w.start_y()
    for k in far_first:
        d_cp(k).start()
    d_own = net.here(dh2h.at[ds(tx * sub, sub), :], dh2_v.at[:, pl.ds(0, dt)])

    for k in far_first:
        g_cp(k).wait_recv()
        h_cp(k).wait_recv()
    g_own.wait()
    h_own.wait()

    @pl.loop(0, sub // 16)
    def _(r):
        x = rows[ds(r * 16, 16), :].astype(F32)
        inv = lax.rsqrt(jnp.sum(x * x, axis=1, keepdims=True) / dim + NORM_EPS)
        n_v[ds(z * sub + r * 16, 16), :] = (x * inv * gains[0:1, :]).astype(BF16)

    ag.start()
    outs = [net.here(rows, h_o), net.here(gains, g_o)]
    for k in far_first:
        e_cp(k, peer[k]).wait_recv()
    e_own.wait()
    ag.step1()
    qkv.y_event(0)
    qkv.x_event(0)
    qkv.finish()
    for k in far_first:
        e_cp(k, tx).wait_send()

    def n2_block(b):
        @pl.loop(0, dim // dtile)
        def _(j):
            w = wq_v[ds(j * dtile, dtile), :]
            p_v[ds(b * sub, sub), ds(j * dtile, dtile)] = dot(eq_v[ds(b * sub, sub), :], w, NT_DIMS).astype(BF16)

    @pl.loop(0, 4)
    def _(i):
        n2_block(pick(3 - i, z))
        for step in range(3):
            pl.when(i == step)(lambda step=step: rsc.send_end(2 - step))

    gate.y_event(0)
    gate.y_event(1)
    gate.x_event(0)
    ag.step2()
    ag.step3_mid()
    up.y_event(0)
    gate.x_event(1)
    gate.finish()

    def gate_block(b):
        @pl.loop(0, ff // wide)
        def _(j):
            cols = ds(j * wide, wide)
            a_v[ds(b * sub, sub), cols] = dot(n_v[ds(b * sub, sub), :], wg_v[:, cols]).astype(BF16)

    def up_block(b):
        @pl.loop(0, ff // wide)
        def _(j):
            cols = ds(j * wide, wide)
            bb = dot(n_v[ds(b * sub, sub), :], wu_v[:, cols]).astype(BF16)
            b_v[ds(b * sub, sub), cols] = bb
            aa = a_v[ds(b * sub, sub), cols].astype(F32)
            wg_v[ds(b * sub, sub), cols] = (aa * jax.nn.sigmoid(aa) * bb.astype(F32)).astype(BF16)

    wg_out = net.here(wg_v, wg_o)
    outs += [net.here(wq_v, wq_o), net.here(eq_v, eq_o)]
    def gate_events_2():
        rsc.send_mid(2)

    def gate_events_3():
        up.y_event(1)
        up.x_event(0)
        ag.step3_end()

    @pl.loop(0, 4)
    def _(i):
        pl.when(i == 2)(gate_events_2)
        pl.when(i == 3)(gate_events_3)
        gate_block(pick(i, z))

    n_out = net.here(n_v, n_o)
    wg_out.wait()
    down.y_event(0)
    up.x_event(1)
    up.finish()
    outs.append(net.here(wu_v, wu_o))

    def up_events_1():
        rsc.send_mid(1)
        rsc.send_mid(0)

    def up_events_2():
        down.y_event(1)
        down.x_event(0)

    def up_events_3():
        down.y_event(2)
        down.x_event(1)

    @pl.loop(0, 4)
    def _(i):
        pl.when(i == 1)(up_events_1)
        pl.when(i == 2)(up_events_2)
        pl.when(i == 3)(up_events_3)
        b = pick(i, z)
        up_block(b)
        ux_cp(2, b).start()
        ux_cp(1, b).start()

    outs.append(net.here(u_v, u_o))
    ag.drain()
    gate.drain()
    n_out.wait()
    down.y_event(3)
    down.x_event(2)
    down.x_event(3)
    down.finish()

    def down_block(b):
        @pl.loop(0, dim // dwide)
        def _(j):
            cols = ds(j * dwide, dwide)
            n_v[ds(b * sub, sub), cols] = dot(wg_v[ds(b * sub, sub), :], wd_v[:, cols]).astype(BF16)

    @pl.loop(0, 4)
    def _(i):
        down_block(pick(3 - i, z))
        for step in range(3):
            pl.when(i == step)(lambda step=step: rs2[0].send_end(2 - step))

    rs2[1].send_end(2)
    dg_v[...] = jnp.zeros_like(dg_v)
    for i in (2, 1, 0):
        rs2[0].send_mid(i)
    rsc.finish()
    for k in far_first:
        d_cp(k).wait_recv()
    d_own.wait()
    step = 16

    def norm_half(half):
        @pl.loop(0, hs // step)
        def _(r):
            at = half * hs + r * step
            view, mine, far = ds(at, step), ds(z * sub + at, step), ds(4 * sub + at, step)

            def whole(part, got):
                right = jnp.where(z < 3, got[mine, :].astype(F32), 0.0)
                left = jnp.where(z > 0, got[far, :].astype(F32), 0.0)
                return part[mine, :].astype(F32) + right + left

            resid = (rows[view, :].astype(F32) + whole(n_v, rbuf2)).astype(BF16)
            dy = whole(p_v, rbuf)
            res_v[view, :] = resid
            x = resid.astype(F32)
            inv = lax.rsqrt(jnp.sum(x * x, axis=1, keepdims=True) / dim + NORM_EPS)
            xhat = x * inv
            gain = gains[1:2, :]
            n2_v[view, :] = (xhat * gain).astype(BF16)
            part = dy * xhat
            dg_v[...] += part[:8] + part[8:]
            inner = jnp.sum(part * gain, axis=1, keepdims=True) / dim
            dres = dh2_v[view, :].astype(F32) + inv * (dy * gain) - xhat * (inv * inner)
            dres_v[view, pl.ds(0, dim)] = dres
            wg_v[ds(tokens + z * sub + at, step), :] = dres.astype(BF16)

    def spread(b, half):
        for k in far_first:
            ex_cp(k, b, half).start()

    def back_block(b):
        view = ds(b * sub, sub)

        @pl.loop(0, ff // tile)
        def _(j):
            cols = ds(j * tile, tile)
            du = dot(wg_v[ds(tokens + b * sub, sub), :], wd_v[ds(j * tile, tile), :], NT_DIMS)
            aa = a_v[view, cols].astype(F32)
            bb = b_v[view, cols].astype(F32)
            sig = jax.nn.sigmoid(aa)
            a_v[view, cols] = (du * bb * sig * (1.0 + aa * (1.0 - sig))).astype(BF16)
            b_v[view, cols] = (du * aa * sig).astype(BF16)

    s1, s2, s3 = ag.slots
    rs2[0].finish()
    tab_out.wait()
    norm_half(0)
    ag2[0].start()
    rs2[1].send_end(1)
    rs2[1].send_end(0)
    rs2[1].send_mid(2)
    ag2[0].near_mid()
    ag2[0].far_mid()
    rs2[1].send_mid(1)
    rs2[1].send_mid(0)
    ag2[0].step3_mid()
    spread(z, 0)
    rs2[1].finish()
    norm_half(1)
    ag2[1].start()
    ag2[0].near_end()
    spread(z, 1)
    for k in far_first:
        o_cp(k, tx).start()
    outs += [net.here(res_v.at[:, pl.ds(0, dt)], home_o.at[ds(tx * sub, sub), :]), net.here(n2_v, n2_o), net.here(dres_v.at[:, pl.ds(0, dim)], dres_o), net.here(dg_v, dg_o)]

    rsc.drain()
    for h in range(2):
        rs2[h].drain()
    n_in = net.here(n_o, p_v)

    def back_events_1():
        ag2[1].near_mid()
        ag2[1].far_mid()
        spread(s1, 0)
        ag2[0].step2()
        spread(s2, 0)
        ag2[1].near_end()
        spread(s1, 1)

    def back_events_2():
        ag2[1].step2()
        spread(s2, 1)
        ag2[0].step3_end()
        spread(s3, 0)
        ag2[1].step3_mid()
        for j in range(4):
            ux_cp(2, ag_order[j]).wait_recv()
            ux_cp(3, ag_order[j]).start()

    def back_events_3():
        ag2[1].step3_end()
        spread(s3, 1)

    ag_order = (z, s1, s2, s3)

    @pl.loop(0, 4)
    def _(i):
        pl.when(i == 1)(back_events_1)
        pl.when(i == 2)(back_events_2)
        pl.when(i == 3)(back_events_3)
        back_block(pick(i, z))

    outs.append(net.here(e_v, e_o))
    outs += [net.here(a_v, da_o), net.here(b_v, db_o)]

    last = pl.ds(ff - ff // 4, ff // 4)

    def down_tile(k, j):
        return dot(wg_v[pl.ds(0, tokens), last], wg_v[pl.ds(tokens, tokens), pl.ds(k * dt, dt)], ROWS_ROWS)

    def gate_tile(k, j):
        return dot(p_v[:, pl.ds(k * dt, dt)], a_v[:, ds(j * (ff // 4), ff // 4)], ROWS_ROWS)

    quarter = [rbuf.at[pl.ds(0, ff // 4), pl.ds(i * dt, dt)] for i in range(4)]
    part_d = GradReduce(net, peer, down_tile, 1, quarter[0], quarter[1], quarter[2], quarter[3], d2_o, d0_o, None, dc_o, None)
    part_g = GradReduce(net, peer, gate_tile, 4, n_v.at[pl.ds(0, dt), :], None, None, None, g2_o, None, None, wg_o, None)
    n_in.wait()
    part_d.step3()
    part_d.step1()
    part_g.step3()
    part_d.step2()
    outs.append(net.here(quarter[2], dc_o))
    for k in far_first:
        o_cp(k, peer[k]).wait_recv()
        for b in range(4):
            ex_cp(k, b, 0).wait_recv()
            ex_cp(k, b, 1).wait_recv()
    for b in range(4):
        ux_cp(1, b).wait_recv()
        ux_cp(3, b).wait_recv()
    for c in outs:
        c.wait()
    for k in far_first:
        g_cp(k).wait_send()
        h_cp(k).wait_send()
        d_cp(k).wait_send()
        o_cp(k, tx).wait_send()
        for b in range(4):
            ux_cp(k, b).wait_send()
            ex_cp(k, b, 0).wait_send()
            ex_cp(k, b, 1).wait_send()
    for w in (qkv, up, down):
        w.drain()
    for h in range(2):
        ag2[h].drain()
    part_d.cp(1).wait_recv()
    part_d.sent_locally()
    part_g.cp(0).wait_recv()
    part_g.cp(0).wait_send()


def call_ab(hid, eqh, ekvh, ang, swap, dh2h, wg, wu, wd, wq, gin):
    tokens, dt = hid.shape
    sub, dim, ff, width, q_width = tokens // 4, dt * 4, wg.shape[1], wq.shape[1], eqh.shape[1]
    s = jax.ShapeDtypeStruct
    tok_ff, tok_d, row = s((tokens, ff), BF16), s((tokens, dim), BF16), s((sub, dim), BF16)
    shapes = (tok_d, tok_ff, tok_ff, tok_ff, s((dim, ff), BF16), s((dim, ff), BF16), s((dim, width), BF16), s((tokens, width), BF16),
              row, s((8, dim), F32), tok_d, row, s((sub, dim), F32), s((tokens, dt), BF16), s((8, dim), F32),
              s((3, tokens, ff - ff // 4), BF16), s((3, tokens, dt), BF16), s((sub, 2048), F32), s((dt, ff), BF16)) + (s((ff // 4, dt), BF16),) * 3
    vrow, vtok, vff = VMEM((sub, dim), BF16), VMEM((tokens, dim), BF16), VMEM((tokens, ff), BF16)
    return pl.pallas_call(
        functools.partial(kernel_ab, q_width), out_shape=shapes, in_specs=[ANY] * 11, out_specs=[ANY] * len(shapes),
        scratch_shapes=[
            vrow, vrow, vrow, vrow, VMEM((sub, max(dim, 2048)), F32), vtok, vff, vff, VMEM((dim, ff), BF16), VMEM((dim, ff), BF16), VMEM((ff, dim), BF16),
            VMEM((dim, width), BF16), VMEM((tokens, width), BF16), vtok, VMEM((5 * sub, dim), BF16), VMEM((5 * sub, dim), BF16),
            VMEM((8, dim), F32), VMEM((8, dim), F32), VMEM((128, 128), BF16),
            pltpu.SemaphoreType.DMA((170,)), pltpu.SemaphoreType.DMA((170,)), pltpu.SemaphoreType.DMA((48,))],
        compiler_params=pltpu.CompilerParams(collective_id=0, has_side_effects=True, vmem_limit_bytes=VMEM_LIMIT),
        cost_estimate=pl.CostEstimate(flops=20 * tokens * dim * ff, bytes_accessed=100000000, transcendentals=0), name="phase_ab",
    )(hid, eqh, ekvh, ang, swap, dh2h, wg, wu, wd, wq, gin)


def kernel_c(q_width, da_h, db_h, wg_h, wu_h, n_h, u_h, ux_h, e_h, ex_h, n2_h, eq_h, wq_h, h_h, dres_h, g_h, dga_h, tabh, swaph, g2, d0, dc,
             wgo, wgy, wuo, wuy, wdo, wqo, wqy, q_o, kv_o, dh_o, dg_o, g0, u2, u0, q2, q0, qx, dy,
             wg_v, wu_v, da_v, db_v, n_v, p_v, rbuf, n2_v, st3, st1, cross_g, cross_u, stage, tiles_v, dres_v, wq_v, eq_v,
             gains, dg_v, dgr, dgz, tab_v, swap_v, send, recv, local):
    dp, z, tx, peer = places()
    tokens, ff = da_v.shape
    sub, dim = dres_v.shape
    dt = dim // 4
    width = eq_v.shape[1]
    tile = ff // 4
    dtile = min(512, dim)
    qt = min(256, tile)
    far_first = (2, 3, 1)
    net = Wires(send, recv, local)
    n2_in = net.here(n2_h, n2_v.at[ds(z * sub, sub), :])
    first = [net.here(n_h, n_v), net.here(da_h, da_v)]
    second = [net.here(db_h, db_v), net.here(wg_h, wg_v), net.here(wu_h, wu_v)]
    third = [net.here(wq_h, wq_v), net.here(eq_h, eq_v), net.here(dres_h, dres_v), net.here(g_h, gains),
             net.here(dga_h, dg_v.at[pl.ds(8, 8), :]), net.here(tabh, tab_v), net.here(swaph, swap_v)]
    sem = pltpu.get_barrier_semaphore()
    zs = tuple((z + i) % 4 for i in range(4))
    for i in (1, 2, 3):
        pl.semaphore_signal(sem, inc=1, device_id={"tx": peer[i]}, device_id_type=MESH)
        pl.semaphore_signal(sem, inc=1, device_id={"ty": zs[i]}, device_id_type=MESH)
    pl.semaphore_wait(sem, 6)
    rsc = LineScatter(net, p_v, rbuf, sub, z)
    ag = LineGather(net, n2_v, sub, z)
    q_id, h_id, t_id, z_id = net.take(4), net.take(4), net.take(4), net.take(4)

    def grad_tile(lhs, rhs, w):
        def go(k, j):
            cols = pl.ds(j * w, w) if isinstance(j, int) else ds(j * w, w)
            return dot(lhs[:, pl.ds(k * dt, dt)], rhs[:, cols], ROWS_ROWS)
        return go

    gate = GradReduce(net, peer, grad_tile(n_v, da_v, tile), ff // tile, st3, st1, cross_g, stage, g2, g0, wgy, wgo, tiles_v)
    up = GradReduce(net, peer, grad_tile(n_v, db_v, tile), ff // tile, st3, st1, cross_u, stage, u2, u0, wuy, wuo, tiles_v)
    d_id = net.take(1)

    def dy_cp():
        return net.copy(dc, dy, d_id, d_id, tx=peer[2])

    dy_cp().start()

    def corner(r, c):
        return da_v.at[pl.ds(r * dt, dt), pl.ds(c * width, width)]

    qkv = GradReduce(net, peer, grad_tile(n2_v, eq_v, qt), width // qt, corner(0, 0), corner(1, 0), corner(0, 1), corner(1, 1),
                     q2, q0, wqy, wqo, tiles_v)

    def dn_block(b):
        rows = ds(b * sub, sub)

        @pl.loop(0, dim // dtile)
        def _(j):
            wr = ds(j * dtile, dtile)
            p_v[rows, wr] = (dot(da_v[rows, :], wg_v[wr, :], NT_DIMS) + dot(db_v[rows, :], wu_v[wr, :], NT_DIMS)).astype(BF16)

    n2_in.wait()
    ag.start()
    for c in first:
        c.wait()
    gate.step2(True)
    gate.send()
    gate.step1()
    for c in second:
        c.wait()

    @pl.loop(0, 4)
    def _(i):
        pl.when(i == 1)(ag.step1)
        dn_block(pick(3 - i, z))
        for step in range(3):
            pl.when(i == step)(lambda step=step: rsc.send_end(2 - step))

    gate.cp(1).wait_send()
    up.step3()
    up.step1()
    up.step2()
    up.send()
    rsc.send_mid(2)
    ag.step2()
    ag.step3_mid()
    up.sent_locally()
    h_in = net.here(h_h, st3.at[pl.ds(0, sub), :])
    gate.step0(st1)
    gate.sent()

    n_tiles = ff // tile
    e_in = [net.here(e_h.at[:, pl.ds(0, dt)], wu_v.at[pl.ds(0, tokens), pl.ds(0, dt)])]
    for k in (1, 2, 3):
        e_in.append(net.here(ex_h.at[k - 1], wu_v.at[pl.ds(0, tokens), pl.ds(k * dt, dt)]))

    def u_place(j, k):
        return wg_v.at[pl.ds((j % 2) * tokens, tokens), pl.ds(k * tile, tile)]

    def u_load(j):
        cols = pl.ds(j * tile, tile)
        if j == n_tiles - 1:
            return [net.here(u_h.at[:, cols], u_place(j, 0)), net.here(d0, stage.at[pl.ds(0, tile), pl.ds(0, dt)]), net.here(dy, stage.at[pl.ds(0, tile), pl.ds(dt, dt)])]
        return [net.here(u_h.at[:, cols] if k == 0 else ux_h.at[k - 1, :, cols], u_place(j, k)) for k in range(4)]

    def down_tile(j, slot, loads):
        for c in loads:
            c.wait()
        acc = None
        if j == n_tiles - 1:
            acc = stage[pl.ds(0, tile), pl.ds(0, dt)].astype(F32) + stage[pl.ds(0, tile), pl.ds(dt, dt)].astype(F32)
        for k in range(1 if j == n_tiles - 1 else 4):
            part = dot(u_place(j, k)[...], wu_v[pl.ds(0, tokens), pl.ds(k * dt, dt)], ROWS_ROWS)
            acc = part if acc is None else acc + part
        tiles_v[slot, pl.ds(0, tile), pl.ds(0, dt)] = acc
        return net.here(tiles_v.at[slot, pl.ds(0, tile), pl.ds(0, dt)], wdo.at[pl.ds(j * tile, tile), :])

    loads = {0: u_load(0), 1: u_load(1)}
    rsc.send_mid(1)
    rsc.send_mid(0)
    for c in e_in:
        c.wait()
    done = [down_tile(0, 0, loads[0]), down_tile(1, 1, loads[1])]
    loads = {2: u_load(2)}
    for c in third:
        c.wait()
    ag.step3_end()

    @pl.loop(0, 4)
    def _(b):
        rows = ds(b * sub, sub)

        @pl.loop(0, width // qt)
        def _(j):
            cols = ds(j * qt, qt)
            wu_v[ds(tokens + b * sub, sub), cols] = dot(n2_v[rows, :], wq_v[:, cols]).astype(BF16)

    def q_cp(k, block):
        return net.copy(wu_v.at[ds(tokens + peer[k] * sub, sub), pl.ds(0, width)], qx.at[ds(block * sub, sub), :], q_id + k, q_id + k, tx=peer[k])

    for k in far_first:
        q_cp(k, tx).start()
    q_own = net.here(wu_v.at[ds(tokens + tx * sub, sub), pl.ds(0, width)], qx.at[ds(tx * sub, sub), :])
    for c in done:
        c.wait()
    qkv.step3()
    qkv.step1()
    dy_cp().wait_recv()
    loads[3] = u_load(3)
    done = [down_tile(2, 0, loads[2]), down_tile(3, 1, loads[3])]
    h_in.wait()
    rsc.finish()
    dg_v[pl.ds(0, 8), :] = jnp.zeros((8, dim), F32)
    step = 16

    @pl.loop(0, sub // step)
    def _(r):
        view, mine, far = ds(r * step, step), ds(z * sub + r * step, step), ds(4 * sub + r * step, step)
        right = jnp.where(z < 3, rbuf[mine, :].astype(F32), 0.0)
        left = jnp.where(z > 0, rbuf[far, :].astype(F32), 0.0)
        dy = p_v[mine, :].astype(F32) + right + left
        x = st3[view, :].astype(F32)
        inv = lax.rsqrt(jnp.sum(x * x, axis=1, keepdims=True) / dim + NORM_EPS)
        xhat = x * inv
        gain = gains[0:1, :]
        part = dy * xhat
        dg_v[pl.ds(0, 8), :] += part[:8] + part[8:]
        inner = jnp.sum(part * gain, axis=1, keepdims=True) / dim
        st1[view, :] = (dres_v[view, :] + inv * (dy * gain) - xhat * (inv * inner)).astype(BF16)

    def h_cp(k, block):
        return net.copy(st1.at[pl.ds(0, sub), pl.ds(k * dt, dt)], dh_o.at[ds(block * sub, sub), :], h_id + k, h_id + k, tx=peer[k])

    def t_cp(k):
        return net.copy(dg_v.at[:, pl.ds(k * dt, dt)], dgr.at[k], t_id + k, t_id + k, tx=peer[k])

    def z_cp(i):
        return net.copy(dgr.at[0], dgz.at[i], z_id + i, z_id + i, ty=zs[i])

    for k in far_first:
        t_cp(k).start()
    for k in far_first:
        h_cp(k, tx).start()
    h_own = net.here(st1.at[pl.ds(0, sub), pl.ds(0, dt)], dh_o.at[ds(tx * sub, sub), :])
    qkv.step2()
    qkv.send()
    up.sent()
    for c in done:
        c.wait()
    up.step0(cross_g)
    for k in far_first:
        q_cp(k, peer[k]).wait_recv()
    q_own.wait()
    turned = wu_v.at[pl.ds(tokens, tokens), pl.ds(width, width)]
    net.here(qx, turned).wait()
    turn(turned, turned, tokens, width, q_width, tab_v, swap_v, False)
    q_out = net.here(wu_v.at[pl.ds(tokens, tokens), pl.ds(width, q_width)], q_o)
    kv_out = net.here(wu_v.at[pl.ds(tokens, tokens), pl.ds(width + q_width, width - q_width)], kv_o)
    for k in far_first:
        t_cp(k).wait_recv()
    dgr[0] = dg_v[:, pl.ds(0, dt)] + dgr[1] + dgr[2] + dgr[3]
    for i in (1, 2, 3):
        z_cp(i).start()
    for i in (1, 2, 3):
        z_cp(i).wait_recv()
    dgz[0] = dgr[0] + dgz[1] + dgz[2] + dgz[3]
    dg_out = net.here(dgz.at[0], dg_o)
    for k in far_first:
        h_cp(k, peer[k]).wait_recv()
    qkv.step0(cross_g.at[:, pl.ds(0, width)])
    for c in (q_out, kv_out, dg_out, h_own):
        c.wait()
    dy_cp().wait_send()
    qkv.sent_locally()
    qkv.sent()
    for k in far_first:
        q_cp(k, tx).wait_send()
        h_cp(k, tx).wait_send()
        t_cp(k).wait_send()
        z_cp(k).wait_send()
    ag.drain()
    rsc.drain()


def call_c(q_width, *args):
    tokens, ff = args[0].shape
    sub, dim = args[9].shape
    dt, width = dim // 4, args[10].shape[1]
    tile = ff // 4
    s = jax.ShapeDtypeStruct
    wf, wb = s((dt, ff), F32), s((dt, ff), BF16)
    qf, qb = s((dt, width), F32), s((dt, width), BF16)
    shapes = (wf, wb, wf, wb, s((ff, dt), F32), qf, qb, s((tokens, q_width), BF16), s((tokens, width - q_width), BF16), s((tokens, dt), BF16), s((16, dt), F32),
              wb, wb, wb, qb, qb, s((tokens, width), BF16), s((tile, dt), BF16))
    return pl.pallas_call(
        functools.partial(kernel_c, q_width), out_shape=shapes, in_specs=[ANY] * len(args), out_specs=[ANY] * len(shapes),
        scratch_shapes=[
            VMEM((dim, ff), BF16), VMEM((dim, ff), BF16), VMEM((tokens, ff), BF16), VMEM((tokens, ff), BF16), VMEM((tokens, dim), BF16),
            VMEM((tokens, dim), BF16), VMEM((5 * sub, dim), BF16), VMEM((tokens, dim), BF16),
            VMEM((dt, ff), BF16), VMEM((dt, ff), BF16), VMEM((dt, ff), BF16), VMEM((dt, ff), BF16), VMEM((dt, ff), BF16),
            VMEM((2, max(dt, tile), max(dt, tile)), F32), VMEM((sub, dim), F32), VMEM((dim, width), BF16), VMEM((tokens, width), BF16),
            VMEM((8, dim), F32), VMEM((16, dim), F32), VMEM((4, 16, dt), F32), VMEM((4, 16, dt), F32), VMEM((sub, 2048), F32), VMEM((128, 128), BF16),
            pltpu.SemaphoreType.DMA((48,)), pltpu.SemaphoreType.DMA((48,)), pltpu.SemaphoreType.DMA((72,))],
        compiler_params=pltpu.CompilerParams(collective_id=2, has_side_effects=True, vmem_limit_bytes=VMEM_LIMIT),
        cost_estimate=pl.CostEstimate(flops=20 * tokens * dim * ff, bytes_accessed=100000000, transcendentals=0), name="phase_c",
    )(*args)


def solution(mesh):
    def local_step(hidden, positions, g_ffn, w_gate, w_up, w_down, g_attn, w_q, w_kv, grad_h2, grad_q, grad_kv):
        tokens, dt = hidden.shape
        q_heads, head_dim = w_q.shape[1:]
        kv_heads = w_kv.shape[1]
        q_width, kv_width = q_heads * head_dim, kv_heads * head_dim

        lane = np.arange(128)
        inv_freq = ROPE_BASE ** (-(lane % head_dim // 2 * 2).astype(np.float32) / head_dim)
        angles = positions.astype(F32)[:, None] * jnp.asarray(inv_freq, F32)[None, :]
        swap = np.zeros((128, 128), np.float32)
        swap[lane, lane ^ 1] = np.where(lane % 2 == 0, 1.0, -1.0)
        swap = jnp.asarray(swap, BF16)
        w_qkv_own = jnp.concatenate([w_q.reshape(dt, q_width), w_kv.reshape(dt, kv_width)], axis=1)
        gin = jnp.where(jnp.arange(8)[:, None] == 0, g_ffn[None, :], g_attn[None, :]).astype(F32)

        (normed_all, grad_gate, grad_up, u_all, gate_w, up_w, w_qkv, back_all, h_rows, gains, res_all, normed2, grad_res, resid_out, gattn8,
         u_other, e_other, table, wg_two, _, wd_zero, wd_cross) = call_ab(
             hidden, grad_q.reshape(tokens, q_width), grad_kv.reshape(tokens, kv_width), angles, swap, grad_h2, w_gate, w_up, w_down, w_qkv_own, gin)
        (grad_wgate, _, grad_wup, _, grad_wdown, grad_wqkv, _, q_flat, kv_flat, grad_hidden, gain_grads, *_) = call_c(
            q_width, grad_gate, grad_up, gate_w, up_w, normed_all, u_all, u_other, res_all, e_other, normed2, back_all, w_qkv,
            h_rows, grad_res, gains, gattn8, table, swap, wg_two, wd_zero, wd_cross)
        grad_wq = grad_wqkv[:, :q_width].reshape(dt, q_heads, head_dim)
        grad_wkv = grad_wqkv[:, q_width:].reshape(dt, kv_heads, head_dim)
        q_out = q_flat.reshape(tokens, q_heads, head_dim)
        kv_out = kv_flat.reshape(tokens, kv_heads, head_dim)
        grad_gffn = jnp.sum(gain_grads[:8], axis=0)
        grad_gattn = jnp.sum(gain_grads[8:], axis=0)
        return (resid_out, q_out, kv_out, grad_hidden, grad_gffn, grad_gattn, grad_wgate, grad_wup, grad_wdown, grad_wq, grad_wkv)

    row_spec = P(("dp", "ty"), "tx")
    head_spec = P(("dp", "tx"), "ty", None)
    in_specs = (row_spec, P(("dp", "tx")), P("tx"), P("tx", "ty"), P("tx", "ty"), P("ty", "tx"), P("tx"), P("tx", "ty", None), P("tx", "ty", None), row_spec, head_spec, head_spec)
    out_specs = (row_spec, head_spec, head_spec, row_spec, P(("dp", "tx")), P(("dp", "tx")), P(("dp", "tx"), "ty"), P(("dp", "tx"), "ty"), P(("dp", "ty"), "tx"), head_spec, head_spec)
    return jax.shard_map(local_step, mesh=mesh, in_specs=in_specs, out_specs=out_specs, check_vma=False)
```

```python
import functools

import jax
import jax.numpy as jnp
import numpy as np
from jax import lax
from jax.experimental import pallas as pl
from jax.experimental.pallas import tpu as pltpu
from jax.sharding import PartitionSpec as P

NORM_EPS = 1e-5
ROPE_BASE = 10000.0
F32 = jnp.float32
BF16 = jnp.bfloat16


def dot(a, b, dims=(((1,), (0,)), ((), ()))):
    return lax.dot_general(a, b, dims, preferred_element_type=F32)


MESH = pl.DeviceIdType.MESH
ANY = pl.BlockSpec(memory_space=pl.ANY)
VMEM = pltpu.VMEM
NT_DIMS = (((1,), (1,)), ((), ()))
VMEM_LIMIT = 67000000


def ds(start, size, align=None):
    if isinstance(start, int):
        return pl.ds(start, size)
    return pl.ds(pl.multiple_of(start, align or size), size)


def mid(z):
    return jnp.logical_and(z > 0, z < 3)


def end(z):
    return jnp.logical_or(z == 0, z == 3)


def slots(z):
    return (z + 1 - 2 * (z % 2), 2 - z // 2, 3 - 3 * (z // 2))


def turn(src, dst, rows, width, q_width, table_ref, swap_ref, back):
    step = rows // 4

    @pl.loop(0, 4)
    def _(r):
        for c in range(width // 128):
            cols = pl.ds(c * 128, 128)
            table = ds(r * 128 + (0 if c * 128 < q_width else 512), 128)
            x = src[ds(r * step, step), cols]
            main = x.astype(F32) * table_ref[:, table]
            side = dot(x, swap_ref[...]) * table_ref[:, ds(r * 128 + (1024 if c * 128 < q_width else 1536), 128)]
            dst[ds(r * step, step), cols] = (main - side if back else main + side).astype(BF16)


def pick(i, z):
    s1, s2, s3 = slots(z)
    first, last = (3 - i) // 3, (i // 2) * (i % 2)
    return z * first + s1 * ((i % 2) * (1 - i // 2)) + s2 * ((i // 2) * (1 - i % 2)) + s3 * last


class Wires:
    def __init__(self, send, recv, local):
        self.send, self.recv, self.local = send, recv, local
        self.n_remote = 0
        self.n_local = 0

    def take(self, n=1):
        base = self.n_remote
        self.n_remote += n
        assert self.n_remote <= self.send.shape[0]
        return base

    def copy(self, src, dst, si, ri, **dev):
        return pltpu.make_async_remote_copy(
            src_ref=src, dst_ref=dst, send_sem=self.send.at[si], recv_sem=self.recv.at[ri],
            device_id=dev, device_id_type=MESH)

    def here(self, src, dst):
        i = self.n_local
        self.n_local += 1
        assert i < self.local.shape[0]
        c = pltpu.make_async_copy(src, dst, self.local.at[i])
        c.start()
        return c


def entry_barrier(axes, z):
    sem = pltpu.get_barrier_semaphore()
    for dev in axes:
        pl.semaphore_signal(sem, inc=1, device_id=dev, device_id_type=MESH)

    @pl.when(z > 0)
    def _():
        pl.semaphore_signal(sem, inc=1, device_id={"ty": z - 1}, device_id_type=MESH)

    @pl.when(z < 3)
    def _():
        pl.semaphore_signal(sem, inc=1, device_id={"ty": z + 1}, device_id_type=MESH)

    @pl.when(mid(z))
    def _():
        pl.semaphore_wait(sem, len(axes) + 2)

    @pl.when(end(z))
    def _():
        pl.semaphore_wait(sem, len(axes) + 1)


class LineGather:
    def __init__(self, net, buf, rows, z, off=0, part=None):
        self.net, self.buf, self.rows, self.z, self.off, self.part = net, buf, rows, z, off, part or rows
        self.base = net.take(8)
        self.slots = slots(z)

    def blk(self, b):
        return self.buf.at[ds(b * self.rows + self.off, self.part), :]

    def cp(self, b, side, target):
        return self.net.copy(self.blk(b), self.blk(b), self.base + side * 4 + b, self.base + b, ty=target)

    def start(self):
        z = self.z

        @pl.when(z < 3)
        def _():
            self.cp(z, 0, z + 1).start()

        @pl.when(z > 0)
        def _():
            self.cp(z, 1, z - 1).start()

    def take(self, i):
        b = self.slots[i]
        self.cp(b, 0, self.z).wait_recv()

    def forward(self, i):
        z, b = self.z, self.slots[i]
        target = 3 - z if i == 0 else 3 * (z - 1)
        self.cp(b, 0, target).start()

    def step1(self):
        self.take(0)

        @pl.when(mid(self.z))
        def _():
            self.forward(0)
            self.take(1)
            self.forward(1)

    def near_end(self):
        @pl.when(end(self.z))
        def _():
            self.take(0)

    def near_mid(self):
        @pl.when(mid(self.z))
        def _():
            self.take(1)
            self.forward(1)

    def far_mid(self):
        @pl.when(mid(self.z))
        def _():
            self.take(0)
            self.forward(0)

    def step2(self):
        @pl.when(end(self.z))
        def _():
            self.take(1)

    def step3_mid(self):
        @pl.when(mid(self.z))
        def _():
            self.take(2)
            self.forward(2)

    def step3_end(self):
        @pl.when(end(self.z))
        def _():
            self.take(2)

    def drain(self):
        z = self.z

        @pl.when(z < 3)
        def _():
            self.cp(z, 0, z + 1).wait_send()

        @pl.when(z > 0)
        def _():
            self.cp(z, 1, z - 1).wait_send()

        @pl.when(mid(z))
        def _():
            for i in range(3):
                self.cp(self.slots[i], 0, 3 - z if i == 0 else 3 * (z - 1)).wait_send()


class LineScatter:
    def __init__(self, net, part, rbuf, rows, z, off=0, size=None):
        self.net, self.part, self.rbuf, self.rows, self.z, self.off, self.size = net, part, rbuf, rows, z, off, size or rows
        self.base = net.take(5)
        self.slots = slots(z)
        one = (z % 2) * (1 - z // 2)
        self.dst = (self.slots[0] + (1 - z % 2) * (3 - z), self.slots[1] + 2 * one, self.slots[2])
        self.target = (z + 1 - 2 * (z % 2), 1 + z % 2, 1 + z % 2)

    def cp(self, i):
        return self.net.copy(
            self.part.at[self.view(self.slots[i]), :], self.rbuf.at[self.view(self.dst[i]), :],
            self.base + i, self.base + self.dst[i], ty=self.target[i])

    def view(self, b):
        return ds(b * self.rows + self.off, self.size)

    def wait_slot(self, s):
        view = self.rbuf.at[self.view(s), :]
        self.net.copy(view, view, self.base, self.base + s, ty=self.z).wait_recv()

    def send_end(self, i):
        @pl.when(end(self.z))
        def _():
            self.cp(i).start()

    def send_mid(self, i):
        @pl.when(mid(self.z))
        def _():
            b = self.slots[i]
            self.wait_slot(b)
            step = 16

            @pl.loop(0, self.size // step)
            def _(r):
                view = ds(b * self.rows + self.off + r * step, step)
                self.part[view, :] = (self.part[view, :].astype(F32) + self.rbuf[view, :].astype(F32)).astype(BF16)

            self.cp(i).start()

    def finish(self):
        z = self.z

        @pl.when(z < 3)
        def _():
            self.wait_slot(z)

        @pl.when(z > 0)
        def _():
            self.wait_slot(4)

    def drain(self):
        for i in range(3):
            self.cp(i).wait_send()


class WeightGather:
    def __init__(self, net, w, full, pos, by_rows, chunks, direct=0):
        self.net, self.w, self.full, self.by_rows = net, w, full, by_rows
        self.dp, self.t1, self.t2 = pos
        self.half = w.shape[0] // 2
        self.width = w.shape[0] if by_rows else w.shape[1]
        self.chunks, self.direct = chunks, direct
        self.base = net.take(1 + 4 * chunks + direct)

    def area(self, half, ch):
        if self.by_rows:
            n = self.w.shape[1] // self.chunks
            return ds(half * self.half, self.half, 16), self.half, pl.ds(ch * n, n)
        n = self.half // self.chunks
        return ds(half * self.half + ch * n, n, 16), n, pl.ds(0, self.width)

    def src(self, half, ch):
        rows, _, cols = self.area(half, ch)
        return self.w.at[rows, cols]

    def dst(self, k, half, ch):
        if self.by_rows:
            _, _, cols = self.area(half, ch)
            return self.full.at[ds(k * self.width + half * self.half, self.half, 16), cols]
        rows, _, _ = self.area(half, ch)
        return self.full.at[rows, pl.ds(k * self.width, self.width)]

    def whole(self, k):
        if self.by_rows:
            return self.full.at[pl.ds(k * self.width, self.width), :]
        return self.full.at[:, pl.ds(k * self.width, self.width)]

    def near(self, ch):
        i = self.base + 1 + ch
        return self.net.copy(self.src(self.dp, ch), self.dst(2, self.dp, ch), i, i, tx=self.t2)

    def cross(self, ch, half):
        i = self.base + 1 + self.chunks + ch
        return self.net.copy(self.dst(2, half, ch), self.dst(2, half, ch), i, i, dp=1 - self.dp)

    def diag(self, ch, which, half):
        i = self.base + 1 + (2 + which) * self.chunks + ch
        return self.net.copy(self.dst(2, half, ch), self.dst(3, half, ch), i, i, tx=self.t1)

    def mate(self):
        return self.net.copy(self.w, self.whole(1), self.base, self.base, tx=self.t1)

    def straight(self, n, half):
        ch = self.chunks - 1 - n
        i = self.base + 1 + 4 * self.chunks + n
        return self.net.copy(self.src(half, ch), self.dst(2, half, ch), i, i, tx=self.t2)

    def start_y(self):
        for ch in range(self.chunks):
            self.near(ch).start()
        for n in range(self.direct):
            self.straight(n, 1 - self.dp).start()

    def start_local(self):
        self.own = self.net.here(self.w, self.whole(0))
        self.mate().start()

    def y_event(self, ch):
        self.near(ch).wait_recv()
        if ch < self.chunks - self.direct:
            self.cross(ch, self.dp).start()
        self.diag(ch, 0, self.dp).start()

    def x_event(self, ch):
        if ch < self.chunks - self.direct:
            self.cross(ch, 1 - self.dp).wait_recv()
        else:
            self.straight(self.chunks - 1 - ch, 1 - self.dp).wait_recv()
        self.diag(ch, 1, 1 - self.dp).start()

    def finish_local(self):
        self.own.wait()
        self.mate().wait_recv()

    def finish(self, ch):
        self.diag(ch, 0, self.dp).wait_recv()
        self.diag(ch, 1, 1 - self.dp).wait_recv()

    def drain(self):
        self.mate().wait_send()
        for ch in range(self.chunks):
            self.near(ch).wait_send()
            if ch < self.chunks - self.direct:
                self.cross(ch, self.dp).wait_send()
            else:
                self.straight(self.chunks - 1 - ch, 1 - self.dp).wait_send()
            self.diag(ch, 0, self.dp).wait_send()
            self.diag(ch, 1, 1 - self.dp).wait_send()


def places():
    dp, z, tx = lax.axis_index("dp"), lax.axis_index("ty"), lax.axis_index("tx")
    return dp, z, tx, (tx, tx + 1 - 2 * (tx % 2), (tx + 2) % 4, 3 - tx)


ROWS_ROWS = (((0,), (0,)), ((), ()))


class GradReduce:
    def __init__(self, net, peer, tile, tiles, st3, st1, cross, stage, got2, got0, got_y, out, out_tiles):
        self.net, self.peer, self.tile, self.tiles = net, peer, tile, tiles
        self.st3, self.st1, self.cross, self.stage = st3, st1, cross, stage
        self.got2, self.got0, self.got_y, self.out, self.out_tiles = got2, got0, got_y, out, out_tiles
        self.src = None
        self.base = net.take(3)
        self.w = out.shape[1] // tiles

    def cp(self, i):
        src, dst, to = ((self.st3, self.got2, 1), (self.st1, self.got0, 1), (self.src or self.cross, self.got_y, 2))[i]
        return self.net.copy(src, dst, self.base + i, self.base + i, tx=self.peer[to])

    def fill(self, k, ref):
        @pl.loop(0, self.tiles)
        def _(j):
            ref[:, ds(j * self.w, self.w)] = self.tile(k, j).astype(BF16)

    def step3(self):
        self.fill(3, self.st3)
        self.cp(0).start()

    def step1(self):
        self.fill(1, self.st1)
        self.cp(1).start()

    def step2(self, received=False):
        if not received:
            self.cp(0).wait_recv()
        self.net.here(self.got2, self.stage).wait()

        @pl.loop(0, self.tiles)
        def _(j):
            cols = ds(j * self.w, self.w)
            self.cross[:, cols] = (self.tile(2, j) + self.stage[:, cols].astype(F32)).astype(BF16)

    def send(self, src=None):
        self.src = src
        self.cp(2).start()

    def step0(self, far):
        self.cp(1).wait_recv()
        self.cp(2).wait_recv()
        loads = [self.net.here(self.got0, self.stage), self.net.here(self.got_y, far)]
        for c in loads:
            c.wait()
        base = self.net.n_local
        self.net.n_local += 2

        def put(j, slot):
            src = self.out_tiles.at[slot, :, pl.ds(0, self.w)]
            return pltpu.make_async_copy(src, self.out.at[:, ds(j * self.w, self.w)], self.net.local.at[base + slot])

        @pl.loop(0, self.tiles)
        def _(j):
            cols = ds(j * self.w, self.w)
            slot = j % 2

            @pl.when(j >= 2)
            def _():
                put(j, slot).wait()

            self.out_tiles[slot, :, pl.ds(0, self.w)] = self.tile(0, j) + (self.stage[:, cols].astype(F32) + far[:, cols].astype(F32))
            put(j, slot).start()

        for slot in range(min(2, self.tiles)):
            put(slot, slot).wait()

    def sent_locally(self):
        self.cp(0).wait_send()
        self.cp(1).wait_send()

    def sent(self):
        self.cp(2).wait_send()


def kernel_ab(q_width, hid, eqh, ekvh, angh, swaph, dh2h, wg, wu, wd, wq, gin,
              n_o, da_o, db_o, u_o, wg_o, wu_o, wq_o, eq_o, h_o, g_o, e_o, n2_o, dres_o, home_o, dg_o, ux_o, ex_o, tab_o, g2_o, d2_o, d0_o, dc_o,
              rows, dh2_v, n2_v, res_v, dres_v, n_v, a_v, b_v, wg_v, wu_v, wd_v, wq_v, eq_v, p_v, rbuf, rbuf2, gains, dg_v, swap_v, send, recv, local):
    dp, z, tx, peer = places()
    sub, dim = rows.shape
    tokens = 4 * sub
    width = eq_v.shape[1]
    dt = dim // 4
    ff = wg.shape[1]
    wide = min(1024, ff)
    tile = min(512, ff)
    dwide = min(1024, dim)
    dtile = min(512, dim)
    hs = sub // 2
    net = Wires(send, recv, local)
    turn_in = [net.here(eqh, p_v.at[:, pl.ds(0, q_width)]), net.here(ekvh, p_v.at[:, pl.ds(q_width, width - q_width)]), net.here(swaph, swap_v)]
    turn_in += [net.here(angh.at[pl.ds(i * sub, sub), :], dres_v.at[:, pl.ds(i * 128, 128)]) for i in range(4)]
    entry_barrier([{"tx": peer[1]}, {"tx": peer[2]}, {"tx": peer[3]}, {"dp": 1 - dp}], z)

    pos = (dp, peer[1], peer[2])
    far_first = (2, 3, 1)
    g_id, h_id, e_id, d_id, o_id, u_id, x_id = (net.take(4), net.take(4), net.take(4), net.take(4), net.take(4), net.take(12), net.take(24))
    u_v = wg_v.at[pl.ds(0, tokens), :]
    e_v = wg_v.at[pl.ds(tokens, tokens), :]

    def g_cp(k):
        return net.copy(gin, gains.at[:, pl.ds(k * dt, dt)], g_id + k, g_id + k, tx=peer[k])

    def h_cp(k):
        return net.copy(hid.at[ds(peer[k] * sub, sub), :], rows.at[:, pl.ds(k * dt, dt)], h_id + k, h_id + k, tx=peer[k])

    def e_cp(k, block):
        return net.copy(p_v.at[ds(peer[k] * sub, sub), pl.ds(0, width)], eq_v.at[ds(block * sub, sub), :], e_id + k, e_id + k, tx=peer[k])

    def d_cp(k):
        return net.copy(dh2h.at[ds(peer[k] * sub, sub), :], dh2_v.at[:, pl.ds(k * dt, dt)], d_id + k, d_id + k, tx=peer[k])

    def o_cp(k, block):
        return net.copy(res_v.at[:, pl.ds(k * dt, dt)], home_o.at[ds(block * sub, sub), :], o_id + k, o_id + k, tx=peer[k])

    def ux_cp(k, b):
        view = ds(b * sub, sub)
        cols = pl.ds(0, ff - ff // 4)
        src = ux_o.at[1, view, :] if k == 3 else wg_v.at[view, cols]
        i = u_id + (k - 1) * 4 + b
        return net.copy(src, ux_o.at[k - 1, view, :], i, i, tx=peer[1] if k == 3 else peer[k])

    def ex_cp(k, b, half):
        i = x_id + half * 12 + (k - 1) * 4 + b
        view = ds(b * sub + half * hs, hs)
        return net.copy(wg_v.at[ds(tokens + b * sub + half * hs, hs), pl.ds(k * dt, dt)], ex_o.at[k - 1, view, :], i, i, tx=peer[k])

    gate = WeightGather(net, wg, wg_v, pos, True, 2)
    up = WeightGather(net, wu, wu_v, pos, True, 2)
    down = WeightGather(net, wd, wd_v, pos, False, 4, 1)
    qkv = WeightGather(net, wq, wq_v, pos, True, 1)
    ag = LineGather(net, n_v, sub, z)
    rsc = LineScatter(net, p_v, rbuf, sub, z)
    rs2 = [LineScatter(net, n_v, rbuf2, sub, z, h * hs, hs) for h in range(2)]
    ag2 = [LineGather(net, e_v, sub, z, h * hs, hs) for h in range(2)]

    for k in far_first:
        g_cp(k).start()
    for k in far_first:
        h_cp(k).start()
    g_own = net.here(gin, gains.at[:, pl.ds(0, dt)])
    h_own = net.here(hid.at[ds(tx * sub, sub), :], rows.at[:, pl.ds(0, dt)])
    for w in (qkv, gate, up, down):
        w.start_local()
    for c in turn_in:
        c.wait()

    @pl.loop(0, 4)
    def _(i):
        cos_q, cos_kv, sin_q, sin_kv = (ds(i * 128 + n * 512, 128) for n in range(4))
        angles = dres_v[:, cos_q]
        dres_v[:, sin_q] = jnp.sin(angles)
        dres_v[:, cos_q] = jnp.cos(angles)

        @pl.when(z < 2)
        def _():
            dres_v[:, cos_kv] = dres_v[:, cos_q]
            dres_v[:, sin_kv] = dres_v[:, sin_q]

        @pl.when(z >= 2)
        def _():
            dres_v[:, cos_kv] = jnp.ones((sub, 128), F32)
            dres_v[:, sin_kv] = jnp.zeros((sub, 128), F32)

    tab_out = net.here(dres_v.at[:, pl.ds(0, 2048)], tab_o)
    turn(p_v, p_v, tokens, width, q_width, dres_v, swap_v, True)
    for k in far_first:
        e_cp(k, tx).start()
    e_own = net.here(p_v.at[ds(tx * sub, sub), pl.ds(0, width)], eq_v.at[ds(tx * sub, sub), :])
    for w in (qkv, gate, up, down):
        w.start_y()
    for k in far_first:
        d_cp(k).start()
    d_own = net.here(dh2h.at[ds(tx * sub, sub), :], dh2_v.at[:, pl.ds(0, dt)])

    for k in far_first:
        g_cp(k).wait_recv()
        h_cp(k).wait_recv()
    g_own.wait()
    h_own.wait()

    @pl.loop(0, sub // 16)
    def _(r):
        x = rows[ds(r * 16, 16), :].astype(F32)
        inv = lax.rsqrt(jnp.sum(x * x, axis=1, keepdims=True) / dim + NORM_EPS)
        n_v[ds(z * sub + r * 16, 16), :] = (x * inv * gains[0:1, :]).astype(BF16)

    ag.start()
    outs = [net.here(rows, h_o), net.here(gains, g_o)]
    for k in far_first:
        e_cp(k, peer[k]).wait_recv()
    e_own.wait()
    ag.step1()
    qkv.y_event(0)
    qkv.x_event(0)
    qkv.finish_local()
    qkv.finish(0)
    for k in far_first:
        e_cp(k, tx).wait_send()

    def n2_block(b):
        @pl.loop(0, dim // dtile)
        def _(j):
            w = wq_v[ds(j * dtile, dtile), :]
            p_v[ds(b * sub, sub), ds(j * dtile, dtile)] = dot(eq_v[ds(b * sub, sub), :], w, NT_DIMS).astype(BF16)

    @pl.loop(0, 4)
    def _(i):
        n2_block(pick(3 - i, z))
        for step in range(3):
            pl.when(i == step)(lambda step=step: rsc.send_end(2 - step))
        pl.when(i == 0)(lambda: gate.y_event(0))

    wide = ff // 2

    def gate_part(b, c):
        cols = pl.ds(c * wide, wide)
        a_v[ds(b * sub, sub), cols] = dot(n_v[ds(b * sub, sub), :], wg_v[:, cols]).astype(BF16)

    def up_part(b, c):
        cols = pl.ds(c * wide, wide)
        bb = dot(n_v[ds(b * sub, sub), :], wu_v[:, cols]).astype(BF16)
        b_v[ds(b * sub, sub), cols] = bb
        aa = a_v[ds(b * sub, sub), cols].astype(F32)
        wg_v[ds(b * sub, sub), cols] = (aa * jax.nn.sigmoid(aa) * bb.astype(F32)).astype(BF16)

    def down_part(b, j):
        cols = pl.ds(j * (dim // 2), dim // 2)
        n_v[ds(b * sub, sub), cols] = dot(wg_v[ds(b * sub, sub), :], wd_v[:, cols]).astype(BF16)

    outs += [net.here(wq_v, wq_o), net.here(eq_v, eq_o)]
    gate.finish_local()
    gate.y_event(1)
    ag.step2()
    ag.step3_mid()
    gate.x_event(0)
    gate.finish(0)

    @pl.loop(0, 3)
    def _(i):
        gate_part(pick(i, z), 0)

    up.y_event(0)
    gate.x_event(1)
    rsc.send_mid(2)
    gate.finish(1)
    wg_out = net.here(wg_v, wg_o)

    @pl.loop(0, 3)
    def _(i):
        gate_part(pick(i, z), 1)

    up.finish_local()
    up.y_event(1)
    up.x_event(0)
    up.finish(0)
    ag.step3_end()

    @pl.loop(0, 2)
    def _(c):
        cols = ds(c * wide, wide)
        b = pick(3, z)
        a_v[ds(b * sub, sub), cols] = dot(n_v[ds(b * sub, sub), :], wg_v[:, cols]).astype(BF16)

    wg_out.wait()
    n_out = net.here(n_v, n_o)

    @pl.loop(0, 4)
    def _(i):
        pl.when(i == 1)(lambda: down.y_event(0))
        pl.when(i == 2)(lambda: down.y_event(1))
        pl.when(i == 3)(lambda: up.x_event(1))
        up_part(pick(i, z), 0)

    def up_events_1():
        rsc.send_mid(1)
        rsc.send_mid(0)
        down.x_event(0)

    def up_events_2():
        down.y_event(2)

    def up_events_3():
        down.y_event(3)
        down.x_event(1)

    up.finish(1)
    outs.append(net.here(wu_v, wu_o))

    @pl.loop(0, 4)
    def _(i):
        pl.when(i == 1)(up_events_1)
        pl.when(i == 2)(up_events_2)
        pl.when(i == 3)(up_events_3)
        b = pick(i, z)
        up_part(b, 1)
        ux_cp(2, b).start()
        ux_cp(1, b).start()

    outs.append(net.here(u_v, u_o))
    ag.drain()
    gate.drain()
    n_out.wait()
    down.finish_local()

    @pl.loop(0, 4)
    def _(i):
        pl.when(i == 2)(lambda: down.x_event(2))
        pl.when(i == 3)(lambda: down.x_event(3))
        down_part(pick(3 - i, z), 0)

    for ch in range(4):
        down.finish(ch)

    @pl.loop(0, 4)
    def _(i):
        down_part(pick(3 - i, z), 1)
        for step in range(3):
            pl.when(i == step)(lambda step=step: rs2[0].send_end(2 - step))

    rs2[1].send_end(2)
    dg_v[...] = jnp.zeros_like(dg_v)
    for i in (2, 1, 0):
        rs2[0].send_mid(i)
    rsc.finish()
    for k in far_first:
        d_cp(k).wait_recv()
    d_own.wait()
    step = 16

    def norm_half(half):
        @pl.loop(0, hs // step)
        def _(r):
            at = half * hs + r * step
            view, mine, far = ds(at, step), ds(z * sub + at, step), ds(4 * sub + at, step)

            def whole(part, got):
                right = jnp.where(z < 3, got[mine, :].astype(F32), 0.0)
                left = jnp.where(z > 0, got[far, :].astype(F32), 0.0)
                return part[mine, :].astype(F32) + right + left

            resid = (rows[view, :].astype(F32) + whole(n_v, rbuf2)).astype(BF16)
            dy = whole(p_v, rbuf)
            res_v[view, :] = resid
            x = resid.astype(F32)
            inv = lax.rsqrt(jnp.sum(x * x, axis=1, keepdims=True) / dim + NORM_EPS)
            xhat = x * inv
            gain = gains[1:2, :]
            n2_v[view, :] = (xhat * gain).astype(BF16)
            part = dy * xhat
            dg_v[...] += part[:8] + part[8:]
            inner = jnp.sum(part * gain, axis=1, keepdims=True) / dim
            dres = dh2_v[view, :].astype(F32) + inv * (dy * gain) - xhat * (inv * inner)
            dres_v[view, pl.ds(0, dim)] = dres
            wg_v[ds(tokens + z * sub + at, step), :] = dres.astype(BF16)

    def spread(b, half):
        for k in far_first:
            ex_cp(k, b, half).start()

    def back_block(b):
        view = ds(b * sub, sub)

        @pl.loop(0, ff // tile)
        def _(j):
            cols = ds(j * tile, tile)
            du = dot(wg_v[ds(tokens + b * sub, sub), :], wd_v[ds(j * tile, tile), :], NT_DIMS)
            aa = a_v[view, cols].astype(F32)
            bb = b_v[view, cols].astype(F32)
            sig = jax.nn.sigmoid(aa)
            a_v[view, cols] = (du * bb * sig * (1.0 + aa * (1.0 - sig))).astype(BF16)
            b_v[view, cols] = (du * aa * sig).astype(BF16)

    s1, s2, s3 = ag.slots
    rs2[0].finish()
    tab_out.wait()
    norm_half(0)
    ag2[0].start()
    spread(z, 0)
    rs2[1].send_end(1)
    rs2[1].send_end(0)
    rs2[1].send_mid(2)
    ag2[0].near_mid()
    ag2[0].far_mid()
    rs2[1].send_mid(1)
    rs2[1].send_mid(0)
    ag2[0].step3_mid()

    @pl.when(mid(z))
    def _():
        for b in (s1, s2, s3):
            spread(b, 0)

    @pl.when(end(z))
    def _():
        ag2[0].take(0)
        spread(s1, 0)
        ag2[0].take(1)
        spread(s2, 0)

    rs2[1].finish()
    norm_half(1)
    ag2[1].start()
    spread(z, 1)
    for k in far_first:
        o_cp(k, tx).start()
    outs += [net.here(res_v.at[:, pl.ds(0, dt)], home_o.at[ds(tx * sub, sub), :]), net.here(n2_v, n2_o), net.here(dres_v.at[:, pl.ds(0, dim)], dres_o), net.here(dg_v, dg_o)]

    rsc.drain()
    for h in range(2):
        rs2[h].drain()
    n_in = net.here(n_o, p_v)

    def back_events_1():
        ag2[1].near_mid()
        ag2[1].far_mid()

        @pl.when(end(z))
        def _():
            ag2[1].take(0)

        spread(s1, 1)

    def back_events_2():
        @pl.when(end(z))
        def _():
            ag2[1].take(1)
            ag2[0].take(2)
            spread(s3, 0)

        ag2[1].step3_mid()
        spread(s2, 1)
        for j in range(4):
            ux_cp(2, ag_order[j]).wait_recv()
            ux_cp(3, ag_order[j]).start()

    def back_events_3():
        ag2[1].step3_end()
        spread(s3, 1)

    ag_order = (z, s1, s2, s3)

    @pl.loop(0, 4)
    def _(i):
        pl.when(i == 1)(back_events_1)
        pl.when(i == 2)(back_events_2)
        pl.when(i == 3)(back_events_3)
        back_block(pick(i, z))

    outs.append(net.here(e_v, e_o))
    outs += [net.here(a_v, da_o), net.here(b_v, db_o)]

    last = pl.ds(ff - ff // 4, ff // 4)

    def down_tile(k, j):
        return dot(wg_v[pl.ds(0, tokens), last], wg_v[pl.ds(tokens, tokens), pl.ds(k * dt, dt)], ROWS_ROWS)

    def gate_tile(k, j):
        return dot(p_v[:, pl.ds(k * dt, dt)], a_v[:, ds(j * (ff // 4), ff // 4)], ROWS_ROWS)

    quarter = [rbuf.at[pl.ds(0, ff // 4), pl.ds(i * dt, dt)] for i in range(4)]
    part_d = GradReduce(net, peer, down_tile, 1, quarter[0], quarter[1], quarter[2], quarter[3], d2_o, d0_o, None, dc_o, None)
    part_g = GradReduce(net, peer, gate_tile, 4, n_v.at[pl.ds(0, dt), :], None, None, None, g2_o, None, None, wg_o, None)
    n_in.wait()
    part_d.step3()
    part_d.step1()
    part_g.step3()
    part_d.step2()
    outs.append(net.here(quarter[2], dc_o))
    for k in far_first:
        o_cp(k, peer[k]).wait_recv()
        for b in range(4):
            ex_cp(k, b, 0).wait_recv()
            ex_cp(k, b, 1).wait_recv()
    for b in range(4):
        ux_cp(1, b).wait_recv()
        ux_cp(3, b).wait_recv()
    for c in outs:
        c.wait()
    for k in far_first:
        g_cp(k).wait_send()
        h_cp(k).wait_send()
        d_cp(k).wait_send()
        o_cp(k, tx).wait_send()
        for b in range(4):
            ux_cp(k, b).wait_send()
            ex_cp(k, b, 0).wait_send()
            ex_cp(k, b, 1).wait_send()
    for w in (qkv, up, down):
        w.drain()
    for h in range(2):
        ag2[h].drain()
    part_d.cp(1).wait_recv()
    part_d.sent_locally()
    part_g.cp(0).wait_recv()
    part_g.cp(0).wait_send()


def call_ab(hid, eqh, ekvh, ang, swap, dh2h, wg, wu, wd, wq, gin):
    tokens, dt = hid.shape
    sub, dim, ff, width, q_width = tokens // 4, dt * 4, wg.shape[1], wq.shape[1], eqh.shape[1]
    s = jax.ShapeDtypeStruct
    tok_ff, tok_d, row = s((tokens, ff), BF16), s((tokens, dim), BF16), s((sub, dim), BF16)
    shapes = (tok_d, tok_ff, tok_ff, tok_ff, s((dim, ff), BF16), s((dim, ff), BF16), s((dim, width), BF16), s((tokens, width), BF16),
              row, s((8, dim), F32), tok_d, row, s((sub, dim), F32), s((tokens, dt), BF16), s((8, dim), F32),
              s((3, tokens, ff - ff // 4), BF16), s((3, tokens, dt), BF16), s((sub, 2048), F32), s((dt, ff), BF16)) + (s((ff // 4, dt), BF16),) * 3
    vrow, vtok, vff = VMEM((sub, dim), BF16), VMEM((tokens, dim), BF16), VMEM((tokens, ff), BF16)
    return pl.pallas_call(
        functools.partial(kernel_ab, q_width), out_shape=shapes, in_specs=[ANY] * 11, out_specs=[ANY] * len(shapes),
        scratch_shapes=[
            vrow, vrow, vrow, vrow, VMEM((sub, max(dim, 2048)), F32), vtok, vff, vff, VMEM((dim, ff), BF16), VMEM((dim, ff), BF16), VMEM((ff, dim), BF16),
            VMEM((dim, width), BF16), VMEM((tokens, width), BF16), vtok, VMEM((5 * sub, dim), BF16), VMEM((5 * sub, dim), BF16),
            VMEM((8, dim), F32), VMEM((8, dim), F32), VMEM((128, 128), BF16),
            pltpu.SemaphoreType.DMA((170,)), pltpu.SemaphoreType.DMA((170,)), pltpu.SemaphoreType.DMA((48,))],
        compiler_params=pltpu.CompilerParams(collective_id=0, has_side_effects=True, vmem_limit_bytes=VMEM_LIMIT),
        cost_estimate=pl.CostEstimate(flops=20 * tokens * dim * ff, bytes_accessed=100000000, transcendentals=0), name="phase_ab",
    )(hid, eqh, ekvh, ang, swap, dh2h, wg, wu, wd, wq, gin)


def kernel_c(q_width, da_h, db_h, wg_h, wu_h, n_h, u_h, ux_h, e_h, ex_h, n2_h, eq_h, wq_h, h_h, dres_h, g_h, dga_h, tabh, swaph, g2, d0, dc,
             wgo, wgy, wuo, wuy, wdo, wqo, wqy, q_o, kv_o, dh_o, dg_o, g0, u2, u0, q2, q0, qx, dy,
             wg_v, wu_v, da_v, db_v, n_v, p_v, rbuf, n2_v, st3, st1, cross_g, cross_u, stage, tiles_v, dres_v, wq_v, eq_v,
             gains, dg_v, dgr, dgz, tab_v, swap_v, send, recv, local):
    dp, z, tx, peer = places()
    tokens, ff = da_v.shape
    sub, dim = dres_v.shape
    dt = dim // 4
    width = eq_v.shape[1]
    tile = ff // 4
    dtile = min(512, dim)
    qt = min(256, tile)
    far_first = (2, 3, 1)
    net = Wires(send, recv, local)
    n2_in = net.here(n2_h, n2_v.at[ds(z * sub, sub), :])
    first = [net.here(n_h, n_v), net.here(da_h, da_v)]
    second = [net.here(db_h, db_v), net.here(wg_h, wg_v), net.here(wu_h, wu_v)]
    third = [net.here(wq_h, wq_v), net.here(eq_h, eq_v), net.here(dres_h, dres_v), net.here(g_h, gains),
             net.here(dga_h, dg_v.at[pl.ds(8, 8), :]), net.here(tabh, tab_v), net.here(swaph, swap_v)]
    sem = pltpu.get_barrier_semaphore()
    zs = tuple((z + i) % 4 for i in range(4))
    for i in (1, 2, 3):
        pl.semaphore_signal(sem, inc=1, device_id={"tx": peer[i]}, device_id_type=MESH)
        pl.semaphore_signal(sem, inc=1, device_id={"ty": zs[i]}, device_id_type=MESH)
    pl.semaphore_wait(sem, 6)
    rsc = LineScatter(net, p_v, rbuf, sub, z)
    ag = LineGather(net, n2_v, sub, z)
    q_id, h_id, t_id, z_id = net.take(4), net.take(4), net.take(4), net.take(4)

    def grad_tile(lhs, rhs, w):
        def go(k, j):
            cols = pl.ds(j * w, w) if isinstance(j, int) else ds(j * w, w)
            return dot(lhs[:, pl.ds(k * dt, dt)], rhs[:, cols], ROWS_ROWS)
        return go

    gate = GradReduce(net, peer, grad_tile(n_v, da_v, tile), ff // tile, st3, st1, cross_g, stage, g2, g0, wgy, wgo, tiles_v)
    up = GradReduce(net, peer, grad_tile(n_v, db_v, tile), ff // tile, st3, st1, cross_u, stage, u2, u0, wuy, wuo, tiles_v)
    d_id = net.take(1)

    def dy_cp():
        return net.copy(dc, dy, d_id, d_id, tx=peer[2])

    dy_cp().start()

    def corner(r, c):
        return da_v.at[pl.ds(r * dt, dt), pl.ds(c * width, width)]

    qkv = GradReduce(net, peer, grad_tile(n2_v, eq_v, qt), width // qt, corner(0, 0), corner(1, 0), corner(0, 1), corner(1, 1),
                     q2, q0, wqy, wqo, tiles_v)

    def dn_block(b):
        rows = ds(b * sub, sub)

        @pl.loop(0, dim // dtile)
        def _(j):
            wr = ds(j * dtile, dtile)
            p_v[rows, wr] = (dot(da_v[rows, :], wg_v[wr, :], NT_DIMS) + dot(db_v[rows, :], wu_v[wr, :], NT_DIMS)).astype(BF16)

    n2_in.wait()
    ag.start()
    for c in first:
        c.wait()
    gate.step2(True)
    gate.send()
    gate.step1()
    for c in second:
        c.wait()

    @pl.loop(0, 4)
    def _(i):
        pl.when(i == 1)(ag.step1)
        dn_block(pick(3 - i, z))
        for step in range(3):
            pl.when(i == step)(lambda step=step: rsc.send_end(2 - step))

    gate.cp(1).wait_send()
    up.step3()
    up.step1()
    up.step2()
    up.send()
    rsc.send_mid(2)
    ag.step2()
    ag.step3_mid()
    up.sent_locally()
    h_in = net.here(h_h, st3.at[pl.ds(0, sub), :])
    gate.step0(st1)
    gate.sent()

    n_tiles = ff // tile
    e_in = [net.here(e_h.at[:, pl.ds(0, dt)], wu_v.at[pl.ds(0, tokens), pl.ds(0, dt)])]
    for k in (1, 2, 3):
        e_in.append(net.here(ex_h.at[k - 1], wu_v.at[pl.ds(0, tokens), pl.ds(k * dt, dt)]))

    def u_place(j, k):
        return wg_v.at[pl.ds((j % 2) * tokens, tokens), pl.ds(k * tile, tile)]

    def u_load(j):
        cols = pl.ds(j * tile, tile)
        if j == n_tiles - 1:
            return [net.here(u_h.at[:, cols], u_place(j, 0)), net.here(d0, stage.at[pl.ds(0, tile), pl.ds(0, dt)]), net.here(dy, stage.at[pl.ds(0, tile), pl.ds(dt, dt)])]
        return [net.here(u_h.at[:, cols] if k == 0 else ux_h.at[k - 1, :, cols], u_place(j, k)) for k in range(4)]

    def down_tile(j, slot, loads):
        for c in loads:
            c.wait()
        acc = None
        if j == n_tiles - 1:
            acc = stage[pl.ds(0, tile), pl.ds(0, dt)].astype(F32) + stage[pl.ds(0, tile), pl.ds(dt, dt)].astype(F32)
        for k in range(1 if j == n_tiles - 1 else 4):
            part = dot(u_place(j, k)[...], wu_v[pl.ds(0, tokens), pl.ds(k * dt, dt)], ROWS_ROWS)
            acc = part if acc is None else acc + part
        tiles_v[slot, pl.ds(0, tile), pl.ds(0, dt)] = acc
        return net.here(tiles_v.at[slot, pl.ds(0, tile), pl.ds(0, dt)], wdo.at[pl.ds(j * tile, tile), :])

    loads = {0: u_load(0), 1: u_load(1)}
    rsc.send_mid(1)
    rsc.send_mid(0)
    for c in e_in:
        c.wait()
    done = [down_tile(0, 0, loads[0]), down_tile(1, 1, loads[1])]
    loads = {2: u_load(2)}
    for c in third:
        c.wait()
    ag.step3_end()

    @pl.loop(0, 4)
    def _(b):
        rows = ds(b * sub, sub)

        @pl.loop(0, width // qt)
        def _(j):
            cols = ds(j * qt, qt)
            wu_v[ds(tokens + b * sub, sub), cols] = dot(n2_v[rows, :], wq_v[:, cols]).astype(BF16)

    def q_cp(k, block):
        return net.copy(wu_v.at[ds(tokens + peer[k] * sub, sub), pl.ds(0, width)], qx.at[ds(block * sub, sub), :], q_id + k, q_id + k, tx=peer[k])

    for k in far_first:
        q_cp(k, tx).start()
    q_own = net.here(wu_v.at[ds(tokens + tx * sub, sub), pl.ds(0, width)], qx.at[ds(tx * sub, sub), :])
    for c in done:
        c.wait()
    qkv.step3()
    qkv.step1()
    dy_cp().wait_recv()
    loads[3] = u_load(3)
    done = [down_tile(2, 0, loads[2]), down_tile(3, 1, loads[3])]
    h_in.wait()
    rsc.finish()
    dg_v[pl.ds(0, 8), :] = jnp.zeros((8, dim), F32)
    step = 16

    @pl.loop(0, sub // step)
    def _(r):
        view, mine, far = ds(r * step, step), ds(z * sub + r * step, step), ds(4 * sub + r * step, step)
        right = jnp.where(z < 3, rbuf[mine, :].astype(F32), 0.0)
        left = jnp.where(z > 0, rbuf[far, :].astype(F32), 0.0)
        dy = p_v[mine, :].astype(F32) + right + left
        x = st3[view, :].astype(F32)
        inv = lax.rsqrt(jnp.sum(x * x, axis=1, keepdims=True) / dim + NORM_EPS)
        xhat = x * inv
        gain = gains[0:1, :]
        part = dy * xhat
        dg_v[pl.ds(0, 8), :] += part[:8] + part[8:]
        inner = jnp.sum(part * gain, axis=1, keepdims=True) / dim
        st1[view, :] = (dres_v[view, :] + inv * (dy * gain) - xhat * (inv * inner)).astype(BF16)

    def h_cp(k, block):
        return net.copy(st1.at[pl.ds(0, sub), pl.ds(k * dt, dt)], dh_o.at[ds(block * sub, sub), :], h_id + k, h_id + k, tx=peer[k])

    def t_cp(k):
        return net.copy(dg_v.at[:, pl.ds(k * dt, dt)], dgr.at[k], t_id + k, t_id + k, tx=peer[k])

    def z_cp(i):
        return net.copy(dgr.at[0], dgz.at[i], z_id + i, z_id + i, ty=zs[i])

    for k in far_first:
        t_cp(k).start()
    for k in far_first:
        h_cp(k, tx).start()
    h_own = net.here(st1.at[pl.ds(0, sub), pl.ds(0, dt)], dh_o.at[ds(tx * sub, sub), :])
    qkv.step2()
    qkv.send()
    up.sent()
    for c in done:
        c.wait()
    up.step0(cross_g)
    for k in far_first:
        q_cp(k, peer[k]).wait_recv()
    q_own.wait()
    turned = wu_v.at[pl.ds(tokens, tokens), pl.ds(width, width)]
    net.here(qx, turned).wait()
    turn(turned, turned, tokens, width, q_width, tab_v, swap_v, False)
    q_out = net.here(wu_v.at[pl.ds(tokens, tokens), pl.ds(width, q_width)], q_o)
    kv_out = net.here(wu_v.at[pl.ds(tokens, tokens), pl.ds(width + q_width, width - q_width)], kv_o)
    for k in far_first:
        t_cp(k).wait_recv()
    dgr[0] = dg_v[:, pl.ds(0, dt)] + dgr[1] + dgr[2] + dgr[3]
    for i in (1, 2, 3):
        z_cp(i).start()
    for i in (1, 2, 3):
        z_cp(i).wait_recv()
    dgz[0] = dgr[0] + dgz[1] + dgz[2] + dgz[3]
    dg_out = net.here(dgz.at[0], dg_o)
    for k in far_first:
        h_cp(k, peer[k]).wait_recv()
    qkv.step0(cross_g.at[:, pl.ds(0, width)])
    for c in (q_out, kv_out, dg_out, h_own):
        c.wait()
    dy_cp().wait_send()
    qkv.sent_locally()
    qkv.sent()
    for k in far_first:
        q_cp(k, tx).wait_send()
        h_cp(k, tx).wait_send()
        t_cp(k).wait_send()
        z_cp(k).wait_send()
    ag.drain()
    rsc.drain()


def call_c(q_width, *args):
    tokens, ff = args[0].shape
    sub, dim = args[9].shape
    dt, width = dim // 4, args[10].shape[1]
    tile = ff // 4
    s = jax.ShapeDtypeStruct
    wf, wb = s((dt, ff), F32), s((dt, ff), BF16)
    qf, qb = s((dt, width), F32), s((dt, width), BF16)
    shapes = (wf, wb, wf, wb, s((ff, dt), F32), qf, qb, s((tokens, q_width), BF16), s((tokens, width - q_width), BF16), s((tokens, dt), BF16), s((16, dt), F32),
              wb, wb, wb, qb, qb, s((tokens, width), BF16), s((tile, dt), BF16))
    return pl.pallas_call(
        functools.partial(kernel_c, q_width), out_shape=shapes, in_specs=[ANY] * len(args), out_specs=[ANY] * len(shapes),
        scratch_shapes=[
            VMEM((dim, ff), BF16), VMEM((dim, ff), BF16), VMEM((tokens, ff), BF16), VMEM((tokens, ff), BF16), VMEM((tokens, dim), BF16),
            VMEM((tokens, dim), BF16), VMEM((5 * sub, dim), BF16), VMEM((tokens, dim), BF16),
            VMEM((dt, ff), BF16), VMEM((dt, ff), BF16), VMEM((dt, ff), BF16), VMEM((dt, ff), BF16), VMEM((dt, ff), BF16),
            VMEM((2, max(dt, tile), max(dt, tile)), F32), VMEM((sub, dim), F32), VMEM((dim, width), BF16), VMEM((tokens, width), BF16),
            VMEM((8, dim), F32), VMEM((16, dim), F32), VMEM((4, 16, dt), F32), VMEM((4, 16, dt), F32), VMEM((sub, 2048), F32), VMEM((128, 128), BF16),
            pltpu.SemaphoreType.DMA((48,)), pltpu.SemaphoreType.DMA((48,)), pltpu.SemaphoreType.DMA((72,))],
        compiler_params=pltpu.CompilerParams(collective_id=2, has_side_effects=True, vmem_limit_bytes=VMEM_LIMIT),
        cost_estimate=pl.CostEstimate(flops=20 * tokens * dim * ff, bytes_accessed=100000000, transcendentals=0), name="phase_c",
    )(*args)


def solution(mesh):
    def local_step(hidden, positions, g_ffn, w_gate, w_up, w_down, g_attn, w_q, w_kv, grad_h2, grad_q, grad_kv):
        tokens, dt = hidden.shape
        q_heads, head_dim = w_q.shape[1:]
        kv_heads = w_kv.shape[1]
        q_width, kv_width = q_heads * head_dim, kv_heads * head_dim

        lane = np.arange(128)
        inv_freq = ROPE_BASE ** (-(lane % head_dim // 2 * 2).astype(np.float32) / head_dim)
        angles = positions.astype(F32)[:, None] * jnp.asarray(inv_freq, F32)[None, :]
        swap = np.zeros((128, 128), np.float32)
        swap[lane, lane ^ 1] = np.where(lane % 2 == 0, 1.0, -1.0)
        swap = jnp.asarray(swap, BF16)
        w_qkv_own = jnp.concatenate([w_q.reshape(dt, q_width), w_kv.reshape(dt, kv_width)], axis=1)
        gin = jnp.where(jnp.arange(8)[:, None] == 0, g_ffn[None, :], g_attn[None, :]).astype(F32)

        (normed_all, grad_gate, grad_up, u_all, gate_w, up_w, w_qkv, back_all, h_rows, gains, res_all, normed2, grad_res, resid_out, gattn8,
         u_other, e_other, table, wg_two, _, wd_zero, wd_cross) = call_ab(
             hidden, grad_q.reshape(tokens, q_width), grad_kv.reshape(tokens, kv_width), angles, swap, grad_h2, w_gate, w_up, w_down, w_qkv_own, gin)
        (grad_wgate, _, grad_wup, _, grad_wdown, grad_wqkv, _, q_flat, kv_flat, grad_hidden, gain_grads, *_) = call_c(
            q_width, grad_gate, grad_up, gate_w, up_w, normed_all, u_all, u_other, res_all, e_other, normed2, back_all, w_qkv,
            h_rows, grad_res, gains, gattn8, table, swap, wg_two, wd_zero, wd_cross)
        grad_wq = grad_wqkv[:, :q_width].reshape(dt, q_heads, head_dim)
        grad_wkv = grad_wqkv[:, q_width:].reshape(dt, kv_heads, head_dim)
        q_out = q_flat.reshape(tokens, q_heads, head_dim)
        kv_out = kv_flat.reshape(tokens, kv_heads, head_dim)
        grad_gffn = jnp.sum(gain_grads[:8], axis=0)
        grad_gattn = jnp.sum(gain_grads[8:], axis=0)
        return (resid_out, q_out, kv_out, grad_hidden, grad_gffn, grad_gattn, grad_wgate, grad_wup, grad_wdown, grad_wq, grad_wkv)

    row_spec = P(("dp", "ty"), "tx")
    head_spec = P(("dp", "tx"), "ty", None)
    in_specs = (row_spec, P(("dp", "tx")), P("tx"), P("tx", "ty"), P("tx", "ty"), P("ty", "tx"), P("tx"), P("tx", "ty", None), P("tx", "ty", None), row_spec, head_spec, head_spec)
    out_specs = (row_spec, head_spec, head_spec, row_spec, P(("dp", "tx")), P(("dp", "tx")), P(("dp", "tx"), "ty"), P(("dp", "tx"), "ty"), P(("dp", "ty"), "tx"), head_spec, head_spec)
    return jax.shard_map(local_step, mesh=mesh, in_specs=in_specs, out_specs=out_specs, check_vma=False)
```

```python
import functools

import jax
import jax.numpy as jnp
import numpy as np
from jax import lax
from jax.experimental import pallas as pl
from jax.experimental.pallas import tpu as pltpu
from jax.sharding import PartitionSpec as P

NORM_EPS = 1e-5
ROPE_BASE = 10000.0
F32 = jnp.float32
BF16 = jnp.bfloat16


def dot(a, b, dims=(((1,), (0,)), ((), ()))):
    return lax.dot_general(a, b, dims, preferred_element_type=F32)


MESH = pl.DeviceIdType.MESH
ANY = pl.BlockSpec(memory_space=pl.ANY)
VMEM = pltpu.VMEM
NT_DIMS = (((1,), (1,)), ((), ()))
VMEM_LIMIT = 67000000


def ds(start, size, align=None):
    if isinstance(start, int):
        return pl.ds(start, size)
    return pl.ds(pl.multiple_of(start, align or size), size)


def mid(z):
    return jnp.logical_and(z > 0, z < 3)


def end(z):
    return jnp.logical_or(z == 0, z == 3)


def slots(z):
    return (z + 1 - 2 * (z % 2), 2 - z // 2, 3 - 3 * (z // 2))


def turn(src, dst, rows, width, q_width, table_ref, swap_ref, back):
    step = rows // 4

    @pl.loop(0, 4)
    def _(r):
        for c in range(width // 128):
            cols = pl.ds(c * 128, 128)
            table = ds(r * 128 + (0 if c * 128 < q_width else 512), 128)
            x = src[ds(r * step, step), cols]
            main = x.astype(F32) * table_ref[:, table]
            side = dot(x, swap_ref[...]) * table_ref[:, ds(r * 128 + (1024 if c * 128 < q_width else 1536), 128)]
            dst[ds(r * step, step), cols] = (main - side if back else main + side).astype(BF16)


def pick(i, z):
    s1, s2, s3 = slots(z)
    first, last = (3 - i) // 3, (i // 2) * (i % 2)
    return z * first + s1 * ((i % 2) * (1 - i // 2)) + s2 * ((i // 2) * (1 - i % 2)) + s3 * last


class Wires:
    def __init__(self, send, recv, local):
        self.send, self.recv, self.local = send, recv, local
        self.n_remote = 0
        self.n_local = 0

    def take(self, n=1):
        base = self.n_remote
        self.n_remote += n
        assert self.n_remote <= self.send.shape[0]
        return base

    def copy(self, src, dst, si, ri, **dev):
        return pltpu.make_async_remote_copy(
            src_ref=src, dst_ref=dst, send_sem=self.send.at[si], recv_sem=self.recv.at[ri],
            device_id=dev, device_id_type=MESH)

    def here(self, src, dst):
        i = self.n_local
        self.n_local += 1
        assert i < self.local.shape[0]
        c = pltpu.make_async_copy(src, dst, self.local.at[i])
        c.start()
        return c


def entry_barrier(axes, z):
    sem = pltpu.get_barrier_semaphore()
    for dev in axes:
        pl.semaphore_signal(sem, inc=1, device_id=dev, device_id_type=MESH)

    @pl.when(z > 0)
    def _():
        pl.semaphore_signal(sem, inc=1, device_id={"ty": z - 1}, device_id_type=MESH)

    @pl.when(z < 3)
    def _():
        pl.semaphore_signal(sem, inc=1, device_id={"ty": z + 1}, device_id_type=MESH)

    @pl.when(mid(z))
    def _():
        pl.semaphore_wait(sem, len(axes) + 2)

    @pl.when(end(z))
    def _():
        pl.semaphore_wait(sem, len(axes) + 1)


class LineGather:
    def __init__(self, net, buf, rows, z, off=0, part=None):
        self.net, self.buf, self.rows, self.z, self.off, self.part = net, buf, rows, z, off, part or rows
        self.base = net.take(8)
        self.slots = slots(z)

    def blk(self, b):
        return self.buf.at[ds(b * self.rows + self.off, self.part), :]

    def cp(self, b, side, target):
        return self.net.copy(self.blk(b), self.blk(b), self.base + side * 4 + b, self.base + b, ty=target)

    def start(self):
        z = self.z

        @pl.when(z < 3)
        def _():
            self.cp(z, 0, z + 1).start()

        @pl.when(z > 0)
        def _():
            self.cp(z, 1, z - 1).start()

    def take(self, i):
        b = self.slots[i]
        self.cp(b, 0, self.z).wait_recv()

    def forward(self, i):
        z, b = self.z, self.slots[i]
        target = 3 - z if i == 0 else 3 * (z - 1)
        self.cp(b, 0, target).start()

    def step1(self):
        self.take(0)

        @pl.when(mid(self.z))
        def _():
            self.forward(0)
            self.take(1)
            self.forward(1)

    def near_end(self):
        @pl.when(end(self.z))
        def _():
            self.take(0)

    def near_mid(self):
        @pl.when(mid(self.z))
        def _():
            self.take(1)
            self.forward(1)

    def far_mid(self):
        @pl.when(mid(self.z))
        def _():
            self.take(0)
            self.forward(0)

    def step2(self):
        @pl.when(end(self.z))
        def _():
            self.take(1)

    def step3_mid(self):
        @pl.when(mid(self.z))
        def _():
            self.take(2)
            self.forward(2)

    def step3_end(self):
        @pl.when(end(self.z))
        def _():
            self.take(2)

    def drain(self):
        z = self.z

        @pl.when(z < 3)
        def _():
            self.cp(z, 0, z + 1).wait_send()

        @pl.when(z > 0)
        def _():
            self.cp(z, 1, z - 1).wait_send()

        @pl.when(mid(z))
        def _():
            for i in range(3):
                self.cp(self.slots[i], 0, 3 - z if i == 0 else 3 * (z - 1)).wait_send()


class LineScatter:
    def __init__(self, net, part, rbuf, rows, z, off=0, size=None):
        self.net, self.part, self.rbuf, self.rows, self.z, self.off, self.size = net, part, rbuf, rows, z, off, size or rows
        self.base = net.take(5)
        self.slots = slots(z)
        one = (z % 2) * (1 - z // 2)
        self.dst = (self.slots[0] + (1 - z % 2) * (3 - z), self.slots[1] + 2 * one, self.slots[2])
        self.target = (z + 1 - 2 * (z % 2), 1 + z % 2, 1 + z % 2)

    def cp(self, i):
        return self.net.copy(
            self.part.at[self.view(self.slots[i]), :], self.rbuf.at[self.view(self.dst[i]), :],
            self.base + i, self.base + self.dst[i], ty=self.target[i])

    def view(self, b):
        return ds(b * self.rows + self.off, self.size)

    def wait_slot(self, s):
        view = self.rbuf.at[self.view(s), :]
        self.net.copy(view, view, self.base, self.base + s, ty=self.z).wait_recv()

    def send_end(self, i):
        @pl.when(end(self.z))
        def _():
            self.cp(i).start()

    def send_mid(self, i):
        @pl.when(mid(self.z))
        def _():
            b = self.slots[i]
            self.wait_slot(b)
            step = 16

            @pl.loop(0, self.size // step)
            def _(r):
                view = ds(b * self.rows + self.off + r * step, step)
                self.part[view, :] = (self.part[view, :].astype(F32) + self.rbuf[view, :].astype(F32)).astype(BF16)

            self.cp(i).start()

    def finish(self):
        z = self.z

        @pl.when(z < 3)
        def _():
            self.wait_slot(z)

        @pl.when(z > 0)
        def _():
            self.wait_slot(4)

    def drain(self):
        for i in range(3):
            self.cp(i).wait_send()


class WeightGather:
    def __init__(self, net, w, full, pos, by_rows, chunks, direct=0):
        self.net, self.w, self.full, self.by_rows = net, w, full, by_rows
        self.dp, self.t1, self.t2 = pos
        self.half = w.shape[0] // 2
        self.width = w.shape[0] if by_rows else w.shape[1]
        self.chunks, self.direct = chunks, direct
        self.base = net.take(1 + 4 * chunks + direct)

    def area(self, half, ch):
        if self.by_rows:
            n = self.w.shape[1] // self.chunks
            return ds(half * self.half, self.half, 16), self.half, pl.ds(ch * n, n)
        n = self.half // self.chunks
        return ds(half * self.half + ch * n, n, 16), n, pl.ds(0, self.width)

    def src(self, half, ch):
        rows, _, cols = self.area(half, ch)
        return self.w.at[rows, cols]

    def dst(self, k, half, ch):
        if self.by_rows:
            _, _, cols = self.area(half, ch)
            return self.full.at[ds(k * self.width + half * self.half, self.half, 16), cols]
        rows, _, _ = self.area(half, ch)
        return self.full.at[rows, pl.ds(k * self.width, self.width)]

    def whole(self, k):
        if self.by_rows:
            return self.full.at[pl.ds(k * self.width, self.width), :]
        return self.full.at[:, pl.ds(k * self.width, self.width)]

    def near(self, ch):
        i = self.base + 1 + ch
        return self.net.copy(self.src(self.dp, ch), self.dst(2, self.dp, ch), i, i, tx=self.t2)

    def cross(self, ch, half):
        i = self.base + 1 + self.chunks + ch
        return self.net.copy(self.dst(2, half, ch), self.dst(2, half, ch), i, i, dp=1 - self.dp)

    def diag(self, ch, which, half):
        i = self.base + 1 + (2 + which) * self.chunks + ch
        return self.net.copy(self.dst(2, half, ch), self.dst(3, half, ch), i, i, tx=self.t1)

    def mate(self):
        return self.net.copy(self.w, self.whole(1), self.base, self.base, tx=self.t1)

    def straight(self, n, half):
        ch = self.chunks - 1 - n
        i = self.base + 1 + 4 * self.chunks + n
        return self.net.copy(self.src(half, ch), self.dst(2, half, ch), i, i, tx=self.t2)

    def start_y(self):
        for ch in range(self.chunks):
            self.near(ch).start()
        for n in range(self.direct):
            self.straight(n, 1 - self.dp).start()

    def start_local(self):
        self.own = self.net.here(self.w, self.whole(0))
        self.mate().start()

    def y_event(self, ch):
        self.near(ch).wait_recv()
        if ch < self.chunks - self.direct:
            self.cross(ch, self.dp).start()
        self.diag(ch, 0, self.dp).start()

    def x_event(self, ch):
        if ch < self.chunks - self.direct:
            self.cross(ch, 1 - self.dp).wait_recv()
        else:
            self.straight(self.chunks - 1 - ch, 1 - self.dp).wait_recv()
        self.diag(ch, 1, 1 - self.dp).start()

    def finish_local(self):
        self.own.wait()
        self.mate().wait_recv()

    def finish(self, ch):
        self.diag(ch, 0, self.dp).wait_recv()
        self.diag(ch, 1, 1 - self.dp).wait_recv()

    def drain(self):
        self.mate().wait_send()
        for ch in range(self.chunks):
            self.near(ch).wait_send()
            if ch < self.chunks - self.direct:
                self.cross(ch, self.dp).wait_send()
            else:
                self.straight(self.chunks - 1 - ch, 1 - self.dp).wait_send()
            self.diag(ch, 0, self.dp).wait_send()
            self.diag(ch, 1, 1 - self.dp).wait_send()


def places():
    dp, z, tx = lax.axis_index("dp"), lax.axis_index("ty"), lax.axis_index("tx")
    return dp, z, tx, (tx, tx + 1 - 2 * (tx % 2), (tx + 2) % 4, 3 - tx)


ROWS_ROWS = (((0,), (0,)), ((), ()))


class GradReduce:
    def __init__(self, net, peer, tile, tiles, st3, st1, cross, stage, got2, got0, got_y, out, out_tiles):
        self.net, self.peer, self.tile, self.tiles = net, peer, tile, tiles
        self.st3, self.st1, self.cross, self.stage = st3, st1, cross, stage
        self.got2, self.got0, self.got_y, self.out, self.out_tiles = got2, got0, got_y, out, out_tiles
        self.src = None
        self.base = net.take(3)
        self.w = out.shape[1] // tiles

    def cp(self, i):
        src, dst, to = ((self.st3, self.got2, 1), (self.st1, self.got0, 1), (self.src or self.cross, self.got_y, 2))[i]
        return self.net.copy(src, dst, self.base + i, self.base + i, tx=self.peer[to])

    def fill(self, k, ref):
        @pl.loop(0, self.tiles)
        def _(j):
            ref[:, ds(j * self.w, self.w)] = self.tile(k, j).astype(BF16)

    def step3(self):
        self.fill(3, self.st3)
        self.cp(0).start()

    def step1(self):
        self.fill(1, self.st1)
        self.cp(1).start()

    def step2(self, received=False):
        if not received:
            self.cp(0).wait_recv()
        self.net.here(self.got2, self.stage).wait()

        @pl.loop(0, self.tiles)
        def _(j):
            cols = ds(j * self.w, self.w)
            self.cross[:, cols] = (self.tile(2, j) + self.stage[:, cols].astype(F32)).astype(BF16)

    def send(self, src=None):
        self.src = src
        self.cp(2).start()

    def step0(self, far):
        self.cp(1).wait_recv()
        self.cp(2).wait_recv()
        loads = [self.net.here(self.got0, self.stage), self.net.here(self.got_y, far)]
        for c in loads:
            c.wait()
        base = self.net.n_local
        self.net.n_local += 2

        def put(j, slot):
            src = self.out_tiles.at[slot, :, pl.ds(0, self.w)]
            return pltpu.make_async_copy(src, self.out.at[:, ds(j * self.w, self.w)], self.net.local.at[base + slot])

        @pl.loop(0, self.tiles)
        def _(j):
            cols = ds(j * self.w, self.w)
            slot = j % 2

            @pl.when(j >= 2)
            def _():
                put(j, slot).wait()

            self.out_tiles[slot, :, pl.ds(0, self.w)] = self.tile(0, j) + (self.stage[:, cols].astype(F32) + far[:, cols].astype(F32))
            put(j, slot).start()

        for slot in range(min(2, self.tiles)):
            put(slot, slot).wait()

    def sent_locally(self):
        self.cp(0).wait_send()
        self.cp(1).wait_send()

    def sent(self):
        self.cp(2).wait_send()


def kernel_ab(q_width, hid, eqh, ekvh, angh, swaph, dh2h, wg, wu, wd, wq, gin,
              n_o, da_o, db_o, u_o, wg_o, wu_o, wq_o, eq_o, h_o, g_o, e_o, n2_o, dres_o, home_o, dg_o, ux_o, ex_o, tab_o, g2_o, d2_o, d0_o, dc_o,
              rows, dh2_v, n2_v, res_v, dres_v, n_v, a_v, b_v, wg_v, wu_v, wd_v, wq_v, eq_v, p_v, rbuf, rbuf2, gains, dg_v, swap_v, send, recv, local):
    dp, z, tx, peer = places()
    sub, dim = rows.shape
    tokens = 4 * sub
    width = eq_v.shape[1]
    dt = dim // 4
    ff = wg.shape[1]
    wide = min(1024, ff)
    tile = min(512, ff)
    dwide = min(1024, dim)
    dtile = min(512, dim)
    hs, cs = sub // 2, sub // 4
    net = Wires(send, recv, local)
    turn_in = [net.here(eqh, p_v.at[:, pl.ds(0, q_width)]), net.here(ekvh, p_v.at[:, pl.ds(q_width, width - q_width)]), net.here(swaph, swap_v)]
    turn_in += [net.here(angh.at[pl.ds(i * sub, sub), :], dres_v.at[:, pl.ds(i * 128, 128)]) for i in range(4)]
    entry_barrier([{"tx": peer[1]}, {"tx": peer[2]}, {"tx": peer[3]}, {"dp": 1 - dp}], z)

    pos = (dp, peer[1], peer[2])
    far_first = (2, 3, 1)
    g_id, h_id, e_id, d_id, o_id, u_id, x_id = (net.take(4), net.take(4), net.take(4), net.take(4), net.take(4), net.take(12), net.take(24))
    u_v = wg_v.at[pl.ds(0, tokens), :]
    e_v = wg_v.at[pl.ds(tokens, tokens), :]

    def g_cp(k):
        return net.copy(gin, gains.at[:, pl.ds(k * dt, dt)], g_id + k, g_id + k, tx=peer[k])

    def h_cp(k):
        return net.copy(hid.at[ds(peer[k] * sub, sub), :], rows.at[:, pl.ds(k * dt, dt)], h_id + k, h_id + k, tx=peer[k])

    def e_cp(k, block):
        return net.copy(p_v.at[ds(peer[k] * sub, sub), pl.ds(0, width)], eq_v.at[ds(block * sub, sub), :], e_id + k, e_id + k, tx=peer[k])

    def d_cp(k):
        return net.copy(dh2h.at[ds(peer[k] * sub, sub), :], dh2_v.at[:, pl.ds(k * dt, dt)], d_id + k, d_id + k, tx=peer[k])

    def o_cp(k, block):
        return net.copy(res_v.at[:, pl.ds(k * dt, dt)], home_o.at[ds(block * sub, sub), :], o_id + k, o_id + k, tx=peer[k])

    def ux_cp(k, b):
        view = ds(b * sub, sub)
        cols = pl.ds(0, ff - ff // 4)
        src = ux_o.at[1, view, :] if k == 3 else wg_v.at[view, cols]
        i = u_id + (k - 1) * 4 + b
        return net.copy(src, ux_o.at[k - 1, view, :], i, i, tx=peer[1] if k == 3 else peer[k])

    def ex_cp(k, b, half):
        i = x_id + half * 12 + (k - 1) * 4 + b
        view = ds(b * sub + half * hs, hs)
        return net.copy(wg_v.at[ds(tokens + b * sub + half * hs, hs), pl.ds(k * dt, dt)], ex_o.at[k - 1, view, :], i, i, tx=peer[k])

    gate = WeightGather(net, wg, wg_v, pos, True, 2)
    up = WeightGather(net, wu, wu_v, pos, True, 2)
    down = WeightGather(net, wd, wd_v, pos, False, 4, 1)
    qkv = WeightGather(net, wq, wq_v, pos, True, 1)
    ag = LineGather(net, n_v, sub, z)
    rsc = LineScatter(net, p_v, rbuf, sub, z)
    rs2 = [LineScatter(net, n_v, rbuf2, sub, z, c * cs, cs) for c in range(4)]
    ag2 = [LineGather(net, e_v, sub, z, c * cs, cs) for c in range(4)]

    for k in far_first:
        g_cp(k).start()
    for k in far_first:
        h_cp(k).start()
    g_own = net.here(gin, gains.at[:, pl.ds(0, dt)])
    h_own = net.here(hid.at[ds(tx * sub, sub), :], rows.at[:, pl.ds(0, dt)])
    for w in (qkv, gate, up, down):
        w.start_local()
    for c in turn_in:
        c.wait()

    @pl.loop(0, 4)
    def _(i):
        cos_q, cos_kv, sin_q, sin_kv = (ds(i * 128 + n * 512, 128) for n in range(4))
        angles = dres_v[:, cos_q]
        dres_v[:, sin_q] = jnp.sin(angles)
        dres_v[:, cos_q] = jnp.cos(angles)

        @pl.when(z < 2)
        def _():
            dres_v[:, cos_kv] = dres_v[:, cos_q]
            dres_v[:, sin_kv] = dres_v[:, sin_q]

        @pl.when(z >= 2)
        def _():
            dres_v[:, cos_kv] = jnp.ones((sub, 128), F32)
            dres_v[:, sin_kv] = jnp.zeros((sub, 128), F32)

    tab_out = net.here(dres_v.at[:, pl.ds(0, 2048)], tab_o)
    turn(p_v, p_v, tokens, width, q_width, dres_v, swap_v, True)
    for k in far_first:
        e_cp(k, tx).start()
    e_own = net.here(p_v.at[ds(tx * sub, sub), pl.ds(0, width)], eq_v.at[ds(tx * sub, sub), :])
    for w in (qkv, gate, up, down):
        w.start_y()
    for k in far_first:
        d_cp(k).start()
    d_own = net.here(dh2h.at[ds(tx * sub, sub), :], dh2_v.at[:, pl.ds(0, dt)])

    for k in far_first:
        g_cp(k).wait_recv()
        h_cp(k).wait_recv()
    g_own.wait()
    h_own.wait()

    @pl.loop(0, sub // 16)
    def _(r):
        x = rows[ds(r * 16, 16), :].astype(F32)
        inv = lax.rsqrt(jnp.sum(x * x, axis=1, keepdims=True) / dim + NORM_EPS)
        n_v[ds(z * sub + r * 16, 16), :] = (x * inv * gains[0:1, :]).astype(BF16)

    ag.start()
    outs = [net.here(rows, h_o), net.here(gains, g_o)]
    for k in far_first:
        e_cp(k, peer[k]).wait_recv()
    e_own.wait()
    ag.step1()
    qkv.y_event(0)
    qkv.x_event(0)
    qkv.finish_local()
    qkv.finish(0)
    for k in far_first:
        e_cp(k, tx).wait_send()

    def n2_block(b):
        @pl.loop(0, dim // dtile)
        def _(j):
            w = wq_v[ds(j * dtile, dtile), :]
            p_v[ds(b * sub, sub), ds(j * dtile, dtile)] = dot(eq_v[ds(b * sub, sub), :], w, NT_DIMS).astype(BF16)

    @pl.loop(0, 4)
    def _(i):
        n2_block(pick(3 - i, z))
        for step in range(3):
            pl.when(i == step)(lambda step=step: rsc.send_end(2 - step))
        pl.when(i == 0)(lambda: gate.y_event(0))

    wide = ff // 2

    def gate_part(b, c):
        cols = pl.ds(c * wide, wide)
        a_v[ds(b * sub, sub), cols] = dot(n_v[ds(b * sub, sub), :], wg_v[:, cols]).astype(BF16)

    def up_part(b, c):
        cols = pl.ds(c * wide, wide)
        bb = dot(n_v[ds(b * sub, sub), :], wu_v[:, cols]).astype(BF16)
        b_v[ds(b * sub, sub), cols] = bb
        aa = a_v[ds(b * sub, sub), cols].astype(F32)
        wg_v[ds(b * sub, sub), cols] = (aa * jax.nn.sigmoid(aa) * bb.astype(F32)).astype(BF16)

    def down_part(b, j):
        cols = pl.ds(j * (dim // 2), dim // 2)
        n_v[ds(b * sub, sub), cols] = dot(wg_v[ds(b * sub, sub), :], wd_v[:, cols]).astype(BF16)

    outs += [net.here(wq_v, wq_o), net.here(eq_v, eq_o)]
    gate.finish_local()
    gate.y_event(1)
    ag.step2()
    ag.step3_mid()
    gate.x_event(0)
    gate.finish(0)

    @pl.loop(0, 3)
    def _(i):
        gate_part(pick(i, z), 0)

    up.y_event(0)
    gate.x_event(1)
    rsc.send_mid(2)
    gate.finish(1)
    wg_out = net.here(wg_v, wg_o)

    @pl.loop(0, 3)
    def _(i):
        gate_part(pick(i, z), 1)

    up.finish_local()
    up.y_event(1)
    up.x_event(0)
    up.finish(0)
    ag.step3_end()

    @pl.loop(0, 2)
    def _(c):
        cols = ds(c * wide, wide)
        b = pick(3, z)
        a_v[ds(b * sub, sub), cols] = dot(n_v[ds(b * sub, sub), :], wg_v[:, cols]).astype(BF16)

    wg_out.wait()
    n_out = net.here(n_v, n_o)

    @pl.loop(0, 4)
    def _(i):
        pl.when(i == 1)(lambda: down.y_event(0))
        pl.when(i == 2)(lambda: down.y_event(1))
        pl.when(i == 3)(lambda: up.x_event(1))
        up_part(pick(i, z), 0)

    def up_events_1():
        rsc.send_mid(1)
        rsc.send_mid(0)
        down.x_event(0)

    def up_events_2():
        down.y_event(2)

    def up_events_3():
        down.y_event(3)
        down.x_event(1)

    up.finish(1)
    outs.append(net.here(wu_v, wu_o))

    @pl.loop(0, 4)
    def _(i):
        pl.when(i == 1)(up_events_1)
        pl.when(i == 2)(up_events_2)
        pl.when(i == 3)(up_events_3)
        b = pick(i, z)
        up_part(b, 1)
        ux_cp(2, b).start()
        ux_cp(1, b).start()

    outs.append(net.here(u_v, u_o))
    ag.drain()
    gate.drain()
    n_out.wait()
    down.finish_local()

    @pl.loop(0, 4)
    def _(i):
        pl.when(i == 2)(lambda: down.x_event(2))
        pl.when(i == 3)(lambda: down.x_event(3))
        down_part(pick(3 - i, z), 0)

    for ch in range(4):
        down.finish(ch)

    @pl.loop(0, 4)
    def _(i):
        down_part(pick(3 - i, z), 1)
        for step in range(3):
            pl.when(i == step)(lambda step=step: rs2[0].send_end(2 - step))

    for c in (1, 2, 3):
        for i in (2, 1, 0):
            rs2[c].send_end(i)
    dg_v[...] = jnp.zeros_like(dg_v)
    step = 16

    def norm_chunk(c):
        @pl.loop(0, cs // step)
        def _(r):
            at = c * cs + r * step
            view, mine, far = ds(at, step), ds(z * sub + at, step), ds(4 * sub + at, step)

            def whole(part, got):
                right = jnp.where(z < 3, got[mine, :].astype(F32), 0.0)
                left = jnp.where(z > 0, got[far, :].astype(F32), 0.0)
                return part[mine, :].astype(F32) + right + left

            resid = (rows[view, :].astype(F32) + whole(n_v, rbuf2)).astype(BF16)
            dy = whole(p_v, rbuf)
            res_v[view, :] = resid
            x = resid.astype(F32)
            inv = lax.rsqrt(jnp.sum(x * x, axis=1, keepdims=True) / dim + NORM_EPS)
            xhat = x * inv
            gain = gains[1:2, :]
            n2_v[view, :] = (xhat * gain).astype(BF16)
            part = dy * xhat
            dg_v[...] += part[:8] + part[8:]
            inner = jnp.sum(part * gain, axis=1, keepdims=True) / dim
            dres = dh2_v[view, :].astype(F32) + inv * (dy * gain) - xhat * (inv * inner)
            dres_v[view, pl.ds(0, dim)] = dres
            wg_v[ds(tokens + z * sub + at, step), :] = dres.astype(BF16)

    def spread(b, half):
        for k in far_first:
            ex_cp(k, b, half).start()

    def back_tile(b, j):
        view, cols = ds(b * sub, sub), ds(j * (ff // 4), ff // 4)
        du = dot(wg_v[ds(tokens + b * sub, sub), :], wd_v[ds(j * (ff // 4), ff // 4), :], NT_DIMS)
        aa = a_v[view, cols].astype(F32)
        bb = b_v[view, cols].astype(F32)
        sig = jax.nn.sigmoid(aa)
        a_v[view, cols] = (du * bb * sig * (1.0 + aa * (1.0 - sig))).astype(BF16)
        b_v[view, cols] = (du * aa * sig).astype(BF16)

    def scatter(i, c):
        return lambda: rs2[c].send_mid(i)

    def gathered(i, c):
        def go():
            ag2[c].take(i)
            pl.when(mid(z))(lambda: ag2[c].forward(i))
            if c % 2 == 1:
                spread(ag.slots[i], c // 2)
        return go

    def run(ops):
        def go():
            for op in ops:
                op()
        return go

    before_mid = (
        (scatter(2, 0), scatter(1, 0), scatter(0, 0)),
        (scatter(2, 1), gathered(1, 0), scatter(1, 1), scatter(0, 1)),
        (scatter(2, 2), scatter(1, 2), gathered(1, 1), scatter(0, 2), scatter(2, 3)),
        (scatter(1, 3), scatter(0, 3), gathered(1, 2), gathered(0, 0)))
    before_end = ((), (gathered(0, 0), gathered(1, 0)), (gathered(0, 1), gathered(1, 1)), (gathered(0, 2),))
    after_mid = {0: (gathered(0, 1),), 1: (gathered(2, 0),), 2: (gathered(0, 2),), 3: (gathered(1, 3),), 5: (gathered(0, 3),), 7: (gathered(2, 1),),
                 10: (gathered(2, 2),), 12: (gathered(2, 3),)}
    after_end = {3: (gathered(1, 2),), 4: (gathered(0, 3),), 7: (gathered(2, 0),), 8: (gathered(1, 3),),
                 12: (gathered(2, 1), gathered(2, 2), gathered(2, 3))}

    for c in range(4):
        pl.when(mid(z))(run(before_mid[c]))
        pl.when(end(z))(run(before_end[c]))
        if c == 0:
            rsc.finish()
            for k in far_first:
                d_cp(k).wait_recv()
            d_own.wait()
            tab_out.wait()
        rs2[c].finish()
        norm_chunk(c)
        ag2[c].start()
        if c % 2 == 1:
            spread(z, c // 2)

    for k in far_first:
        o_cp(k, tx).start()
    outs += [net.here(res_v.at[:, pl.ds(0, dt)], home_o.at[ds(tx * sub, sub), :]), net.here(n2_v, n2_o), net.here(dres_v.at[:, pl.ds(0, dim)], dres_o), net.here(dg_v, dg_o)]
    rsc.drain()
    for c in range(4):
        rs2[c].drain()
    n_in = net.here(n_o, p_v)
    middle = (z + 1) // 2 % 2

    def u_forward():
        for b in range(4):
            ux_cp(2, b).wait_recv()
            ux_cp(3, b).start()

    @pl.loop(0, 16)
    def _(t):
        for at, ops in after_mid.items():
            pl.when(jnp.logical_and(t == at, mid(z)))(run(ops))
        for at, ops in after_end.items():
            pl.when(jnp.logical_and(t == at, end(z)))(run(ops))
        pl.when(t == 8)(u_forward)
        i = t // 4
        inner = (i + 1) // 2 % 2
        back_tile(pick(i + middle * inner * (3 - 2 * i), z), t % 4)

    outs.append(net.here(e_v, e_o))
    outs += [net.here(a_v, da_o), net.here(b_v, db_o)]

    last = pl.ds(ff - ff // 4, ff // 4)

    def down_tile(k, j):
        return dot(wg_v[pl.ds(0, tokens), last], wg_v[pl.ds(tokens, tokens), pl.ds(k * dt, dt)], ROWS_ROWS)

    def gate_tile(k, j):
        return dot(p_v[:, pl.ds(k * dt, dt)], a_v[:, ds(j * (ff // 4), ff // 4)], ROWS_ROWS)

    quarter = [rbuf.at[pl.ds(0, ff // 4), pl.ds(i * dt, dt)] for i in range(4)]
    part_d = GradReduce(net, peer, down_tile, 1, quarter[0], quarter[1], quarter[2], quarter[3], d2_o, d0_o, None, dc_o, None)
    part_g = GradReduce(net, peer, gate_tile, 4, n_v.at[pl.ds(0, dt), :], None, None, None, g2_o, None, None, wg_o, None)
    n_in.wait()
    part_d.step3()
    part_d.step1()
    part_g.step3()
    part_d.step2()
    outs.append(net.here(quarter[2], dc_o))
    for k in far_first:
        o_cp(k, peer[k]).wait_recv()
        for b in range(4):
            ex_cp(k, b, 0).wait_recv()
            ex_cp(k, b, 1).wait_recv()
    for b in range(4):
        ux_cp(1, b).wait_recv()
        ux_cp(3, b).wait_recv()
    for c in outs:
        c.wait()
    for k in far_first:
        g_cp(k).wait_send()
        h_cp(k).wait_send()
        d_cp(k).wait_send()
        o_cp(k, tx).wait_send()
        for b in range(4):
            ux_cp(k, b).wait_send()
            ex_cp(k, b, 0).wait_send()
            ex_cp(k, b, 1).wait_send()
    for w in (qkv, up, down):
        w.drain()
    for c in range(4):
        ag2[c].drain()
    part_d.cp(1).wait_recv()
    part_d.sent_locally()
    part_g.cp(0).wait_recv()
    part_g.cp(0).wait_send()


def call_ab(hid, eqh, ekvh, ang, swap, dh2h, wg, wu, wd, wq, gin):
    tokens, dt = hid.shape
    sub, dim, ff, width, q_width = tokens // 4, dt * 4, wg.shape[1], wq.shape[1], eqh.shape[1]
    s = jax.ShapeDtypeStruct
    tok_ff, tok_d, row = s((tokens, ff), BF16), s((tokens, dim), BF16), s((sub, dim), BF16)
    shapes = (tok_d, tok_ff, tok_ff, tok_ff, s((dim, ff), BF16), s((dim, ff), BF16), s((dim, width), BF16), s((tokens, width), BF16),
              row, s((8, dim), F32), tok_d, row, s((sub, dim), F32), s((tokens, dt), BF16), s((8, dim), F32),
              s((3, tokens, ff - ff // 4), BF16), s((3, tokens, dt), BF16), s((sub, 2048), F32), s((dt, ff), BF16)) + (s((ff // 4, dt), BF16),) * 3
    vrow, vtok, vff = VMEM((sub, dim), BF16), VMEM((tokens, dim), BF16), VMEM((tokens, ff), BF16)
    return pl.pallas_call(
        functools.partial(kernel_ab, q_width), out_shape=shapes, in_specs=[ANY] * 11, out_specs=[ANY] * len(shapes),
        scratch_shapes=[
            vrow, vrow, vrow, vrow, VMEM((sub, max(dim, 2048)), F32), vtok, vff, vff, VMEM((dim, ff), BF16), VMEM((dim, ff), BF16), VMEM((ff, dim), BF16),
            VMEM((dim, width), BF16), VMEM((tokens, width), BF16), vtok, VMEM((5 * sub, dim), BF16), VMEM((5 * sub, dim), BF16),
            VMEM((8, dim), F32), VMEM((8, dim), F32), VMEM((128, 128), BF16),
            pltpu.SemaphoreType.DMA((180,)), pltpu.SemaphoreType.DMA((180,)), pltpu.SemaphoreType.DMA((48,))],
        compiler_params=pltpu.CompilerParams(collective_id=0, has_side_effects=True, vmem_limit_bytes=VMEM_LIMIT),
        cost_estimate=pl.CostEstimate(flops=20 * tokens * dim * ff, bytes_accessed=100000000, transcendentals=0), name="phase_ab",
    )(hid, eqh, ekvh, ang, swap, dh2h, wg, wu, wd, wq, gin)


def kernel_c(q_width, da_h, db_h, wg_h, wu_h, n_h, u_h, ux_h, e_h, ex_h, n2_h, eq_h, wq_h, h_h, dres_h, g_h, dga_h, tabh, swaph, g2, d0, dc,
             wgo, wgy, wuo, wuy, wdo, wqo, wqy, q_o, kv_o, dh_o, dg_o, g0, u2, u0, q2, q0, qx, dy,
             wg_v, wu_v, da_v, db_v, n_v, p_v, rbuf, n2_v, st3, st1, cross_g, cross_u, stage, tiles_v, dres_v, wq_v, eq_v,
             gains, dg_v, dgr, dgz, tab_v, swap_v, send, recv, local):
    dp, z, tx, peer = places()
    tokens, ff = da_v.shape
    sub, dim = dres_v.shape
    dt = dim // 4
    width = eq_v.shape[1]
    tile = ff // 4
    dtile = min(512, dim)
    qt = min(256, tile)
    far_first = (2, 3, 1)
    net = Wires(send, recv, local)
    n2_in = net.here(n2_h, n2_v.at[ds(z * sub, sub), :])
    first = [net.here(n_h, n_v), net.here(da_h, da_v)]
    second = [net.here(db_h, db_v), net.here(wg_h, wg_v), net.here(wu_h, wu_v)]
    third = [net.here(wq_h, wq_v), net.here(eq_h, eq_v), net.here(dres_h, dres_v), net.here(g_h, gains),
             net.here(dga_h, dg_v.at[pl.ds(8, 8), :]), net.here(tabh, tab_v), net.here(swaph, swap_v)]
    sem = pltpu.get_barrier_semaphore()
    zs = tuple((z + i) % 4 for i in range(4))
    for i in (1, 2, 3):
        pl.semaphore_signal(sem, inc=1, device_id={"tx": peer[i]}, device_id_type=MESH)
        pl.semaphore_signal(sem, inc=1, device_id={"ty": zs[i]}, device_id_type=MESH)
    pl.semaphore_wait(sem, 6)
    rsc = LineScatter(net, p_v, rbuf, sub, z)
    ag = LineGather(net, n2_v, sub, z)
    q_id, h_id, t_id, z_id = net.take(4), net.take(4), net.take(4), net.take(4)

    def grad_tile(lhs, rhs, w):
        def go(k, j):
            cols = pl.ds(j * w, w) if isinstance(j, int) else ds(j * w, w)
            return dot(lhs[:, pl.ds(k * dt, dt)], rhs[:, cols], ROWS_ROWS)
        return go

    gate = GradReduce(net, peer, grad_tile(n_v, da_v, tile), ff // tile, st3, st1, cross_g, stage, g2, g0, wgy, wgo, tiles_v)
    up = GradReduce(net, peer, grad_tile(n_v, db_v, tile), ff // tile, st3, st1, cross_u, stage, u2, u0, wuy, wuo, tiles_v)
    d_id = net.take(1)

    def dy_cp():
        return net.copy(dc, dy, d_id, d_id, tx=peer[2])

    dy_cp().start()

    def corner(r, c):
        return da_v.at[pl.ds(r * dt, dt), pl.ds(c * width, width)]

    qkv = GradReduce(net, peer, grad_tile(n2_v, eq_v, qt), width // qt, corner(0, 0), corner(1, 0), corner(0, 1), corner(1, 1),
                     q2, q0, wqy, wqo, tiles_v)

    def dn_block(b):
        rows = ds(b * sub, sub)

        @pl.loop(0, dim // dtile)
        def _(j):
            wr = ds(j * dtile, dtile)
            p_v[rows, wr] = (dot(da_v[rows, :], wg_v[wr, :], NT_DIMS) + dot(db_v[rows, :], wu_v[wr, :], NT_DIMS)).astype(BF16)

    n2_in.wait()
    ag.start()
    for c in first:
        c.wait()
    gate.step2(True)
    gate.send()
    gate.step1()
    for c in second:
        c.wait()

    @pl.loop(0, 4)
    def _(i):
        pl.when(i == 1)(ag.step1)
        dn_block(pick(3 - i, z))
        for step in range(3):
            pl.when(i == step)(lambda step=step: rsc.send_end(2 - step))

    gate.cp(1).wait_send()
    up.step3()
    up.step1()
    up.step2()
    up.send()
    rsc.send_mid(2)
    ag.step2()
    ag.step3_mid()
    up.sent_locally()
    h_in = net.here(h_h, st3.at[pl.ds(0, sub), :])
    gate.step0(st1)
    gate.sent()

    n_tiles = ff // tile
    e_in = [net.here(e_h.at[:, pl.ds(0, dt)], wu_v.at[pl.ds(0, tokens), pl.ds(0, dt)])]
    for k in (1, 2, 3):
        e_in.append(net.here(ex_h.at[k - 1], wu_v.at[pl.ds(0, tokens), pl.ds(k * dt, dt)]))

    def u_place(j, k):
        return wg_v.at[pl.ds((j % 2) * tokens, tokens), pl.ds(k * tile, tile)]

    def u_load(j):
        cols = pl.ds(j * tile, tile)
        if j == n_tiles - 1:
            return [net.here(u_h.at[:, cols], u_place(j, 0)), net.here(d0, stage.at[pl.ds(0, tile), pl.ds(0, dt)]), net.here(dy, stage.at[pl.ds(0, tile), pl.ds(dt, dt)])]
        return [net.here(u_h.at[:, cols] if k == 0 else ux_h.at[k - 1, :, cols], u_place(j, k)) for k in range(4)]

    def down_tile(j, slot, loads):
        for c in loads:
            c.wait()
        acc = None
        if j == n_tiles - 1:
            acc = stage[pl.ds(0, tile), pl.ds(0, dt)].astype(F32) + stage[pl.ds(0, tile), pl.ds(dt, dt)].astype(F32)
        for k in range(1 if j == n_tiles - 1 else 4):
            part = dot(u_place(j, k)[...], wu_v[pl.ds(0, tokens), pl.ds(k * dt, dt)], ROWS_ROWS)
            acc = part if acc is None else acc + part
        tiles_v[slot, pl.ds(0, tile), pl.ds(0, dt)] = acc
        return net.here(tiles_v.at[slot, pl.ds(0, tile), pl.ds(0, dt)], wdo.at[pl.ds(j * tile, tile), :])

    loads = {0: u_load(0), 1: u_load(1)}
    rsc.send_mid(1)
    rsc.send_mid(0)
    for c in e_in:
        c.wait()
    done = [down_tile(0, 0, loads[0]), down_tile(1, 1, loads[1])]
    loads = {2: u_load(2)}
    for c in third:
        c.wait()
    ag.step3_end()

    @pl.loop(0, 4)
    def _(b):
        rows = ds(b * sub, sub)

        @pl.loop(0, width // qt)
        def _(j):
            cols = ds(j * qt, qt)
            wu_v[ds(tokens + b * sub, sub), cols] = dot(n2_v[rows, :], wq_v[:, cols]).astype(BF16)

    def q_cp(k, block):
        return net.copy(wu_v.at[ds(tokens + peer[k] * sub, sub), pl.ds(0, width)], qx.at[ds(block * sub, sub), :], q_id + k, q_id + k, tx=peer[k])

    for k in far_first:
        q_cp(k, tx).start()
    q_own = net.here(wu_v.at[ds(tokens + tx * sub, sub), pl.ds(0, width)], qx.at[ds(tx * sub, sub), :])
    for c in done:
        c.wait()
    qkv.step3()
    qkv.step1()
    dy_cp().wait_recv()
    loads[3] = u_load(3)
    done = [down_tile(2, 0, loads[2]), down_tile(3, 1, loads[3])]
    h_in.wait()
    rsc.finish()
    dg_v[pl.ds(0, 8), :] = jnp.zeros((8, dim), F32)
    step = 16

    @pl.loop(0, sub // step)
    def _(r):
        view, mine, far = ds(r * step, step), ds(z * sub + r * step, step), ds(4 * sub + r * step, step)
        right = jnp.where(z < 3, rbuf[mine, :].astype(F32), 0.0)
        left = jnp.where(z > 0, rbuf[far, :].astype(F32), 0.0)
        dy = p_v[mine, :].astype(F32) + right + left
        x = st3[view, :].astype(F32)
        inv = lax.rsqrt(jnp.sum(x * x, axis=1, keepdims=True) / dim + NORM_EPS)
        xhat = x * inv
        gain = gains[0:1, :]
        part = dy * xhat
        dg_v[pl.ds(0, 8), :] += part[:8] + part[8:]
        inner = jnp.sum(part * gain, axis=1, keepdims=True) / dim
        st1[view, :] = (dres_v[view, :] + inv * (dy * gain) - xhat * (inv * inner)).astype(BF16)

    def h_cp(k, block):
        return net.copy(st1.at[pl.ds(0, sub), pl.ds(k * dt, dt)], dh_o.at[ds(block * sub, sub), :], h_id + k, h_id + k, tx=peer[k])

    def t_cp(k):
        return net.copy(dg_v.at[:, pl.ds(k * dt, dt)], dgr.at[k], t_id + k, t_id + k, tx=peer[k])

    def z_cp(i):
        return net.copy(dgr.at[0], dgz.at[i], z_id + i, z_id + i, ty=zs[i])

    for k in far_first:
        t_cp(k).start()
    for k in far_first:
        h_cp(k, tx).start()
    h_own = net.here(st1.at[pl.ds(0, sub), pl.ds(0, dt)], dh_o.at[ds(tx * sub, sub), :])
    qkv.step2()
    qkv.send()
    up.sent()
    for c in done:
        c.wait()
    up.step0(cross_g)
    for k in far_first:
        q_cp(k, peer[k]).wait_recv()
    q_own.wait()
    turned = wu_v.at[pl.ds(tokens, tokens), pl.ds(width, width)]
    net.here(qx, turned).wait()
    turn(turned, turned, tokens, width, q_width, tab_v, swap_v, False)
    q_out = net.here(wu_v.at[pl.ds(tokens, tokens), pl.ds(width, q_width)], q_o)
    kv_out = net.here(wu_v.at[pl.ds(tokens, tokens), pl.ds(width + q_width, width - q_width)], kv_o)
    for k in far_first:
        t_cp(k).wait_recv()
    dgr[0] = dg_v[:, pl.ds(0, dt)] + dgr[1] + dgr[2] + dgr[3]
    for i in (1, 2, 3):
        z_cp(i).start()
    for i in (1, 2, 3):
        z_cp(i).wait_recv()
    dgz[0] = dgr[0] + dgz[1] + dgz[2] + dgz[3]
    dg_out = net.here(dgz.at[0], dg_o)
    for k in far_first:
        h_cp(k, peer[k]).wait_recv()
    qkv.step0(cross_g.at[:, pl.ds(0, width)])
    for c in (q_out, kv_out, dg_out, h_own):
        c.wait()
    dy_cp().wait_send()
    qkv.sent_locally()
    qkv.sent()
    for k in far_first:
        q_cp(k, tx).wait_send()
        h_cp(k, tx).wait_send()
        t_cp(k).wait_send()
        z_cp(k).wait_send()
    ag.drain()
    rsc.drain()


def call_c(q_width, *args):
    tokens, ff = args[0].shape
    sub, dim = args[9].shape
    dt, width = dim // 4, args[10].shape[1]
    tile = ff // 4
    s = jax.ShapeDtypeStruct
    wf, wb = s((dt, ff), F32), s((dt, ff), BF16)
    qf, qb = s((dt, width), F32), s((dt, width), BF16)
    shapes = (wf, wb, wf, wb, s((ff, dt), F32), qf, qb, s((tokens, q_width), BF16), s((tokens, width - q_width), BF16), s((tokens, dt), BF16), s((16, dt), F32),
              wb, wb, wb, qb, qb, s((tokens, width), BF16), s((tile, dt), BF16))
    return pl.pallas_call(
        functools.partial(kernel_c, q_width), out_shape=shapes, in_specs=[ANY] * len(args), out_specs=[ANY] * len(shapes),
        scratch_shapes=[
            VMEM((dim, ff), BF16), VMEM((dim, ff), BF16), VMEM((tokens, ff), BF16), VMEM((tokens, ff), BF16), VMEM((tokens, dim), BF16),
            VMEM((tokens, dim), BF16), VMEM((5 * sub, dim), BF16), VMEM((tokens, dim), BF16),
            VMEM((dt, ff), BF16), VMEM((dt, ff), BF16), VMEM((dt, ff), BF16), VMEM((dt, ff), BF16), VMEM((dt, ff), BF16),
            VMEM((2, max(dt, tile), max(dt, tile)), F32), VMEM((sub, dim), F32), VMEM((dim, width), BF16), VMEM((tokens, width), BF16),
            VMEM((8, dim), F32), VMEM((16, dim), F32), VMEM((4, 16, dt), F32), VMEM((4, 16, dt), F32), VMEM((sub, 2048), F32), VMEM((128, 128), BF16),
            pltpu.SemaphoreType.DMA((48,)), pltpu.SemaphoreType.DMA((48,)), pltpu.SemaphoreType.DMA((72,))],
        compiler_params=pltpu.CompilerParams(collective_id=2, has_side_effects=True, vmem_limit_bytes=VMEM_LIMIT),
        cost_estimate=pl.CostEstimate(flops=20 * tokens * dim * ff, bytes_accessed=100000000, transcendentals=0), name="phase_c",
    )(*args)


def solution(mesh):
    def local_step(hidden, positions, g_ffn, w_gate, w_up, w_down, g_attn, w_q, w_kv, grad_h2, grad_q, grad_kv):
        tokens, dt = hidden.shape
        q_heads, head_dim = w_q.shape[1:]
        kv_heads = w_kv.shape[1]
        q_width, kv_width = q_heads * head_dim, kv_heads * head_dim

        lane = np.arange(128)
        inv_freq = ROPE_BASE ** (-(lane % head_dim // 2 * 2).astype(np.float32) / head_dim)
        angles = positions.astype(F32)[:, None] * jnp.asarray(inv_freq, F32)[None, :]
        swap = np.zeros((128, 128), np.float32)
        swap[lane, lane ^ 1] = np.where(lane % 2 == 0, 1.0, -1.0)
        swap = jnp.asarray(swap, BF16)
        w_qkv_own = jnp.concatenate([w_q.reshape(dt, q_width), w_kv.reshape(dt, kv_width)], axis=1)
        gin = jnp.where(jnp.arange(8)[:, None] == 0, g_ffn[None, :], g_attn[None, :]).astype(F32)

        (normed_all, grad_gate, grad_up, u_all, gate_w, up_w, w_qkv, back_all, h_rows, gains, res_all, normed2, grad_res, resid_out, gattn8,
         u_other, e_other, table, wg_two, _, wd_zero, wd_cross) = call_ab(
             hidden, grad_q.reshape(tokens, q_width), grad_kv.reshape(tokens, kv_width), angles, swap, grad_h2, w_gate, w_up, w_down, w_qkv_own, gin)
        (grad_wgate, _, grad_wup, _, grad_wdown, grad_wqkv, _, q_flat, kv_flat, grad_hidden, gain_grads, *_) = call_c(
            q_width, grad_gate, grad_up, gate_w, up_w, normed_all, u_all, u_other, res_all, e_other, normed2, back_all, w_qkv,
            h_rows, grad_res, gains, gattn8, table, swap, wg_two, wd_zero, wd_cross)
        grad_wq = grad_wqkv[:, :q_width].reshape(dt, q_heads, head_dim)
        grad_wkv = grad_wqkv[:, q_width:].reshape(dt, kv_heads, head_dim)
        q_out = q_flat.reshape(tokens, q_heads, head_dim)
        kv_out = kv_flat.reshape(tokens, kv_heads, head_dim)
        grad_gffn = jnp.sum(gain_grads[:8], axis=0)
        grad_gattn = jnp.sum(gain_grads[8:], axis=0)
        return (resid_out, q_out, kv_out, grad_hidden, grad_gffn, grad_gattn, grad_wgate, grad_wup, grad_wdown, grad_wq, grad_wkv)

    row_spec = P(("dp", "ty"), "tx")
    head_spec = P(("dp", "tx"), "ty", None)
    in_specs = (row_spec, P(("dp", "tx")), P("tx"), P("tx", "ty"), P("tx", "ty"), P("ty", "tx"), P("tx"), P("tx", "ty", None), P("tx", "ty", None), row_spec, head_spec, head_spec)
    out_specs = (row_spec, head_spec, head_spec, row_spec, P(("dp", "tx")), P(("dp", "tx")), P(("dp", "tx"), "ty"), P(("dp", "tx"), "ty"), P(("dp", "ty"), "tx"), head_spec, head_spec)
    return jax.shard_map(local_step, mesh=mesh, in_specs=in_specs, out_specs=out_specs, check_vma=False)
```

```python
import functools

import jax
import jax.numpy as jnp
import numpy as np
from jax import lax
from jax.experimental import pallas as pl
from jax.experimental.pallas import tpu as pltpu
from jax.sharding import PartitionSpec as P

NORM_EPS = 1e-5
ROPE_BASE = 10000.0
F32 = jnp.float32
BF16 = jnp.bfloat16


def dot(a, b, dims=(((1,), (0,)), ((), ()))):
    return lax.dot_general(a, b, dims, preferred_element_type=F32)


MESH = pl.DeviceIdType.MESH
ANY = pl.BlockSpec(memory_space=pl.ANY)
VMEM = pltpu.VMEM
NT_DIMS = (((1,), (1,)), ((), ()))
VMEM_LIMIT = 67000000


def ds(start, size, align=None):
    if isinstance(start, int):
        return pl.ds(start, size)
    return pl.ds(pl.multiple_of(start, align or size), size)


def mid(z):
    return jnp.logical_and(z > 0, z < 3)


def end(z):
    return jnp.logical_or(z == 0, z == 3)


def slots(z):
    return (z + 1 - 2 * (z % 2), 2 - z // 2, 3 - 3 * (z // 2))


def turn(src, dst, rows, width, q_width, table_ref, swap_ref, back):
    step = rows // 4

    @pl.loop(0, 4)
    def _(r):
        for c in range(width // 128):
            cols = pl.ds(c * 128, 128)
            table = ds(r * 128 + (0 if c * 128 < q_width else 512), 128)
            x = src[ds(r * step, step), cols]
            main = x.astype(F32) * table_ref[:, table]
            side = dot(x, swap_ref[...]) * table_ref[:, ds(r * 128 + (1024 if c * 128 < q_width else 1536), 128)]
            dst[ds(r * step, step), cols] = (main - side if back else main + side).astype(BF16)


def pick(i, z):
    s1, s2, s3 = slots(z)
    first, last = (3 - i) // 3, (i // 2) * (i % 2)
    return z * first + s1 * ((i % 2) * (1 - i // 2)) + s2 * ((i // 2) * (1 - i % 2)) + s3 * last


class Wires:
    def __init__(self, send, recv, local):
        self.send, self.recv, self.local = send, recv, local
        self.n_remote = 0
        self.n_local = 0

    def take(self, n=1):
        base = self.n_remote
        self.n_remote += n
        assert self.n_remote <= self.send.shape[0]
        return base

    def copy(self, src, dst, si, ri, **dev):
        return pltpu.make_async_remote_copy(
            src_ref=src, dst_ref=dst, send_sem=self.send.at[si], recv_sem=self.recv.at[ri],
            device_id=dev, device_id_type=MESH)

    def here(self, src, dst):
        i = self.n_local
        self.n_local += 1
        assert i < self.local.shape[0]
        c = pltpu.make_async_copy(src, dst, self.local.at[i])
        c.start()
        return c


def entry_barrier(axes, z):
    sem = pltpu.get_barrier_semaphore()
    for dev in axes:
        pl.semaphore_signal(sem, inc=1, device_id=dev, device_id_type=MESH)

    @pl.when(z > 0)
    def _():
        pl.semaphore_signal(sem, inc=1, device_id={"ty": z - 1}, device_id_type=MESH)

    @pl.when(z < 3)
    def _():
        pl.semaphore_signal(sem, inc=1, device_id={"ty": z + 1}, device_id_type=MESH)

    @pl.when(mid(z))
    def _():
        pl.semaphore_wait(sem, len(axes) + 2)

    @pl.when(end(z))
    def _():
        pl.semaphore_wait(sem, len(axes) + 1)


class LineGather:
    def __init__(self, net, buf, rows, z, off=0, part=None):
        self.net, self.buf, self.rows, self.z, self.off, self.part = net, buf, rows, z, off, part or rows
        self.base = net.take(8)
        self.slots = slots(z)

    def blk(self, b):
        return self.buf.at[ds(b * self.rows + self.off, self.part), :]

    def cp(self, b, side, target):
        return self.net.copy(self.blk(b), self.blk(b), self.base + side * 4 + b, self.base + b, ty=target)

    def start(self):
        z = self.z

        @pl.when(z < 3)
        def _():
            self.cp(z, 0, z + 1).start()

        @pl.when(z > 0)
        def _():
            self.cp(z, 1, z - 1).start()

    def take(self, i):
        b = self.slots[i]
        self.cp(b, 0, self.z).wait_recv()

    def forward(self, i):
        z, b = self.z, self.slots[i]
        target = 3 - z if i == 0 else 3 * (z - 1)
        self.cp(b, 0, target).start()

    def step1(self):
        self.take(0)

        @pl.when(mid(self.z))
        def _():
            self.forward(0)
            self.take(1)
            self.forward(1)

    def near_end(self):
        @pl.when(end(self.z))
        def _():
            self.take(0)

    def near_mid(self):
        @pl.when(mid(self.z))
        def _():
            self.take(1)
            self.forward(1)

    def far_mid(self):
        @pl.when(mid(self.z))
        def _():
            self.take(0)
            self.forward(0)

    def step2(self):
        @pl.when(end(self.z))
        def _():
            self.take(1)

    def step3_mid(self):
        @pl.when(mid(self.z))
        def _():
            self.take(2)
            self.forward(2)

    def step3_end(self):
        @pl.when(end(self.z))
        def _():
            self.take(2)

    def drain(self):
        z = self.z

        @pl.when(z < 3)
        def _():
            self.cp(z, 0, z + 1).wait_send()

        @pl.when(z > 0)
        def _():
            self.cp(z, 1, z - 1).wait_send()

        @pl.when(mid(z))
        def _():
            for i in range(3):
                self.cp(self.slots[i], 0, 3 - z if i == 0 else 3 * (z - 1)).wait_send()


class LineScatter:
    def __init__(self, net, part, rbuf, rows, z, off=0, size=None):
        self.net, self.part, self.rbuf, self.rows, self.z, self.off, self.size = net, part, rbuf, rows, z, off, size or rows
        self.base = net.take(5)
        self.slots = slots(z)
        one = (z % 2) * (1 - z // 2)
        self.dst = (self.slots[0] + (1 - z % 2) * (3 - z), self.slots[1] + 2 * one, self.slots[2])
        self.target = (z + 1 - 2 * (z % 2), 1 + z % 2, 1 + z % 2)

    def cp(self, i):
        return self.net.copy(
            self.part.at[self.view(self.slots[i]), :], self.rbuf.at[self.view(self.dst[i]), :],
            self.base + i, self.base + self.dst[i], ty=self.target[i])

    def view(self, b):
        return ds(b * self.rows + self.off, self.size)

    def wait_slot(self, s):
        view = self.rbuf.at[self.view(s), :]
        self.net.copy(view, view, self.base, self.base + s, ty=self.z).wait_recv()

    def send_end(self, i):
        @pl.when(end(self.z))
        def _():
            self.cp(i).start()

    def send_mid(self, i):
        @pl.when(mid(self.z))
        def _():
            b = self.slots[i]
            self.wait_slot(b)
            step = 16

            @pl.loop(0, self.size // step)
            def _(r):
                view = ds(b * self.rows + self.off + r * step, step)
                self.part[view, :] = (self.part[view, :].astype(F32) + self.rbuf[view, :].astype(F32)).astype(BF16)

            self.cp(i).start()

    def finish(self):
        z = self.z

        @pl.when(z < 3)
        def _():
            self.wait_slot(z)

        @pl.when(z > 0)
        def _():
            self.wait_slot(4)

    def drain(self):
        for i in range(3):
            self.cp(i).wait_send()


class WeightGather:
    def __init__(self, net, w, full, pos, by_rows, chunks, direct=0):
        self.net, self.w, self.full, self.by_rows = net, w, full, by_rows
        self.dp, self.t1, self.t2 = pos
        self.half = w.shape[0] // 2
        self.width = w.shape[0] if by_rows else w.shape[1]
        self.chunks, self.direct = chunks, direct
        self.base = net.take(1 + 4 * chunks + direct)

    def area(self, half, ch):
        if self.by_rows:
            n = self.w.shape[1] // self.chunks
            return ds(half * self.half, self.half, 16), self.half, pl.ds(ch * n, n)
        n = self.half // self.chunks
        return ds(half * self.half + ch * n, n, 16), n, pl.ds(0, self.width)

    def src(self, half, ch):
        rows, _, cols = self.area(half, ch)
        return self.w.at[rows, cols]

    def dst(self, k, half, ch):
        if self.by_rows:
            _, _, cols = self.area(half, ch)
            return self.full.at[ds(k * self.width + half * self.half, self.half, 16), cols]
        rows, _, _ = self.area(half, ch)
        return self.full.at[rows, pl.ds(k * self.width, self.width)]

    def whole(self, k):
        if self.by_rows:
            return self.full.at[pl.ds(k * self.width, self.width), :]
        return self.full.at[:, pl.ds(k * self.width, self.width)]

    def near(self, ch):
        i = self.base + 1 + ch
        return self.net.copy(self.src(self.dp, ch), self.dst(2, self.dp, ch), i, i, tx=self.t2)

    def cross(self, ch, half):
        i = self.base + 1 + self.chunks + ch
        return self.net.copy(self.dst(2, half, ch), self.dst(2, half, ch), i, i, dp=1 - self.dp)

    def diag(self, ch, which, half):
        i = self.base + 1 + (2 + which) * self.chunks + ch
        return self.net.copy(self.dst(2, half, ch), self.dst(3, half, ch), i, i, tx=self.t1)

    def mate(self):
        return self.net.copy(self.w, self.whole(1), self.base, self.base, tx=self.t1)

    def straight(self, n, half):
        ch = self.chunks - 1 - n
        i = self.base + 1 + 4 * self.chunks + n
        return self.net.copy(self.src(half, ch), self.dst(2, half, ch), i, i, tx=self.t2)

    def start_y(self):
        for ch in range(self.chunks):
            self.near(ch).start()
        for n in range(self.direct):
            self.straight(n, 1 - self.dp).start()

    def start_local(self):
        self.own = self.net.here(self.w, self.whole(0))
        self.mate().start()

    def y_event(self, ch):
        self.near(ch).wait_recv()
        if ch < self.chunks - self.direct:
            self.cross(ch, self.dp).start()
        self.diag(ch, 0, self.dp).start()

    def x_event(self, ch):
        if ch < self.chunks - self.direct:
            self.cross(ch, 1 - self.dp).wait_recv()
        else:
            self.straight(self.chunks - 1 - ch, 1 - self.dp).wait_recv()
        self.diag(ch, 1, 1 - self.dp).start()

    def finish_local(self):
        self.own.wait()
        self.mate().wait_recv()

    def finish(self, ch):
        self.diag(ch, 0, self.dp).wait_recv()
        self.diag(ch, 1, 1 - self.dp).wait_recv()

    def drain(self):
        self.mate().wait_send()
        for ch in range(self.chunks):
            self.near(ch).wait_send()
            if ch < self.chunks - self.direct:
                self.cross(ch, self.dp).wait_send()
            else:
                self.straight(self.chunks - 1 - ch, 1 - self.dp).wait_send()
            self.diag(ch, 0, self.dp).wait_send()
            self.diag(ch, 1, 1 - self.dp).wait_send()


def places():
    dp, z, tx = lax.axis_index("dp"), lax.axis_index("ty"), lax.axis_index("tx")
    return dp, z, tx, (tx, tx + 1 - 2 * (tx % 2), (tx + 2) % 4, 3 - tx)


ROWS_ROWS = (((0,), (0,)), ((), ()))


class GradReduce:
    def __init__(self, net, peer, tile, tiles, st3, st1, cross, stage, got2, got0, got_y, out, out_tiles):
        self.net, self.peer, self.tile, self.tiles = net, peer, tile, tiles
        self.st3, self.st1, self.cross, self.stage = st3, st1, cross, stage
        self.got2, self.got0, self.got_y, self.out, self.out_tiles = got2, got0, got_y, out, out_tiles
        self.src = None
        self.base = net.take(3)
        self.w = out.shape[1] // tiles

    def cp(self, i):
        src, dst, to = ((self.st3, self.got2, 1), (self.st1, self.got0, 1), (self.src or self.cross, self.got_y, 2))[i]
        return self.net.copy(src, dst, self.base + i, self.base + i, tx=self.peer[to])

    def fill(self, k, ref):
        @pl.loop(0, self.tiles)
        def _(j):
            ref[:, ds(j * self.w, self.w)] = self.tile(k, j).astype(BF16)

    def step3(self):
        self.fill(3, self.st3)
        self.cp(0).start()

    def step1(self):
        self.fill(1, self.st1)
        self.cp(1).start()

    def step2(self, received=False):
        if not received:
            self.cp(0).wait_recv()
        self.net.here(self.got2, self.stage).wait()

        @pl.loop(0, self.tiles)
        def _(j):
            cols = ds(j * self.w, self.w)
            self.cross[:, cols] = (self.tile(2, j) + self.stage[:, cols].astype(F32)).astype(BF16)

    def send(self, src=None):
        self.src = src
        self.cp(2).start()

    def step0(self, far):
        self.cp(1).wait_recv()
        self.cp(2).wait_recv()
        loads = [self.net.here(self.got0, self.stage), self.net.here(self.got_y, far)]
        for c in loads:
            c.wait()
        base = self.net.n_local
        self.net.n_local += 2

        def put(j, slot):
            src = self.out_tiles.at[slot, :, pl.ds(0, self.w)]
            return pltpu.make_async_copy(src, self.out.at[:, ds(j * self.w, self.w)], self.net.local.at[base + slot])

        @pl.loop(0, self.tiles)
        def _(j):
            cols = ds(j * self.w, self.w)
            slot = j % 2

            @pl.when(j >= 2)
            def _():
                put(j, slot).wait()

            self.out_tiles[slot, :, pl.ds(0, self.w)] = self.tile(0, j) + (self.stage[:, cols].astype(F32) + far[:, cols].astype(F32))
            put(j, slot).start()

        for slot in range(min(2, self.tiles)):
            put(slot, slot).wait()

    def sent_locally(self):
        self.cp(0).wait_send()
        self.cp(1).wait_send()

    def sent(self):
        self.cp(2).wait_send()


def kernel_ab(q_width, hid, eqh, ekvh, angh, swaph, dh2h, wg, wu, wd, wq, gin,
              n_o, da_o, db_o, u_o, wg_o, wu_o, wq_o, eq_o, h_o, g_o, e_o, n2_o, dres_o, home_o, dg_o, ux_o, ex_o, tab_o, g2_o, d2_o, d0_o, dc_o,
              rows, dh2_v, n2_v, res_v, dres_v, n_v, a_v, b_v, wg_v, wu_v, wd_v, wq_v, eq_v, p_v, rbuf, rbuf2, gains, dg_v, swap_v, send, recv, local):
    dp, z, tx, peer = places()
    sub, dim = rows.shape
    tokens = 4 * sub
    width = eq_v.shape[1]
    dt = dim // 4
    ff = wg.shape[1]
    wide = min(1024, ff)
    tile = min(512, ff)
    dwide = min(1024, dim)
    dtile = min(512, dim)
    hs, cs = sub // 2, sub // 4
    net = Wires(send, recv, local)
    turn_in = [net.here(eqh, p_v.at[:, pl.ds(0, q_width)]), net.here(ekvh, p_v.at[:, pl.ds(q_width, width - q_width)]), net.here(swaph, swap_v)]
    turn_in += [net.here(angh.at[pl.ds(i * sub, sub), :], dres_v.at[:, pl.ds(i * 128, 128)]) for i in range(4)]
    entry_barrier([{"tx": peer[1]}, {"tx": peer[2]}, {"tx": peer[3]}, {"dp": 1 - dp}], z)

    pos = (dp, peer[1], peer[2])
    far_first = (2, 3, 1)
    g_id, h_id, e_id, d_id, o_id, u_id, x_id = (net.take(4), net.take(4), net.take(4), net.take(4), net.take(4), net.take(12), net.take(24))
    u_v = wg_v.at[pl.ds(0, tokens), :]
    e_v = wg_v.at[pl.ds(tokens, tokens), :]

    def g_cp(k):
        return net.copy(gin, gains.at[:, pl.ds(k * dt, dt)], g_id + k, g_id + k, tx=peer[k])

    def h_cp(k):
        return net.copy(hid.at[ds(peer[k] * sub, sub), :], rows.at[:, pl.ds(k * dt, dt)], h_id + k, h_id + k, tx=peer[k])

    def e_cp(k, block):
        return net.copy(p_v.at[ds(peer[k] * sub, sub), pl.ds(0, width)], eq_v.at[ds(block * sub, sub), :], e_id + k, e_id + k, tx=peer[k])

    def d_cp(k):
        return net.copy(dh2h.at[ds(peer[k] * sub, sub), :], dh2_v.at[:, pl.ds(k * dt, dt)], d_id + k, d_id + k, tx=peer[k])

    def o_cp(k, block):
        return net.copy(res_v.at[:, pl.ds(k * dt, dt)], home_o.at[ds(block * sub, sub), :], o_id + k, o_id + k, tx=peer[k])

    def ux_cp(k, b):
        view = ds(b * sub, sub)
        cols = pl.ds(0, ff - ff // 4)
        src = ux_o.at[1, view, :] if k == 3 else wg_v.at[view, cols]
        i = u_id + (k - 1) * 4 + b
        return net.copy(src, ux_o.at[k - 1, view, :], i, i, tx=peer[1] if k == 3 else peer[k])

    def ex_cp(k, b, half):
        i = x_id + half * 12 + (k - 1) * 4 + b
        view = ds(b * sub + half * hs, hs)
        return net.copy(wg_v.at[ds(tokens + b * sub + half * hs, hs), pl.ds(k * dt, dt)], ex_o.at[k - 1, view, :], i, i, tx=peer[k])

    gate = WeightGather(net, wg, wg_v, pos, True, 2)
    up = WeightGather(net, wu, wu_v, pos, True, 2)
    down = WeightGather(net, wd, wd_v, pos, False, 4, 1)
    qkv = WeightGather(net, wq, wq_v, pos, True, 1)
    ag = LineGather(net, n_v, sub, z)
    rsc = LineScatter(net, p_v, rbuf, sub, z)
    rs2 = [LineScatter(net, n_v, rbuf2, sub, z, c * cs, cs) for c in range(4)]
    ag2 = [LineGather(net, e_v, sub, z, c * cs, cs) for c in range(4)]

    for k in far_first:
        g_cp(k).start()
    for k in far_first:
        h_cp(k).start()
    g_own = net.here(gin, gains.at[:, pl.ds(0, dt)])
    h_own = net.here(hid.at[ds(tx * sub, sub), :], rows.at[:, pl.ds(0, dt)])
    for w in (qkv, gate, up, down):
        w.start_local()
    for c in turn_in:
        c.wait()

    @pl.loop(0, 4)
    def _(i):
        cos_q, cos_kv, sin_q, sin_kv = (ds(i * 128 + n * 512, 128) for n in range(4))
        angles = dres_v[:, cos_q]
        dres_v[:, sin_q] = jnp.sin(angles)
        dres_v[:, cos_q] = jnp.cos(angles)

        @pl.when(z < 2)
        def _():
            dres_v[:, cos_kv] = dres_v[:, cos_q]
            dres_v[:, sin_kv] = dres_v[:, sin_q]

        @pl.when(z >= 2)
        def _():
            dres_v[:, cos_kv] = jnp.ones((sub, 128), F32)
            dres_v[:, sin_kv] = jnp.zeros((sub, 128), F32)

    tab_out = net.here(dres_v.at[:, pl.ds(0, 2048)], tab_o)
    turn(p_v, p_v, tokens, width, q_width, dres_v, swap_v, True)
    for k in far_first:
        e_cp(k, tx).start()
    e_own = net.here(p_v.at[ds(tx * sub, sub), pl.ds(0, width)], eq_v.at[ds(tx * sub, sub), :])
    for w in (qkv, gate, up, down):
        w.start_y()
    for k in far_first:
        d_cp(k).start()
    d_own = net.here(dh2h.at[ds(tx * sub, sub), :], dh2_v.at[:, pl.ds(0, dt)])

    for k in far_first:
        g_cp(k).wait_recv()
        h_cp(k).wait_recv()
    g_own.wait()
    h_own.wait()

    @pl.loop(0, sub // 16)
    def _(r):
        x = rows[ds(r * 16, 16), :].astype(F32)
        inv = lax.rsqrt(jnp.sum(x * x, axis=1, keepdims=True) / dim + NORM_EPS)
        n_v[ds(z * sub + r * 16, 16), :] = (x * inv * gains[0:1, :]).astype(BF16)

    ag.start()
    outs = [net.here(rows, h_o), net.here(gains, g_o)]
    for k in far_first:
        e_cp(k, peer[k]).wait_recv()
    e_own.wait()
    ag.step1()
    qkv.y_event(0)
    qkv.x_event(0)
    qkv.finish_local()
    qkv.finish(0)
    for k in far_first:
        e_cp(k, tx).wait_send()

    def n2_block(b):
        @pl.loop(0, dim // dtile)
        def _(j):
            w = wq_v[ds(j * dtile, dtile), :]
            p_v[ds(b * sub, sub), ds(j * dtile, dtile)] = dot(eq_v[ds(b * sub, sub), :], w, NT_DIMS).astype(BF16)

    @pl.loop(0, 4)
    def _(i):
        n2_block(pick(3 - i, z))
        for step in range(3):
            pl.when(i == step)(lambda step=step: rsc.send_end(2 - step))
        pl.when(i == 0)(lambda: gate.y_event(0))

    wide = ff // 2

    def gate_part(b, c):
        cols = pl.ds(c * wide, wide)
        a_v[ds(b * sub, sub), cols] = dot(n_v[ds(b * sub, sub), :], wg_v[:, cols]).astype(BF16)

    def up_part(b, c):
        cols = pl.ds(c * wide, wide)
        bb = dot(n_v[ds(b * sub, sub), :], wu_v[:, cols]).astype(BF16)
        b_v[ds(b * sub, sub), cols] = bb
        aa = a_v[ds(b * sub, sub), cols].astype(F32)
        wg_v[ds(b * sub, sub), cols] = (aa * jax.nn.sigmoid(aa) * bb.astype(F32)).astype(BF16)

    def down_part(b, j):
        cols = pl.ds(j * (dim // 2), dim // 2)
        n_v[ds(b * sub, sub), cols] = dot(wg_v[ds(b * sub, sub), :], wd_v[:, cols]).astype(BF16)

    outs += [net.here(wq_v, wq_o), net.here(eq_v, eq_o)]
    gate.finish_local()
    gate.y_event(1)
    ag.step2()
    ag.step3_mid()
    gate.x_event(0)
    gate.finish(0)

    @pl.loop(0, 3)
    def _(i):
        gate_part(pick(i, z), 0)

    up.y_event(0)
    gate.x_event(1)
    rsc.send_mid(2)
    gate.finish(1)
    wg_out = net.here(wg_v, wg_o)

    @pl.loop(0, 3)
    def _(i):
        gate_part(pick(i, z), 1)

    up.finish_local()
    up.y_event(1)
    up.x_event(0)
    up.finish(0)
    ag.step3_end()

    @pl.loop(0, 2)
    def _(c):
        cols = ds(c * wide, wide)
        b = pick(3, z)
        a_v[ds(b * sub, sub), cols] = dot(n_v[ds(b * sub, sub), :], wg_v[:, cols]).astype(BF16)

    wg_out.wait()
    n_out = net.here(n_v, n_o)

    @pl.loop(0, 4)
    def _(i):
        pl.when(i == 1)(lambda: down.y_event(0))
        pl.when(i == 2)(lambda: down.y_event(1))
        pl.when(i == 3)(lambda: up.x_event(1))
        up_part(pick(i, z), 0)

    def up_events_1():
        rsc.send_mid(1)
        rsc.send_mid(0)
        down.x_event(0)

    def up_events_2():
        down.y_event(2)

    def up_events_3():
        down.y_event(3)
        down.x_event(1)

    up.finish(1)
    outs.append(net.here(wu_v, wu_o))

    @pl.loop(0, 4)
    def _(i):
        pl.when(i == 1)(up_events_1)
        pl.when(i == 2)(up_events_2)
        pl.when(i == 3)(up_events_3)
        b = pick(i, z)
        up_part(b, 1)
        ux_cp(2, b).start()
        ux_cp(1, b).start()

    outs.append(net.here(u_v, u_o))
    ag.drain()
    gate.drain()
    n_out.wait()
    down.finish_local()

    @pl.loop(0, 4)
    def _(i):
        pl.when(i == 2)(lambda: down.x_event(2))
        pl.when(i == 3)(lambda: down.x_event(3))
        down_part(pick(3 - i, z), 0)

    for ch in range(4):
        down.finish(ch)

    @pl.loop(0, 4)
    def _(i):
        down_part(pick(3 - i, z), 1)
        for step in range(3):
            pl.when(i == step)(lambda step=step: rs2[0].send_end(2 - step))

    for c in (1, 2, 3):
        for i in (2, 1, 0):
            rs2[c].send_end(i)
    dg_v[...] = jnp.zeros_like(dg_v)
    step = 16

    def norm_chunk(c):
        @pl.loop(0, cs // step)
        def _(r):
            at = c * cs + r * step
            view, mine, far = ds(at, step), ds(z * sub + at, step), ds(4 * sub + at, step)

            def whole(part, got):
                right = jnp.where(z < 3, got[mine, :].astype(F32), 0.0)
                left = jnp.where(z > 0, got[far, :].astype(F32), 0.0)
                return part[mine, :].astype(F32) + right + left

            resid = (rows[view, :].astype(F32) + whole(n_v, rbuf2)).astype(BF16)
            dy = whole(p_v, rbuf)
            res_v[view, :] = resid
            x = resid.astype(F32)
            inv = lax.rsqrt(jnp.sum(x * x, axis=1, keepdims=True) / dim + NORM_EPS)
            xhat = x * inv
            gain = gains[1:2, :]
            n2_v[view, :] = (xhat * gain).astype(BF16)
            part = dy * xhat
            dg_v[...] += part[:8] + part[8:]
            inner = jnp.sum(part * gain, axis=1, keepdims=True) / dim
            dres = dh2_v[view, :].astype(F32) + inv * (dy * gain) - xhat * (inv * inner)
            dres_v[view, pl.ds(0, dim)] = dres
            wg_v[ds(tokens + z * sub + at, step), :] = dres.astype(BF16)

    def spread(b, half):
        for k in far_first:
            ex_cp(k, b, half).start()

    def back_tile(b, j):
        view, cols = ds(b * sub, sub), ds(j * (ff // 4), ff // 4)
        du = dot(wg_v[ds(tokens + b * sub, sub), :], wd_v[ds(j * (ff // 4), ff // 4), :], NT_DIMS)
        aa = a_v[view, cols].astype(F32)
        bb = b_v[view, cols].astype(F32)
        sig = jax.nn.sigmoid(aa)
        a_v[view, cols] = (du * bb * sig * (1.0 + aa * (1.0 - sig))).astype(BF16)
        b_v[view, cols] = (du * aa * sig).astype(BF16)

    def scatter(i, c):
        return lambda: rs2[c].send_mid(i)

    def gathered(i, c):
        def go():
            ag2[c].take(i)
            pl.when(mid(z))(lambda: ag2[c].forward(i))
            if c % 2 == 1:
                spread(ag.slots[i], c // 2)
        return go

    def run(ops):
        def go():
            for op in ops:
                op()
        return go

    before_mid = (
        (scatter(2, 0), scatter(1, 0), scatter(0, 0)),
        (scatter(2, 1), gathered(1, 0), scatter(1, 1), scatter(0, 1)),
        (scatter(2, 2), scatter(1, 2), gathered(1, 1), scatter(0, 2), scatter(2, 3)),
        (scatter(1, 3), scatter(0, 3), gathered(1, 2), gathered(0, 0)))
    before_end = ((), (gathered(0, 0), gathered(1, 0)), (gathered(0, 1), gathered(1, 1)), (gathered(0, 2),))
    after_mid = {0: (gathered(0, 1),), 1: (gathered(2, 0),), 2: (gathered(0, 2),), 3: (gathered(1, 3),), 5: (gathered(0, 3),), 7: (gathered(2, 1),),
                 10: (gathered(2, 2),), 12: (gathered(2, 3),)}
    after_end = {3: (gathered(1, 2),), 4: (gathered(0, 3),), 7: (gathered(2, 0),), 8: (gathered(1, 3),),
                 12: (gathered(2, 1), gathered(2, 2), gathered(2, 3))}

    for c in range(4):
        pl.when(mid(z))(run(before_mid[c]))
        pl.when(end(z))(run(before_end[c]))
        if c == 0:
            rsc.finish()
            for k in far_first:
                d_cp(k).wait_recv()
            d_own.wait()
            tab_out.wait()
        rs2[c].finish()
        norm_chunk(c)
        ag2[c].start()
        if c % 2 == 1:
            spread(z, c // 2)

    for k in far_first:
        o_cp(k, tx).start()
    outs += [net.here(res_v.at[:, pl.ds(0, dt)], home_o.at[ds(tx * sub, sub), :]), net.here(n2_v, n2_o), net.here(dres_v.at[:, pl.ds(0, dim)], dres_o), net.here(dg_v, dg_o)]
    rsc.drain()
    for c in range(4):
        rs2[c].drain()
    n_in = net.here(n_o, p_v)
    middle = (z + 1) // 2 % 2

    def u_forward():
        for b in range(4):
            ux_cp(2, b).wait_recv()
            ux_cp(3, b).start()

    @pl.loop(0, 16)
    def _(t):
        for at, ops in after_mid.items():
            pl.when(jnp.logical_and(t == at, mid(z)))(run(ops))
        for at, ops in after_end.items():
            pl.when(jnp.logical_and(t == at, end(z)))(run(ops))
        pl.when(t == 8)(u_forward)
        i = t // 4
        inner = (i + 1) // 2 % 2
        back_tile(pick(i + middle * inner * (3 - 2 * i), z), t % 4)

    outs.append(net.here(e_v, e_o))
    outs += [net.here(a_v, da_o), net.here(b_v, db_o)]

    last = pl.ds(ff - ff // 4, ff // 4)

    def down_tile(k, j):
        return dot(wg_v[pl.ds(0, tokens), last], wg_v[pl.ds(tokens, tokens), pl.ds(k * dt, dt)], ROWS_ROWS)

    def gate_tile(k, j):
        return dot(p_v[:, pl.ds(k * dt, dt)], a_v[:, ds(j * (ff // 4), ff // 4)], ROWS_ROWS)

    quarter = [rbuf.at[pl.ds(0, ff // 4), pl.ds(i * dt, dt)] for i in range(4)]
    part_d = GradReduce(net, peer, down_tile, 1, quarter[0], quarter[1], quarter[2], quarter[3], d2_o, d0_o, None, dc_o, None)
    part_g = GradReduce(net, peer, gate_tile, 4, n_v.at[pl.ds(0, dt), :], None, None, None, g2_o, None, None, wg_o, None)
    n_in.wait()
    part_d.step3()
    part_d.step1()
    part_g.step3()
    part_d.step2()
    outs.append(net.here(quarter[2], dc_o))
    for k in far_first:
        o_cp(k, peer[k]).wait_recv()
        for b in range(4):
            ex_cp(k, b, 0).wait_recv()
            ex_cp(k, b, 1).wait_recv()
    for b in range(4):
        ux_cp(1, b).wait_recv()
        ux_cp(3, b).wait_recv()
    for c in outs:
        c.wait()
    for k in far_first:
        g_cp(k).wait_send()
        h_cp(k).wait_send()
        d_cp(k).wait_send()
        o_cp(k, tx).wait_send()
        for b in range(4):
            ux_cp(k, b).wait_send()
            ex_cp(k, b, 0).wait_send()
            ex_cp(k, b, 1).wait_send()
    for w in (qkv, up, down):
        w.drain()
    for c in range(4):
        ag2[c].drain()
    part_d.cp(1).wait_recv()
    part_d.sent_locally()
    part_g.cp(0).wait_recv()
    part_g.cp(0).wait_send()


def call_ab(hid, eqh, ekvh, ang, swap, dh2h, wg, wu, wd, wq, gin):
    tokens, dt = hid.shape
    sub, dim, ff, width, q_width = tokens // 4, dt * 4, wg.shape[1], wq.shape[1], eqh.shape[1]
    s = jax.ShapeDtypeStruct
    tok_ff, tok_d, row = s((tokens, ff), BF16), s((tokens, dim), BF16), s((sub, dim), BF16)
    shapes = (tok_d, tok_ff, tok_ff, tok_ff, s((dim, ff), BF16), s((dim, ff), BF16), s((dim, width), BF16), s((tokens, width), BF16),
              row, s((8, dim), F32), tok_d, row, s((sub, dim), F32), s((tokens, dt), BF16), s((8, dim), F32),
              s((3, tokens, ff - ff // 4), BF16), s((3, tokens, dt), BF16), s((sub, 2048), F32), s((dt, ff), BF16)) + (s((ff // 4, dt), BF16),) * 3
    vrow, vtok, vff = VMEM((sub, dim), BF16), VMEM((tokens, dim), BF16), VMEM((tokens, ff), BF16)
    return pl.pallas_call(
        functools.partial(kernel_ab, q_width), out_shape=shapes, in_specs=[ANY] * 11, out_specs=[ANY] * len(shapes),
        scratch_shapes=[
            vrow, vrow, vrow, vrow, VMEM((sub, max(dim, 2048)), F32), vtok, vff, vff, VMEM((dim, ff), BF16), VMEM((dim, ff), BF16), VMEM((ff, dim), BF16),
            VMEM((dim, width), BF16), VMEM((tokens, width), BF16), vtok, VMEM((5 * sub, dim), BF16), VMEM((5 * sub, dim), BF16),
            VMEM((8, dim), F32), VMEM((8, dim), F32), VMEM((128, 128), BF16),
            pltpu.SemaphoreType.DMA((180,)), pltpu.SemaphoreType.DMA((180,)), pltpu.SemaphoreType.DMA((48,))],
        compiler_params=pltpu.CompilerParams(collective_id=0, has_side_effects=True, vmem_limit_bytes=VMEM_LIMIT),
        cost_estimate=pl.CostEstimate(flops=20 * tokens * dim * ff, bytes_accessed=100000000, transcendentals=0), name="phase_ab",
    )(hid, eqh, ekvh, ang, swap, dh2h, wg, wu, wd, wq, gin)


def kernel_c(q_width, da_h, db_h, wg_h, wu_h, n_h, u_h, ux_h, e_h, ex_h, n2_h, eq_h, wq_h, h_h, dres_h, g_h, dga_h, tabh, swaph, g2, d0, dc,
             wgo, wgy, wuo, wuy, wdo, wqo, wqy, q_o, kv_o, dh_o, dg_o, g0, u2, u0, q2, q0, qx, dy,
             wg_v, wu_v, da_v, db_v, n_v, p_v, rbuf, n2_v, st3, st1, cross_g, cross_u, stage, tiles_v, dres_v, wq_v, eq_v,
             gains, dg_v, dgr, dgz, tab_v, swap_v, send, recv, local):
    dp, z, tx, peer = places()
    tokens, ff = da_v.shape
    sub, dim = dres_v.shape
    dt = dim // 4
    width = eq_v.shape[1]
    tile = ff // 4
    dtile = min(512, dim)
    qt = min(256, tile)
    far_first = (2, 3, 1)
    net = Wires(send, recv, local)
    n2_in = net.here(n2_h, n2_v.at[ds(z * sub, sub), :])
    first = [net.here(n_h, n_v), net.here(da_h, da_v)]
    second = [net.here(db_h, db_v), net.here(wg_h, wg_v), net.here(wu_h, wu_v)]
    third = [net.here(wq_h, wq_v), net.here(eq_h, eq_v), net.here(dres_h, dres_v), net.here(g_h, gains),
             net.here(dga_h, dg_v.at[pl.ds(8, 8), :]), net.here(tabh, tab_v), net.here(swaph, swap_v)]
    sem = pltpu.get_barrier_semaphore()
    zs = tuple((z + i) % 4 for i in range(4))
    for i in (1, 2, 3):
        pl.semaphore_signal(sem, inc=1, device_id={"tx": peer[i]}, device_id_type=MESH)
        pl.semaphore_signal(sem, inc=1, device_id={"ty": zs[i]}, device_id_type=MESH)
    pl.semaphore_wait(sem, 6)
    rsc = LineScatter(net, p_v, rbuf, sub, z)
    ag = LineGather(net, n2_v, sub, z)
    q_id, h_id, t_id, z_id = net.take(4), net.take(4), net.take(4), net.take(4)

    def grad_tile(lhs, rhs, w):
        def go(k, j):
            cols = pl.ds(j * w, w) if isinstance(j, int) else ds(j * w, w)
            return dot(lhs[:, pl.ds(k * dt, dt)], rhs[:, cols], ROWS_ROWS)
        return go

    gate = GradReduce(net, peer, grad_tile(n_v, da_v, tile), ff // tile, st3, st1, cross_g, stage, g2, g0, wgy, wgo, tiles_v)
    up = GradReduce(net, peer, grad_tile(n_v, db_v, tile), ff // tile, st3, st1, cross_u, stage, u2, u0, wuy, wuo, tiles_v)
    d_id = net.take(1)

    def dy_cp():
        return net.copy(dc, dy, d_id, d_id, tx=peer[2])

    dy_cp().start()

    def corner(r, c):
        return da_v.at[pl.ds(r * dt, dt), pl.ds(c * width, width)]

    qkv = GradReduce(net, peer, grad_tile(n2_v, eq_v, qt), width // qt, corner(0, 0), corner(1, 0), corner(0, 1), corner(1, 1),
                     q2, q0, wqy, wqo, tiles_v)

    def dn_block(b):
        rows = ds(b * sub, sub)

        @pl.loop(0, dim // dtile)
        def _(j):
            wr = ds(j * dtile, dtile)
            p_v[rows, wr] = (dot(da_v[rows, :], wg_v[wr, :], NT_DIMS) + dot(db_v[rows, :], wu_v[wr, :], NT_DIMS)).astype(BF16)

    n2_in.wait()
    ag.start()
    for c in first:
        c.wait()
    gate.step2(True)
    gate.send()
    gate.step1()
    for c in second:
        c.wait()

    @pl.loop(0, 4)
    def _(i):
        @pl.when(i == 1)
        def _():
            up.step3()
            gate.cp(1).wait_send()
            up.step1()
            ag.step1()

        dn_block(pick(3 - i, z))
        for step in range(3):
            pl.when(i == step)(lambda step=step: rsc.send_end(2 - step))

    up.step2()
    up.send()
    rsc.send_mid(2)
    ag.step2()
    ag.step3_mid()
    up.sent_locally()
    h_in = net.here(h_h, st3.at[pl.ds(0, sub), :])
    gate.step0(st1)
    gate.sent()

    n_tiles = ff // tile
    e_in = [net.here(e_h.at[:, pl.ds(0, dt)], wu_v.at[pl.ds(0, tokens), pl.ds(0, dt)])]
    for k in (1, 2, 3):
        e_in.append(net.here(ex_h.at[k - 1], wu_v.at[pl.ds(0, tokens), pl.ds(k * dt, dt)]))

    def u_place(j, k):
        return wg_v.at[pl.ds((j % 2) * tokens, tokens), pl.ds(k * tile, tile)]

    def u_load(j):
        cols = pl.ds(j * tile, tile)
        if j == n_tiles - 1:
            return [net.here(u_h.at[:, cols], u_place(j, 0)), net.here(d0, stage.at[pl.ds(0, tile), pl.ds(0, dt)]), net.here(dy, stage.at[pl.ds(0, tile), pl.ds(dt, dt)])]
        return [net.here(u_h.at[:, cols] if k == 0 else ux_h.at[k - 1, :, cols], u_place(j, k)) for k in range(4)]

    def down_tile(j, slot, loads):
        for c in loads:
            c.wait()
        acc = None
        if j == n_tiles - 1:
            acc = stage[pl.ds(0, tile), pl.ds(0, dt)].astype(F32) + stage[pl.ds(0, tile), pl.ds(dt, dt)].astype(F32)
        for k in range(1 if j == n_tiles - 1 else 4):
            part = dot(u_place(j, k)[...], wu_v[pl.ds(0, tokens), pl.ds(k * dt, dt)], ROWS_ROWS)
            acc = part if acc is None else acc + part
        tiles_v[slot, pl.ds(0, tile), pl.ds(0, dt)] = acc
        return net.here(tiles_v.at[slot, pl.ds(0, tile), pl.ds(0, dt)], wdo.at[pl.ds(j * tile, tile), :])

    loads = {0: u_load(0), 1: u_load(1)}
    rsc.send_mid(1)
    rsc.send_mid(0)
    for c in e_in:
        c.wait()
    done = [down_tile(0, 0, loads[0]), down_tile(1, 1, loads[1])]
    loads = {2: u_load(2)}
    for c in third:
        c.wait()
    ag.step3_end()

    @pl.loop(0, 4)
    def _(b):
        rows = ds(b * sub, sub)

        @pl.loop(0, width // qt)
        def _(j):
            cols = ds(j * qt, qt)
            wu_v[ds(tokens + b * sub, sub), cols] = dot(n2_v[rows, :], wq_v[:, cols]).astype(BF16)

    def q_cp(k, block):
        return net.copy(wu_v.at[ds(tokens + peer[k] * sub, sub), pl.ds(0, width)], qx.at[ds(block * sub, sub), :], q_id + k, q_id + k, tx=peer[k])

    for k in far_first:
        q_cp(k, tx).start()
    q_own = net.here(wu_v.at[ds(tokens + tx * sub, sub), pl.ds(0, width)], qx.at[ds(tx * sub, sub), :])
    for c in done:
        c.wait()
    qkv.step3()
    qkv.step1()
    dy_cp().wait_recv()
    loads[3] = u_load(3)
    qkv.step2()
    qkv.send()
    done = [down_tile(2, 0, loads[2]), down_tile(3, 1, loads[3])]
    h_in.wait()
    rsc.finish()
    dg_v[pl.ds(0, 8), :] = jnp.zeros((8, dim), F32)
    step = 16

    @pl.loop(0, sub // step)
    def _(r):
        view, mine, far = ds(r * step, step), ds(z * sub + r * step, step), ds(4 * sub + r * step, step)
        right = jnp.where(z < 3, rbuf[mine, :].astype(F32), 0.0)
        left = jnp.where(z > 0, rbuf[far, :].astype(F32), 0.0)
        dy = p_v[mine, :].astype(F32) + right + left
        x = st3[view, :].astype(F32)
        inv = lax.rsqrt(jnp.sum(x * x, axis=1, keepdims=True) / dim + NORM_EPS)
        xhat = x * inv
        gain = gains[0:1, :]
        part = dy * xhat
        dg_v[pl.ds(0, 8), :] += part[:8] + part[8:]
        inner = jnp.sum(part * gain, axis=1, keepdims=True) / dim
        st1[view, :] = (dres_v[view, :] + inv * (dy * gain) - xhat * (inv * inner)).astype(BF16)

    def h_cp(k, block):
        return net.copy(st1.at[pl.ds(0, sub), pl.ds(k * dt, dt)], dh_o.at[ds(block * sub, sub), :], h_id + k, h_id + k, tx=peer[k])

    def t_cp(k):
        return net.copy(dg_v.at[:, pl.ds(k * dt, dt)], dgr.at[k], t_id + k, t_id + k, tx=peer[k])

    def z_cp(i):
        return net.copy(dgr.at[0], dgz.at[i], z_id + i, z_id + i, ty=zs[i])

    for k in far_first:
        t_cp(k).start()
    for k in far_first:
        h_cp(k, tx).start()
    h_own = net.here(st1.at[pl.ds(0, sub), pl.ds(0, dt)], dh_o.at[ds(tx * sub, sub), :])
    up.sent()
    for c in done:
        c.wait()
    up.step0(cross_g)
    for k in far_first:
        q_cp(k, peer[k]).wait_recv()
    q_own.wait()
    turned = wu_v.at[pl.ds(tokens, tokens), pl.ds(width, width)]
    net.here(qx, turned).wait()
    turn(turned, turned, tokens, width, q_width, tab_v, swap_v, False)
    q_out = net.here(wu_v.at[pl.ds(tokens, tokens), pl.ds(width, q_width)], q_o)
    kv_out = net.here(wu_v.at[pl.ds(tokens, tokens), pl.ds(width + q_width, width - q_width)], kv_o)
    qkv.step0(cross_g.at[:, pl.ds(0, width)])
    for k in far_first:
        t_cp(k).wait_recv()
    dgr[0] = dg_v[:, pl.ds(0, dt)] + dgr[1] + dgr[2] + dgr[3]
    for i in (1, 2, 3):
        z_cp(i).start()
    for i in (1, 2, 3):
        z_cp(i).wait_recv()
    dgz[0] = dgr[0] + dgz[1] + dgz[2] + dgz[3]
    dg_out = net.here(dgz.at[0], dg_o)
    for k in far_first:
        h_cp(k, peer[k]).wait_recv()
    for c in (q_out, kv_out, dg_out, h_own):
        c.wait()
    dy_cp().wait_send()
    qkv.sent_locally()
    qkv.sent()
    for k in far_first:
        q_cp(k, tx).wait_send()
        h_cp(k, tx).wait_send()
        t_cp(k).wait_send()
        z_cp(k).wait_send()
    ag.drain()
    rsc.drain()


def call_c(q_width, *args):
    tokens, ff = args[0].shape
    sub, dim = args[9].shape
    dt, width = dim // 4, args[10].shape[1]
    tile = ff // 4
    s = jax.ShapeDtypeStruct
    wf, wb = s((dt, ff), F32), s((dt, ff), BF16)
    qf, qb = s((dt, width), F32), s((dt, width), BF16)
    shapes = (wf, wb, wf, wb, s((ff, dt), F32), qf, qb, s((tokens, q_width), BF16), s((tokens, width - q_width), BF16), s((tokens, dt), BF16), s((16, dt), F32),
              wb, wb, wb, qb, qb, s((tokens, width), BF16), s((tile, dt), BF16))
    return pl.pallas_call(
        functools.partial(kernel_c, q_width), out_shape=shapes, in_specs=[ANY] * len(args), out_specs=[ANY] * len(shapes),
        scratch_shapes=[
            VMEM((dim, ff), BF16), VMEM((dim, ff), BF16), VMEM((tokens, ff), BF16), VMEM((tokens, ff), BF16), VMEM((tokens, dim), BF16),
            VMEM((tokens, dim), BF16), VMEM((5 * sub, dim), BF16), VMEM((tokens, dim), BF16),
            VMEM((dt, ff), BF16), VMEM((dt, ff), BF16), VMEM((dt, ff), BF16), VMEM((dt, ff), BF16), VMEM((dt, ff), BF16),
            VMEM((2, max(dt, tile), max(dt, tile)), F32), VMEM((sub, dim), F32), VMEM((dim, width), BF16), VMEM((tokens, width), BF16),
            VMEM((8, dim), F32), VMEM((16, dim), F32), VMEM((4, 16, dt), F32), VMEM((4, 16, dt), F32), VMEM((sub, 2048), F32), VMEM((128, 128), BF16),
            pltpu.SemaphoreType.DMA((48,)), pltpu.SemaphoreType.DMA((48,)), pltpu.SemaphoreType.DMA((72,))],
        compiler_params=pltpu.CompilerParams(collective_id=2, has_side_effects=True, vmem_limit_bytes=VMEM_LIMIT),
        cost_estimate=pl.CostEstimate(flops=20 * tokens * dim * ff, bytes_accessed=100000000, transcendentals=0), name="phase_c",
    )(*args)


def solution(mesh):
    def local_step(hidden, positions, g_ffn, w_gate, w_up, w_down, g_attn, w_q, w_kv, grad_h2, grad_q, grad_kv):
        tokens, dt = hidden.shape
        q_heads, head_dim = w_q.shape[1:]
        kv_heads = w_kv.shape[1]
        q_width, kv_width = q_heads * head_dim, kv_heads * head_dim

        lane = np.arange(128)
        inv_freq = ROPE_BASE ** (-(lane % head_dim // 2 * 2).astype(np.float32) / head_dim)
        angles = positions.astype(F32)[:, None] * jnp.asarray(inv_freq, F32)[None, :]
        swap = np.zeros((128, 128), np.float32)
        swap[lane, lane ^ 1] = np.where(lane % 2 == 0, 1.0, -1.0)
        swap = jnp.asarray(swap, BF16)
        w_qkv_own = jnp.concatenate([w_q.reshape(dt, q_width), w_kv.reshape(dt, kv_width)], axis=1)
        gin = jnp.where(jnp.arange(8)[:, None] == 0, g_ffn[None, :], g_attn[None, :]).astype(F32)

        (normed_all, grad_gate, grad_up, u_all, gate_w, up_w, w_qkv, back_all, h_rows, gains, res_all, normed2, grad_res, resid_out, gattn8,
         u_other, e_other, table, wg_two, _, wd_zero, wd_cross) = call_ab(
             hidden, grad_q.reshape(tokens, q_width), grad_kv.reshape(tokens, kv_width), angles, swap, grad_h2, w_gate, w_up, w_down, w_qkv_own, gin)
        (grad_wgate, _, grad_wup, _, grad_wdown, grad_wqkv, _, q_flat, kv_flat, grad_hidden, gain_grads, *_) = call_c(
            q_width, grad_gate, grad_up, gate_w, up_w, normed_all, u_all, u_other, res_all, e_other, normed2, back_all, w_qkv,
            h_rows, grad_res, gains, gattn8, table, swap, wg_two, wd_zero, wd_cross)
        grad_wq = grad_wqkv[:, :q_width].reshape(dt, q_heads, head_dim)
        grad_wkv = grad_wqkv[:, q_width:].reshape(dt, kv_heads, head_dim)
        q_out = q_flat.reshape(tokens, q_heads, head_dim)
        kv_out = kv_flat.reshape(tokens, kv_heads, head_dim)
        grad_gffn = jnp.sum(gain_grads[:8], axis=0)
        grad_gattn = jnp.sum(gain_grads[8:], axis=0)
        return (resid_out, q_out, kv_out, grad_hidden, grad_gffn, grad_gattn, grad_wgate, grad_wup, grad_wdown, grad_wq, grad_wkv)

    row_spec = P(("dp", "ty"), "tx")
    head_spec = P(("dp", "tx"), "ty", None)
    in_specs = (row_spec, P(("dp", "tx")), P("tx"), P("tx", "ty"), P("tx", "ty"), P("ty", "tx"), P("tx"), P("tx", "ty", None), P("tx", "ty", None), row_spec, head_spec, head_spec)
    out_specs = (row_spec, head_spec, head_spec, row_spec, P(("dp", "tx")), P(("dp", "tx")), P(("dp", "tx"), "ty"), P(("dp", "tx"), "ty"), P(("dp", "ty"), "tx"), head_spec, head_spec)
    return jax.shard_map(local_step, mesh=mesh, in_specs=in_specs, out_specs=out_specs, check_vma=False)
```

```python
import functools

import jax
import jax.numpy as jnp
import numpy as np
from jax import lax
from jax.experimental import pallas as pl
from jax.experimental.pallas import tpu as pltpu
from jax.sharding import PartitionSpec as P

NORM_EPS = 1e-5
ROPE_BASE = 10000.0
F32 = jnp.float32
BF16 = jnp.bfloat16


def dot(a, b, dims=(((1,), (0,)), ((), ()))):
    return lax.dot_general(a, b, dims, preferred_element_type=F32)


MESH = pl.DeviceIdType.MESH
ANY = pl.BlockSpec(memory_space=pl.ANY)
VMEM = pltpu.VMEM
NT_DIMS = (((1,), (1,)), ((), ()))
VMEM_LIMIT = 67000000


def ds(start, size, align=None):
    if isinstance(start, int):
        return pl.ds(start, size)
    return pl.ds(pl.multiple_of(start, align or size), size)


def mid(z):
    return jnp.logical_and(z > 0, z < 3)


def end(z):
    return jnp.logical_or(z == 0, z == 3)


def slots(z):
    return (z + 1 - 2 * (z % 2), 2 - z // 2, 3 - 3 * (z // 2))


def turn(x_ref, width, q_width, tokens, table_ref, swap_ref, back):
    step = min(256, tokens)

    @pl.loop(0, tokens // step)
    def _(r):
        cols = ds(r * step, step)
        for g in range(width // 128):
            rows = pl.ds(g * 128, 128)
            base = pl.ds(0 if g * 128 < q_width else 128, 128)
            x = x_ref[rows, cols]
            main = x.astype(F32) * table_ref[base, cols]
            side = dot(swap_ref[...], x) * table_ref[base, ds(tokens + r * step, step)]
            x_ref[rows, cols] = (main - side if back else main + side).astype(BF16)


def pick(i, z):
    s1, s2, s3 = slots(z)
    first, last = (3 - i) // 3, (i // 2) * (i % 2)
    return z * first + s1 * ((i % 2) * (1 - i // 2)) + s2 * ((i // 2) * (1 - i % 2)) + s3 * last


class Wires:
    def __init__(self, send, recv, local):
        self.send, self.recv, self.local = send, recv, local
        self.n_remote = 0
        self.n_local = 0

    def take(self, n=1):
        base = self.n_remote
        self.n_remote += n
        assert self.n_remote <= self.send.shape[0]
        return base

    def copy(self, src, dst, si, ri, **dev):
        return pltpu.make_async_remote_copy(
            src_ref=src, dst_ref=dst, send_sem=self.send.at[si], recv_sem=self.recv.at[ri],
            device_id=dev, device_id_type=MESH)

    def here(self, src, dst):
        i = self.n_local
        self.n_local += 1
        assert i < self.local.shape[0]
        c = pltpu.make_async_copy(src, dst, self.local.at[i])
        c.start()
        return c


def entry_barrier(axes, z):
    sem = pltpu.get_barrier_semaphore()
    for dev in axes:
        pl.semaphore_signal(sem, inc=1, device_id=dev, device_id_type=MESH)

    @pl.when(z > 0)
    def _():
        pl.semaphore_signal(sem, inc=1, device_id={"ty": z - 1}, device_id_type=MESH)

    @pl.when(z < 3)
    def _():
        pl.semaphore_signal(sem, inc=1, device_id={"ty": z + 1}, device_id_type=MESH)

    @pl.when(mid(z))
    def _():
        pl.semaphore_wait(sem, len(axes) + 2)

    @pl.when(end(z))
    def _():
        pl.semaphore_wait(sem, len(axes) + 1)


class LineGather:
    def __init__(self, net, buf, rows, z, off=0, part=None):
        self.net, self.buf, self.rows, self.z, self.off, self.part = net, buf, rows, z, off, part or rows
        self.base = net.take(8)
        self.slots = slots(z)

    def blk(self, b):
        return self.buf.at[ds(b * self.rows + self.off, self.part), :]

    def cp(self, b, side, target):
        return self.net.copy(self.blk(b), self.blk(b), self.base + side * 4 + b, self.base + b, ty=target)

    def start(self):
        z = self.z

        @pl.when(z < 3)
        def _():
            self.cp(z, 0, z + 1).start()

        @pl.when(z > 0)
        def _():
            self.cp(z, 1, z - 1).start()

    def take(self, i):
        b = self.slots[i]
        self.cp(b, 0, self.z).wait_recv()

    def forward(self, i):
        z, b = self.z, self.slots[i]
        target = 3 - z if i == 0 else 3 * (z - 1)
        self.cp(b, 0, target).start()

    def step1(self):
        self.take(0)

        @pl.when(mid(self.z))
        def _():
            self.forward(0)
            self.take(1)
            self.forward(1)

    def near_end(self):
        @pl.when(end(self.z))
        def _():
            self.take(0)

    def near_mid(self):
        @pl.when(mid(self.z))
        def _():
            self.take(1)
            self.forward(1)

    def far_mid(self):
        @pl.when(mid(self.z))
        def _():
            self.take(0)
            self.forward(0)

    def step2(self):
        @pl.when(end(self.z))
        def _():
            self.take(1)

    def step3_mid(self):
        @pl.when(mid(self.z))
        def _():
            self.take(2)
            self.forward(2)

    def step3_end(self):
        @pl.when(end(self.z))
        def _():
            self.take(2)

    def drain(self):
        z = self.z

        @pl.when(z < 3)
        def _():
            self.cp(z, 0, z + 1).wait_send()

        @pl.when(z > 0)
        def _():
            self.cp(z, 1, z - 1).wait_send()

        @pl.when(mid(z))
        def _():
            for i in range(3):
                self.cp(self.slots[i], 0, 3 - z if i == 0 else 3 * (z - 1)).wait_send()


class LineScatter:
    def __init__(self, net, part, rbuf, rows, z, off=0, size=None):
        self.net, self.part, self.rbuf, self.rows, self.z, self.off, self.size = net, part, rbuf, rows, z, off, size or rows
        self.base = net.take(5)
        self.slots = slots(z)
        one = (z % 2) * (1 - z // 2)
        self.dst = (self.slots[0] + (1 - z % 2) * (3 - z), self.slots[1] + 2 * one, self.slots[2])
        self.target = (z + 1 - 2 * (z % 2), 1 + z % 2, 1 + z % 2)

    def cp(self, i):
        return self.net.copy(
            self.part.at[self.view(self.slots[i]), :], self.rbuf.at[self.view(self.dst[i]), :],
            self.base + i, self.base + self.dst[i], ty=self.target[i])

    def view(self, b):
        return ds(b * self.rows + self.off, self.size)

    def wait_slot(self, s):
        view = self.rbuf.at[self.view(s), :]
        self.net.copy(view, view, self.base, self.base + s, ty=self.z).wait_recv()

    def send_end(self, i):
        @pl.when(end(self.z))
        def _():
            self.cp(i).start()

    def send_mid(self, i):
        @pl.when(mid(self.z))
        def _():
            b = self.slots[i]
            self.wait_slot(b)
            step = 16

            @pl.loop(0, self.size // step)
            def _(r):
                view = ds(b * self.rows + self.off + r * step, step)
                self.part[view, :] = (self.part[view, :].astype(F32) + self.rbuf[view, :].astype(F32)).astype(BF16)

            self.cp(i).start()

    def finish(self):
        z = self.z

        @pl.when(z < 3)
        def _():
            self.wait_slot(z)

        @pl.when(z > 0)
        def _():
            self.wait_slot(4)

    def drain(self):
        for i in range(3):
            self.cp(i).wait_send()


class WeightGather:
    def __init__(self, net, w, full, pos, by_rows, chunks, direct=0):
        self.net, self.w, self.full, self.by_rows = net, w, full, by_rows
        self.dp, self.t1, self.t2 = pos
        self.half = w.shape[0] // 2
        self.width = w.shape[0] if by_rows else w.shape[1]
        self.chunks, self.direct = chunks, direct
        self.base = net.take(1 + 4 * chunks + direct)

    def area(self, half, ch):
        if self.by_rows:
            n = self.w.shape[1] // self.chunks
            return ds(half * self.half, self.half, 16), self.half, pl.ds(ch * n, n)
        n = self.half // self.chunks
        return ds(half * self.half + ch * n, n, 16), n, pl.ds(0, self.width)

    def src(self, half, ch):
        rows, _, cols = self.area(half, ch)
        return self.w.at[rows, cols]

    def dst(self, k, half, ch):
        if self.by_rows:
            _, _, cols = self.area(half, ch)
            return self.full.at[ds(k * self.width + half * self.half, self.half, 16), cols]
        rows, _, _ = self.area(half, ch)
        return self.full.at[rows, pl.ds(k * self.width, self.width)]

    def whole(self, k):
        if self.by_rows:
            return self.full.at[pl.ds(k * self.width, self.width), :]
        return self.full.at[:, pl.ds(k * self.width, self.width)]

    def near(self, ch):
        i = self.base + 1 + ch
        return self.net.copy(self.src(self.dp, ch), self.dst(2, self.dp, ch), i, i, tx=self.t2)

    def cross(self, ch, half):
        i = self.base + 1 + self.chunks + ch
        return self.net.copy(self.dst(2, half, ch), self.dst(2, half, ch), i, i, dp=1 - self.dp)

    def diag(self, ch, which, half):
        i = self.base + 1 + (2 + which) * self.chunks + ch
        return self.net.copy(self.dst(2, half, ch), self.dst(3, half, ch), i, i, tx=self.t1)

    def mate(self):
        return self.net.copy(self.w, self.whole(1), self.base, self.base, tx=self.t1)

    def straight(self, n, half):
        ch = self.chunks - 1 - n
        i = self.base + 1 + 4 * self.chunks + n
        return self.net.copy(self.src(half, ch), self.dst(2, half, ch), i, i, tx=self.t2)

    def start_y(self):
        for ch in range(self.chunks):
            self.near(ch).start()
        for n in range(self.direct):
            self.straight(n, 1 - self.dp).start()

    def start_local(self):
        self.own = self.net.here(self.w, self.whole(0))
        self.mate().start()

    def y_event(self, ch):
        self.near(ch).wait_recv()
        if ch < self.chunks - self.direct:
            self.cross(ch, self.dp).start()
        self.diag(ch, 0, self.dp).start()

    def x_event(self, ch):
        if ch < self.chunks - self.direct:
            self.cross(ch, 1 - self.dp).wait_recv()
        else:
            self.straight(self.chunks - 1 - ch, 1 - self.dp).wait_recv()
        self.diag(ch, 1, 1 - self.dp).start()

    def finish_local(self):
        self.own.wait()
        self.mate().wait_recv()

    def finish(self, ch):
        self.diag(ch, 0, self.dp).wait_recv()
        self.diag(ch, 1, 1 - self.dp).wait_recv()

    def drain(self):
        self.mate().wait_send()
        for ch in range(self.chunks):
            self.near(ch).wait_send()
            if ch < self.chunks - self.direct:
                self.cross(ch, self.dp).wait_send()
            else:
                self.straight(self.chunks - 1 - ch, 1 - self.dp).wait_send()
            self.diag(ch, 0, self.dp).wait_send()
            self.diag(ch, 1, 1 - self.dp).wait_send()


def places():
    dp, z, tx = lax.axis_index("dp"), lax.axis_index("ty"), lax.axis_index("tx")
    return dp, z, tx, (tx, tx + 1 - 2 * (tx % 2), (tx + 2) % 4, 3 - tx)


ROWS_ROWS = (((0,), (0,)), ((), ()))


class GradReduce:
    def __init__(self, net, peer, tile, tiles, st3, st1, cross, stage, got2, got0, got_y, out, out_tiles):
        self.net, self.peer, self.tile, self.tiles = net, peer, tile, tiles
        self.st3, self.st1, self.cross, self.stage = st3, st1, cross, stage
        self.got2, self.got0, self.got_y, self.out, self.out_tiles = got2, got0, got_y, out, out_tiles
        self.src = None
        self.base = net.take(3)
        self.rows, self.w = out.shape[0], out.shape[1] // tiles

    def cp(self, i):
        src, dst, to = ((self.st3, self.got2, 1), (self.st1, self.got0, 1), (self.src or self.cross, self.got_y, 2))[i]
        return self.net.copy(src, dst, self.base + i, self.base + i, tx=self.peer[to])

    def fill(self, k, ref):
        @pl.loop(0, self.tiles)
        def _(j):
            ref[:, ds(j * self.w, self.w)] = self.tile(k, j).astype(BF16)

    def step3(self):
        self.fill(3, self.st3)
        self.cp(0).start()

    def step1(self):
        self.fill(1, self.st1)
        self.cp(1).start()

    def step2(self, received=False):
        if not received:
            self.cp(0).wait_recv()
        self.net.here(self.got2, self.stage).wait()

        @pl.loop(0, self.tiles)
        def _(j):
            cols = ds(j * self.w, self.w)
            self.cross[:, cols] = (self.tile(2, j) + self.stage[:, cols].astype(F32)).astype(BF16)

    def send(self, src=None):
        self.src = src
        self.cp(2).start()

    def step0(self, far):
        self.cp(1).wait_recv()
        self.cp(2).wait_recv()
        loads = [self.net.here(self.got0, self.stage), self.net.here(self.got_y, far)]
        for c in loads:
            c.wait()
        base = self.net.n_local
        self.net.n_local += 2

        def put(j, slot):
            src = self.out_tiles.at[slot, pl.ds(0, self.rows), pl.ds(0, self.w)]
            return pltpu.make_async_copy(src, self.out.at[:, ds(j * self.w, self.w)], self.net.local.at[base + slot])

        @pl.loop(0, self.tiles)
        def _(j):
            cols = ds(j * self.w, self.w)
            slot = j % 2

            @pl.when(j >= 2)
            def _():
                put(j, slot).wait()

            self.out_tiles[slot, pl.ds(0, self.rows), pl.ds(0, self.w)] = self.tile(0, j) + (self.stage[:, cols].astype(F32) + far[:, cols].astype(F32))
            put(j, slot).start()

        for slot in range(min(2, self.tiles)):
            put(slot, slot).wait()

    def sent_locally(self):
        self.cp(0).wait_send()
        self.cp(1).wait_send()

    def sent(self):
        self.cp(2).wait_send()


def kernel_ab(q_width, hid, eqh, ekvh, angh, swaph, dh2h, wg, wu, wd, wq, wkv, gin,
              n_o, da_o, db_o, u_o, wg_o, wu_o, wq_o, eq_o, h_o, g_o, e_o, n2_o, dres_o, home_o, dg_o, ux_o, ex_o, tab_o, g2_o, d2_o, d0_o, dc_o,
              rows, dh2_v, n2_v, res_v, dres_v, n_v, a_v, b_v, wg_v, wu_v, wd_v, wq_v, eq_v, p_v, rbuf, rbuf2, gains, dg_v, swap_v, send, recv, local):
    dp, z, tx, peer = places()
    sub, dim = rows.shape
    tokens = 4 * sub
    width = eq_v.shape[0]
    dt = dim // 4
    ff = wg.shape[1]
    wide = min(1024, ff)
    tile = min(512, ff)
    dwide = min(1024, dim)
    dtile = min(512, dim)
    hs, cs = sub // 2, sub // 4
    net = Wires(send, recv, local)
    turn_in = [net.here(eqh, p_v.at[pl.ds(0, q_width), pl.ds(0, tokens)]), net.here(ekvh, p_v.at[pl.ds(q_width, width - q_width), pl.ds(0, tokens)]),
               net.here(swaph, swap_v), net.here(angh, dres_v.at[pl.ds(0, 128), pl.ds(0, tokens)])]
    entry_barrier([{"tx": peer[1]}, {"tx": peer[2]}, {"tx": peer[3]}, {"dp": 1 - dp}], z)

    pos = (dp, peer[1], peer[2])
    far_first = (2, 3, 1)
    g_id, h_id, e_id, d_id, o_id, u_id, x_id = (net.take(4), net.take(4), net.take(4), net.take(4), net.take(4), net.take(12), net.take(24))
    u_v = wg_v.at[pl.ds(0, tokens), :]
    e_v = wg_v.at[pl.ds(tokens, tokens), :]

    def g_cp(k):
        return net.copy(gin, gains.at[:, pl.ds(k * dt, dt)], g_id + k, g_id + k, tx=peer[k])

    def h_cp(k):
        return net.copy(hid.at[ds(peer[k] * sub, sub), :], rows.at[:, pl.ds(k * dt, dt)], h_id + k, h_id + k, tx=peer[k])

    def e_cp(k, block):
        return net.copy(p_v.at[pl.ds(0, width), ds(peer[k] * sub, sub)], eq_v.at[:, ds(block * sub, sub)], e_id + k, e_id + k, tx=peer[k])

    def d_cp(k):
        return net.copy(dh2h.at[ds(peer[k] * sub, sub), :], dh2_v.at[:, pl.ds(k * dt, dt)], d_id + k, d_id + k, tx=peer[k])

    def o_cp(k, block):
        return net.copy(res_v.at[:, pl.ds(k * dt, dt)], home_o.at[ds(block * sub, sub), :], o_id + k, o_id + k, tx=peer[k])

    def ux_cp(k, b):
        view = ds(b * sub, sub)
        cols = pl.ds(0, ff - ff // 4)
        src = ux_o.at[1, view, :] if k == 3 else wg_v.at[view, cols]
        i = u_id + (k - 1) * 4 + b
        return net.copy(src, ux_o.at[k - 1, view, :], i, i, tx=peer[1] if k == 3 else peer[k])

    def ex_cp(k, b, half):
        i = x_id + half * 12 + (k - 1) * 4 + b
        view = ds(b * sub + half * hs, hs)
        return net.copy(wg_v.at[ds(tokens + b * sub + half * hs, hs), pl.ds(k * dt, dt)], ex_o.at[k - 1, view, :], i, i, tx=peer[k])

    gate = WeightGather(net, wg, wg_v, pos, True, 2)
    up = WeightGather(net, wu, wu_v, pos, True, 2)
    down = WeightGather(net, wd, wd_v, pos, False, 4, 1)
    q_w = WeightGather(net, wq, wq_v.at[pl.ds(0, q_width), :], pos, False, 1)
    kv_w = WeightGather(net, wkv, wq_v.at[pl.ds(q_width, width - q_width), :], pos, False, 1)
    ag = LineGather(net, n_v, sub, z)
    rsc = LineScatter(net, p_v, rbuf, sub, z)
    rs2 = [LineScatter(net, n_v, rbuf2, sub, z, c * cs, cs) for c in range(4)]
    ag2 = [LineGather(net, e_v, sub, z, c * cs, cs) for c in range(4)]

    for k in far_first:
        g_cp(k).start()
    for k in far_first:
        h_cp(k).start()
    g_own = net.here(gin, gains.at[:, pl.ds(0, dt)])
    h_own = net.here(hid.at[ds(tx * sub, sub), :], rows.at[:, pl.ds(0, dt)])
    for w in (q_w, kv_w, gate, up, down):
        w.start_local()
    for c in turn_in:
        c.wait()

    @pl.loop(0, 4)
    def _(i):
        part = tokens // 4
        cos_c, sin_c = ds(i * part, part), ds(tokens + i * part, part)
        q_r, kv_r = pl.ds(0, 128), pl.ds(128, 128)
        angles = dres_v[q_r, cos_c]
        dres_v[q_r, sin_c] = jnp.sin(angles)
        dres_v[q_r, cos_c] = jnp.cos(angles)

        @pl.when(z < 2)
        def _():
            dres_v[kv_r, cos_c] = dres_v[q_r, cos_c]
            dres_v[kv_r, sin_c] = dres_v[q_r, sin_c]

        @pl.when(z >= 2)
        def _():
            dres_v[kv_r, cos_c] = jnp.ones((128, part), F32)
            dres_v[kv_r, sin_c] = jnp.zeros((128, part), F32)

    tab_out = net.here(dres_v.at[pl.ds(0, 256), pl.ds(0, 2 * tokens)], tab_o)
    turn(p_v, width, q_width, tokens, dres_v, swap_v, True)
    for k in far_first:
        e_cp(k, tx).start()
    e_own = net.here(p_v.at[pl.ds(0, width), ds(tx * sub, sub)], eq_v.at[:, ds(tx * sub, sub)])
    for w in (q_w, kv_w, gate, up, down):
        w.start_y()
    for k in far_first:
        d_cp(k).start()
    d_own = net.here(dh2h.at[ds(tx * sub, sub), :], dh2_v.at[:, pl.ds(0, dt)])

    for k in far_first:
        g_cp(k).wait_recv()
        h_cp(k).wait_recv()
    g_own.wait()
    h_own.wait()

    @pl.loop(0, sub // 16)
    def _(r):
        x = rows[ds(r * 16, 16), :].astype(F32)
        inv = lax.rsqrt(jnp.sum(x * x, axis=1, keepdims=True) / dim + NORM_EPS)
        n_v[ds(z * sub + r * 16, 16), :] = (x * inv * gains[0:1, :]).astype(BF16)

    ag.start()
    outs = [net.here(rows, h_o), net.here(gains, g_o)]
    for k in far_first:
        e_cp(k, peer[k]).wait_recv()
    e_own.wait()
    ag.step1()
    for w in (q_w, kv_w):
        w.y_event(0)
    for w in (q_w, kv_w):
        w.x_event(0)
    for w in (q_w, kv_w):
        w.finish_local()
        w.finish(0)
    for k in far_first:
        e_cp(k, tx).wait_send()

    def n2_block(b):
        @pl.loop(0, dim // dtile)
        def _(j):
            cols = ds(j * dtile, dtile)
            p_v[ds(b * sub, sub), cols] = dot(eq_v[:, ds(b * sub, sub)], wq_v[:, cols], ROWS_ROWS).astype(BF16)

    @pl.loop(0, 4)
    def _(i):
        n2_block(pick(3 - i, z))
        for step in range(3):
            pl.when(i == step)(lambda step=step: rsc.send_end(2 - step))
        pl.when(i == 0)(lambda: gate.y_event(0))

    wide = ff // 2

    def gate_part(b, c):
        cols = pl.ds(c * wide, wide)
        a_v[ds(b * sub, sub), cols] = dot(n_v[ds(b * sub, sub), :], wg_v[:, cols]).astype(BF16)

    def up_part(b, c):
        cols = pl.ds(c * wide, wide)
        bb = dot(n_v[ds(b * sub, sub), :], wu_v[:, cols]).astype(BF16)
        b_v[ds(b * sub, sub), cols] = bb
        aa = a_v[ds(b * sub, sub), cols].astype(F32)
        wg_v[ds(b * sub, sub), cols] = (aa * jax.nn.sigmoid(aa) * bb.astype(F32)).astype(BF16)

    def down_part(b, j):
        cols = pl.ds(j * (dim // 2), dim // 2)
        n_v[ds(b * sub, sub), cols] = dot(wg_v[ds(b * sub, sub), :], wd_v[:, cols]).astype(BF16)

    outs += [net.here(wq_v, wq_o), net.here(eq_v, eq_o)]
    gate.finish_local()
    gate.y_event(1)
    ag.step2()
    ag.step3_mid()
    gate.x_event(0)
    gate.finish(0)

    @pl.loop(0, 3)
    def _(i):
        gate_part(pick(i, z), 0)

    up.y_event(0)
    gate.x_event(1)
    rsc.send_mid(2)
    gate.finish(1)
    wg_out = net.here(wg_v, wg_o)

    @pl.loop(0, 3)
    def _(i):
        gate_part(pick(i, z), 1)

    up.finish_local()
    up.y_event(1)
    up.x_event(0)
    up.finish(0)
    ag.step3_end()

    @pl.loop(0, 2)
    def _(c):
        cols = ds(c * wide, wide)
        b = pick(3, z)
        a_v[ds(b * sub, sub), cols] = dot(n_v[ds(b * sub, sub), :], wg_v[:, cols]).astype(BF16)

    wg_out.wait()
    n_out = net.here(n_v, n_o)

    @pl.loop(0, 4)
    def _(i):
        pl.when(i == 1)(lambda: down.y_event(0))
        pl.when(i == 2)(lambda: down.y_event(1))
        pl.when(i == 3)(lambda: up.x_event(1))
        up_part(pick(i, z), 0)

    def up_events_1():
        rsc.send_mid(1)
        rsc.send_mid(0)
        down.x_event(0)

    def up_events_2():
        down.y_event(2)

    def up_events_3():
        down.y_event(3)
        down.x_event(1)

    up.finish(1)
    outs.append(net.here(wu_v, wu_o))

    @pl.loop(0, 4)
    def _(i):
        pl.when(i == 1)(up_events_1)
        pl.when(i == 2)(up_events_2)
        pl.when(i == 3)(up_events_3)
        b = pick(i, z)
        up_part(b, 1)
        ux_cp(2, b).start()
        ux_cp(1, b).start()

    outs.append(net.here(u_v, u_o))
    ag.drain()
    gate.drain()
    n_out.wait()
    down.finish_local()

    @pl.loop(0, 4)
    def _(i):
        pl.when(i == 2)(lambda: down.x_event(2))
        pl.when(i == 3)(lambda: down.x_event(3))
        down_part(pick(3 - i, z), 0)

    for ch in range(4):
        down.finish(ch)

    @pl.loop(0, 4)
    def _(i):
        down_part(pick(3 - i, z), 1)
        for step in range(3):
            pl.when(i == step)(lambda step=step: rs2[0].send_end(2 - step))

    for c in (1, 2, 3):
        for i in (2, 1, 0):
            rs2[c].send_end(i)
    dg_v[...] = jnp.zeros_like(dg_v)
    step = 16

    def norm_chunk(c):
        @pl.loop(0, cs // step)
        def _(r):
            at = c * cs + r * step
            view, mine, far = ds(at, step), ds(z * sub + at, step), ds(4 * sub + at, step)

            def whole(part, got):
                right = jnp.where(z < 3, got[mine, :].astype(F32), 0.0)
                left = jnp.where(z > 0, got[far, :].astype(F32), 0.0)
                return part[mine, :].astype(F32) + right + left

            resid = (rows[view, :].astype(F32) + whole(n_v, rbuf2)).astype(BF16)
            dy = whole(p_v, rbuf)
            res_v[view, :] = resid
            x = resid.astype(F32)
            inv = lax.rsqrt(jnp.sum(x * x, axis=1, keepdims=True) / dim + NORM_EPS)
            xhat = x * inv
            gain = gains[1:2, :]
            n2_v[view, :] = (xhat * gain).astype(BF16)
            part = dy * xhat
            dg_v[...] += part[:8] + part[8:]
            inner = jnp.sum(part * gain, axis=1, keepdims=True) / dim
            dres = dh2_v[view, :].astype(F32) + inv * (dy * gain) - xhat * (inv * inner)
            dres_v[view, pl.ds(0, dim)] = dres
            wg_v[ds(tokens + z * sub + at, step), :] = dres.astype(BF16)

    def spread(b, half):
        for k in far_first:
            ex_cp(k, b, half).start()

    def back_tile(b, j):
        view, cols = ds(b * sub, sub), ds(j * (ff // 4), ff // 4)
        du = dot(wg_v[ds(tokens + b * sub, sub), :], wd_v[ds(j * (ff // 4), ff // 4), :], NT_DIMS)
        aa = a_v[view, cols].astype(F32)
        bb = b_v[view, cols].astype(F32)
        sig = jax.nn.sigmoid(aa)
        a_v[view, cols] = (du * bb * sig * (1.0 + aa * (1.0 - sig))).astype(BF16)
        b_v[view, cols] = (du * aa * sig).astype(BF16)

    def scatter(i, c):
        return lambda: rs2[c].send_mid(i)

    def gathered(i, c):
        def go():
            ag2[c].take(i)
            pl.when(mid(z))(lambda: ag2[c].forward(i))
            if c % 2 == 1:
                spread(ag.slots[i], c // 2)
        return go

    def run(ops):
        def go():
            for op in ops:
                op()
        return go

    before_mid = (
        (scatter(2, 0), scatter(1, 0), scatter(0, 0)),
        (scatter(2, 1), gathered(1, 0), scatter(1, 1), scatter(0, 1)),
        (scatter(2, 2), scatter(1, 2), gathered(1, 1), scatter(0, 2), scatter(2, 3)),
        (scatter(1, 3), scatter(0, 3), gathered(1, 2), gathered(0, 0)))
    before_end = ((), (gathered(0, 0), gathered(1, 0)), (gathered(0, 1), gathered(1, 1)), (gathered(0, 2),))
    after_mid = {0: (gathered(0, 1),), 1: (gathered(2, 0),), 2: (gathered(0, 2),), 3: (gathered(1, 3),), 5: (gathered(0, 3),), 7: (gathered(2, 1),),
                 10: (gathered(2, 2),), 12: (gathered(2, 3),)}
    after_end = {3: (gathered(1, 2),), 4: (gathered(0, 3),), 7: (gathered(2, 0),), 8: (gathered(1, 3),),
                 12: (gathered(2, 1), gathered(2, 2), gathered(2, 3))}

    for c in range(4):
        pl.when(mid(z))(run(before_mid[c]))
        pl.when(end(z))(run(before_end[c]))
        if c == 0:
            rsc.finish()
            for k in far_first:
                d_cp(k).wait_recv()
            d_own.wait()
            tab_out.wait()
        rs2[c].finish()
        norm_chunk(c)
        ag2[c].start()
        if c % 2 == 1:
            spread(z, c // 2)

    for k in far_first:
        o_cp(k, tx).start()
    outs += [net.here(res_v.at[:, pl.ds(0, dt)], home_o.at[ds(tx * sub, sub), :]), net.here(n2_v, n2_o), net.here(dres_v.at[pl.ds(0, sub), pl.ds(0, dim)], dres_o), net.here(dg_v, dg_o)]
    rsc.drain()
    for c in range(4):
        rs2[c].drain()
    n_in = net.here(n_o, p_v)
    middle = (z + 1) // 2 % 2

    def u_forward():
        for b in range(4):
            ux_cp(2, b).wait_recv()
            ux_cp(3, b).start()

    @pl.loop(0, 16)
    def _(t):
        for at, ops in after_mid.items():
            pl.when(jnp.logical_and(t == at, mid(z)))(run(ops))
        for at, ops in after_end.items():
            pl.when(jnp.logical_and(t == at, end(z)))(run(ops))
        pl.when(t == 8)(u_forward)
        i = t // 4
        inner = (i + 1) // 2 % 2
        back_tile(pick(i + middle * inner * (3 - 2 * i), z), t % 4)

    outs.append(net.here(e_v, e_o))
    outs += [net.here(a_v, da_o), net.here(b_v, db_o)]

    last = pl.ds(ff - ff // 4, ff // 4)

    def down_tile(k, j):
        return dot(wg_v[pl.ds(0, tokens), last], wg_v[pl.ds(tokens, tokens), pl.ds(k * dt, dt)], ROWS_ROWS)

    def gate_tile(k, j):
        return dot(p_v[:, pl.ds(k * dt, dt)], a_v[:, ds(j * (ff // 4), ff // 4)], ROWS_ROWS)

    quarter = [rbuf.at[pl.ds(0, ff // 4), pl.ds(i * dt, dt)] for i in range(4)]
    part_d = GradReduce(net, peer, down_tile, 1, quarter[0], quarter[1], quarter[2], quarter[3], d2_o, d0_o, None, dc_o, None)
    part_g = GradReduce(net, peer, gate_tile, 4, n_v.at[pl.ds(0, dt), :], None, None, None, g2_o, None, None, wg_o, None)
    n_in.wait()
    part_d.step3()
    part_d.step1()
    part_g.step3()
    part_d.step2()
    outs.append(net.here(quarter[2], dc_o))
    for k in far_first:
        o_cp(k, peer[k]).wait_recv()
        for b in range(4):
            ex_cp(k, b, 0).wait_recv()
            ex_cp(k, b, 1).wait_recv()
    for b in range(4):
        ux_cp(1, b).wait_recv()
        ux_cp(3, b).wait_recv()
    for c in outs:
        c.wait()
    for k in far_first:
        g_cp(k).wait_send()
        h_cp(k).wait_send()
        d_cp(k).wait_send()
        o_cp(k, tx).wait_send()
        for b in range(4):
            ux_cp(k, b).wait_send()
            ex_cp(k, b, 0).wait_send()
            ex_cp(k, b, 1).wait_send()
    for w in (q_w, kv_w, up, down):
        w.drain()
    for c in range(4):
        ag2[c].drain()
    part_d.cp(1).wait_recv()
    part_d.sent_locally()
    part_g.cp(0).wait_recv()
    part_g.cp(0).wait_send()


def call_ab(hid, eqh, ekvh, ang, swap, dh2h, wg, wu, wd, wq, wkv, gin):
    tokens, dt = hid.shape
    sub, dim, ff, q_width = tokens // 4, dt * 4, wg.shape[1], wq.shape[0]
    width = q_width + wkv.shape[0]
    s = jax.ShapeDtypeStruct
    tok_ff, tok_d, row = s((tokens, ff), BF16), s((tokens, dim), BF16), s((sub, dim), BF16)
    shapes = (tok_d, tok_ff, tok_ff, tok_ff, s((dim, ff), BF16), s((dim, ff), BF16), s((width, dim), BF16), s((width, tokens), BF16),
              row, s((8, dim), F32), tok_d, row, s((sub, dim), F32), s((tokens, dt), BF16), s((8, dim), F32),
              s((3, tokens, ff - ff // 4), BF16), s((3, tokens, dt), BF16), s((256, 2 * tokens), F32), s((dt, ff), BF16)) + (s((ff // 4, dt), BF16),) * 3
    vrow, vtok, vff = VMEM((sub, dim), BF16), VMEM((tokens, dim), BF16), VMEM((tokens, ff), BF16)
    return pl.pallas_call(
        functools.partial(kernel_ab, q_width), out_shape=shapes, in_specs=[ANY] * 12, out_specs=[ANY] * len(shapes),
        scratch_shapes=[
            vrow, vrow, vrow, vrow, VMEM((max(sub, 256), max(dim, 2 * tokens)), F32), vtok, vff, vff, VMEM((dim, ff), BF16), VMEM((dim, ff), BF16), VMEM((ff, dim), BF16),
            VMEM((width, dim), BF16), VMEM((width, tokens), BF16), vtok, VMEM((5 * sub, dim), BF16), VMEM((5 * sub, dim), BF16),
            VMEM((8, dim), F32), VMEM((8, dim), F32), VMEM((128, 128), BF16),
            pltpu.SemaphoreType.DMA((180,)), pltpu.SemaphoreType.DMA((180,)), pltpu.SemaphoreType.DMA((48,))],
        compiler_params=pltpu.CompilerParams(collective_id=0, has_side_effects=True, vmem_limit_bytes=VMEM_LIMIT),
        cost_estimate=pl.CostEstimate(flops=20 * tokens * dim * ff, bytes_accessed=100000000, transcendentals=0), name="phase_ab",
    )(hid, eqh, ekvh, ang, swap, dh2h, wg, wu, wd, wq, wkv, gin)


def kernel_c(q_width, da_h, db_h, wg_h, wu_h, n_h, u_h, ux_h, e_h, ex_h, n2_h, eq_h, wq_h, h_h, dres_h, g_h, dga_h, tabh, swaph, g2, d0, dc,
             wgo, wgy, wuo, wuy, wdo, wqo, wqy, wvo, wvy, q_o, kv_o, dh_o, dg_o, g0, u2, u0, q2, q0, v2, v0, qx, dy,
             wg_v, wu_v, da_v, db_v, n_v, p_v, rbuf, n2_v, st3, st1, cross_g, cross_u, stage, tiles_v, dres_v, wq_v, eq_v,
             gains, dg_v, dgr, dgz, tab_v, swap_v, send, recv, local):
    dp, z, tx, peer = places()
    tokens, ff = da_v.shape
    sub, dim = dres_v.shape
    dt = dim // 4
    width = eq_v.shape[0]
    tile = ff // 4
    dtile = min(512, dim)
    qt = min(256, tile)
    far_first = (2, 3, 1)
    net = Wires(send, recv, local)
    n2_in = net.here(n2_h, n2_v.at[ds(z * sub, sub), :])
    first = [net.here(n_h, n_v), net.here(da_h, da_v)]
    second = [net.here(db_h, db_v), net.here(wg_h, wg_v), net.here(wu_h, wu_v)]
    third = [net.here(wq_h, wq_v), net.here(eq_h, eq_v), net.here(dres_h, dres_v), net.here(g_h, gains),
             net.here(dga_h, dg_v.at[pl.ds(8, 8), :]), net.here(tabh, tab_v), net.here(swaph, swap_v)]
    sem = pltpu.get_barrier_semaphore()
    zs = tuple((z + i) % 4 for i in range(4))
    for i in (1, 2, 3):
        pl.semaphore_signal(sem, inc=1, device_id={"tx": peer[i]}, device_id_type=MESH)
        pl.semaphore_signal(sem, inc=1, device_id={"ty": zs[i]}, device_id_type=MESH)
    pl.semaphore_wait(sem, 6)
    rsc = LineScatter(net, p_v, rbuf, sub, z)
    ag = LineGather(net, n2_v, sub, z)
    q_id, h_id, t_id, z_id = net.take(4), net.take(4), net.take(4), net.take(4)

    def grad_tile(lhs, rhs, w):
        def go(k, j):
            cols = pl.ds(j * w, w) if isinstance(j, int) else ds(j * w, w)
            return dot(lhs[:, pl.ds(k * dt, dt)], rhs[:, cols], ROWS_ROWS)
        return go

    gate = GradReduce(net, peer, grad_tile(n_v, da_v, tile), ff // tile, st3, st1, cross_g, stage, g2, g0, wgy, wgo, tiles_v)
    up = GradReduce(net, peer, grad_tile(n_v, db_v, tile), ff // tile, st3, st1, cross_u, stage, u2, u0, wuy, wuo, tiles_v)
    d_id = net.take(1)

    def dy_cp():
        return net.copy(dc, dy, d_id, d_id, tx=peer[2])

    dy_cp().start()

    def head_grad(first, rows, got2, got0, got_y, out):
        corner = [da_v.at[pl.ds(first, rows), pl.ds(c * dt, dt)] for c in range(4)]

        def tile_of(k, j):
            return dot(eq_v[pl.ds(first, rows), :], n2_v[:, ds(k * dt + j * qt, qt)])

        return GradReduce(net, peer, tile_of, dt // qt, *corner, got2, got0, got_y, out, tiles_v)

    heads = (head_grad(0, q_width, q2, q0, wqy, wqo), head_grad(q_width, width - q_width, v2, v0, wvy, wvo))

    def dn_block(b):
        rows = ds(b * sub, sub)

        @pl.loop(0, dim // dtile)
        def _(j):
            wr = ds(j * dtile, dtile)
            p_v[rows, wr] = (dot(da_v[rows, :], wg_v[wr, :], NT_DIMS) + dot(db_v[rows, :], wu_v[wr, :], NT_DIMS)).astype(BF16)

    n2_in.wait()
    ag.start()
    for c in first:
        c.wait()
    gate.step2(True)
    gate.send()
    gate.step1()
    for c in second:
        c.wait()

    @pl.loop(0, 4)
    def _(i):
        @pl.when(i == 1)
        def _():
            up.step3()
            gate.cp(1).wait_send()
            up.step1()
            ag.step1()

        dn_block(pick(3 - i, z))
        for step in range(3):
            pl.when(i == step)(lambda step=step: rsc.send_end(2 - step))

    up.step2()
    up.send()
    rsc.send_mid(2)
    ag.step2()
    ag.step3_mid()
    up.sent_locally()
    h_in = net.here(h_h, st3.at[pl.ds(0, sub), :])
    gate.step0(st1)
    gate.sent()

    n_tiles = ff // tile
    e_in = [net.here(e_h.at[:, pl.ds(0, dt)], wu_v.at[pl.ds(0, tokens), pl.ds(0, dt)])]
    for k in (1, 2, 3):
        e_in.append(net.here(ex_h.at[k - 1], wu_v.at[pl.ds(0, tokens), pl.ds(k * dt, dt)]))

    def u_place(j, k):
        return wg_v.at[pl.ds((j % 2) * tokens, tokens), pl.ds(k * tile, tile)]

    def u_load(j):
        cols = pl.ds(j * tile, tile)
        if j == n_tiles - 1:
            return [net.here(u_h.at[:, cols], u_place(j, 0)), net.here(d0, stage.at[pl.ds(0, tile), pl.ds(0, dt)]), net.here(dy, stage.at[pl.ds(0, tile), pl.ds(dt, dt)])]
        return [net.here(u_h.at[:, cols] if k == 0 else ux_h.at[k - 1, :, cols], u_place(j, k)) for k in range(4)]

    def down_tile(j, slot, loads):
        for c in loads:
            c.wait()
        acc = None
        if j == n_tiles - 1:
            acc = stage[pl.ds(0, tile), pl.ds(0, dt)].astype(F32) + stage[pl.ds(0, tile), pl.ds(dt, dt)].astype(F32)
        for k in range(1 if j == n_tiles - 1 else 4):
            part = dot(u_place(j, k)[...], wu_v[pl.ds(0, tokens), pl.ds(k * dt, dt)], ROWS_ROWS)
            acc = part if acc is None else acc + part
        tiles_v[slot, pl.ds(0, tile), pl.ds(0, dt)] = acc
        return net.here(tiles_v.at[slot, pl.ds(0, tile), pl.ds(0, dt)], wdo.at[pl.ds(j * tile, tile), :])

    loads = {0: u_load(0), 1: u_load(1)}
    rsc.send_mid(1)
    rsc.send_mid(0)
    for c in e_in:
        c.wait()
    done = [down_tile(0, 0, loads[0]), down_tile(1, 1, loads[1])]
    loads = {2: u_load(2)}
    for c in third:
        c.wait()
    ag.step3_end()

    @pl.loop(0, width // qt)
    def _(j):
        wu_v[ds(tokens + j * qt, qt), pl.ds(0, tokens)] = dot(wq_v[ds(j * qt, qt), :], n2_v[...], NT_DIMS).astype(BF16)

    def q_cp(k, block):
        return net.copy(wu_v.at[pl.ds(tokens, width), ds(peer[k] * sub, sub)], qx.at[:, ds(block * sub, sub)], q_id + k, q_id + k, tx=peer[k])

    for k in far_first:
        q_cp(k, tx).start()
    q_own = net.here(wu_v.at[pl.ds(tokens, width), ds(tx * sub, sub)], qx.at[:, ds(tx * sub, sub)])
    for c in done:
        c.wait()
    for part in heads:
        part.step3()
        part.step1()
    dy_cp().wait_recv()
    loads[3] = u_load(3)
    for part in heads:
        part.step2()
        part.send()
    done = [down_tile(2, 0, loads[2]), down_tile(3, 1, loads[3])]
    h_in.wait()
    rsc.finish()
    dg_v[pl.ds(0, 8), :] = jnp.zeros((8, dim), F32)
    step = 16

    @pl.loop(0, sub // step)
    def _(r):
        view, mine, far = ds(r * step, step), ds(z * sub + r * step, step), ds(4 * sub + r * step, step)
        right = jnp.where(z < 3, rbuf[mine, :].astype(F32), 0.0)
        left = jnp.where(z > 0, rbuf[far, :].astype(F32), 0.0)
        dy = p_v[mine, :].astype(F32) + right + left
        x = st3[view, :].astype(F32)
        inv = lax.rsqrt(jnp.sum(x * x, axis=1, keepdims=True) / dim + NORM_EPS)
        xhat = x * inv
        gain = gains[0:1, :]
        part = dy * xhat
        dg_v[pl.ds(0, 8), :] += part[:8] + part[8:]
        inner = jnp.sum(part * gain, axis=1, keepdims=True) / dim
        st1[view, :] = (dres_v[view, :] + inv * (dy * gain) - xhat * (inv * inner)).astype(BF16)

    def h_cp(k, block):
        return net.copy(st1.at[pl.ds(0, sub), pl.ds(k * dt, dt)], dh_o.at[ds(block * sub, sub), :], h_id + k, h_id + k, tx=peer[k])

    def t_cp(k):
        return net.copy(dg_v.at[:, pl.ds(k * dt, dt)], dgr.at[k], t_id + k, t_id + k, tx=peer[k])

    def z_cp(i):
        return net.copy(dgr.at[0], dgz.at[i], z_id + i, z_id + i, ty=zs[i])

    for k in far_first:
        t_cp(k).start()
    for k in far_first:
        h_cp(k, tx).start()
    h_own = net.here(st1.at[pl.ds(0, sub), pl.ds(0, dt)], dh_o.at[ds(tx * sub, sub), :])
    up.sent()
    for c in done:
        c.wait()
    up.step0(cross_g)
    for k in far_first:
        q_cp(k, peer[k]).wait_recv()
    q_own.wait()
    turned = wu_v.at[pl.ds(tokens, width), pl.ds(tokens, tokens)]
    net.here(qx, turned).wait()
    turn(turned, width, q_width, tokens, tab_v, swap_v, False)
    q_out = net.here(wu_v.at[pl.ds(tokens, q_width), pl.ds(tokens, tokens)], q_o)
    kv_out = net.here(wu_v.at[pl.ds(tokens + q_width, width - q_width), pl.ds(tokens, tokens)], kv_o)
    heads[0].step0(cross_g.at[pl.ds(0, q_width), pl.ds(0, dt)])
    heads[1].step0(cross_g.at[pl.ds(0, width - q_width), pl.ds(dt, dt)])
    for k in far_first:
        t_cp(k).wait_recv()
    dgr[0] = dg_v[:, pl.ds(0, dt)] + dgr[1] + dgr[2] + dgr[3]
    for i in (1, 2, 3):
        z_cp(i).start()
    for i in (1, 2, 3):
        z_cp(i).wait_recv()
    dgz[0] = dgr[0] + dgz[1] + dgz[2] + dgz[3]
    dg_out = net.here(dgz.at[0], dg_o)
    for k in far_first:
        h_cp(k, peer[k]).wait_recv()
    for c in (q_out, kv_out, dg_out, h_own):
        c.wait()
    dy_cp().wait_send()
    for part in heads:
        part.sent_locally()
        part.sent()
    for k in far_first:
        q_cp(k, tx).wait_send()
        h_cp(k, tx).wait_send()
        t_cp(k).wait_send()
        z_cp(k).wait_send()
    ag.drain()
    rsc.drain()


def call_c(q_width, *args):
    tokens, ff = args[0].shape
    sub, dim = args[9].shape
    dt, width = dim // 4, args[10].shape[0]
    rest = width - q_width
    tile = ff // 4
    s = jax.ShapeDtypeStruct
    wf, wb = s((dt, ff), F32), s((dt, ff), BF16)
    qf, qb, vf, vb = s((q_width, dt), F32), s((q_width, dt), BF16), s((rest, dt), F32), s((rest, dt), BF16)
    shapes = (wf, wb, wf, wb, s((ff, dt), F32), qf, qb, vf, vb, s((q_width, tokens), BF16), s((rest, tokens), BF16), s((tokens, dt), BF16), s((16, dt), F32),
              wb, wb, wb, qb, qb, vb, vb, s((width, tokens), BF16), s((tile, dt), BF16))
    return pl.pallas_call(
        functools.partial(kernel_c, q_width), out_shape=shapes, in_specs=[ANY] * len(args), out_specs=[ANY] * len(shapes),
        scratch_shapes=[
            VMEM((dim, ff), BF16), VMEM((dim, ff), BF16), VMEM((tokens, ff), BF16), VMEM((tokens, ff), BF16), VMEM((tokens, dim), BF16),
            VMEM((tokens, dim), BF16), VMEM((5 * sub, dim), BF16), VMEM((tokens, dim), BF16),
            VMEM((dt, ff), BF16), VMEM((dt, ff), BF16), VMEM((dt, ff), BF16), VMEM((dt, ff), BF16), VMEM((dt, ff), BF16),
            VMEM((2, max(dt, tile), max(dt, tile)), F32), VMEM((sub, dim), F32), VMEM((width, dim), BF16), VMEM((width, tokens), BF16),
            VMEM((8, dim), F32), VMEM((16, dim), F32), VMEM((4, 16, dt), F32), VMEM((4, 16, dt), F32), VMEM((256, 2 * tokens), F32), VMEM((128, 128), BF16),
            pltpu.SemaphoreType.DMA((48,)), pltpu.SemaphoreType.DMA((48,)), pltpu.SemaphoreType.DMA((72,))],
        compiler_params=pltpu.CompilerParams(collective_id=2, has_side_effects=True, vmem_limit_bytes=VMEM_LIMIT),
        cost_estimate=pl.CostEstimate(flops=20 * tokens * dim * ff, bytes_accessed=100000000, transcendentals=0), name="phase_c",
    )(*args)


def solution(mesh):
    def local_step(hidden, positions, g_ffn, w_gate, w_up, w_down, g_attn, w_q, w_kv, grad_h2, grad_q, grad_kv):
        tokens, dt = hidden.shape
        q_heads, head_dim = w_q.shape[1:]
        q_width = q_heads * head_dim

        lane = np.arange(128)
        inv_freq = ROPE_BASE ** (-(lane % head_dim // 2 * 2).astype(np.float32) / head_dim)
        angles = jnp.asarray(inv_freq, F32)[:, None] * positions.astype(F32)[None, :]
        swap = np.zeros((128, 128), np.float32)
        swap[lane, lane ^ 1] = np.where(lane % 2 == 0, -1.0, 1.0)
        swap = jnp.asarray(swap, BF16)

        def heads_first(x):
            return x.transpose(1, 2, 0).reshape(-1, x.shape[0])

        def heads_last(x):
            return x.reshape(-1, head_dim, x.shape[1]).transpose(2, 0, 1)

        gin = jnp.where(jnp.arange(8)[:, None] == 0, g_ffn[None, :], g_attn[None, :]).astype(F32)

        (normed_all, grad_gate, grad_up, u_all, gate_w, up_w, w_qkv, back_all, h_rows, gains, res_all, normed2, grad_res, resid_out, gattn8,
         u_other, e_other, table, wg_two, _, wd_zero, wd_cross) = call_ab(
             hidden, heads_first(grad_q), heads_first(grad_kv), angles, swap, grad_h2, w_gate, w_up, w_down, heads_first(w_q), heads_first(w_kv), gin)
        (grad_wgate, _, grad_wup, _, grad_wdown, grad_wq, _, grad_wkv, _, q_out, kv_out, grad_hidden, gain_grads, *_) = call_c(
            q_width, grad_gate, grad_up, gate_w, up_w, normed_all, u_all, u_other, res_all, e_other, normed2, back_all, w_qkv,
            h_rows, grad_res, gains, gattn8, table, swap, wg_two, wd_zero, wd_cross)
        q_out, kv_out, grad_wq, grad_wkv = (heads_last(x) for x in (q_out, kv_out, grad_wq, grad_wkv))
        grad_gffn = jnp.sum(gain_grads[:8], axis=0)
        grad_gattn = jnp.sum(gain_grads[8:], axis=0)
        return (resid_out, q_out, kv_out, grad_hidden, grad_gffn, grad_gattn, grad_wgate, grad_wup, grad_wdown, grad_wq, grad_wkv)

    row_spec = P(("dp", "ty"), "tx")
    head_spec = P(("dp", "tx"), "ty", None)
    in_specs = (row_spec, P(("dp", "tx")), P("tx"), P("tx", "ty"), P("tx", "ty"), P("ty", "tx"), P("tx"), P("tx", "ty", None), P("tx", "ty", None), row_spec, head_spec, head_spec)
    out_specs = (row_spec, head_spec, head_spec, row_spec, P(("dp", "tx")), P(("dp", "tx")), P(("dp", "tx"), "ty"), P(("dp", "tx"), "ty"), P(("dp", "ty"), "tx"), head_spec, head_spec)
    return jax.shard_map(local_step, mesh=mesh, in_specs=in_specs, out_specs=out_specs, check_vma=False)
```

```python
import functools

import jax
import jax.numpy as jnp
import numpy as np
from jax import lax
from jax.experimental import pallas as pl
from jax.experimental.pallas import tpu as pltpu
from jax.sharding import PartitionSpec as P

NORM_EPS = 1e-5
ROPE_BASE = 10000.0
F32 = jnp.float32
BF16 = jnp.bfloat16


def dot(a, b, dims=(((1,), (0,)), ((), ()))):
    return lax.dot_general(a, b, dims, preferred_element_type=F32)


MESH = pl.DeviceIdType.MESH
ANY = pl.BlockSpec(memory_space=pl.ANY)
VMEM = pltpu.VMEM
NT_DIMS = (((1,), (1,)), ((), ()))
VMEM_LIMIT = 67000000


def ds(start, size, align=None):
    if isinstance(start, int):
        return pl.ds(start, size)
    return pl.ds(pl.multiple_of(start, align or size), size)


def mid(z):
    return jnp.logical_and(z > 0, z < 3)


def end(z):
    return jnp.logical_or(z == 0, z == 3)


def slots(z):
    return (z + 1 - 2 * (z % 2), 2 - z // 2, 3 - 3 * (z // 2))


def turn(x_ref, width, q_width, tokens, table_ref, swap_ref, back):
    step = min(256, tokens)

    @pl.loop(0, tokens // step)
    def _(r):
        cols = ds(r * step, step)
        for g in range(width // 128):
            rows = pl.ds(g * 128, 128)
            base = pl.ds(0 if g * 128 < q_width else 128, 128)
            x = x_ref[rows, cols]
            main = x.astype(F32) * table_ref[base, cols]
            side = dot(swap_ref[...], x) * table_ref[base, ds(tokens + r * step, step)]
            x_ref[rows, cols] = (main - side if back else main + side).astype(BF16)


def pick(i, z):
    s1, s2, s3 = slots(z)
    first, last = (3 - i) // 3, (i // 2) * (i % 2)
    return z * first + s1 * ((i % 2) * (1 - i // 2)) + s2 * ((i // 2) * (1 - i % 2)) + s3 * last


class Wires:
    def __init__(self, send, recv, local):
        self.send, self.recv, self.local = send, recv, local
        self.n_remote = 0
        self.n_local = 0

    def take(self, n=1):
        base = self.n_remote
        self.n_remote += n
        assert self.n_remote <= self.send.shape[0]
        return base

    def copy(self, src, dst, si, ri, **dev):
        return pltpu.make_async_remote_copy(
            src_ref=src, dst_ref=dst, send_sem=self.send.at[si], recv_sem=self.recv.at[ri],
            device_id=dev, device_id_type=MESH)

    def here(self, src, dst):
        i = self.n_local
        self.n_local += 1
        assert i < self.local.shape[0]
        c = pltpu.make_async_copy(src, dst, self.local.at[i])
        c.start()
        return c


def entry_barrier(axes, z):
    sem = pltpu.get_barrier_semaphore()
    for dev in axes:
        pl.semaphore_signal(sem, inc=1, device_id=dev, device_id_type=MESH)

    @pl.when(z > 0)
    def _():
        pl.semaphore_signal(sem, inc=1, device_id={"ty": z - 1}, device_id_type=MESH)

    @pl.when(z < 3)
    def _():
        pl.semaphore_signal(sem, inc=1, device_id={"ty": z + 1}, device_id_type=MESH)

    @pl.when(mid(z))
    def _():
        pl.semaphore_wait(sem, len(axes) + 2)

    @pl.when(end(z))
    def _():
        pl.semaphore_wait(sem, len(axes) + 1)


class LineGather:
    def __init__(self, net, buf, rows, z, off=0, part=None):
        self.net, self.buf, self.rows, self.z, self.off, self.part = net, buf, rows, z, off, part or rows
        self.base = net.take(8)
        self.slots = slots(z)

    def blk(self, b):
        return self.buf.at[ds(b * self.rows + self.off, self.part), :]

    def cp(self, b, side, target):
        return self.net.copy(self.blk(b), self.blk(b), self.base + side * 4 + b, self.base + b, ty=target)

    def start(self):
        z = self.z

        @pl.when(z < 3)
        def _():
            self.cp(z, 0, z + 1).start()

        @pl.when(z > 0)
        def _():
            self.cp(z, 1, z - 1).start()

    def take(self, i):
        b = self.slots[i]
        self.cp(b, 0, self.z).wait_recv()

    def forward(self, i):
        z, b = self.z, self.slots[i]
        target = 3 - z if i == 0 else 3 * (z - 1)
        self.cp(b, 0, target).start()

    def step1(self):
        self.take(0)

        @pl.when(mid(self.z))
        def _():
            self.forward(0)
            self.take(1)
            self.forward(1)

    def near_end(self):
        @pl.when(end(self.z))
        def _():
            self.take(0)

    def near_mid(self):
        @pl.when(mid(self.z))
        def _():
            self.take(1)
            self.forward(1)

    def far_mid(self):
        @pl.when(mid(self.z))
        def _():
            self.take(0)
            self.forward(0)

    def step2(self):
        @pl.when(end(self.z))
        def _():
            self.take(1)

    def step3_mid(self):
        @pl.when(mid(self.z))
        def _():
            self.take(2)
            self.forward(2)

    def step3_end(self):
        @pl.when(end(self.z))
        def _():
            self.take(2)

    def drain(self):
        z = self.z

        @pl.when(z < 3)
        def _():
            self.cp(z, 0, z + 1).wait_send()

        @pl.when(z > 0)
        def _():
            self.cp(z, 1, z - 1).wait_send()

        @pl.when(mid(z))
        def _():
            for i in range(3):
                self.cp(self.slots[i], 0, 3 - z if i == 0 else 3 * (z - 1)).wait_send()


class LineScatter:
    def __init__(self, net, part, rbuf, rows, z, off=0, size=None):
        self.net, self.part, self.rbuf, self.rows, self.z, self.off, self.size = net, part, rbuf, rows, z, off, size or rows
        self.base = net.take(5)
        self.slots = slots(z)
        one = (z % 2) * (1 - z // 2)
        self.dst = (self.slots[0] + (1 - z % 2) * (3 - z), self.slots[1] + 2 * one, self.slots[2])
        self.target = (z + 1 - 2 * (z % 2), 1 + z % 2, 1 + z % 2)

    def cp(self, i):
        return self.net.copy(
            self.part.at[self.view(self.slots[i]), :], self.rbuf.at[self.view(self.dst[i]), :],
            self.base + i, self.base + self.dst[i], ty=self.target[i])

    def view(self, b):
        return ds(b * self.rows + self.off, self.size)

    def wait_slot(self, s):
        view = self.rbuf.at[self.view(s), :]
        self.net.copy(view, view, self.base, self.base + s, ty=self.z).wait_recv()

    def send_end(self, i):
        @pl.when(end(self.z))
        def _():
            self.cp(i).start()

    def send_mid(self, i):
        @pl.when(mid(self.z))
        def _():
            b = self.slots[i]
            self.wait_slot(b)
            step = 16

            @pl.loop(0, self.size // step)
            def _(r):
                view = ds(b * self.rows + self.off + r * step, step)
                self.part[view, :] = (self.part[view, :].astype(F32) + self.rbuf[view, :].astype(F32)).astype(BF16)

            self.cp(i).start()

    def finish(self):
        z = self.z

        @pl.when(z < 3)
        def _():
            self.wait_slot(z)

        @pl.when(z > 0)
        def _():
            self.wait_slot(4)

    def drain(self):
        for i in range(3):
            self.cp(i).wait_send()


class WeightGather:
    def __init__(self, net, w, full, pos, by_rows, chunks, direct=0):
        self.net, self.w, self.full, self.by_rows = net, w, full, by_rows
        self.dp, self.t1, self.t2 = pos
        self.half = w.shape[0] // 2
        self.width = w.shape[0] if by_rows else w.shape[1]
        self.chunks, self.direct = chunks, direct
        self.base = net.take(1 + 4 * chunks + direct)

    def area(self, half, ch):
        if self.by_rows:
            n = self.w.shape[1] // self.chunks
            return ds(half * self.half, self.half, 16), self.half, pl.ds(ch * n, n)
        n = self.half // self.chunks
        return ds(half * self.half + ch * n, n, 16), n, pl.ds(0, self.width)

    def src(self, half, ch):
        rows, _, cols = self.area(half, ch)
        return self.w.at[rows, cols]

    def dst(self, k, half, ch):
        if self.by_rows:
            _, _, cols = self.area(half, ch)
            return self.full.at[ds(k * self.width + half * self.half, self.half, 16), cols]
        rows, _, _ = self.area(half, ch)
        return self.full.at[rows, pl.ds(k * self.width, self.width)]

    def whole(self, k):
        if self.by_rows:
            return self.full.at[pl.ds(k * self.width, self.width), :]
        return self.full.at[:, pl.ds(k * self.width, self.width)]

    def near(self, ch):
        i = self.base + 1 + ch
        return self.net.copy(self.src(self.dp, ch), self.dst(2, self.dp, ch), i, i, tx=self.t2)

    def cross(self, ch, half):
        i = self.base + 1 + self.chunks + ch
        return self.net.copy(self.dst(2, half, ch), self.dst(2, half, ch), i, i, dp=1 - self.dp)

    def diag(self, ch, which, half):
        i = self.base + 1 + (2 + which) * self.chunks + ch
        return self.net.copy(self.dst(2, half, ch), self.dst(3, half, ch), i, i, tx=self.t1)

    def mate(self):
        return self.net.copy(self.w, self.whole(1), self.base, self.base, tx=self.t1)

    def straight(self, n, half):
        ch = self.chunks - 1 - n
        i = self.base + 1 + 4 * self.chunks + n
        return self.net.copy(self.src(half, ch), self.dst(2, half, ch), i, i, tx=self.t2)

    def start_y(self):
        for ch in range(self.chunks):
            self.near(ch).start()
        for n in range(self.direct):
            self.straight(n, 1 - self.dp).start()

    def start_local(self):
        self.own = self.net.here(self.w, self.whole(0))
        self.mate().start()

    def y_event(self, ch):
        self.near(ch).wait_recv()
        if ch < self.chunks - self.direct:
            self.cross(ch, self.dp).start()
        self.diag(ch, 0, self.dp).start()

    def x_event(self, ch):
        if ch < self.chunks - self.direct:
            self.cross(ch, 1 - self.dp).wait_recv()
        else:
            self.straight(self.chunks - 1 - ch, 1 - self.dp).wait_recv()
        self.diag(ch, 1, 1 - self.dp).start()

    def finish_local(self):
        self.own.wait()
        self.mate().wait_recv()

    def finish(self, ch):
        self.diag(ch, 0, self.dp).wait_recv()
        self.diag(ch, 1, 1 - self.dp).wait_recv()

    def drain(self):
        self.mate().wait_send()
        for ch in range(self.chunks):
            self.near(ch).wait_send()
            if ch < self.chunks - self.direct:
                self.cross(ch, self.dp).wait_send()
            else:
                self.straight(self.chunks - 1 - ch, 1 - self.dp).wait_send()
            self.diag(ch, 0, self.dp).wait_send()
            self.diag(ch, 1, 1 - self.dp).wait_send()


def places():
    dp, z, tx = lax.axis_index("dp"), lax.axis_index("ty"), lax.axis_index("tx")
    return dp, z, tx, (tx, tx + 1 - 2 * (tx % 2), (tx + 2) % 4, 3 - tx)


ROWS_ROWS = (((0,), (0,)), ((), ()))


class GradReduce:
    def __init__(self, net, peer, tile, tiles, st3, st1, cross, stage, got2, got0, got_y, out, out_tiles):
        self.net, self.peer, self.tile, self.tiles = net, peer, tile, tiles
        self.st3, self.st1, self.cross, self.stage = st3, st1, cross, stage
        self.got2, self.got0, self.got_y, self.out, self.out_tiles = got2, got0, got_y, out, out_tiles
        self.src = None
        self.base = net.take(3)
        self.rows, self.w = out.shape[0], out.shape[1] // tiles

    def cp(self, i):
        src, dst, to = ((self.st3, self.got2, 1), (self.st1, self.got0, 1), (self.src or self.cross, self.got_y, 2))[i]
        return self.net.copy(src, dst, self.base + i, self.base + i, tx=self.peer[to])

    def fill(self, k, ref):
        @pl.loop(0, self.tiles)
        def _(j):
            ref[:, ds(j * self.w, self.w)] = self.tile(k, j).astype(BF16)

    def step3(self):
        self.fill(3, self.st3)
        self.cp(0).start()

    def step1(self):
        self.fill(1, self.st1)
        self.cp(1).start()

    def step2(self, received=False):
        if not received:
            self.cp(0).wait_recv()
        self.net.here(self.got2, self.stage).wait()

        @pl.loop(0, self.tiles)
        def _(j):
            cols = ds(j * self.w, self.w)
            self.cross[:, cols] = (self.tile(2, j) + self.stage[:, cols].astype(F32)).astype(BF16)

    def send(self, src=None):
        self.src = src
        self.cp(2).start()

    def step0(self, far):
        self.cp(1).wait_recv()
        self.cp(2).wait_recv()
        loads = [self.net.here(self.got0, self.stage), self.net.here(self.got_y, far)]
        for c in loads:
            c.wait()
        base = self.net.n_local
        self.net.n_local += 2

        def put(j, slot):
            src = self.out_tiles.at[slot, pl.ds(0, self.rows), pl.ds(0, self.w)]
            return pltpu.make_async_copy(src, self.out.at[:, ds(j * self.w, self.w)], self.net.local.at[base + slot])

        @pl.loop(0, self.tiles)
        def _(j):
            cols = ds(j * self.w, self.w)
            slot = j % 2

            @pl.when(j >= 2)
            def _():
                put(j, slot).wait()

            self.out_tiles[slot, pl.ds(0, self.rows), pl.ds(0, self.w)] = self.tile(0, j) + (self.stage[:, cols].astype(F32) + far[:, cols].astype(F32))
            put(j, slot).start()

        for slot in range(min(2, self.tiles)):
            put(slot, slot).wait()

    def sent_locally(self):
        self.cp(0).wait_send()
        self.cp(1).wait_send()

    def sent(self):
        self.cp(2).wait_send()


def kernel_ab(q_width, hid, eqh, ekvh, posh, invh, swaph, dh2h, wg, wu, wd, wq, wkv, gfh, gah,
              n_o, da_o, db_o, u_o, wg_o, wu_o, wq_o, eq_o, h_o, g_o, e_o, n2_o, dres_o, home_o, dg_o, ux_o, ex_o, tab_o, g2_o, d2_o, d0_o, dc_o,
              rows, dh2_v, n2_v, res_v, dres_v, n_v, a_v, b_v, wg_v, wu_v, wd_v, wq_v, eq_v, p_v, rbuf, rbuf2, gains, dg_v, swap_v, pos_v, inv_v, gf_v, ga_v, gin, send, recv, local):
    dp, z, tx, peer = places()
    sub, dim = rows.shape
    tokens = 4 * sub
    width = eq_v.shape[0]
    dt = dim // 4
    ff = wg.shape[1]
    wide = min(1024, ff)
    tile = min(512, ff)
    dwide = min(1024, dim)
    dtile = min(512, dim)
    hs, cs = sub // 2, sub // 4
    net = Wires(send, recv, local)
    gain_in = [net.here(gfh, gf_v), net.here(gah, ga_v)]
    turn_in = [net.here(eqh, p_v.at[pl.ds(0, q_width), pl.ds(0, tokens)]), net.here(ekvh, p_v.at[pl.ds(q_width, width - q_width), pl.ds(0, tokens)]),
               net.here(swaph, swap_v), net.here(posh, pos_v), net.here(invh, inv_v)]
    entry_barrier([{"tx": peer[1]}, {"tx": peer[2]}, {"tx": peer[3]}, {"dp": 1 - dp}], z)

    pos = (dp, peer[1], peer[2])
    far_first = (2, 3, 1)
    g_id, h_id, e_id, d_id, o_id, u_id, x_id = (net.take(4), net.take(4), net.take(4), net.take(4), net.take(4), net.take(12), net.take(24))
    u_v = wg_v.at[pl.ds(0, tokens), :]
    e_v = wg_v.at[pl.ds(tokens, tokens), :]

    def g_cp(k):
        return net.copy(gin, gains.at[:, pl.ds(k * dt, dt)], g_id + k, g_id + k, tx=peer[k])

    def h_cp(k):
        return net.copy(hid.at[ds(peer[k] * sub, sub), :], rows.at[:, pl.ds(k * dt, dt)], h_id + k, h_id + k, tx=peer[k])

    def e_cp(k, block):
        return net.copy(p_v.at[pl.ds(0, width), ds(peer[k] * sub, sub)], eq_v.at[:, ds(block * sub, sub)], e_id + k, e_id + k, tx=peer[k])

    def d_cp(k):
        return net.copy(dh2h.at[ds(peer[k] * sub, sub), :], dh2_v.at[:, pl.ds(k * dt, dt)], d_id + k, d_id + k, tx=peer[k])

    def o_cp(k, block):
        return net.copy(res_v.at[:, pl.ds(k * dt, dt)], home_o.at[ds(block * sub, sub), :], o_id + k, o_id + k, tx=peer[k])

    def ux_cp(k, b):
        view = ds(b * sub, sub)
        cols = pl.ds(0, ff - ff // 4)
        src = ux_o.at[1, view, :] if k == 3 else wg_v.at[view, cols]
        i = u_id + (k - 1) * 4 + b
        return net.copy(src, ux_o.at[k - 1, view, :], i, i, tx=peer[1] if k == 3 else peer[k])

    def ex_cp(k, b, half):
        i = x_id + half * 12 + (k - 1) * 4 + b
        view = ds(b * sub + half * hs, hs)
        return net.copy(wg_v.at[ds(tokens + b * sub + half * hs, hs), pl.ds(k * dt, dt)], ex_o.at[k - 1, view, :], i, i, tx=peer[k])

    gate = WeightGather(net, wg, wg_v, pos, True, 2)
    up = WeightGather(net, wu, wu_v, pos, True, 2)
    down = WeightGather(net, wd, wd_v, pos, False, 4, 1)
    q_w = WeightGather(net, wq, wq_v.at[pl.ds(0, q_width), :], pos, False, 1)
    kv_w = WeightGather(net, wkv, wq_v.at[pl.ds(q_width, width - q_width), :], pos, False, 1)
    ag = LineGather(net, n_v, sub, z)
    rsc = LineScatter(net, p_v, rbuf, sub, z)
    rs2 = [LineScatter(net, n_v, rbuf2, sub, z, c * cs, cs) for c in range(4)]
    ag2 = [LineGather(net, e_v, sub, z, c * cs, cs) for c in range(4)]

    for k in far_first:
        h_cp(k).start()
    for c in gain_in:
        c.wait()
    gin[...] = jnp.broadcast_to(gf_v[...].astype(F32), gin.shape)
    gin[1:2, :] = ga_v[...].astype(F32)
    g_own = net.here(gin, gains.at[:, pl.ds(0, dt)])
    h_own = net.here(hid.at[ds(tx * sub, sub), :], rows.at[:, pl.ds(0, dt)])
    for w in (q_w, kv_w, gate, up, down):
        w.start_local()
    for k in far_first:
        g_cp(k).start()
    for c in turn_in:
        c.wait()

    @pl.loop(0, tokens // 128)
    def _(i):
        part = 128
        cos_c, sin_c = ds(i * part, part), ds(tokens + i * part, part)
        q_r, kv_r = pl.ds(0, 128), pl.ds(128, 128)
        angles = inv_v[...] * pos_v[:, cos_c].astype(F32)
        dres_v[q_r, sin_c] = jnp.sin(angles)
        dres_v[q_r, cos_c] = jnp.cos(angles)

        @pl.when(z < 2)
        def _():
            dres_v[kv_r, cos_c] = dres_v[q_r, cos_c]
            dres_v[kv_r, sin_c] = dres_v[q_r, sin_c]

        @pl.when(z >= 2)
        def _():
            dres_v[kv_r, cos_c] = jnp.ones((128, part), F32)
            dres_v[kv_r, sin_c] = jnp.zeros((128, part), F32)

    tab_out = net.here(dres_v.at[pl.ds(0, 256), pl.ds(0, 2 * tokens)], tab_o)
    turn(p_v, width, q_width, tokens, dres_v, swap_v, True)
    for k in far_first:
        e_cp(k, tx).start()
    e_own = net.here(p_v.at[pl.ds(0, width), ds(tx * sub, sub)], eq_v.at[:, ds(tx * sub, sub)])
    for w in (q_w, kv_w, gate, up, down):
        w.start_y()
    for k in far_first:
        d_cp(k).start()
    d_own = net.here(dh2h.at[ds(tx * sub, sub), :], dh2_v.at[:, pl.ds(0, dt)])

    for k in far_first:
        g_cp(k).wait_recv()
        h_cp(k).wait_recv()
    g_own.wait()
    h_own.wait()

    @pl.loop(0, sub // 16)
    def _(r):
        x = rows[ds(r * 16, 16), :].astype(F32)
        inv = lax.rsqrt(jnp.sum(x * x, axis=1, keepdims=True) / dim + NORM_EPS)
        n_v[ds(z * sub + r * 16, 16), :] = (x * inv * gains[0:1, :]).astype(BF16)

    ag.start()
    outs = [net.here(rows, h_o), net.here(gains, g_o)]
    for k in far_first:
        e_cp(k, peer[k]).wait_recv()
    e_own.wait()
    ag.step1()
    for w in (q_w, kv_w):
        w.y_event(0)
    for w in (q_w, kv_w):
        w.x_event(0)
    for w in (q_w, kv_w):
        w.finish_local()
        w.finish(0)
    for k in far_first:
        e_cp(k, tx).wait_send()

    def n2_block(b):
        @pl.loop(0, dim // dtile)
        def _(j):
            cols = ds(j * dtile, dtile)
            p_v[ds(b * sub, sub), cols] = dot(eq_v[:, ds(b * sub, sub)], wq_v[:, cols], ROWS_ROWS).astype(BF16)

    @pl.loop(0, 4)
    def _(i):
        n2_block(pick(3 - i, z))
        for step in range(3):
            pl.when(i == step)(lambda step=step: rsc.send_end(2 - step))
        pl.when(i == 0)(lambda: gate.y_event(0))

    wide = ff // 2

    def gate_part(b, c):
        cols = pl.ds(c * wide, wide)
        a_v[ds(b * sub, sub), cols] = dot(n_v[ds(b * sub, sub), :], wg_v[:, cols]).astype(BF16)

    def up_part(b, c):
        cols = pl.ds(c * wide, wide)
        bb = dot(n_v[ds(b * sub, sub), :], wu_v[:, cols]).astype(BF16)
        b_v[ds(b * sub, sub), cols] = bb
        aa = a_v[ds(b * sub, sub), cols].astype(F32)
        wg_v[ds(b * sub, sub), cols] = (aa * jax.nn.sigmoid(aa) * bb.astype(F32)).astype(BF16)

    def down_part(b, j):
        cols = pl.ds(j * (dim // 2), dim // 2)
        n_v[ds(b * sub, sub), cols] = dot(wg_v[ds(b * sub, sub), :], wd_v[:, cols]).astype(BF16)

    outs += [net.here(wq_v, wq_o), net.here(eq_v, eq_o)]
    gate.finish_local()
    gate.y_event(1)
    ag.step2()
    ag.step3_mid()
    gate.x_event(0)
    gate.finish(0)

    @pl.loop(0, 3)
    def _(i):
        gate_part(pick(i, z), 0)

    up.y_event(0)
    gate.x_event(1)
    rsc.send_mid(2)
    gate.finish(1)
    wg_out = net.here(wg_v, wg_o)

    @pl.loop(0, 3)
    def _(i):
        gate_part(pick(i, z), 1)

    up.finish_local()
    up.y_event(1)
    up.x_event(0)
    up.finish(0)
    ag.step3_end()

    @pl.loop(0, 2)
    def _(c):
        cols = ds(c * wide, wide)
        b = pick(3, z)
        a_v[ds(b * sub, sub), cols] = dot(n_v[ds(b * sub, sub), :], wg_v[:, cols]).astype(BF16)

    wg_out.wait()
    n_out = net.here(n_v, n_o)

    @pl.loop(0, 4)
    def _(i):
        pl.when(i == 1)(lambda: down.y_event(0))
        pl.when(i == 2)(lambda: down.y_event(1))
        pl.when(i == 3)(lambda: up.x_event(1))
        up_part(pick(i, z), 0)

    def up_events_1():
        rsc.send_mid(1)
        rsc.send_mid(0)
        down.x_event(0)

    def up_events_2():
        down.y_event(2)

    def up_events_3():
        down.y_event(3)
        down.x_event(1)

    up.finish(1)
    outs.append(net.here(wu_v, wu_o))

    @pl.loop(0, 4)
    def _(i):
        pl.when(i == 1)(up_events_1)
        pl.when(i == 2)(up_events_2)
        pl.when(i == 3)(up_events_3)
        b = pick(i, z)
        up_part(b, 1)
        ux_cp(2, b).start()
        ux_cp(1, b).start()

    outs.append(net.here(u_v, u_o))
    ag.drain()
    gate.drain()
    n_out.wait()
    down.finish_local()

    @pl.loop(0, 4)
    def _(i):
        pl.when(i == 2)(lambda: down.x_event(2))
        pl.when(i == 3)(lambda: down.x_event(3))
        down_part(pick(3 - i, z), 0)

    for ch in range(4):
        down.finish(ch)

    @pl.loop(0, 4)
    def _(i):
        down_part(pick(3 - i, z), 1)
        for step in range(3):
            pl.when(i == step)(lambda step=step: rs2[0].send_end(2 - step))

    for c in (1, 2, 3):
        for i in (2, 1, 0):
            rs2[c].send_end(i)
    dg_v[...] = jnp.zeros_like(dg_v)
    step = 16

    def norm_chunk(c):
        @pl.loop(0, cs // step)
        def _(r):
            at = c * cs + r * step
            view, mine, far = ds(at, step), ds(z * sub + at, step), ds(4 * sub + at, step)

            def whole(part, got):
                right = jnp.where(z < 3, got[mine, :].astype(F32), 0.0)
                left = jnp.where(z > 0, got[far, :].astype(F32), 0.0)
                return part[mine, :].astype(F32) + right + left

            resid = (rows[view, :].astype(F32) + whole(n_v, rbuf2)).astype(BF16)
            dy = whole(p_v, rbuf)
            res_v[view, :] = resid
            x = resid.astype(F32)
            inv = lax.rsqrt(jnp.sum(x * x, axis=1, keepdims=True) / dim + NORM_EPS)
            xhat = x * inv
            gain = gains[1:2, :]
            n2_v[view, :] = (xhat * gain).astype(BF16)
            part = dy * xhat
            dg_v[...] += part[:8] + part[8:]
            inner = jnp.sum(part * gain, axis=1, keepdims=True) / dim
            dres = dh2_v[view, :].astype(F32) + inv * (dy * gain) - xhat * (inv * inner)
            dres_v[view, pl.ds(0, dim)] = dres
            wg_v[ds(tokens + z * sub + at, step), :] = dres.astype(BF16)

    def spread(b, half):
        for k in far_first:
            ex_cp(k, b, half).start()

    def back_tile(b, j):
        view, cols = ds(b * sub, sub), ds(j * (ff // 4), ff // 4)
        du = dot(wg_v[ds(tokens + b * sub, sub), :], wd_v[ds(j * (ff // 4), ff // 4), :], NT_DIMS)
        aa = a_v[view, cols].astype(F32)
        bb = b_v[view, cols].astype(F32)
        sig = jax.nn.sigmoid(aa)
        a_v[view, cols] = (du * bb * sig * (1.0 + aa * (1.0 - sig))).astype(BF16)
        b_v[view, cols] = (du * aa * sig).astype(BF16)

    def scatter(i, c):
        return lambda: rs2[c].send_mid(i)

    def gathered(i, c):
        def go():
            ag2[c].take(i)
            pl.when(mid(z))(lambda: ag2[c].forward(i))
            if c % 2 == 1:
                spread(ag.slots[i], c // 2)
        return go

    def run(ops):
        def go():
            for op in ops:
                op()
        return go

    before_mid = (
        (scatter(2, 0), scatter(1, 0), scatter(0, 0)),
        (scatter(2, 1), gathered(1, 0), scatter(1, 1), scatter(0, 1)),
        (scatter(2, 2), scatter(1, 2), gathered(1, 1), scatter(0, 2), scatter(2, 3)),
        (scatter(1, 3), scatter(0, 3), gathered(1, 2), gathered(0, 0)))
    before_end = ((), (gathered(0, 0), gathered(1, 0)), (gathered(0, 1), gathered(1, 1)), (gathered(0, 2),))
    after_mid = {0: (gathered(0, 1),), 1: (gathered(2, 0),), 2: (gathered(0, 2),), 3: (gathered(1, 3),), 5: (gathered(0, 3),), 7: (gathered(2, 1),),
                 10: (gathered(2, 2),), 12: (gathered(2, 3),)}
    after_end = {3: (gathered(1, 2),), 4: (gathered(0, 3),), 7: (gathered(2, 0),), 8: (gathered(1, 3),),
                 12: (gathered(2, 1), gathered(2, 2), gathered(2, 3))}

    for c in range(4):
        pl.when(mid(z))(run(before_mid[c]))
        pl.when(end(z))(run(before_end[c]))
        if c == 0:
            rsc.finish()
            for k in far_first:
                d_cp(k).wait_recv()
            d_own.wait()
            tab_out.wait()
        rs2[c].finish()
        norm_chunk(c)
        ag2[c].start()
        if c % 2 == 1:
            spread(z, c // 2)

    for k in far_first:
        o_cp(k, tx).start()
    outs += [net.here(res_v.at[:, pl.ds(0, dt)], home_o.at[ds(tx * sub, sub), :]), net.here(n2_v, n2_o), net.here(dres_v.at[pl.ds(0, sub), pl.ds(0, dim)], dres_o), net.here(dg_v, dg_o)]
    rsc.drain()
    for c in range(4):
        rs2[c].drain()
    n_in = net.here(n_o, p_v)
    middle = (z + 1) // 2 % 2

    def u_forward():
        for b in range(4):
            ux_cp(2, b).wait_recv()
            ux_cp(3, b).start()

    @pl.loop(0, 16)
    def _(t):
        for at, ops in after_mid.items():
            pl.when(jnp.logical_and(t == at, mid(z)))(run(ops))
        for at, ops in after_end.items():
            pl.when(jnp.logical_and(t == at, end(z)))(run(ops))
        pl.when(t == 8)(u_forward)
        i = t // 4
        inner = (i + 1) // 2 % 2
        back_tile(pick(i + middle * inner * (3 - 2 * i), z), t % 4)

    outs.append(net.here(e_v, e_o))
    outs += [net.here(a_v, da_o), net.here(b_v, db_o)]

    last = pl.ds(ff - ff // 4, ff // 4)

    def down_tile(k, j):
        return dot(wg_v[pl.ds(0, tokens), last], wg_v[pl.ds(tokens, tokens), pl.ds(k * dt, dt)], ROWS_ROWS)

    def gate_tile(k, j):
        return dot(p_v[:, pl.ds(k * dt, dt)], a_v[:, ds(j * (ff // 4), ff // 4)], ROWS_ROWS)

    quarter = [rbuf.at[pl.ds(0, ff // 4), pl.ds(i * dt, dt)] for i in range(4)]
    part_d = GradReduce(net, peer, down_tile, 1, quarter[0], quarter[1], quarter[2], quarter[3], d2_o, d0_o, None, dc_o, None)
    part_g = GradReduce(net, peer, gate_tile, 4, n_v.at[pl.ds(0, dt), :], None, None, None, g2_o, None, None, wg_o, None)
    n_in.wait()
    part_d.step3()
    part_d.step1()
    part_g.step3()
    part_d.step2()
    outs.append(net.here(quarter[2], dc_o))
    for k in far_first:
        o_cp(k, peer[k]).wait_recv()
        for b in range(4):
            ex_cp(k, b, 0).wait_recv()
            ex_cp(k, b, 1).wait_recv()
    for b in range(4):
        ux_cp(1, b).wait_recv()
        ux_cp(3, b).wait_recv()
    for c in outs:
        c.wait()
    for k in far_first:
        g_cp(k).wait_send()
        h_cp(k).wait_send()
        d_cp(k).wait_send()
        o_cp(k, tx).wait_send()
        for b in range(4):
            ux_cp(k, b).wait_send()
            ex_cp(k, b, 0).wait_send()
            ex_cp(k, b, 1).wait_send()
    for w in (q_w, kv_w, up, down):
        w.drain()
    for c in range(4):
        ag2[c].drain()
    part_d.cp(1).wait_recv()
    part_d.sent_locally()
    part_g.cp(0).wait_recv()
    part_g.cp(0).wait_send()


def call_ab(hid, eqh, ekvh, pos, inv, swap, dh2h, wg, wu, wd, wq, wkv, gf, ga):
    tokens, dt = hid.shape
    sub, dim, ff, q_width = tokens // 4, dt * 4, wg.shape[1], wq.shape[0]
    width = q_width + wkv.shape[0]
    s = jax.ShapeDtypeStruct
    tok_ff, tok_d, row = s((tokens, ff), BF16), s((tokens, dim), BF16), s((sub, dim), BF16)
    shapes = (tok_d, tok_ff, tok_ff, tok_ff, s((dim, ff), BF16), s((dim, ff), BF16), s((width, dim), BF16), s((width, tokens), BF16),
              row, s((8, dim), F32), tok_d, row, s((sub, dim), F32), s((tokens, dt), BF16), s((8, dim), F32),
              s((3, tokens, ff - ff // 4), BF16), s((3, tokens, dt), BF16), s((256, 2 * tokens), F32), s((dt, ff), BF16)) + (s((ff // 4, dt), BF16),) * 3
    vrow, vtok, vff = VMEM((sub, dim), BF16), VMEM((tokens, dim), BF16), VMEM((tokens, ff), BF16)
    return pl.pallas_call(
        functools.partial(kernel_ab, q_width), out_shape=shapes, in_specs=[ANY] * 14, out_specs=[ANY] * len(shapes),
        scratch_shapes=[
            vrow, vrow, vrow, vrow, VMEM((max(sub, 256), max(dim, 2 * tokens)), F32), vtok, vff, vff, VMEM((dim, ff), BF16), VMEM((dim, ff), BF16), VMEM((ff, dim), BF16),
            VMEM((width, dim), BF16), VMEM((width, tokens), BF16), vtok, VMEM((5 * sub, dim), BF16), VMEM((5 * sub, dim), BF16),
            VMEM((8, dim), F32), VMEM((8, dim), F32), VMEM((128, 128), BF16), VMEM((1, tokens), jnp.int32), VMEM((128, 128), F32),
            VMEM((1, dt), BF16), VMEM((1, dt), BF16), VMEM((8, dt), F32),
            pltpu.SemaphoreType.DMA((180,)), pltpu.SemaphoreType.DMA((180,)), pltpu.SemaphoreType.DMA((48,))],
        compiler_params=pltpu.CompilerParams(collective_id=0, has_side_effects=True, vmem_limit_bytes=VMEM_LIMIT),
        cost_estimate=pl.CostEstimate(flops=20 * tokens * dim * ff, bytes_accessed=100000000, transcendentals=0), name="phase_ab",
    )(hid, eqh, ekvh, pos, inv, swap, dh2h, wg, wu, wd, wq, wkv, gf, ga)


def kernel_c(q_width, da_h, db_h, wg_h, wu_h, n_h, u_h, ux_h, e_h, ex_h, n2_h, eq_h, wq_h, h_h, dres_h, g_h, dga_h, tabh, swaph, g2, d0, dc,
             wgo, wgy, wuo, wuy, wdo, wqo, wqy, wvo, wvy, q_o, kv_o, dh_o, dg_o, g0, u2, u0, q2, q0, v2, v0, qx, dy,
             wg_v, wu_v, da_v, db_v, n_v, p_v, rbuf, n2_v, st3, st1, cross_g, cross_u, stage, tiles_v, dres_v, wq_v, eq_v,
             gains, dg_v, dgr, dgz, tab_v, swap_v, send, recv, local):
    dp, z, tx, peer = places()
    tokens, ff = da_v.shape
    sub, dim = dres_v.shape
    dt = dim // 4
    width = eq_v.shape[0]
    tile = ff // 4
    dtile = min(512, dim)
    qt = min(256, tile)
    far_first = (2, 3, 1)
    net = Wires(send, recv, local)
    n2_in = net.here(n2_h, n2_v.at[ds(z * sub, sub), :])
    first = [net.here(n_h, n_v), net.here(da_h, da_v)]
    second = [net.here(db_h, db_v), net.here(wg_h, wg_v), net.here(wu_h, wu_v)]
    third = [net.here(wq_h, wq_v), net.here(eq_h, eq_v), net.here(dres_h, dres_v), net.here(g_h, gains),
             net.here(dga_h, dg_v.at[pl.ds(8, 8), :]), net.here(tabh, tab_v), net.here(swaph, swap_v)]
    sem = pltpu.get_barrier_semaphore()
    zs = tuple((z + i) % 4 for i in range(4))
    for i in (1, 2, 3):
        pl.semaphore_signal(sem, inc=1, device_id={"tx": peer[i]}, device_id_type=MESH)
        pl.semaphore_signal(sem, inc=1, device_id={"ty": zs[i]}, device_id_type=MESH)
    pl.semaphore_wait(sem, 6)
    rsc = LineScatter(net, p_v, rbuf, sub, z)
    ag = LineGather(net, n2_v, sub, z)
    q_id, h_id, t_id, z_id = net.take(4), net.take(4), net.take(4), net.take(4)

    def grad_tile(lhs, rhs, w):
        def go(k, j):
            cols = pl.ds(j * w, w) if isinstance(j, int) else ds(j * w, w)
            return dot(lhs[:, pl.ds(k * dt, dt)], rhs[:, cols], ROWS_ROWS)
        return go

    gate = GradReduce(net, peer, grad_tile(n_v, da_v, tile), ff // tile, st3, st1, cross_g, stage, g2, g0, wgy, wgo, tiles_v)
    up = GradReduce(net, peer, grad_tile(n_v, db_v, tile), ff // tile, st3, st1, cross_u, stage, u2, u0, wuy, wuo, tiles_v)
    d_id = net.take(1)

    def dy_cp():
        return net.copy(dc, dy, d_id, d_id, tx=peer[2])

    dy_cp().start()

    def head_grad(first, rows, got2, got0, got_y, out):
        corner = [da_v.at[pl.ds(first, rows), pl.ds(c * dt, dt)] for c in range(4)]

        def tile_of(k, j):
            return dot(eq_v[pl.ds(first, rows), :], n2_v[:, ds(k * dt + j * qt, qt)])

        return GradReduce(net, peer, tile_of, dt // qt, *corner, got2, got0, got_y, out, tiles_v)

    heads = (head_grad(0, q_width, q2, q0, wqy, wqo), head_grad(q_width, width - q_width, v2, v0, wvy, wvo))

    def dn_block(b):
        rows = ds(b * sub, sub)

        @pl.loop(0, dim // dtile)
        def _(j):
            wr = ds(j * dtile, dtile)
            p_v[rows, wr] = (dot(da_v[rows, :], wg_v[wr, :], NT_DIMS) + dot(db_v[rows, :], wu_v[wr, :], NT_DIMS)).astype(BF16)

    n2_in.wait()
    ag.start()
    for c in first:
        c.wait()
    gate.step2(True)
    gate.send()
    gate.step1()
    for c in second:
        c.wait()

    @pl.loop(0, 4)
    def _(i):
        @pl.when(i == 1)
        def _():
            up.step3()
            gate.cp(1).wait_send()
            up.step1()
            ag.step1()

        dn_block(pick(3 - i, z))
        for step in range(3):
            pl.when(i == step)(lambda step=step: rsc.send_end(2 - step))

    up.step2()
    up.send()
    rsc.send_mid(2)
    ag.step2()
    ag.step3_mid()
    up.sent_locally()
    h_in = net.here(h_h, st3.at[pl.ds(0, sub), :])
    gate.step0(st1)
    gate.sent()

    n_tiles = ff // tile
    e_in = [net.here(e_h.at[:, pl.ds(0, dt)], wu_v.at[pl.ds(0, tokens), pl.ds(0, dt)])]
    for k in (1, 2, 3):
        e_in.append(net.here(ex_h.at[k - 1], wu_v.at[pl.ds(0, tokens), pl.ds(k * dt, dt)]))

    def u_place(j, k):
        return wg_v.at[pl.ds((j % 2) * tokens, tokens), pl.ds(k * tile, tile)]

    def u_load(j):
        cols = pl.ds(j * tile, tile)
        if j == n_tiles - 1:
            return [net.here(u_h.at[:, cols], u_place(j, 0)), net.here(d0, stage.at[pl.ds(0, tile), pl.ds(0, dt)]), net.here(dy, stage.at[pl.ds(0, tile), pl.ds(dt, dt)])]
        return [net.here(u_h.at[:, cols] if k == 0 else ux_h.at[k - 1, :, cols], u_place(j, k)) for k in range(4)]

    def down_tile(j, slot, loads):
        for c in loads:
            c.wait()
        acc = None
        if j == n_tiles - 1:
            acc = stage[pl.ds(0, tile), pl.ds(0, dt)].astype(F32) + stage[pl.ds(0, tile), pl.ds(dt, dt)].astype(F32)
        for k in range(1 if j == n_tiles - 1 else 4):
            part = dot(u_place(j, k)[...], wu_v[pl.ds(0, tokens), pl.ds(k * dt, dt)], ROWS_ROWS)
            acc = part if acc is None else acc + part
        tiles_v[slot, pl.ds(0, tile), pl.ds(0, dt)] = acc
        return net.here(tiles_v.at[slot, pl.ds(0, tile), pl.ds(0, dt)], wdo.at[pl.ds(j * tile, tile), :])

    loads = {0: u_load(0), 1: u_load(1)}
    rsc.send_mid(1)
    rsc.send_mid(0)
    for c in e_in:
        c.wait()
    done = [down_tile(0, 0, loads[0]), down_tile(1, 1, loads[1])]
    loads = {2: u_load(2)}
    for c in third:
        c.wait()
    ag.step3_end()

    @pl.loop(0, width // qt)
    def _(j):
        wu_v[ds(tokens + j * qt, qt), pl.ds(0, tokens)] = dot(wq_v[ds(j * qt, qt), :], n2_v[...], NT_DIMS).astype(BF16)

    def q_cp(k, block):
        return net.copy(wu_v.at[pl.ds(tokens, width), ds(peer[k] * sub, sub)], qx.at[:, ds(block * sub, sub)], q_id + k, q_id + k, tx=peer[k])

    for k in far_first:
        q_cp(k, tx).start()
    q_own = net.here(wu_v.at[pl.ds(tokens, width), ds(tx * sub, sub)], qx.at[:, ds(tx * sub, sub)])
    for c in done:
        c.wait()
    for part in heads:
        part.step3()
        part.step1()
    dy_cp().wait_recv()
    loads[3] = u_load(3)
    for part in heads:
        part.step2()
        part.send()
    done = [down_tile(2, 0, loads[2]), down_tile(3, 1, loads[3])]
    h_in.wait()
    rsc.finish()
    dg_v[pl.ds(0, 8), :] = jnp.zeros((8, dim), F32)
    step = 16

    @pl.loop(0, sub // step)
    def _(r):
        view, mine, far = ds(r * step, step), ds(z * sub + r * step, step), ds(4 * sub + r * step, step)
        right = jnp.where(z < 3, rbuf[mine, :].astype(F32), 0.0)
        left = jnp.where(z > 0, rbuf[far, :].astype(F32), 0.0)
        dy = p_v[mine, :].astype(F32) + right + left
        x = st3[view, :].astype(F32)
        inv = lax.rsqrt(jnp.sum(x * x, axis=1, keepdims=True) / dim + NORM_EPS)
        xhat = x * inv
        gain = gains[0:1, :]
        part = dy * xhat
        dg_v[pl.ds(0, 8), :] += part[:8] + part[8:]
        inner = jnp.sum(part * gain, axis=1, keepdims=True) / dim
        st1[view, :] = (dres_v[view, :] + inv * (dy * gain) - xhat * (inv * inner)).astype(BF16)

    def h_cp(k, block):
        return net.copy(st1.at[pl.ds(0, sub), pl.ds(k * dt, dt)], dh_o.at[ds(block * sub, sub), :], h_id + k, h_id + k, tx=peer[k])

    def t_cp(k):
        return net.copy(dg_v.at[:, pl.ds(k * dt, dt)], dgr.at[k], t_id + k, t_id + k, tx=peer[k])

    def z_cp(i):
        return net.copy(dgr.at[0], dgz.at[i], z_id + i, z_id + i, ty=zs[i])

    for k in far_first:
        t_cp(k).start()
    for k in far_first:
        h_cp(k, tx).start()
    h_own = net.here(st1.at[pl.ds(0, sub), pl.ds(0, dt)], dh_o.at[ds(tx * sub, sub), :])
    up.sent()
    for c in done:
        c.wait()
    up.step0(cross_g)
    for k in far_first:
        q_cp(k, peer[k]).wait_recv()
    q_own.wait()
    turned = wu_v.at[pl.ds(tokens, width), pl.ds(tokens, tokens)]
    net.here(qx, turned).wait()
    turn(turned, width, q_width, tokens, tab_v, swap_v, False)
    q_out = net.here(wu_v.at[pl.ds(tokens, q_width), pl.ds(tokens, tokens)], q_o)
    kv_out = net.here(wu_v.at[pl.ds(tokens + q_width, width - q_width), pl.ds(tokens, tokens)], kv_o)
    heads[0].step0(cross_g.at[pl.ds(0, q_width), pl.ds(0, dt)])
    heads[1].step0(cross_g.at[pl.ds(0, width - q_width), pl.ds(dt, dt)])
    for k in far_first:
        t_cp(k).wait_recv()
    dgr[0] = dg_v[:, pl.ds(0, dt)] + dgr[1] + dgr[2] + dgr[3]
    for i in (1, 2, 3):
        z_cp(i).start()
    for i in (1, 2, 3):
        z_cp(i).wait_recv()
    dgz[0] = dgr[0] + dgz[1] + dgz[2] + dgz[3]
    dg_out = net.here(dgz.at[0], dg_o)
    for k in far_first:
        h_cp(k, peer[k]).wait_recv()
    for c in (q_out, kv_out, dg_out, h_own):
        c.wait()
    dy_cp().wait_send()
    for part in heads:
        part.sent_locally()
        part.sent()
    for k in far_first:
        q_cp(k, tx).wait_send()
        h_cp(k, tx).wait_send()
        t_cp(k).wait_send()
        z_cp(k).wait_send()
    ag.drain()
    rsc.drain()


def call_c(q_width, *args):
    tokens, ff = args[0].shape
    sub, dim = args[9].shape
    dt, width = dim // 4, args[10].shape[0]
    rest = width - q_width
    tile = ff // 4
    s = jax.ShapeDtypeStruct
    wf, wb = s((dt, ff), F32), s((dt, ff), BF16)
    qf, qb, vf, vb = s((q_width, dt), F32), s((q_width, dt), BF16), s((rest, dt), F32), s((rest, dt), BF16)
    shapes = (wf, wb, wf, wb, s((ff, dt), F32), qf, qb, vf, vb, s((q_width, tokens), BF16), s((rest, tokens), BF16), s((tokens, dt), BF16), s((16, dt), F32),
              wb, wb, wb, qb, qb, vb, vb, s((width, tokens), BF16), s((tile, dt), BF16))
    return pl.pallas_call(
        functools.partial(kernel_c, q_width), out_shape=shapes, in_specs=[ANY] * len(args), out_specs=[ANY] * len(shapes),
        scratch_shapes=[
            VMEM((dim, ff), BF16), VMEM((dim, ff), BF16), VMEM((tokens, ff), BF16), VMEM((tokens, ff), BF16), VMEM((tokens, dim), BF16),
            VMEM((tokens, dim), BF16), VMEM((5 * sub, dim), BF16), VMEM((tokens, dim), BF16),
            VMEM((dt, ff), BF16), VMEM((dt, ff), BF16), VMEM((dt, ff), BF16), VMEM((dt, ff), BF16), VMEM((dt, ff), BF16),
            VMEM((2, max(dt, tile), max(dt, tile)), F32), VMEM((sub, dim), F32), VMEM((width, dim), BF16), VMEM((width, tokens), BF16),
            VMEM((8, dim), F32), VMEM((16, dim), F32), VMEM((4, 16, dt), F32), VMEM((4, 16, dt), F32), VMEM((256, 2 * tokens), F32), VMEM((128, 128), BF16),
            pltpu.SemaphoreType.DMA((48,)), pltpu.SemaphoreType.DMA((48,)), pltpu.SemaphoreType.DMA((72,))],
        compiler_params=pltpu.CompilerParams(collective_id=2, has_side_effects=True, vmem_limit_bytes=VMEM_LIMIT),
        cost_estimate=pl.CostEstimate(flops=20 * tokens * dim * ff, bytes_accessed=100000000, transcendentals=0), name="phase_c",
    )(*args)


def kernel_out(pieces, n, *refs):
    ins, outs, bufs = refs[:n], refs[n + 1:2 * n + 1], refs[2 * n + 3:3 * n + 3]
    gains, gain_a, gain_b = refs[n], refs[2 * n + 1], refs[2 * n + 2]
    read, write = refs[3 * n + 3:]

    def part(ref, i, c):
        rows = ref.shape[0] // pieces[i]
        return ref.at[pl.ds(c * rows, rows), :]

    jobs = [(i, c) for i in range(n) for c in range(pieces[i])]
    get = [pltpu.make_async_copy(part(ins[i], i, c), part(bufs[i], i, c), read.at[m]) for m, (i, c) in enumerate(jobs)]
    put = [pltpu.make_async_copy(part(bufs[i], i, c), part(outs[i], i, c), write.at[m]) for m, (i, c) in enumerate(jobs)]
    for g in get:
        g.start()
    gain_a[...] = jnp.sum(gains[pl.ds(0, 8), :], axis=0, keepdims=True)
    gain_b[...] = jnp.sum(gains[pl.ds(8, 8), :], axis=0, keepdims=True)
    for g, p in zip(get, put):
        g.wait()
        p.start()
    for p in put:
        p.wait()


def call_out(results, gains):
    n = len(results)
    pieces = tuple(max(1, x.size * x.dtype.itemsize // 2**20) for x in results)
    row = jax.ShapeDtypeStruct((1, gains.shape[1]), F32)
    whole = pl.BlockSpec(memory_space=pltpu.VMEM)
    return pl.pallas_call(
        functools.partial(kernel_out, pieces, n), out_shape=tuple(jax.ShapeDtypeStruct(x.shape, x.dtype) for x in results) + (row, row),
        in_specs=[ANY] * n + [whole], out_specs=[ANY] * n + [whole, whole],
        scratch_shapes=[VMEM(x.shape, x.dtype) for x in results] + [pltpu.SemaphoreType.DMA((sum(pieces),))] * 2,
        compiler_params=pltpu.CompilerParams(vmem_limit_bytes=VMEM_LIMIT),
        cost_estimate=pl.CostEstimate(flops=1000000, bytes_accessed=35000000, transcendentals=0), name="results",
    )(*results, gains)


def solution(mesh):
    def local_step(hidden, positions, g_ffn, w_gate, w_up, w_down, g_attn, w_q, w_kv, grad_h2, grad_q, grad_kv):
        tokens, dt = hidden.shape
        q_heads, head_dim = w_q.shape[1:]
        q_width = q_heads * head_dim

        lane = np.arange(128)
        inv_freq = ROPE_BASE ** (-(lane % head_dim // 2 * 2).astype(np.float32) / head_dim)
        inv_freq = jnp.asarray(np.tile(inv_freq.astype(np.float32)[:, None], (1, 128)))
        swap = np.zeros((128, 128), np.float32)
        swap[lane, lane ^ 1] = np.where(lane % 2 == 0, -1.0, 1.0)
        swap = jnp.asarray(swap, BF16)

        def heads_first(x):
            return x.transpose(1, 2, 0).reshape(-1, x.shape[0])

        def heads_last(x):
            return x.reshape(-1, head_dim, x.shape[1]).transpose(2, 0, 1)

        (normed_all, grad_gate, grad_up, u_all, gate_w, up_w, w_qkv, back_all, h_rows, gains, res_all, normed2, grad_res, resid_out, gattn8,
         u_other, e_other, table, wg_two, _, wd_zero, wd_cross) = call_ab(
             hidden, heads_first(grad_q), heads_first(grad_kv), positions.reshape(1, tokens), inv_freq, swap, grad_h2,
             w_gate, w_up, w_down, heads_first(w_q), heads_first(w_kv), g_ffn.reshape(1, dt), g_attn.reshape(1, dt))
        (grad_wgate, _, grad_wup, _, grad_wdown, grad_wq, _, grad_wkv, _, q_out, kv_out, grad_hidden, gain_grads, *_) = call_c(
            q_width, grad_gate, grad_up, gate_w, up_w, normed_all, u_all, u_other, res_all, e_other, normed2, back_all, w_qkv,
            h_rows, grad_res, gains, gattn8, table, swap, wg_two, wd_zero, wd_cross)
        (resid_out, grad_wgate, grad_wup, grad_wdown, grad_wq, grad_wkv, q_out, kv_out, grad_hidden, grad_gffn, grad_gattn) = call_out(
            (resid_out, grad_wgate, grad_wup, grad_wdown, grad_wq, grad_wkv, q_out, kv_out, grad_hidden), gain_grads)
        q_out, kv_out, grad_wq, grad_wkv = (heads_last(x) for x in (q_out, kv_out, grad_wq, grad_wkv))
        grad_gffn, grad_gattn = grad_gffn[0], grad_gattn[0]
        return (resid_out, q_out, kv_out, grad_hidden, grad_gffn, grad_gattn, grad_wgate, grad_wup, grad_wdown, grad_wq, grad_wkv)

    row_spec = P(("dp", "ty"), "tx")
    head_spec = P(("dp", "tx"), "ty", None)
    in_specs = (row_spec, P(("dp", "tx")), P("tx"), P("tx", "ty"), P("tx", "ty"), P("ty", "tx"), P("tx"), P("tx", "ty", None), P("tx", "ty", None), row_spec, head_spec, head_spec)
    out_specs = (row_spec, head_spec, head_spec, row_spec, P(("dp", "tx")), P(("dp", "tx")), P(("dp", "tx"), "ty"), P(("dp", "tx"), "ty"), P(("dp", "ty"), "tx"), head_spec, head_spec)
    return jax.shard_map(local_step, mesh=mesh, in_specs=in_specs, out_specs=out_specs, check_vma=False)
```

```python
import functools

import jax
import jax.numpy as jnp
import numpy as np
from jax import lax
from jax.experimental import pallas as pl
from jax.experimental.pallas import tpu as pltpu
from jax.sharding import PartitionSpec as P

NORM_EPS = 1e-5
ROPE_BASE = 10000.0
F32 = jnp.float32
BF16 = jnp.bfloat16


def dot(a, b, dims=(((1,), (0,)), ((), ()))):
    return lax.dot_general(a, b, dims, preferred_element_type=F32)


MESH = pl.DeviceIdType.MESH
ANY = pl.BlockSpec(memory_space=pl.ANY)
VMEM = pltpu.VMEM
NT_DIMS = (((1,), (1,)), ((), ()))
VMEM_LIMIT = 67000000


def ds(start, size, align=None):
    if isinstance(start, int):
        return pl.ds(start, size)
    return pl.ds(pl.multiple_of(start, align or size), size)


def mid(z):
    return jnp.logical_and(z > 0, z < 3)


def end(z):
    return jnp.logical_or(z == 0, z == 3)


def slots(z):
    return (z + 1 - 2 * (z % 2), 2 - z // 2, 3 - 3 * (z // 2))


def turn(x_ref, width, q_width, tokens, table_ref, swap_ref, back):
    step = min(256, tokens)

    @pl.loop(0, tokens // step)
    def _(r):
        cols = ds(r * step, step)
        for g in range(width // 128):
            rows = pl.ds(g * 128, 128)
            base = pl.ds(0 if g * 128 < q_width else 128, 128)
            x = x_ref[rows, cols]
            main = x.astype(F32) * table_ref[base, cols]
            side = dot(swap_ref[...], x) * table_ref[base, ds(tokens + r * step, step)]
            x_ref[rows, cols] = (main - side if back else main + side).astype(BF16)


def pick(i, z):
    s1, s2, s3 = slots(z)
    first, last = (3 - i) // 3, (i // 2) * (i % 2)
    return z * first + s1 * ((i % 2) * (1 - i // 2)) + s2 * ((i // 2) * (1 - i % 2)) + s3 * last


class Wires:
    def __init__(self, send, recv, local):
        self.send, self.recv, self.local = send, recv, local
        self.n_remote = 0
        self.n_local = 0

    def take(self, n=1):
        base = self.n_remote
        self.n_remote += n
        assert self.n_remote <= self.send.shape[0]
        return base

    def copy(self, src, dst, si, ri, **dev):
        return pltpu.make_async_remote_copy(
            src_ref=src, dst_ref=dst, send_sem=self.send.at[si], recv_sem=self.recv.at[ri],
            device_id=dev, device_id_type=MESH)

    def here(self, src, dst):
        i = self.n_local
        self.n_local += 1
        assert i < self.local.shape[0]
        c = pltpu.make_async_copy(src, dst, self.local.at[i])
        c.start()
        return c


def entry_barrier(axes, z):
    sem = pltpu.get_barrier_semaphore()
    for dev in axes:
        pl.semaphore_signal(sem, inc=1, device_id=dev, device_id_type=MESH)

    @pl.when(z > 0)
    def _():
        pl.semaphore_signal(sem, inc=1, device_id={"ty": z - 1}, device_id_type=MESH)

    @pl.when(z < 3)
    def _():
        pl.semaphore_signal(sem, inc=1, device_id={"ty": z + 1}, device_id_type=MESH)

    @pl.when(mid(z))
    def _():
        pl.semaphore_wait(sem, len(axes) + 2)

    @pl.when(end(z))
    def _():
        pl.semaphore_wait(sem, len(axes) + 1)


class LineGather:
    def __init__(self, net, buf, rows, z, off=0, part=None):
        self.net, self.buf, self.rows, self.z, self.off, self.part = net, buf, rows, z, off, part or rows
        self.base = net.take(8)
        self.slots = slots(z)

    def blk(self, b):
        return self.buf.at[ds(b * self.rows + self.off, self.part), :]

    def cp(self, b, side, target):
        return self.net.copy(self.blk(b), self.blk(b), self.base + side * 4 + b, self.base + b, ty=target)

    def start(self):
        z = self.z

        @pl.when(z < 3)
        def _():
            self.cp(z, 0, z + 1).start()

        @pl.when(z > 0)
        def _():
            self.cp(z, 1, z - 1).start()

    def take(self, i):
        b = self.slots[i]
        self.cp(b, 0, self.z).wait_recv()

    def forward(self, i):
        z, b = self.z, self.slots[i]
        target = 3 - z if i == 0 else 3 * (z - 1)
        self.cp(b, 0, target).start()

    def step1(self):
        self.take(0)

        @pl.when(mid(self.z))
        def _():
            self.forward(0)
            self.take(1)
            self.forward(1)

    def near_end(self):
        @pl.when(end(self.z))
        def _():
            self.take(0)

    def near_mid(self):
        @pl.when(mid(self.z))
        def _():
            self.take(1)
            self.forward(1)

    def far_mid(self):
        @pl.when(mid(self.z))
        def _():
            self.take(0)
            self.forward(0)

    def step2(self):
        @pl.when(end(self.z))
        def _():
            self.take(1)

    def step3_mid(self):
        @pl.when(mid(self.z))
        def _():
            self.take(2)
            self.forward(2)

    def step3_end(self):
        @pl.when(end(self.z))
        def _():
            self.take(2)

    def drain(self):
        z = self.z

        @pl.when(z < 3)
        def _():
            self.cp(z, 0, z + 1).wait_send()

        @pl.when(z > 0)
        def _():
            self.cp(z, 1, z - 1).wait_send()

        @pl.when(mid(z))
        def _():
            for i in range(3):
                self.cp(self.slots[i], 0, 3 - z if i == 0 else 3 * (z - 1)).wait_send()


class LineScatter:
    def __init__(self, net, part, rbuf, rows, z, off=0, size=None):
        self.net, self.part, self.rbuf, self.rows, self.z, self.off, self.size = net, part, rbuf, rows, z, off, size or rows
        self.base = net.take(5)
        self.slots = slots(z)
        one = (z % 2) * (1 - z // 2)
        self.dst = (self.slots[0] + (1 - z % 2) * (3 - z), self.slots[1] + 2 * one, self.slots[2])
        self.target = (z + 1 - 2 * (z % 2), 1 + z % 2, 1 + z % 2)

    def cp(self, i):
        return self.net.copy(
            self.part.at[self.view(self.slots[i]), :], self.rbuf.at[self.view(self.dst[i]), :],
            self.base + i, self.base + self.dst[i], ty=self.target[i])

    def view(self, b):
        return ds(b * self.rows + self.off, self.size)

    def wait_slot(self, s):
        view = self.rbuf.at[self.view(s), :]
        self.net.copy(view, view, self.base, self.base + s, ty=self.z).wait_recv()

    def send_end(self, i):
        @pl.when(end(self.z))
        def _():
            self.cp(i).start()

    def send_mid(self, i):
        @pl.when(mid(self.z))
        def _():
            b = self.slots[i]
            self.wait_slot(b)
            step = 16

            @pl.loop(0, self.size // step)
            def _(r):
                view = ds(b * self.rows + self.off + r * step, step)
                self.part[view, :] = (self.part[view, :].astype(F32) + self.rbuf[view, :].astype(F32)).astype(BF16)

            self.cp(i).start()

    def finish(self):
        z = self.z

        @pl.when(z < 3)
        def _():
            self.wait_slot(z)

        @pl.when(z > 0)
        def _():
            self.wait_slot(4)

    def drain(self):
        for i in range(3):
            self.cp(i).wait_send()


class WeightGather:
    def __init__(self, net, w, full, pos, by_rows, chunks, direct=0):
        self.net, self.w, self.full, self.by_rows = net, w, full, by_rows
        self.dp, self.t1, self.t2 = pos
        self.half = w.shape[0] // 2
        self.width = w.shape[0] if by_rows else w.shape[1]
        self.chunks, self.direct = chunks, direct
        self.base = net.take(1 + 4 * chunks + direct)

    def area(self, half, ch):
        if self.by_rows:
            n = self.w.shape[1] // self.chunks
            return ds(half * self.half, self.half, 16), self.half, pl.ds(ch * n, n)
        n = self.half // self.chunks
        return ds(half * self.half + ch * n, n, 16), n, pl.ds(0, self.width)

    def src(self, half, ch):
        rows, _, cols = self.area(half, ch)
        return self.w.at[rows, cols]

    def dst(self, k, half, ch):
        if self.by_rows:
            _, _, cols = self.area(half, ch)
            return self.full.at[ds(k * self.width + half * self.half, self.half, 16), cols]
        rows, _, _ = self.area(half, ch)
        return self.full.at[rows, pl.ds(k * self.width, self.width)]

    def whole(self, k):
        if self.by_rows:
            return self.full.at[pl.ds(k * self.width, self.width), :]
        return self.full.at[:, pl.ds(k * self.width, self.width)]

    def near(self, ch):
        i = self.base + 1 + ch
        return self.net.copy(self.src(self.dp, ch), self.dst(2, self.dp, ch), i, i, tx=self.t2)

    def cross(self, ch, half):
        i = self.base + 1 + self.chunks + ch
        return self.net.copy(self.dst(2, half, ch), self.dst(2, half, ch), i, i, dp=1 - self.dp)

    def diag(self, ch, which, half):
        i = self.base + 1 + (2 + which) * self.chunks + ch
        return self.net.copy(self.dst(2, half, ch), self.dst(3, half, ch), i, i, tx=self.t1)

    def mate(self):
        return self.net.copy(self.w, self.whole(1), self.base, self.base, tx=self.t1)

    def straight(self, n, half):
        ch = self.chunks - 1 - n
        i = self.base + 1 + 4 * self.chunks + n
        return self.net.copy(self.src(half, ch), self.dst(2, half, ch), i, i, tx=self.t2)

    def start_y(self):
        for ch in range(self.chunks):
            self.near(ch).start()
        for n in range(self.direct):
            self.straight(n, 1 - self.dp).start()

    def start_local(self):
        self.own = self.net.here(self.w, self.whole(0))
        self.mate().start()

    def y_event(self, ch):
        self.near(ch).wait_recv()
        if ch < self.chunks - self.direct:
            self.cross(ch, self.dp).start()
        self.diag(ch, 0, self.dp).start()

    def x_event(self, ch):
        if ch < self.chunks - self.direct:
            self.cross(ch, 1 - self.dp).wait_recv()
        else:
            self.straight(self.chunks - 1 - ch, 1 - self.dp).wait_recv()
        self.diag(ch, 1, 1 - self.dp).start()

    def finish_local(self):
        self.own.wait()
        self.mate().wait_recv()

    def finish(self, ch):
        self.diag(ch, 0, self.dp).wait_recv()
        self.diag(ch, 1, 1 - self.dp).wait_recv()

    def drain(self):
        self.mate().wait_send()
        for ch in range(self.chunks):
            self.near(ch).wait_send()
            if ch < self.chunks - self.direct:
                self.cross(ch, self.dp).wait_send()
            else:
                self.straight(self.chunks - 1 - ch, 1 - self.dp).wait_send()
            self.diag(ch, 0, self.dp).wait_send()
            self.diag(ch, 1, 1 - self.dp).wait_send()


def down_split(ff):
    return ff * 5 // 8


def places():
    dp, z, tx = lax.axis_index("dp"), lax.axis_index("ty"), lax.axis_index("tx")
    return dp, z, tx, (tx, tx + 1 - 2 * (tx % 2), (tx + 2) % 4, 3 - tx)


ROWS_ROWS = (((0,), (0,)), ((), ()))


class GradReduce:
    def __init__(self, net, peer, tile, tiles, st3, st1, cross, stage, got2, got0, got_y, out, out_tiles):
        self.net, self.peer, self.tile, self.tiles = net, peer, tile, tiles
        self.st3, self.st1, self.cross, self.stage = st3, st1, cross, stage
        self.got2, self.got0, self.got_y, self.out, self.out_tiles = got2, got0, got_y, out, out_tiles
        self.src = None
        self.base = net.take(3)
        self.rows, self.w = out.shape[0], out.shape[1] // tiles

    def cp(self, i):
        src, dst, to = ((self.st3, self.got2, 1), (self.st1, self.got0, 1), (self.src or self.cross, self.got_y, 2))[i]
        return self.net.copy(src, dst, self.base + i, self.base + i, tx=self.peer[to])

    def fill(self, k, ref):
        @pl.loop(0, self.tiles)
        def _(j):
            ref[:, ds(j * self.w, self.w)] = self.tile(k, j).astype(BF16)

    def step3(self):
        self.fill(3, self.st3)
        self.cp(0).start()

    def step1(self):
        self.fill(1, self.st1)
        self.cp(1).start()

    def step2(self, received=False):
        if not received:
            self.cp(0).wait_recv()
        self.net.here(self.got2, self.stage).wait()

        @pl.loop(0, self.tiles)
        def _(j):
            cols = ds(j * self.w, self.w)
            self.cross[:, cols] = (self.tile(2, j) + self.stage[:, cols].astype(F32)).astype(BF16)

    def send(self, src=None):
        self.src = src
        self.cp(2).start()

    def step0(self, far):
        self.cp(1).wait_recv()
        self.cp(2).wait_recv()
        loads = [self.net.here(self.got0, self.stage), self.net.here(self.got_y, far)]
        for c in loads:
            c.wait()
        base = self.net.n_local
        self.net.n_local += 2

        def put(j, slot):
            src = self.out_tiles.at[slot, pl.ds(0, self.rows), pl.ds(0, self.w)]
            return pltpu.make_async_copy(src, self.out.at[:, ds(j * self.w, self.w)], self.net.local.at[base + slot])

        @pl.loop(0, self.tiles)
        def _(j):
            cols = ds(j * self.w, self.w)
            slot = j % 2

            @pl.when(j >= 2)
            def _():
                put(j, slot).wait()

            self.out_tiles[slot, pl.ds(0, self.rows), pl.ds(0, self.w)] = self.tile(0, j) + (self.stage[:, cols].astype(F32) + far[:, cols].astype(F32))
            put(j, slot).start()

        for slot in range(min(2, self.tiles)):
            put(slot, slot).wait()

    def sent_locally(self):
        self.cp(0).wait_send()
        self.cp(1).wait_send()

    def sent(self):
        self.cp(2).wait_send()


def kernel_ab(q_width, hid, eqh, ekvh, posh, invh, swaph, dh2h, wg, wu, wd, wq, wkv, gh,
              n_o, da_o, db_o, u_o, wg_o, wu_o, wq_o, eq_o, h_o, g_o, e_o, n2_o, dres_o, home_o, dg_o, ux_o, ex_o, tab_o, d2_o, d0_o, dc_o,
              rows, dh2_v, n2_v, res_v, dres_v, n_v, a_v, b_v, wg_v, wu_v, wd_v, wq_v, eq_v, p_v, rbuf, rbuf2, gains, dg_v, swap_v, pos_v, inv_v, g_v, gin, send, recv, local):
    dp, z, tx, peer = places()
    sub, dim = rows.shape
    tokens = 4 * sub
    width = eq_v.shape[0]
    dt = dim // 4
    ff = wg.shape[1]
    wide = min(1024, ff)
    tile = min(512, ff)
    dwide = min(1024, dim)
    dtile = min(512, dim)
    hs, cs = sub // 2, sub // 8
    split = down_split(ff)
    net = Wires(send, recv, local)
    gain_in = net.here(gh, g_v)
    turn_in = [net.here(eqh, p_v.at[pl.ds(0, q_width), pl.ds(0, tokens)]), net.here(ekvh, p_v.at[pl.ds(q_width, width - q_width), pl.ds(0, tokens)]),
               net.here(swaph, swap_v), net.here(posh, pos_v), net.here(invh, inv_v)]
    entry_barrier([{"tx": peer[1]}, {"tx": peer[2]}, {"tx": peer[3]}, {"dp": 1 - dp}], z)

    pos = (dp, peer[1], peer[2])
    far_first = (2, 3, 1)
    g_id, h_id, e_id, d_id, o_id, u_id, x_id = (net.take(4), net.take(4), net.take(4), net.take(4), net.take(4), net.take(12), net.take(24))
    u_v = wg_v.at[pl.ds(0, tokens), :]
    e_v = wg_v.at[pl.ds(tokens, tokens), :]

    def g_cp(k):
        return net.copy(gin, gains.at[:, pl.ds(k * dt, dt)], g_id + k, g_id + k, tx=peer[k])

    def h_cp(k):
        return net.copy(hid.at[ds(peer[k] * sub, sub), :], rows.at[:, pl.ds(k * dt, dt)], h_id + k, h_id + k, tx=peer[k])

    def e_cp(k, block):
        return net.copy(p_v.at[pl.ds(0, width), ds(peer[k] * sub, sub)], eq_v.at[:, ds(block * sub, sub)], e_id + k, e_id + k, tx=peer[k])

    def d_cp(k):
        return net.copy(dh2h.at[ds(peer[k] * sub, sub), :], dh2_v.at[:, pl.ds(k * dt, dt)], d_id + k, d_id + k, tx=peer[k])

    def o_cp(k, block):
        return net.copy(res_v.at[:, pl.ds(k * dt, dt)], home_o.at[ds(block * sub, sub), :], o_id + k, o_id + k, tx=peer[k])

    def ux_cp(k, b):
        view = ds(b * sub, sub)
        cols = pl.ds(0, split)
        src = ux_o.at[1, view, :] if k == 3 else wg_v.at[view, cols]
        i = u_id + (k - 1) * 4 + b
        return net.copy(src, ux_o.at[k - 1, view, :], i, i, tx=peer[1] if k == 3 else peer[k])

    def ex_cp(k, b, half):
        i = x_id + half * 12 + (k - 1) * 4 + b
        view = ds(b * sub + half * hs, hs)
        return net.copy(wg_v.at[ds(tokens + b * sub + half * hs, hs), pl.ds(k * dt, dt)], ex_o.at[k - 1, view, :], i, i, tx=peer[k])

    gate = WeightGather(net, wg, wg_v, pos, True, 2)
    up = WeightGather(net, wu, wu_v, pos, True, 2)
    down = WeightGather(net, wd, wd_v, pos, False, 4, 1)
    q_w = WeightGather(net, wq, wq_v.at[pl.ds(0, q_width), :], pos, False, 1)
    kv_w = WeightGather(net, wkv, wq_v.at[pl.ds(q_width, width - q_width), :], pos, False, 1)
    ag = LineGather(net, n_v, sub, z)
    rsc = LineScatter(net, p_v, rbuf, sub, z)
    rs2 = [LineScatter(net, n_v, rbuf2, sub, z, c * cs, cs) for c in range(8)]
    ag2 = [LineGather(net, e_v, sub, z, c * cs, cs) for c in range(8)]

    for k in far_first:
        h_cp(k).start()
    gain_in.wait()
    both = g_v[...].astype(F32)
    gin[...] = jnp.broadcast_to(both[0:1, :], gin.shape)
    gin[1:2, :] = both[1:2, :]
    g_own = net.here(gin, gains.at[:, pl.ds(0, dt)])
    h_own = net.here(hid.at[ds(tx * sub, sub), :], rows.at[:, pl.ds(0, dt)])
    for w in (q_w, kv_w, gate, up, down):
        w.start_local()
    for k in far_first:
        g_cp(k).start()
    for c in turn_in:
        c.wait()

    @pl.loop(0, tokens // 128)
    def _(i):
        part = 128
        cos_c, sin_c = ds(i * part, part), ds(tokens + i * part, part)
        q_r, kv_r = pl.ds(0, 128), pl.ds(128, 128)
        angles = inv_v[...] * pos_v[:, cos_c].astype(F32)
        dres_v[q_r, sin_c] = jnp.sin(angles)
        dres_v[q_r, cos_c] = jnp.cos(angles)

        @pl.when(z < 2)
        def _():
            dres_v[kv_r, cos_c] = dres_v[q_r, cos_c]
            dres_v[kv_r, sin_c] = dres_v[q_r, sin_c]

        @pl.when(z >= 2)
        def _():
            dres_v[kv_r, cos_c] = jnp.ones((128, part), F32)
            dres_v[kv_r, sin_c] = jnp.zeros((128, part), F32)

    tab_out = net.here(dres_v.at[pl.ds(0, 256), pl.ds(0, 2 * tokens)], tab_o)
    turn(p_v, width, q_width, tokens, dres_v, swap_v, True)
    for k in far_first:
        e_cp(k, tx).start()
    e_own = net.here(p_v.at[pl.ds(0, width), ds(tx * sub, sub)], eq_v.at[:, ds(tx * sub, sub)])
    for w in (q_w, kv_w, gate, up, down):
        w.start_y()
    for k in far_first:
        d_cp(k).start()
    d_own = net.here(dh2h.at[ds(tx * sub, sub), :], dh2_v.at[:, pl.ds(0, dt)])

    for k in far_first:
        g_cp(k).wait_recv()
        h_cp(k).wait_recv()
    g_own.wait()
    h_own.wait()

    @pl.loop(0, sub // 16)
    def _(r):
        x = rows[ds(r * 16, 16), :].astype(F32)
        inv = lax.rsqrt(jnp.sum(x * x, axis=1, keepdims=True) / dim + NORM_EPS)
        n_v[ds(z * sub + r * 16, 16), :] = (x * inv * gains[0:1, :]).astype(BF16)

    ag.start()
    outs = [net.here(rows, h_o), net.here(gains, g_o)]
    for k in far_first:
        e_cp(k, peer[k]).wait_recv()
    e_own.wait()
    ag.step1()
    for w in (q_w, kv_w):
        w.y_event(0)
    for w in (q_w, kv_w):
        w.x_event(0)
    for w in (q_w, kv_w):
        w.finish_local()
        w.finish(0)
    for k in far_first:
        e_cp(k, tx).wait_send()

    def n2_block(b):
        @pl.loop(0, dim // dtile)
        def _(j):
            cols = ds(j * dtile, dtile)
            p_v[ds(b * sub, sub), cols] = dot(eq_v[:, ds(b * sub, sub)], wq_v[:, cols], ROWS_ROWS).astype(BF16)

    @pl.loop(0, 4)
    def _(i):
        n2_block(pick(3 - i, z))
        for step in range(3):
            pl.when(i == step)(lambda step=step: rsc.send_end(2 - step))
        pl.when(i == 0)(lambda: gate.y_event(0))

    wide = ff // 2

    def gate_part(b, c):
        cols = pl.ds(c * wide, wide)
        a_v[ds(b * sub, sub), cols] = dot(n_v[ds(b * sub, sub), :], wg_v[:, cols]).astype(BF16)

    def up_part(b, c):
        cols = pl.ds(c * wide, wide)
        bb = dot(n_v[ds(b * sub, sub), :], wu_v[:, cols]).astype(BF16)
        b_v[ds(b * sub, sub), cols] = bb
        aa = a_v[ds(b * sub, sub), cols].astype(F32)
        wg_v[ds(b * sub, sub), cols] = (aa * jax.nn.sigmoid(aa) * bb.astype(F32)).astype(BF16)

    def down_part(b, j):
        cols = pl.ds(j * (dim // 2), dim // 2)
        n_v[ds(b * sub, sub), cols] = dot(wg_v[ds(b * sub, sub), :], wd_v[:, cols]).astype(BF16)

    outs += [net.here(wq_v, wq_o), net.here(eq_v, eq_o)]
    gate.finish_local()
    gate.y_event(1)
    ag.step2()
    ag.step3_mid()
    gate.x_event(0)
    gate.finish(0)

    @pl.loop(0, 3)
    def _(i):
        gate_part(pick(i, z), 0)

    up.y_event(0)
    gate.x_event(1)
    rsc.send_mid(2)
    gate.finish(1)
    wg_out = net.here(wg_v, wg_o)

    @pl.loop(0, 3)
    def _(i):
        gate_part(pick(i, z), 1)

    up.finish_local()
    up.y_event(1)
    up.x_event(0)
    up.finish(0)
    ag.step3_end()

    @pl.loop(0, 2)
    def _(c):
        cols = ds(c * wide, wide)
        b = pick(3, z)
        a_v[ds(b * sub, sub), cols] = dot(n_v[ds(b * sub, sub), :], wg_v[:, cols]).astype(BF16)

    wg_out.wait()
    n_out = net.here(n_v, n_o)

    @pl.loop(0, 4)
    def _(i):
        pl.when(i == 1)(lambda: down.y_event(0))
        pl.when(i == 2)(lambda: down.y_event(1))
        pl.when(i == 3)(lambda: up.x_event(1))
        up_part(pick(i, z), 0)

    def up_events_1():
        rsc.send_mid(1)
        rsc.send_mid(0)
        down.x_event(0)

    def up_events_2():
        down.y_event(2)

    def up_events_3():
        down.y_event(3)
        down.x_event(1)

    up.finish(1)
    outs.append(net.here(wu_v, wu_o))

    @pl.loop(0, 4)
    def _(i):
        pl.when(i == 1)(up_events_1)
        pl.when(i == 2)(up_events_2)
        pl.when(i == 3)(up_events_3)
        b = pick(i, z)
        up_part(b, 1)
        ux_cp(2, b).start()
        ux_cp(1, b).start()

    outs.append(net.here(u_v, u_o))
    ag.drain()
    gate.drain()
    n_out.wait()
    down.finish_local()

    @pl.loop(0, 4)
    def _(i):
        pl.when(i == 2)(lambda: down.x_event(2))
        pl.when(i == 3)(lambda: down.x_event(3))
        down_part(pick(3 - i, z), 0)

    for ch in range(4):
        down.finish(ch)

    @pl.loop(0, 4)
    def _(i):
        down_part(pick(3 - i, z), 1)
        for step in range(3):
            pl.when(i == step)(lambda step=step: rs2[0].send_end(2 - step))

    for c in range(1, 8):
        for i in (2, 1, 0):
            rs2[c].send_end(i)
    dg_v[...] = jnp.zeros_like(dg_v)
    step = 16

    def norm_chunk(c):
        @pl.loop(0, cs // step)
        def _(r):
            at = c * cs + r * step
            view, mine, far = ds(at, step), ds(z * sub + at, step), ds(4 * sub + at, step)

            def whole(part, got):
                right = jnp.where(z < 3, got[mine, :].astype(F32), 0.0)
                left = jnp.where(z > 0, got[far, :].astype(F32), 0.0)
                return part[mine, :].astype(F32) + right + left

            resid = (rows[view, :].astype(F32) + whole(n_v, rbuf2)).astype(BF16)
            dy = whole(p_v, rbuf)
            res_v[view, :] = resid
            x = resid.astype(F32)
            inv = lax.rsqrt(jnp.sum(x * x, axis=1, keepdims=True) / dim + NORM_EPS)
            xhat = x * inv
            gain = gains[1:2, :]
            n2_v[view, :] = (xhat * gain).astype(BF16)
            part = dy * xhat
            dg_v[...] += part[:8] + part[8:]
            inner = jnp.sum(part * gain, axis=1, keepdims=True) / dim
            dres = dh2_v[view, :].astype(F32) + inv * (dy * gain) - xhat * (inv * inner)
            dres_v[view, pl.ds(0, dim)] = dres
            wg_v[ds(tokens + z * sub + at, step), :] = dres.astype(BF16)

    def spread(b, half):
        for k in far_first:
            ex_cp(k, b, half).start()

    def back_tile(b, j):
        view, cols = ds(b * sub, sub), ds(j * (ff // 4), ff // 4)
        du = dot(wg_v[ds(tokens + b * sub, sub), :], wd_v[ds(j * (ff // 4), ff // 4), :], NT_DIMS)
        aa = a_v[view, cols].astype(F32)
        bb = b_v[view, cols].astype(F32)
        sig = jax.nn.sigmoid(aa)
        a_v[view, cols] = (du * bb * sig * (1.0 + aa * (1.0 - sig))).astype(BF16)
        b_v[view, cols] = (du * aa * sig).astype(BF16)

    def scatter(i, c):
        return lambda: rs2[c].send_mid(i)

    def gathered(i, c):
        def go():
            ag2[c].take(i)
            pl.when(mid(z))(lambda: ag2[c].forward(i))
            if c % 4 == 3:
                spread(ag.slots[i], c // 4)
        return go

    def run(ops):
        def go():
            for op in ops:
                op()
        return go

    before_mid = (
        (scatter(2, 0), scatter(1, 0), scatter(0, 0)),
        (scatter(2, 1), scatter(1, 1), gathered(1, 0), scatter(0, 1), scatter(2, 2)),
        (scatter(1, 2), scatter(0, 2), gathered(1, 1), scatter(2, 3)),
        (scatter(1, 3), scatter(0, 3), gathered(1, 2), scatter(2, 4)),
        (scatter(1, 4), scatter(0, 4), gathered(1, 3), scatter(2, 5)),
        (scatter(1, 5), scatter(0, 5), gathered(1, 4), scatter(2, 6)),
        (scatter(1, 6), scatter(0, 6), gathered(1, 5), scatter(2, 7)),
        (scatter(1, 7), scatter(0, 7), gathered(1, 6), gathered(0, 0)))
    before_end = (
        (),
        (gathered(0, 0), gathered(1, 0)),
        (gathered(0, 1),),
        (gathered(1, 1), gathered(0, 2)),
        (gathered(1, 2), gathered(0, 3)),
        (gathered(1, 3), gathered(0, 4)),
        (gathered(1, 4), gathered(0, 5)),
        (gathered(1, 5), gathered(0, 6)))
    after_mid = {1: (gathered(0, 1),),
                 2: (gathered(2, 0),),
                 3: (gathered(0, 2),),
                 4: (gathered(1, 7),),
                 5: (gathered(0, 3),),
                 6: (gathered(2, 1),),
                 7: (gathered(0, 4),),
                 8: (gathered(2, 2), gathered(0, 5), gathered(2, 3), gathered(0, 6), gathered(2, 4), gathered(0, 7)),
                 10: (gathered(2, 5),),
                 12: (gathered(2, 6), gathered(2, 7))}
    after_end = {2: (gathered(1, 6),),
                 4: (gathered(0, 7),),
                 7: (gathered(2, 0),),
                 8: (gathered(1, 7),),
                 11: (gathered(2, 1),),
                 12: (gathered(2, 2), gathered(2, 3), gathered(2, 4), gathered(2, 5), gathered(2, 6), gathered(2, 7))}

    for c in range(8):
        pl.when(mid(z))(run(before_mid[c]))
        pl.when(end(z))(run(before_end[c]))
        if c == 0:
            rsc.finish()
            for k in far_first:
                d_cp(k).wait_recv()
            d_own.wait()
            tab_out.wait()
        rs2[c].finish()
        norm_chunk(c)
        ag2[c].start()
        if c % 4 == 3:
            spread(z, c // 4)

    for k in far_first:
        o_cp(k, tx).start()
    outs += [net.here(res_v.at[:, pl.ds(0, dt)], home_o.at[ds(tx * sub, sub), :]), net.here(n2_v, n2_o), net.here(dres_v.at[pl.ds(0, sub), pl.ds(0, dim)], dres_o), net.here(dg_v, dg_o)]
    rsc.drain()
    for c in range(8):
        rs2[c].drain()
    middle = (z + 1) // 2 % 2

    def u_forward():
        for b in range(4):
            ux_cp(2, b).wait_recv()
            ux_cp(3, b).start()

    @pl.loop(0, 16)
    def _(t):
        for at, ops in after_mid.items():
            pl.when(jnp.logical_and(t == at, mid(z)))(run(ops))
        for at, ops in after_end.items():
            pl.when(jnp.logical_and(t == at, end(z)))(run(ops))
        pl.when(t == 8)(u_forward)
        i = t // 4
        inner = (i + 1) // 2 % 2
        back_tile(pick(i + middle * inner * (3 - 2 * i), z), t % 4)

    outs.append(net.here(e_v, e_o))
    outs += [net.here(a_v, da_o), net.here(b_v, db_o)]

    def down_tile(k, j):
        return dot(wg_v[pl.ds(0, tokens), pl.ds(split, ff - split)], wg_v[pl.ds(tokens, tokens), ds(k * dt + j * (dt // 2), dt // 2)], ROWS_ROWS)

    quarter = [rbuf.at[pl.ds(0, ff - split), pl.ds(i * dt, dt)] for i in range(4)]
    part_d = GradReduce(net, peer, down_tile, 2, quarter[0], quarter[1], quarter[2], quarter[3], d2_o, d0_o, None, dc_o, None)
    part_d.step3()
    part_d.step1()
    part_d.step2()
    outs.append(net.here(quarter[2], dc_o))
    for k in far_first:
        o_cp(k, peer[k]).wait_recv()
        for b in range(4):
            ex_cp(k, b, 0).wait_recv()
            ex_cp(k, b, 1).wait_recv()
    for b in range(4):
        ux_cp(1, b).wait_recv()
        ux_cp(3, b).wait_recv()
    for c in outs:
        c.wait()
    for k in far_first:
        g_cp(k).wait_send()
        h_cp(k).wait_send()
        d_cp(k).wait_send()
        o_cp(k, tx).wait_send()
        for b in range(4):
            ux_cp(k, b).wait_send()
            ex_cp(k, b, 0).wait_send()
            ex_cp(k, b, 1).wait_send()
    for w in (q_w, kv_w, up, down):
        w.drain()
    for c in range(8):
        ag2[c].drain()
    part_d.cp(1).wait_recv()
    part_d.sent_locally()


def call_ab(hid, eqh, ekvh, pos, inv, swap, dh2h, wg, wu, wd, wq, wkv, g):
    tokens, dt = hid.shape
    sub, dim, ff, q_width = tokens // 4, dt * 4, wg.shape[1], wq.shape[0]
    width = q_width + wkv.shape[0]
    s = jax.ShapeDtypeStruct
    tok_ff, tok_d, row = s((tokens, ff), BF16), s((tokens, dim), BF16), s((sub, dim), BF16)
    shapes = (tok_d, tok_ff, tok_ff, tok_ff, s((dim, ff), BF16), s((dim, ff), BF16), s((width, dim), BF16), s((width, tokens), BF16),
              row, s((8, dim), F32), tok_d, row, s((sub, dim), F32), s((tokens, dt), BF16), s((8, dim), F32),
              s((3, tokens, down_split(ff)), BF16), s((3, tokens, dt), BF16), s((256, 2 * tokens), F32)) + (s((ff - down_split(ff), dt), BF16),) * 3
    vrow, vtok, vff = VMEM((sub, dim), BF16), VMEM((tokens, dim), BF16), VMEM((tokens, ff), BF16)
    return pl.pallas_call(
        functools.partial(kernel_ab, q_width), out_shape=shapes, in_specs=[ANY] * 13, out_specs=[ANY] * len(shapes),
        scratch_shapes=[
            vrow, vrow, vrow, vrow, VMEM((max(sub, 256), max(dim, 2 * tokens)), F32), vtok, vff, vff, VMEM((dim, ff), BF16), VMEM((dim, ff), BF16), VMEM((ff, dim), BF16),
            VMEM((width, dim), BF16), VMEM((width, tokens), BF16), vtok, VMEM((5 * sub, dim), BF16), VMEM((5 * sub, dim), BF16),
            VMEM((8, dim), F32), VMEM((8, dim), F32), VMEM((128, 128), BF16), VMEM((1, tokens), jnp.int32), VMEM((128, 128), F32),
            VMEM((2, dt), BF16), VMEM((8, dt), F32),
            pltpu.SemaphoreType.DMA((232,)), pltpu.SemaphoreType.DMA((232,)), pltpu.SemaphoreType.DMA((48,))],
        compiler_params=pltpu.CompilerParams(collective_id=0, has_side_effects=True, vmem_limit_bytes=VMEM_LIMIT),
        cost_estimate=pl.CostEstimate(flops=20 * tokens * dim * ff, bytes_accessed=100000000, transcendentals=0), name="phase_ab",
    )(hid, eqh, ekvh, pos, inv, swap, dh2h, wg, wu, wd, wq, wkv, g)


def kernel_c(q_width, da_h, db_h, wg_h, wu_h, n_h, u_h, ux_h, e_h, ex_h, n2_h, eq_h, wq_h, h_h, dres_h, g_h, dga_h, tabh, swaph, d0, dc,
             wgo, wgy, wuo, wuy, wdo, wqo, wqy, wvo, wvy, q_o, kv_o, dh_o, dg_o, g2, g0, u2, u0, q2, q0, v2, v0, qx, dy,
             wg_v, wu_v, da_v, db_v, n_v, p_v, rbuf, n2_v, st3, st1, cross_g, cross_u, stage, tiles_v, dres_v, wq_v, eq_v,
             gains, dg_v, dgr, dgz, tab_v, swap_v, send, recv, local):
    dp, z, tx, peer = places()
    tokens, ff = da_v.shape
    sub, dim = dres_v.shape
    dt = dim // 4
    width = eq_v.shape[0]
    tile = ff // 4
    dtile = min(512, dim)
    qt = min(256, tile)
    far_first = (2, 3, 1)
    net = Wires(send, recv, local)
    n2_in = net.here(n2_h, n2_v.at[ds(z * sub, sub), :])
    first = [net.here(n_h, n_v), net.here(da_h, da_v)]
    second = [net.here(db_h, db_v), net.here(wg_h, wg_v), net.here(wu_h, wu_v)]
    third = [net.here(wq_h, wq_v), net.here(eq_h, eq_v), net.here(dres_h, dres_v), net.here(g_h, gains),
             net.here(dga_h, dg_v.at[pl.ds(8, 8), :]), net.here(tabh, tab_v), net.here(swaph, swap_v)]
    sem = pltpu.get_barrier_semaphore()
    zs = tuple((z + i) % 4 for i in range(4))
    for i in (1, 2, 3):
        pl.semaphore_signal(sem, inc=1, device_id={"tx": peer[i]}, device_id_type=MESH)
        pl.semaphore_signal(sem, inc=1, device_id={"ty": zs[i]}, device_id_type=MESH)
    pl.semaphore_wait(sem, 6)
    rsc = LineScatter(net, p_v, rbuf, sub, z)
    ag = LineGather(net, n2_v, sub, z)
    q_id, h_id, t_id, z_id = net.take(4), net.take(4), net.take(4), net.take(4)

    def grad_tile(lhs, rhs, w):
        def go(k, j):
            cols = pl.ds(j * w, w) if isinstance(j, int) else ds(j * w, w)
            return dot(lhs[:, pl.ds(k * dt, dt)], rhs[:, cols], ROWS_ROWS)
        return go

    gate = GradReduce(net, peer, grad_tile(n_v, da_v, tile), ff // tile, st3, st1, cross_g, stage, g2, g0, wgy, wgo, tiles_v)
    up = GradReduce(net, peer, grad_tile(n_v, db_v, tile), ff // tile, st3, st1, cross_u, stage, u2, u0, wuy, wuo, tiles_v)
    d_id = net.take(1)

    def dy_cp():
        return net.copy(dc, dy, d_id, d_id, tx=peer[2])

    dy_cp().start()

    def head_grad(first, rows, got2, got0, got_y, out):
        corner = [da_v.at[pl.ds(first, rows), pl.ds(c * dt, dt)] for c in range(4)]

        def tile_of(k, j):
            return dot(eq_v[pl.ds(first, rows), :], n2_v[:, ds(k * dt + j * qt, qt)])

        return GradReduce(net, peer, tile_of, dt // qt, *corner, got2, got0, got_y, out, tiles_v)

    heads = (head_grad(0, q_width, q2, q0, wqy, wqo), head_grad(q_width, width - q_width, v2, v0, wvy, wvo))

    def dn_block(b):
        rows = ds(b * sub, sub)

        @pl.loop(0, dim // dtile)
        def _(j):
            wr = ds(j * dtile, dtile)
            p_v[rows, wr] = (dot(da_v[rows, :], wg_v[wr, :], NT_DIMS) + dot(db_v[rows, :], wu_v[wr, :], NT_DIMS)).astype(BF16)

    n2_in.wait()
    ag.start()
    for c in first:
        c.wait()
    gate.step3()
    gate.step1()
    gate.step2()
    gate.send()
    for c in second:
        c.wait()

    @pl.loop(0, 4)
    def _(i):
        @pl.when(i == 1)
        def _():
            gate.sent_locally()
            up.step3()
            up.step1()
            ag.step1()

        dn_block(pick(3 - i, z))
        for step in range(3):
            pl.when(i == step)(lambda step=step: rsc.send_end(2 - step))

    up.step2()
    up.send()
    rsc.send_mid(2)
    ag.step2()
    ag.step3_mid()
    up.sent_locally()
    h_in = net.here(h_h, st3.at[pl.ds(0, sub), :])
    gate.step0(st1)
    gate.sent()

    e_in = [net.here(e_h.at[:, pl.ds(0, dt)], wu_v.at[pl.ds(0, tokens), pl.ds(0, dt)])]
    for k in (1, 2, 3):
        e_in.append(net.here(ex_h.at[k - 1], wu_v.at[pl.ds(0, tokens), pl.ds(k * dt, dt)]))

    piece = ff // 8
    exchanged, n_pieces = down_split(ff) // piece, 8

    def u_place(j, k):
        return wg_v.at[pl.ds((j % 2) * tokens, tokens), pl.ds(k * piece, piece)]

    def sums(j, n):
        return stage.at[pl.ds((j % 2) * piece, piece), pl.ds(n * dt, dt)]

    def u_load(j):
        cols = pl.ds(j * piece, piece)
        if j < exchanged:
            return [net.here(u_h.at[:, cols] if k == 0 else ux_h.at[k - 1, :, cols], u_place(j, k)) for k in range(4)]
        rows = pl.ds((j - exchanged) * piece, piece)
        return [net.here(u_h.at[:, cols], u_place(j, 0)), net.here(d0.at[rows, :], sums(j, 0)), net.here(dy.at[rows, :], sums(j, 1))]

    loads, stores = {}, {}

    def down_run(js):
        for j in js:
            for c in loads.pop(j):
                c.wait()
            if j >= 2:
                stores.pop(j - 2).wait()
            acc = None if j < exchanged else sums(j, 0)[...].astype(F32) + sums(j, 1)[...].astype(F32)
            for k in range(4 if j < exchanged else 1):
                part = dot(u_place(j, k)[...], wu_v[pl.ds(0, tokens), pl.ds(k * dt, dt)], ROWS_ROWS)
                acc = part if acc is None else acc + part
            place = tiles_v.at[j % 2, pl.ds(0, piece), pl.ds(0, dt)]
            tiles_v[j % 2, pl.ds(0, piece), pl.ds(0, dt)] = acc
            stores[j] = net.here(place, wdo.at[pl.ds(j * piece, piece), :])
            if j + 2 < n_pieces:
                loads[j + 2] = u_load(j + 2)

    loads[0], loads[1] = u_load(0), u_load(1)
    rsc.send_mid(1)
    rsc.send_mid(0)
    for c in e_in:
        c.wait()
    down_run((0, 1))
    for c in third:
        c.wait()
    ag.step3_end()

    @pl.loop(0, width // qt)
    def _(j):
        wu_v[ds(tokens + j * qt, qt), pl.ds(0, tokens)] = dot(wq_v[ds(j * qt, qt), :], n2_v[...], NT_DIMS).astype(BF16)

    def q_cp(k, block):
        return net.copy(wu_v.at[pl.ds(tokens, width), ds(peer[k] * sub, sub)], qx.at[:, ds(block * sub, sub)], q_id + k, q_id + k, tx=peer[k])

    for k in far_first:
        q_cp(k, tx).start()
    q_own = net.here(wu_v.at[pl.ds(tokens, width), ds(tx * sub, sub)], qx.at[:, ds(tx * sub, sub)])
    for part in heads:
        part.step3()
        part.step1()
    dy_cp().wait_recv()
    for part in heads:
        part.step2()
        part.send()
    down_run(range(2, n_pieces))
    h_in.wait()
    rsc.finish()
    dg_v[pl.ds(0, 8), :] = jnp.zeros((8, dim), F32)
    step = 16

    @pl.loop(0, sub // step)
    def _(r):
        view, mine, far = ds(r * step, step), ds(z * sub + r * step, step), ds(4 * sub + r * step, step)
        right = jnp.where(z < 3, rbuf[mine, :].astype(F32), 0.0)
        left = jnp.where(z > 0, rbuf[far, :].astype(F32), 0.0)
        dy = p_v[mine, :].astype(F32) + right + left
        x = st3[view, :].astype(F32)
        inv = lax.rsqrt(jnp.sum(x * x, axis=1, keepdims=True) / dim + NORM_EPS)
        xhat = x * inv
        gain = gains[0:1, :]
        part = dy * xhat
        dg_v[pl.ds(0, 8), :] += part[:8] + part[8:]
        inner = jnp.sum(part * gain, axis=1, keepdims=True) / dim
        st1[view, :] = (dres_v[view, :] + inv * (dy * gain) - xhat * (inv * inner)).astype(BF16)

    def h_cp(k, block):
        return net.copy(st1.at[pl.ds(0, sub), pl.ds(k * dt, dt)], dh_o.at[ds(block * sub, sub), :], h_id + k, h_id + k, tx=peer[k])

    def t_cp(k):
        return net.copy(dg_v.at[:, pl.ds(k * dt, dt)], dgr.at[k], t_id + k, t_id + k, tx=peer[k])

    def z_cp(i):
        return net.copy(dgr.at[0], dgz.at[i], z_id + i, z_id + i, ty=zs[i])

    for k in far_first:
        t_cp(k).start()
    for k in far_first:
        h_cp(k, tx).start()
    h_own = net.here(st1.at[pl.ds(0, sub), pl.ds(0, dt)], dh_o.at[ds(tx * sub, sub), :])
    up.sent()
    for c in stores.values():
        c.wait()
    up.step0(cross_g)
    for k in far_first:
        q_cp(k, peer[k]).wait_recv()
    q_own.wait()
    turned = wu_v.at[pl.ds(tokens, width), pl.ds(tokens, tokens)]
    net.here(qx, turned).wait()
    turn(turned, width, q_width, tokens, tab_v, swap_v, False)
    q_out = net.here(wu_v.at[pl.ds(tokens, q_width), pl.ds(tokens, tokens)], q_o)
    kv_out = net.here(wu_v.at[pl.ds(tokens + q_width, width - q_width), pl.ds(tokens, tokens)], kv_o)
    heads[0].step0(cross_g.at[pl.ds(0, q_width), pl.ds(0, dt)])
    heads[1].step0(cross_g.at[pl.ds(0, width - q_width), pl.ds(dt, dt)])
    for k in far_first:
        t_cp(k).wait_recv()
    dgr[0] = dg_v[:, pl.ds(0, dt)] + dgr[1] + dgr[2] + dgr[3]
    for i in (1, 2, 3):
        z_cp(i).start()
    for i in (1, 2, 3):
        z_cp(i).wait_recv()
    dgz[0] = dgr[0] + dgz[1] + dgz[2] + dgz[3]
    dg_out = net.here(dgz.at[0], dg_o)
    for k in far_first:
        h_cp(k, peer[k]).wait_recv()
    for c in (q_out, kv_out, dg_out, h_own):
        c.wait()
    dy_cp().wait_send()
    for part in heads:
        part.sent_locally()
        part.sent()
    for k in far_first:
        q_cp(k, tx).wait_send()
        h_cp(k, tx).wait_send()
        t_cp(k).wait_send()
        z_cp(k).wait_send()
    ag.drain()
    rsc.drain()


def call_c(q_width, *args):
    tokens, ff = args[0].shape
    sub, dim = args[9].shape
    dt, width = dim // 4, args[10].shape[0]
    rest = width - q_width
    tile = ff // 4
    s = jax.ShapeDtypeStruct
    wf, wb = s((dt, ff), F32), s((dt, ff), BF16)
    qf, qb, vf, vb = s((q_width, dt), F32), s((q_width, dt), BF16), s((rest, dt), F32), s((rest, dt), BF16)
    shapes = (wf, wb, wf, wb, s((ff, dt), F32), qf, qb, vf, vb, s((q_width, tokens), BF16), s((rest, tokens), BF16), s((tokens, dt), BF16), s((16, dt), F32),
              wb, wb, wb, wb, qb, qb, vb, vb, s((width, tokens), BF16), s((ff - down_split(ff), dt), BF16))
    return pl.pallas_call(
        functools.partial(kernel_c, q_width), out_shape=shapes, in_specs=[ANY] * len(args), out_specs=[ANY] * len(shapes),
        scratch_shapes=[
            VMEM((dim, ff), BF16), VMEM((dim, ff), BF16), VMEM((tokens, ff), BF16), VMEM((tokens, ff), BF16), VMEM((tokens, dim), BF16),
            VMEM((tokens, dim), BF16), VMEM((5 * sub, dim), BF16), VMEM((tokens, dim), BF16),
            VMEM((dt, ff), BF16), VMEM((dt, ff), BF16), VMEM((dt, ff), BF16), VMEM((dt, ff), BF16), VMEM((dt, ff), BF16),
            VMEM((2, max(dt, tile), max(dt, tile)), F32), VMEM((sub, dim), F32), VMEM((width, dim), BF16), VMEM((width, tokens), BF16),
            VMEM((8, dim), F32), VMEM((16, dim), F32), VMEM((4, 16, dt), F32), VMEM((4, 16, dt), F32), VMEM((256, 2 * tokens), F32), VMEM((128, 128), BF16),
            pltpu.SemaphoreType.DMA((48,)), pltpu.SemaphoreType.DMA((48,)), pltpu.SemaphoreType.DMA((96,))],
        compiler_params=pltpu.CompilerParams(collective_id=2, has_side_effects=True, vmem_limit_bytes=VMEM_LIMIT),
        cost_estimate=pl.CostEstimate(flops=20 * tokens * dim * ff, bytes_accessed=100000000, transcendentals=0), name="phase_c",
    )(*args)


def kernel_out(pieces, n, *refs):
    ins, outs, bufs = refs[:n], refs[n + 1:2 * n + 1], refs[2 * n + 3:3 * n + 3]
    gains, gain_a, gain_b = refs[n], refs[2 * n + 1], refs[2 * n + 2]
    read, write = refs[3 * n + 3:]

    def part(ref, i, c):
        rows = ref.shape[0] // pieces[i]
        return ref.at[pl.ds(c * rows, rows), :]

    jobs = [(i, c) for i in range(n) for c in range(pieces[i])]
    get = [pltpu.make_async_copy(part(ins[i], i, c), part(bufs[i], i, c), read.at[m]) for m, (i, c) in enumerate(jobs)]
    put = [pltpu.make_async_copy(part(bufs[i], i, c), part(outs[i], i, c), write.at[m]) for m, (i, c) in enumerate(jobs)]
    for g in get:
        g.start()
    gain_a[...] = jnp.sum(gains[pl.ds(0, 8), :], axis=0, keepdims=True)
    gain_b[...] = jnp.sum(gains[pl.ds(8, 8), :], axis=0, keepdims=True)
    for g, p in zip(get, put):
        g.wait()
        p.start()
    for p in put:
        p.wait()


def call_out(results, gains):
    n = len(results)
    pieces = tuple(max(1, x.size * x.dtype.itemsize // 2**20) for x in results)
    row = jax.ShapeDtypeStruct((1, gains.shape[1]), F32)
    whole = pl.BlockSpec(memory_space=pltpu.VMEM)
    return pl.pallas_call(
        functools.partial(kernel_out, pieces, n), out_shape=tuple(jax.ShapeDtypeStruct(x.shape, x.dtype) for x in results) + (row, row),
        in_specs=[ANY] * n + [whole], out_specs=[ANY] * n + [whole, whole],
        scratch_shapes=[VMEM(x.shape, x.dtype) for x in results] + [pltpu.SemaphoreType.DMA((sum(pieces),))] * 2,
        compiler_params=pltpu.CompilerParams(vmem_limit_bytes=VMEM_LIMIT),
        cost_estimate=pl.CostEstimate(flops=1000000, bytes_accessed=35000000, transcendentals=0), name="results",
    )(*results, gains)


def solution(mesh):
    def local_step(hidden, positions, g_ffn, w_gate, w_up, w_down, g_attn, w_q, w_kv, grad_h2, grad_q, grad_kv):
        tokens, dt = hidden.shape
        q_heads, head_dim = w_q.shape[1:]
        q_width = q_heads * head_dim

        lane = np.arange(128)
        inv_freq = ROPE_BASE ** (-(lane % head_dim // 2 * 2).astype(np.float32) / head_dim)
        inv_freq = jnp.asarray(np.tile(inv_freq.astype(np.float32)[:, None], (1, 128)))
        swap = np.zeros((128, 128), np.float32)
        swap[lane, lane ^ 1] = np.where(lane % 2 == 0, -1.0, 1.0)
        swap = jnp.asarray(swap, BF16)

        def heads_first(x):
            return x.transpose(1, 2, 0).reshape(-1, x.shape[0])

        def heads_last(x):
            return x.reshape(-1, head_dim, x.shape[1]).transpose(2, 0, 1)

        (normed_all, grad_gate, grad_up, u_all, gate_w, up_w, w_qkv, back_all, h_rows, gains, res_all, normed2, grad_res, resid_out, gattn8,
         u_other, e_other, table, _, wd_zero, wd_cross) = call_ab(
             hidden, heads_first(grad_q), heads_first(grad_kv), positions.reshape(1, tokens), inv_freq, swap, grad_h2,
             w_gate, w_up, w_down, heads_first(w_q), heads_first(w_kv), jnp.where(jnp.arange(2)[:, None] == 0, g_ffn[None, :], g_attn[None, :]))
        (grad_wgate, _, grad_wup, _, grad_wdown, grad_wq, _, grad_wkv, _, q_out, kv_out, grad_hidden, gain_grads, *_) = call_c(
            q_width, grad_gate, grad_up, gate_w, up_w, normed_all, u_all, u_other, res_all, e_other, normed2, back_all, w_qkv,
            h_rows, grad_res, gains, gattn8, table, swap, wd_zero, wd_cross)
        (resid_out, grad_wgate, grad_wup, grad_wdown, grad_wq, grad_wkv, q_out, kv_out, grad_hidden, grad_gffn, grad_gattn) = call_out(
            (resid_out, grad_wgate, grad_wup, grad_wdown, grad_wq, grad_wkv, q_out, kv_out, grad_hidden), gain_grads)
        q_out, kv_out, grad_wq, grad_wkv = (heads_last(x) for x in (q_out, kv_out, grad_wq, grad_wkv))
        grad_gffn, grad_gattn = grad_gffn[0], grad_gattn[0]
        return (resid_out, q_out, kv_out, grad_hidden, grad_gffn, grad_gattn, grad_wgate, grad_wup, grad_wdown, grad_wq, grad_wkv)

    row_spec = P(("dp", "ty"), "tx")
    head_spec = P(("dp", "tx"), "ty", None)
    in_specs = (row_spec, P(("dp", "tx")), P("tx"), P("tx", "ty"), P("tx", "ty"), P("ty", "tx"), P("tx"), P("tx", "ty", None), P("tx", "ty", None), row_spec, head_spec, head_spec)
    out_specs = (row_spec, head_spec, head_spec, row_spec, P(("dp", "tx")), P(("dp", "tx")), P(("dp", "tx"), "ty"), P(("dp", "tx"), "ty"), P(("dp", "ty"), "tx"), head_spec, head_spec)
    return jax.shard_map(local_step, mesh=mesh, in_specs=in_specs, out_specs=out_specs, check_vma=False)
```

```python
import functools

import jax
import jax.numpy as jnp
import numpy as np
from jax import lax
from jax.experimental import pallas as pl
from jax.experimental.pallas import tpu as pltpu
from jax.sharding import PartitionSpec as P

NORM_EPS = 1e-5
ROPE_BASE = 10000.0
F32 = jnp.float32
BF16 = jnp.bfloat16


def dot(a, b, dims=(((1,), (0,)), ((), ()))):
    return lax.dot_general(a, b, dims, preferred_element_type=F32)


MESH = pl.DeviceIdType.MESH
ANY = pl.BlockSpec(memory_space=pl.ANY)
VMEM = pltpu.VMEM
NT_DIMS = (((1,), (1,)), ((), ()))
VMEM_LIMIT = 67000000


def ds(start, size, align=None):
    if isinstance(start, int):
        return pl.ds(start, size)
    return pl.ds(pl.multiple_of(start, align or size), size)


def mid(z):
    return jnp.logical_and(z > 0, z < 3)


def end(z):
    return jnp.logical_or(z == 0, z == 3)


def slots(z):
    return (z + 1 - 2 * (z % 2), 2 - z // 2, 3 - 3 * (z // 2))


def turn(x_ref, width, q_width, tokens, table_ref, swap_ref, back):
    step = min(256, tokens)

    @pl.loop(0, tokens // step)
    def _(r):
        cols = ds(r * step, step)
        for g in range(width // 128):
            rows = pl.ds(g * 128, 128)
            base = pl.ds(0 if g * 128 < q_width else 128, 128)
            x = x_ref[rows, cols]
            main = x.astype(F32) * table_ref[base, cols]
            side = dot(swap_ref[...], x) * table_ref[base, ds(tokens + r * step, step)]
            x_ref[rows, cols] = (main - side if back else main + side).astype(BF16)


def pick(i, z):
    s1, s2, s3 = slots(z)
    first, last = (3 - i) // 3, (i // 2) * (i % 2)
    return z * first + s1 * ((i % 2) * (1 - i // 2)) + s2 * ((i // 2) * (1 - i % 2)) + s3 * last


class Wires:
    def __init__(self, send, recv, local):
        self.send, self.recv, self.local = send, recv, local
        self.n_remote = 0
        self.n_local = 0

    def take(self, n=1):
        base = self.n_remote
        self.n_remote += n
        assert self.n_remote <= self.send.shape[0]
        return base

    def copy(self, src, dst, si, ri, **dev):
        return pltpu.make_async_remote_copy(
            src_ref=src, dst_ref=dst, send_sem=self.send.at[si], recv_sem=self.recv.at[ri],
            device_id=dev, device_id_type=MESH)

    def here(self, src, dst):
        i = self.n_local
        self.n_local += 1
        assert i < self.local.shape[0]
        c = pltpu.make_async_copy(src, dst, self.local.at[i])
        c.start()
        return c


def entry_barrier(axes, z):
    sem = pltpu.get_barrier_semaphore()
    for dev in axes:
        pl.semaphore_signal(sem, inc=1, device_id=dev, device_id_type=MESH)

    @pl.when(z > 0)
    def _():
        pl.semaphore_signal(sem, inc=1, device_id={"ty": z - 1}, device_id_type=MESH)

    @pl.when(z < 3)
    def _():
        pl.semaphore_signal(sem, inc=1, device_id={"ty": z + 1}, device_id_type=MESH)

    @pl.when(mid(z))
    def _():
        pl.semaphore_wait(sem, len(axes) + 2)

    @pl.when(end(z))
    def _():
        pl.semaphore_wait(sem, len(axes) + 1)


class LineGather:
    def __init__(self, net, buf, rows, z, off=0, part=None):
        self.net, self.buf, self.rows, self.z, self.off, self.part = net, buf, rows, z, off, part or rows
        self.base = net.take(8)
        self.slots = slots(z)

    def blk(self, b):
        return self.buf.at[ds(b * self.rows + self.off, self.part), :]

    def cp(self, b, side, target):
        return self.net.copy(self.blk(b), self.blk(b), self.base + side * 4 + b, self.base + b, ty=target)

    def start(self):
        z = self.z

        @pl.when(z < 3)
        def _():
            self.cp(z, 0, z + 1).start()

        @pl.when(z > 0)
        def _():
            self.cp(z, 1, z - 1).start()

    def take(self, i):
        b = self.slots[i]
        self.cp(b, 0, self.z).wait_recv()

    def forward(self, i):
        z, b = self.z, self.slots[i]
        target = 3 - z if i == 0 else 3 * (z - 1)
        self.cp(b, 0, target).start()

    def step1(self):
        self.take(0)

        @pl.when(mid(self.z))
        def _():
            self.forward(0)
            self.take(1)
            self.forward(1)

    def near_end(self):
        @pl.when(end(self.z))
        def _():
            self.take(0)

    def near_mid(self):
        @pl.when(mid(self.z))
        def _():
            self.take(1)
            self.forward(1)

    def far_mid(self):
        @pl.when(mid(self.z))
        def _():
            self.take(0)
            self.forward(0)

    def step2(self):
        @pl.when(end(self.z))
        def _():
            self.take(1)

    def step3_mid(self):
        @pl.when(mid(self.z))
        def _():
            self.take(2)
            self.forward(2)

    def step3_end(self):
        @pl.when(end(self.z))
        def _():
            self.take(2)

    def drain(self):
        z = self.z

        @pl.when(z < 3)
        def _():
            self.cp(z, 0, z + 1).wait_send()

        @pl.when(z > 0)
        def _():
            self.cp(z, 1, z - 1).wait_send()

        @pl.when(mid(z))
        def _():
            for i in range(3):
                self.cp(self.slots[i], 0, 3 - z if i == 0 else 3 * (z - 1)).wait_send()


class LineScatter:
    def __init__(self, net, part, rbuf, rows, z, off=0, size=None):
        self.net, self.part, self.rbuf, self.rows, self.z, self.off, self.size = net, part, rbuf, rows, z, off, size or rows
        self.base = net.take(5)
        self.slots = slots(z)
        one = (z % 2) * (1 - z // 2)
        self.dst = (self.slots[0] + (1 - z % 2) * (3 - z), self.slots[1] + 2 * one, self.slots[2])
        self.target = (z + 1 - 2 * (z % 2), 1 + z % 2, 1 + z % 2)

    def cp(self, i):
        return self.net.copy(
            self.part.at[self.view(self.slots[i]), :], self.rbuf.at[self.view(self.dst[i]), :],
            self.base + i, self.base + self.dst[i], ty=self.target[i])

    def view(self, b):
        return ds(b * self.rows + self.off, self.size)

    def wait_slot(self, s):
        view = self.rbuf.at[self.view(s), :]
        self.net.copy(view, view, self.base, self.base + s, ty=self.z).wait_recv()

    def send_end(self, i):
        @pl.when(end(self.z))
        def _():
            self.cp(i).start()

    def send_mid(self, i):
        @pl.when(mid(self.z))
        def _():
            b = self.slots[i]
            self.wait_slot(b)
            step = 16

            @pl.loop(0, self.size // step)
            def _(r):
                view = ds(b * self.rows + self.off + r * step, step)
                self.part[view, :] = (self.part[view, :].astype(F32) + self.rbuf[view, :].astype(F32)).astype(BF16)

            self.cp(i).start()

    def finish(self):
        z = self.z

        @pl.when(z < 3)
        def _():
            self.wait_slot(z)

        @pl.when(z > 0)
        def _():
            self.wait_slot(4)

    def drain(self):
        for i in range(3):
            self.cp(i).wait_send()


class WeightGather:
    def __init__(self, net, w, full, pos, by_rows, chunks, direct=0):
        self.net, self.w, self.full, self.by_rows = net, w, full, by_rows
        self.dp, self.t1, self.t2 = pos
        self.half = w.shape[0] // 2
        self.width = w.shape[0] if by_rows else w.shape[1]
        self.chunks, self.direct = chunks, direct
        self.base = net.take(1 + 4 * chunks + direct)

    def area(self, half, ch):
        if self.by_rows:
            n = self.w.shape[1] // self.chunks
            return ds(half * self.half, self.half, 16), self.half, pl.ds(ch * n, n)
        n = self.half // self.chunks
        return ds(half * self.half + ch * n, n, 16), n, pl.ds(0, self.width)

    def src(self, half, ch):
        rows, _, cols = self.area(half, ch)
        return self.w.at[rows, cols]

    def dst(self, k, half, ch):
        if self.by_rows:
            _, _, cols = self.area(half, ch)
            return self.full.at[ds(k * self.width + half * self.half, self.half, 16), cols]
        rows, _, _ = self.area(half, ch)
        return self.full.at[rows, pl.ds(k * self.width, self.width)]

    def whole(self, k):
        if self.by_rows:
            return self.full.at[pl.ds(k * self.width, self.width), :]
        return self.full.at[:, pl.ds(k * self.width, self.width)]

    def near(self, ch):
        i = self.base + 1 + ch
        return self.net.copy(self.src(self.dp, ch), self.dst(2, self.dp, ch), i, i, tx=self.t2)

    def cross(self, ch, half):
        i = self.base + 1 + self.chunks + ch
        return self.net.copy(self.dst(2, half, ch), self.dst(2, half, ch), i, i, dp=1 - self.dp)

    def diag(self, ch, which, half):
        i = self.base + 1 + (2 + which) * self.chunks + ch
        return self.net.copy(self.dst(2, half, ch), self.dst(3, half, ch), i, i, tx=self.t1)

    def mate(self):
        return self.net.copy(self.w, self.whole(1), self.base, self.base, tx=self.t1)

    def straight(self, n, half):
        ch = self.chunks - 1 - n
        i = self.base + 1 + 4 * self.chunks + n
        return self.net.copy(self.src(half, ch), self.dst(2, half, ch), i, i, tx=self.t2)

    def start_y(self):
        for ch in range(self.chunks):
            self.near(ch).start()
        for n in range(self.direct):
            self.straight(n, 1 - self.dp).start()

    def start_local(self):
        self.own = self.net.here(self.w, self.whole(0))
        self.mate().start()

    def y_event(self, ch):
        self.near(ch).wait_recv()
        if ch < self.chunks - self.direct:
            self.cross(ch, self.dp).start()
        self.diag(ch, 0, self.dp).start()

    def x_event(self, ch):
        if ch < self.chunks - self.direct:
            self.cross(ch, 1 - self.dp).wait_recv()
        else:
            self.straight(self.chunks - 1 - ch, 1 - self.dp).wait_recv()
        self.diag(ch, 1, 1 - self.dp).start()

    def finish_local(self):
        self.own.wait()
        self.mate().wait_recv()

    def finish(self, ch):
        self.diag(ch, 0, self.dp).wait_recv()
        self.diag(ch, 1, 1 - self.dp).wait_recv()

    def drain(self):
        self.mate().wait_send()
        for ch in range(self.chunks):
            self.near(ch).wait_send()
            if ch < self.chunks - self.direct:
                self.cross(ch, self.dp).wait_send()
            else:
                self.straight(self.chunks - 1 - ch, 1 - self.dp).wait_send()
            self.diag(ch, 0, self.dp).wait_send()
            self.diag(ch, 1, 1 - self.dp).wait_send()


def down_split(ff):
    return ff * 5 // 8


def places():
    dp, z, tx = lax.axis_index("dp"), lax.axis_index("ty"), lax.axis_index("tx")
    return dp, z, tx, (tx, tx + 1 - 2 * (tx % 2), (tx + 2) % 4, 3 - tx)


ROWS_ROWS = (((0,), (0,)), ((), ()))


class GradReduce:
    def __init__(self, net, peer, tile, tiles, st3, st1, cross, stage, got2, got0, got_y, out, out_tiles):
        self.net, self.peer, self.tile, self.tiles = net, peer, tile, tiles
        self.st3, self.st1, self.cross, self.stage = st3, st1, cross, stage
        self.got2, self.got0, self.got_y, self.out, self.out_tiles = got2, got0, got_y, out, out_tiles
        self.src = None
        self.base = net.take(3)
        self.rows, self.w = out.shape[0], out.shape[1] // tiles

    def cp(self, i):
        src, dst, to = ((self.st3, self.got2, 1), (self.st1, self.got0, 1), (self.src or self.cross, self.got_y, 2))[i]
        return self.net.copy(src, dst, self.base + i, self.base + i, tx=self.peer[to])

    def fill(self, k, ref):
        @pl.loop(0, self.tiles)
        def _(j):
            ref[:, ds(j * self.w, self.w)] = self.tile(k, j).astype(BF16)

    def step3(self):
        self.fill(3, self.st3)
        self.cp(0).start()

    def step1(self):
        self.fill(1, self.st1)
        self.cp(1).start()

    def step2(self, received=False):
        if not received:
            self.cp(0).wait_recv()
        self.net.here(self.got2, self.stage).wait()

        @pl.loop(0, self.tiles)
        def _(j):
            cols = ds(j * self.w, self.w)
            self.cross[:, cols] = (self.tile(2, j) + self.stage[:, cols].astype(F32)).astype(BF16)

    def send(self, src=None):
        self.src = src
        self.cp(2).start()

    def step0(self, far):
        self.cp(1).wait_recv()
        self.cp(2).wait_recv()
        loads = [self.net.here(self.got0, self.stage), self.net.here(self.got_y, far)]
        for c in loads:
            c.wait()
        base = self.net.n_local
        self.net.n_local += 2

        def put(j, slot):
            src = self.out_tiles.at[slot, pl.ds(0, self.rows), pl.ds(0, self.w)]
            return pltpu.make_async_copy(src, self.out.at[:, ds(j * self.w, self.w)], self.net.local.at[base + slot])

        @pl.loop(0, self.tiles)
        def _(j):
            cols = ds(j * self.w, self.w)
            slot = j % 2

            @pl.when(j >= 2)
            def _():
                put(j, slot).wait()

            self.out_tiles[slot, pl.ds(0, self.rows), pl.ds(0, self.w)] = self.tile(0, j) + (self.stage[:, cols].astype(F32) + far[:, cols].astype(F32))
            put(j, slot).start()

        for slot in range(min(2, self.tiles)):
            put(slot, slot).wait()

    def sent_locally(self):
        self.cp(0).wait_send()
        self.cp(1).wait_send()

    def sent(self):
        self.cp(2).wait_send()


def kernel_ab(q_width, hid, eqh, ekvh, posh, invh, swaph, dh2h, wg, wu, wd, wq, wkv, gh,
              n_o, da_o, db_o, u_o, wg_o, wu_o, wq_o, eq_o, h_o, g_o, e_o, n2_o, dres_o, home_o, dg_o, ux_o, ex_o, tab_o, d2_o, d0_o, dc_o,
              rows, dh2_v, n2_v, res_v, dres_v, n_v, a_v, b_v, wg_v, wu_v, wd_v, wq_v, eq_v, p_v, rbuf, rbuf2, gains, dg_v, swap_v, pos_v, inv_v, g_v, gin, send, recv, local):
    dp, z, tx, peer = places()
    sub, dim = rows.shape
    tokens = 4 * sub
    width = eq_v.shape[0]
    dt = dim // 4
    ff = wg.shape[1]
    wide = min(1024, ff)
    tile = min(512, ff)
    dwide = min(1024, dim)
    dtile = min(512, dim)
    hs, cs = sub // 2, sub // 8
    split = down_split(ff)
    net = Wires(send, recv, local)
    gain_in = net.here(gh, g_v)
    turn_in = [net.here(eqh, p_v.at[pl.ds(0, q_width), pl.ds(0, tokens)]), net.here(ekvh, p_v.at[pl.ds(q_width, width - q_width), pl.ds(0, tokens)]),
               net.here(swaph, swap_v), net.here(posh, pos_v), net.here(invh, inv_v)]
    entry_barrier([{"tx": peer[1]}, {"tx": peer[2]}, {"tx": peer[3]}, {"dp": 1 - dp}], z)

    pos = (dp, peer[1], peer[2])
    far_first = (2, 3, 1)
    g_id, h_id, e_id, d_id, o_id, u_id, x_id = (net.take(4), net.take(4), net.take(4), net.take(4), net.take(8), net.take(12), net.take(24))
    u_v = wg_v.at[pl.ds(0, tokens), :]
    e_v = wg_v.at[pl.ds(tokens, tokens), :]

    def g_cp(k):
        return net.copy(gin, gains.at[:, pl.ds(k * dt, dt)], g_id + k, g_id + k, tx=peer[k])

    def h_cp(k):
        return net.copy(hid.at[ds(peer[k] * sub, sub), :], rows.at[:, pl.ds(k * dt, dt)], h_id + k, h_id + k, tx=peer[k])

    def e_cp(k, block):
        return net.copy(p_v.at[pl.ds(0, width), ds(peer[k] * sub, sub)], eq_v.at[:, ds(block * sub, sub)], e_id + k, e_id + k, tx=peer[k])

    def d_cp(k):
        return net.copy(dh2h.at[ds(peer[k] * sub, sub), :], dh2_v.at[:, pl.ds(k * dt, dt)], d_id + k, d_id + k, tx=peer[k])

    def o_cp(k, block, half):
        i = o_id + half * 4 + k
        return net.copy(res_v.at[pl.ds(half * hs, hs), pl.ds(k * dt, dt)], home_o.at[ds(block * sub + half * hs, hs), :], i, i, tx=peer[k])

    def ux_cp(k, b):
        view = ds(b * sub, sub)
        cols = pl.ds(0, split)
        src = ux_o.at[1, view, :] if k == 3 else wg_v.at[view, cols]
        i = u_id + (k - 1) * 4 + b
        return net.copy(src, ux_o.at[k - 1, view, :], i, i, tx=peer[1] if k == 3 else peer[k])

    def ex_cp(k, b, half):
        i = x_id + half * 12 + (k - 1) * 4 + b
        view = ds(b * sub + half * hs, hs)
        return net.copy(wg_v.at[ds(tokens + b * sub + half * hs, hs), pl.ds(k * dt, dt)], ex_o.at[k - 1, view, :], i, i, tx=peer[k])

    gate = WeightGather(net, wg, wg_v, pos, True, 2)
    up = WeightGather(net, wu, wu_v, pos, True, 2)
    down = WeightGather(net, wd, wd_v, pos, False, 4, 1)
    q_w = WeightGather(net, wq, wq_v.at[pl.ds(0, q_width), :], pos, False, 1)
    kv_w = WeightGather(net, wkv, wq_v.at[pl.ds(q_width, width - q_width), :], pos, False, 1)
    ag = LineGather(net, n_v, sub, z)
    rsc = LineScatter(net, p_v, rbuf, sub, z)
    rs2 = [LineScatter(net, n_v, rbuf2, sub, z, c * cs, cs) for c in range(8)]
    ag2 = [LineGather(net, e_v, sub, z, c * cs, cs) for c in range(8)]

    for k in far_first:
        h_cp(k).start()
    gain_in.wait()
    both = g_v[...].astype(F32)
    gin[...] = jnp.broadcast_to(both[0:1, :], gin.shape)
    gin[1:2, :] = both[1:2, :]
    g_own = net.here(gin, gains.at[:, pl.ds(0, dt)])
    h_own = net.here(hid.at[ds(tx * sub, sub), :], rows.at[:, pl.ds(0, dt)])
    for w in (q_w, kv_w, gate, up, down):
        w.start_local()
    for k in far_first:
        g_cp(k).start()
    for c in turn_in:
        c.wait()

    @pl.loop(0, tokens // 128)
    def _(i):
        part = 128
        cos_c, sin_c = ds(i * part, part), ds(tokens + i * part, part)
        q_r, kv_r = pl.ds(0, 128), pl.ds(128, 128)
        angles = inv_v[...] * pos_v[:, cos_c].astype(F32)
        dres_v[q_r, sin_c] = jnp.sin(angles)
        dres_v[q_r, cos_c] = jnp.cos(angles)

        @pl.when(z < 2)
        def _():
            dres_v[kv_r, cos_c] = dres_v[q_r, cos_c]
            dres_v[kv_r, sin_c] = dres_v[q_r, sin_c]

        @pl.when(z >= 2)
        def _():
            dres_v[kv_r, cos_c] = jnp.ones((128, part), F32)
            dres_v[kv_r, sin_c] = jnp.zeros((128, part), F32)

    tab_out = net.here(dres_v.at[pl.ds(0, 256), pl.ds(0, 2 * tokens)], tab_o)
    turn(p_v, width, q_width, tokens, dres_v, swap_v, True)
    for k in far_first:
        e_cp(k, tx).start()
    e_own = net.here(p_v.at[pl.ds(0, width), ds(tx * sub, sub)], eq_v.at[:, ds(tx * sub, sub)])
    for w in (q_w, kv_w, gate, up, down):
        w.start_y()
    for k in far_first:
        d_cp(k).start()
    d_own = net.here(dh2h.at[ds(tx * sub, sub), :], dh2_v.at[:, pl.ds(0, dt)])

    for k in far_first:
        g_cp(k).wait_recv()
        h_cp(k).wait_recv()
    g_own.wait()
    h_own.wait()

    @pl.loop(0, sub // 16)
    def _(r):
        x = rows[ds(r * 16, 16), :].astype(F32)
        inv = lax.rsqrt(jnp.sum(x * x, axis=1, keepdims=True) / dim + NORM_EPS)
        n_v[ds(z * sub + r * 16, 16), :] = (x * inv * gains[0:1, :]).astype(BF16)

    ag.start()
    outs = [net.here(rows, h_o), net.here(gains, g_o)]
    for k in far_first:
        e_cp(k, peer[k]).wait_recv()
    e_own.wait()
    ag.step1()
    for w in (q_w, kv_w):
        w.y_event(0)
    for w in (q_w, kv_w):
        w.x_event(0)
    for w in (q_w, kv_w):
        w.finish_local()
        w.finish(0)
    for k in far_first:
        e_cp(k, tx).wait_send()

    def n2_block(b):
        @pl.loop(0, dim // dtile)
        def _(j):
            cols = ds(j * dtile, dtile)
            p_v[ds(b * sub, sub), cols] = dot(eq_v[:, ds(b * sub, sub)], wq_v[:, cols], ROWS_ROWS).astype(BF16)

    @pl.loop(0, 4)
    def _(i):
        n2_block(pick(3 - i, z))
        for step in range(3):
            pl.when(i == step)(lambda step=step: rsc.send_end(2 - step))
        pl.when(i == 0)(lambda: gate.y_event(0))

    wide = ff // 2

    def gate_part(b, c):
        cols = pl.ds(c * wide, wide)
        a_v[ds(b * sub, sub), cols] = dot(n_v[ds(b * sub, sub), :], wg_v[:, cols]).astype(BF16)

    def up_part(b, c):
        cols = pl.ds(c * wide, wide)
        bb = dot(n_v[ds(b * sub, sub), :], wu_v[:, cols]).astype(BF16)
        b_v[ds(b * sub, sub), cols] = bb
        aa = a_v[ds(b * sub, sub), cols].astype(F32)
        wg_v[ds(b * sub, sub), cols] = (aa * jax.nn.sigmoid(aa) * bb.astype(F32)).astype(BF16)

    def down_part(b, j):
        cols = pl.ds(j * (dim // 2), dim // 2)
        n_v[ds(b * sub, sub), cols] = dot(wg_v[ds(b * sub, sub), :], wd_v[:, cols]).astype(BF16)

    outs += [net.here(wq_v, wq_o), net.here(eq_v, eq_o)]
    gate.finish_local()
    gate.y_event(1)
    ag.step2()
    ag.step3_mid()
    gate.x_event(0)
    gate.finish(0)

    @pl.loop(0, 3)
    def _(i):
        gate_part(pick(i, z), 0)

    up.y_event(0)
    gate.x_event(1)
    rsc.send_mid(2)
    gate.finish(1)
    wg_out = net.here(wg_v, wg_o)

    @pl.loop(0, 3)
    def _(i):
        gate_part(pick(i, z), 1)

    up.finish_local()
    up.y_event(1)
    up.x_event(0)
    up.finish(0)
    ag.step3_end()

    @pl.loop(0, 2)
    def _(c):
        cols = ds(c * wide, wide)
        b = pick(3, z)
        a_v[ds(b * sub, sub), cols] = dot(n_v[ds(b * sub, sub), :], wg_v[:, cols]).astype(BF16)

    wg_out.wait()
    n_out = net.here(n_v, n_o)

    @pl.loop(0, 4)
    def _(i):
        pl.when(i == 1)(lambda: down.y_event(0))
        pl.when(i == 2)(lambda: down.y_event(1))
        pl.when(i == 3)(lambda: up.x_event(1))
        up_part(pick(i, z), 0)

    def up_events_1():
        rsc.send_mid(1)
        rsc.send_mid(0)
        down.x_event(0)

    def up_events_2():
        down.y_event(2)

    def up_events_3():
        down.y_event(3)
        down.x_event(1)

    up.finish(1)
    outs.append(net.here(wu_v, wu_o))

    @pl.loop(0, 4)
    def _(i):
        pl.when(i == 1)(up_events_1)
        pl.when(i == 2)(up_events_2)
        pl.when(i == 3)(up_events_3)
        b = pick(i, z)
        up_part(b, 1)
        ux_cp(2, b).start()
        ux_cp(1, b).start()

    outs.append(net.here(u_v, u_o))
    ag.drain()
    gate.drain()
    n_out.wait()
    down.finish_local()

    @pl.loop(0, 4)
    def _(i):
        pl.when(i == 2)(lambda: down.x_event(2))
        pl.when(i == 3)(lambda: down.x_event(3))
        down_part(pick(3 - i, z), 0)

    for ch in range(4):
        down.finish(ch)

    @pl.loop(0, 4)
    def _(i):
        down_part(pick(3 - i, z), 1)
        for step in range(3):
            pl.when(i == step)(lambda step=step: rs2[0].send_end(2 - step))

    for c in range(1, 8):
        for i in (2, 1, 0):
            rs2[c].send_end(i)
    dg_v[...] = jnp.zeros_like(dg_v)
    step = 16

    def norm_chunk(c):
        @pl.loop(0, cs // step)
        def _(r):
            at = c * cs + r * step
            view, mine, far = ds(at, step), ds(z * sub + at, step), ds(4 * sub + at, step)

            def whole(part, got):
                right = jnp.where(z < 3, got[mine, :].astype(F32), 0.0)
                left = jnp.where(z > 0, got[far, :].astype(F32), 0.0)
                return part[mine, :].astype(F32) + right + left

            resid = (rows[view, :].astype(F32) + whole(n_v, rbuf2)).astype(BF16)
            dy = whole(p_v, rbuf)
            res_v[view, :] = resid
            x = resid.astype(F32)
            inv = lax.rsqrt(jnp.sum(x * x, axis=1, keepdims=True) / dim + NORM_EPS)
            xhat = x * inv
            gain = gains[1:2, :]
            n2_v[view, :] = (xhat * gain).astype(BF16)
            part = dy * xhat
            dg_v[...] += part[:8] + part[8:]
            inner = jnp.sum(part * gain, axis=1, keepdims=True) / dim
            dres = dh2_v[view, :].astype(F32) + inv * (dy * gain) - xhat * (inv * inner)
            dres_v[view, pl.ds(0, dim)] = dres
            wg_v[ds(tokens + z * sub + at, step), :] = dres.astype(BF16)

    def spread(b, half):
        for k in far_first:
            ex_cp(k, b, half).start()

    def back_tile(b, j):
        view, cols = ds(b * sub, sub), ds(j * (ff // 4), ff // 4)
        du = dot(wg_v[ds(tokens + b * sub, sub), :], wd_v[ds(j * (ff // 4), ff // 4), :], NT_DIMS)
        aa = a_v[view, cols].astype(F32)
        bb = b_v[view, cols].astype(F32)
        sig = jax.nn.sigmoid(aa)
        a_v[view, cols] = (du * bb * sig * (1.0 + aa * (1.0 - sig))).astype(BF16)
        b_v[view, cols] = (du * aa * sig).astype(BF16)

    def scatter(i, c):
        return lambda: rs2[c].send_mid(i)

    def gathered(i, c):
        def go():
            ag2[c].take(i)
            pl.when(mid(z))(lambda: ag2[c].forward(i))
            if c % 4 == 3:
                spread(ag.slots[i], c // 4)
        return go

    def run(ops):
        def go():
            for op in ops:
                op()
        return go

    before_mid = (
        (scatter(2, 0), scatter(1, 0), scatter(0, 0)),
        (scatter(2, 1), scatter(1, 1), gathered(1, 0), scatter(0, 1), scatter(2, 2)),
        (scatter(1, 2), scatter(0, 2), gathered(1, 1), scatter(2, 3)),
        (scatter(1, 3), scatter(0, 3), gathered(1, 2), scatter(2, 4)),
        (scatter(1, 4), scatter(0, 4), gathered(1, 3), scatter(2, 5)),
        (scatter(1, 5), scatter(0, 5), gathered(1, 4), scatter(2, 6)),
        (scatter(1, 6), scatter(0, 6), gathered(1, 5), scatter(2, 7)),
        (scatter(1, 7), scatter(0, 7), gathered(1, 6), gathered(0, 0)))
    before_end = (
        (),
        (gathered(0, 0), gathered(1, 0)),
        (gathered(0, 1),),
        (gathered(1, 1), gathered(0, 2)),
        (gathered(1, 2), gathered(0, 3)),
        (gathered(1, 3), gathered(0, 4)),
        (gathered(1, 4), gathered(0, 5)),
        (gathered(1, 5), gathered(0, 6)))
    after_mid = {1: (gathered(0, 1),),
                 2: (gathered(2, 0),),
                 3: (gathered(0, 2),),
                 4: (gathered(1, 7),),
                 5: (gathered(0, 3),),
                 6: (gathered(2, 1),),
                 7: (gathered(0, 4),),
                 8: (gathered(2, 2), gathered(0, 5), gathered(2, 3), gathered(0, 6), gathered(2, 4), gathered(0, 7)),
                 10: (gathered(2, 5),),
                 12: (gathered(2, 6), gathered(2, 7))}
    after_end = {2: (gathered(1, 6),),
                 4: (gathered(0, 7),),
                 7: (gathered(2, 0),),
                 8: (gathered(1, 7),),
                 11: (gathered(2, 1),),
                 12: (gathered(2, 2), gathered(2, 3), gathered(2, 4), gathered(2, 5), gathered(2, 6), gathered(2, 7))}

    for c in range(8):
        pl.when(mid(z))(run(before_mid[c]))
        pl.when(end(z))(run(before_end[c]))
        if c == 0:
            rsc.finish()
            for k in far_first:
                d_cp(k).wait_recv()
            d_own.wait()
            tab_out.wait()
        rs2[c].finish()
        norm_chunk(c)
        ag2[c].start()
        if c % 4 == 3:
            spread(z, c // 4)
            for k in far_first:
                o_cp(k, tx, c // 4).start()

    outs += [net.here(res_v.at[:, pl.ds(0, dt)], home_o.at[ds(tx * sub, sub), :]), net.here(n2_v, n2_o), net.here(dres_v.at[pl.ds(0, sub), pl.ds(0, dim)], dres_o), net.here(dg_v, dg_o)]
    rsc.drain()
    for c in range(8):
        rs2[c].drain()
    middle = (z + 1) // 2 % 2

    def u_forward():
        for b in range(4):
            ux_cp(2, b).wait_recv()
            ux_cp(3, b).start()

    @pl.loop(0, 16)
    def _(t):
        for at, ops in after_mid.items():
            pl.when(jnp.logical_and(t == at, mid(z)))(run(ops))
        for at, ops in after_end.items():
            pl.when(jnp.logical_and(t == at, end(z)))(run(ops))
        pl.when(t == 8)(u_forward)
        i = t // 4
        inner = (i + 1) // 2 % 2
        back_tile(pick(i + middle * inner * (3 - 2 * i), z), t % 4)

    outs.append(net.here(e_v, e_o))
    outs += [net.here(a_v, da_o), net.here(b_v, db_o)]

    def down_tile(k, j):
        return dot(wg_v[pl.ds(0, tokens), pl.ds(split, ff - split)], wg_v[pl.ds(tokens, tokens), ds(k * dt + j * (dt // 2), dt // 2)], ROWS_ROWS)

    quarter = [rbuf.at[pl.ds(0, ff - split), pl.ds(i * dt, dt)] for i in range(4)]
    part_d = GradReduce(net, peer, down_tile, 2, quarter[0], quarter[1], quarter[2], quarter[3], d2_o, d0_o, None, dc_o, None)
    part_d.step3()
    part_d.step1()
    part_d.step2()
    outs.append(net.here(quarter[2], dc_o))
    for k in far_first:
        o_cp(k, peer[k], 0).wait_recv()
        o_cp(k, peer[k], 1).wait_recv()
        for b in range(4):
            ex_cp(k, b, 0).wait_recv()
            ex_cp(k, b, 1).wait_recv()
    for b in range(4):
        ux_cp(1, b).wait_recv()
        ux_cp(3, b).wait_recv()
    for c in outs:
        c.wait()
    for k in far_first:
        g_cp(k).wait_send()
        h_cp(k).wait_send()
        d_cp(k).wait_send()
        o_cp(k, tx, 0).wait_send()
        o_cp(k, tx, 1).wait_send()
        for b in range(4):
            ux_cp(k, b).wait_send()
            ex_cp(k, b, 0).wait_send()
            ex_cp(k, b, 1).wait_send()
    for w in (q_w, kv_w, up, down):
        w.drain()
    for c in range(8):
        ag2[c].drain()
    part_d.cp(1).wait_recv()
    part_d.sent_locally()


def call_ab(hid, eqh, ekvh, pos, inv, swap, dh2h, wg, wu, wd, wq, wkv, g):
    tokens, dt = hid.shape
    sub, dim, ff, q_width = tokens // 4, dt * 4, wg.shape[1], wq.shape[0]
    width = q_width + wkv.shape[0]
    s = jax.ShapeDtypeStruct
    tok_ff, tok_d, row = s((tokens, ff), BF16), s((tokens, dim), BF16), s((sub, dim), BF16)
    shapes = (tok_d, tok_ff, tok_ff, tok_ff, s((dim, ff), BF16), s((dim, ff), BF16), s((width, dim), BF16), s((width, tokens), BF16),
              row, s((8, dim), F32), tok_d, row, s((sub, dim), F32), s((tokens, dt), BF16), s((8, dim), F32),
              s((3, tokens, down_split(ff)), BF16), s((3, tokens, dt), BF16), s((256, 2 * tokens), F32)) + (s((ff - down_split(ff), dt), BF16),) * 3
    vrow, vtok, vff = VMEM((sub, dim), BF16), VMEM((tokens, dim), BF16), VMEM((tokens, ff), BF16)
    return pl.pallas_call(
        functools.partial(kernel_ab, q_width), out_shape=shapes, in_specs=[ANY] * 13, out_specs=[ANY] * len(shapes),
        scratch_shapes=[
            vrow, vrow, vrow, vrow, VMEM((max(sub, 256), max(dim, 2 * tokens)), F32), vtok, vff, vff, VMEM((dim, ff), BF16), VMEM((dim, ff), BF16), VMEM((ff, dim), BF16),
            VMEM((width, dim), BF16), VMEM((width, tokens), BF16), vtok, VMEM((5 * sub, dim), BF16), VMEM((5 * sub, dim), BF16),
            VMEM((8, dim), F32), VMEM((8, dim), F32), VMEM((128, 128), BF16), VMEM((1, tokens), jnp.int32), VMEM((128, 128), F32),
            VMEM((2, dt), BF16), VMEM((8, dt), F32),
            pltpu.SemaphoreType.DMA((236,)), pltpu.SemaphoreType.DMA((236,)), pltpu.SemaphoreType.DMA((48,))],
        compiler_params=pltpu.CompilerParams(collective_id=0, has_side_effects=True, vmem_limit_bytes=VMEM_LIMIT),
        cost_estimate=pl.CostEstimate(flops=20 * tokens * dim * ff, bytes_accessed=100000000, transcendentals=0), name="phase_ab",
    )(hid, eqh, ekvh, pos, inv, swap, dh2h, wg, wu, wd, wq, wkv, g)


def kernel_c(q_width, da_h, db_h, wg_h, wu_h, n_h, u_h, ux_h, e_h, ex_h, n2_h, eq_h, wq_h, h_h, dres_h, g_h, dga_h, tabh, swaph, d0, dc,
             wgo, wgy, wuo, wuy, wdo, wqo, wqy, wvo, wvy, q_o, kv_o, dh_o, dg_o, g2, g0, u2, u0, q2, q0, v2, v0, qx, dy,
             wg_v, wu_v, da_v, db_v, n_v, p_v, rbuf, n2_v, st3, st1, cross_g, cross_u, stage, tiles_v, dres_v, wq_v, eq_v,
             gains, dg_v, dgr, dgz, tab_v, swap_v, send, recv, local):
    dp, z, tx, peer = places()
    tokens, ff = da_v.shape
    sub, dim = dres_v.shape
    dt = dim // 4
    width = eq_v.shape[0]
    tile = ff // 4
    dtile = min(512, dim)
    qt = min(256, tile)
    far_first = (2, 3, 1)
    net = Wires(send, recv, local)
    n2_in = net.here(n2_h, n2_v.at[ds(z * sub, sub), :])
    first = [net.here(n_h, n_v), net.here(da_h, da_v)]
    second = [net.here(db_h, db_v), net.here(wg_h, wg_v), net.here(wu_h, wu_v)]
    third = [net.here(wq_h, wq_v), net.here(eq_h, eq_v), net.here(dres_h, dres_v), net.here(g_h, gains),
             net.here(dga_h, dg_v.at[pl.ds(8, 8), :]), net.here(tabh, tab_v), net.here(swaph, swap_v)]
    sem = pltpu.get_barrier_semaphore()
    zs = tuple((z + i) % 4 for i in range(4))
    for i in (1, 2, 3):
        pl.semaphore_signal(sem, inc=1, device_id={"tx": peer[i]}, device_id_type=MESH)
        pl.semaphore_signal(sem, inc=1, device_id={"ty": zs[i]}, device_id_type=MESH)
    pl.semaphore_wait(sem, 6)
    rsc = LineScatter(net, p_v, rbuf, sub, z)
    ag = LineGather(net, n2_v, sub, z)
    q_id, h_id, t_id, z_id = net.take(4), net.take(4), net.take(4), net.take(4)

    def grad_tile(lhs, rhs, w):
        def go(k, j):
            cols = pl.ds(j * w, w) if isinstance(j, int) else ds(j * w, w)
            return dot(lhs[:, pl.ds(k * dt, dt)], rhs[:, cols], ROWS_ROWS)
        return go

    gate = GradReduce(net, peer, grad_tile(n_v, da_v, tile), ff // tile, st3, st1, cross_g, stage, g2, g0, wgy, wgo, tiles_v)
    up = GradReduce(net, peer, grad_tile(n_v, db_v, tile), ff // tile, st3, st1, cross_u, stage, u2, u0, wuy, wuo, tiles_v)
    d_id = net.take(1)

    def dy_cp():
        return net.copy(dc, dy, d_id, d_id, tx=peer[2])

    dy_cp().start()

    def head_grad(first, rows, got2, got0, got_y, out):
        corner = [da_v.at[pl.ds(first, rows), pl.ds(c * dt, dt)] for c in range(4)]

        def tile_of(k, j):
            return dot(eq_v[pl.ds(first, rows), :], n2_v[:, ds(k * dt + j * qt, qt)])

        return GradReduce(net, peer, tile_of, dt // qt, *corner, got2, got0, got_y, out, tiles_v)

    heads = (head_grad(0, q_width, q2, q0, wqy, wqo), head_grad(q_width, width - q_width, v2, v0, wvy, wvo))

    def dn_block(b):
        rows = ds(b * sub, sub)

        @pl.loop(0, dim // dtile)
        def _(j):
            wr = ds(j * dtile, dtile)
            p_v[rows, wr] = (dot(da_v[rows, :], wg_v[wr, :], NT_DIMS) + dot(db_v[rows, :], wu_v[wr, :], NT_DIMS)).astype(BF16)

    n2_in.wait()
    ag.start()
    for c in first:
        c.wait()
    gate.step3()
    gate.step1()
    gate.step2()
    gate.send()
    for c in second:
        c.wait()

    @pl.loop(0, 4)
    def _(i):
        @pl.when(i == 1)
        def _():
            gate.sent_locally()
            up.step3()
            up.step1()
            ag.step1()

        dn_block(pick(3 - i, z))
        for step in range(3):
            pl.when(i == step)(lambda step=step: rsc.send_end(2 - step))

    up.step2()
    up.send()
    rsc.send_mid(2)
    ag.step2()
    ag.step3_mid()
    up.sent_locally()
    h_in = net.here(h_h, st3.at[pl.ds(0, sub), :])
    gate.step0(st1)
    gate.sent()

    e_in = [net.here(e_h.at[:, pl.ds(0, dt)], wu_v.at[pl.ds(0, tokens), pl.ds(0, dt)])]
    for k in (1, 2, 3):
        e_in.append(net.here(ex_h.at[k - 1], wu_v.at[pl.ds(0, tokens), pl.ds(k * dt, dt)]))

    piece = ff // 8
    exchanged, n_pieces = down_split(ff) // piece, 8

    def u_place(j, k):
        return wg_v.at[pl.ds((j % 2) * tokens, tokens), pl.ds(k * piece, piece)]

    def sums(j, n):
        return stage.at[pl.ds((j % 2) * piece, piece), pl.ds(n * dt, dt)]

    def u_load(j):
        cols = pl.ds(j * piece, piece)
        if j < exchanged:
            return [net.here(u_h.at[:, cols] if k == 0 else ux_h.at[k - 1, :, cols], u_place(j, k)) for k in range(4)]
        rows = pl.ds((j - exchanged) * piece, piece)
        return [net.here(u_h.at[:, cols], u_place(j, 0)), net.here(d0.at[rows, :], sums(j, 0)), net.here(dy.at[rows, :], sums(j, 1))]

    loads, stores = {}, {}

    def down_run(js):
        for j in js:
            for c in loads.pop(j):
                c.wait()
            if j >= 2:
                stores.pop(j - 2).wait()
            acc = None if j < exchanged else sums(j, 0)[...].astype(F32) + sums(j, 1)[...].astype(F32)
            for k in range(4 if j < exchanged else 1):
                part = dot(u_place(j, k)[...], wu_v[pl.ds(0, tokens), pl.ds(k * dt, dt)], ROWS_ROWS)
                acc = part if acc is None else acc + part
            place = tiles_v.at[j % 2, pl.ds(0, piece), pl.ds(0, dt)]
            tiles_v[j % 2, pl.ds(0, piece), pl.ds(0, dt)] = acc
            stores[j] = net.here(place, wdo.at[pl.ds(j * piece, piece), :])
            if j + 2 < n_pieces:
                loads[j + 2] = u_load(j + 2)

    loads[0], loads[1] = u_load(0), u_load(1)
    rsc.send_mid(1)
    rsc.send_mid(0)
    for c in e_in:
        c.wait()
    down_run((0, 1))
    for c in third:
        c.wait()
    ag.step3_end()

    @pl.loop(0, width // qt)
    def _(j):
        wu_v[ds(tokens + j * qt, qt), pl.ds(0, tokens)] = dot(wq_v[ds(j * qt, qt), :], n2_v[...], NT_DIMS).astype(BF16)

    def q_cp(k, block):
        return net.copy(wu_v.at[pl.ds(tokens, width), ds(peer[k] * sub, sub)], qx.at[:, ds(block * sub, sub)], q_id + k, q_id + k, tx=peer[k])

    for k in far_first:
        q_cp(k, tx).start()
    q_own = net.here(wu_v.at[pl.ds(tokens, width), ds(tx * sub, sub)], qx.at[:, ds(tx * sub, sub)])
    for part in heads:
        part.step3()
        part.step1()
    dy_cp().wait_recv()
    for part in heads:
        part.step2()
        part.send()
    down_run(range(2, n_pieces))
    h_in.wait()
    rsc.finish()
    dg_v[pl.ds(0, 8), :] = jnp.zeros((8, dim), F32)
    step = 16

    @pl.loop(0, sub // step)
    def _(r):
        view, mine, far = ds(r * step, step), ds(z * sub + r * step, step), ds(4 * sub + r * step, step)
        right = jnp.where(z < 3, rbuf[mine, :].astype(F32), 0.0)
        left = jnp.where(z > 0, rbuf[far, :].astype(F32), 0.0)
        dy = p_v[mine, :].astype(F32) + right + left
        x = st3[view, :].astype(F32)
        inv = lax.rsqrt(jnp.sum(x * x, axis=1, keepdims=True) / dim + NORM_EPS)
        xhat = x * inv
        gain = gains[0:1, :]
        part = dy * xhat
        dg_v[pl.ds(0, 8), :] += part[:8] + part[8:]
        inner = jnp.sum(part * gain, axis=1, keepdims=True) / dim
        st1[view, :] = (dres_v[view, :] + inv * (dy * gain) - xhat * (inv * inner)).astype(BF16)

    def h_cp(k, block):
        return net.copy(st1.at[pl.ds(0, sub), pl.ds(k * dt, dt)], dh_o.at[ds(block * sub, sub), :], h_id + k, h_id + k, tx=peer[k])

    def t_cp(k):
        return net.copy(dg_v.at[:, pl.ds(k * dt, dt)], dgr.at[k], t_id + k, t_id + k, tx=peer[k])

    def z_cp(i):
        return net.copy(dgr.at[0], dgz.at[i], z_id + i, z_id + i, ty=zs[i])

    for k in far_first:
        t_cp(k).start()
    for k in far_first:
        h_cp(k, tx).start()
    h_own = net.here(st1.at[pl.ds(0, sub), pl.ds(0, dt)], dh_o.at[ds(tx * sub, sub), :])
    up.sent()
    for c in stores.values():
        c.wait()
    up.step0(cross_g)
    for k in far_first:
        q_cp(k, peer[k]).wait_recv()
    q_own.wait()
    turned = wu_v.at[pl.ds(tokens, width), pl.ds(tokens, tokens)]
    net.here(qx, turned).wait()
    turn(turned, width, q_width, tokens, tab_v, swap_v, False)
    q_out = net.here(wu_v.at[pl.ds(tokens, q_width), pl.ds(tokens, tokens)], q_o)
    kv_out = net.here(wu_v.at[pl.ds(tokens + q_width, width - q_width), pl.ds(tokens, tokens)], kv_o)
    heads[0].step0(cross_g.at[pl.ds(0, q_width), pl.ds(0, dt)])
    heads[1].step0(cross_g.at[pl.ds(0, width - q_width), pl.ds(dt, dt)])
    for k in far_first:
        t_cp(k).wait_recv()
    dgr[0] = dg_v[:, pl.ds(0, dt)] + dgr[1] + dgr[2] + dgr[3]
    for i in (1, 2, 3):
        z_cp(i).start()
    for i in (1, 2, 3):
        z_cp(i).wait_recv()
    dgz[0] = dgr[0] + dgz[1] + dgz[2] + dgz[3]
    dg_out = net.here(dgz.at[0], dg_o)
    for k in far_first:
        h_cp(k, peer[k]).wait_recv()
    for c in (q_out, kv_out, dg_out, h_own):
        c.wait()
    dy_cp().wait_send()
    for part in heads:
        part.sent_locally()
        part.sent()
    for k in far_first:
        q_cp(k, tx).wait_send()
        h_cp(k, tx).wait_send()
        t_cp(k).wait_send()
        z_cp(k).wait_send()
    ag.drain()
    rsc.drain()


def call_c(q_width, *args):
    tokens, ff = args[0].shape
    sub, dim = args[9].shape
    dt, width = dim // 4, args[10].shape[0]
    rest = width - q_width
    tile = ff // 4
    s = jax.ShapeDtypeStruct
    wf, wb = s((dt, ff), F32), s((dt, ff), BF16)
    qf, qb, vf, vb = s((q_width, dt), F32), s((q_width, dt), BF16), s((rest, dt), F32), s((rest, dt), BF16)
    shapes = (wf, wb, wf, wb, s((ff, dt), F32), qf, qb, vf, vb, s((q_width, tokens), BF16), s((rest, tokens), BF16), s((tokens, dt), BF16), s((16, dt), F32),
              wb, wb, wb, wb, qb, qb, vb, vb, s((width, tokens), BF16), s((ff - down_split(ff), dt), BF16))
    return pl.pallas_call(
        functools.partial(kernel_c, q_width), out_shape=shapes, in_specs=[ANY] * len(args), out_specs=[ANY] * len(shapes),
        scratch_shapes=[
            VMEM((dim, ff), BF16), VMEM((dim, ff), BF16), VMEM((tokens, ff), BF16), VMEM((tokens, ff), BF16), VMEM((tokens, dim), BF16),
            VMEM((tokens, dim), BF16), VMEM((5 * sub, dim), BF16), VMEM((tokens, dim), BF16),
            VMEM((dt, ff), BF16), VMEM((dt, ff), BF16), VMEM((dt, ff), BF16), VMEM((dt, ff), BF16), VMEM((dt, ff), BF16),
            VMEM((2, max(dt, tile), max(dt, tile)), F32), VMEM((sub, dim), F32), VMEM((width, dim), BF16), VMEM((width, tokens), BF16),
            VMEM((8, dim), F32), VMEM((16, dim), F32), VMEM((4, 16, dt), F32), VMEM((4, 16, dt), F32), VMEM((256, 2 * tokens), F32), VMEM((128, 128), BF16),
            pltpu.SemaphoreType.DMA((48,)), pltpu.SemaphoreType.DMA((48,)), pltpu.SemaphoreType.DMA((96,))],
        compiler_params=pltpu.CompilerParams(collective_id=2, has_side_effects=True, vmem_limit_bytes=VMEM_LIMIT),
        cost_estimate=pl.CostEstimate(flops=20 * tokens * dim * ff, bytes_accessed=100000000, transcendentals=0), name="phase_c",
    )(*args)


def kernel_out(pieces, n, *refs):
    ins, outs, bufs = refs[:n], refs[n + 1:2 * n + 1], refs[2 * n + 3:3 * n + 3]
    gains, gain_a, gain_b = refs[n], refs[2 * n + 1], refs[2 * n + 2]
    read, write = refs[3 * n + 3:]

    def part(ref, i, c):
        rows = ref.shape[0] // pieces[i]
        return ref.at[pl.ds(c * rows, rows), :]

    jobs = [(i, c) for i in range(n) for c in range(pieces[i])]
    get = [pltpu.make_async_copy(part(ins[i], i, c), part(bufs[i], i, c), read.at[m]) for m, (i, c) in enumerate(jobs)]
    put = [pltpu.make_async_copy(part(bufs[i], i, c), part(outs[i], i, c), write.at[m]) for m, (i, c) in enumerate(jobs)]
    for g in get:
        g.start()
    gain_a[...] = jnp.sum(gains[pl.ds(0, 8), :], axis=0, keepdims=True)
    gain_b[...] = jnp.sum(gains[pl.ds(8, 8), :], axis=0, keepdims=True)
    for g, p in zip(get, put):
        g.wait()
        p.start()
    for p in put:
        p.wait()


def call_out(results, gains):
    n = len(results)
    pieces = tuple(max(1, x.size * x.dtype.itemsize // 2**20) for x in results)
    row = jax.ShapeDtypeStruct((1, gains.shape[1]), F32)
    whole = pl.BlockSpec(memory_space=pltpu.VMEM)
    return pl.pallas_call(
        functools.partial(kernel_out, pieces, n), out_shape=tuple(jax.ShapeDtypeStruct(x.shape, x.dtype) for x in results) + (row, row),
        in_specs=[ANY] * n + [whole], out_specs=[ANY] * n + [whole, whole],
        scratch_shapes=[VMEM(x.shape, x.dtype) for x in results] + [pltpu.SemaphoreType.DMA((sum(pieces),))] * 2,
        compiler_params=pltpu.CompilerParams(vmem_limit_bytes=VMEM_LIMIT),
        cost_estimate=pl.CostEstimate(flops=1000000, bytes_accessed=35000000, transcendentals=0), name="results",
    )(*results, gains)


def solution(mesh):
    def local_step(hidden, positions, g_ffn, w_gate, w_up, w_down, g_attn, w_q, w_kv, grad_h2, grad_q, grad_kv):
        tokens, dt = hidden.shape
        q_heads, head_dim = w_q.shape[1:]
        q_width = q_heads * head_dim

        lane = np.arange(128)
        inv_freq = ROPE_BASE ** (-(lane % head_dim // 2 * 2).astype(np.float32) / head_dim)
        inv_freq = jnp.asarray(np.tile(inv_freq.astype(np.float32)[:, None], (1, 128)))
        swap = np.zeros((128, 128), np.float32)
        swap[lane, lane ^ 1] = np.where(lane % 2 == 0, -1.0, 1.0)
        swap = jnp.asarray(swap, BF16)

        def heads_first(x):
            return x.transpose(1, 2, 0).reshape(-1, x.shape[0])

        def heads_last(x):
            return x.reshape(-1, head_dim, x.shape[1]).transpose(2, 0, 1)

        (normed_all, grad_gate, grad_up, u_all, gate_w, up_w, w_qkv, back_all, h_rows, gains, res_all, normed2, grad_res, resid_out, gattn8,
         u_other, e_other, table, _, wd_zero, wd_cross) = call_ab(
             hidden, heads_first(grad_q), heads_first(grad_kv), positions.reshape(1, tokens), inv_freq, swap, grad_h2,
             w_gate, w_up, w_down, heads_first(w_q), heads_first(w_kv), jnp.where(jnp.arange(2)[:, None] == 0, g_ffn[None, :], g_attn[None, :]))
        (grad_wgate, _, grad_wup, _, grad_wdown, grad_wq, _, grad_wkv, _, q_out, kv_out, grad_hidden, gain_grads, *_) = call_c(
            q_width, grad_gate, grad_up, gate_w, up_w, normed_all, u_all, u_other, res_all, e_other, normed2, back_all, w_qkv,
            h_rows, grad_res, gains, gattn8, table, swap, wd_zero, wd_cross)
        (resid_out, grad_wgate, grad_wup, grad_wdown, grad_wq, grad_wkv, q_out, kv_out, grad_hidden, grad_gffn, grad_gattn) = call_out(
            (resid_out, grad_wgate, grad_wup, grad_wdown, grad_wq, grad_wkv, q_out, kv_out, grad_hidden), gain_grads)
        q_out, kv_out, grad_wq, grad_wkv = (heads_last(x) for x in (q_out, kv_out, grad_wq, grad_wkv))
        grad_gffn, grad_gattn = grad_gffn[0], grad_gattn[0]
        return (resid_out, q_out, kv_out, grad_hidden, grad_gffn, grad_gattn, grad_wgate, grad_wup, grad_wdown, grad_wq, grad_wkv)

    row_spec = P(("dp", "ty"), "tx")
    head_spec = P(("dp", "tx"), "ty", None)
    in_specs = (row_spec, P(("dp", "tx")), P("tx"), P("tx", "ty"), P("tx", "ty"), P("ty", "tx"), P("tx"), P("tx", "ty", None), P("tx", "ty", None), row_spec, head_spec, head_spec)
    out_specs = (row_spec, head_spec, head_spec, row_spec, P(("dp", "tx")), P(("dp", "tx")), P(("dp", "tx"), "ty"), P(("dp", "tx"), "ty"), P(("dp", "ty"), "tx"), head_spec, head_spec)
    return jax.shard_map(local_step, mesh=mesh, in_specs=in_specs, out_specs=out_specs, check_vma=False)
```

```python
import functools

import jax
import jax.numpy as jnp
import numpy as np
from jax import lax
from jax.experimental import pallas as pl
from jax.experimental.pallas import tpu as pltpu
from jax.sharding import PartitionSpec as P

NORM_EPS = 1e-5
ROPE_BASE = 10000.0
F32 = jnp.float32
BF16 = jnp.bfloat16


def dot(a, b, dims=(((1,), (0,)), ((), ()))):
    return lax.dot_general(a, b, dims, preferred_element_type=F32)


MESH = pl.DeviceIdType.MESH
ANY = pl.BlockSpec(memory_space=pl.ANY)
VMEM = pltpu.VMEM
NT_DIMS = (((1,), (1,)), ((), ()))
VMEM_LIMIT = 67000000


def ds(start, size, align=None):
    if isinstance(start, int):
        return pl.ds(start, size)
    return pl.ds(pl.multiple_of(start, align or size), size)


def mid(z):
    return jnp.logical_and(z > 0, z < 3)


def end(z):
    return jnp.logical_or(z == 0, z == 3)


def slots(z):
    return (z + 1 - 2 * (z % 2), 2 - z // 2, 3 - 3 * (z // 2))


def turn(x_ref, width, q_width, tokens, table_ref, swap_ref, back):
    step = min(256, tokens)

    @pl.loop(0, tokens // step)
    def _(r):
        cols = ds(r * step, step)
        for g in range(width // 128):
            rows = pl.ds(g * 128, 128)
            base = pl.ds(0 if g * 128 < q_width else 128, 128)
            x = x_ref[rows, cols]
            main = x.astype(F32) * table_ref[base, cols]
            side = dot(swap_ref[...], x) * table_ref[base, ds(tokens + r * step, step)]
            x_ref[rows, cols] = (main - side if back else main + side).astype(BF16)


def pick(i, z):
    s1, s2, s3 = slots(z)
    first, last = (3 - i) // 3, (i // 2) * (i % 2)
    return z * first + s1 * ((i % 2) * (1 - i // 2)) + s2 * ((i // 2) * (1 - i % 2)) + s3 * last


class Wires:
    def __init__(self, send, recv, local):
        self.send, self.recv, self.local = send, recv, local
        self.n_remote = 0
        self.n_local = 0

    def take(self, n=1):
        base = self.n_remote
        self.n_remote += n
        assert self.n_remote <= self.send.shape[0]
        return base

    def copy(self, src, dst, si, ri, **dev):
        return pltpu.make_async_remote_copy(
            src_ref=src, dst_ref=dst, send_sem=self.send.at[si], recv_sem=self.recv.at[ri],
            device_id=dev, device_id_type=MESH)

    def here(self, src, dst):
        i = self.n_local
        self.n_local += 1
        assert i < self.local.shape[0]
        c = pltpu.make_async_copy(src, dst, self.local.at[i])
        c.start()
        return c


def entry_barrier(axes, z):
    sem = pltpu.get_barrier_semaphore()
    for dev in axes:
        pl.semaphore_signal(sem, inc=1, device_id=dev, device_id_type=MESH)

    @pl.when(z > 0)
    def _():
        pl.semaphore_signal(sem, inc=1, device_id={"ty": z - 1}, device_id_type=MESH)

    @pl.when(z < 3)
    def _():
        pl.semaphore_signal(sem, inc=1, device_id={"ty": z + 1}, device_id_type=MESH)

    @pl.when(mid(z))
    def _():
        pl.semaphore_wait(sem, len(axes) + 2)

    @pl.when(end(z))
    def _():
        pl.semaphore_wait(sem, len(axes) + 1)


class LineGather:
    def __init__(self, net, buf, rows, z, off=0, part=None):
        self.net, self.buf, self.rows, self.z, self.off, self.part = net, buf, rows, z, off, part or rows
        self.base = net.take(8)
        self.slots = slots(z)

    def blk(self, b):
        return self.buf.at[ds(b * self.rows + self.off, self.part), :]

    def cp(self, b, side, target):
        return self.net.copy(self.blk(b), self.blk(b), self.base + side * 4 + b, self.base + b, ty=target)

    def start(self):
        z = self.z

        @pl.when(z < 3)
        def _():
            self.cp(z, 0, z + 1).start()

        @pl.when(z > 0)
        def _():
            self.cp(z, 1, z - 1).start()

    def take(self, i):
        b = self.slots[i]
        self.cp(b, 0, self.z).wait_recv()

    def forward(self, i):
        z, b = self.z, self.slots[i]
        target = 3 - z if i == 0 else 3 * (z - 1)
        self.cp(b, 0, target).start()

    def step1(self):
        self.take(0)

        @pl.when(mid(self.z))
        def _():
            self.forward(0)
            self.take(1)
            self.forward(1)

    def near_end(self):
        @pl.when(end(self.z))
        def _():
            self.take(0)

    def near_mid(self):
        @pl.when(mid(self.z))
        def _():
            self.take(1)
            self.forward(1)

    def far_mid(self):
        @pl.when(mid(self.z))
        def _():
            self.take(0)
            self.forward(0)

    def step2(self):
        @pl.when(end(self.z))
        def _():
            self.take(1)

    def step3_mid(self):
        @pl.when(mid(self.z))
        def _():
            self.take(2)
            self.forward(2)

    def step3_end(self):
        @pl.when(end(self.z))
        def _():
            self.take(2)

    def drain(self):
        z = self.z

        @pl.when(z < 3)
        def _():
            self.cp(z, 0, z + 1).wait_send()

        @pl.when(z > 0)
        def _():
            self.cp(z, 1, z - 1).wait_send()

        @pl.when(mid(z))
        def _():
            for i in range(3):
                self.cp(self.slots[i], 0, 3 - z if i == 0 else 3 * (z - 1)).wait_send()


class LineScatter:
    def __init__(self, net, part, rbuf, rows, z, off=0, size=None):
        self.net, self.part, self.rbuf, self.rows, self.z, self.off, self.size = net, part, rbuf, rows, z, off, size or rows
        self.base = net.take(5)
        self.slots = slots(z)
        one = (z % 2) * (1 - z // 2)
        self.dst = (self.slots[0] + (1 - z % 2) * (3 - z), self.slots[1] + 2 * one, self.slots[2])
        self.target = (z + 1 - 2 * (z % 2), 1 + z % 2, 1 + z % 2)

    def cp(self, i):
        return self.net.copy(
            self.part.at[self.view(self.slots[i]), :], self.rbuf.at[self.view(self.dst[i]), :],
            self.base + i, self.base + self.dst[i], ty=self.target[i])

    def view(self, b):
        return ds(b * self.rows + self.off, self.size)

    def wait_slot(self, s):
        view = self.rbuf.at[self.view(s), :]
        self.net.copy(view, view, self.base, self.base + s, ty=self.z).wait_recv()

    def send_end(self, i):
        @pl.when(end(self.z))
        def _():
            self.cp(i).start()

    def send_mid(self, i):
        @pl.when(mid(self.z))
        def _():
            b = self.slots[i]
            self.wait_slot(b)
            step = 16

            @pl.loop(0, self.size // step)
            def _(r):
                view = ds(b * self.rows + self.off + r * step, step)
                self.part[view, :] = (self.part[view, :].astype(F32) + self.rbuf[view, :].astype(F32)).astype(BF16)

            self.cp(i).start()

    def finish(self):
        z = self.z

        @pl.when(z < 3)
        def _():
            self.wait_slot(z)

        @pl.when(z > 0)
        def _():
            self.wait_slot(4)

    def drain(self):
        for i in range(3):
            self.cp(i).wait_send()


class WeightGather:
    def __init__(self, net, w, full, pos, by_rows, chunks, direct=0):
        self.net, self.w, self.full, self.by_rows = net, w, full, by_rows
        self.dp, self.t1, self.t2 = pos
        self.half = w.shape[0] // 2
        self.width = w.shape[0] if by_rows else w.shape[1]
        self.chunks, self.direct = chunks, direct
        self.base = net.take(1 + 4 * chunks + direct)

    def area(self, half, ch):
        if self.by_rows:
            n = self.w.shape[1] // self.chunks
            return ds(half * self.half, self.half, 16), self.half, pl.ds(ch * n, n)
        n = self.half // self.chunks
        return ds(half * self.half + ch * n, n, 16), n, pl.ds(0, self.width)

    def src(self, half, ch):
        rows, _, cols = self.area(half, ch)
        return self.w.at[rows, cols]

    def dst(self, k, half, ch):
        if self.by_rows:
            _, _, cols = self.area(half, ch)
            return self.full.at[ds(k * self.width + half * self.half, self.half, 16), cols]
        rows, _, _ = self.area(half, ch)
        return self.full.at[rows, pl.ds(k * self.width, self.width)]

    def whole(self, k):
        if self.by_rows:
            return self.full.at[pl.ds(k * self.width, self.width), :]
        return self.full.at[:, pl.ds(k * self.width, self.width)]

    def near(self, ch):
        i = self.base + 1 + ch
        return self.net.copy(self.src(self.dp, ch), self.dst(2, self.dp, ch), i, i, tx=self.t2)

    def cross(self, ch, half):
        i = self.base + 1 + self.chunks + ch
        return self.net.copy(self.dst(2, half, ch), self.dst(2, half, ch), i, i, dp=1 - self.dp)

    def diag(self, ch, which, half):
        i = self.base + 1 + (2 + which) * self.chunks + ch
        return self.net.copy(self.dst(2, half, ch), self.dst(3, half, ch), i, i, tx=self.t1)

    def mate(self):
        return self.net.copy(self.w, self.whole(1), self.base, self.base, tx=self.t1)

    def straight(self, n, half):
        ch = self.chunks - 1 - n
        i = self.base + 1 + 4 * self.chunks + n
        return self.net.copy(self.src(half, ch), self.dst(2, half, ch), i, i, tx=self.t2)

    def start_y(self):
        for ch in range(self.chunks):
            self.near(ch).start()
        for n in range(self.direct):
            self.straight(n, 1 - self.dp).start()

    def start_local(self):
        self.own = self.net.here(self.w, self.whole(0))
        self.mate().start()

    def y_event(self, ch):
        self.near(ch).wait_recv()
        if ch < self.chunks - self.direct:
            self.cross(ch, self.dp).start()
        self.diag(ch, 0, self.dp).start()

    def x_event(self, ch):
        if ch < self.chunks - self.direct:
            self.cross(ch, 1 - self.dp).wait_recv()
        else:
            self.straight(self.chunks - 1 - ch, 1 - self.dp).wait_recv()
        self.diag(ch, 1, 1 - self.dp).start()

    def finish_local(self):
        self.own.wait()
        self.mate().wait_recv()

    def finish(self, ch):
        self.diag(ch, 0, self.dp).wait_recv()
        self.diag(ch, 1, 1 - self.dp).wait_recv()

    def drain(self):
        self.mate().wait_send()
        for ch in range(self.chunks):
            self.near(ch).wait_send()
            if ch < self.chunks - self.direct:
                self.cross(ch, self.dp).wait_send()
            else:
                self.straight(self.chunks - 1 - ch, 1 - self.dp).wait_send()
            self.diag(ch, 0, self.dp).wait_send()
            self.diag(ch, 1, 1 - self.dp).wait_send()


def down_split(ff):
    return ff * 5 // 8


def places():
    dp, z, tx = lax.axis_index("dp"), lax.axis_index("ty"), lax.axis_index("tx")
    return dp, z, tx, (tx, tx + 1 - 2 * (tx % 2), (tx + 2) % 4, 3 - tx)


ROWS_ROWS = (((0,), (0,)), ((), ()))


class GradReduce:
    def __init__(self, net, peer, tile, tiles, st3, st1, cross, stage, got2, got0, got_y, out, out_tiles):
        self.net, self.peer, self.tile, self.tiles = net, peer, tile, tiles
        self.st3, self.st1, self.cross, self.stage = st3, st1, cross, stage
        self.got2, self.got0, self.got_y, self.out, self.out_tiles = got2, got0, got_y, out, out_tiles
        self.src = None
        self.base = net.take(3)
        self.rows, self.w = out.shape[0], out.shape[1] // tiles

    def cp(self, i):
        src, dst, to = ((self.st3, self.got2, 1), (self.st1, self.got0, 1), (self.src or self.cross, self.got_y, 2))[i]
        return self.net.copy(src, dst, self.base + i, self.base + i, tx=self.peer[to])

    def fill(self, k, ref):
        @pl.loop(0, self.tiles)
        def _(j):
            ref[:, ds(j * self.w, self.w)] = self.tile(k, j).astype(BF16)

    def step3(self):
        self.fill(3, self.st3)
        self.cp(0).start()

    def step1(self):
        self.fill(1, self.st1)
        self.cp(1).start()

    def step2(self, received=False):
        if not received:
            self.cp(0).wait_recv()
        self.net.here(self.got2, self.stage).wait()

        @pl.loop(0, self.tiles)
        def _(j):
            cols = ds(j * self.w, self.w)
            self.cross[:, cols] = (self.tile(2, j) + self.stage[:, cols].astype(F32)).astype(BF16)

    def send(self, src=None):
        self.src = src
        self.cp(2).start()

    def step0(self, far):
        self.cp(1).wait_recv()
        self.cp(2).wait_recv()
        loads = [self.net.here(self.got0, self.stage), self.net.here(self.got_y, far)]
        for c in loads:
            c.wait()
        base = self.net.n_local
        self.net.n_local += 2

        def put(j, slot):
            src = self.out_tiles.at[slot, pl.ds(0, self.rows), pl.ds(0, self.w)]
            return pltpu.make_async_copy(src, self.out.at[:, ds(j * self.w, self.w)], self.net.local.at[base + slot])

        @pl.loop(0, self.tiles)
        def _(j):
            cols = ds(j * self.w, self.w)
            slot = j % 2

            @pl.when(j >= 2)
            def _():
                put(j, slot).wait()

            self.out_tiles[slot, pl.ds(0, self.rows), pl.ds(0, self.w)] = self.tile(0, j) + (self.stage[:, cols].astype(F32) + far[:, cols].astype(F32))
            put(j, slot).start()

        for slot in range(min(2, self.tiles)):
            put(slot, slot).wait()

    def sent_locally(self):
        self.cp(0).wait_send()
        self.cp(1).wait_send()

    def sent(self):
        self.cp(2).wait_send()


def kernel_ab(q_width, hid, eqh, ekvh, posh, invh, swaph, dh2h, wg, wu, wd, wq, wkv, gfh, gah,
              n_o, da_o, db_o, u_o, wg_o, wu_o, wq_o, eq_o, h_o, g_o, e_o, n2_o, dres_o, home_o, dg_o, ux_o, ex_o, tab_o, d2_o, d0_o, dc_o,
              rows, dh2_v, n2_v, res_v, dres_v, n_v, a_v, b_v, wg_v, wu_v, wd_v, wq_v, eq_v, p_v, rbuf, rbuf2, gains, dg_v, swap_v, pos_v, inv_v, gf_v, ga_v, gin, send, recv, local):
    dp, z, tx, peer = places()
    sub, dim = rows.shape
    tokens = 4 * sub
    width = eq_v.shape[0]
    dt = dim // 4
    ff = wg.shape[1]
    wide = min(1024, ff)
    tile = min(512, ff)
    dwide = min(1024, dim)
    dtile = min(512, dim)
    hs, cs = sub // 2, sub // 8
    split = down_split(ff)
    net = Wires(send, recv, local)
    gain_in = [net.here(gfh, gf_v), net.here(gah, ga_v)]
    turn_in = [net.here(eqh, p_v.at[pl.ds(0, q_width), pl.ds(0, tokens)]), net.here(ekvh, p_v.at[pl.ds(q_width, width - q_width), pl.ds(0, tokens)]),
               net.here(swaph, swap_v), net.here(posh, pos_v), net.here(invh, inv_v)]
    entry_barrier([{"tx": peer[1]}, {"tx": peer[2]}, {"tx": peer[3]}, {"dp": 1 - dp}], z)

    pos = (dp, peer[1], peer[2])
    far_first = (2, 3, 1)
    g_id, h_id, e_id, d_id, o_id, u_id, x_id = (net.take(4), net.take(4), net.take(4), net.take(4), net.take(8), net.take(12), net.take(24))
    u_v = wg_v.at[pl.ds(0, tokens), :]
    e_v = wg_v.at[pl.ds(tokens, tokens), :]

    def g_cp(k):
        return net.copy(gin, gains.at[:, pl.ds(k * dt, dt)], g_id + k, g_id + k, tx=peer[k])

    def h_cp(k):
        return net.copy(hid.at[ds(peer[k] * sub, sub), :], rows.at[:, pl.ds(k * dt, dt)], h_id + k, h_id + k, tx=peer[k])

    def e_cp(k, block):
        return net.copy(p_v.at[pl.ds(0, width), ds(peer[k] * sub, sub)], eq_v.at[:, ds(block * sub, sub)], e_id + k, e_id + k, tx=peer[k])

    def d_cp(k):
        return net.copy(dh2h.at[ds(peer[k] * sub, sub), :], dh2_v.at[:, pl.ds(k * dt, dt)], d_id + k, d_id + k, tx=peer[k])

    def o_cp(k, block, half):
        i = o_id + half * 4 + k
        return net.copy(res_v.at[pl.ds(half * hs, hs), pl.ds(k * dt, dt)], home_o.at[ds(block * sub + half * hs, hs), :], i, i, tx=peer[k])

    def ux_cp(k, b):
        view = ds(b * sub, sub)
        cols = pl.ds(0, split)
        src = ux_o.at[1, view, :] if k == 3 else wg_v.at[view, cols]
        i = u_id + (k - 1) * 4 + b
        return net.copy(src, ux_o.at[k - 1, view, :], i, i, tx=peer[1] if k == 3 else peer[k])

    def ex_cp(k, b, half):
        i = x_id + half * 12 + (k - 1) * 4 + b
        view = ds(b * sub + half * hs, hs)
        return net.copy(wg_v.at[ds(tokens + b * sub + half * hs, hs), pl.ds(k * dt, dt)], ex_o.at[k - 1, view, :], i, i, tx=peer[k])

    gate = WeightGather(net, wg, wg_v, pos, True, 2)
    up = WeightGather(net, wu, wu_v, pos, True, 2)
    down = WeightGather(net, wd, wd_v, pos, False, 4, 1)
    q_w = WeightGather(net, wq, wq_v.at[pl.ds(0, q_width), :], pos, False, 1)
    kv_w = WeightGather(net, wkv, wq_v.at[pl.ds(q_width, width - q_width), :], pos, False, 1)
    ag = LineGather(net, n_v, sub, z)
    rsc = LineScatter(net, p_v, rbuf, sub, z)
    rs2 = [LineScatter(net, n_v, rbuf2, sub, z, c * cs, cs) for c in range(8)]
    ag2 = [LineGather(net, e_v, sub, z, c * cs, cs) for c in range(8)]

    for k in far_first:
        h_cp(k).start()
    for c in gain_in:
        c.wait()
    gin[...] = jnp.broadcast_to(gf_v[...].astype(F32)[None, :], gin.shape)
    gin[1:2, :] = ga_v[...].astype(F32)[None, :]
    g_own = net.here(gin, gains.at[:, pl.ds(0, dt)])
    h_own = net.here(hid.at[ds(tx * sub, sub), :], rows.at[:, pl.ds(0, dt)])
    for w in (q_w, kv_w, gate, up, down):
        w.start_local()
    for k in far_first:
        g_cp(k).start()
    for c in turn_in:
        c.wait()

    @pl.loop(0, tokens // 128)
    def _(i):
        part = 128
        cos_c, sin_c = ds(i * part, part), ds(tokens + i * part, part)
        q_r, kv_r = pl.ds(0, 128), pl.ds(128, 128)
        angles = inv_v[...] * pos_v[:, cos_c].astype(F32)
        dres_v[q_r, sin_c] = jnp.sin(angles)
        dres_v[q_r, cos_c] = jnp.cos(angles)

        @pl.when(z < 2)
        def _():
            dres_v[kv_r, cos_c] = dres_v[q_r, cos_c]
            dres_v[kv_r, sin_c] = dres_v[q_r, sin_c]

        @pl.when(z >= 2)
        def _():
            dres_v[kv_r, cos_c] = jnp.ones((128, part), F32)
            dres_v[kv_r, sin_c] = jnp.zeros((128, part), F32)

    tab_out = net.here(dres_v.at[pl.ds(0, 256), pl.ds(0, 2 * tokens)], tab_o)
    turn(p_v, width, q_width, tokens, dres_v, swap_v, True)
    for k in far_first:
        e_cp(k, tx).start()
    e_own = net.here(p_v.at[pl.ds(0, width), ds(tx * sub, sub)], eq_v.at[:, ds(tx * sub, sub)])
    for w in (q_w, kv_w, gate, up, down):
        w.start_y()
    for k in far_first:
        d_cp(k).start()
    d_own = net.here(dh2h.at[ds(tx * sub, sub), :], dh2_v.at[:, pl.ds(0, dt)])

    for k in far_first:
        g_cp(k).wait_recv()
        h_cp(k).wait_recv()
    g_own.wait()
    h_own.wait()

    @pl.loop(0, sub // 16)
    def _(r):
        x = rows[ds(r * 16, 16), :].astype(F32)
        inv = lax.rsqrt(jnp.sum(x * x, axis=1, keepdims=True) / dim + NORM_EPS)
        n_v[ds(z * sub + r * 16, 16), :] = (x * inv * gains[0:1, :]).astype(BF16)

    ag.start()
    outs = [net.here(rows, h_o), net.here(gains, g_o)]
    for k in far_first:
        e_cp(k, peer[k]).wait_recv()
    e_own.wait()
    ag.step1()
    for w in (q_w, kv_w):
        w.y_event(0)
    for w in (q_w, kv_w):
        w.x_event(0)
    for w in (q_w, kv_w):
        w.finish_local()
        w.finish(0)
    for k in far_first:
        e_cp(k, tx).wait_send()

    def n2_block(b):
        @pl.loop(0, dim // dtile)
        def _(j):
            cols = ds(j * dtile, dtile)
            p_v[ds(b * sub, sub), cols] = dot(eq_v[:, ds(b * sub, sub)], wq_v[:, cols], ROWS_ROWS).astype(BF16)

    @pl.loop(0, 4)
    def _(i):
        n2_block(pick(3 - i, z))
        for step in range(3):
            pl.when(i == step)(lambda step=step: rsc.send_end(2 - step))
        pl.when(i == 0)(lambda: gate.y_event(0))

    wide = ff // 2

    def gate_part(b, c):
        cols = pl.ds(c * wide, wide)
        a_v[ds(b * sub, sub), cols] = dot(n_v[ds(b * sub, sub), :], wg_v[:, cols]).astype(BF16)

    def up_part(b, c):
        cols = pl.ds(c * wide, wide)
        bb = dot(n_v[ds(b * sub, sub), :], wu_v[:, cols]).astype(BF16)
        b_v[ds(b * sub, sub), cols] = bb
        aa = a_v[ds(b * sub, sub), cols].astype(F32)
        wg_v[ds(b * sub, sub), cols] = (aa * jax.nn.sigmoid(aa) * bb.astype(F32)).astype(BF16)

    def down_part(b, j):
        cols = pl.ds(j * (dim // 2), dim // 2)
        n_v[ds(b * sub, sub), cols] = dot(wg_v[ds(b * sub, sub), :], wd_v[:, cols]).astype(BF16)

    outs += [net.here(wq_v, wq_o), net.here(eq_v, eq_o)]
    gate.finish_local()
    gate.y_event(1)
    ag.step2()
    ag.step3_mid()
    gate.x_event(0)
    gate.finish(0)

    @pl.loop(0, 3)
    def _(i):
        gate_part(pick(i, z), 0)

    up.y_event(0)
    gate.x_event(1)
    rsc.send_mid(2)
    gate.finish(1)
    wg_out = net.here(wg_v, wg_o)

    @pl.loop(0, 3)
    def _(i):
        gate_part(pick(i, z), 1)

    up.finish_local()
    up.y_event(1)
    up.x_event(0)
    up.finish(0)
    ag.step3_end()

    @pl.loop(0, 2)
    def _(c):
        cols = ds(c * wide, wide)
        b = pick(3, z)
        a_v[ds(b * sub, sub), cols] = dot(n_v[ds(b * sub, sub), :], wg_v[:, cols]).astype(BF16)

    wg_out.wait()
    n_out = net.here(n_v, n_o)

    @pl.loop(0, 4)
    def _(i):
        pl.when(i == 1)(lambda: down.y_event(0))
        pl.when(i == 2)(lambda: down.y_event(1))
        pl.when(i == 3)(lambda: up.x_event(1))
        up_part(pick(i, z), 0)

    def up_events_1():
        rsc.send_mid(1)
        rsc.send_mid(0)
        down.x_event(0)

    def up_events_2():
        down.y_event(2)

    def up_events_3():
        down.y_event(3)
        down.x_event(1)

    up.finish(1)
    outs.append(net.here(wu_v, wu_o))

    @pl.loop(0, 4)
    def _(i):
        pl.when(i == 1)(up_events_1)
        pl.when(i == 2)(up_events_2)
        pl.when(i == 3)(up_events_3)
        b = pick(i, z)
        up_part(b, 1)
        ux_cp(2, b).start()
        ux_cp(1, b).start()

    outs.append(net.here(u_v, u_o))
    ag.drain()
    gate.drain()
    n_out.wait()
    down.finish_local()

    @pl.loop(0, 4)
    def _(i):
        pl.when(i == 2)(lambda: down.x_event(2))
        pl.when(i == 3)(lambda: down.x_event(3))
        down_part(pick(3 - i, z), 0)

    for ch in range(4):
        down.finish(ch)

    @pl.loop(0, 4)
    def _(i):
        down_part(pick(3 - i, z), 1)
        for step in range(3):
            pl.when(i == step)(lambda step=step: rs2[0].send_end(2 - step))

    for c in range(1, 8):
        for i in (2, 1, 0):
            rs2[c].send_end(i)
    dg_v[...] = jnp.zeros_like(dg_v)
    step = 16

    def norm_chunk(c):
        @pl.loop(0, cs // step)
        def _(r):
            at = c * cs + r * step
            view, mine, far = ds(at, step), ds(z * sub + at, step), ds(4 * sub + at, step)

            def whole(part, got):
                right = jnp.where(z < 3, got[mine, :].astype(F32), 0.0)
                left = jnp.where(z > 0, got[far, :].astype(F32), 0.0)
                return part[mine, :].astype(F32) + right + left

            resid = (rows[view, :].astype(F32) + whole(n_v, rbuf2)).astype(BF16)
            dy = whole(p_v, rbuf)
            res_v[view, :] = resid
            x = resid.astype(F32)
            inv = lax.rsqrt(jnp.sum(x * x, axis=1, keepdims=True) / dim + NORM_EPS)
            xhat = x * inv
            gain = gains[1:2, :]
            n2_v[view, :] = (xhat * gain).astype(BF16)
            part = dy * xhat
            dg_v[...] += part[:8] + part[8:]
            inner = jnp.sum(part * gain, axis=1, keepdims=True) / dim
            dres = dh2_v[view, :].astype(F32) + inv * (dy * gain) - xhat * (inv * inner)
            dres_v[view, pl.ds(0, dim)] = dres
            wg_v[ds(tokens + z * sub + at, step), :] = dres.astype(BF16)

    def spread(b, half):
        for k in far_first:
            ex_cp(k, b, half).start()

    def back_tile(b, j):
        view, cols = ds(b * sub, sub), ds(j * (ff // 4), ff // 4)
        du = dot(wg_v[ds(tokens + b * sub, sub), :], wd_v[ds(j * (ff // 4), ff // 4), :], NT_DIMS)
        aa = a_v[view, cols].astype(F32)
        bb = b_v[view, cols].astype(F32)
        sig = jax.nn.sigmoid(aa)
        a_v[view, cols] = (du * bb * sig * (1.0 + aa * (1.0 - sig))).astype(BF16)
        b_v[view, cols] = (du * aa * sig).astype(BF16)

    def scatter(i, c):
        return lambda: rs2[c].send_mid(i)

    def gathered(i, c):
        def go():
            ag2[c].take(i)
            pl.when(mid(z))(lambda: ag2[c].forward(i))
            if c % 4 == 3:
                spread(ag.slots[i], c // 4)
        return go

    def run(ops):
        def go():
            for op in ops:
                op()
        return go

    before_mid = (
        (scatter(2, 0), scatter(1, 0), scatter(0, 0)),
        (scatter(2, 1), scatter(1, 1), gathered(1, 0), scatter(0, 1), scatter(2, 2)),
        (scatter(1, 2), scatter(0, 2), gathered(1, 1), scatter(2, 3)),
        (scatter(1, 3), scatter(0, 3), gathered(1, 2), scatter(2, 4)),
        (scatter(1, 4), scatter(0, 4), gathered(1, 3), scatter(2, 5)),
        (scatter(1, 5), scatter(0, 5), gathered(1, 4), scatter(2, 6)),
        (scatter(1, 6), scatter(0, 6), gathered(1, 5), scatter(2, 7)),
        (scatter(1, 7), scatter(0, 7), gathered(1, 6), gathered(0, 0)))
    before_end = (
        (),
        (gathered(0, 0), gathered(1, 0)),
        (gathered(0, 1),),
        (gathered(1, 1), gathered(0, 2)),
        (gathered(1, 2), gathered(0, 3)),
        (gathered(1, 3), gathered(0, 4)),
        (gathered(1, 4), gathered(0, 5)),
        (gathered(1, 5), gathered(0, 6)))
    after_mid = {1: (gathered(0, 1),),
                 2: (gathered(2, 0),),
                 3: (gathered(0, 2),),
                 4: (gathered(1, 7),),
                 5: (gathered(0, 3),),
                 6: (gathered(2, 1),),
                 7: (gathered(0, 4),),
                 8: (gathered(2, 2), gathered(0, 5), gathered(2, 3), gathered(0, 6), gathered(2, 4), gathered(0, 7)),
                 10: (gathered(2, 5),),
                 12: (gathered(2, 6), gathered(2, 7))}
    after_end = {2: (gathered(1, 6),),
                 4: (gathered(0, 7),),
                 7: (gathered(2, 0),),
                 8: (gathered(1, 7),),
                 11: (gathered(2, 1),),
                 12: (gathered(2, 2), gathered(2, 3), gathered(2, 4), gathered(2, 5), gathered(2, 6), gathered(2, 7))}

    for c in range(8):
        pl.when(mid(z))(run(before_mid[c]))
        pl.when(end(z))(run(before_end[c]))
        if c == 0:
            rsc.finish()
            for k in far_first:
                d_cp(k).wait_recv()
            d_own.wait()
            tab_out.wait()
        rs2[c].finish()
        norm_chunk(c)
        ag2[c].start()
        if c % 4 == 3:
            spread(z, c // 4)
            for k in far_first:
                o_cp(k, tx, c // 4).start()

    outs += [net.here(res_v.at[:, pl.ds(0, dt)], home_o.at[ds(tx * sub, sub), :]), net.here(n2_v, n2_o), net.here(dres_v.at[pl.ds(0, sub), pl.ds(0, dim)], dres_o), net.here(dg_v, dg_o)]
    rsc.drain()
    for c in range(8):
        rs2[c].drain()
    middle = (z + 1) // 2 % 2

    def u_forward():
        for b in range(4):
            ux_cp(2, b).wait_recv()
            ux_cp(3, b).start()

    @pl.loop(0, 16)
    def _(t):
        for at, ops in after_mid.items():
            pl.when(jnp.logical_and(t == at, mid(z)))(run(ops))
        for at, ops in after_end.items():
            pl.when(jnp.logical_and(t == at, end(z)))(run(ops))
        pl.when(t == 8)(u_forward)
        i = t // 4
        inner = (i + 1) // 2 % 2
        back_tile(pick(i + middle * inner * (3 - 2 * i), z), t % 4)

    outs.append(net.here(e_v, e_o))
    outs += [net.here(a_v, da_o), net.here(b_v, db_o)]

    def down_tile(k, j):
        return dot(wg_v[pl.ds(0, tokens), pl.ds(split, ff - split)], wg_v[pl.ds(tokens, tokens), ds(k * dt + j * (dt // 2), dt // 2)], ROWS_ROWS)

    quarter = [rbuf.at[pl.ds(0, ff - split), pl.ds(i * dt, dt)] for i in range(4)]
    part_d = GradReduce(net, peer, down_tile, 2, quarter[0], quarter[1], quarter[2], quarter[3], d2_o, d0_o, None, dc_o, None)
    part_d.step3()
    part_d.step1()
    part_d.step2()
    outs.append(net.here(quarter[2], dc_o))
    for k in far_first:
        o_cp(k, peer[k], 0).wait_recv()
        o_cp(k, peer[k], 1).wait_recv()
        for b in range(4):
            ex_cp(k, b, 0).wait_recv()
            ex_cp(k, b, 1).wait_recv()
    for b in range(4):
        ux_cp(1, b).wait_recv()
        ux_cp(3, b).wait_recv()
    for c in outs:
        c.wait()
    for k in far_first:
        g_cp(k).wait_send()
        h_cp(k).wait_send()
        d_cp(k).wait_send()
        o_cp(k, tx, 0).wait_send()
        o_cp(k, tx, 1).wait_send()
        for b in range(4):
            ux_cp(k, b).wait_send()
            ex_cp(k, b, 0).wait_send()
            ex_cp(k, b, 1).wait_send()
    for w in (q_w, kv_w, up, down):
        w.drain()
    for c in range(8):
        ag2[c].drain()
    part_d.cp(1).wait_recv()
    part_d.sent_locally()


def call_ab(hid, eqh, ekvh, pos, inv, swap, dh2h, wg, wu, wd, wq, wkv, gf, ga):
    tokens, dt = hid.shape
    sub, dim, ff, q_width = tokens // 4, dt * 4, wg.shape[1], wq.shape[0]
    width = q_width + wkv.shape[0]
    s = jax.ShapeDtypeStruct
    tok_ff, tok_d, row = s((tokens, ff), BF16), s((tokens, dim), BF16), s((sub, dim), BF16)
    shapes = (tok_d, tok_ff, tok_ff, tok_ff, s((dim, ff), BF16), s((dim, ff), BF16), s((width, dim), BF16), s((width, tokens), BF16),
              row, s((8, dim), F32), tok_d, row, s((sub, dim), F32), s((tokens, dt), BF16), s((8, dim), F32),
              s((3, tokens, down_split(ff)), BF16), s((3, tokens, dt), BF16), s((256, 2 * tokens), F32)) + (s((ff - down_split(ff), dt), BF16),) * 3
    vrow, vtok, vff = VMEM((sub, dim), BF16), VMEM((tokens, dim), BF16), VMEM((tokens, ff), BF16)
    return pl.pallas_call(
        functools.partial(kernel_ab, q_width), out_shape=shapes, in_specs=[ANY] * 14, out_specs=[ANY] * len(shapes),
        scratch_shapes=[
            vrow, vrow, vrow, vrow, VMEM((max(sub, 256), max(dim, 2 * tokens)), F32), vtok, vff, vff, VMEM((dim, ff), BF16), VMEM((dim, ff), BF16), VMEM((ff, dim), BF16),
            VMEM((width, dim), BF16), VMEM((width, tokens), BF16), vtok, VMEM((5 * sub, dim), BF16), VMEM((5 * sub, dim), BF16),
            VMEM((8, dim), F32), VMEM((8, dim), F32), VMEM((128, 128), BF16), VMEM((1, tokens), jnp.int32), VMEM((128, 128), F32),
            VMEM((dt,), BF16), VMEM((dt,), BF16), VMEM((8, dt), F32),
            pltpu.SemaphoreType.DMA((236,)), pltpu.SemaphoreType.DMA((236,)), pltpu.SemaphoreType.DMA((48,))],
        compiler_params=pltpu.CompilerParams(collective_id=0, has_side_effects=True, vmem_limit_bytes=VMEM_LIMIT),
        cost_estimate=pl.CostEstimate(flops=20 * tokens * dim * ff, bytes_accessed=100000000, transcendentals=0), name="phase_ab",
    )(hid, eqh, ekvh, pos, inv, swap, dh2h, wg, wu, wd, wq, wkv, gf, ga)


def kernel_c(q_width, da_h, db_h, wg_h, wu_h, n_h, u_h, ux_h, e_h, ex_h, n2_h, eq_h, wq_h, h_h, dres_h, g_h, dga_h, tabh, swaph, d0, dc,
             wgo, wgy, wuo, wuy, wdo, wqo, wqy, wvo, wvy, q_o, kv_o, dh_o, dg_o, g2, g0, u2, u0, q2, q0, v2, v0, qx, dy,
             wg_v, wu_v, da_v, db_v, n_v, p_v, rbuf, n2_v, st3, st1, cross_g, cross_u, stage, tiles_v, dres_v, wq_v, eq_v,
             gains, dg_v, dgr, dgz, tab_v, swap_v, send, recv, local):
    dp, z, tx, peer = places()
    tokens, ff = da_v.shape
    sub, dim = dres_v.shape
    dt = dim // 4
    width = eq_v.shape[0]
    tile = ff // 4
    dtile = min(512, dim)
    qt = min(256, tile)
    far_first = (2, 3, 1)
    net = Wires(send, recv, local)
    n2_in = net.here(n2_h, n2_v.at[ds(z * sub, sub), :])
    first = [net.here(n_h, n_v), net.here(da_h, da_v)]
    second = [net.here(db_h, db_v), net.here(wg_h, wg_v), net.here(wu_h, wu_v)]
    third = [net.here(wq_h, wq_v), net.here(eq_h, eq_v), net.here(dres_h, dres_v), net.here(g_h, gains),
             net.here(dga_h, dg_v.at[pl.ds(8, 8), :]), net.here(tabh, tab_v), net.here(swaph, swap_v)]
    sem = pltpu.get_barrier_semaphore()
    zs = tuple((z + i) % 4 for i in range(4))
    for i in (1, 2, 3):
        pl.semaphore_signal(sem, inc=1, device_id={"tx": peer[i]}, device_id_type=MESH)
        pl.semaphore_signal(sem, inc=1, device_id={"ty": zs[i]}, device_id_type=MESH)
    pl.semaphore_wait(sem, 6)
    rsc = LineScatter(net, p_v, rbuf, sub, z)
    ag = LineGather(net, n2_v, sub, z)
    q_id, h_id, t_id, z_id = net.take(4), net.take(4), net.take(4), net.take(4)

    def grad_tile(lhs, rhs, w):
        def go(k, j):
            cols = pl.ds(j * w, w) if isinstance(j, int) else ds(j * w, w)
            return dot(lhs[:, pl.ds(k * dt, dt)], rhs[:, cols], ROWS_ROWS)
        return go

    gate = GradReduce(net, peer, grad_tile(n_v, da_v, tile), ff // tile, st3, st1, cross_g, stage, g2, g0, wgy, wgo, tiles_v)
    up = GradReduce(net, peer, grad_tile(n_v, db_v, tile), ff // tile, st3, st1, cross_u, stage, u2, u0, wuy, wuo, tiles_v)
    d_id = net.take(1)

    def dy_cp():
        return net.copy(dc, dy, d_id, d_id, tx=peer[2])

    dy_cp().start()

    def head_grad(first, rows, got2, got0, got_y, out):
        corner = [da_v.at[pl.ds(first, rows), pl.ds(c * dt, dt)] for c in range(4)]

        def tile_of(k, j):
            return dot(eq_v[pl.ds(first, rows), :], n2_v[:, ds(k * dt + j * qt, qt)])

        return GradReduce(net, peer, tile_of, dt // qt, *corner, got2, got0, got_y, out, tiles_v)

    heads = (head_grad(0, q_width, q2, q0, wqy, wqo), head_grad(q_width, width - q_width, v2, v0, wvy, wvo))

    def dn_block(b):
        rows = ds(b * sub, sub)

        @pl.loop(0, dim // dtile)
        def _(j):
            wr = ds(j * dtile, dtile)
            p_v[rows, wr] = (dot(da_v[rows, :], wg_v[wr, :], NT_DIMS) + dot(db_v[rows, :], wu_v[wr, :], NT_DIMS)).astype(BF16)

    n2_in.wait()
    ag.start()
    for c in first:
        c.wait()
    gate.step3()
    gate.step1()
    gate.step2()
    gate.send()
    for c in second:
        c.wait()

    @pl.loop(0, 4)
    def _(i):
        @pl.when(i == 1)
        def _():
            gate.sent_locally()
            up.step3()
            up.step1()
            ag.step1()

        dn_block(pick(3 - i, z))
        for step in range(3):
            pl.when(i == step)(lambda step=step: rsc.send_end(2 - step))

    up.step2()
    up.send()
    rsc.send_mid(2)
    ag.step2()
    ag.step3_mid()
    up.sent_locally()
    h_in = net.here(h_h, st3.at[pl.ds(0, sub), :])
    gate.step0(st1)
    gate.sent()

    e_in = [net.here(e_h.at[:, pl.ds(0, dt)], wu_v.at[pl.ds(0, tokens), pl.ds(0, dt)])]
    for k in (1, 2, 3):
        e_in.append(net.here(ex_h.at[k - 1], wu_v.at[pl.ds(0, tokens), pl.ds(k * dt, dt)]))

    piece = ff // 8
    exchanged, n_pieces = down_split(ff) // piece, 8

    def u_place(j, k):
        return wg_v.at[pl.ds((j % 2) * tokens, tokens), pl.ds(k * piece, piece)]

    def sums(j, n):
        return stage.at[pl.ds((j % 2) * piece, piece), pl.ds(n * dt, dt)]

    def u_load(j):
        cols = pl.ds(j * piece, piece)
        if j < exchanged:
            return [net.here(u_h.at[:, cols] if k == 0 else ux_h.at[k - 1, :, cols], u_place(j, k)) for k in range(4)]
        rows = pl.ds((j - exchanged) * piece, piece)
        return [net.here(u_h.at[:, cols], u_place(j, 0)), net.here(d0.at[rows, :], sums(j, 0)), net.here(dy.at[rows, :], sums(j, 1))]

    loads, stores = {}, {}

    def down_run(js):
        for j in js:
            for c in loads.pop(j):
                c.wait()
            if j >= 2:
                stores.pop(j - 2).wait()
            acc = None if j < exchanged else sums(j, 0)[...].astype(F32) + sums(j, 1)[...].astype(F32)
            for k in range(4 if j < exchanged else 1):
                part = dot(u_place(j, k)[...], wu_v[pl.ds(0, tokens), pl.ds(k * dt, dt)], ROWS_ROWS)
                acc = part if acc is None else acc + part
            place = tiles_v.at[j % 2, pl.ds(0, piece), pl.ds(0, dt)]
            tiles_v[j % 2, pl.ds(0, piece), pl.ds(0, dt)] = acc
            stores[j] = net.here(place, wdo.at[pl.ds(j * piece, piece), :])
            if j + 2 < n_pieces:
                loads[j + 2] = u_load(j + 2)

    loads[0], loads[1] = u_load(0), u_load(1)
    rsc.send_mid(1)
    rsc.send_mid(0)
    for c in e_in:
        c.wait()
    down_run((0, 1))
    for c in third:
        c.wait()
    ag.step3_end()

    @pl.loop(0, width // qt)
    def _(j):
        wu_v[ds(tokens + j * qt, qt), pl.ds(0, tokens)] = dot(wq_v[ds(j * qt, qt), :], n2_v[...], NT_DIMS).astype(BF16)

    def q_cp(k, block):
        return net.copy(wu_v.at[pl.ds(tokens, width), ds(peer[k] * sub, sub)], qx.at[:, ds(block * sub, sub)], q_id + k, q_id + k, tx=peer[k])

    for k in far_first:
        q_cp(k, tx).start()
    q_own = net.here(wu_v.at[pl.ds(tokens, width), ds(tx * sub, sub)], qx.at[:, ds(tx * sub, sub)])
    for part in heads:
        part.step3()
        part.step1()
    dy_cp().wait_recv()
    for part in heads:
        part.step2()
        part.send()
    down_run(range(2, n_pieces))
    h_in.wait()
    rsc.finish()
    dg_v[pl.ds(0, 8), :] = jnp.zeros((8, dim), F32)
    step = 16

    @pl.loop(0, sub // step)
    def _(r):
        view, mine, far = ds(r * step, step), ds(z * sub + r * step, step), ds(4 * sub + r * step, step)
        right = jnp.where(z < 3, rbuf[mine, :].astype(F32), 0.0)
        left = jnp.where(z > 0, rbuf[far, :].astype(F32), 0.0)
        dy = p_v[mine, :].astype(F32) + right + left
        x = st3[view, :].astype(F32)
        inv = lax.rsqrt(jnp.sum(x * x, axis=1, keepdims=True) / dim + NORM_EPS)
        xhat = x * inv
        gain = gains[0:1, :]
        part = dy * xhat
        dg_v[pl.ds(0, 8), :] += part[:8] + part[8:]
        inner = jnp.sum(part * gain, axis=1, keepdims=True) / dim
        st1[view, :] = (dres_v[view, :] + inv * (dy * gain) - xhat * (inv * inner)).astype(BF16)

    def h_cp(k, block):
        return net.copy(st1.at[pl.ds(0, sub), pl.ds(k * dt, dt)], dh_o.at[ds(block * sub, sub), :], h_id + k, h_id + k, tx=peer[k])

    def t_cp(k):
        return net.copy(dg_v.at[:, pl.ds(k * dt, dt)], dgr.at[k], t_id + k, t_id + k, tx=peer[k])

    def z_cp(i):
        return net.copy(dgr.at[0], dgz.at[i], z_id + i, z_id + i, ty=zs[i])

    for k in far_first:
        t_cp(k).start()
    for k in far_first:
        h_cp(k, tx).start()
    h_own = net.here(st1.at[pl.ds(0, sub), pl.ds(0, dt)], dh_o.at[ds(tx * sub, sub), :])
    up.sent()
    for c in stores.values():
        c.wait()
    up.step0(cross_g)
    for k in far_first:
        q_cp(k, peer[k]).wait_recv()
    q_own.wait()
    turned = wu_v.at[pl.ds(tokens, width), pl.ds(tokens, tokens)]
    net.here(qx, turned).wait()
    turn(turned, width, q_width, tokens, tab_v, swap_v, False)
    q_out = net.here(wu_v.at[pl.ds(tokens, q_width), pl.ds(tokens, tokens)], q_o)
    kv_out = net.here(wu_v.at[pl.ds(tokens + q_width, width - q_width), pl.ds(tokens, tokens)], kv_o)
    heads[0].step0(cross_g.at[pl.ds(0, q_width), pl.ds(0, dt)])
    heads[1].step0(cross_g.at[pl.ds(0, width - q_width), pl.ds(dt, dt)])
    for k in far_first:
        t_cp(k).wait_recv()
    dgr[0] = dg_v[:, pl.ds(0, dt)] + dgr[1] + dgr[2] + dgr[3]
    for i in (1, 2, 3):
        z_cp(i).start()
    for i in (1, 2, 3):
        z_cp(i).wait_recv()
    dgz[0] = dgr[0] + dgz[1] + dgz[2] + dgz[3]
    dg_out = net.here(dgz.at[0], dg_o)
    for k in far_first:
        h_cp(k, peer[k]).wait_recv()
    for c in (q_out, kv_out, dg_out, h_own):
        c.wait()
    dy_cp().wait_send()
    for part in heads:
        part.sent_locally()
        part.sent()
    for k in far_first:
        q_cp(k, tx).wait_send()
        h_cp(k, tx).wait_send()
        t_cp(k).wait_send()
        z_cp(k).wait_send()
    ag.drain()
    rsc.drain()


def call_c(q_width, *args):
    tokens, ff = args[0].shape
    sub, dim = args[9].shape
    dt, width = dim // 4, args[10].shape[0]
    rest = width - q_width
    tile = ff // 4
    s = jax.ShapeDtypeStruct
    wf, wb = s((dt, ff), F32), s((dt, ff), BF16)
    qf, qb, vf, vb = s((q_width, dt), F32), s((q_width, dt), BF16), s((rest, dt), F32), s((rest, dt), BF16)
    shapes = (wf, wb, wf, wb, s((ff, dt), F32), qf, qb, vf, vb, s((q_width, tokens), BF16), s((rest, tokens), BF16), s((tokens, dt), BF16), s((16, dt), F32),
              wb, wb, wb, wb, qb, qb, vb, vb, s((width, tokens), BF16), s((ff - down_split(ff), dt), BF16))
    return pl.pallas_call(
        functools.partial(kernel_c, q_width), out_shape=shapes, in_specs=[ANY] * len(args), out_specs=[ANY] * len(shapes),
        scratch_shapes=[
            VMEM((dim, ff), BF16), VMEM((dim, ff), BF16), VMEM((tokens, ff), BF16), VMEM((tokens, ff), BF16), VMEM((tokens, dim), BF16),
            VMEM((tokens, dim), BF16), VMEM((5 * sub, dim), BF16), VMEM((tokens, dim), BF16),
            VMEM((dt, ff), BF16), VMEM((dt, ff), BF16), VMEM((dt, ff), BF16), VMEM((dt, ff), BF16), VMEM((dt, ff), BF16),
            VMEM((2, max(dt, tile), max(dt, tile)), F32), VMEM((sub, dim), F32), VMEM((width, dim), BF16), VMEM((width, tokens), BF16),
            VMEM((8, dim), F32), VMEM((16, dim), F32), VMEM((4, 16, dt), F32), VMEM((4, 16, dt), F32), VMEM((256, 2 * tokens), F32), VMEM((128, 128), BF16),
            pltpu.SemaphoreType.DMA((48,)), pltpu.SemaphoreType.DMA((48,)), pltpu.SemaphoreType.DMA((96,))],
        compiler_params=pltpu.CompilerParams(collective_id=2, has_side_effects=True, vmem_limit_bytes=VMEM_LIMIT),
        cost_estimate=pl.CostEstimate(flops=20 * tokens * dim * ff, bytes_accessed=100000000, transcendentals=0), name="phase_c",
    )(*args)


def kernel_out(pieces, n, *refs):
    ins, outs, bufs = refs[:n], refs[n + 1:2 * n + 1], refs[2 * n + 3:3 * n + 3]
    gains, gain_a, gain_b = refs[n], refs[2 * n + 1], refs[2 * n + 2]
    read, write = refs[3 * n + 3:]

    def part(ref, i, c):
        rows = ref.shape[0] // pieces[i]
        return ref.at[pl.ds(c * rows, rows), :]

    jobs = [(i, c) for i in range(n) for c in range(pieces[i])]
    get = [pltpu.make_async_copy(part(ins[i], i, c), part(bufs[i], i, c), read.at[m]) for m, (i, c) in enumerate(jobs)]
    put = [pltpu.make_async_copy(part(bufs[i], i, c), part(outs[i], i, c), write.at[m]) for m, (i, c) in enumerate(jobs)]
    for g in get:
        g.start()
    gain_a[...] = jnp.sum(gains[pl.ds(0, 8), :], axis=0, keepdims=True)
    gain_b[...] = jnp.sum(gains[pl.ds(8, 8), :], axis=0, keepdims=True)
    for g, p in zip(get, put):
        g.wait()
        p.start()
    for p in put:
        p.wait()


def call_out(results, gains):
    n = len(results)
    pieces = tuple(max(1, x.size * x.dtype.itemsize // 2**20) for x in results)
    row = jax.ShapeDtypeStruct((1, gains.shape[1]), F32)
    whole = pl.BlockSpec(memory_space=pltpu.VMEM)
    return pl.pallas_call(
        functools.partial(kernel_out, pieces, n), out_shape=tuple(jax.ShapeDtypeStruct(x.shape, x.dtype) for x in results) + (row, row),
        in_specs=[ANY] * n + [whole], out_specs=[ANY] * n + [whole, whole],
        scratch_shapes=[VMEM(x.shape, x.dtype) for x in results] + [pltpu.SemaphoreType.DMA((sum(pieces),))] * 2,
        compiler_params=pltpu.CompilerParams(vmem_limit_bytes=VMEM_LIMIT),
        cost_estimate=pl.CostEstimate(flops=1000000, bytes_accessed=35000000, transcendentals=0), name="results",
    )(*results, gains)


def solution(mesh):
    def local_step(hidden, positions, g_ffn, w_gate, w_up, w_down, g_attn, w_q, w_kv, grad_h2, grad_q, grad_kv):
        tokens, dt = hidden.shape
        q_heads, head_dim = w_q.shape[1:]
        q_width = q_heads * head_dim

        lane = np.arange(128)
        inv_freq = ROPE_BASE ** (-(lane % head_dim // 2 * 2).astype(np.float32) / head_dim)
        inv_freq = jnp.asarray(np.tile(inv_freq.astype(np.float32)[:, None], (1, 128)))
        swap = np.zeros((128, 128), np.float32)
        swap[lane, lane ^ 1] = np.where(lane % 2 == 0, -1.0, 1.0)
        swap = jnp.asarray(swap, BF16)

        def heads_first(x):
            return x.transpose(1, 2, 0).reshape(-1, x.shape[0])

        def heads_last(x):
            return x.reshape(-1, head_dim, x.shape[1]).transpose(2, 0, 1)

        (normed_all, grad_gate, grad_up, u_all, gate_w, up_w, w_qkv, back_all, h_rows, gains, res_all, normed2, grad_res, resid_out, gattn8,
         u_other, e_other, table, _, wd_zero, wd_cross) = call_ab(
             hidden, heads_first(grad_q), heads_first(grad_kv), positions.reshape(1, tokens), inv_freq, swap, grad_h2,
             w_gate, w_up, w_down, heads_first(w_q), heads_first(w_kv), g_ffn, g_attn)
        (grad_wgate, _, grad_wup, _, grad_wdown, grad_wq, _, grad_wkv, _, q_out, kv_out, grad_hidden, gain_grads, *_) = call_c(
            q_width, grad_gate, grad_up, gate_w, up_w, normed_all, u_all, u_other, res_all, e_other, normed2, back_all, w_qkv,
            h_rows, grad_res, gains, gattn8, table, swap, wd_zero, wd_cross)
        (resid_out, grad_wgate, grad_wup, grad_wdown, grad_wq, grad_wkv, q_out, kv_out, grad_hidden, grad_gffn, grad_gattn) = call_out(
            (resid_out, grad_wgate, grad_wup, grad_wdown, grad_wq, grad_wkv, q_out, kv_out, grad_hidden), gain_grads)
        q_out, kv_out, grad_wq, grad_wkv = (heads_last(x) for x in (q_out, kv_out, grad_wq, grad_wkv))
        grad_gffn, grad_gattn = grad_gffn[0], grad_gattn[0]
        return (resid_out, q_out, kv_out, grad_hidden, grad_gffn, grad_gattn, grad_wgate, grad_wup, grad_wdown, grad_wq, grad_wkv)

    row_spec = P(("dp", "ty"), "tx")
    head_spec = P(("dp", "tx"), "ty", None)
    in_specs = (row_spec, P(("dp", "tx")), P("tx"), P("tx", "ty"), P("tx", "ty"), P("ty", "tx"), P("tx"), P("tx", "ty", None), P("tx", "ty", None), row_spec, head_spec, head_spec)
    out_specs = (row_spec, head_spec, head_spec, row_spec, P(("dp", "tx")), P(("dp", "tx")), P(("dp", "tx"), "ty"), P(("dp", "tx"), "ty"), P(("dp", "ty"), "tx"), head_spec, head_spec)
    return jax.shard_map(local_step, mesh=mesh, in_specs=in_specs, out_specs=out_specs, check_vma=False)
```

```python
import functools

import jax
import jax.numpy as jnp
import numpy as np
from jax import lax
from jax.experimental import pallas as pl
from jax.experimental.pallas import tpu as pltpu
from jax.sharding import PartitionSpec as P

NORM_EPS = 1e-5
ROPE_BASE = 10000.0
F32 = jnp.float32
BF16 = jnp.bfloat16


def dot(a, b, dims=(((1,), (0,)), ((), ()))):
    return lax.dot_general(a, b, dims, preferred_element_type=F32)


MESH = pl.DeviceIdType.MESH
ANY = pl.BlockSpec(memory_space=pl.ANY)
VMEM = pltpu.VMEM
NT_DIMS = (((1,), (1,)), ((), ()))
VMEM_LIMIT = 67000000


def ds(start, size, align=None):
    if isinstance(start, int):
        return pl.ds(start, size)
    return pl.ds(pl.multiple_of(start, align or size), size)


def mid(z):
    return jnp.logical_and(z > 0, z < 3)


def end(z):
    return jnp.logical_or(z == 0, z == 3)


def slots(z):
    return (z + 1 - 2 * (z % 2), 2 - z // 2, 3 - 3 * (z // 2))


def turn(x_ref, width, q_width, tokens, table_ref, swap_ref, back):
    step = min(256, tokens)

    @pl.loop(0, tokens // step)
    def _(r):
        cols = ds(r * step, step)
        for g in range(width // 128):
            rows = pl.ds(g * 128, 128)
            base = pl.ds(0 if g * 128 < q_width else 128, 128)
            x = x_ref[rows, cols]
            main = x.astype(F32) * table_ref[base, cols]
            side = dot(swap_ref[...], x) * table_ref[base, ds(tokens + r * step, step)]
            x_ref[rows, cols] = (main - side if back else main + side).astype(BF16)


def pick(i, z):
    s1, s2, s3 = slots(z)
    first, last = (3 - i) // 3, (i // 2) * (i % 2)
    return z * first + s1 * ((i % 2) * (1 - i // 2)) + s2 * ((i // 2) * (1 - i % 2)) + s3 * last


class Wires:
    def __init__(self, send, recv, local):
        self.send, self.recv, self.local = send, recv, local
        self.n_remote = 0
        self.n_local = 0

    def take(self, n=1):
        base = self.n_remote
        self.n_remote += n
        assert self.n_remote <= self.send.shape[0]
        return base

    def copy(self, src, dst, si, ri, **dev):
        return pltpu.make_async_remote_copy(
            src_ref=src, dst_ref=dst, send_sem=self.send.at[si], recv_sem=self.recv.at[ri],
            device_id=dev, device_id_type=MESH)

    def here(self, src, dst):
        i = self.n_local
        self.n_local += 1
        assert i < self.local.shape[0]
        c = pltpu.make_async_copy(src, dst, self.local.at[i])
        c.start()
        return c


def entry_barrier(axes, z):
    sem = pltpu.get_barrier_semaphore()
    for dev in axes:
        pl.semaphore_signal(sem, inc=1, device_id=dev, device_id_type=MESH)

    @pl.when(z > 0)
    def _():
        pl.semaphore_signal(sem, inc=1, device_id={"ty": z - 1}, device_id_type=MESH)

    @pl.when(z < 3)
    def _():
        pl.semaphore_signal(sem, inc=1, device_id={"ty": z + 1}, device_id_type=MESH)

    @pl.when(mid(z))
    def _():
        pl.semaphore_wait(sem, len(axes) + 2)

    @pl.when(end(z))
    def _():
        pl.semaphore_wait(sem, len(axes) + 1)


class LineGather:
    def __init__(self, net, buf, rows, z, off=0, part=None):
        self.net, self.buf, self.rows, self.z, self.off, self.part = net, buf, rows, z, off, part or rows
        self.base = net.take(8)
        self.slots = slots(z)

    def blk(self, b):
        return self.buf.at[ds(b * self.rows + self.off, self.part), :]

    def cp(self, b, side, target):
        return self.net.copy(self.blk(b), self.blk(b), self.base + side * 4 + b, self.base + b, ty=target)

    def start(self):
        z = self.z

        @pl.when(z < 3)
        def _():
            self.cp(z, 0, z + 1).start()

        @pl.when(z > 0)
        def _():
            self.cp(z, 1, z - 1).start()

    def take(self, i):
        b = self.slots[i]
        self.cp(b, 0, self.z).wait_recv()

    def forward(self, i):
        z, b = self.z, self.slots[i]
        target = 3 - z if i == 0 else 3 * (z - 1)
        self.cp(b, 0, target).start()

    def step1(self):
        self.take(0)

        @pl.when(mid(self.z))
        def _():
            self.forward(0)
            self.take(1)
            self.forward(1)

    def near_end(self):
        @pl.when(end(self.z))
        def _():
            self.take(0)

    def near_mid(self):
        @pl.when(mid(self.z))
        def _():
            self.take(1)
            self.forward(1)

    def far_mid(self):
        @pl.when(mid(self.z))
        def _():
            self.take(0)
            self.forward(0)

    def step2(self):
        @pl.when(end(self.z))
        def _():
            self.take(1)

    def step3_mid(self):
        @pl.when(mid(self.z))
        def _():
            self.take(2)
            self.forward(2)

    def step3_end(self):
        @pl.when(end(self.z))
        def _():
            self.take(2)

    def drain(self):
        z = self.z

        @pl.when(z < 3)
        def _():
            self.cp(z, 0, z + 1).wait_send()

        @pl.when(z > 0)
        def _():
            self.cp(z, 1, z - 1).wait_send()

        @pl.when(mid(z))
        def _():
            for i in range(3):
                self.cp(self.slots[i], 0, 3 - z if i == 0 else 3 * (z - 1)).wait_send()


class LineScatter:
    def __init__(self, net, part, rbuf, rows, z, off=0, size=None):
        self.net, self.part, self.rbuf, self.rows, self.z, self.off, self.size = net, part, rbuf, rows, z, off, size or rows
        self.base = net.take(5)
        self.slots = slots(z)
        one = (z % 2) * (1 - z // 2)
        self.dst = (self.slots[0] + (1 - z % 2) * (3 - z), self.slots[1] + 2 * one, self.slots[2])
        self.target = (z + 1 - 2 * (z % 2), 1 + z % 2, 1 + z % 2)

    def cp(self, i):
        return self.net.copy(
            self.part.at[self.view(self.slots[i]), :], self.rbuf.at[self.view(self.dst[i]), :],
            self.base + i, self.base + self.dst[i], ty=self.target[i])

    def view(self, b):
        return ds(b * self.rows + self.off, self.size)

    def wait_slot(self, s):
        view = self.rbuf.at[self.view(s), :]
        self.net.copy(view, view, self.base, self.base + s, ty=self.z).wait_recv()

    def send_end(self, i):
        @pl.when(end(self.z))
        def _():
            self.cp(i).start()

    def send_mid(self, i):
        @pl.when(mid(self.z))
        def _():
            b = self.slots[i]
            self.wait_slot(b)
            step = 16

            @pl.loop(0, self.size // step)
            def _(r):
                view = ds(b * self.rows + self.off + r * step, step)
                self.part[view, :] = (self.part[view, :].astype(F32) + self.rbuf[view, :].astype(F32)).astype(BF16)

            self.cp(i).start()

    def finish(self):
        z = self.z

        @pl.when(z < 3)
        def _():
            self.wait_slot(z)

        @pl.when(z > 0)
        def _():
            self.wait_slot(4)

    def drain(self):
        for i in range(3):
            self.cp(i).wait_send()


class WeightGather:
    def __init__(self, net, w, full, pos, by_rows, chunks, direct=0):
        self.net, self.w, self.full, self.by_rows = net, w, full, by_rows
        self.dp, self.t1, self.t2 = pos
        self.half = w.shape[0] // 2
        self.width = w.shape[0] if by_rows else w.shape[1]
        self.chunks, self.direct = chunks, direct
        self.base = net.take(1 + 4 * chunks + direct)

    def area(self, half, ch):
        if self.by_rows:
            n = self.w.shape[1] // self.chunks
            return ds(half * self.half, self.half, 16), self.half, pl.ds(ch * n, n)
        n = self.half // self.chunks
        return ds(half * self.half + ch * n, n, 16), n, pl.ds(0, self.width)

    def src(self, half, ch):
        rows, _, cols = self.area(half, ch)
        return self.w.at[rows, cols]

    def dst(self, k, half, ch):
        if self.by_rows:
            _, _, cols = self.area(half, ch)
            return self.full.at[ds(k * self.width + half * self.half, self.half, 16), cols]
        rows, _, _ = self.area(half, ch)
        return self.full.at[rows, pl.ds(k * self.width, self.width)]

    def whole(self, k):
        if self.by_rows:
            return self.full.at[pl.ds(k * self.width, self.width), :]
        return self.full.at[:, pl.ds(k * self.width, self.width)]

    def near(self, ch):
        i = self.base + 1 + ch
        return self.net.copy(self.src(self.dp, ch), self.dst(2, self.dp, ch), i, i, tx=self.t2)

    def cross(self, ch, half):
        i = self.base + 1 + self.chunks + ch
        return self.net.copy(self.dst(2, half, ch), self.dst(2, half, ch), i, i, dp=1 - self.dp)

    def diag(self, ch, which, half):
        i = self.base + 1 + (2 + which) * self.chunks + ch
        return self.net.copy(self.dst(2, half, ch), self.dst(3, half, ch), i, i, tx=self.t1)

    def mate(self):
        return self.net.copy(self.w, self.whole(1), self.base, self.base, tx=self.t1)

    def straight(self, n, half):
        ch = self.chunks - 1 - n
        i = self.base + 1 + 4 * self.chunks + n
        return self.net.copy(self.src(half, ch), self.dst(2, half, ch), i, i, tx=self.t2)

    def start_y(self):
        for ch in range(self.chunks):
            self.near(ch).start()
        for n in range(self.direct):
            self.straight(n, 1 - self.dp).start()

    def start_local(self):
        self.own = self.net.here(self.w, self.whole(0))
        self.mate().start()

    def y_event(self, ch):
        self.near(ch).wait_recv()
        if ch < self.chunks - self.direct:
            self.cross(ch, self.dp).start()
        self.diag(ch, 0, self.dp).start()

    def x_event(self, ch):
        if ch < self.chunks - self.direct:
            self.cross(ch, 1 - self.dp).wait_recv()
        else:
            self.straight(self.chunks - 1 - ch, 1 - self.dp).wait_recv()
        self.diag(ch, 1, 1 - self.dp).start()

    def finish_local(self):
        self.own.wait()
        self.mate().wait_recv()

    def finish(self, ch):
        self.diag(ch, 0, self.dp).wait_recv()
        self.diag(ch, 1, 1 - self.dp).wait_recv()

    def drain(self):
        self.mate().wait_send()
        for ch in range(self.chunks):
            self.near(ch).wait_send()
            if ch < self.chunks - self.direct:
                self.cross(ch, self.dp).wait_send()
            else:
                self.straight(self.chunks - 1 - ch, 1 - self.dp).wait_send()
            self.diag(ch, 0, self.dp).wait_send()
            self.diag(ch, 1, 1 - self.dp).wait_send()


def down_split(ff):
    return ff * 5 // 8


def places():
    dp, z, tx = lax.axis_index("dp"), lax.axis_index("ty"), lax.axis_index("tx")
    return dp, z, tx, (tx, tx + 1 - 2 * (tx % 2), (tx + 2) % 4, 3 - tx)


ROWS_ROWS = (((0,), (0,)), ((), ()))


class GradReduce:
    def __init__(self, net, peer, tile, tiles, st3, st1, cross, stage, got2, got0, got_y, out, out_tiles):
        self.net, self.peer, self.tile, self.tiles = net, peer, tile, tiles
        self.st3, self.st1, self.cross, self.stage = st3, st1, cross, stage
        self.got2, self.got0, self.got_y, self.out, self.out_tiles = got2, got0, got_y, out, out_tiles
        self.src = None
        self.base = net.take(3)
        self.rows, self.w = out.shape[0], out.shape[1] // tiles

    def cp(self, i):
        src, dst, to = ((self.st3, self.got2, 1), (self.st1, self.got0, 1), (self.src or self.cross, self.got_y, 2))[i]
        return self.net.copy(src, dst, self.base + i, self.base + i, tx=self.peer[to])

    def fill(self, k, ref):
        @pl.loop(0, self.tiles)
        def _(j):
            ref[:, ds(j * self.w, self.w)] = self.tile(k, j).astype(BF16)

    def step3(self):
        self.fill(3, self.st3)
        self.cp(0).start()

    def step1(self):
        self.fill(1, self.st1)
        self.cp(1).start()

    def step2(self, received=False):
        if not received:
            self.cp(0).wait_recv()
        self.net.here(self.got2, self.stage).wait()

        @pl.loop(0, self.tiles)
        def _(j):
            cols = ds(j * self.w, self.w)
            self.cross[:, cols] = (self.tile(2, j) + self.stage[:, cols].astype(F32)).astype(BF16)

    def send(self, src=None):
        self.src = src
        self.cp(2).start()

    def step0(self, far):
        self.cp(1).wait_recv()
        self.cp(2).wait_recv()
        loads = [self.net.here(self.got0, self.stage), self.net.here(self.got_y, far)]
        for c in loads:
            c.wait()
        base = self.net.n_local
        self.net.n_local += 2

        def put(j, slot):
            src = self.out_tiles.at[slot, pl.ds(0, self.rows), pl.ds(0, self.w)]
            return pltpu.make_async_copy(src, self.out.at[:, ds(j * self.w, self.w)], self.net.local.at[base + slot])

        @pl.loop(0, self.tiles)
        def _(j):
            cols = ds(j * self.w, self.w)
            slot = j % 2

            @pl.when(j >= 2)
            def _():
                put(j, slot).wait()

            self.out_tiles[slot, pl.ds(0, self.rows), pl.ds(0, self.w)] = self.tile(0, j) + (self.stage[:, cols].astype(F32) + far[:, cols].astype(F32))
            put(j, slot).start()

        for slot in range(min(2, self.tiles)):
            put(slot, slot).wait()

    def sent_locally(self):
        self.cp(0).wait_send()
        self.cp(1).wait_send()

    def sent(self):
        self.cp(2).wait_send()


def kernel_ab(q_width, hid, eqh, ekvh, posh, invh, swaph, dh2h, wg, wu, wd, wq, wkv, gfh, gah,
              n_o, da_o, db_o, u_o, wg_o, wu_o, wq_o, eq_o, h_o, g_o, e_o, n2_o, dres_o, home_o, dg_o, ux_o, ex_o, tab_o, d2_o, d0_o, dc_o,
              rows, dh2_v, n2_v, res_v, dres_v, n_v, a_v, b_v, wg_v, wu_v, wd_v, wq_v, eq_v, p_v, rbuf, rbuf2, gains, dg_v, swap_v, pos_v, inv_v, gf_v, ga_v, gin, send, recv, local):
    dp, z, tx, peer = places()
    sub, dim = rows.shape
    tokens = 4 * sub
    width = eq_v.shape[0]
    dt = dim // 4
    ff = wg.shape[1]
    wide = min(1024, ff)
    tile = min(512, ff)
    dwide = min(1024, dim)
    dtile = min(512, dim)
    hs, cs = sub // 2, sub // 8
    split = down_split(ff)
    net = Wires(send, recv, local)
    gain_in = [net.here(gfh, gf_v), net.here(gah, ga_v)]
    turn_in = [net.here(eqh, p_v.at[pl.ds(0, q_width), pl.ds(0, tokens)]), net.here(ekvh, p_v.at[pl.ds(q_width, width - q_width), pl.ds(0, tokens)]),
               net.here(swaph, swap_v), net.here(posh, pos_v), net.here(invh, inv_v)]
    entry_barrier([{"tx": peer[1]}, {"tx": peer[2]}, {"tx": peer[3]}, {"dp": 1 - dp}], z)

    pos = (dp, peer[1], peer[2])
    far_first = (2, 3, 1)
    g_id, h_id, e_id, d_id, o_id, u_id, x_id = (net.take(4), net.take(4), net.take(4), net.take(4), net.take(8), net.take(12), net.take(24))
    u_v = wg_v.at[pl.ds(0, tokens), :]
    e_v = wg_v.at[pl.ds(tokens, tokens), :]

    def g_cp(k):
        return net.copy(gin, gains.at[:, pl.ds(k * dt, dt)], g_id + k, g_id + k, tx=peer[k])

    def h_cp(k):
        return net.copy(hid.at[ds(peer[k] * sub, sub), :], rows.at[:, pl.ds(k * dt, dt)], h_id + k, h_id + k, tx=peer[k])

    def e_cp(k, block):
        return net.copy(p_v.at[pl.ds(0, width), ds(peer[k] * sub, sub)], eq_v.at[:, ds(block * sub, sub)], e_id + k, e_id + k, tx=peer[k])

    def d_cp(k):
        return net.copy(dh2h.at[ds(peer[k] * sub, sub), :], dh2_v.at[:, pl.ds(k * dt, dt)], d_id + k, d_id + k, tx=peer[k])

    def o_cp(k, block, half):
        i = o_id + half * 4 + k
        return net.copy(res_v.at[pl.ds(half * hs, hs), pl.ds(k * dt, dt)], home_o.at[ds(block * sub + half * hs, hs), :], i, i, tx=peer[k])

    def ux_cp(k, b):
        view = ds(b * sub, sub)
        cols = pl.ds(0, split)
        src = ux_o.at[1, view, :] if k == 3 else wg_v.at[view, cols]
        i = u_id + (k - 1) * 4 + b
        return net.copy(src, ux_o.at[k - 1, view, :], i, i, tx=peer[1] if k == 3 else peer[k])

    def ex_cp(k, b, half):
        i = x_id + half * 12 + (k - 1) * 4 + b
        view = ds(b * sub + half * hs, hs)
        return net.copy(wg_v.at[ds(tokens + b * sub + half * hs, hs), pl.ds(k * dt, dt)], ex_o.at[k - 1, view, :], i, i, tx=peer[k])

    gate = WeightGather(net, wg, wg_v, pos, True, 2)
    up = WeightGather(net, wu, wu_v, pos, True, 2)
    down = WeightGather(net, wd, wd_v, pos, False, 4, 1)
    q_w = WeightGather(net, wq, wq_v.at[pl.ds(0, q_width), :], pos, False, 1)
    kv_w = WeightGather(net, wkv, wq_v.at[pl.ds(q_width, width - q_width), :], pos, False, 1)
    ag = LineGather(net, n_v, sub, z)
    rsc = LineScatter(net, p_v, rbuf, sub, z)
    rs2 = [LineScatter(net, n_v, rbuf2, sub, z, c * cs, cs) for c in range(8)]
    ag2 = [LineGather(net, e_v, sub, z, c * cs, cs) for c in range(8)]

    for k in far_first:
        h_cp(k).start()
    for c in gain_in:
        c.wait()
    gin[...] = jnp.broadcast_to(gf_v[...].astype(F32)[None, :], gin.shape)
    gin[1:2, :] = ga_v[...].astype(F32)[None, :]
    g_own = net.here(gin, gains.at[:, pl.ds(0, dt)])
    h_own = net.here(hid.at[ds(tx * sub, sub), :], rows.at[:, pl.ds(0, dt)])
    for w in (q_w, kv_w, gate, up, down):
        w.start_local()
    for k in far_first:
        g_cp(k).start()
    for c in turn_in:
        c.wait()

    @pl.loop(0, tokens // 128)
    def _(i):
        part = 128
        cos_c, sin_c = ds(i * part, part), ds(tokens + i * part, part)
        q_r, kv_r = pl.ds(0, 128), pl.ds(128, 128)
        angles = inv_v[...] * pos_v[:, cos_c].astype(F32)
        dres_v[q_r, sin_c] = jnp.sin(angles)
        dres_v[q_r, cos_c] = jnp.cos(angles)

        @pl.when(z < 2)
        def _():
            dres_v[kv_r, cos_c] = dres_v[q_r, cos_c]
            dres_v[kv_r, sin_c] = dres_v[q_r, sin_c]

        @pl.when(z >= 2)
        def _():
            dres_v[kv_r, cos_c] = jnp.ones((128, part), F32)
            dres_v[kv_r, sin_c] = jnp.zeros((128, part), F32)

    tab_out = net.here(dres_v.at[pl.ds(0, 256), pl.ds(0, 2 * tokens)], tab_o)
    turn(p_v, width, q_width, tokens, dres_v, swap_v, True)
    for k in far_first:
        e_cp(k, tx).start()
    e_own = net.here(p_v.at[pl.ds(0, width), ds(tx * sub, sub)], eq_v.at[:, ds(tx * sub, sub)])
    for w in (q_w, kv_w, gate, up, down):
        w.start_y()
    for k in far_first:
        d_cp(k).start()
    d_own = net.here(dh2h.at[ds(tx * sub, sub), :], dh2_v.at[:, pl.ds(0, dt)])

    for k in far_first:
        g_cp(k).wait_recv()
        h_cp(k).wait_recv()
    g_own.wait()
    h_own.wait()

    @pl.loop(0, sub // 16)
    def _(r):
        x = rows[ds(r * 16, 16), :].astype(F32)
        inv = lax.rsqrt(jnp.sum(x * x, axis=1, keepdims=True) / dim + NORM_EPS)
        n_v[ds(z * sub + r * 16, 16), :] = (x * inv * gains[0:1, :]).astype(BF16)

    ag.start()
    outs = [net.here(rows, h_o), net.here(gains, g_o)]
    for k in far_first:
        e_cp(k, peer[k]).wait_recv()
    e_own.wait()
    ag.step1()
    for w in (q_w, kv_w):
        w.y_event(0)
    for w in (q_w, kv_w):
        w.x_event(0)
    for w in (q_w, kv_w):
        w.finish_local()
        w.finish(0)
    for k in far_first:
        e_cp(k, tx).wait_send()

    def n2_block(b):
        @pl.loop(0, dim // dtile)
        def _(j):
            cols = ds(j * dtile, dtile)
            p_v[ds(b * sub, sub), cols] = dot(eq_v[:, ds(b * sub, sub)], wq_v[:, cols], ROWS_ROWS).astype(BF16)

    @pl.loop(0, 4)
    def _(i):
        n2_block(pick(3 - i, z))
        for step in range(3):
            pl.when(i == step)(lambda step=step: rsc.send_end(2 - step))
        pl.when(i == 0)(lambda: gate.y_event(0))

    wide = ff // 2

    def gate_part(b, c):
        cols = pl.ds(c * wide, wide)
        a_v[ds(b * sub, sub), cols] = dot(n_v[ds(b * sub, sub), :], wg_v[:, cols]).astype(BF16)

    def up_part(b, c):
        cols = pl.ds(c * wide, wide)
        bb = dot(n_v[ds(b * sub, sub), :], wu_v[:, cols]).astype(BF16)
        b_v[ds(b * sub, sub), cols] = bb
        aa = a_v[ds(b * sub, sub), cols].astype(F32)
        wg_v[ds(b * sub, sub), cols] = (aa * jax.nn.sigmoid(aa) * bb.astype(F32)).astype(BF16)

    def down_part(b, j):
        cols = pl.ds(j * (dim // 2), dim // 2)
        n_v[ds(b * sub, sub), cols] = dot(wg_v[ds(b * sub, sub), :], wd_v[:, cols]).astype(BF16)

    outs += [net.here(wq_v, wq_o), net.here(eq_v, eq_o)]
    gate.finish_local()
    gate.y_event(1)
    ag.step2()
    ag.step3_mid()
    gate.x_event(0)
    gate.finish(0)

    @pl.loop(0, 3)
    def _(i):
        gate_part(pick(i, z), 0)

    up.y_event(0)
    gate.x_event(1)
    rsc.send_mid(2)
    gate.finish(1)
    wg_out = net.here(wg_v, wg_o)

    @pl.loop(0, 3)
    def _(i):
        gate_part(pick(i, z), 1)

    up.finish_local()
    up.y_event(1)
    up.x_event(0)
    up.finish(0)
    ag.step3_end()

    @pl.loop(0, 2)
    def _(c):
        cols = ds(c * wide, wide)
        b = pick(3, z)
        a_v[ds(b * sub, sub), cols] = dot(n_v[ds(b * sub, sub), :], wg_v[:, cols]).astype(BF16)

    wg_out.wait()
    n_out = net.here(n_v, n_o)

    @pl.loop(0, 4)
    def _(i):
        pl.when(i == 1)(lambda: down.y_event(0))
        pl.when(i == 2)(lambda: down.y_event(1))
        pl.when(i == 3)(lambda: up.x_event(1))
        up_part(pick(i, z), 0)

    def up_events_1():
        rsc.send_mid(1)
        rsc.send_mid(0)
        down.x_event(0)

    def up_events_2():
        down.y_event(2)

    def up_events_3():
        down.y_event(3)
        down.x_event(1)

    up.finish(1)
    outs.append(net.here(wu_v, wu_o))

    @pl.loop(0, 4)
    def _(i):
        pl.when(i == 1)(up_events_1)
        pl.when(i == 2)(up_events_2)
        pl.when(i == 3)(up_events_3)
        b = pick(i, z)
        up_part(b, 1)
        ux_cp(2, b).start()
        ux_cp(1, b).start()

    outs.append(net.here(u_v, u_o))
    ag.drain()
    gate.drain()
    n_out.wait()
    down.finish_local()

    @pl.loop(0, 4)
    def _(i):
        pl.when(i == 2)(lambda: down.x_event(2))
        pl.when(i == 3)(lambda: down.x_event(3))
        down_part(pick(3 - i, z), 0)

    for ch in range(4):
        down.finish(ch)

    @pl.loop(0, 4)
    def _(i):
        down_part(pick(3 - i, z), 1)
        for step in range(3):
            pl.when(i == step)(lambda step=step: rs2[0].send_end(2 - step))

    for c in range(1, 8):
        for i in (2, 1, 0):
            rs2[c].send_end(i)
    dg_v[...] = jnp.zeros_like(dg_v)
    step = 16

    def norm_chunk(c):
        @pl.loop(0, cs // step)
        def _(r):
            at = c * cs + r * step
            view, mine, far = ds(at, step), ds(z * sub + at, step), ds(4 * sub + at, step)

            def whole(part, got):
                right = jnp.where(z < 3, got[mine, :].astype(F32), 0.0)
                left = jnp.where(z > 0, got[far, :].astype(F32), 0.0)
                return part[mine, :].astype(F32) + right + left

            resid = (rows[view, :].astype(F32) + whole(n_v, rbuf2)).astype(BF16)
            dy = whole(p_v, rbuf)
            res_v[view, :] = resid
            x = resid.astype(F32)
            inv = lax.rsqrt(jnp.sum(x * x, axis=1, keepdims=True) / dim + NORM_EPS)
            xhat = x * inv
            gain = gains[1:2, :]
            n2_v[view, :] = (xhat * gain).astype(BF16)
            part = dy * xhat
            dg_v[...] += part[:8] + part[8:]
            inner = jnp.sum(part * gain, axis=1, keepdims=True) / dim
            dres = dh2_v[view, :].astype(F32) + inv * (dy * gain) - xhat * (inv * inner)
            dres_v[view, pl.ds(0, dim)] = dres
            wg_v[ds(tokens + z * sub + at, step), :] = dres.astype(BF16)

    def spread(b, half):
        for k in far_first:
            ex_cp(k, b, half).start()

    def back_tile(b, j):
        view, cols = ds(b * sub, sub), ds(j * (ff // 4), ff // 4)
        du = dot(wg_v[ds(tokens + b * sub, sub), :], wd_v[ds(j * (ff // 4), ff // 4), :], NT_DIMS)
        aa = a_v[view, cols].astype(F32)
        bb = b_v[view, cols].astype(F32)
        sig = jax.nn.sigmoid(aa)
        a_v[view, cols] = (du * bb * sig * (1.0 + aa * (1.0 - sig))).astype(BF16)
        b_v[view, cols] = (du * aa * sig).astype(BF16)

    def scatter(i, c):
        return lambda: rs2[c].send_mid(i)

    def gathered(i, c):
        def go():
            ag2[c].take(i)
            pl.when(mid(z))(lambda: ag2[c].forward(i))
            if c % 4 == 3:
                spread(ag.slots[i], c // 4)
        return go

    def run(ops):
        def go():
            for op in ops:
                op()
        return go

    before_mid = (
        (scatter(2, 0), scatter(1, 0), scatter(0, 0)),
        (scatter(2, 1), scatter(1, 1), gathered(1, 0), scatter(0, 1), scatter(2, 2)),
        (scatter(1, 2), scatter(0, 2), gathered(1, 1), scatter(2, 3)),
        (scatter(1, 3), scatter(0, 3), gathered(1, 2), scatter(2, 4)),
        (scatter(1, 4), scatter(0, 4), gathered(1, 3), scatter(2, 5)),
        (scatter(1, 5), scatter(0, 5), gathered(1, 4), scatter(2, 6)),
        (scatter(1, 6), scatter(0, 6), gathered(1, 5), scatter(2, 7)),
        (scatter(1, 7), scatter(0, 7), gathered(1, 6), gathered(0, 0)))
    before_end = (
        (),
        (gathered(0, 0), gathered(1, 0)),
        (gathered(0, 1),),
        (gathered(1, 1), gathered(0, 2)),
        (gathered(1, 2), gathered(0, 3)),
        (gathered(1, 3), gathered(0, 4)),
        (gathered(1, 4), gathered(0, 5)),
        (gathered(1, 5), gathered(0, 6)))
    after_mid = {1: (gathered(0, 1),),
                 2: (gathered(2, 0),),
                 3: (gathered(0, 2),),
                 4: (gathered(1, 7),),
                 5: (gathered(0, 3),),
                 6: (gathered(2, 1),),
                 7: (gathered(0, 4),),
                 8: (gathered(2, 2), gathered(0, 5), gathered(2, 3), gathered(0, 6), gathered(2, 4), gathered(0, 7)),
                 10: (gathered(2, 5),),
                 12: (gathered(2, 6), gathered(2, 7))}
    after_end = {2: (gathered(1, 6),),
                 4: (gathered(0, 7),),
                 7: (gathered(2, 0),),
                 8: (gathered(1, 7),),
                 11: (gathered(2, 1),),
                 12: (gathered(2, 2), gathered(2, 3), gathered(2, 4), gathered(2, 5), gathered(2, 6), gathered(2, 7))}

    for c in range(8):
        pl.when(mid(z))(run(before_mid[c]))
        pl.when(end(z))(run(before_end[c]))
        if c == 0:
            rsc.finish()
            for k in far_first:
                d_cp(k).wait_recv()
            d_own.wait()
            tab_out.wait()
        rs2[c].finish()
        norm_chunk(c)
        ag2[c].start()
        if c % 4 == 3:
            spread(z, c // 4)
            for k in far_first:
                o_cp(k, tx, c // 4).start()

    outs += [net.here(res_v.at[:, pl.ds(0, dt)], home_o.at[ds(tx * sub, sub), :]), net.here(n2_v, n2_o), net.here(dres_v.at[pl.ds(0, sub), pl.ds(0, dim)], dres_o), net.here(dg_v, dg_o)]
    rsc.drain()
    for c in range(8):
        rs2[c].drain()
    middle = (z + 1) // 2 % 2

    def u_forward():
        for b in range(4):
            ux_cp(2, b).wait_recv()
            ux_cp(3, b).start()

    @pl.loop(0, 16)
    def _(t):
        for at, ops in after_mid.items():
            pl.when(jnp.logical_and(t == at, mid(z)))(run(ops))
        for at, ops in after_end.items():
            pl.when(jnp.logical_and(t == at, end(z)))(run(ops))
        pl.when(t == 8)(u_forward)
        i = t // 4
        inner = (i + 1) // 2 % 2
        back_tile(pick(i + middle * inner * (3 - 2 * i), z), t % 4)

    outs.append(net.here(e_v, e_o))
    outs += [net.here(a_v, da_o), net.here(b_v, db_o)]

    def down_tile(k, j):
        return dot(wg_v[pl.ds(0, tokens), pl.ds(split, ff - split)], wg_v[pl.ds(tokens, tokens), ds(k * dt + j * (dt // 2), dt // 2)], ROWS_ROWS)

    quarter = [rbuf.at[pl.ds(0, ff - split), pl.ds(i * dt, dt)] for i in range(4)]
    part_d = GradReduce(net, peer, down_tile, 2, quarter[0], quarter[1], quarter[2], quarter[3], d2_o, d0_o, None, dc_o, None)
    part_d.step3()
    part_d.step1()
    part_d.step2()
    outs.append(net.here(quarter[2], dc_o))
    for k in far_first:
        o_cp(k, peer[k], 0).wait_recv()
        o_cp(k, peer[k], 1).wait_recv()
        for b in range(4):
            ex_cp(k, b, 0).wait_recv()
            ex_cp(k, b, 1).wait_recv()
    for b in range(4):
        ux_cp(1, b).wait_recv()
        ux_cp(3, b).wait_recv()
    for c in outs:
        c.wait()
    for k in far_first:
        g_cp(k).wait_send()
        h_cp(k).wait_send()
        d_cp(k).wait_send()
        o_cp(k, tx, 0).wait_send()
        o_cp(k, tx, 1).wait_send()
        for b in range(4):
            ux_cp(k, b).wait_send()
            ex_cp(k, b, 0).wait_send()
            ex_cp(k, b, 1).wait_send()
    for w in (q_w, kv_w, up, down):
        w.drain()
    for c in range(8):
        ag2[c].drain()
    part_d.cp(1).wait_recv()
    part_d.sent_locally()


def call_ab(hid, eqh, ekvh, pos, inv, swap, dh2h, wg, wu, wd, wq, wkv, gf, ga):
    tokens, dt = hid.shape
    sub, dim, ff, q_width = tokens // 4, dt * 4, wg.shape[1], wq.shape[0]
    width = q_width + wkv.shape[0]
    s = jax.ShapeDtypeStruct
    tok_ff, tok_d, row = s((tokens, ff), BF16), s((tokens, dim), BF16), s((sub, dim), BF16)
    shapes = (tok_d, tok_ff, tok_ff, tok_ff, s((dim, ff), BF16), s((dim, ff), BF16), s((width, dim), BF16), s((width, tokens), BF16),
              row, s((8, dim), F32), tok_d, row, s((sub, dim), F32), s((tokens, dt), BF16), s((8, dim), F32),
              s((3, tokens, down_split(ff)), BF16), s((3, tokens, dt), BF16), s((256, 2 * tokens), F32)) + (s((ff - down_split(ff), dt), BF16),) * 3
    vrow, vtok, vff = VMEM((sub, dim), BF16), VMEM((tokens, dim), BF16), VMEM((tokens, ff), BF16)
    return pl.pallas_call(
        functools.partial(kernel_ab, q_width), out_shape=shapes, in_specs=[ANY] * 14, out_specs=[ANY] * len(shapes),
        scratch_shapes=[
            vrow, vrow, vrow, vrow, VMEM((max(sub, 256), max(dim, 2 * tokens)), F32), vtok, vff, vff, VMEM((dim, ff), BF16), VMEM((dim, ff), BF16), VMEM((ff, dim), BF16),
            VMEM((width, dim), BF16), VMEM((width, tokens), BF16), vtok, VMEM((5 * sub, dim), BF16), VMEM((5 * sub, dim), BF16),
            VMEM((8, dim), F32), VMEM((8, dim), F32), VMEM((128, 128), BF16), VMEM((1, tokens), jnp.int32), VMEM((128, 128), F32),
            VMEM((dt,), BF16), VMEM((dt,), BF16), VMEM((8, dt), F32),
            pltpu.SemaphoreType.DMA((236,)), pltpu.SemaphoreType.DMA((236,)), pltpu.SemaphoreType.DMA((48,))],
        compiler_params=pltpu.CompilerParams(collective_id=0, has_side_effects=True, vmem_limit_bytes=VMEM_LIMIT),
        cost_estimate=pl.CostEstimate(flops=20 * tokens * dim * ff, bytes_accessed=100000000, transcendentals=0), name="phase_ab",
    )(hid, eqh, ekvh, pos, inv, swap, dh2h, wg, wu, wd, wq, wkv, gf, ga)


def kernel_c(q_width, da_h, db_h, wg_h, wu_h, n_h, u_h, ux_h, e_h, ex_h, n2_h, eq_h, wq_h, h_h, dres_h, g_h, dga_h, tabh, swaph, d0, dc,
             wgo, wgy, wuo, wuy, wdo, wqo, wqy, wvo, wvy, q_o, kv_o, dh_o, dg_o, g2, g0, u2, u0, q2, q0, v2, v0, qx, dy,
             wg_v, wu_v, da_v, db_v, n_v, p_v, rbuf, n2_v, st3, st1, cross_g, cross_u, stage, tiles_v, dres_v, wq_v, eq_v,
             gains, dg_v, dgr, dgz, tab_v, swap_v, send, recv, local):
    dp, z, tx, peer = places()
    tokens, ff = da_v.shape
    sub, dim = dres_v.shape
    dt = dim // 4
    width = eq_v.shape[0]
    tile = ff // 4
    dtile = min(512, dim)
    qt = min(256, tile)
    far_first = (2, 3, 1)
    net = Wires(send, recv, local)
    n2_in = net.here(n2_h, n2_v.at[ds(z * sub, sub), :])
    first = [net.here(n_h, n_v), net.here(da_h, da_v)]
    second = [net.here(db_h, db_v), net.here(wg_h, wg_v), net.here(wu_h, wu_v)]
    third = [net.here(wq_h, wq_v), net.here(eq_h, eq_v), net.here(dres_h, dres_v), net.here(g_h, gains),
             net.here(dga_h, dg_v.at[pl.ds(8, 8), :]), net.here(tabh, tab_v), net.here(swaph, swap_v)]
    sem = pltpu.get_barrier_semaphore()
    zs = tuple((z + i) % 4 for i in range(4))
    for i in (1, 2, 3):
        pl.semaphore_signal(sem, inc=1, device_id={"tx": peer[i]}, device_id_type=MESH)
        pl.semaphore_signal(sem, inc=1, device_id={"ty": zs[i]}, device_id_type=MESH)
    pl.semaphore_wait(sem, 6)
    rsc = LineScatter(net, p_v, rbuf, sub, z)
    ag = LineGather(net, n2_v, sub, z)
    q_id, h_id, t_id, z_id = net.take(4), net.take(4), net.take(4), net.take(4)

    def grad_tile(lhs, rhs, w):
        def go(k, j):
            cols = pl.ds(j * w, w) if isinstance(j, int) else ds(j * w, w)
            return dot(lhs[:, pl.ds(k * dt, dt)], rhs[:, cols], ROWS_ROWS)
        return go

    gate = GradReduce(net, peer, grad_tile(n_v, da_v, tile), ff // tile, st3, st1, cross_g, stage, g2, g0, wgy, wgo, tiles_v)
    up = GradReduce(net, peer, grad_tile(n_v, db_v, tile), ff // tile, st3, st1, cross_u, stage, u2, u0, wuy, wuo, tiles_v)
    d_id = net.take(1)

    def dy_cp():
        return net.copy(dc, dy, d_id, d_id, tx=peer[2])

    dy_cp().start()

    def head_grad(first, rows, got2, got0, got_y, out):
        corner = [da_v.at[pl.ds(first, rows), pl.ds(c * dt, dt)] for c in range(4)]

        def tile_of(k, j):
            return dot(eq_v[pl.ds(first, rows), :], n2_v[:, ds(k * dt + j * qt, qt)])

        return GradReduce(net, peer, tile_of, dt // qt, *corner, got2, got0, got_y, out, tiles_v)

    heads = (head_grad(0, q_width, q2, q0, wqy, wqo), head_grad(q_width, width - q_width, v2, v0, wvy, wvo))

    def dn_block(b):
        rows = ds(b * sub, sub)

        @pl.loop(0, dim // dtile)
        def _(j):
            wr = ds(j * dtile, dtile)
            p_v[rows, wr] = (dot(da_v[rows, :], wg_v[wr, :], NT_DIMS) + dot(db_v[rows, :], wu_v[wr, :], NT_DIMS)).astype(BF16)

    n2_in.wait()
    ag.start()
    for c in first:
        c.wait()
    gate.step3()
    gate.step1()
    gate.step2()
    gate.send()
    for c in second:
        c.wait()

    @pl.loop(0, 4)
    def _(i):
        @pl.when(i == 1)
        def _():
            gate.sent_locally()
            up.step3()
            up.step1()
            ag.step1()

        dn_block(pick(3 - i, z))
        for step in range(3):
            pl.when(i == step)(lambda step=step: rsc.send_end(2 - step))

    up.step2()
    up.send()
    rsc.send_mid(2)
    ag.step2()
    ag.step3_mid()
    up.sent_locally()
    h_in = net.here(h_h, st3.at[pl.ds(0, sub), :])
    gate.step0(st1)
    gate.sent()

    e_in = [net.here(e_h.at[:, pl.ds(0, dt)], wu_v.at[pl.ds(0, tokens), pl.ds(0, dt)])]
    for k in (1, 2, 3):
        e_in.append(net.here(ex_h.at[k - 1], wu_v.at[pl.ds(0, tokens), pl.ds(k * dt, dt)]))

    piece = ff // 8
    exchanged, n_pieces = down_split(ff) // piece, 8

    def u_place(j, k):
        return wg_v.at[pl.ds((j % 2) * tokens, tokens), pl.ds(k * piece, piece)]

    def sums(j, n):
        return stage.at[pl.ds((j % 2) * piece, piece), pl.ds(n * dt, dt)]

    def u_load(j):
        cols = pl.ds(j * piece, piece)
        if j < exchanged:
            return [net.here(u_h.at[:, cols] if k == 0 else ux_h.at[k - 1, :, cols], u_place(j, k)) for k in range(4)]
        rows = pl.ds((j - exchanged) * piece, piece)
        return [net.here(u_h.at[:, cols], u_place(j, 0)), net.here(d0.at[rows, :], sums(j, 0)), net.here(dy.at[rows, :], sums(j, 1))]

    loads, stores = {}, {}

    def down_run(js):
        for j in js:
            for c in loads.pop(j):
                c.wait()
            if j >= 2:
                stores.pop(j - 2).wait()
            acc = None if j < exchanged else sums(j, 0)[...].astype(F32) + sums(j, 1)[...].astype(F32)
            for k in range(4 if j < exchanged else 1):
                part = dot(u_place(j, k)[...], wu_v[pl.ds(0, tokens), pl.ds(k * dt, dt)], ROWS_ROWS)
                acc = part if acc is None else acc + part
            place = tiles_v.at[j % 2, pl.ds(0, piece), pl.ds(0, dt)]
            tiles_v[j % 2, pl.ds(0, piece), pl.ds(0, dt)] = acc
            stores[j] = net.here(place, wdo.at[pl.ds(j * piece, piece), :])
            if j + 2 < n_pieces:
                loads[j + 2] = u_load(j + 2)

    loads[0], loads[1] = u_load(0), u_load(1)
    rsc.send_mid(1)
    rsc.send_mid(0)
    for c in e_in:
        c.wait()
    down_run((0, 1))
    for c in third:
        c.wait()
    ag.step3_end()

    @pl.loop(0, width // qt)
    def _(j):
        wu_v[ds(tokens + j * qt, qt), pl.ds(0, tokens)] = dot(wq_v[ds(j * qt, qt), :], n2_v[...], NT_DIMS).astype(BF16)

    def q_cp(k, block):
        return net.copy(wu_v.at[pl.ds(tokens, width), ds(peer[k] * sub, sub)], qx.at[:, ds(block * sub, sub)], q_id + k, q_id + k, tx=peer[k])

    for k in far_first:
        q_cp(k, tx).start()
    q_own = net.here(wu_v.at[pl.ds(tokens, width), ds(tx * sub, sub)], qx.at[:, ds(tx * sub, sub)])
    for part in heads:
        part.step3()
        part.step1()
    dy_cp().wait_recv()
    for part in heads:
        part.step2()
        part.send()
    down_run(range(2, n_pieces))
    h_in.wait()
    rsc.finish()
    dg_v[pl.ds(0, 8), :] = jnp.zeros((8, dim), F32)
    step = 16

    @pl.loop(0, sub // step)
    def _(r):
        view, mine, far = ds(r * step, step), ds(z * sub + r * step, step), ds(4 * sub + r * step, step)
        right = jnp.where(z < 3, rbuf[mine, :].astype(F32), 0.0)
        left = jnp.where(z > 0, rbuf[far, :].astype(F32), 0.0)
        dy = p_v[mine, :].astype(F32) + right + left
        x = st3[view, :].astype(F32)
        inv = lax.rsqrt(jnp.sum(x * x, axis=1, keepdims=True) / dim + NORM_EPS)
        xhat = x * inv
        gain = gains[0:1, :]
        part = dy * xhat
        dg_v[pl.ds(0, 8), :] += part[:8] + part[8:]
        inner = jnp.sum(part * gain, axis=1, keepdims=True) / dim
        st1[view, :] = (dres_v[view, :] + inv * (dy * gain) - xhat * (inv * inner)).astype(BF16)

    def h_cp(k, block):
        return net.copy(st1.at[pl.ds(0, sub), pl.ds(k * dt, dt)], dh_o.at[ds(block * sub, sub), :], h_id + k, h_id + k, tx=peer[k])

    def t_cp(k):
        return net.copy(dg_v.at[:, pl.ds(k * dt, dt)], dgr.at[k], t_id + k, t_id + k, tx=peer[k])

    def z_cp(i):
        return net.copy(dgr.at[0], dgz.at[i], z_id + i, z_id + i, ty=zs[i])

    for k in far_first:
        t_cp(k).start()
    for k in far_first:
        h_cp(k, tx).start()
    h_own = net.here(st1.at[pl.ds(0, sub), pl.ds(0, dt)], dh_o.at[ds(tx * sub, sub), :])
    up.sent()
    for c in stores.values():
        c.wait()
    up.step0(cross_g)
    for k in far_first:
        q_cp(k, peer[k]).wait_recv()
    q_own.wait()
    turned = wu_v.at[pl.ds(tokens, width), pl.ds(tokens, tokens)]
    net.here(qx, turned).wait()
    turn(turned, width, q_width, tokens, tab_v, swap_v, False)
    q_out = net.here(wu_v.at[pl.ds(tokens, q_width), pl.ds(tokens, tokens)], q_o)
    kv_out = net.here(wu_v.at[pl.ds(tokens + q_width, width - q_width), pl.ds(tokens, tokens)], kv_o)
    heads[0].step0(cross_g.at[pl.ds(0, q_width), pl.ds(0, dt)])
    heads[1].step0(cross_g.at[pl.ds(0, width - q_width), pl.ds(dt, dt)])
    for k in far_first:
        t_cp(k).wait_recv()
    dgr[0] = dg_v[:, pl.ds(0, dt)] + dgr[1] + dgr[2] + dgr[3]
    for i in (1, 2, 3):
        z_cp(i).start()
    for i in (1, 2, 3):
        z_cp(i).wait_recv()
    dgz[0] = dgr[0] + dgz[1] + dgz[2] + dgz[3]
    dg_out = net.here(dgz.at[0], dg_o)
    for k in far_first:
        h_cp(k, peer[k]).wait_recv()
    for c in (q_out, kv_out, dg_out, h_own):
        c.wait()
    dy_cp().wait_send()
    for part in heads:
        part.sent_locally()
        part.sent()
    for k in far_first:
        q_cp(k, tx).wait_send()
        h_cp(k, tx).wait_send()
        t_cp(k).wait_send()
        z_cp(k).wait_send()
    ag.drain()
    rsc.drain()


def call_c(q_width, *args):
    tokens, ff = args[0].shape
    sub, dim = args[9].shape
    dt, width = dim // 4, args[10].shape[0]
    rest = width - q_width
    tile = ff // 4
    s = jax.ShapeDtypeStruct
    wf, wb = s((dt, ff), F32), s((dt, ff), BF16)
    qf, qb, vf, vb = s((q_width, dt), F32), s((q_width, dt), BF16), s((rest, dt), F32), s((rest, dt), BF16)
    shapes = (wf, wb, wf, wb, s((ff, dt), F32), qf, qb, vf, vb, s((q_width, tokens), BF16), s((rest, tokens), BF16), s((tokens, dt), BF16), s((16, dt), F32),
              wb, wb, wb, wb, qb, qb, vb, vb, s((width, tokens), BF16), s((ff - down_split(ff), dt), BF16))
    return pl.pallas_call(
        functools.partial(kernel_c, q_width), out_shape=shapes, in_specs=[ANY] * len(args), out_specs=[ANY] * len(shapes),
        scratch_shapes=[
            VMEM((dim, ff), BF16), VMEM((dim, ff), BF16), VMEM((tokens, ff), BF16), VMEM((tokens, ff), BF16), VMEM((tokens, dim), BF16),
            VMEM((tokens, dim), BF16), VMEM((5 * sub, dim), BF16), VMEM((tokens, dim), BF16),
            VMEM((dt, ff), BF16), VMEM((dt, ff), BF16), VMEM((dt, ff), BF16), VMEM((dt, ff), BF16), VMEM((dt, ff), BF16),
            VMEM((2, max(dt, tile), max(dt, tile)), F32), VMEM((sub, dim), F32), VMEM((width, dim), BF16), VMEM((width, tokens), BF16),
            VMEM((8, dim), F32), VMEM((16, dim), F32), VMEM((4, 16, dt), F32), VMEM((4, 16, dt), F32), VMEM((256, 2 * tokens), F32), VMEM((128, 128), BF16),
            pltpu.SemaphoreType.DMA((48,)), pltpu.SemaphoreType.DMA((48,)), pltpu.SemaphoreType.DMA((96,))],
        compiler_params=pltpu.CompilerParams(collective_id=2, has_side_effects=True, vmem_limit_bytes=VMEM_LIMIT),
        cost_estimate=pl.CostEstimate(flops=20 * tokens * dim * ff, bytes_accessed=100000000, transcendentals=0), name="phase_c",
    )(*args)


def kernel_out(pieces, n, *refs):
    ins, outs, bufs = refs[:n], refs[n + 1:2 * n + 1], refs[2 * n + 3:3 * n + 3]
    gains, gain_a, gain_b = refs[n], refs[2 * n + 1], refs[2 * n + 2]
    read, write = refs[3 * n + 3:]

    def part(ref, i, c):
        rows = ref.shape[0] // pieces[i]
        return ref.at[pl.ds(c * rows, rows), :]

    jobs = [(i, c) for i in range(n) for c in range(pieces[i])]
    get = [pltpu.make_async_copy(part(ins[i], i, c), part(bufs[i], i, c), read.at[m]) for m, (i, c) in enumerate(jobs)]
    put = [pltpu.make_async_copy(part(bufs[i], i, c), part(outs[i], i, c), write.at[m]) for m, (i, c) in enumerate(jobs)]
    ahead = min(8, len(get))
    for g in get[:ahead]:
        g.start()
    gain_a[...] = jnp.sum(gains[pl.ds(0, 8), :], axis=0, keepdims=True)
    gain_b[...] = jnp.sum(gains[pl.ds(8, 8), :], axis=0, keepdims=True)
    for m, (g, p) in enumerate(zip(get, put)):
        g.wait()
        p.start()
        if m + ahead < len(get):
            get[m + ahead].start()
    for p in put:
        p.wait()


def call_out(results, gains):
    n = len(results)
    pieces = tuple(max(1, x.size * x.dtype.itemsize // 2**20) for x in results)
    row = jax.ShapeDtypeStruct((1, gains.shape[1]), F32)
    whole = pl.BlockSpec(memory_space=pltpu.VMEM)
    return pl.pallas_call(
        functools.partial(kernel_out, pieces, n), out_shape=tuple(jax.ShapeDtypeStruct(x.shape, x.dtype) for x in results) + (row, row),
        in_specs=[ANY] * n + [whole], out_specs=[ANY] * n + [whole, whole],
        scratch_shapes=[VMEM(x.shape, x.dtype) for x in results] + [pltpu.SemaphoreType.DMA((sum(pieces),))] * 2,
        compiler_params=pltpu.CompilerParams(vmem_limit_bytes=VMEM_LIMIT),
        cost_estimate=pl.CostEstimate(flops=1000000, bytes_accessed=35000000, transcendentals=0), name="results",
    )(*results, gains)


def solution(mesh):
    def local_step(hidden, positions, g_ffn, w_gate, w_up, w_down, g_attn, w_q, w_kv, grad_h2, grad_q, grad_kv):
        tokens, dt = hidden.shape
        q_heads, head_dim = w_q.shape[1:]
        q_width = q_heads * head_dim

        lane = np.arange(128)
        inv_freq = ROPE_BASE ** (-(lane % head_dim // 2 * 2).astype(np.float32) / head_dim)
        inv_freq = jnp.asarray(np.tile(inv_freq.astype(np.float32)[:, None], (1, 128)))
        swap = np.zeros((128, 128), np.float32)
        swap[lane, lane ^ 1] = np.where(lane % 2 == 0, -1.0, 1.0)
        swap = jnp.asarray(swap, BF16)

        def heads_first(x):
            return x.transpose(1, 2, 0).reshape(-1, x.shape[0])

        def heads_last(x):
            return x.reshape(-1, head_dim, x.shape[1]).transpose(2, 0, 1)

        (normed_all, grad_gate, grad_up, u_all, gate_w, up_w, w_qkv, back_all, h_rows, gains, res_all, normed2, grad_res, resid_out, gattn8,
         u_other, e_other, table, _, wd_zero, wd_cross) = call_ab(
             hidden, heads_first(grad_q), heads_first(grad_kv), positions.reshape(1, tokens), inv_freq, swap, grad_h2,
             w_gate, w_up, w_down, heads_first(w_q), heads_first(w_kv), g_ffn, g_attn)
        (grad_wgate, _, grad_wup, _, grad_wdown, grad_wq, _, grad_wkv, _, q_out, kv_out, grad_hidden, gain_grads, *_) = call_c(
            q_width, grad_gate, grad_up, gate_w, up_w, normed_all, u_all, u_other, res_all, e_other, normed2, back_all, w_qkv,
            h_rows, grad_res, gains, gattn8, table, swap, wd_zero, wd_cross)
        (resid_out, grad_wgate, grad_wup, grad_wdown, grad_wq, grad_wkv, q_out, kv_out, grad_hidden, grad_gffn, grad_gattn) = call_out(
            (resid_out, grad_wgate, grad_wup, grad_wdown, grad_wq, grad_wkv, q_out, kv_out, grad_hidden), gain_grads)
        q_out, kv_out, grad_wq, grad_wkv = (heads_last(x) for x in (q_out, kv_out, grad_wq, grad_wkv))
        grad_gffn, grad_gattn = grad_gffn[0], grad_gattn[0]
        return (resid_out, q_out, kv_out, grad_hidden, grad_gffn, grad_gattn, grad_wgate, grad_wup, grad_wdown, grad_wq, grad_wkv)

    row_spec = P(("dp", "ty"), "tx")
    head_spec = P(("dp", "tx"), "ty", None)
    in_specs = (row_spec, P(("dp", "tx")), P("tx"), P("tx", "ty"), P("tx", "ty"), P("ty", "tx"), P("tx"), P("tx", "ty", None), P("tx", "ty", None), row_spec, head_spec, head_spec)
    out_specs = (row_spec, head_spec, head_spec, row_spec, P(("dp", "tx")), P(("dp", "tx")), P(("dp", "tx"), "ty"), P(("dp", "tx"), "ty"), P(("dp", "ty"), "tx"), head_spec, head_spec)
    return jax.shard_map(local_step, mesh=mesh, in_specs=in_specs, out_specs=out_specs, check_vma=False)
```

```python
import functools

import jax
import jax.numpy as jnp
import numpy as np
from jax import lax
from jax.experimental import pallas as pl
from jax.experimental.pallas import tpu as pltpu
from jax.sharding import PartitionSpec as P

NORM_EPS = 1e-5
ROPE_BASE = 10000.0
F32 = jnp.float32
BF16 = jnp.bfloat16


def dot(a, b, dims=(((1,), (0,)), ((), ()))):
    return lax.dot_general(a, b, dims, preferred_element_type=F32)


MESH = pl.DeviceIdType.MESH
ANY = pl.BlockSpec(memory_space=pl.ANY)
VMEM = pltpu.VMEM
NT_DIMS = (((1,), (1,)), ((), ()))
VMEM_LIMIT = 67000000


def ds(start, size, align=None):
    if isinstance(start, int):
        return pl.ds(start, size)
    return pl.ds(pl.multiple_of(start, align or size), size)


def mid(z):
    return jnp.logical_and(z > 0, z < 3)


def end(z):
    return jnp.logical_or(z == 0, z == 3)


def slots(z):
    return (z + 1 - 2 * (z % 2), 2 - z // 2, 3 - 3 * (z // 2))


def turn(x_ref, width, q_width, tokens, table_ref, swap_ref, back):
    step = min(256, tokens)

    @pl.loop(0, tokens // step)
    def _(r):
        cols = ds(r * step, step)
        for g in range(width // 128):
            rows = pl.ds(g * 128, 128)
            base = pl.ds(0 if g * 128 < q_width else 128, 128)
            x = x_ref[rows, cols]
            main = x.astype(F32) * table_ref[base, cols]
            side = dot(swap_ref[...], x) * table_ref[base, ds(tokens + r * step, step)]
            x_ref[rows, cols] = (main - side if back else main + side).astype(BF16)


def pick(i, z):
    s1, s2, s3 = slots(z)
    first, last = (3 - i) // 3, (i // 2) * (i % 2)
    return z * first + s1 * ((i % 2) * (1 - i // 2)) + s2 * ((i // 2) * (1 - i % 2)) + s3 * last


class Wires:
    def __init__(self, send, recv, local):
        self.send, self.recv, self.local = send, recv, local
        self.n_remote = 0
        self.n_local = 0

    def take(self, n=1):
        base = self.n_remote
        self.n_remote += n
        assert self.n_remote <= self.send.shape[0]
        return base

    def copy(self, src, dst, si, ri, **dev):
        return pltpu.make_async_remote_copy(
            src_ref=src, dst_ref=dst, send_sem=self.send.at[si], recv_sem=self.recv.at[ri],
            device_id=dev, device_id_type=MESH)

    def here(self, src, dst):
        i = self.n_local
        self.n_local += 1
        assert i < self.local.shape[0]
        c = pltpu.make_async_copy(src, dst, self.local.at[i])
        c.start()
        return c


def entry_barrier(axes, z):
    sem = pltpu.get_barrier_semaphore()
    for dev in axes:
        pl.semaphore_signal(sem, inc=1, device_id=dev, device_id_type=MESH)

    @pl.when(z > 0)
    def _():
        pl.semaphore_signal(sem, inc=1, device_id={"ty": z - 1}, device_id_type=MESH)

    @pl.when(z < 3)
    def _():
        pl.semaphore_signal(sem, inc=1, device_id={"ty": z + 1}, device_id_type=MESH)

    @pl.when(mid(z))
    def _():
        pl.semaphore_wait(sem, len(axes) + 2)

    @pl.when(end(z))
    def _():
        pl.semaphore_wait(sem, len(axes) + 1)


class LineGather:
    def __init__(self, net, buf, rows, z, off=0, part=None):
        self.net, self.buf, self.rows, self.z, self.off, self.part = net, buf, rows, z, off, part or rows
        self.base = net.take(8)
        self.slots = slots(z)

    def blk(self, b):
        return self.buf.at[ds(b * self.rows + self.off, self.part), :]

    def cp(self, b, side, target):
        return self.net.copy(self.blk(b), self.blk(b), self.base + side * 4 + b, self.base + b, ty=target)

    def start(self):
        z = self.z

        @pl.when(z < 3)
        def _():
            self.cp(z, 0, z + 1).start()

        @pl.when(z > 0)
        def _():
            self.cp(z, 1, z - 1).start()

    def take(self, i):
        b = self.slots[i]
        self.cp(b, 0, self.z).wait_recv()

    def forward(self, i):
        z, b = self.z, self.slots[i]
        target = 3 - z if i == 0 else 3 * (z - 1)
        self.cp(b, 0, target).start()

    def step1(self):
        self.take(0)

        @pl.when(mid(self.z))
        def _():
            self.forward(0)
            self.take(1)
            self.forward(1)

    def near_end(self):
        @pl.when(end(self.z))
        def _():
            self.take(0)

    def near_mid(self):
        @pl.when(mid(self.z))
        def _():
            self.take(1)
            self.forward(1)

    def far_mid(self):
        @pl.when(mid(self.z))
        def _():
            self.take(0)
            self.forward(0)

    def step2(self):
        @pl.when(end(self.z))
        def _():
            self.take(1)

    def step3_mid(self):
        @pl.when(mid(self.z))
        def _():
            self.take(2)
            self.forward(2)

    def step3_end(self):
        @pl.when(end(self.z))
        def _():
            self.take(2)

    def drain(self):
        z = self.z

        @pl.when(z < 3)
        def _():
            self.cp(z, 0, z + 1).wait_send()

        @pl.when(z > 0)
        def _():
            self.cp(z, 1, z - 1).wait_send()

        @pl.when(mid(z))
        def _():
            for i in range(3):
                self.cp(self.slots[i], 0, 3 - z if i == 0 else 3 * (z - 1)).wait_send()


class LineScatter:
    def __init__(self, net, part, rbuf, rows, z, off=0, size=None):
        self.net, self.part, self.rbuf, self.rows, self.z, self.off, self.size = net, part, rbuf, rows, z, off, size or rows
        self.base = net.take(5)
        self.slots = slots(z)
        one = (z % 2) * (1 - z // 2)
        self.dst = (self.slots[0] + (1 - z % 2) * (3 - z), self.slots[1] + 2 * one, self.slots[2])
        self.target = (z + 1 - 2 * (z % 2), 1 + z % 2, 1 + z % 2)

    def cp(self, i):
        return self.net.copy(
            self.part.at[self.view(self.slots[i]), :], self.rbuf.at[self.view(self.dst[i]), :],
            self.base + i, self.base + self.dst[i], ty=self.target[i])

    def view(self, b):
        return ds(b * self.rows + self.off, self.size)

    def wait_slot(self, s):
        view = self.rbuf.at[self.view(s), :]
        self.net.copy(view, view, self.base, self.base + s, ty=self.z).wait_recv()

    def send_end(self, i):
        @pl.when(end(self.z))
        def _():
            self.cp(i).start()

    def send_mid(self, i):
        @pl.when(mid(self.z))
        def _():
            b = self.slots[i]
            self.wait_slot(b)
            step = 16

            @pl.loop(0, self.size // step)
            def _(r):
                view = ds(b * self.rows + self.off + r * step, step)
                self.part[view, :] = (self.part[view, :].astype(F32) + self.rbuf[view, :].astype(F32)).astype(BF16)

            self.cp(i).start()

    def finish(self):
        z = self.z

        @pl.when(z < 3)
        def _():
            self.wait_slot(z)

        @pl.when(z > 0)
        def _():
            self.wait_slot(4)

    def drain(self):
        for i in range(3):
            self.cp(i).wait_send()


class WeightGather:
    def __init__(self, net, w, full, pos, by_rows, chunks, direct=0):
        self.net, self.w, self.full, self.by_rows = net, w, full, by_rows
        self.dp, self.t1, self.t2 = pos
        self.half = w.shape[0] // 2
        self.width = w.shape[0] if by_rows else w.shape[1]
        self.chunks, self.direct = chunks, direct
        self.base = net.take(1 + 4 * chunks + direct)

    def area(self, half, ch):
        if self.by_rows:
            n = self.w.shape[1] // self.chunks
            return ds(half * self.half, self.half, 16), self.half, pl.ds(ch * n, n)
        n = self.half // self.chunks
        return ds(half * self.half + ch * n, n, 16), n, pl.ds(0, self.width)

    def src(self, half, ch):
        rows, _, cols = self.area(half, ch)
        return self.w.at[rows, cols]

    def dst(self, k, half, ch):
        if self.by_rows:
            _, _, cols = self.area(half, ch)
            return self.full.at[ds(k * self.width + half * self.half, self.half, 16), cols]
        rows, _, _ = self.area(half, ch)
        return self.full.at[rows, pl.ds(k * self.width, self.width)]

    def whole(self, k):
        if self.by_rows:
            return self.full.at[pl.ds(k * self.width, self.width), :]
        return self.full.at[:, pl.ds(k * self.width, self.width)]

    def near(self, ch):
        i = self.base + 1 + ch
        return self.net.copy(self.src(self.dp, ch), self.dst(2, self.dp, ch), i, i, tx=self.t2)

    def cross(self, ch, half):
        i = self.base + 1 + self.chunks + ch
        return self.net.copy(self.dst(2, half, ch), self.dst(2, half, ch), i, i, dp=1 - self.dp)

    def diag(self, ch, which, half):
        i = self.base + 1 + (2 + which) * self.chunks + ch
        return self.net.copy(self.dst(2, half, ch), self.dst(3, half, ch), i, i, tx=self.t1)

    def mate(self):
        return self.net.copy(self.w, self.whole(1), self.base, self.base, tx=self.t1)

    def straight(self, n, half):
        ch = self.chunks - 1 - n
        i = self.base + 1 + 4 * self.chunks + n
        return self.net.copy(self.src(half, ch), self.dst(2, half, ch), i, i, tx=self.t2)

    def start_y(self):
        for ch in range(self.chunks):
            self.near(ch).start()
        for n in range(self.direct):
            self.straight(n, 1 - self.dp).start()

    def start_local(self):
        self.own = self.net.here(self.w, self.whole(0))
        self.mate().start()

    def y_event(self, ch):
        self.near(ch).wait_recv()
        if ch < self.chunks - self.direct:
            self.cross(ch, self.dp).start()
        self.diag(ch, 0, self.dp).start()

    def x_event(self, ch):
        if ch < self.chunks - self.direct:
            self.cross(ch, 1 - self.dp).wait_recv()
        else:
            self.straight(self.chunks - 1 - ch, 1 - self.dp).wait_recv()
        self.diag(ch, 1, 1 - self.dp).start()

    def finish_local(self):
        self.own.wait()
        self.mate().wait_recv()

    def finish(self, ch):
        self.diag(ch, 0, self.dp).wait_recv()
        self.diag(ch, 1, 1 - self.dp).wait_recv()

    def drain(self):
        self.mate().wait_send()
        for ch in range(self.chunks):
            self.near(ch).wait_send()
            if ch < self.chunks - self.direct:
                self.cross(ch, self.dp).wait_send()
            else:
                self.straight(self.chunks - 1 - ch, 1 - self.dp).wait_send()
            self.diag(ch, 0, self.dp).wait_send()
            self.diag(ch, 1, 1 - self.dp).wait_send()


def down_split(ff):
    return ff * 5 // 8


def places():
    dp, z, tx = lax.axis_index("dp"), lax.axis_index("ty"), lax.axis_index("tx")
    return dp, z, tx, (tx, tx + 1 - 2 * (tx % 2), (tx + 2) % 4, 3 - tx)


ROWS_ROWS = (((0,), (0,)), ((), ()))


class GradReduce:
    def __init__(self, net, peer, tile, tiles, st3, st1, cross, stage, got2, got0, got_y, out, out_tiles):
        self.net, self.peer, self.tile, self.tiles = net, peer, tile, tiles
        self.st3, self.st1, self.cross, self.stage = st3, st1, cross, stage
        self.got2, self.got0, self.got_y, self.out, self.out_tiles = got2, got0, got_y, out, out_tiles
        self.src = None
        self.base = net.take(3)
        self.rows, self.w = out.shape[0], out.shape[1] // tiles

    def cp(self, i):
        src, dst, to = ((self.st3, self.got2, 1), (self.st1, self.got0, 1), (self.src or self.cross, self.got_y, 2))[i]
        return self.net.copy(src, dst, self.base + i, self.base + i, tx=self.peer[to])

    def fill(self, k, ref):
        @pl.loop(0, self.tiles)
        def _(j):
            ref[:, ds(j * self.w, self.w)] = self.tile(k, j).astype(BF16)

    def step3(self):
        self.fill(3, self.st3)
        self.cp(0).start()

    def step1(self):
        self.fill(1, self.st1)
        self.cp(1).start()

    def step2(self, received=False):
        if not received:
            self.cp(0).wait_recv()
        self.net.here(self.got2, self.stage).wait()

        @pl.loop(0, self.tiles)
        def _(j):
            cols = ds(j * self.w, self.w)
            self.cross[:, cols] = (self.tile(2, j) + self.stage[:, cols].astype(F32)).astype(BF16)

    def send(self, src=None):
        self.src = src
        self.cp(2).start()

    def step0(self, far):
        self.cp(1).wait_recv()
        self.cp(2).wait_recv()
        loads = [self.net.here(self.got0, self.stage), self.net.here(self.got_y, far)]
        for c in loads:
            c.wait()
        base = self.net.n_local
        self.net.n_local += 2

        def put(j, slot):
            src = self.out_tiles.at[slot, pl.ds(0, self.rows), pl.ds(0, self.w)]
            return pltpu.make_async_copy(src, self.out.at[:, ds(j * self.w, self.w)], self.net.local.at[base + slot])

        @pl.loop(0, self.tiles)
        def _(j):
            cols = ds(j * self.w, self.w)
            slot = j % 2

            @pl.when(j >= 2)
            def _():
                put(j, slot).wait()

            self.out_tiles[slot, pl.ds(0, self.rows), pl.ds(0, self.w)] = self.tile(0, j) + (self.stage[:, cols].astype(F32) + far[:, cols].astype(F32))
            put(j, slot).start()

        for slot in range(min(2, self.tiles)):
            put(slot, slot).wait()

    def sent_locally(self):
        self.cp(0).wait_send()
        self.cp(1).wait_send()

    def sent(self):
        self.cp(2).wait_send()


def kernel_ab(q_width, hid, eqh, ekvh, posh, invh, swaph, dh2h, wg, wu, wd, wq, wkv, gfh, gah,
              n_o, da_o, db_o, u_o, wg_o, wu_o, wq_o, eq_o, h_o, g_o, e_o, n2_o, dres_o, home_o, dg_o, ux_o, ex_o, tab_o, d2_o, d0_o, dc_o,
              rows, dh2_v, n2_v, res_v, dres_v, n_v, a_v, b_v, wg_v, wu_v, wd_v, wq_v, eq_v, p_v, rbuf, rbuf2, gains, dg_v, swap_v, pos_v, inv_v, gf_v, ga_v, gin, send, recv, local):
    dp, z, tx, peer = places()
    sub, dim = rows.shape
    tokens = 4 * sub
    width = eq_v.shape[0]
    dt = dim // 4
    ff = wg.shape[1]
    wide = min(1024, ff)
    tile = min(512, ff)
    dwide = min(1024, dim)
    dtile = min(512, dim)
    hs, cs = sub // 2, sub // 8
    split = down_split(ff)
    net = Wires(send, recv, local)
    gain_in = [net.here(gfh, gf_v), net.here(gah, ga_v)]
    turn_in = [net.here(eqh, p_v.at[pl.ds(0, q_width), pl.ds(0, tokens)]), net.here(ekvh, p_v.at[pl.ds(q_width, width - q_width), pl.ds(0, tokens)]),
               net.here(swaph, swap_v), net.here(posh, pos_v), net.here(invh, inv_v)]
    entry_barrier([{"tx": peer[1]}, {"tx": peer[2]}, {"tx": peer[3]}, {"dp": 1 - dp}], z)

    pos = (dp, peer[1], peer[2])
    far_first = (2, 3, 1)
    g_id, h_id, e_id, d_id, o_id, u_id, x_id = (net.take(4), net.take(4), net.take(4), net.take(4), net.take(8), net.take(12), net.take(24))
    u_v = wg_v.at[pl.ds(0, tokens), :]
    e_v = wg_v.at[pl.ds(tokens, tokens), :]

    def g_cp(k):
        return net.copy(gin, gains.at[:, pl.ds(k * dt, dt)], g_id + k, g_id + k, tx=peer[k])

    def h_cp(k):
        return net.copy(hid.at[ds(peer[k] * sub, sub), :], rows.at[:, pl.ds(k * dt, dt)], h_id + k, h_id + k, tx=peer[k])

    def e_cp(k, block):
        return net.copy(p_v.at[pl.ds(0, width), ds(peer[k] * sub, sub)], eq_v.at[:, ds(block * sub, sub)], e_id + k, e_id + k, tx=peer[k])

    def d_cp(k):
        return net.copy(dh2h.at[ds(peer[k] * sub, sub), :], dh2_v.at[:, pl.ds(k * dt, dt)], d_id + k, d_id + k, tx=peer[k])

    def o_cp(k, block, half):
        i = o_id + half * 4 + k
        return net.copy(res_v.at[pl.ds(half * hs, hs), pl.ds(k * dt, dt)], home_o.at[ds(block * sub + half * hs, hs), :], i, i, tx=peer[k])

    def ux_cp(k, b):
        view = ds(b * sub, sub)
        cols = pl.ds(0, split)
        src = ux_o.at[1, view, :] if k == 3 else wg_v.at[view, cols]
        i = u_id + (k - 1) * 4 + b
        return net.copy(src, ux_o.at[k - 1, view, :], i, i, tx=peer[1] if k == 3 else peer[k])

    def ex_cp(k, b, half):
        i = x_id + half * 12 + (k - 1) * 4 + b
        view = ds(b * sub + half * hs, hs)
        return net.copy(wg_v.at[ds(tokens + b * sub + half * hs, hs), pl.ds(k * dt, dt)], ex_o.at[k - 1, view, :], i, i, tx=peer[k])

    gate = WeightGather(net, wg, wg_v, pos, True, 2)
    up = WeightGather(net, wu, wu_v, pos, True, 2)
    down = WeightGather(net, wd, wd_v, pos, False, 8, 1)
    q_w = WeightGather(net, wq, wq_v.at[pl.ds(0, q_width), :], pos, False, 1)
    kv_w = WeightGather(net, wkv, wq_v.at[pl.ds(q_width, width - q_width), :], pos, False, 1)
    ag = LineGather(net, n_v, sub, z)
    rsc = LineScatter(net, p_v, rbuf, sub, z)
    rs2 = [LineScatter(net, n_v, rbuf2, sub, z, c * cs, cs) for c in range(8)]
    ag2 = [LineGather(net, e_v, sub, z, c * cs, cs) for c in range(8)]

    for k in far_first:
        h_cp(k).start()
    for c in gain_in:
        c.wait()
    gin[...] = jnp.broadcast_to(gf_v[...].astype(F32)[None, :], gin.shape)
    gin[1:2, :] = ga_v[...].astype(F32)[None, :]
    g_own = net.here(gin, gains.at[:, pl.ds(0, dt)])
    h_own = net.here(hid.at[ds(tx * sub, sub), :], rows.at[:, pl.ds(0, dt)])
    for w in (q_w, kv_w, gate, up, down):
        w.start_local()
    for k in far_first:
        g_cp(k).start()
    for c in turn_in:
        c.wait()

    @pl.loop(0, tokens // 128)
    def _(i):
        part = 128
        cos_c, sin_c = ds(i * part, part), ds(tokens + i * part, part)
        q_r, kv_r = pl.ds(0, 128), pl.ds(128, 128)
        angles = inv_v[...] * pos_v[:, cos_c].astype(F32)
        dres_v[q_r, sin_c] = jnp.sin(angles)
        dres_v[q_r, cos_c] = jnp.cos(angles)

        @pl.when(z < 2)
        def _():
            dres_v[kv_r, cos_c] = dres_v[q_r, cos_c]
            dres_v[kv_r, sin_c] = dres_v[q_r, sin_c]

        @pl.when(z >= 2)
        def _():
            dres_v[kv_r, cos_c] = jnp.ones((128, part), F32)
            dres_v[kv_r, sin_c] = jnp.zeros((128, part), F32)

    tab_out = net.here(dres_v.at[pl.ds(0, 256), pl.ds(0, 2 * tokens)], tab_o)
    turn(p_v, width, q_width, tokens, dres_v, swap_v, True)
    for k in far_first:
        e_cp(k, tx).start()
    e_own = net.here(p_v.at[pl.ds(0, width), ds(tx * sub, sub)], eq_v.at[:, ds(tx * sub, sub)])
    for w in (q_w, kv_w, gate, up, down):
        w.start_y()
    for k in far_first:
        d_cp(k).start()
    d_own = net.here(dh2h.at[ds(tx * sub, sub), :], dh2_v.at[:, pl.ds(0, dt)])

    for k in far_first:
        g_cp(k).wait_recv()
        h_cp(k).wait_recv()
    g_own.wait()
    h_own.wait()

    @pl.loop(0, sub // 16)
    def _(r):
        x = rows[ds(r * 16, 16), :].astype(F32)
        inv = lax.rsqrt(jnp.sum(x * x, axis=1, keepdims=True) / dim + NORM_EPS)
        n_v[ds(z * sub + r * 16, 16), :] = (x * inv * gains[0:1, :]).astype(BF16)

    ag.start()
    outs = [net.here(rows, h_o), net.here(gains, g_o)]
    for k in far_first:
        e_cp(k, peer[k]).wait_recv()
    e_own.wait()
    ag.step1()
    for w in (q_w, kv_w):
        w.y_event(0)
    for w in (q_w, kv_w):
        w.x_event(0)
    for w in (q_w, kv_w):
        w.finish_local()
        w.finish(0)
    for k in far_first:
        e_cp(k, tx).wait_send()

    def n2_block(b):
        @pl.loop(0, dim // dtile)
        def _(j):
            cols = ds(j * dtile, dtile)
            p_v[ds(b * sub, sub), cols] = dot(eq_v[:, ds(b * sub, sub)], wq_v[:, cols], ROWS_ROWS).astype(BF16)

    @pl.loop(0, 4)
    def _(i):
        n2_block(pick(3 - i, z))
        for step in range(3):
            pl.when(i == step)(lambda step=step: rsc.send_end(2 - step))
        pl.when(i == 0)(lambda: gate.y_event(0))

    wide = ff // 2

    def gate_part(b, c):
        cols = pl.ds(c * wide, wide)
        a_v[ds(b * sub, sub), cols] = dot(n_v[ds(b * sub, sub), :], wg_v[:, cols]).astype(BF16)

    def up_part(b, c):
        cols = pl.ds(c * wide, wide)
        bb = dot(n_v[ds(b * sub, sub), :], wu_v[:, cols]).astype(BF16)
        b_v[ds(b * sub, sub), cols] = bb
        aa = a_v[ds(b * sub, sub), cols].astype(F32)
        wg_v[ds(b * sub, sub), cols] = (aa * jax.nn.sigmoid(aa) * bb.astype(F32)).astype(BF16)

    def down_part(b, j):
        cols = pl.ds(j * (dim // 2), dim // 2)
        n_v[ds(b * sub, sub), cols] = dot(wg_v[ds(b * sub, sub), :], wd_v[:, cols]).astype(BF16)

    def both(event, ch):
        event(ch)
        event(ch + 1)

    outs += [net.here(wq_v, wq_o), net.here(eq_v, eq_o)]
    gate.finish_local()
    gate.y_event(1)
    ag.step2()
    ag.step3_mid()
    gate.x_event(0)
    gate.finish(0)

    @pl.loop(0, 3)
    def _(i):
        gate_part(pick(i, z), 0)

    up.y_event(0)
    gate.x_event(1)
    rsc.send_mid(2)
    gate.finish(1)
    wg_out = net.here(wg_v, wg_o)

    @pl.loop(0, 3)
    def _(i):
        gate_part(pick(i, z), 1)

    up.finish_local()
    up.y_event(1)
    up.x_event(0)
    up.finish(0)
    ag.step3_end()

    @pl.loop(0, 2)
    def _(c):
        cols = ds(c * wide, wide)
        b = pick(3, z)
        a_v[ds(b * sub, sub), cols] = dot(n_v[ds(b * sub, sub), :], wg_v[:, cols]).astype(BF16)

    wg_out.wait()
    n_out = net.here(n_v, n_o)

    @pl.loop(0, 4)
    def _(i):
        pl.when(i == 1)(lambda: both(down.y_event, 0))
        pl.when(i == 2)(lambda: both(down.y_event, 2))
        pl.when(i == 3)(lambda: up.x_event(1))
        up_part(pick(i, z), 0)

    def up_events_1():
        rsc.send_mid(1)
        rsc.send_mid(0)
        down.x_event(0)
        down.x_event(1)

    def up_events_2():
        down.y_event(4)
        down.y_event(5)

    def up_events_3():
        down.y_event(6)
        down.y_event(7)
        down.x_event(2)
        down.x_event(3)

    up.finish(1)
    outs.append(net.here(wu_v, wu_o))

    @pl.loop(0, 4)
    def _(i):
        pl.when(i == 1)(up_events_1)
        pl.when(i == 2)(up_events_2)
        pl.when(i == 3)(up_events_3)
        b = pick(i, z)
        up_part(b, 1)
        ux_cp(2, b).start()
        ux_cp(1, b).start()

    outs.append(net.here(u_v, u_o))
    ag.drain()
    gate.drain()
    n_out.wait()
    down.finish_local()

    @pl.loop(0, 4)
    def _(i):
        pl.when(i == 2)(lambda: both(down.x_event, 4))
        pl.when(i == 3)(lambda: both(down.x_event, 6))
        down_part(pick(3 - i, z), 0)

    for ch in range(8):
        down.finish(ch)

    @pl.loop(0, 4)
    def _(i):
        down_part(pick(3 - i, z), 1)
        for step in range(3):
            pl.when(i == step)(lambda step=step: rs2[0].send_end(2 - step))

    for c in range(1, 8):
        for i in (2, 1, 0):
            rs2[c].send_end(i)
    dg_v[...] = jnp.zeros_like(dg_v)
    step = 16

    def norm_chunk(c):
        @pl.loop(0, cs // step)
        def _(r):
            at = c * cs + r * step
            view, mine, far = ds(at, step), ds(z * sub + at, step), ds(4 * sub + at, step)

            def whole(part, got):
                right = jnp.where(z < 3, got[mine, :].astype(F32), 0.0)
                left = jnp.where(z > 0, got[far, :].astype(F32), 0.0)
                return part[mine, :].astype(F32) + right + left

            resid = (rows[view, :].astype(F32) + whole(n_v, rbuf2)).astype(BF16)
            dy = whole(p_v, rbuf)
            res_v[view, :] = resid
            x = resid.astype(F32)
            inv = lax.rsqrt(jnp.sum(x * x, axis=1, keepdims=True) / dim + NORM_EPS)
            xhat = x * inv
            gain = gains[1:2, :]
            n2_v[view, :] = (xhat * gain).astype(BF16)
            part = dy * xhat
            dg_v[...] += part[:8] + part[8:]
            inner = jnp.sum(part * gain, axis=1, keepdims=True) / dim
            dres = dh2_v[view, :].astype(F32) + inv * (dy * gain) - xhat * (inv * inner)
            dres_v[view, pl.ds(0, dim)] = dres
            wg_v[ds(tokens + z * sub + at, step), :] = dres.astype(BF16)

    def spread(b, half):
        for k in far_first:
            ex_cp(k, b, half).start()

    def back_tile(b, j):
        view, cols = ds(b * sub, sub), ds(j * (ff // 4), ff // 4)
        du = dot(wg_v[ds(tokens + b * sub, sub), :], wd_v[ds(j * (ff // 4), ff // 4), :], NT_DIMS)
        aa = a_v[view, cols].astype(F32)
        bb = b_v[view, cols].astype(F32)
        sig = jax.nn.sigmoid(aa)
        a_v[view, cols] = (du * bb * sig * (1.0 + aa * (1.0 - sig))).astype(BF16)
        b_v[view, cols] = (du * aa * sig).astype(BF16)

    def scatter(i, c):
        return lambda: rs2[c].send_mid(i)

    def gathered(i, c):
        def go():
            ag2[c].take(i)
            pl.when(mid(z))(lambda: ag2[c].forward(i))
            if c % 4 == 3:
                spread(ag.slots[i], c // 4)
        return go

    def run(ops):
        def go():
            for op in ops:
                op()
        return go

    before_mid = (
        (scatter(2, 0), scatter(1, 0), scatter(0, 0)),
        (scatter(2, 1), scatter(1, 1), gathered(1, 0), scatter(0, 1), scatter(2, 2)),
        (scatter(1, 2), scatter(0, 2), gathered(1, 1), scatter(2, 3)),
        (scatter(1, 3), scatter(0, 3), gathered(1, 2), scatter(2, 4)),
        (scatter(1, 4), scatter(0, 4), gathered(1, 3), scatter(2, 5)),
        (scatter(1, 5), scatter(0, 5), gathered(1, 4), scatter(2, 6)),
        (scatter(1, 6), scatter(0, 6), gathered(1, 5), scatter(2, 7)),
        (scatter(1, 7), scatter(0, 7), gathered(1, 6), gathered(0, 0)))
    before_end = (
        (),
        (gathered(0, 0), gathered(1, 0)),
        (gathered(0, 1),),
        (gathered(1, 1), gathered(0, 2)),
        (gathered(1, 2), gathered(0, 3)),
        (gathered(1, 3), gathered(0, 4)),
        (gathered(1, 4), gathered(0, 5)),
        (gathered(1, 5), gathered(0, 6)))
    after_mid = {1: (gathered(0, 1),),
                 2: (gathered(2, 0),),
                 3: (gathered(0, 2),),
                 4: (gathered(1, 7),),
                 5: (gathered(0, 3),),
                 6: (gathered(2, 1),),
                 7: (gathered(0, 4),),
                 8: (gathered(2, 2), gathered(0, 5), gathered(2, 3), gathered(0, 6), gathered(2, 4), gathered(0, 7)),
                 10: (gathered(2, 5),),
                 12: (gathered(2, 6), gathered(2, 7))}
    after_end = {2: (gathered(1, 6),),
                 4: (gathered(0, 7),),
                 7: (gathered(2, 0),),
                 8: (gathered(1, 7),),
                 11: (gathered(2, 1),),
                 12: (gathered(2, 2), gathered(2, 3), gathered(2, 4), gathered(2, 5), gathered(2, 6), gathered(2, 7))}

    for c in range(8):
        pl.when(mid(z))(run(before_mid[c]))
        pl.when(end(z))(run(before_end[c]))
        if c == 0:
            rsc.finish()
            for k in far_first:
                d_cp(k).wait_recv()
            d_own.wait()
            tab_out.wait()
        rs2[c].finish()
        norm_chunk(c)
        ag2[c].start()
        if c % 4 == 3:
            spread(z, c // 4)
            for k in far_first:
                o_cp(k, tx, c // 4).start()

    outs += [net.here(res_v.at[:, pl.ds(0, dt)], home_o.at[ds(tx * sub, sub), :]), net.here(n2_v, n2_o), net.here(dres_v.at[pl.ds(0, sub), pl.ds(0, dim)], dres_o), net.here(dg_v, dg_o)]
    rsc.drain()
    for c in range(8):
        rs2[c].drain()
    middle = (z + 1) // 2 % 2

    def u_forward():
        for b in range(4):
            ux_cp(2, b).wait_recv()
            ux_cp(3, b).start()

    @pl.loop(0, 16)
    def _(t):
        for at, ops in after_mid.items():
            pl.when(jnp.logical_and(t == at, mid(z)))(run(ops))
        for at, ops in after_end.items():
            pl.when(jnp.logical_and(t == at, end(z)))(run(ops))
        pl.when(t == 8)(u_forward)
        i = t // 4
        inner = (i + 1) // 2 % 2
        back_tile(pick(i + middle * inner * (3 - 2 * i), z), t % 4)

    outs.append(net.here(e_v, e_o))
    outs += [net.here(a_v, da_o), net.here(b_v, db_o)]

    def down_tile(k, j):
        return dot(wg_v[pl.ds(0, tokens), pl.ds(split, ff - split)], wg_v[pl.ds(tokens, tokens), ds(k * dt + j * (dt // 2), dt // 2)], ROWS_ROWS)

    quarter = [rbuf.at[pl.ds(0, ff - split), pl.ds(i * dt, dt)] for i in range(4)]
    part_d = GradReduce(net, peer, down_tile, 2, quarter[0], quarter[1], quarter[2], quarter[3], d2_o, d0_o, None, dc_o, None)
    part_d.step3()
    part_d.step1()
    part_d.step2()
    outs.append(net.here(quarter[2], dc_o))
    for k in far_first:
        o_cp(k, peer[k], 0).wait_recv()
        o_cp(k, peer[k], 1).wait_recv()
        for b in range(4):
            ex_cp(k, b, 0).wait_recv()
            ex_cp(k, b, 1).wait_recv()
    for b in range(4):
        ux_cp(1, b).wait_recv()
        ux_cp(3, b).wait_recv()
    for c in outs:
        c.wait()
    for k in far_first:
        g_cp(k).wait_send()
        h_cp(k).wait_send()
        d_cp(k).wait_send()
        o_cp(k, tx, 0).wait_send()
        o_cp(k, tx, 1).wait_send()
        for b in range(4):
            ux_cp(k, b).wait_send()
            ex_cp(k, b, 0).wait_send()
            ex_cp(k, b, 1).wait_send()
    for w in (q_w, kv_w, up, down):
        w.drain()
    for c in range(8):
        ag2[c].drain()
    part_d.cp(1).wait_recv()
    part_d.sent_locally()


def call_ab(hid, eqh, ekvh, pos, inv, swap, dh2h, wg, wu, wd, wq, wkv, gf, ga):
    tokens, dt = hid.shape
    sub, dim, ff, q_width = tokens // 4, dt * 4, wg.shape[1], wq.shape[0]
    width = q_width + wkv.shape[0]
    s = jax.ShapeDtypeStruct
    tok_ff, tok_d, row = s((tokens, ff), BF16), s((tokens, dim), BF16), s((sub, dim), BF16)
    shapes = (tok_d, tok_ff, tok_ff, tok_ff, s((dim, ff), BF16), s((dim, ff), BF16), s((width, dim), BF16), s((width, tokens), BF16),
              row, s((8, dim), F32), tok_d, row, s((sub, dim), F32), s((tokens, dt), BF16), s((8, dim), F32),
              s((3, tokens, down_split(ff)), BF16), s((3, tokens, dt), BF16), s((256, 2 * tokens), F32)) + (s((ff - down_split(ff), dt), BF16),) * 3
    vrow, vtok, vff = VMEM((sub, dim), BF16), VMEM((tokens, dim), BF16), VMEM((tokens, ff), BF16)
    return pl.pallas_call(
        functools.partial(kernel_ab, q_width), out_shape=shapes, in_specs=[ANY] * 14, out_specs=[ANY] * len(shapes),
        scratch_shapes=[
            vrow, vrow, vrow, vrow, VMEM((max(sub, 256), max(dim, 2 * tokens)), F32), vtok, vff, vff, VMEM((dim, ff), BF16), VMEM((dim, ff), BF16), VMEM((ff, dim), BF16),
            VMEM((width, dim), BF16), VMEM((width, tokens), BF16), vtok, VMEM((5 * sub, dim), BF16), VMEM((5 * sub, dim), BF16),
            VMEM((8, dim), F32), VMEM((8, dim), F32), VMEM((128, 128), BF16), VMEM((1, tokens), jnp.int32), VMEM((128, 128), F32),
            VMEM((dt,), BF16), VMEM((dt,), BF16), VMEM((8, dt), F32),
            pltpu.SemaphoreType.DMA((256,)), pltpu.SemaphoreType.DMA((256,)), pltpu.SemaphoreType.DMA((48,))],
        compiler_params=pltpu.CompilerParams(collective_id=0, has_side_effects=True, vmem_limit_bytes=VMEM_LIMIT),
        cost_estimate=pl.CostEstimate(flops=20 * tokens * dim * ff, bytes_accessed=100000000, transcendentals=0), name="phase_ab",
    )(hid, eqh, ekvh, pos, inv, swap, dh2h, wg, wu, wd, wq, wkv, gf, ga)


def kernel_c(q_width, da_h, db_h, wg_h, wu_h, n_h, u_h, ux_h, e_h, ex_h, n2_h, eq_h, wq_h, h_h, dres_h, g_h, dga_h, tabh, swaph, d0, dc,
             wgo, wgy, wuo, wuy, wdo, wqo, wqy, wvo, wvy, q_o, kv_o, dh_o, dg_o, g2, g0, u2, u0, q2, q0, v2, v0, qx, dy,
             wg_v, wu_v, da_v, db_v, n_v, p_v, rbuf, n2_v, st3, st1, cross_g, cross_u, stage, tiles_v, dres_v, wq_v, eq_v,
             gains, dg_v, dgr, dgz, tab_v, swap_v, send, recv, local):
    dp, z, tx, peer = places()
    tokens, ff = da_v.shape
    sub, dim = dres_v.shape
    dt = dim // 4
    width = eq_v.shape[0]
    tile = ff // 4
    dtile = min(512, dim)
    qt = min(256, tile)
    far_first = (2, 3, 1)
    net = Wires(send, recv, local)
    n2_in = net.here(n2_h, n2_v.at[ds(z * sub, sub), :])
    first = [net.here(n_h, n_v), net.here(da_h, da_v)]
    second = [net.here(db_h, db_v), net.here(wg_h, wg_v), net.here(wu_h, wu_v)]
    third = [net.here(wq_h, wq_v), net.here(eq_h, eq_v), net.here(dres_h, dres_v), net.here(g_h, gains),
             net.here(dga_h, dg_v.at[pl.ds(8, 8), :]), net.here(tabh, tab_v), net.here(swaph, swap_v)]
    sem = pltpu.get_barrier_semaphore()
    zs = tuple((z + i) % 4 for i in range(4))
    for i in (1, 2, 3):
        pl.semaphore_signal(sem, inc=1, device_id={"tx": peer[i]}, device_id_type=MESH)
        pl.semaphore_signal(sem, inc=1, device_id={"ty": zs[i]}, device_id_type=MESH)
    pl.semaphore_wait(sem, 6)
    rsc = LineScatter(net, p_v, rbuf, sub, z)
    ag = LineGather(net, n2_v, sub, z)
    q_id, h_id, t_id, z_id = net.take(4), net.take(4), net.take(4), net.take(4)

    def grad_tile(lhs, rhs, w):
        def go(k, j):
            cols = pl.ds(j * w, w) if isinstance(j, int) else ds(j * w, w)
            return dot(lhs[:, pl.ds(k * dt, dt)], rhs[:, cols], ROWS_ROWS)
        return go

    gate = GradReduce(net, peer, grad_tile(n_v, da_v, tile), ff // tile, st3, st1, cross_g, stage, g2, g0, wgy, wgo, tiles_v)
    up = GradReduce(net, peer, grad_tile(n_v, db_v, tile), ff // tile, st3, st1, cross_u, stage, u2, u0, wuy, wuo, tiles_v)
    d_id = net.take(1)

    def dy_cp():
        return net.copy(dc, dy, d_id, d_id, tx=peer[2])

    dy_cp().start()

    def head_grad(first, rows, got2, got0, got_y, out):
        corner = [da_v.at[pl.ds(first, rows), pl.ds(c * dt, dt)] for c in range(4)]

        def tile_of(k, j):
            return dot(eq_v[pl.ds(first, rows), :], n2_v[:, ds(k * dt + j * qt, qt)])

        return GradReduce(net, peer, tile_of, dt // qt, *corner, got2, got0, got_y, out, tiles_v)

    heads = (head_grad(0, q_width, q2, q0, wqy, wqo), head_grad(q_width, width - q_width, v2, v0, wvy, wvo))

    def dn_block(b):
        rows = ds(b * sub, sub)

        @pl.loop(0, dim // dtile)
        def _(j):
            wr = ds(j * dtile, dtile)
            p_v[rows, wr] = (dot(da_v[rows, :], wg_v[wr, :], NT_DIMS) + dot(db_v[rows, :], wu_v[wr, :], NT_DIMS)).astype(BF16)

    n2_in.wait()
    ag.start()
    for c in first:
        c.wait()
    gate.step3()
    gate.step1()
    gate.step2()
    gate.send()
    for c in second:
        c.wait()

    @pl.loop(0, 4)
    def _(i):
        @pl.when(i == 1)
        def _():
            gate.sent_locally()
            up.step3()
            up.step1()
            ag.step1()

        dn_block(pick(3 - i, z))
        for step in range(3):
            pl.when(i == step)(lambda step=step: rsc.send_end(2 - step))

    up.step2()
    up.send()
    rsc.send_mid(2)
    ag.step2()
    ag.step3_mid()
    up.sent_locally()
    h_in = net.here(h_h, st3.at[pl.ds(0, sub), :])
    gate.step0(st1)
    gate.sent()

    e_in = [net.here(e_h.at[:, pl.ds(0, dt)], wu_v.at[pl.ds(0, tokens), pl.ds(0, dt)])]
    for k in (1, 2, 3):
        e_in.append(net.here(ex_h.at[k - 1], wu_v.at[pl.ds(0, tokens), pl.ds(k * dt, dt)]))

    piece = ff // 8
    exchanged, n_pieces = down_split(ff) // piece, 8

    def u_place(j, k):
        return wg_v.at[pl.ds((j % 2) * tokens, tokens), pl.ds(k * piece, piece)]

    def sums(j, n):
        return stage.at[pl.ds((j % 2) * piece, piece), pl.ds(n * dt, dt)]

    def u_load(j):
        cols = pl.ds(j * piece, piece)
        if j < exchanged:
            return [net.here(u_h.at[:, cols] if k == 0 else ux_h.at[k - 1, :, cols], u_place(j, k)) for k in range(4)]
        rows = pl.ds((j - exchanged) * piece, piece)
        return [net.here(u_h.at[:, cols], u_place(j, 0)), net.here(d0.at[rows, :], sums(j, 0)), net.here(dy.at[rows, :], sums(j, 1))]

    loads, stores = {}, {}

    def down_run(js):
        for j in js:
            for c in loads.pop(j):
                c.wait()
            if j >= 2:
                stores.pop(j - 2).wait()
            acc = None if j < exchanged else sums(j, 0)[...].astype(F32) + sums(j, 1)[...].astype(F32)
            for k in range(4 if j < exchanged else 1):
                part = dot(u_place(j, k)[...], wu_v[pl.ds(0, tokens), pl.ds(k * dt, dt)], ROWS_ROWS)
                acc = part if acc is None else acc + part
            place = tiles_v.at[j % 2, pl.ds(0, piece), pl.ds(0, dt)]
            tiles_v[j % 2, pl.ds(0, piece), pl.ds(0, dt)] = acc
            stores[j] = net.here(place, wdo.at[pl.ds(j * piece, piece), :])
            if j + 2 < n_pieces:
                loads[j + 2] = u_load(j + 2)

    loads[0], loads[1] = u_load(0), u_load(1)
    rsc.send_mid(1)
    rsc.send_mid(0)
    for c in e_in:
        c.wait()
    down_run((0, 1))
    for c in third:
        c.wait()
    ag.step3_end()

    @pl.loop(0, width // qt)
    def _(j):
        wu_v[ds(tokens + j * qt, qt), pl.ds(0, tokens)] = dot(wq_v[ds(j * qt, qt), :], n2_v[...], NT_DIMS).astype(BF16)

    def q_cp(k, block):
        return net.copy(wu_v.at[pl.ds(tokens, width), ds(peer[k] * sub, sub)], qx.at[:, ds(block * sub, sub)], q_id + k, q_id + k, tx=peer[k])

    for k in far_first:
        q_cp(k, tx).start()
    q_own = net.here(wu_v.at[pl.ds(tokens, width), ds(tx * sub, sub)], qx.at[:, ds(tx * sub, sub)])
    for part in heads:
        part.step3()
        part.step1()
    dy_cp().wait_recv()
    for part in heads:
        part.step2()
        part.send()
    down_run(range(2, n_pieces))
    h_in.wait()
    rsc.finish()
    dg_v[pl.ds(0, 8), :] = jnp.zeros((8, dim), F32)
    step = 16

    @pl.loop(0, sub // step)
    def _(r):
        view, mine, far = ds(r * step, step), ds(z * sub + r * step, step), ds(4 * sub + r * step, step)
        right = jnp.where(z < 3, rbuf[mine, :].astype(F32), 0.0)
        left = jnp.where(z > 0, rbuf[far, :].astype(F32), 0.0)
        dy = p_v[mine, :].astype(F32) + right + left
        x = st3[view, :].astype(F32)
        inv = lax.rsqrt(jnp.sum(x * x, axis=1, keepdims=True) / dim + NORM_EPS)
        xhat = x * inv
        gain = gains[0:1, :]
        part = dy * xhat
        dg_v[pl.ds(0, 8), :] += part[:8] + part[8:]
        inner = jnp.sum(part * gain, axis=1, keepdims=True) / dim
        st1[view, :] = (dres_v[view, :] + inv * (dy * gain) - xhat * (inv * inner)).astype(BF16)

    def h_cp(k, block):
        return net.copy(st1.at[pl.ds(0, sub), pl.ds(k * dt, dt)], dh_o.at[ds(block * sub, sub), :], h_id + k, h_id + k, tx=peer[k])

    def t_cp(k):
        return net.copy(dg_v.at[:, pl.ds(k * dt, dt)], dgr.at[k], t_id + k, t_id + k, tx=peer[k])

    def z_cp(i):
        return net.copy(dgr.at[0], dgz.at[i], z_id + i, z_id + i, ty=zs[i])

    for k in far_first:
        t_cp(k).start()
    for k in far_first:
        h_cp(k, tx).start()
    h_own = net.here(st1.at[pl.ds(0, sub), pl.ds(0, dt)], dh_o.at[ds(tx * sub, sub), :])
    up.sent()
    for c in stores.values():
        c.wait()
    up.step0(cross_g)
    for k in far_first:
        q_cp(k, peer[k]).wait_recv()
    q_own.wait()
    turned = wu_v.at[pl.ds(tokens, width), pl.ds(tokens, tokens)]
    net.here(qx, turned).wait()
    turn(turned, width, q_width, tokens, tab_v, swap_v, False)
    q_out = net.here(wu_v.at[pl.ds(tokens, q_width), pl.ds(tokens, tokens)], q_o)
    kv_out = net.here(wu_v.at[pl.ds(tokens + q_width, width - q_width), pl.ds(tokens, tokens)], kv_o)
    heads[0].step0(cross_g.at[pl.ds(0, q_width), pl.ds(0, dt)])
    heads[1].step0(cross_g.at[pl.ds(0, width - q_width), pl.ds(dt, dt)])
    for k in far_first:
        t_cp(k).wait_recv()
    dgr[0] = dg_v[:, pl.ds(0, dt)] + dgr[1] + dgr[2] + dgr[3]
    for i in (1, 2, 3):
        z_cp(i).start()
    for i in (1, 2, 3):
        z_cp(i).wait_recv()
    dgz[0] = dgr[0] + dgz[1] + dgz[2] + dgz[3]
    dg_out = net.here(dgz.at[0], dg_o)
    for k in far_first:
        h_cp(k, peer[k]).wait_recv()
    for c in (q_out, kv_out, dg_out, h_own):
        c.wait()
    dy_cp().wait_send()
    for part in heads:
        part.sent_locally()
        part.sent()
    for k in far_first:
        q_cp(k, tx).wait_send()
        h_cp(k, tx).wait_send()
        t_cp(k).wait_send()
        z_cp(k).wait_send()
    ag.drain()
    rsc.drain()


def call_c(q_width, *args):
    tokens, ff = args[0].shape
    sub, dim = args[9].shape
    dt, width = dim // 4, args[10].shape[0]
    rest = width - q_width
    tile = ff // 4
    s = jax.ShapeDtypeStruct
    wf, wb = s((dt, ff), F32), s((dt, ff), BF16)
    qf, qb, vf, vb = s((q_width, dt), F32), s((q_width, dt), BF16), s((rest, dt), F32), s((rest, dt), BF16)
    shapes = (wf, wb, wf, wb, s((ff, dt), F32), qf, qb, vf, vb, s((q_width, tokens), BF16), s((rest, tokens), BF16), s((tokens, dt), BF16), s((16, dt), F32),
              wb, wb, wb, wb, qb, qb, vb, vb, s((width, tokens), BF16), s((ff - down_split(ff), dt), BF16))
    return pl.pallas_call(
        functools.partial(kernel_c, q_width), out_shape=shapes, in_specs=[ANY] * len(args), out_specs=[ANY] * len(shapes),
        scratch_shapes=[
            VMEM((dim, ff), BF16), VMEM((dim, ff), BF16), VMEM((tokens, ff), BF16), VMEM((tokens, ff), BF16), VMEM((tokens, dim), BF16),
            VMEM((tokens, dim), BF16), VMEM((5 * sub, dim), BF16), VMEM((tokens, dim), BF16),
            VMEM((dt, ff), BF16), VMEM((dt, ff), BF16), VMEM((dt, ff), BF16), VMEM((dt, ff), BF16), VMEM((dt, ff), BF16),
            VMEM((2, max(dt, tile), max(dt, tile)), F32), VMEM((sub, dim), F32), VMEM((width, dim), BF16), VMEM((width, tokens), BF16),
            VMEM((8, dim), F32), VMEM((16, dim), F32), VMEM((4, 16, dt), F32), VMEM((4, 16, dt), F32), VMEM((256, 2 * tokens), F32), VMEM((128, 128), BF16),
            pltpu.SemaphoreType.DMA((48,)), pltpu.SemaphoreType.DMA((48,)), pltpu.SemaphoreType.DMA((96,))],
        compiler_params=pltpu.CompilerParams(collective_id=2, has_side_effects=True, vmem_limit_bytes=VMEM_LIMIT),
        cost_estimate=pl.CostEstimate(flops=20 * tokens * dim * ff, bytes_accessed=100000000, transcendentals=0), name="phase_c",
    )(*args)


def kernel_out(pieces, n, *refs):
    ins, outs, bufs = refs[:n], refs[n + 1:2 * n + 1], refs[2 * n + 3:3 * n + 3]
    gains, gain_a, gain_b = refs[n], refs[2 * n + 1], refs[2 * n + 2]
    read, write = refs[3 * n + 3:]

    def part(ref, i, c):
        rows = ref.shape[0] // pieces[i]
        return ref.at[pl.ds(c * rows, rows), :]

    jobs = [(i, c) for i in range(n) for c in range(pieces[i])]
    get = [pltpu.make_async_copy(part(ins[i], i, c), part(bufs[i], i, c), read.at[m]) for m, (i, c) in enumerate(jobs)]
    put = [pltpu.make_async_copy(part(bufs[i], i, c), part(outs[i], i, c), write.at[m]) for m, (i, c) in enumerate(jobs)]
    ahead = min(8, len(get))
    for g in get[:ahead]:
        g.start()
    gain_a[...] = jnp.sum(gains[pl.ds(0, 8), :], axis=0, keepdims=True)
    gain_b[...] = jnp.sum(gains[pl.ds(8, 8), :], axis=0, keepdims=True)
    for m, (g, p) in enumerate(zip(get, put)):
        g.wait()
        p.start()
        if m + ahead < len(get):
            get[m + ahead].start()
    for p in put:
        p.wait()


def call_out(results, gains):
    n = len(results)
    pieces = tuple(max(1, x.size * x.dtype.itemsize // 2**20) for x in results)
    row = jax.ShapeDtypeStruct((1, gains.shape[1]), F32)
    whole = pl.BlockSpec(memory_space=pltpu.VMEM)
    return pl.pallas_call(
        functools.partial(kernel_out, pieces, n), out_shape=tuple(jax.ShapeDtypeStruct(x.shape, x.dtype) for x in results) + (row, row),
        in_specs=[ANY] * n + [whole], out_specs=[ANY] * n + [whole, whole],
        scratch_shapes=[VMEM(x.shape, x.dtype) for x in results] + [pltpu.SemaphoreType.DMA((sum(pieces),))] * 2,
        compiler_params=pltpu.CompilerParams(vmem_limit_bytes=VMEM_LIMIT),
        cost_estimate=pl.CostEstimate(flops=1000000, bytes_accessed=35000000, transcendentals=0), name="results",
    )(*results, gains)


def solution(mesh):
    def local_step(hidden, positions, g_ffn, w_gate, w_up, w_down, g_attn, w_q, w_kv, grad_h2, grad_q, grad_kv):
        tokens, dt = hidden.shape
        q_heads, head_dim = w_q.shape[1:]
        q_width = q_heads * head_dim

        lane = np.arange(128)
        inv_freq = ROPE_BASE ** (-(lane % head_dim // 2 * 2).astype(np.float32) / head_dim)
        inv_freq = jnp.asarray(np.tile(inv_freq.astype(np.float32)[:, None], (1, 128)))
        swap = np.zeros((128, 128), np.float32)
        swap[lane, lane ^ 1] = np.where(lane % 2 == 0, -1.0, 1.0)
        swap = jnp.asarray(swap, BF16)

        def heads_first(x):
            return x.transpose(1, 2, 0).reshape(-1, x.shape[0])

        def heads_last(x):
            return x.reshape(-1, head_dim, x.shape[1]).transpose(2, 0, 1)

        (normed_all, grad_gate, grad_up, u_all, gate_w, up_w, w_qkv, back_all, h_rows, gains, res_all, normed2, grad_res, resid_out, gattn8,
         u_other, e_other, table, _, wd_zero, wd_cross) = call_ab(
             hidden, heads_first(grad_q), heads_first(grad_kv), positions.reshape(1, tokens), inv_freq, swap, grad_h2,
             w_gate, w_up, w_down, heads_first(w_q), heads_first(w_kv), g_ffn, g_attn)
        (grad_wgate, _, grad_wup, _, grad_wdown, grad_wq, _, grad_wkv, _, q_out, kv_out, grad_hidden, gain_grads, *_) = call_c(
            q_width, grad_gate, grad_up, gate_w, up_w, normed_all, u_all, u_other, res_all, e_other, normed2, back_all, w_qkv,
            h_rows, grad_res, gains, gattn8, table, swap, wd_zero, wd_cross)
        (resid_out, grad_wgate, grad_wup, grad_wdown, grad_wq, grad_wkv, q_out, kv_out, grad_hidden, grad_gffn, grad_gattn) = call_out(
            (resid_out, grad_wgate, grad_wup, grad_wdown, grad_wq, grad_wkv, q_out, kv_out, grad_hidden), gain_grads)
        q_out, kv_out, grad_wq, grad_wkv = (heads_last(x) for x in (q_out, kv_out, grad_wq, grad_wkv))
        grad_gffn, grad_gattn = grad_gffn[0], grad_gattn[0]
        return (resid_out, q_out, kv_out, grad_hidden, grad_gffn, grad_gattn, grad_wgate, grad_wup, grad_wdown, grad_wq, grad_wkv)

    row_spec = P(("dp", "ty"), "tx")
    head_spec = P(("dp", "tx"), "ty", None)
    in_specs = (row_spec, P(("dp", "tx")), P("tx"), P("tx", "ty"), P("tx", "ty"), P("ty", "tx"), P("tx"), P("tx", "ty", None), P("tx", "ty", None), row_spec, head_spec, head_spec)
    out_specs = (row_spec, head_spec, head_spec, row_spec, P(("dp", "tx")), P(("dp", "tx")), P(("dp", "tx"), "ty"), P(("dp", "tx"), "ty"), P(("dp", "ty"), "tx"), head_spec, head_spec)
    return jax.shard_map(local_step, mesh=mesh, in_specs=in_specs, out_specs=out_specs, check_vma=False)
```

```python
import functools

import jax
import jax.numpy as jnp
import numpy as np
from jax import lax
from jax.experimental import pallas as pl
from jax.experimental.pallas import tpu as pltpu
from jax.sharding import PartitionSpec as P

NORM_EPS = 1e-5
ROPE_BASE = 10000.0
F32 = jnp.float32
BF16 = jnp.bfloat16


def dot(a, b, dims=(((1,), (0,)), ((), ()))):
    return lax.dot_general(a, b, dims, preferred_element_type=F32)


MESH = pl.DeviceIdType.MESH
ANY = pl.BlockSpec(memory_space=pl.ANY)
VMEM = pltpu.VMEM
NT_DIMS = (((1,), (1,)), ((), ()))
VMEM_LIMIT = 67000000


def ds(start, size, align=None):
    if isinstance(start, int):
        return pl.ds(start, size)
    return pl.ds(pl.multiple_of(start, align or size), size)


def mid(z):
    return jnp.logical_and(z > 0, z < 3)


def end(z):
    return jnp.logical_or(z == 0, z == 3)


def slots(z):
    return (z + 1 - 2 * (z % 2), 2 - z // 2, 3 - 3 * (z // 2))


def turn(x_ref, width, q_width, tokens, table_ref, swap_ref, back):
    step = min(256, tokens)

    @pl.loop(0, tokens // step)
    def _(r):
        cols = ds(r * step, step)
        for g in range(width // 128):
            rows = pl.ds(g * 128, 128)
            base = pl.ds(0 if g * 128 < q_width else 128, 128)
            x = x_ref[rows, cols]
            main = x.astype(F32) * table_ref[base, cols]
            side = dot(swap_ref[...], x) * table_ref[base, ds(tokens + r * step, step)]
            x_ref[rows, cols] = (main - side if back else main + side).astype(BF16)


def pick(i, z):
    s1, s2, s3 = slots(z)
    first, last = (3 - i) // 3, (i // 2) * (i % 2)
    return z * first + s1 * ((i % 2) * (1 - i // 2)) + s2 * ((i // 2) * (1 - i % 2)) + s3 * last


class Wires:
    def __init__(self, send, recv, local):
        self.send, self.recv, self.local = send, recv, local
        self.n_remote = 0
        self.n_local = 0

    def take(self, n=1):
        base = self.n_remote
        self.n_remote += n
        assert self.n_remote <= self.send.shape[0]
        return base

    def copy(self, src, dst, si, ri, **dev):
        return pltpu.make_async_remote_copy(
            src_ref=src, dst_ref=dst, send_sem=self.send.at[si], recv_sem=self.recv.at[ri],
            device_id=dev, device_id_type=MESH)

    def here(self, src, dst):
        i = self.n_local
        self.n_local += 1
        assert i < self.local.shape[0]
        c = pltpu.make_async_copy(src, dst, self.local.at[i])
        c.start()
        return c


def entry_barrier(axes, z):
    sem = pltpu.get_barrier_semaphore()
    for dev in axes:
        pl.semaphore_signal(sem, inc=1, device_id=dev, device_id_type=MESH)

    @pl.when(z > 0)
    def _():
        pl.semaphore_signal(sem, inc=1, device_id={"ty": z - 1}, device_id_type=MESH)

    @pl.when(z < 3)
    def _():
        pl.semaphore_signal(sem, inc=1, device_id={"ty": z + 1}, device_id_type=MESH)

    @pl.when(mid(z))
    def _():
        pl.semaphore_wait(sem, len(axes) + 2)

    @pl.when(end(z))
    def _():
        pl.semaphore_wait(sem, len(axes) + 1)


class LineGather:
    def __init__(self, net, buf, rows, z, off=0, part=None):
        self.net, self.buf, self.rows, self.z, self.off, self.part = net, buf, rows, z, off, part or rows
        self.base = net.take(8)
        self.slots = slots(z)

    def blk(self, b):
        return self.buf.at[ds(b * self.rows + self.off, self.part), :]

    def cp(self, b, side, target):
        return self.net.copy(self.blk(b), self.blk(b), self.base + side * 4 + b, self.base + b, ty=target)

    def start(self):
        z = self.z

        @pl.when(z < 3)
        def _():
            self.cp(z, 0, z + 1).start()

        @pl.when(z > 0)
        def _():
            self.cp(z, 1, z - 1).start()

    def take(self, i):
        b = self.slots[i]
        self.cp(b, 0, self.z).wait_recv()

    def forward(self, i):
        z, b = self.z, self.slots[i]
        target = 3 - z if i == 0 else 3 * (z - 1)
        self.cp(b, 0, target).start()

    def step1(self):
        self.take(0)

        @pl.when(mid(self.z))
        def _():
            self.forward(0)
            self.take(1)
            self.forward(1)

    def near_end(self):
        @pl.when(end(self.z))
        def _():
            self.take(0)

    def near_mid(self):
        @pl.when(mid(self.z))
        def _():
            self.take(1)
            self.forward(1)

    def far_mid(self):
        @pl.when(mid(self.z))
        def _():
            self.take(0)
            self.forward(0)

    def step2(self):
        @pl.when(end(self.z))
        def _():
            self.take(1)

    def step3_mid(self):
        @pl.when(mid(self.z))
        def _():
            self.take(2)
            self.forward(2)

    def step3_end(self):
        @pl.when(end(self.z))
        def _():
            self.take(2)

    def drain(self):
        z = self.z

        @pl.when(z < 3)
        def _():
            self.cp(z, 0, z + 1).wait_send()

        @pl.when(z > 0)
        def _():
            self.cp(z, 1, z - 1).wait_send()

        @pl.when(mid(z))
        def _():
            for i in range(3):
                self.cp(self.slots[i], 0, 3 - z if i == 0 else 3 * (z - 1)).wait_send()


class LineScatter:
    def __init__(self, net, part, rbuf, rows, z, off=0, size=None):
        self.net, self.part, self.rbuf, self.rows, self.z, self.off, self.size = net, part, rbuf, rows, z, off, size or rows
        self.base = net.take(5)
        self.slots = slots(z)
        one = (z % 2) * (1 - z // 2)
        self.dst = (self.slots[0] + (1 - z % 2) * (3 - z), self.slots[1] + 2 * one, self.slots[2])
        self.target = (z + 1 - 2 * (z % 2), 1 + z % 2, 1 + z % 2)

    def cp(self, i):
        return self.net.copy(
            self.part.at[self.view(self.slots[i]), :], self.rbuf.at[self.view(self.dst[i]), :],
            self.base + i, self.base + self.dst[i], ty=self.target[i])

    def view(self, b):
        return ds(b * self.rows + self.off, self.size)

    def wait_slot(self, s):
        view = self.rbuf.at[self.view(s), :]
        self.net.copy(view, view, self.base, self.base + s, ty=self.z).wait_recv()

    def send_end(self, i):
        @pl.when(end(self.z))
        def _():
            self.cp(i).start()

    def send_mid(self, i):
        @pl.when(mid(self.z))
        def _():
            b = self.slots[i]
            self.wait_slot(b)
            step = 16

            @pl.loop(0, self.size // step)
            def _(r):
                view = ds(b * self.rows + self.off + r * step, step)
                self.part[view, :] = (self.part[view, :].astype(F32) + self.rbuf[view, :].astype(F32)).astype(BF16)

            self.cp(i).start()

    def finish(self):
        z = self.z

        @pl.when(z < 3)
        def _():
            self.wait_slot(z)

        @pl.when(z > 0)
        def _():
            self.wait_slot(4)

    def drain(self):
        for i in range(3):
            self.cp(i).wait_send()


class WeightGather:
    def __init__(self, net, w, full, pos, by_rows, chunks, direct=0):
        self.net, self.w, self.full, self.by_rows = net, w, full, by_rows
        self.dp, self.t1, self.t2 = pos
        self.half = w.shape[0] // 2
        self.width = w.shape[0] if by_rows else w.shape[1]
        self.chunks, self.direct = chunks, direct
        self.base = net.take(1 + 4 * chunks + direct)

    def area(self, half, ch):
        if self.by_rows:
            n = self.w.shape[1] // self.chunks
            return ds(half * self.half, self.half, 16), self.half, pl.ds(ch * n, n)
        n = self.half // self.chunks
        return ds(half * self.half + ch * n, n, 16), n, pl.ds(0, self.width)

    def src(self, half, ch):
        rows, _, cols = self.area(half, ch)
        return self.w.at[rows, cols]

    def dst(self, k, half, ch):
        if self.by_rows:
            _, _, cols = self.area(half, ch)
            return self.full.at[ds(k * self.width + half * self.half, self.half, 16), cols]
        rows, _, _ = self.area(half, ch)
        return self.full.at[rows, pl.ds(k * self.width, self.width)]

    def whole(self, k):
        if self.by_rows:
            return self.full.at[pl.ds(k * self.width, self.width), :]
        return self.full.at[:, pl.ds(k * self.width, self.width)]

    def near(self, ch):
        i = self.base + 1 + ch
        return self.net.copy(self.src(self.dp, ch), self.dst(2, self.dp, ch), i, i, tx=self.t2)

    def cross(self, ch, half):
        i = self.base + 1 + self.chunks + ch
        return self.net.copy(self.dst(2, half, ch), self.dst(2, half, ch), i, i, dp=1 - self.dp)

    def diag(self, ch, which, half):
        i = self.base + 1 + (2 + which) * self.chunks + ch
        return self.net.copy(self.dst(2, half, ch), self.dst(3, half, ch), i, i, tx=self.t1)

    def mate(self):
        return self.net.copy(self.w, self.whole(1), self.base, self.base, tx=self.t1)

    def straight(self, n, half):
        ch = self.chunks - 1 - n
        i = self.base + 1 + 4 * self.chunks + n
        return self.net.copy(self.src(half, ch), self.dst(2, half, ch), i, i, tx=self.t2)

    def start_y(self):
        for ch in range(self.chunks):
            self.near(ch).start()
        for n in range(self.direct):
            self.straight(n, 1 - self.dp).start()

    def start_local(self):
        self.own = self.net.here(self.w, self.whole(0))
        self.mate().start()

    def y_event(self, ch):
        self.near(ch).wait_recv()
        if ch < self.chunks - self.direct:
            self.cross(ch, self.dp).start()
        self.diag(ch, 0, self.dp).start()

    def x_event(self, ch):
        if ch < self.chunks - self.direct:
            self.cross(ch, 1 - self.dp).wait_recv()
        else:
            self.straight(self.chunks - 1 - ch, 1 - self.dp).wait_recv()
        self.diag(ch, 1, 1 - self.dp).start()

    def finish_local(self):
        self.own.wait()
        self.mate().wait_recv()

    def finish(self, ch):
        self.diag(ch, 0, self.dp).wait_recv()
        self.diag(ch, 1, 1 - self.dp).wait_recv()

    def drain(self):
        self.mate().wait_send()
        for ch in range(self.chunks):
            self.near(ch).wait_send()
            if ch < self.chunks - self.direct:
                self.cross(ch, self.dp).wait_send()
            else:
                self.straight(self.chunks - 1 - ch, 1 - self.dp).wait_send()
            self.diag(ch, 0, self.dp).wait_send()
            self.diag(ch, 1, 1 - self.dp).wait_send()


def down_split(ff):
    return ff * 5 // 8


def places():
    dp, z, tx = lax.axis_index("dp"), lax.axis_index("ty"), lax.axis_index("tx")
    return dp, z, tx, (tx, tx + 1 - 2 * (tx % 2), (tx + 2) % 4, 3 - tx)


ROWS_ROWS = (((0,), (0,)), ((), ()))


class GradReduce:
    def __init__(self, net, peer, tile, tiles, st3, st1, cross, stage, got2, got0, got_y, out, out_tiles):
        self.net, self.peer, self.tile, self.tiles = net, peer, tile, tiles
        self.st3, self.st1, self.cross, self.stage = st3, st1, cross, stage
        self.got2, self.got0, self.got_y, self.out, self.out_tiles = got2, got0, got_y, out, out_tiles
        self.src = None
        self.base = net.take(3)
        self.rows, self.w = out.shape[0], out.shape[1] // tiles

    def cp(self, i):
        src, dst, to = ((self.st3, self.got2, 1), (self.st1, self.got0, 1), (self.src or self.cross, self.got_y, 2))[i]
        return self.net.copy(src, dst, self.base + i, self.base + i, tx=self.peer[to])

    def fill(self, k, ref):
        @pl.loop(0, self.tiles)
        def _(j):
            ref[:, ds(j * self.w, self.w)] = self.tile(k, j).astype(BF16)

    def step3(self):
        self.fill(3, self.st3)
        self.cp(0).start()

    def step1(self):
        self.fill(1, self.st1)
        self.cp(1).start()

    def step2(self, received=False):
        if not received:
            self.cp(0).wait_recv()
        self.net.here(self.got2, self.stage).wait()

        @pl.loop(0, self.tiles)
        def _(j):
            cols = ds(j * self.w, self.w)
            self.cross[:, cols] = (self.tile(2, j) + self.stage[:, cols].astype(F32)).astype(BF16)

    def send(self, src=None):
        self.src = src
        self.cp(2).start()

    def step0(self, far):
        self.cp(1).wait_recv()
        self.cp(2).wait_recv()
        loads = [self.net.here(self.got0, self.stage), self.net.here(self.got_y, far)]
        for c in loads:
            c.wait()
        base = self.net.n_local
        self.net.n_local += 2

        def put(j, slot):
            src = self.out_tiles.at[slot, pl.ds(0, self.rows), pl.ds(0, self.w)]
            return pltpu.make_async_copy(src, self.out.at[:, ds(j * self.w, self.w)], self.net.local.at[base + slot])

        @pl.loop(0, self.tiles)
        def _(j):
            cols = ds(j * self.w, self.w)
            slot = j % 2

            @pl.when(j >= 2)
            def _():
                put(j, slot).wait()

            self.out_tiles[slot, pl.ds(0, self.rows), pl.ds(0, self.w)] = self.tile(0, j) + (self.stage[:, cols].astype(F32) + far[:, cols].astype(F32))
            put(j, slot).start()

        for slot in range(min(2, self.tiles)):
            put(slot, slot).wait()

    def sent_locally(self):
        self.cp(0).wait_send()
        self.cp(1).wait_send()

    def sent(self):
        self.cp(2).wait_send()


def kernel_ab(q_width, hid, eqh, ekvh, posh, invh, swaph, dh2h, wg, wu, wd, wq, wkv, gfh, gah,
              n_o, da_o, db_o, u_o, wg_o, wu_o, wq_o, eq_o, h_o, g_o, e_o, n2_o, dres_o, home_o, dg_o, ux_o, ex_o, tab_o, d2_o, d0_o, dc_o,
              rows, dh2_v, n2_v, res_v, dres_v, n_v, a_v, b_v, wg_v, wu_v, wd_v, wq_v, eq_v, p_v, rbuf, rbuf2, gains, dg_v, swap_v, pos_v, inv_v, gf_v, ga_v, gin, send, recv, local):
    dp, z, tx, peer = places()
    sub, dim = rows.shape
    tokens = 4 * sub
    width = eq_v.shape[0]
    dt = dim // 4
    ff = wg.shape[1]
    wide = min(1024, ff)
    tile = min(512, ff)
    dwide = min(1024, dim)
    dtile = min(512, dim)
    hs, cs = sub // 2, sub // 8
    split = down_split(ff)
    net = Wires(send, recv, local)
    gain_in = [net.here(gfh, gf_v), net.here(gah, ga_v)]
    turn_in = [net.here(eqh, p_v.at[pl.ds(0, q_width), pl.ds(0, tokens)]), net.here(ekvh, p_v.at[pl.ds(q_width, width - q_width), pl.ds(0, tokens)]),
               net.here(swaph, swap_v), net.here(posh, pos_v), net.here(invh, inv_v)]
    entry_barrier([{"tx": peer[1]}, {"tx": peer[2]}, {"tx": peer[3]}, {"dp": 1 - dp}], z)

    pos = (dp, peer[1], peer[2])
    far_first = (2, 3, 1)
    g_id, h_id, e_id, d_id, o_id, u_id, x_id = (net.take(4), net.take(4), net.take(4), net.take(4), net.take(8), net.take(12), net.take(24))
    u_v = wg_v.at[pl.ds(0, tokens), :]
    e_v = wg_v.at[pl.ds(tokens, tokens), :]

    def g_cp(k):
        return net.copy(gin, gains.at[:, pl.ds(k * dt, dt)], g_id + k, g_id + k, tx=peer[k])

    def h_cp(k):
        return net.copy(hid.at[ds(peer[k] * sub, sub), :], rows.at[:, pl.ds(k * dt, dt)], h_id + k, h_id + k, tx=peer[k])

    def e_cp(k, block):
        return net.copy(p_v.at[pl.ds(0, width), ds(peer[k] * sub, sub)], eq_v.at[:, ds(block * sub, sub)], e_id + k, e_id + k, tx=peer[k])

    def d_cp(k):
        return net.copy(dh2h.at[ds(peer[k] * sub, sub), :], dh2_v.at[:, pl.ds(k * dt, dt)], d_id + k, d_id + k, tx=peer[k])

    def o_cp(k, block, half):
        i = o_id + half * 4 + k
        return net.copy(res_v.at[pl.ds(half * hs, hs), pl.ds(k * dt, dt)], home_o.at[ds(block * sub + half * hs, hs), :], i, i, tx=peer[k])

    def ux_cp(k, b):
        view = ds(b * sub, sub)
        cols = pl.ds(0, split)
        src = ux_o.at[1, view, :] if k == 3 else wg_v.at[view, cols]
        i = u_id + (k - 1) * 4 + b
        return net.copy(src, ux_o.at[k - 1, view, :], i, i, tx=peer[1] if k == 3 else peer[k])

    def ex_cp(k, b, half):
        i = x_id + half * 12 + (k - 1) * 4 + b
        view = ds(b * sub + half * hs, hs)
        return net.copy(wg_v.at[ds(tokens + b * sub + half * hs, hs), pl.ds(k * dt, dt)], ex_o.at[k - 1, view, :], i, i, tx=peer[k])

    gate = WeightGather(net, wg, wg_v, pos, True, 2)
    up = WeightGather(net, wu, wu_v, pos, True, 2)
    down = WeightGather(net, wd, wd_v, pos, False, 4, 1)
    q_w = WeightGather(net, wq, wq_v.at[pl.ds(0, q_width), :], pos, False, 1)
    kv_w = WeightGather(net, wkv, wq_v.at[pl.ds(q_width, width - q_width), :], pos, False, 1)
    ag = LineGather(net, n_v, sub, z)
    rsc = LineScatter(net, p_v, rbuf, sub, z)
    rs2 = [LineScatter(net, n_v, rbuf2, sub, z, c * cs, cs) for c in range(8)]
    ag2 = [LineGather(net, e_v, sub, z, c * cs, cs) for c in range(8)]

    for k in far_first:
        h_cp(k).start()
    for c in gain_in:
        c.wait()
    gin[...] = jnp.broadcast_to(gf_v[...].astype(F32)[None, :], gin.shape)
    gin[1:2, :] = ga_v[...].astype(F32)[None, :]
    g_own = net.here(gin, gains.at[:, pl.ds(0, dt)])
    h_own = net.here(hid.at[ds(tx * sub, sub), :], rows.at[:, pl.ds(0, dt)])
    for w in (q_w, kv_w, gate, up, down):
        w.start_local()
    for k in far_first:
        g_cp(k).start()
    for c in turn_in:
        c.wait()

    @pl.loop(0, tokens // 128)
    def _(i):
        part = 128
        cos_c, sin_c = ds(i * part, part), ds(tokens + i * part, part)
        q_r, kv_r = pl.ds(0, 128), pl.ds(128, 128)
        angles = inv_v[...] * pos_v[:, cos_c].astype(F32)
        dres_v[q_r, sin_c] = jnp.sin(angles)
        dres_v[q_r, cos_c] = jnp.cos(angles)

        @pl.when(z < 2)
        def _():
            dres_v[kv_r, cos_c] = dres_v[q_r, cos_c]
            dres_v[kv_r, sin_c] = dres_v[q_r, sin_c]

        @pl.when(z >= 2)
        def _():
            dres_v[kv_r, cos_c] = jnp.ones((128, part), F32)
            dres_v[kv_r, sin_c] = jnp.zeros((128, part), F32)

    tab_out = net.here(dres_v.at[pl.ds(0, 256), pl.ds(0, 2 * tokens)], tab_o)
    turn(p_v, width, q_width, tokens, dres_v, swap_v, True)
    for k in far_first:
        e_cp(k, tx).start()
    e_own = net.here(p_v.at[pl.ds(0, width), ds(tx * sub, sub)], eq_v.at[:, ds(tx * sub, sub)])
    for w in (q_w, kv_w, gate, up, down):
        w.start_y()
    for k in far_first:
        d_cp(k).start()
    d_own = net.here(dh2h.at[ds(tx * sub, sub), :], dh2_v.at[:, pl.ds(0, dt)])

    for k in far_first:
        g_cp(k).wait_recv()
        h_cp(k).wait_recv()
    g_own.wait()
    h_own.wait()

    @pl.loop(0, sub // 16)
    def _(r):
        x = rows[ds(r * 16, 16), :].astype(F32)
        inv = lax.rsqrt(jnp.sum(x * x, axis=1, keepdims=True) / dim + NORM_EPS)
        n_v[ds(z * sub + r * 16, 16), :] = (x * inv * gains[0:1, :]).astype(BF16)

    ag.start()
    outs = [net.here(rows, h_o), net.here(gains, g_o)]
    for k in far_first:
        e_cp(k, peer[k]).wait_recv()
    e_own.wait()
    ag.step1()
    for w in (q_w, kv_w):
        w.y_event(0)
    for w in (q_w, kv_w):
        w.x_event(0)
    for w in (q_w, kv_w):
        w.finish_local()
        w.finish(0)
    for k in far_first:
        e_cp(k, tx).wait_send()

    def n2_block(b):
        @pl.loop(0, dim // dtile)
        def _(j):
            cols = ds(j * dtile, dtile)
            p_v[ds(b * sub, sub), cols] = dot(eq_v[:, ds(b * sub, sub)], wq_v[:, cols], ROWS_ROWS).astype(BF16)

    @pl.loop(0, 4)
    def _(i):
        n2_block(pick(3 - i, z))
        for step in range(3):
            pl.when(i == step)(lambda step=step: rsc.send_end(2 - step))
        pl.when(i == 0)(lambda: gate.y_event(0))

    wide = ff // 2

    def gate_part(b, c):
        cols = pl.ds(c * wide, wide)
        a_v[ds(b * sub, sub), cols] = dot(n_v[ds(b * sub, sub), :], wg_v[:, cols]).astype(BF16)

    def up_part(b, c):
        cols = pl.ds(c * wide, wide)
        bb = dot(n_v[ds(b * sub, sub), :], wu_v[:, cols]).astype(BF16)
        b_v[ds(b * sub, sub), cols] = bb
        aa = a_v[ds(b * sub, sub), cols].astype(F32)
        wg_v[ds(b * sub, sub), cols] = (aa * jax.nn.sigmoid(aa) * bb.astype(F32)).astype(BF16)

    def down_part(b, j):
        cols = pl.ds(j * (dim // 2), dim // 2)
        n_v[ds(b * sub, sub), cols] = dot(wg_v[ds(b * sub, sub), :], wd_v[:, cols]).astype(BF16)

    outs += [net.here(wq_v, wq_o), net.here(eq_v, eq_o)]
    gate.finish_local()
    gate.y_event(1)
    ag.step2()
    ag.step3_mid()
    gate.x_event(0)
    gate.finish(0)

    @pl.loop(0, 3)
    def _(i):
        gate_part(pick(i, z), 0)

    up.y_event(0)
    gate.x_event(1)
    rsc.send_mid(2)
    gate.finish(1)
    wg_out = net.here(wg_v, wg_o)

    @pl.loop(0, 3)
    def _(i):
        gate_part(pick(i, z), 1)

    up.finish_local()
    up.y_event(1)
    up.x_event(0)
    up.finish(0)
    ag.step3_end()

    @pl.loop(0, 2)
    def _(c):
        cols = ds(c * wide, wide)
        b = pick(3, z)
        a_v[ds(b * sub, sub), cols] = dot(n_v[ds(b * sub, sub), :], wg_v[:, cols]).astype(BF16)

    wg_out.wait()
    n_out = net.here(n_v, n_o)

    @pl.loop(0, 4)
    def _(i):
        pl.when(i == 1)(lambda: down.y_event(0))
        pl.when(i == 2)(lambda: down.y_event(1))
        pl.when(i == 3)(lambda: up.x_event(1))
        up_part(pick(i, z), 0)

    def up_events_1():
        rsc.send_mid(1)
        rsc.send_mid(0)
        down.x_event(0)

    def up_events_2():
        down.y_event(2)

    def up_events_3():
        down.y_event(3)
        down.x_event(1)

    up.finish(1)
    outs.append(net.here(wu_v, wu_o))

    @pl.loop(0, 4)
    def _(i):
        pl.when(i == 1)(up_events_1)
        pl.when(i == 2)(up_events_2)
        pl.when(i == 3)(up_events_3)
        b = pick(i, z)
        up_part(b, 1)
        ux_cp(2, b).start()
        ux_cp(1, b).start()

    outs.append(net.here(u_v, u_o))
    ag.drain()
    gate.drain()
    n_out.wait()
    down.finish_local()

    @pl.loop(0, 4)
    def _(i):
        pl.when(i == 2)(lambda: down.x_event(2))
        pl.when(i == 3)(lambda: down.x_event(3))
        down_part(pick(3 - i, z), 0)

    for ch in range(4):
        down.finish(ch)

    @pl.loop(0, 4)
    def _(i):
        down_part(pick(3 - i, z), 1)
        for step in range(3):
            pl.when(i == step)(lambda step=step: rs2[0].send_end(2 - step))

    for c in range(1, 8):
        for i in (2, 1, 0):
            rs2[c].send_end(i)
    dg_v[...] = jnp.zeros_like(dg_v)
    step = 16

    def norm_chunk(c):
        @pl.loop(0, cs // step)
        def _(r):
            at = c * cs + r * step
            view, mine, far = ds(at, step), ds(z * sub + at, step), ds(4 * sub + at, step)

            def whole(part, got):
                right = jnp.where(z < 3, got[mine, :].astype(F32), 0.0)
                left = jnp.where(z > 0, got[far, :].astype(F32), 0.0)
                return part[mine, :].astype(F32) + right + left

            resid = (rows[view, :].astype(F32) + whole(n_v, rbuf2)).astype(BF16)
            dy = whole(p_v, rbuf)
            res_v[view, :] = resid
            x = resid.astype(F32)
            inv = lax.rsqrt(jnp.sum(x * x, axis=1, keepdims=True) / dim + NORM_EPS)
            xhat = x * inv
            gain = gains[1:2, :]
            n2_v[view, :] = (xhat * gain).astype(BF16)
            part = dy * xhat
            dg_v[...] += part[:8] + part[8:]
            inner = jnp.sum(part * gain, axis=1, keepdims=True) / dim
            dres = dh2_v[view, :].astype(F32) + inv * (dy * gain) - xhat * (inv * inner)
            dres_v[view, pl.ds(0, dim)] = dres
            wg_v[ds(tokens + z * sub + at, step), :] = dres.astype(BF16)

    def spread(b, half):
        for k in far_first:
            ex_cp(k, b, half).start()

    def back_tile(b, j):
        view, cols = ds(b * sub, sub), ds(j * (ff // 4), ff // 4)
        du = dot(wg_v[ds(tokens + b * sub, sub), :], wd_v[ds(j * (ff // 4), ff // 4), :], NT_DIMS)
        aa = a_v[view, cols].astype(F32)
        bb = b_v[view, cols].astype(F32)
        sig = jax.nn.sigmoid(aa)
        a_v[view, cols] = (du * bb * sig * (1.0 + aa * (1.0 - sig))).astype(BF16)
        b_v[view, cols] = (du * aa * sig).astype(BF16)

    def scatter(i, c):
        return lambda: rs2[c].send_mid(i)

    def gathered(i, c):
        def go():
            ag2[c].take(i)
            pl.when(mid(z))(lambda: ag2[c].forward(i))
            if c % 4 == 3:
                spread(ag.slots[i], c // 4)
        return go

    def run(ops):
        def go():
            for op in ops:
                op()
        return go

    before_mid = (
        (scatter(2, 0), scatter(1, 0), scatter(0, 0)),
        (scatter(2, 1), scatter(1, 1), gathered(1, 0), scatter(0, 1), scatter(2, 2)),
        (scatter(1, 2), scatter(0, 2), gathered(1, 1), scatter(2, 3)),
        (scatter(1, 3), scatter(0, 3), gathered(1, 2), scatter(2, 4)),
        (scatter(1, 4), scatter(0, 4), gathered(1, 3), scatter(2, 5)),
        (scatter(1, 5), scatter(0, 5), gathered(1, 4), scatter(2, 6)),
        (scatter(1, 6), scatter(0, 6), gathered(1, 5), scatter(2, 7)),
        (scatter(1, 7), scatter(0, 7), gathered(1, 6), gathered(0, 0)))
    before_end = (
        (),
        (gathered(0, 0), gathered(1, 0)),
        (gathered(0, 1),),
        (gathered(1, 1), gathered(0, 2)),
        (gathered(1, 2), gathered(0, 3)),
        (gathered(1, 3), gathered(0, 4)),
        (gathered(1, 4), gathered(0, 5)),
        (gathered(1, 5), gathered(0, 6)))
    after_mid = {1: (gathered(0, 1),),
                 2: (gathered(2, 0),),
                 3: (gathered(0, 2),),
                 4: (gathered(1, 7),),
                 5: (gathered(0, 3),),
                 6: (gathered(2, 1),),
                 7: (gathered(0, 4),),
                 8: (gathered(2, 2), gathered(0, 5), gathered(2, 3), gathered(0, 6), gathered(2, 4), gathered(0, 7)),
                 10: (gathered(2, 5),),
                 12: (gathered(2, 6), gathered(2, 7))}
    after_end = {2: (gathered(1, 6),),
                 4: (gathered(0, 7),),
                 7: (gathered(2, 0),),
                 8: (gathered(1, 7),),
                 11: (gathered(2, 1),),
                 12: (gathered(2, 2), gathered(2, 3), gathered(2, 4), gathered(2, 5), gathered(2, 6), gathered(2, 7))}

    for c in range(8):
        pl.when(mid(z))(run(before_mid[c]))
        pl.when(end(z))(run(before_end[c]))
        if c == 0:
            rsc.finish()
            for k in far_first:
                d_cp(k).wait_recv()
            d_own.wait()
            tab_out.wait()
        rs2[c].finish()
        norm_chunk(c)
        ag2[c].start()
        if c % 4 == 3:
            spread(z, c // 4)
            for k in far_first:
                o_cp(k, tx, c // 4).start()

    outs += [net.here(res_v.at[:, pl.ds(0, dt)], home_o.at[ds(tx * sub, sub), :]), net.here(n2_v, n2_o), net.here(dres_v.at[pl.ds(0, sub), pl.ds(0, dim)], dres_o), net.here(dg_v, dg_o)]
    rsc.drain()
    for c in range(8):
        rs2[c].drain()
    middle = (z + 1) // 2 % 2

    def u_forward():
        for b in range(4):
            ux_cp(2, b).wait_recv()
            ux_cp(3, b).start()

    @pl.loop(0, 16)
    def _(t):
        for at, ops in after_mid.items():
            pl.when(jnp.logical_and(t == at, mid(z)))(run(ops))
        for at, ops in after_end.items():
            pl.when(jnp.logical_and(t == at, end(z)))(run(ops))
        pl.when(t == 8)(u_forward)
        i = t // 4
        inner = (i + 1) // 2 % 2
        back_tile(pick(i + middle * inner * (3 - 2 * i), z), t % 4)

    outs.append(net.here(e_v, e_o))
    outs += [net.here(a_v, da_o), net.here(b_v, db_o)]

    def down_tile(k, j):
        return dot(wg_v[pl.ds(0, tokens), pl.ds(split, ff - split)], wg_v[pl.ds(tokens, tokens), ds(k * dt + j * (dt // 2), dt // 2)], ROWS_ROWS)

    quarter = [rbuf.at[pl.ds(0, ff - split), pl.ds(i * dt, dt)] for i in range(4)]
    part_d = GradReduce(net, peer, down_tile, 2, quarter[0], quarter[1], quarter[2], quarter[3], d2_o, d0_o, None, dc_o, None)
    part_d.step3()
    part_d.step1()
    part_d.step2()
    outs.append(net.here(quarter[2], dc_o))
    for k in far_first:
        o_cp(k, peer[k], 0).wait_recv()
        o_cp(k, peer[k], 1).wait_recv()
        for b in range(4):
            ex_cp(k, b, 0).wait_recv()
            ex_cp(k, b, 1).wait_recv()
    for b in range(4):
        ux_cp(1, b).wait_recv()
        ux_cp(3, b).wait_recv()
    for c in outs:
        c.wait()
    for k in far_first:
        g_cp(k).wait_send()
        h_cp(k).wait_send()
        d_cp(k).wait_send()
        o_cp(k, tx, 0).wait_send()
        o_cp(k, tx, 1).wait_send()
        for b in range(4):
            ux_cp(k, b).wait_send()
            ex_cp(k, b, 0).wait_send()
            ex_cp(k, b, 1).wait_send()
    for w in (q_w, kv_w, up, down):
        w.drain()
    for c in range(8):
        ag2[c].drain()
    part_d.cp(1).wait_recv()
    part_d.sent_locally()


def call_ab(hid, eqh, ekvh, pos, inv, swap, dh2h, wg, wu, wd, wq, wkv, gf, ga):
    tokens, dt = hid.shape
    sub, dim, ff, q_width = tokens // 4, dt * 4, wg.shape[1], wq.shape[0]
    width = q_width + wkv.shape[0]
    s = jax.ShapeDtypeStruct
    tok_ff, tok_d, row = s((tokens, ff), BF16), s((tokens, dim), BF16), s((sub, dim), BF16)
    shapes = (tok_d, tok_ff, tok_ff, tok_ff, s((dim, ff), BF16), s((dim, ff), BF16), s((width, dim), BF16), s((width, tokens), BF16),
              row, s((8, dim), F32), tok_d, row, s((sub, dim), F32), s((tokens, dt), BF16), s((8, dim), F32),
              s((3, tokens, down_split(ff)), BF16), s((3, tokens, dt), BF16), s((256, 2 * tokens), F32)) + (s((ff - down_split(ff), dt), BF16),) * 3
    vrow, vtok, vff = VMEM((sub, dim), BF16), VMEM((tokens, dim), BF16), VMEM((tokens, ff), BF16)
    return pl.pallas_call(
        functools.partial(kernel_ab, q_width), out_shape=shapes, in_specs=[ANY] * 14, out_specs=[ANY] * len(shapes),
        scratch_shapes=[
            vrow, vrow, vrow, vrow, VMEM((max(sub, 256), max(dim, 2 * tokens)), F32), vtok, vff, vff, VMEM((dim, ff), BF16), VMEM((dim, ff), BF16), VMEM((ff, dim), BF16),
            VMEM((width, dim), BF16), VMEM((width, tokens), BF16), vtok, VMEM((5 * sub, dim), BF16), VMEM((5 * sub, dim), BF16),
            VMEM((8, dim), F32), VMEM((8, dim), F32), VMEM((128, 128), BF16), VMEM((1, tokens), jnp.int32), VMEM((128, 128), F32),
            VMEM((dt,), BF16), VMEM((dt,), BF16), VMEM((8, dt), F32),
            pltpu.SemaphoreType.DMA((236,)), pltpu.SemaphoreType.DMA((236,)), pltpu.SemaphoreType.DMA((48,))],
        compiler_params=pltpu.CompilerParams(collective_id=0, has_side_effects=True, vmem_limit_bytes=VMEM_LIMIT),
        cost_estimate=pl.CostEstimate(flops=20 * tokens * dim * ff, bytes_accessed=100000000, transcendentals=0), name="phase_ab",
    )(hid, eqh, ekvh, pos, inv, swap, dh2h, wg, wu, wd, wq, wkv, gf, ga)


def kernel_c(q_width, da_h, db_h, wg_h, wu_h, n_h, u_h, ux_h, e_h, ex_h, n2_h, eq_h, wq_h, h_h, dres_h, g_h, dga_h, tabh, swaph, d0, dc,
             wgo, wgy, wuo, wuy, wdo, wqo, wqy, wvo, wvy, q_o, kv_o, dh_o, dg_o, g2, g0, u2, u0, q2, q0, v2, v0, qx, dy,
             wg_v, wu_v, da_v, db_v, n_v, p_v, rbuf, n2_v, st3, st1, cross_g, cross_u, stage, tiles_v, dres_v, wq_v, eq_v,
             gains, dg_v, dgr, dgz, tab_v, swap_v, send, recv, local):
    dp, z, tx, peer = places()
    tokens, ff = da_v.shape
    sub, dim = dres_v.shape
    dt = dim // 4
    width = eq_v.shape[0]
    tile = ff // 4
    dtile = min(512, dim)
    qt = min(256, tile)
    far_first = (2, 3, 1)
    net = Wires(send, recv, local)
    n2_in = net.here(n2_h, n2_v.at[ds(z * sub, sub), :])
    first = [net.here(n_h, n_v), net.here(da_h, da_v)]
    second = [net.here(db_h, db_v), net.here(wg_h, wg_v), net.here(wu_h, wu_v)]
    third = [net.here(wq_h, wq_v), net.here(eq_h, eq_v), net.here(dres_h, dres_v), net.here(g_h, gains),
             net.here(dga_h, dg_v.at[pl.ds(8, 8), :]), net.here(tabh, tab_v), net.here(swaph, swap_v)]
    sem = pltpu.get_barrier_semaphore()
    zs = tuple((z + i) % 4 for i in range(4))
    for i in (1, 2, 3):
        pl.semaphore_signal(sem, inc=1, device_id={"tx": peer[i]}, device_id_type=MESH)
        pl.semaphore_signal(sem, inc=1, device_id={"ty": zs[i]}, device_id_type=MESH)
    pl.semaphore_wait(sem, 6)
    rsc = LineScatter(net, p_v, rbuf, sub, z)
    ag = LineGather(net, n2_v, sub, z)
    q_id, h_id, t_id, z_id = net.take(4), net.take(4), net.take(4), net.take(4)

    def grad_tile(lhs, rhs, w):
        def go(k, j):
            cols = pl.ds(j * w, w) if isinstance(j, int) else ds(j * w, w)
            return dot(lhs[:, pl.ds(k * dt, dt)], rhs[:, cols], ROWS_ROWS)
        return go

    gate = GradReduce(net, peer, grad_tile(n_v, da_v, tile), ff // tile, st3, st1, cross_g, stage, g2, g0, wgy, wgo, tiles_v)
    up = GradReduce(net, peer, grad_tile(n_v, db_v, tile), ff // tile, st3, st1, cross_u, stage, u2, u0, wuy, wuo, tiles_v)
    d_id = net.take(1)

    def dy_cp():
        return net.copy(dc, dy, d_id, d_id, tx=peer[2])

    dy_cp().start()

    def head_grad(first, rows, got2, got0, got_y, out):
        corner = [da_v.at[pl.ds(first, rows), pl.ds(c * dt, dt)] for c in range(4)]

        def tile_of(k, j):
            return dot(eq_v[pl.ds(first, rows), :], n2_v[:, ds(k * dt + j * qt, qt)])

        return GradReduce(net, peer, tile_of, dt // qt, *corner, got2, got0, got_y, out, tiles_v)

    heads = (head_grad(0, q_width, q2, q0, wqy, wqo), head_grad(q_width, width - q_width, v2, v0, wvy, wvo))

    def dn_block(b):
        rows = ds(b * sub, sub)

        @pl.loop(0, dim // dtile)
        def _(j):
            wr = ds(j * dtile, dtile)
            p_v[rows, wr] = (dot(da_v[rows, :], wg_v[wr, :], NT_DIMS) + dot(db_v[rows, :], wu_v[wr, :], NT_DIMS)).astype(BF16)

    n2_in.wait()
    ag.start()
    for c in first:
        c.wait()
    gate.step3()
    gate.step1()
    gate.step2()
    gate.send()
    for c in second:
        c.wait()

    @pl.loop(0, 4)
    def _(i):
        @pl.when(i == 1)
        def _():
            gate.sent_locally()
            up.step3()
            up.step1()
            ag.step1()

        dn_block(pick(3 - i, z))
        for step in range(3):
            pl.when(i == step)(lambda step=step: rsc.send_end(2 - step))

    up.step2()
    up.send()
    rsc.send_mid(2)
    ag.step2()
    ag.step3_mid()
    up.sent_locally()
    h_in = net.here(h_h, st3.at[pl.ds(0, sub), :])
    gate.step0(st1)
    gate.sent()

    e_in = [net.here(e_h.at[:, pl.ds(0, dt)], wu_v.at[pl.ds(0, tokens), pl.ds(0, dt)])]
    for k in (1, 2, 3):
        e_in.append(net.here(ex_h.at[k - 1], wu_v.at[pl.ds(0, tokens), pl.ds(k * dt, dt)]))

    piece = ff // 8
    exchanged, n_pieces = down_split(ff) // piece, 8

    def u_place(j, k):
        return wg_v.at[pl.ds((j % 2) * tokens, tokens), pl.ds(k * piece, piece)]

    def sums(j, n):
        return stage.at[pl.ds((j % 2) * piece, piece), pl.ds(n * dt, dt)]

    def u_load(j):
        cols = pl.ds(j * piece, piece)
        if j < exchanged:
            return [net.here(u_h.at[:, cols] if k == 0 else ux_h.at[k - 1, :, cols], u_place(j, k)) for k in range(4)]
        rows = pl.ds((j - exchanged) * piece, piece)
        return [net.here(u_h.at[:, cols], u_place(j, 0)), net.here(d0.at[rows, :], sums(j, 0)), net.here(dy.at[rows, :], sums(j, 1))]

    loads, stores = {}, {}

    def down_run(js):
        for j in js:
            for c in loads.pop(j):
                c.wait()
            if j >= 2:
                stores.pop(j - 2).wait()
            acc = None if j < exchanged else sums(j, 0)[...].astype(F32) + sums(j, 1)[...].astype(F32)
            for k in range(4 if j < exchanged else 1):
                part = dot(u_place(j, k)[...], wu_v[pl.ds(0, tokens), pl.ds(k * dt, dt)], ROWS_ROWS)
                acc = part if acc is None else acc + part
            place = tiles_v.at[j % 2, pl.ds(0, piece), pl.ds(0, dt)]
            tiles_v[j % 2, pl.ds(0, piece), pl.ds(0, dt)] = acc
            stores[j] = net.here(place, wdo.at[pl.ds(j * piece, piece), :])
            if j + 2 < n_pieces:
                loads[j + 2] = u_load(j + 2)

    loads[0], loads[1] = u_load(0), u_load(1)
    rsc.send_mid(1)
    rsc.send_mid(0)
    for c in e_in:
        c.wait()
    down_run((0, 1))
    for c in third:
        c.wait()
    ag.step3_end()

    @pl.loop(0, width // qt)
    def _(j):
        wu_v[ds(tokens + j * qt, qt), pl.ds(0, tokens)] = dot(wq_v[ds(j * qt, qt), :], n2_v[...], NT_DIMS).astype(BF16)

    def q_cp(k, block):
        return net.copy(wu_v.at[pl.ds(tokens, width), ds(peer[k] * sub, sub)], qx.at[:, ds(block * sub, sub)], q_id + k, q_id + k, tx=peer[k])

    for k in far_first:
        q_cp(k, tx).start()
    q_own = net.here(wu_v.at[pl.ds(tokens, width), ds(tx * sub, sub)], qx.at[:, ds(tx * sub, sub)])
    for part in heads:
        part.step3()
        part.step1()
    dy_cp().wait_recv()
    for part in heads:
        part.step2()
        part.send()
    down_run(range(2, n_pieces))
    h_in.wait()
    rsc.finish()
    dg_v[pl.ds(0, 8), :] = jnp.zeros((8, dim), F32)
    step = 16

    @pl.loop(0, sub // step)
    def _(r):
        view, mine, far = ds(r * step, step), ds(z * sub + r * step, step), ds(4 * sub + r * step, step)
        right = jnp.where(z < 3, rbuf[mine, :].astype(F32), 0.0)
        left = jnp.where(z > 0, rbuf[far, :].astype(F32), 0.0)
        dy = p_v[mine, :].astype(F32) + right + left
        x = st3[view, :].astype(F32)
        inv = lax.rsqrt(jnp.sum(x * x, axis=1, keepdims=True) / dim + NORM_EPS)
        xhat = x * inv
        gain = gains[0:1, :]
        part = dy * xhat
        dg_v[pl.ds(0, 8), :] += part[:8] + part[8:]
        inner = jnp.sum(part * gain, axis=1, keepdims=True) / dim
        st1[view, :] = (dres_v[view, :] + inv * (dy * gain) - xhat * (inv * inner)).astype(BF16)

    def h_cp(k, block):
        return net.copy(st1.at[pl.ds(0, sub), pl.ds(k * dt, dt)], dh_o.at[ds(block * sub, sub), :], h_id + k, h_id + k, tx=peer[k])

    def t_cp(k):
        return net.copy(dg_v.at[:, pl.ds(k * dt, dt)], dgr.at[k], t_id + k, t_id + k, tx=peer[k])

    def z_cp(i):
        return net.copy(dgr.at[0], dgz.at[i], z_id + i, z_id + i, ty=zs[i])

    for k in far_first:
        t_cp(k).start()
    for k in far_first:
        h_cp(k, tx).start()
    h_own = net.here(st1.at[pl.ds(0, sub), pl.ds(0, dt)], dh_o.at[ds(tx * sub, sub), :])
    up.sent()
    for c in stores.values():
        c.wait()
    up.step0(cross_g)
    for k in far_first:
        q_cp(k, peer[k]).wait_recv()
    q_own.wait()
    turned = wu_v.at[pl.ds(tokens, width), pl.ds(tokens, tokens)]
    net.here(qx, turned).wait()
    turn(turned, width, q_width, tokens, tab_v, swap_v, False)
    q_out = net.here(wu_v.at[pl.ds(tokens, q_width), pl.ds(tokens, tokens)], q_o)
    kv_out = net.here(wu_v.at[pl.ds(tokens + q_width, width - q_width), pl.ds(tokens, tokens)], kv_o)
    heads[0].step0(cross_g.at[pl.ds(0, q_width), pl.ds(0, dt)])
    heads[1].step0(cross_g.at[pl.ds(0, width - q_width), pl.ds(dt, dt)])
    for k in far_first:
        t_cp(k).wait_recv()
    dgr[0] = dg_v[:, pl.ds(0, dt)] + dgr[1] + dgr[2] + dgr[3]
    for i in (1, 2, 3):
        z_cp(i).start()
    for i in (1, 2, 3):
        z_cp(i).wait_recv()
    dgz[0] = dgr[0] + dgz[1] + dgz[2] + dgz[3]
    dg_out = net.here(dgz.at[0], dg_o)
    for k in far_first:
        h_cp(k, peer[k]).wait_recv()
    for c in (q_out, kv_out, dg_out, h_own):
        c.wait()
    dy_cp().wait_send()
    for part in heads:
        part.sent_locally()
        part.sent()
    for k in far_first:
        q_cp(k, tx).wait_send()
        h_cp(k, tx).wait_send()
        t_cp(k).wait_send()
        z_cp(k).wait_send()
    ag.drain()
    rsc.drain()


def call_c(q_width, *args):
    tokens, ff = args[0].shape
    sub, dim = args[9].shape
    dt, width = dim // 4, args[10].shape[0]
    rest = width - q_width
    tile = ff // 4
    s = jax.ShapeDtypeStruct
    wf, wb = s((dt, ff), F32), s((dt, ff), BF16)
    qf, qb, vf, vb = s((q_width, dt), F32), s((q_width, dt), BF16), s((rest, dt), F32), s((rest, dt), BF16)
    shapes = (wf, wb, wf, wb, s((ff, dt), F32), qf, qb, vf, vb, s((q_width, tokens), BF16), s((rest, tokens), BF16), s((tokens, dt), BF16), s((16, dt), F32),
              wb, wb, wb, wb, qb, qb, vb, vb, s((width, tokens), BF16), s((ff - down_split(ff), dt), BF16))
    return pl.pallas_call(
        functools.partial(kernel_c, q_width), out_shape=shapes, in_specs=[ANY] * len(args), out_specs=[ANY] * len(shapes),
        scratch_shapes=[
            VMEM((dim, ff), BF16), VMEM((dim, ff), BF16), VMEM((tokens, ff), BF16), VMEM((tokens, ff), BF16), VMEM((tokens, dim), BF16),
            VMEM((tokens, dim), BF16), VMEM((5 * sub, dim), BF16), VMEM((tokens, dim), BF16),
            VMEM((dt, ff), BF16), VMEM((dt, ff), BF16), VMEM((dt, ff), BF16), VMEM((dt, ff), BF16), VMEM((dt, ff), BF16),
            VMEM((2, max(dt, tile), max(dt, tile)), F32), VMEM((sub, dim), F32), VMEM((width, dim), BF16), VMEM((width, tokens), BF16),
            VMEM((8, dim), F32), VMEM((16, dim), F32), VMEM((4, 16, dt), F32), VMEM((4, 16, dt), F32), VMEM((256, 2 * tokens), F32), VMEM((128, 128), BF16),
            pltpu.SemaphoreType.DMA((48,)), pltpu.SemaphoreType.DMA((48,)), pltpu.SemaphoreType.DMA((96,))],
        compiler_params=pltpu.CompilerParams(collective_id=2, has_side_effects=True, vmem_limit_bytes=VMEM_LIMIT),
        cost_estimate=pl.CostEstimate(flops=20 * tokens * dim * ff, bytes_accessed=100000000, transcendentals=0), name="phase_c",
    )(*args)


def kernel_out(pieces, n, *refs):
    ins, outs, bufs = refs[:n], refs[n + 1:2 * n + 1], refs[2 * n + 3:3 * n + 3]
    gains, gain_a, gain_b = refs[n], refs[2 * n + 1], refs[2 * n + 2]
    read, write = refs[3 * n + 3:]

    def part(ref, i, c):
        rows = ref.shape[0] // pieces[i]
        return ref.at[pl.ds(c * rows, rows), :]

    jobs = [(i, c) for i in range(n) for c in range(pieces[i])]
    get = [pltpu.make_async_copy(part(ins[i], i, c), part(bufs[i], i, c), read.at[m]) for m, (i, c) in enumerate(jobs)]
    put = [pltpu.make_async_copy(part(bufs[i], i, c), part(outs[i], i, c), write.at[m]) for m, (i, c) in enumerate(jobs)]
    ahead = min(6, len(get))
    for g in get[:ahead]:
        g.start()
    gain_a[...] = jnp.sum(gains[pl.ds(0, 8), :], axis=0, keepdims=True)
    gain_b[...] = jnp.sum(gains[pl.ds(8, 8), :], axis=0, keepdims=True)
    for m, (g, p) in enumerate(zip(get, put)):
        g.wait()
        p.start()
        if m + ahead < len(get):
            get[m + ahead].start()
    for p in put:
        p.wait()


def call_out(results, gains):
    n = len(results)
    pieces = tuple(max(1, x.size * x.dtype.itemsize // 2**21) for x in results)
    row = jax.ShapeDtypeStruct((1, gains.shape[1]), F32)
    whole = pl.BlockSpec(memory_space=pltpu.VMEM)
    return pl.pallas_call(
        functools.partial(kernel_out, pieces, n), out_shape=tuple(jax.ShapeDtypeStruct(x.shape, x.dtype) for x in results) + (row, row),
        in_specs=[ANY] * n + [whole], out_specs=[ANY] * n + [whole, whole],
        scratch_shapes=[VMEM(x.shape, x.dtype) for x in results] + [pltpu.SemaphoreType.DMA((sum(pieces),))] * 2,
        compiler_params=pltpu.CompilerParams(vmem_limit_bytes=VMEM_LIMIT),
        cost_estimate=pl.CostEstimate(flops=1000000, bytes_accessed=35000000, transcendentals=0), name="results",
    )(*results, gains)


def solution(mesh):
    def local_step(hidden, positions, g_ffn, w_gate, w_up, w_down, g_attn, w_q, w_kv, grad_h2, grad_q, grad_kv):
        tokens, dt = hidden.shape
        q_heads, head_dim = w_q.shape[1:]
        q_width = q_heads * head_dim

        lane = np.arange(128)
        inv_freq = ROPE_BASE ** (-(lane % head_dim // 2 * 2).astype(np.float32) / head_dim)
        inv_freq = jnp.asarray(np.tile(inv_freq.astype(np.float32)[:, None], (1, 128)))
        swap = np.zeros((128, 128), np.float32)
        swap[lane, lane ^ 1] = np.where(lane % 2 == 0, -1.0, 1.0)
        swap = jnp.asarray(swap, BF16)

        def heads_first(x):
            return x.transpose(1, 2, 0).reshape(-1, x.shape[0])

        def heads_last(x):
            return x.reshape(-1, head_dim, x.shape[1]).transpose(2, 0, 1)

        (normed_all, grad_gate, grad_up, u_all, gate_w, up_w, w_qkv, back_all, h_rows, gains, res_all, normed2, grad_res, resid_out, gattn8,
         u_other, e_other, table, _, wd_zero, wd_cross) = call_ab(
             hidden, heads_first(grad_q), heads_first(grad_kv), positions.reshape(1, tokens), inv_freq, swap, grad_h2,
             w_gate, w_up, w_down, heads_first(w_q), heads_first(w_kv), g_ffn, g_attn)
        (grad_wgate, _, grad_wup, _, grad_wdown, grad_wq, _, grad_wkv, _, q_out, kv_out, grad_hidden, gain_grads, *_) = call_c(
            q_width, grad_gate, grad_up, gate_w, up_w, normed_all, u_all, u_other, res_all, e_other, normed2, back_all, w_qkv,
            h_rows, grad_res, gains, gattn8, table, swap, wd_zero, wd_cross)
        (resid_out, grad_wgate, grad_wup, grad_wdown, grad_wq, grad_wkv, q_out, kv_out, grad_hidden, grad_gffn, grad_gattn) = call_out(
            (resid_out, grad_wgate, grad_wup, grad_wdown, grad_wq, grad_wkv, q_out, kv_out, grad_hidden), gain_grads)
        q_out, kv_out, grad_wq, grad_wkv = (heads_last(x) for x in (q_out, kv_out, grad_wq, grad_wkv))
        grad_gffn, grad_gattn = grad_gffn[0], grad_gattn[0]
        return (resid_out, q_out, kv_out, grad_hidden, grad_gffn, grad_gattn, grad_wgate, grad_wup, grad_wdown, grad_wq, grad_wkv)

    row_spec = P(("dp", "ty"), "tx")
    head_spec = P(("dp", "tx"), "ty", None)
    in_specs = (row_spec, P(("dp", "tx")), P("tx"), P("tx", "ty"), P("tx", "ty"), P("ty", "tx"), P("tx"), P("tx", "ty", None), P("tx", "ty", None), row_spec, head_spec, head_spec)
    out_specs = (row_spec, head_spec, head_spec, row_spec, P(("dp", "tx")), P(("dp", "tx")), P(("dp", "tx"), "ty"), P(("dp", "tx"), "ty"), P(("dp", "ty"), "tx"), head_spec, head_spec)
    return jax.shard_map(local_step, mesh=mesh, in_specs=in_specs, out_specs=out_specs, check_vma=False)
```
